32 devices in a mesh: dp: 8 (over z, core), tensor: 4 (over y, x).
Axes of the slice: x: 2, y: 2, z: 4, core: 2. Of those that a mesh axis runs over, the one named last changes fastest.
Arguments:
- block_input: bfloat16 [8192, 2048], P(('dp', 'tensor')), may hold values from -6 to 6
- attention_gain: float32 [2048], replicated, may hold values from 0.1 to 1.9
- query_weight: bfloat16 [2048, 2048], P('dp', 'tensor'), may hold values from -0.125 to 0.125
- key_matrix: bfloat16 [2048, 1024], P('dp', 'tensor'), may hold values from -0.125 to 0.125
- value_matrix: bfloat16 [2048, 1024], P('dp', 'tensor'), may hold values from -0.125 to 0.125
- query_gain: float32 [128], replicated, may hold values from 0.4 to 2
- key_gain: float32 [128], replicated, may hold values from 0.4 to 2
- output_weight: bfloat16 [2048, 2048], P('tensor', 'dp'), may hold values from -1 to 1
- feed_gain: float32 [2048], replicated, may hold values from 0.1 to 1.9
- gate_weight: bfloat16 [2048, 6144], P('dp', 'tensor'), may hold values from -0.125 to 0.125
- up_weight: bfloat16 [2048, 6144], P('dp', 'tensor'), may hold values from -0.125 to 0.125
- down_weight: bfloat16 [6144, 2048], P('tensor', 'dp'), may hold values from -0.078125 to 0.078125
- out_cotangent: bfloat16 [8192, 2048], P(('dp', 'tensor')), may hold values from -6 to 6
Outputs:
- block_output: bfloat16 [8192, 2048], P(('dp', 'tensor'))
- input_gradient: bfloat16 [8192, 2048], P(('dp', 'tensor'))
- attention_gain_gradient: float32 [2048], replicated
- query_gradient: float32 [2048, 2048], P('dp', 'tensor')
- key_gradient: float32 [2048, 1024], P('dp', 'tensor')
- value_gradient: float32 [2048, 1024], P('dp', 'tensor')
- query_gain_gradient: float32 [128], replicated
- key_gain_gradient: float32 [128], replicated
- output_gradient: float32 [2048, 2048], P('tensor', 'dp')
- feed_gain_gradient: float32 [2048], replicated
- gate_gradient: float32 [2048, 6144], P('dp', 'tensor')
- up_gradient: float32 [2048, 6144], P('dp', 'tensor')
- down_gradient: float32 [6144, 2048], P('tensor', 'dp')
The draws below stay inside these ranges and needn't reach their ends.
All inputs are finite; a program needn't handle non-finite values.
Results may differ from the reference program's by a relative error of at most 0.019.
Values may be sent and summed in bfloat16 or wider, within the bound.
A program may use at most 256 MiB of HBM per device.

```python
import math
import jax
import jax.numpy as jnp
from jax import lax

MODEL_WIDTH = 2048
QUERY_HEAD_COUNT = 16
KEY_VALUE_HEADS = 8
HEAD_WIDTH = 128
HIDDEN_UNITS = 6144
SEQUENCE_LENGTH = 1024
SEQUENCE_COUNT = 1
TOKENS = 8192
N_DP = 8


def spiked(entries, key, source, target, shards_of, factor):
    def block_of(axis_at):
        return (jnp.arange(entries.shape[axis_at]) // (entries.shape[axis_at] // shards_of)).reshape((-1,) + (1,) * (entries.ndim - 1 - axis_at))

    near = jax.random.permutation(key, shards_of)[block_of(target)]
    other_side = (block_of(target) + shards_of // 2) % shards_of
    return jnp.where((block_of(source) == near) | (block_of(source) == other_side), factor * entries, entries)


def shard_levels(stream_key, dims, shards, least, top_value):
    def one(dim, parts):
        steps = jax.random.uniform(jax.random.fold_in(jax.random.fold_in(stream_key, 6), dim), (parts,), jnp.float32, least / len(shards), top_value / len(shards))
        return jnp.repeat(jnp.exp(steps), dims[dim] // parts).reshape((-1,) + (1,) * (len(dims) - dim - 1))

    loudness = one(*shards[0])
    for cut in shards[1:]:
        loudness = loudness * one(*cut)
    return loudness


def scatter_about(own_key, dims, deviation, most, cuts=(), dtype=jnp.bfloat16):
    values = jax.random.normal(own_key, dims, jnp.float32) * deviation
    if len(cuts) > 0:
        values = shard_levels(own_key, dims, cuts, -0.22, 0.18) * values
    return jnp.clip(values, min=-most, max=most).astype(dtype)


def heavy_noise(own_key, dims, width, reach, pieces, heavy, kind=jnp.bfloat16):
    drawn = width * jax.random.normal(own_key, dims, jnp.float32)
    if pieces:
        drawn = drawn * shard_levels(own_key, dims, pieces, -0.22, 0.18)
    return jnp.clip(spiked(drawn, jax.random.fold_in(own_key, 3), *heavy), -reach, reach).astype(kind)


def setup_inputs(seed: int = 0) -> dict:
    seeds = jax.random.split(jax.random.key(seed), 14)
    return {
        "block_input": scatter_about(seeds[0], (TOKENS, MODEL_WIDTH), 1.0, 6.0, ((0, 32),)),
        "attention_gain": jnp.clip(1.0 + 0.18 * jax.random.normal(seeds[1], (MODEL_WIDTH,), jnp.float32), 0.1, 1.9),
        "query_weight": scatter_about(seeds[2], (MODEL_WIDTH, QUERY_HEAD_COUNT * HEAD_WIDTH), MODEL_WIDTH ** -0.5, 0.125, ((0, 8), (1, 4))),
        "key_matrix": scatter_about(seeds[3], (MODEL_WIDTH, KEY_VALUE_HEADS * HEAD_WIDTH), MODEL_WIDTH ** -0.5, 0.125, ((0, 8), (1, 4))),
        "value_matrix": scatter_about(seeds[4], (MODEL_WIDTH, KEY_VALUE_HEADS * HEAD_WIDTH), MODEL_WIDTH ** -0.5, 0.125, ((0, 8), (1, 4))),
        "query_gain": jnp.clip(jnp.exp(jax.random.uniform(seeds[5], (HEAD_WIDTH,), jnp.float32, math.log(0.4), math.log(2.0))), 0.4, 2.0),
        "key_gain": jnp.clip(jnp.exp(jax.random.uniform(seeds[6], (HEAD_WIDTH,), jnp.float32, math.log(0.4), math.log(2.0))), 0.4, 2.0),
        "output_weight": scatter_about(seeds[7], (QUERY_HEAD_COUNT * HEAD_WIDTH, MODEL_WIDTH), (QUERY_HEAD_COUNT * HEAD_WIDTH // 64) ** -0.5, 1.0, ((0, 4), (1, 8))),
        "feed_gain": jnp.clip(1.0 + 0.18 * jax.random.normal(seeds[8], (MODEL_WIDTH,), jnp.float32), 0.1, 1.9),
        "gate_weight": scatter_about(seeds[9], (MODEL_WIDTH, HIDDEN_UNITS), MODEL_WIDTH ** -0.5, 0.125, ((0, 8), (1, 4))),
        "up_weight": scatter_about(seeds[10], (MODEL_WIDTH, HIDDEN_UNITS), MODEL_WIDTH ** -0.5, 0.125, ((0, 8), (1, 4))),
        "down_weight": scatter_about(seeds[11], (HIDDEN_UNITS, MODEL_WIDTH), HIDDEN_UNITS ** -0.5, 0.078125, ((0, 4), (1, 8))),
        "out_cotangent": heavy_noise(seeds[12], (TOKENS, MODEL_WIDTH), 1.0, 6.0, ((0, 32),), (0, 1, 32, 2.75)),
    }


epsilon = 1e-06
rope_base = 1000000.0

def row_scale(values):
    return lax.rsqrt(lax.optimization_barrier(jnp.mean(values * values, axis=-1, keepdims=True)) + epsilon)

def rotate_half(values):
    half_size = values.shape[-1] // 2
    return jnp.concatenate([-values[..., half_size:], values[..., :half_size]], axis=-1)

def rope_tables(positions, head_size):
    half_size = head_size // 2
    frequency = rope_base ** (-(jnp.arange(half_size).astype(jnp.float32) * 2.0 / head_size))
    angles = positions[:, None] * frequency[None, :]
    angles = jnp.concatenate([angles, angles], axis=1)
    return (jnp.cos(angles)[:, None, :], jnp.sin(angles)[:, None, :])

def widen(values):
    return lax.optimization_barrier(values).astype(jnp.float32)

def masked_scores(query_seq, key_seq):
    scale_factor = HEAD_WIDTH ** (-0.5)
    scores = jnp.einsum('qhgd,khd->hgqk', widen(query_seq), widen(key_seq), precision=lax.Precision.HIGHEST) * scale_factor
    positions = jnp.arange(SEQUENCE_LENGTH)
    visible = positions[:, None] >= positions[None, :]
    return jnp.where(visible, scores, -1e+30)

def attention_forward(operands):
    query_seq, key_seq, value_seq = operands
    scores = masked_scores(query_seq, key_seq)
    highest = lax.optimization_barrier(jnp.max(scores, axis=-1, keepdims=True))
    log_total = highest[..., 0] + jnp.log(lax.optimization_barrier(jnp.sum(jnp.exp(scores - highest), axis=-1)))
    weights = jnp.exp(scores - log_total[..., None]).astype(jnp.bfloat16)
    mixed_seq = jnp.einsum('hgqk,khd->qhgd', widen(weights), widen(value_seq), precision=lax.Precision.HIGHEST)
    return (mixed_seq.astype(jnp.bfloat16), log_total)

def attention_backward(operands):
    query_seq, key_seq, value_seq, mixed_seq, slope_seq, total_seq = operands
    scale_factor = HEAD_WIDTH ** (-0.5)
    scores = masked_scores(query_seq, key_seq)
    weights = jnp.exp(scores - total_seq[..., None])
    slope_float = widen(slope_seq)
    value_rows_gradient = jnp.einsum('hgqk,qhgd->khd', widen(weights.astype(jnp.bfloat16)), slope_float, precision=lax.Precision.HIGHEST)
    weight_slope = jnp.einsum('qhgd,khd->hgqk', slope_float, widen(value_seq), precision=lax.Precision.HIGHEST)
    centre = jnp.transpose(lax.optimization_barrier(jnp.sum(slope_float * widen(mixed_seq), axis=-1)), (1, 2, 0))
    score_slope = widen((weights * (weight_slope - centre[..., None])).astype(jnp.bfloat16))
    query_slope = jnp.einsum('hgqk,khd->qhgd', score_slope, widen(key_seq), precision=lax.Precision.HIGHEST) * scale_factor
    key_rows_gradient = jnp.einsum('hgqk,qhgd->khd', score_slope, widen(query_seq), precision=lax.Precision.HIGHEST) * scale_factor
    return (query_slope, key_rows_gradient, value_rows_gradient.astype(jnp.bfloat16))

def simple_product(first_operand, second_operand):
    return jnp.dot(first_operand, second_operand, preferred_element_type=jnp.float32)

def reference(block_input, attention_gain, query_weight, key_matrix, value_matrix, query_gain, key_gain, output_weight, feed_gain, gate_weight, up_weight, down_weight, out_cotangent):
    grouped_rows = SEQUENCE_COUNT * SEQUENCE_LENGTH
    grouping_width = QUERY_HEAD_COUNT // KEY_VALUE_HEADS
    cosine, sine = rope_tables((jnp.arange(grouped_rows) % SEQUENCE_LENGTH).astype(jnp.float32), HEAD_WIDTH)
    inputs = block_input.reshape(N_DP, grouped_rows, MODEL_WIDTH)
    slopes = out_cotangent.reshape(N_DP, grouped_rows, MODEL_WIDTH)

    def group_step(carry, operands):
        rows_in, rows_slope = operands
        input_float = rows_in.astype(jnp.float32)
        first_scale = row_scale(input_float)
        first_unit = input_float * first_scale
        attention_output_rows = (first_unit * attention_gain).astype(jnp.bfloat16)
        query_raw = simple_product(attention_output_rows, query_weight).reshape(grouped_rows, QUERY_HEAD_COUNT, HEAD_WIDTH)
        unnormed_key = simple_product(attention_output_rows, key_matrix).reshape(grouped_rows, KEY_VALUE_HEADS, HEAD_WIDTH)
        value_token_rows = simple_product(attention_output_rows, value_matrix).astype(jnp.bfloat16).reshape(grouped_rows, KEY_VALUE_HEADS, HEAD_WIDTH)
        query_scale = row_scale(query_raw)
        query_unit = query_raw * query_scale
        query_normed = query_unit * query_gain
        rotated_query = (query_normed * cosine + rotate_half(query_normed) * sine).astype(jnp.bfloat16)
        key_norm_scale = row_scale(unnormed_key)
        normalized_key = unnormed_key * key_norm_scale
        key_normed = normalized_key * key_gain
        rotated_key = (key_normed * cosine + rotate_half(key_normed) * sine).astype(jnp.bfloat16)
        query_sequences = rotated_query.reshape(SEQUENCE_COUNT, SEQUENCE_LENGTH, KEY_VALUE_HEADS, grouping_width, HEAD_WIDTH)
        key_sequences = rotated_key.reshape(SEQUENCE_COUNT, SEQUENCE_LENGTH, KEY_VALUE_HEADS, HEAD_WIDTH)
        value_sequences = value_token_rows.reshape(SEQUENCE_COUNT, SEQUENCE_LENGTH, KEY_VALUE_HEADS, HEAD_WIDTH)
        mixed_seqs, totals = lax.map(attention_forward, (query_sequences, key_sequences, value_sequences))
        mixed_rows = mixed_seqs.reshape(grouped_rows, QUERY_HEAD_COUNT * HEAD_WIDTH)
        hidden_state = input_float + simple_product(mixed_rows, output_weight)
        second_scale = row_scale(hidden_state)
        second_unit = hidden_state * second_scale
        feed_rows = (second_unit * feed_gain).astype(jnp.bfloat16)
        gate_values = simple_product(feed_rows, gate_weight)
        up_values = simple_product(feed_rows, up_weight)
        gate_sigmoid = jax.nn.sigmoid(gate_values)
        hidden_rows = (gate_values * gate_sigmoid * up_values).astype(jnp.bfloat16)
        block_output = (hidden_state + simple_product(hidden_rows, down_weight)).astype(jnp.bfloat16)
        hidden_slope = simple_product(rows_slope, down_weight.T)
        down_grad = simple_product(hidden_rows.T, rows_slope)
        gate_slope = (hidden_slope * up_values * gate_sigmoid * (1.0 + gate_values * (1.0 - gate_sigmoid))).astype(jnp.bfloat16)
        up_slope = (hidden_slope * gate_values * gate_sigmoid).astype(jnp.bfloat16)
        gate_grad = simple_product(feed_rows.T, gate_slope)
        up_grad = simple_product(feed_rows.T, up_slope)
        feed_back = simple_product(gate_slope, gate_weight.T) + simple_product(up_slope, up_weight.T)
        feed_gain_term = lax.optimization_barrier(jnp.sum(feed_back * second_unit, axis=0))
        feed_unit_slope = feed_back * feed_gain
        state_slope = rows_slope.astype(jnp.float32) + second_scale * (feed_unit_slope - second_unit * lax.optimization_barrier(jnp.mean(feed_unit_slope * second_unit, axis=-1, keepdims=True)))
        state_rounded = state_slope.astype(jnp.bfloat16)
        mixed_gradient = simple_product(state_rounded, output_weight.T).astype(jnp.bfloat16)
        output_grad = simple_product(mixed_rows.T, state_rounded)
        gradient_sequences = mixed_gradient.reshape(SEQUENCE_COUNT, SEQUENCE_LENGTH, KEY_VALUE_HEADS, grouping_width, HEAD_WIDTH)
        query_slope, key_rows_gradient, value_rows_gradient = lax.map(attention_backward, (query_sequences, key_sequences, value_sequences, mixed_seqs, gradient_sequences, totals))
        query_slope = query_slope.reshape(grouped_rows, QUERY_HEAD_COUNT, HEAD_WIDTH)
        key_rows_gradient = key_rows_gradient.reshape(grouped_rows, KEY_VALUE_HEADS, HEAD_WIDTH)
        query_norm_slope = query_slope * cosine - rotate_half(query_slope) * sine
        query_gain_term = lax.optimization_barrier(jnp.sum(query_norm_slope * query_unit, axis=(0, 1)))
        query_unit_slope = query_norm_slope * query_gain
        query_raw_slope = (query_scale * (query_unit_slope - query_unit * lax.optimization_barrier(jnp.mean(query_unit_slope * query_unit, axis=-1, keepdims=True)))).astype(jnp.bfloat16).reshape(grouped_rows, QUERY_HEAD_COUNT * HEAD_WIDTH)
        key_norm_slope = key_rows_gradient * cosine - rotate_half(key_rows_gradient) * sine
        key_gain_term = lax.optimization_barrier(jnp.sum(key_norm_slope * normalized_key, axis=(0, 1)))
        normalized_key_gradient = key_norm_slope * key_gain
        unnormed_key_gradient = (key_norm_scale * (normalized_key_gradient - normalized_key * lax.optimization_barrier(jnp.mean(normalized_key_gradient * normalized_key, axis=-1, keepdims=True)))).astype(jnp.bfloat16).reshape(grouped_rows, KEY_VALUE_HEADS * HEAD_WIDTH)
        value_gradient_rows = value_rows_gradient.reshape(grouped_rows, KEY_VALUE_HEADS * HEAD_WIDTH)
        query_grad = simple_product(attention_output_rows.T, query_raw_slope)
        key_grad = simple_product(attention_output_rows.T, unnormed_key_gradient)
        value_grad = simple_product(attention_output_rows.T, value_gradient_rows)
        mixer_back = simple_product(query_raw_slope, query_weight.T) + simple_product(unnormed_key_gradient, key_matrix.T) + simple_product(value_gradient_rows, value_matrix.T)
        attention_gain_term = lax.optimization_barrier(jnp.sum(mixer_back * first_unit, axis=0))
        mixer_unit_slope = mixer_back * attention_gain
        input_gradient = (state_slope + first_scale * (mixer_unit_slope - first_unit * lax.optimization_barrier(jnp.mean(mixer_unit_slope * first_unit, axis=-1, keepdims=True)))).astype(jnp.bfloat16)
        terms = (attention_gain_term, query_grad, key_grad, value_grad, query_gain_term, key_gain_term, output_grad, feed_gain_term, gate_grad, up_grad, down_grad)
        return (jax.tree.map(jnp.add, carry, terms), (block_output, input_gradient))
    starting_value = (jnp.zeros((MODEL_WIDTH,), jnp.float32), jnp.zeros((MODEL_WIDTH, QUERY_HEAD_COUNT * HEAD_WIDTH), jnp.float32), jnp.zeros((MODEL_WIDTH, KEY_VALUE_HEADS * HEAD_WIDTH), jnp.float32), jnp.zeros((MODEL_WIDTH, KEY_VALUE_HEADS * HEAD_WIDTH), jnp.float32), jnp.zeros((HEAD_WIDTH,), jnp.float32), jnp.zeros((HEAD_WIDTH,), jnp.float32), jnp.zeros((QUERY_HEAD_COUNT * HEAD_WIDTH, MODEL_WIDTH), jnp.float32), jnp.zeros((MODEL_WIDTH,), jnp.float32), jnp.zeros((MODEL_WIDTH, HIDDEN_UNITS), jnp.float32), jnp.zeros((MODEL_WIDTH, HIDDEN_UNITS), jnp.float32), jnp.zeros((HIDDEN_UNITS, MODEL_WIDTH), jnp.float32))
    sums, stacked = lax.scan(group_step, starting_value, (inputs, slopes))
    block_output = stacked[0].reshape(N_DP * grouped_rows, MODEL_WIDTH)
    input_gradient = stacked[1].reshape(N_DP * grouped_rows, MODEL_WIDTH)
    return (block_output, input_gradient, sums[0], sums[1], sums[2], sums[3], sums[4], sums[5], sums[6], sums[7], sums[8], sums[9], sums[10])
```

```python
import functools

import jax
import jax.numpy as jnp
from jax import lax
from jax.experimental import pallas as pl
from jax.experimental.pallas import tpu as pltpu
from jax.sharding import PartitionSpec as P

SEQUENCE_LENGTH = 1024

epsilon = 1e-06
rope_base = 1000000.0

MESH = pl.DeviceIdType.MESH
VMEM_LIMIT = 62 * 1024 * 1024


def row_scale(values):
    return lax.rsqrt(jnp.mean(values * values, axis=-1, keepdims=True) + epsilon)


def rotate_half(values):
    half_size = values.shape[-1] // 2
    return jnp.concatenate([-values[..., half_size:], values[..., :half_size]], axis=-1)


def rope_tables(positions, head_size):
    half_size = head_size // 2
    frequency = rope_base ** (-(jnp.arange(half_size).astype(jnp.float32) * 2.0 / head_size))
    angles = positions[:, None] * frequency[None, :]
    angles = jnp.concatenate([angles, angles], axis=1)
    return (jnp.cos(angles)[:, None, :], jnp.sin(angles)[:, None, :])


def contract_rows(first_operand, second_operand):
    return lax.dot_general(
        first_operand, second_operand, (((0,), (0,)), ((), ())), preferred_element_type=jnp.float32
    )


def times_transposed(first_operand, second_operand):
    return lax.dot_general(
        first_operand, second_operand, (((1,), (1,)), ((), ())), preferred_element_type=jnp.float32
    )


def simple_product(first_operand, second_operand):
    return jnp.dot(first_operand, second_operand, preferred_element_type=jnp.float32)


def remote(source, target, send_sem, recv_sem, peer):
    return pltpu.make_async_remote_copy(
        src_ref=source,
        dst_ref=target,
        send_sem=send_sem,
        recv_sem=recv_sem,
        device_id={"tensor": peer},
        device_id_type=MESH,
    )


def greet(peers):
    barrier = pltpu.get_barrier_semaphore()
    for peer in peers:
        pl.semaphore_signal(barrier, inc=1, device_id={"tensor": peer}, device_id_type=MESH)
    pl.semaphore_wait(barrier, len(peers))


def square_peers(me):
    column = lax.rem(me, 2)
    row = me // 2
    return row * 2 + (1 - column), (1 - row) * 2 + column, (1 - row) * 2 + (1 - column)


def gather_kernel_square(count, *refs):
    own_refs, out_refs, held_refs = refs[:count], refs[count : 2 * count], refs[2 * count : 3 * count]
    send_sem, recv_sem, local_sem = refs[3 * count :]
    me = lax.axis_index("tensor")
    beside, below, across = square_peers(me)
    greet((beside, below))
    rows = own_refs[0].shape[0]
    half = rows // 2
    first, second = pl.ds(0, half), pl.ds(half, half)
    copies = []
    stores = []

    def store(k, source, slot, part, sem):
        start = slot * rows + (half if part == 1 else 0)
        size = rows if part is None else half
        copy = pltpu.make_async_copy(
            source, out_refs[k].at[pl.ds(pl.multiple_of(start, half), size)], local_sem.at[k, sem]
        )
        copy.start()
        stores.append(copy)

    for k in range(count):
        own, held = own_refs[k], held_refs[k]

        def send(index, source, slot, part, peer):
            copy = remote(
                source, held.at[slot, part], send_sem.at[k, index], recv_sem.at[k, index], peer
            )
            copy.start()
            copies.append(copy)
            return copy

        x_first = send(0, own.at[first], me, first, beside)
        y_second = send(1, own.at[second], me, second, below)
        x_second = send(2, own.at[second], me, second, beside)
        y_first = send(3, own.at[first], me, first, below)
        store(k, own, me, None, 0)
        x_first.wait_recv()
        y_pass = send(4, held.at[beside, first], beside, first, below)
        y_second.wait_recv()
        x_pass = send(5, held.at[below, second], below, second, beside)
        store(k, held.at[beside, first], beside, 0, 1)
        store(k, held.at[below, second], below, 1, 2)
    for k in range(count):
        held = held_refs[k]
        x_second, y_first, y_pass, x_pass = copies[6 * k + 2 : 6 * k + 6]
        x_second.wait_recv()
        store(k, held.at[beside, second], beside, 1, 3)
        y_first.wait_recv()
        store(k, held.at[below, first], below, 0, 4)
        y_pass.wait_recv()
        store(k, held.at[across, first], across, 0, 5)
        x_pass.wait_recv()
        store(k, held.at[across, second], across, 1, 6)
    for copy in copies:
        copy.wait_send()
    for copy in stores:
        copy.wait()


def gather_kernel_direct(size, count, *refs):
    own_refs, out_refs, held_refs = refs[:count], refs[count : 2 * count], refs[2 * count : 3 * count]
    send_sem, recv_sem, local_sem = refs[3 * count :]
    me = lax.axis_index("tensor")
    peers = [lax.rem(me + step, size) for step in range(1, size)]
    greet(peers)
    rows = own_refs[0].shape[0]
    copies = []
    stores = []
    for k in range(count):
        for step, peer in enumerate(peers):
            copy = remote(
                own_refs[k], held_refs[k].at[me], send_sem.at[k, step], recv_sem.at[k, step], peer
            )
            copy.start()
            copies.append(copy)
    for k in range(count):
        for step in range(size):
            source = own_refs[k]
            slot = lax.rem(me + size - step, size)
            if step > 0:
                copies[k * (size - 1) + step - 1].wait_recv()
                source = held_refs[k].at[slot]
            copy = pltpu.make_async_copy(
                source,
                out_refs[k].at[pl.ds(pl.multiple_of(slot * rows, rows), rows)],
                local_sem.at[k, step],
            )
            copy.start()
            stores.append(copy)
    for copy in copies:
        copy.wait_send()
    for copy in stores:
        copy.wait()


def gather_rows(arrays, size, collective_id):
    count = len(arrays)
    rows, columns = arrays[0].shape
    square = size == 4
    body = (
        functools.partial(gather_kernel_square, count)
        if square
        else functools.partial(gather_kernel_direct, size, count)
    )
    sends = 6 if square else size - 1
    locals_ = 7 if square else size
    return pl.pallas_call(
        body,
        out_shape=[jax.ShapeDtypeStruct((size * rows, columns), a.dtype) for a in arrays],
        in_specs=[pl.BlockSpec(memory_space=pltpu.VMEM)] * count,
        out_specs=[pl.BlockSpec(memory_space=pl.ANY)] * count,
        scratch_shapes=[pltpu.VMEM((size, rows, columns), a.dtype) for a in arrays]
        + [
            pltpu.SemaphoreType.DMA((count, sends)),
            pltpu.SemaphoreType.DMA((count, sends)),
            pltpu.SemaphoreType.DMA((count, locals_)),
        ],
        compiler_params=pltpu.CompilerParams(
            collective_id=collective_id, has_side_effects=True, vmem_limit_bytes=VMEM_LIMIT
        ),
        cost_estimate=pl.CostEstimate(
            flops=0, bytes_accessed=count * 30 * size * rows * columns, transcendentals=0
        ),
        name="gather_rows",
    )(*arrays)


def block_product(left_ref, start, rows, weight_ref, write):
    total = weight_ref.shape[0]
    tile = min(512, total)
    left = left_ref[pl.ds(pl.multiple_of(start, rows), rows), :]

    def step(index, carry):
        columns = pl.ds(pl.multiple_of(index * tile, tile), tile)
        write(columns, times_transposed(left, weight_ref[columns, :]))
        return carry

    lax.fori_loop(0, total // tile, step, 0)


def scatter_kernel_square(
    left_ref, weight_ref, out_ref, outgoing, passing, arriving, send_sem, recv_sem
):
    me = lax.axis_index("tensor")
    beside, below, across = square_peers(me)
    rows = out_ref.shape[0]
    half = rows // 2
    first, second = pl.ds(0, half), pl.ds(half, half)
    greet((beside, below))

    def fill(slot, owner):
        def write(columns, values):
            outgoing[slot, :, columns] = values.astype(outgoing.dtype)

        block_product(left_ref, owner * rows, rows, weight_ref, write)

    def send(index, source, target, peer):
        copy = remote(source, target, send_sem.at[index], recv_sem.at[index], peer)
        copy.start()
        return copy

    fill(0, across)
    x_pass = send(0, outgoing.at[0, first], passing.at[0], beside)
    y_pass = send(1, outgoing.at[0, second], passing.at[1], below)
    fill(1, beside)
    x_first = send(2, outgoing.at[1, first], arriving.at[0, first], beside)
    fill(2, below)
    y_second = send(3, outgoing.at[2, second], arriving.at[1, second], below)

    def write_own(columns, values):
        out_ref[:, columns] = values

    block_product(left_ref, me * rows, rows, weight_ref, write_own)
    y_pass.wait_recv()
    outgoing[1, second, :] = (
        outgoing[1, second, :].astype(jnp.float32) + passing[1].astype(jnp.float32)
    ).astype(outgoing.dtype)
    x_second = send(4, outgoing.at[1, second], arriving.at[0, second], beside)
    x_pass.wait_recv()
    outgoing[2, first, :] = (
        outgoing[2, first, :].astype(jnp.float32) + passing[0].astype(jnp.float32)
    ).astype(outgoing.dtype)
    y_first = send(5, outgoing.at[2, first], arriving.at[1, first], below)
    x_first.wait_recv()
    y_second.wait_recv()
    out_ref[first, :] += arriving[0, first, :].astype(jnp.float32)
    out_ref[second, :] += arriving[1, second, :].astype(jnp.float32)
    x_second.wait_recv()
    y_first.wait_recv()
    out_ref[second, :] += arriving[0, second, :].astype(jnp.float32)
    out_ref[first, :] += arriving[1, first, :].astype(jnp.float32)
    for copy in (x_pass, y_pass, x_first, y_second, x_second, y_first):
        copy.wait_send()


def scatter_kernel_direct(size, left_ref, weight_ref, out_ref, outgoing, arriving, send_sem, recv_sem):
    me = lax.axis_index("tensor")
    rows = out_ref.shape[0]
    peers = [lax.rem(me + step, size) for step in range(1, size)]
    greet(peers)
    copies = []
    for step, peer in enumerate(peers):

        def write(columns, values, step=step):
            outgoing[step, :, columns] = values.astype(outgoing.dtype)

        block_product(left_ref, peer * rows, rows, weight_ref, write)
        copy = remote(
            outgoing.at[step], arriving.at[step], send_sem.at[step], recv_sem.at[step], peer
        )
        copy.start()
        copies.append(copy)

    def write_own(columns, values):
        out_ref[:, columns] = values

    block_product(left_ref, me * rows, rows, weight_ref, write_own)
    for step, copy in enumerate(copies):
        copy.wait_recv()
        out_ref[...] += arriving[step].astype(jnp.float32)
    for copy in copies:
        copy.wait_send()


def product_scatter(left, weight, size, collective_id):
    total_rows, depth = left.shape
    columns = weight.shape[0]
    rows = total_rows // size
    square = size == 4
    if square:
        body = scatter_kernel_square
        buffers = [
            pltpu.VMEM((3, rows, columns), jnp.bfloat16),
            pltpu.VMEM((2, rows // 2, columns), jnp.bfloat16),
            pltpu.VMEM((2, rows, columns), jnp.bfloat16),
        ]
        sends = 6
    else:
        body = functools.partial(scatter_kernel_direct, size)
        buffers = [pltpu.VMEM((size - 1, rows, columns), jnp.bfloat16)] * 2
        sends = size - 1
    return pl.pallas_call(
        body,
        out_shape=jax.ShapeDtypeStruct((rows, columns), jnp.float32),
        in_specs=[pl.BlockSpec(memory_space=pltpu.VMEM)] * 2,
        out_specs=pl.BlockSpec(memory_space=pltpu.VMEM),
        scratch_shapes=buffers
        + [pltpu.SemaphoreType.DMA((sends,)), pltpu.SemaphoreType.DMA((sends,))],
        compiler_params=pltpu.CompilerParams(
            collective_id=collective_id, has_side_effects=True, vmem_limit_bytes=VMEM_LIMIT
        ),
        cost_estimate=pl.CostEstimate(
            flops=2 * total_rows * depth * columns,
            bytes_accessed=30 * total_rows * columns,
            transcendentals=0,
        ),
        name="product_scatter",
    )(left, weight)


def masked_scores(query_block, key_seq, first_row):
    scale_factor = query_block.shape[-1] ** (-0.5)
    scores = (
        jnp.einsum("qhgd,khd->hgqk", query_block, key_seq, preferred_element_type=jnp.float32)
        * scale_factor
    )
    visible = (first_row + jnp.arange(query_block.shape[0]))[:, None] >= jnp.arange(
        key_seq.shape[0]
    )[None, :]
    return jnp.where(visible, scores, -1e30)


def attend_forward(query_block, key_seq, value_seq, first_row):
    scores = masked_scores(query_block, key_seq, first_row)
    highest = jnp.max(scores, axis=-1, keepdims=True)
    log_total = highest[..., 0] + jnp.log(jnp.sum(jnp.exp(scores - highest), axis=-1))
    weights = jnp.exp(scores - log_total[..., None]).astype(jnp.bfloat16)
    mixed_block = jnp.einsum(
        "hgqk,khd->qhgd", weights, value_seq, preferred_element_type=jnp.float32
    ).astype(jnp.bfloat16)
    return (mixed_block, log_total)


def attend_backward(
    query_block, key_seq, value_seq, mixed_block, slope_block, total_block, first_row
):
    scale_factor = query_block.shape[-1] ** (-0.5)
    scores = masked_scores(query_block, key_seq, first_row)
    weights = jnp.exp(scores - total_block[..., None])
    value_part = jnp.einsum(
        "hgqk,qhgd->khd",
        weights.astype(jnp.bfloat16),
        slope_block,
        preferred_element_type=jnp.float32,
    )
    weight_slope = jnp.einsum(
        "qhgd,khd->hgqk", slope_block, value_seq, preferred_element_type=jnp.float32
    )
    centre = jnp.transpose(
        jnp.sum(slope_block.astype(jnp.float32) * mixed_block.astype(jnp.float32), axis=-1),
        (1, 2, 0),
    )
    score_slope = (weights * (weight_slope - centre[..., None])).astype(jnp.bfloat16)
    query_part = (
        jnp.einsum("hgqk,khd->qhgd", score_slope, key_seq, preferred_element_type=jnp.float32)
        * scale_factor
    )
    key_part = (
        jnp.einsum("hgqk,qhgd->khd", score_slope, query_block, preferred_element_type=jnp.float32)
        * scale_factor
    )
    return (query_part, key_part, value_part)


def head_norm_back(turn_slope, cosine, sine, unit_values, scale_values, gain_values):
    norm_slope = turn_slope * cosine - rotate_half(turn_slope) * sine
    gain_term = jnp.sum(norm_slope * unit_values, axis=(0, 1))
    unit_slope = norm_slope * gain_values
    raw_slope = (
        scale_values
        * (unit_slope - unit_values * jnp.mean(unit_slope * unit_values, axis=-1, keepdims=True))
    ).astype(jnp.bfloat16)
    return (raw_slope.reshape(raw_slope.shape[0], -1), gain_term)


def per_device(
    block_input,
    attention_gain,
    query_weight,
    key_matrix,
    value_matrix,
    query_gain,
    key_gain,
    output_weight,
    feed_gain,
    gate_weight,
    up_weight,
    down_weight,
    out_cotangent,
):
    size = lax.axis_size("tensor")
    local_rows = block_input.shape[0]
    grouped_rows = local_rows * size
    head_size = query_gain.shape[0]
    query_columns = query_weight.shape[1]
    key_columns = key_matrix.shape[1]
    query_heads = query_columns // head_size
    value_heads = key_columns // head_size
    hidden_columns = gate_weight.shape[1]
    grouping_width = query_heads // value_heads
    sequences = grouped_rows // SEQUENCE_LENGTH
    block_rows = min(512, SEQUENCE_LENGTH)
    block_count = SEQUENCE_LENGTH // block_rows
    qkv_columns = query_columns + 2 * key_columns

    mixing_full = lax.all_gather(
        jnp.concatenate([query_weight, key_matrix, value_matrix, output_weight.T], axis=1),
        "dp",
        axis=0,
        tiled=True,
    )
    feeding_full = lax.all_gather(
        jnp.concatenate([gate_weight, up_weight], axis=1), "dp", axis=0, tiled=True
    )
    down_full = lax.all_gather(down_weight.T, "dp", axis=0, tiled=True)

    input_float = block_input.astype(jnp.float32)
    first_scale = row_scale(input_float)
    first_unit = input_float * first_scale
    mixer_local = (first_unit * attention_gain).astype(jnp.bfloat16)
    mixer_rows, cotangent_rows = gather_rows((mixer_local, out_cotangent), size, 0)

    cosine, sine = rope_tables(
        (jnp.arange(grouped_rows) % SEQUENCE_LENGTH).astype(jnp.float32), head_size
    )
    qkv_full = mixing_full[:, :qkv_columns]
    output_full = mixing_full[:, qkv_columns:]
    qkv_raw = simple_product(mixer_rows, qkv_full)
    query_raw = qkv_raw[:, :query_columns].reshape(grouped_rows, query_heads, head_size)
    unnormed_key = qkv_raw[:, query_columns : query_columns + key_columns].reshape(
        grouped_rows, value_heads, head_size
    )
    value_token_rows = qkv_raw[:, query_columns + key_columns :].astype(jnp.bfloat16)
    query_scale = row_scale(query_raw)
    query_unit = query_raw * query_scale
    query_normed = query_unit * query_gain
    rotated_query = (query_normed * cosine + rotate_half(query_normed) * sine).astype(jnp.bfloat16)
    key_norm_scale = row_scale(unnormed_key)
    normalized_key = unnormed_key * key_norm_scale
    key_normed = normalized_key * key_gain
    rotated_key = (key_normed * cosine + rotate_half(key_normed) * sine).astype(jnp.bfloat16)
    query_sequences = rotated_query.reshape(
        sequences, SEQUENCE_LENGTH, value_heads, grouping_width, head_size
    )
    key_sequences = rotated_key.reshape(sequences, SEQUENCE_LENGTH, value_heads, head_size)
    value_sequences = value_token_rows.reshape(sequences, SEQUENCE_LENGTH, value_heads, head_size)

    def forward_sequence(operands):
        query_seq, key_seq, value_seq = operands
        mixed_parts = []
        total_parts = []
        for block_index in range(block_count):
            first_row = block_index * block_rows
            mixed_block, log_total = attend_forward(
                query_seq[first_row : first_row + block_rows], key_seq, value_seq, first_row
            )
            mixed_parts.append(mixed_block)
            total_parts.append(log_total)
        return (jnp.concatenate(mixed_parts, axis=0), jnp.concatenate(total_parts, axis=-1))

    mixed_seqs, totals = lax.map(
        forward_sequence, (query_sequences, key_sequences, value_sequences)
    )
    mixed_rows = mixed_seqs.reshape(grouped_rows, query_heads * head_size)
    hidden_state = input_float + product_scatter(mixed_rows, output_full, size, 1)
    second_scale = row_scale(hidden_state)
    second_unit = hidden_state * second_scale
    feed_local = (second_unit * feed_gain).astype(jnp.bfloat16)
    (feed_rows,) = gather_rows((feed_local,), size, 2)
    both_values = simple_product(feed_rows, feeding_full)
    gate_values = both_values[:, :hidden_columns]
    up_values = both_values[:, hidden_columns:]
    gate_sigmoid = jax.nn.sigmoid(gate_values)
    hidden_rows = (gate_values * gate_sigmoid * up_values).astype(jnp.bfloat16)
    down_grad = contract_rows(cotangent_rows, hidden_rows).astype(jnp.bfloat16)
    down_total = lax.psum_scatter(down_grad, "dp", scatter_dimension=0, tiled=True)

    hidden_slope = simple_product(cotangent_rows, down_full)
    gate_slope = (
        hidden_slope * up_values * gate_sigmoid * (1.0 + gate_values * (1.0 - gate_sigmoid))
    ).astype(jnp.bfloat16)
    up_slope = (hidden_slope * gate_values * gate_sigmoid).astype(jnp.bfloat16)
    feed_slope = jnp.concatenate([gate_slope, up_slope], axis=1)
    feed_grad = contract_rows(feed_rows, feed_slope).astype(jnp.bfloat16)
    feed_total = lax.psum_scatter(feed_grad, "dp", scatter_dimension=0, tiled=True)
    feed_back = product_scatter(feed_slope, feeding_full, size, 3)
    feed_gain_term = jnp.sum(feed_back * second_unit, axis=0)
    feed_unit_slope = feed_back * feed_gain
    state_slope = out_cotangent.astype(jnp.float32) + second_scale * (
        feed_unit_slope
        - second_unit * jnp.mean(feed_unit_slope * second_unit, axis=-1, keepdims=True)
    )
    (state_rows,) = gather_rows((state_slope.astype(jnp.bfloat16),), size, 4)
    mixed_gradient = simple_product(state_rows, output_full).astype(jnp.bfloat16)
    output_grad = contract_rows(state_rows, mixed_rows).astype(jnp.bfloat16)
    gradient_sequences = mixed_gradient.reshape(
        sequences, SEQUENCE_LENGTH, value_heads, grouping_width, head_size
    )

    def backward_sequence(operands):
        query_seq, key_seq, value_seq, mixed_seq, slope_seq, total_seq = operands
        key_total = jnp.zeros(key_seq.shape, jnp.float32)
        value_total = jnp.zeros(value_seq.shape, jnp.float32)
        query_parts = []
        for block_index in range(block_count):
            first_row = block_index * block_rows
            last_row = first_row + block_rows
            query_part, key_part, value_part = attend_backward(
                query_seq[first_row:last_row],
                key_seq,
                value_seq,
                mixed_seq[first_row:last_row],
                slope_seq[first_row:last_row],
                total_seq[..., first_row:last_row],
                first_row,
            )
            query_parts.append(query_part)
            key_total = key_total + key_part
            value_total = value_total + value_part
        return (jnp.concatenate(query_parts, axis=0), key_total, value_total.astype(jnp.bfloat16))

    query_slope, key_rows_gradient, value_rows_gradient = lax.map(
        backward_sequence,
        (query_sequences, key_sequences, value_sequences, mixed_seqs, gradient_sequences, totals),
    )
    query_raw_slope, query_gain_term = head_norm_back(
        query_slope.reshape(grouped_rows, query_heads, head_size),
        cosine,
        sine,
        query_unit,
        query_scale,
        query_gain,
    )
    unnormed_key_gradient, key_gain_term = head_norm_back(
        key_rows_gradient.reshape(grouped_rows, value_heads, head_size),
        cosine,
        sine,
        normalized_key,
        key_norm_scale,
        key_gain,
    )
    value_gradient_rows = value_rows_gradient.reshape(grouped_rows, value_heads * head_size)
    qkv_slope = jnp.concatenate(
        [query_raw_slope, unnormed_key_gradient, value_gradient_rows], axis=1
    )
    qkv_grad = contract_rows(mixer_rows, qkv_slope).astype(jnp.bfloat16)
    mixing_total = lax.psum_scatter(
        jnp.concatenate([qkv_grad, output_grad], axis=1), "dp", scatter_dimension=0, tiled=True
    ).astype(jnp.float32)
    mixer_back = product_scatter(qkv_slope, qkv_full, size, 5)
    attention_gain_term = jnp.sum(mixer_back * first_unit, axis=0)
    mixer_unit_slope = mixer_back * attention_gain
    input_gradient = (
        state_slope
        + first_scale
        * (
            mixer_unit_slope
            - first_unit * jnp.mean(mixer_unit_slope * first_unit, axis=-1, keepdims=True)
        )
    ).astype(jnp.bfloat16)
    feed_sum = product_scatter(hidden_rows, down_full, size, 6)
    block_output = (hidden_state + feed_sum).astype(jnp.bfloat16)
    gain_totals = lax.psum(
        (attention_gain_term, feed_gain_term, query_gain_term, key_gain_term), ("dp", "tensor")
    )
    feed_total = feed_total.astype(jnp.float32)
    return (
        block_output,
        input_gradient,
        gain_totals[0],
        mixing_total[:, :query_columns],
        mixing_total[:, query_columns : query_columns + key_columns],
        mixing_total[:, query_columns + key_columns : qkv_columns],
        gain_totals[2],
        gain_totals[3],
        mixing_total[:, qkv_columns:].T,
        gain_totals[1],
        feed_total[:, :hidden_columns],
        feed_total[:, hidden_columns:],
        down_total.astype(jnp.float32).T,
    )


def solution(mesh):
    in_specs = (
        P(("dp", "tensor"), None),
        P(),
        P("dp", "tensor"),
        P("dp", "tensor"),
        P("dp", "tensor"),
        P(),
        P(),
        P("tensor", "dp"),
        P(),
        P("dp", "tensor"),
        P("dp", "tensor"),
        P("tensor", "dp"),
        P(("dp", "tensor"), None),
    )
    out_specs = (
        P(("dp", "tensor"), None),
        P(("dp", "tensor"), None),
        P(),
        P("dp", "tensor"),
        P("dp", "tensor"),
        P("dp", "tensor"),
        P(),
        P(),
        P("tensor", "dp"),
        P(),
        P("dp", "tensor"),
        P("dp", "tensor"),
        P("tensor", "dp"),
    )
    return jax.shard_map(
        per_device, mesh=mesh, in_specs=in_specs, out_specs=out_specs, check_vma=False
    )
```

```python
import functools

import jax
import jax.numpy as jnp
import numpy as np
from jax import lax
from jax.experimental import pallas as pl
from jax.experimental.pallas import tpu as pltpu
from jax.sharding import PartitionSpec as P


SEQUENCE_LENGTH = 1024

epsilon = 1e-06
rope_base = 1000000.0

MESH = pl.DeviceIdType.MESH
VMEM_LIMIT = 62 * 1024 * 1024


def row_scale(values):
    return lax.rsqrt(jnp.mean(values * values, axis=-1, keepdims=True) + epsilon)


def contract_rows(first_operand, second_operand):
    return lax.dot_general(
        first_operand, second_operand, (((0,), (0,)), ((), ())), preferred_element_type=jnp.float32
    )


def times_transposed(first_operand, second_operand):
    return lax.dot_general(
        first_operand, second_operand, (((1,), (1,)), ((), ())), preferred_element_type=jnp.float32
    )


def simple_product(first_operand, second_operand):
    return jnp.dot(first_operand, second_operand, preferred_element_type=jnp.float32)


def remote(source, target, send_sem, recv_sem, peer, axis="tensor"):
    return pltpu.make_async_remote_copy(
        src_ref=source,
        dst_ref=target,
        send_sem=send_sem,
        recv_sem=recv_sem,
        device_id={axis: peer},
        device_id_type=MESH,
    )


def greet(peers):
    barrier = pltpu.get_barrier_semaphore()
    for axis, peer in peers:
        pl.semaphore_signal(barrier, inc=1, device_id={axis: peer}, device_id_type=MESH)
    pl.semaphore_wait(barrier, len(peers))


def square_peers(me):
    column = lax.rem(me, 2)
    row = me // 2
    return row * 2 + (1 - column), (1 - row) * 2 + column, (1 - row) * 2 + (1 - column)


def gather_kernel_square(count, *refs):
    own_refs, out_refs, held_refs = refs[:count], refs[count : 2 * count], refs[2 * count : 3 * count]
    send_sem, recv_sem, local_sem = refs[3 * count :]
    me = lax.axis_index("tensor")
    beside, below, across = square_peers(me)
    greet((("tensor", beside), ("tensor", below)))
    rows = own_refs[0].shape[0]
    half = rows // 2
    first, second = pl.ds(0, half), pl.ds(half, half)
    copies = []
    stores = []

    def store(k, source, slot, part, sem):
        start = slot * rows + (half if part == 1 else 0)
        size = rows if part is None else half
        copy = pltpu.make_async_copy(
            source, out_refs[k].at[pl.ds(pl.multiple_of(start, half), size)], local_sem.at[k, sem]
        )
        copy.start()
        stores.append(copy)

    for k in range(count):
        own, held = own_refs[k], held_refs[k]

        def send(index, source, slot, part, peer):
            copy = remote(
                source, held.at[slot, part], send_sem.at[k, index], recv_sem.at[k, index], peer
            )
            copy.start()
            copies.append(copy)
            return copy

        x_first = send(0, own.at[first], me, first, beside)
        y_second = send(1, own.at[second], me, second, below)
        x_second = send(2, own.at[second], me, second, beside)
        y_first = send(3, own.at[first], me, first, below)
        store(k, own, me, None, 0)
        x_first.wait_recv()
        y_pass = send(4, held.at[beside, first], beside, first, below)
        y_second.wait_recv()
        x_pass = send(5, held.at[below, second], below, second, beside)
        store(k, held.at[beside, first], beside, 0, 1)
        store(k, held.at[below, second], below, 1, 2)
    for k in range(count):
        held = held_refs[k]
        x_second, y_first, y_pass, x_pass = copies[6 * k + 2 : 6 * k + 6]
        x_second.wait_recv()
        store(k, held.at[beside, second], beside, 1, 3)
        y_first.wait_recv()
        store(k, held.at[below, first], below, 0, 4)
        y_pass.wait_recv()
        store(k, held.at[across, first], across, 0, 5)
        x_pass.wait_recv()
        store(k, held.at[across, second], across, 1, 6)
    for copy in copies:
        copy.wait_send()
    for copy in stores:
        copy.wait()


def gather_kernel_direct(size, count, *refs):
    own_refs, out_refs, held_refs = refs[:count], refs[count : 2 * count], refs[2 * count : 3 * count]
    send_sem, recv_sem, local_sem = refs[3 * count :]
    me = lax.axis_index("tensor")
    peers = [lax.rem(me + step, size) for step in range(1, size)]
    greet([("tensor", peer) for peer in peers])
    rows = own_refs[0].shape[0]
    copies = []
    stores = []
    for k in range(count):
        for step, peer in enumerate(peers):
            copy = remote(
                own_refs[k], held_refs[k].at[me], send_sem.at[k, step], recv_sem.at[k, step], peer
            )
            copy.start()
            copies.append(copy)
    for k in range(count):
        for step in range(size):
            source = own_refs[k]
            slot = lax.rem(me + size - step, size)
            if step > 0:
                copies[k * (size - 1) + step - 1].wait_recv()
                source = held_refs[k].at[slot]
            copy = pltpu.make_async_copy(
                source,
                out_refs[k].at[pl.ds(pl.multiple_of(slot * rows, rows), rows)],
                local_sem.at[k, step],
            )
            copy.start()
            stores.append(copy)
    for copy in copies:
        copy.wait_send()
    for copy in stores:
        copy.wait()


def gather_rows(arrays, size, collective_id):
    count = len(arrays)
    rows, columns = arrays[0].shape
    square = size == 4
    body = (
        functools.partial(gather_kernel_square, count)
        if square
        else functools.partial(gather_kernel_direct, size, count)
    )
    sends = 6 if square else size - 1
    locals_ = 7 if square else size
    return pl.pallas_call(
        body,
        out_shape=[jax.ShapeDtypeStruct((size * rows, columns), a.dtype) for a in arrays],
        in_specs=[pl.BlockSpec(memory_space=pltpu.VMEM)] * count,
        out_specs=[pl.BlockSpec(memory_space=pl.ANY)] * count,
        scratch_shapes=[pltpu.VMEM((size, rows, columns), a.dtype) for a in arrays]
        + [
            pltpu.SemaphoreType.DMA((count, sends)),
            pltpu.SemaphoreType.DMA((count, sends)),
            pltpu.SemaphoreType.DMA((count, locals_)),
        ],
        compiler_params=pltpu.CompilerParams(
            collective_id=collective_id, has_side_effects=True, vmem_limit_bytes=VMEM_LIMIT
        ),
        cost_estimate=pl.CostEstimate(
            flops=0, bytes_accessed=count * 30 * size * rows * columns, transcendentals=0
        ),
        name="gather_rows",
    )(*arrays)


def block_product(left_ref, start, rows, weight_ref, write):
    total = weight_ref.shape[0]
    tile = min(512, total)
    left = left_ref[pl.ds(pl.multiple_of(start, rows), rows), :]

    def step(index, carry):
        columns = pl.ds(pl.multiple_of(index * tile, tile), tile)
        write(columns, times_transposed(left, weight_ref[columns, :]))
        return carry

    lax.fori_loop(0, total // tile, step, 0)


def other_members(axis, count):
    me = lax.axis_index(axis)
    return [lax.rem(me + step, count) for step in range(1, count)]


def send_terms(axis, peers, source, landing, send_sem, recv_sem):
    me = lax.axis_index(axis)
    landing[me] = source[...]
    copies = []
    for step, peer in enumerate(peers):
        copy = remote(source, landing.at[me], send_sem.at[step], recv_sem.at[step], peer, axis)
        copy.start()
        copies.append(copy)
    return copies


def add_terms(landing, copies):
    for copy in copies:
        copy.wait_recv()
    total = landing[0]
    for index in range(1, landing.shape[0]):
        total = total + landing[index]
    return total


def scatter_kernel(sizes, with_terms, *refs):
    if with_terms:
        left_ref, weight_ref, terms_ref, out_ref, terms_out_ref = refs[:5]
        inner, outer, partial_ref = refs[-7:-4]
        inner_send, inner_recv, outer_send, outer_recv = refs[-4:]
        buffers = refs[5:-7]
    else:
        left_ref, weight_ref, out_ref = refs[:3]
        buffers = refs[3:]
    data_size, size = sizes
    if size == 4:
        beside, below, across = square_peers(lax.axis_index("tensor"))
        near = [("tensor", beside), ("tensor", below)]
    else:
        near = [("tensor", peer) for peer in other_members("tensor", size)]
    if with_terms:
        if size == 4:
            near.append(("tensor", across))
        near += [("dp", peer) for peer in other_members("dp", data_size)]
    greet(near)
    if with_terms:
        inner_copies = send_terms(
            "tensor", other_members("tensor", size), terms_ref, inner, inner_send, inner_recv
        )
    if size == 4:
        scatter_square(left_ref, weight_ref, out_ref, *buffers)
    else:
        scatter_direct(size, left_ref, weight_ref, out_ref, *buffers)
    if with_terms:
        partial_ref[...] = add_terms(inner, inner_copies)
        outer_copies = send_terms(
            "dp", other_members("dp", data_size), partial_ref, outer, outer_send, outer_recv
        )
        terms_out_ref[...] = add_terms(outer, outer_copies)
        for copy in inner_copies + outer_copies:
            copy.wait_send()


def scatter_square(left_ref, weight_ref, out_ref, outgoing, passing, arriving, send_sem, recv_sem):
    me = lax.axis_index("tensor")
    beside, below, across = square_peers(me)
    rows = out_ref.shape[0]
    half = rows // 2
    first, second = pl.ds(0, half), pl.ds(half, half)

    def fill(slot, owner):
        def write(columns, values):
            outgoing[slot, :, columns] = values.astype(outgoing.dtype)

        block_product(left_ref, owner * rows, rows, weight_ref, write)

    def send(index, source, target, peer):
        copy = remote(source, target, send_sem.at[index], recv_sem.at[index], peer)
        copy.start()
        return copy

    fill(0, across)
    x_pass = send(0, outgoing.at[0, first], passing.at[0], beside)
    y_pass = send(1, outgoing.at[0, second], passing.at[1], below)
    fill(1, beside)
    x_first = send(2, outgoing.at[1, first], arriving.at[0, first], beside)
    fill(2, below)
    y_second = send(3, outgoing.at[2, second], arriving.at[1, second], below)

    def write_own(columns, values):
        out_ref[:, columns] = values

    block_product(left_ref, me * rows, rows, weight_ref, write_own)
    y_pass.wait_recv()
    outgoing[1, second, :] = (
        outgoing[1, second, :].astype(jnp.float32) + passing[1].astype(jnp.float32)
    ).astype(outgoing.dtype)
    x_second = send(4, outgoing.at[1, second], arriving.at[0, second], beside)
    x_pass.wait_recv()
    outgoing[2, first, :] = (
        outgoing[2, first, :].astype(jnp.float32) + passing[0].astype(jnp.float32)
    ).astype(outgoing.dtype)
    y_first = send(5, outgoing.at[2, first], arriving.at[1, first], below)
    x_first.wait_recv()
    y_second.wait_recv()
    out_ref[first, :] += arriving[0, first, :].astype(jnp.float32)
    out_ref[second, :] += arriving[1, second, :].astype(jnp.float32)
    x_second.wait_recv()
    y_first.wait_recv()
    out_ref[second, :] += arriving[0, second, :].astype(jnp.float32)
    out_ref[first, :] += arriving[1, first, :].astype(jnp.float32)
    for copy in (x_pass, y_pass, x_first, y_second, x_second, y_first):
        copy.wait_send()


def scatter_direct(size, left_ref, weight_ref, out_ref, outgoing, arriving, send_sem, recv_sem):
    me = lax.axis_index("tensor")
    rows = out_ref.shape[0]
    copies = []
    for step, peer in enumerate(other_members("tensor", size)):

        def write(columns, values, step=step):
            outgoing[step, :, columns] = values.astype(outgoing.dtype)

        block_product(left_ref, peer * rows, rows, weight_ref, write)
        copy = remote(
            outgoing.at[step], arriving.at[step], send_sem.at[step], recv_sem.at[step], peer
        )
        copy.start()
        copies.append(copy)

    def write_own(columns, values):
        out_ref[:, columns] = values

    block_product(left_ref, me * rows, rows, weight_ref, write_own)
    for step, copy in enumerate(copies):
        copy.wait_recv()
        out_ref[...] += arriving[step].astype(jnp.float32)
    for copy in copies:
        copy.wait_send()


def product_scatter(left, weight, first_column, sizes, collective_id, terms=None):
    total_rows, depth = left.shape
    columns = weight.shape[0]
    data_size, size = sizes
    rows = total_rows // size
    if size == 4:
        buffers = [
            pltpu.VMEM((3, rows, columns), jnp.bfloat16),
            pltpu.VMEM((2, rows // 2, columns), jnp.bfloat16),
            pltpu.VMEM((2, rows, columns), jnp.bfloat16),
        ]
        sends = 6
    else:
        buffers = [pltpu.VMEM((size - 1, rows, columns), jnp.bfloat16)] * 2
        sends = size - 1
    buffers += [pltpu.SemaphoreType.DMA((sends,)), pltpu.SemaphoreType.DMA((sends,))]
    block = first_column // depth
    whole = pl.BlockSpec(memory_space=pltpu.VMEM)
    in_specs = [
        pl.BlockSpec((total_rows, depth), lambda i: (0, 0), pipeline_mode=pl.Buffered(1)),
        pl.BlockSpec((columns, depth), lambda i: (0, block), pipeline_mode=pl.Buffered(1)),
    ]
    out_specs = [pl.BlockSpec((rows, columns), lambda i: (0, 0))]
    out_shape = [jax.ShapeDtypeStruct((rows, columns), jnp.float32)]
    operands = [left, weight]
    if terms is not None:
        operands.append(terms)
        in_specs.append(pl.BlockSpec(terms.shape, lambda i: (0, 0)))
        out_specs.append(pl.BlockSpec(terms.shape, lambda i: (0, 0)))
        out_shape.append(jax.ShapeDtypeStruct(terms.shape, terms.dtype))
        buffers += [
            pltpu.VMEM((size, *terms.shape), terms.dtype),
            pltpu.VMEM((data_size, *terms.shape), terms.dtype),
            pltpu.VMEM(terms.shape, terms.dtype),
        ]
        for count in (size, size, data_size, data_size):
            buffers.append(pltpu.SemaphoreType.DMA((count - 1,)))
    out = pl.pallas_call(
        functools.partial(scatter_kernel, sizes, terms is not None),
        grid=(1,),
        out_shape=out_shape,
        in_specs=in_specs,
        out_specs=out_specs,
        scratch_shapes=buffers,
        compiler_params=pltpu.CompilerParams(
            collective_id=collective_id, has_side_effects=True, vmem_limit_bytes=VMEM_LIMIT
        ),
        cost_estimate=pl.CostEstimate(
            flops=2 * total_rows * depth * columns,
            bytes_accessed=30 * total_rows * columns,
            transcendentals=0,
        ),
        name="product_scatter",
    )(*operands)
    return out[0] if terms is None else out


LOG2E = 1.4426950408889634


def turn_tables(head_size):
    half_size = head_size // 2
    frequency = np.float32(rope_base) ** (
        -(np.arange(half_size, dtype=np.float32) * np.float32(2.0) / np.float32(head_size))
    )
    angles = np.arange(SEQUENCE_LENGTH, dtype=np.float32)[:, None] * frequency[None, :]
    cosine, sine = np.cos(angles), np.sin(angles)
    return (
        np.concatenate([cosine, cosine], axis=1).astype(np.float32),
        np.concatenate([-sine, sine], axis=1).astype(np.float32),
    )


def turn(values, cosine, sine):
    return values * cosine + pltpu.roll(values, values.shape[-1] // 2, 1) * sine


def turn_back(values, cosine, sine):
    return values * cosine - pltpu.roll(values, values.shape[-1] // 2, 1) * sine


def contract_first(first_operand, second_operand):
    return lax.dot_general(
        first_operand, second_operand, (((0,), (0,)), ((), ())), preferred_element_type=jnp.float32
    )


def visible_scores(key_rows, query_rows, first_row, multiplier):
    scores = times_transposed(key_rows, query_rows) * multiplier
    _, queries = scores.shape
    key_at = lax.broadcasted_iota(jnp.int32, (queries, queries), 0)
    query_at = lax.broadcasted_iota(jnp.int32, (queries, queries), 1)
    corner = jnp.where(query_at >= key_at, scores[first_row:], -1e30)
    if first_row == 0:
        return corner
    return jnp.concatenate([scores[:first_row], corner], axis=0)


def attention_forward_kernel(
    grouping, head_size, block, rows_ref, weight_ref, cosine_ref, sine_ref, query_gain_ref, key_gain_ref,
    raw_ref, mixed_ref, total_ref, query_ref, key_ref, value_ref,
):
    sequence = rows_ref.shape[0]
    multiplier = head_size ** (-0.5) * LOG2E
    cosine, sine = cosine_ref[...], sine_ref[...]
    raw_ref[...] = simple_product(rows_ref[...], weight_ref[...])
    for part in range(grouping + 1):
        raw = raw_ref[:, part * head_size : (part + 1) * head_size]
        gain = key_gain_ref[...] if part == grouping else query_gain_ref[...]
        turned = turn(raw * row_scale(raw) * gain, cosine, sine).astype(jnp.bfloat16)
        if part == grouping:
            key_ref[...] = turned
        else:
            query_ref[part] = turned
    value_ref[...] = raw_ref[:, (grouping + 1) * head_size :].astype(jnp.bfloat16)
    for part in range(grouping):
        totals = []
        for first_row in range(0, sequence, block):
            last_row = first_row + block
            scores = visible_scores(
                key_ref[:last_row, :], query_ref[part, first_row:last_row, :], first_row, multiplier
            )
            highest = jnp.max(scores, axis=0, keepdims=True)
            weights = jnp.exp2(scores - highest)
            total = jnp.sum(weights, axis=0, keepdims=True)
            weights = (weights * (1.0 / total)).astype(jnp.bfloat16)
            mixed_ref[first_row:last_row, part * head_size : (part + 1) * head_size] = contract_first(
                weights, value_ref[:last_row, :]
            ).astype(mixed_ref.dtype)
            totals.append(highest + jnp.log2(total))
        total_ref[0, part : part + 1, :] = jnp.concatenate(totals, axis=1)


def attention_forward(rows, weight, cosine, sine, query_gain, key_gain, heads, grouping):
    total_rows, depth = rows.shape
    head_size = query_gain.shape[0]
    sequences = total_rows // SEQUENCE_LENGTH
    width = (grouping + 2) * head_size
    block = min(256, SEQUENCE_LENGTH)
    table = pl.BlockSpec((SEQUENCE_LENGTH, head_size), lambda s, h: (0, 0))
    gain = pl.BlockSpec((1, head_size), lambda s, h: (0, 0))
    elements = heads * grouping * total_rows * SEQUENCE_LENGTH // 2
    return pl.pallas_call(
        functools.partial(attention_forward_kernel, grouping, head_size, block),
        grid=(sequences, heads),
        out_shape=[
            jax.ShapeDtypeStruct((total_rows, heads * width), jnp.float32),
            jax.ShapeDtypeStruct((total_rows, heads * grouping * head_size), jnp.bfloat16),
            jax.ShapeDtypeStruct((heads, grouping, total_rows), jnp.float32),
        ],
        in_specs=[
            pl.BlockSpec((SEQUENCE_LENGTH, depth), lambda s, h: (s, 0)),
            pl.BlockSpec((depth, width), lambda s, h: (0, h)),
            table,
            table,
            gain,
            gain,
        ],
        out_specs=[
            pl.BlockSpec((SEQUENCE_LENGTH, width), lambda s, h: (s, h)),
            pl.BlockSpec((SEQUENCE_LENGTH, grouping * head_size), lambda s, h: (s, h)),
            pl.BlockSpec((1, grouping, SEQUENCE_LENGTH), lambda s, h: (h, 0, s)),
        ],
        scratch_shapes=[
            pltpu.VMEM((grouping, SEQUENCE_LENGTH, head_size), jnp.bfloat16),
            pltpu.VMEM((SEQUENCE_LENGTH, head_size), jnp.bfloat16),
            pltpu.VMEM((SEQUENCE_LENGTH, head_size), jnp.bfloat16),
        ],
        compiler_params=pltpu.CompilerParams(vmem_limit_bytes=VMEM_LIMIT),
        cost_estimate=pl.CostEstimate(
            flops=2 * total_rows * depth * heads * width + 4 * elements * head_size,
            bytes_accessed=2 * (total_rows * depth + depth * heads * width),
            transcendentals=elements,
        ),
        name="attention_forward",
    )(rows, weight, cosine, sine, query_gain.reshape(1, -1), key_gain.reshape(1, -1))


def norm_back(turned_slope, raw, gain, cosine, sine):
    norm_slope = turn_back(turned_slope, cosine, sine)
    scale = row_scale(raw)
    unit = raw * scale
    term = norm_slope * unit
    unit_slope = norm_slope * gain
    slope = scale * (unit_slope - unit * jnp.mean(unit_slope * unit, axis=-1, keepdims=True))
    return slope.astype(jnp.bfloat16), jnp.sum(term, axis=0, keepdims=True)


def attention_backward_kernel(
    grouping, head_size, block, state_ref, weight_ref, raw_ref, mixed_ref, total_ref, cosine_ref, sine_ref,
    query_gain_ref, key_gain_ref, slope_ref, gain_ref, query_ref, key_ref, value_ref, out_slope_ref,
    turned_ref, key_sum_ref, value_sum_ref,
):
    sequence = state_ref.shape[0]
    scale_factor = head_size ** (-0.5)
    multiplier = scale_factor * LOG2E
    cosine, sine = cosine_ref[...], sine_ref[...]

    @pl.when((pl.program_id(0) == 0) & (pl.program_id(1) == 0))
    def _():
        gain_ref[...] = jnp.zeros_like(gain_ref)

    out_slope_ref[...] = simple_product(state_ref[...], weight_ref[...]).astype(jnp.bfloat16)
    for part in range(grouping + 1):
        raw = raw_ref[:, part * head_size : (part + 1) * head_size]
        gain = key_gain_ref[...] if part == grouping else query_gain_ref[...]
        turned = turn(raw * row_scale(raw) * gain, cosine, sine).astype(jnp.bfloat16)
        if part == grouping:
            key_ref[...] = turned
        else:
            query_ref[part] = turned
    value_ref[...] = raw_ref[:, (grouping + 1) * head_size :].astype(jnp.bfloat16)
    key_sum_ref[...] = jnp.zeros_like(key_sum_ref)
    value_sum_ref[...] = jnp.zeros_like(value_sum_ref)
    ones = jnp.ones((8, head_size), jnp.float32)
    for part in range(grouping):
        lanes = slice(part * head_size, (part + 1) * head_size)
        for first_row in range(0, sequence, block):
            last_row = first_row + block
            query_rows = query_ref[part, first_row:last_row, :]
            slope_rows = out_slope_ref[first_row:last_row, lanes]
            scores = visible_scores(key_ref[:last_row, :], query_rows, first_row, multiplier)
            weights = jnp.exp2(scores - total_ref[0, part : part + 1, first_row:last_row])
            value_sum_ref[:last_row, :] += simple_product(weights.astype(jnp.bfloat16), slope_rows)
            product = slope_rows.astype(jnp.float32) * mixed_ref[first_row:last_row, lanes].astype(jnp.float32)
            centre = lax.dot_general(
                ones,
                product,
                (((1,), (1,)), ((), ())),
                preferred_element_type=jnp.float32,
                precision=lax.Precision.HIGHEST,
            )[:1]
            weight_slope = times_transposed(value_ref[:last_row, :], slope_rows)
            score_slope = (weights * (weight_slope - centre)).astype(jnp.bfloat16)
            key_sum_ref[:last_row, :] += simple_product(score_slope, query_rows)
            turned_ref[first_row:last_row, :] = (
                contract_first(score_slope, key_ref[:last_row, :]) * scale_factor
            )
        slope, term = norm_back(
            turned_ref[...], raw_ref[:, lanes], query_gain_ref[...], cosine, sine
        )
        slope_ref[:, lanes] = slope
        gain_ref[0:1, :] += term
    lanes = slice(grouping * head_size, (grouping + 1) * head_size)
    slope, term = norm_back(
        key_sum_ref[...] * scale_factor, raw_ref[:, lanes], key_gain_ref[...], cosine, sine
    )
    slope_ref[:, lanes] = slope
    gain_ref[1:2, :] += term
    slope_ref[:, (grouping + 1) * head_size :] = value_sum_ref[...].astype(jnp.bfloat16)


def attention_backward(
    state_rows, weight, weight_start, raw, mixed, totals, cosine, sine, query_gain, key_gain, heads, grouping
):
    total_rows, depth = state_rows.shape
    head_size = query_gain.shape[0]
    sequences = total_rows // SEQUENCE_LENGTH
    width = (grouping + 2) * head_size
    out_width = grouping * head_size
    block = min(256, SEQUENCE_LENGTH)
    first_block = weight_start // out_width
    table = pl.BlockSpec((SEQUENCE_LENGTH, head_size), lambda s, h: (0, 0))
    gain = pl.BlockSpec((1, head_size), lambda s, h: (0, 0))
    elements = heads * grouping * total_rows * SEQUENCE_LENGTH // 2
    return pl.pallas_call(
        functools.partial(attention_backward_kernel, grouping, head_size, block),
        grid=(sequences, heads),
        out_shape=[
            jax.ShapeDtypeStruct((total_rows, heads * width), jnp.bfloat16),
            jax.ShapeDtypeStruct((8, head_size), jnp.float32),
        ],
        in_specs=[
            pl.BlockSpec((SEQUENCE_LENGTH, depth), lambda s, h: (s, 0)),
            pl.BlockSpec((depth, out_width), lambda s, h: (0, first_block + h)),
            pl.BlockSpec((SEQUENCE_LENGTH, width), lambda s, h: (s, h)),
            pl.BlockSpec((SEQUENCE_LENGTH, out_width), lambda s, h: (s, h)),
            pl.BlockSpec((1, grouping, SEQUENCE_LENGTH), lambda s, h: (h, 0, s)),
            table,
            table,
            gain,
            gain,
        ],
        out_specs=[
            pl.BlockSpec((SEQUENCE_LENGTH, width), lambda s, h: (s, h)),
            pl.BlockSpec((8, head_size), lambda s, h: (0, 0)),
        ],
        scratch_shapes=[
            pltpu.VMEM((grouping, SEQUENCE_LENGTH, head_size), jnp.bfloat16),
            pltpu.VMEM((SEQUENCE_LENGTH, head_size), jnp.bfloat16),
            pltpu.VMEM((SEQUENCE_LENGTH, head_size), jnp.bfloat16),
            pltpu.VMEM((SEQUENCE_LENGTH, out_width), jnp.bfloat16),
            pltpu.VMEM((SEQUENCE_LENGTH, head_size), jnp.float32),
            pltpu.VMEM((SEQUENCE_LENGTH, head_size), jnp.float32),
            pltpu.VMEM((SEQUENCE_LENGTH, head_size), jnp.float32),
        ],
        compiler_params=pltpu.CompilerParams(vmem_limit_bytes=VMEM_LIMIT),
        cost_estimate=pl.CostEstimate(
            flops=2 * total_rows * depth * heads * out_width + 10 * elements * head_size,
            bytes_accessed=2 * (total_rows * depth + depth * heads * out_width),
            transcendentals=elements,
        ),
        name="attention_backward",
    )(
        state_rows, weight, raw, mixed, totals, cosine, sine,
        query_gain.reshape(1, -1), key_gain.reshape(1, -1),
    )


def per_device(
    block_input,
    attention_gain,
    query_weight,
    key_matrix,
    value_matrix,
    query_gain,
    key_gain,
    output_weight,
    feed_gain,
    gate_weight,
    up_weight,
    down_weight,
    out_cotangent,
):
    size = lax.axis_size("tensor")
    sizes = (lax.axis_size("dp"), size)
    model_width = block_input.shape[1]
    head_size = query_gain.shape[0]
    query_columns = query_weight.shape[1]
    key_columns = key_matrix.shape[1]
    heads = key_columns // head_size
    grouping = query_columns // key_columns
    hidden_columns = gate_weight.shape[1]
    qkv_columns = query_columns + 2 * key_columns
    query_width = grouping * head_size
    width = query_width + 2 * head_size
    cosine, sine = turn_tables(head_size)

    mixing_parts = []
    for head in range(heads):
        mixing_parts += [
            query_weight[:, head * query_width : (head + 1) * query_width],
            key_matrix[:, head * head_size : (head + 1) * head_size],
            value_matrix[:, head * head_size : (head + 1) * head_size],
        ]
    mixing_full = lax.all_gather(
        jnp.concatenate([*mixing_parts, output_weight.T], axis=1), "dp", axis=0, tiled=True
    )
    feeding_full = lax.all_gather(
        jnp.concatenate([gate_weight, up_weight], axis=1), "dp", axis=0, tiled=True
    )
    down_full = lax.all_gather(down_weight.T, "dp", axis=0, tiled=True)

    input_float = block_input.astype(jnp.float32)
    first_scale = row_scale(input_float)
    first_unit = input_float * first_scale
    mixer_local = (first_unit * attention_gain).astype(jnp.bfloat16)
    mixer_rows, cotangent_rows = gather_rows((mixer_local, out_cotangent), size, 0)

    raw, mixed_rows, totals = attention_forward(
        mixer_rows, mixing_full, cosine, sine, query_gain, key_gain, heads, grouping
    )
    hidden_state = input_float + product_scatter(mixed_rows, mixing_full, qkv_columns, sizes, 1)
    second_scale = row_scale(hidden_state)
    second_unit = hidden_state * second_scale
    feed_local = (second_unit * feed_gain).astype(jnp.bfloat16)
    (feed_rows,) = gather_rows((feed_local,), size, 2)
    both_values = simple_product(feed_rows, feeding_full).astype(jnp.bfloat16)
    gate_values = both_values[:, :hidden_columns].astype(jnp.float32)
    up_values = both_values[:, hidden_columns:].astype(jnp.float32)
    gate_sigmoid = jax.nn.sigmoid(gate_values)
    hidden_rows = (gate_values * gate_sigmoid * up_values).astype(jnp.bfloat16)
    down_grad = contract_rows(cotangent_rows, hidden_rows).astype(jnp.bfloat16)
    down_grad, down_full = lax.optimization_barrier((down_grad, down_full))
    down_total = lax.psum_scatter(down_grad, "dp", scatter_dimension=0, tiled=True)

    hidden_slope = simple_product(cotangent_rows, down_full)
    gate_slope = (
        hidden_slope * up_values * gate_sigmoid * (1.0 + gate_values * (1.0 - gate_sigmoid))
    ).astype(jnp.bfloat16)
    up_slope = (hidden_slope * gate_values * gate_sigmoid).astype(jnp.bfloat16)
    feed_slope = jnp.concatenate([gate_slope, up_slope], axis=1)
    feed_grad = contract_rows(feed_rows, feed_slope).astype(jnp.bfloat16)
    feed_grad, feed_slope = lax.optimization_barrier((feed_grad, feed_slope))
    feed_total = lax.psum_scatter(feed_grad, "dp", scatter_dimension=0, tiled=True)
    feed_back = product_scatter(feed_slope, feeding_full, 0, sizes, 3)
    feed_gain_term = jnp.sum(feed_back * second_unit, axis=0)
    feed_unit_slope = feed_back * feed_gain
    state_slope = out_cotangent.astype(jnp.float32) + second_scale * (
        feed_unit_slope
        - second_unit * jnp.mean(feed_unit_slope * second_unit, axis=-1, keepdims=True)
    )
    (state_rows,) = gather_rows((state_slope.astype(jnp.bfloat16),), size, 4)
    qkv_slope, head_terms = attention_backward(
        state_rows, mixing_full, qkv_columns, raw, mixed_rows, totals, cosine, sine,
        query_gain, key_gain, heads, grouping,
    )
    mixing_grad = jnp.concatenate(
        [contract_rows(mixer_rows, qkv_slope), contract_rows(state_rows, mixed_rows)], axis=1
    ).astype(jnp.bfloat16)
    mixing_grad, qkv_slope = lax.optimization_barrier((mixing_grad, qkv_slope))
    mixing_total = lax.psum_scatter(
        mixing_grad, "dp", scatter_dimension=0, tiled=True
    ).astype(jnp.float32)
    mixer_back = product_scatter(qkv_slope, mixing_full, 0, sizes, 5)
    attention_gain_term = jnp.sum(mixer_back * first_unit, axis=0)
    mixer_unit_slope = mixer_back * attention_gain
    input_gradient = (
        state_slope
        + first_scale
        * (
            mixer_unit_slope
            - first_unit * jnp.mean(mixer_unit_slope * first_unit, axis=-1, keepdims=True)
        )
    ).astype(jnp.bfloat16)
    gain_rows = model_width // head_size
    terms = jnp.concatenate(
        [
            attention_gain_term.reshape(gain_rows, head_size),
            feed_gain_term.reshape(gain_rows, head_size),
            head_terms,
        ],
        axis=0,
    )
    feed_sum, terms = product_scatter(hidden_rows, down_full, 0, sizes, 6, terms)
    block_output = (hidden_state + feed_sum).astype(jnp.bfloat16)
    feed_total = feed_total.astype(jnp.float32)

    def column_parts(start, part_width):
        return jnp.concatenate(
            [
                mixing_total[:, head * width + start : head * width + start + part_width]
                for head in range(heads)
            ],
            axis=1,
        )

    return (
        block_output,
        input_gradient,
        terms[:gain_rows].reshape(-1),
        column_parts(0, query_width),
        column_parts(query_width, head_size),
        column_parts(query_width + head_size, head_size),
        terms[2 * gain_rows],
        terms[2 * gain_rows + 1],
        mixing_total[:, qkv_columns:].T,
        terms[gain_rows : 2 * gain_rows].reshape(-1),
        feed_total[:, :hidden_columns],
        feed_total[:, hidden_columns:],
        down_total.astype(jnp.float32).T,
    )


def solution(mesh):
    in_specs = (
        P(("dp", "tensor"), None),
        P(),
        P("dp", "tensor"),
        P("dp", "tensor"),
        P("dp", "tensor"),
        P(),
        P(),
        P("tensor", "dp"),
        P(),
        P("dp", "tensor"),
        P("dp", "tensor"),
        P("tensor", "dp"),
        P(("dp", "tensor"), None),
    )
    out_specs = (
        P(("dp", "tensor"), None),
        P(("dp", "tensor"), None),
        P(),
        P("dp", "tensor"),
        P("dp", "tensor"),
        P("dp", "tensor"),
        P(),
        P(),
        P("tensor", "dp"),
        P(),
        P("dp", "tensor"),
        P("dp", "tensor"),
        P("tensor", "dp"),
    )

    return jax.shard_map(
        per_device, mesh=mesh, in_specs=in_specs, out_specs=out_specs, check_vma=False
    )
```

```python
import functools

import jax
import jax.numpy as jnp
import numpy as np
from jax import lax
from jax.experimental import pallas as pl
from jax.experimental.pallas import tpu as pltpu
from jax.sharding import PartitionSpec as P


SEQUENCE_LENGTH = 1024

epsilon = 1e-06
rope_base = 1000000.0


MESH = pl.DeviceIdType.MESH
VMEM_LIMIT = 62 * 1024 * 1024


def row_scale(values):
    return lax.rsqrt(jnp.mean(values * values, axis=-1, keepdims=True) + epsilon)


def times_transposed(first_operand, second_operand):
    return lax.dot_general(
        first_operand, second_operand, (((1,), (1,)), ((), ())), preferred_element_type=jnp.float32
    )


def simple_product(first_operand, second_operand):
    return jnp.dot(first_operand, second_operand, preferred_element_type=jnp.float32)


def remote(source, target, send_sem, recv_sem, peer, axis="tensor"):
    return pltpu.make_async_remote_copy(
        src_ref=source,
        dst_ref=target,
        send_sem=send_sem,
        recv_sem=recv_sem,
        device_id={axis: peer},
        device_id_type=MESH,
    )


def greet(peers):
    barrier = pltpu.get_barrier_semaphore()
    for axis, peer in peers:
        pl.semaphore_signal(barrier, inc=1, device_id={axis: peer}, device_id_type=MESH)
    pl.semaphore_wait(barrier, len(peers))


def square_peers(me):
    column = lax.rem(me, 2)
    row = me // 2
    return row * 2 + (1 - column), (1 - row) * 2 + column, (1 - row) * 2 + (1 - column)


def gather_kernel_square(count, *refs):
    own_refs, out_refs, held_refs = refs[:count], refs[count : 2 * count], refs[2 * count : 3 * count]
    send_sem, recv_sem, local_sem = refs[3 * count :]
    me = lax.axis_index("tensor")
    beside, below, across = square_peers(me)
    greet((("tensor", beside), ("tensor", below)))
    rows = own_refs[0].shape[0]
    half = rows // 2
    first, second = pl.ds(0, half), pl.ds(half, half)
    copies = []
    stores = []

    def store(k, source, slot, part, sem):
        start = slot * rows + (half if part == 1 else 0)
        size = rows if part is None else half
        copy = pltpu.make_async_copy(
            source, out_refs[k].at[pl.ds(pl.multiple_of(start, half), size)], local_sem.at[k, sem]
        )
        copy.start()
        stores.append(copy)

    for k in range(count):
        own, held = own_refs[k], held_refs[k]

        def send(index, source, slot, part, peer):
            copy = remote(
                source, held.at[slot, part], send_sem.at[k, index], recv_sem.at[k, index], peer
            )
            copy.start()
            copies.append(copy)
            return copy

        x_first = send(0, own.at[first], me, first, beside)
        y_second = send(1, own.at[second], me, second, below)
        x_second = send(2, own.at[second], me, second, beside)
        y_first = send(3, own.at[first], me, first, below)
        store(k, own, me, None, 0)
        x_first.wait_recv()
        y_pass = send(4, held.at[beside, first], beside, first, below)
        y_second.wait_recv()
        x_pass = send(5, held.at[below, second], below, second, beside)
        store(k, held.at[beside, first], beside, 0, 1)
        store(k, held.at[below, second], below, 1, 2)
    for k in range(count):
        held = held_refs[k]
        x_second, y_first, y_pass, x_pass = copies[6 * k + 2 : 6 * k + 6]
        x_second.wait_recv()
        store(k, held.at[beside, second], beside, 1, 3)
        y_first.wait_recv()
        store(k, held.at[below, first], below, 0, 4)
        y_pass.wait_recv()
        store(k, held.at[across, first], across, 0, 5)
        x_pass.wait_recv()
        store(k, held.at[across, second], across, 1, 6)
    for copy in copies:
        copy.wait_send()
    for copy in stores:
        copy.wait()


def gather_kernel_direct(size, count, *refs):
    own_refs, out_refs, held_refs = refs[:count], refs[count : 2 * count], refs[2 * count : 3 * count]
    send_sem, recv_sem, local_sem = refs[3 * count :]
    me = lax.axis_index("tensor")
    peers = [lax.rem(me + step, size) for step in range(1, size)]
    greet([("tensor", peer) for peer in peers])
    rows = own_refs[0].shape[0]
    copies = []
    stores = []
    for k in range(count):
        for step, peer in enumerate(peers):
            copy = remote(
                own_refs[k], held_refs[k].at[me], send_sem.at[k, step], recv_sem.at[k, step], peer
            )
            copy.start()
            copies.append(copy)
    for k in range(count):
        for step in range(size):
            source = own_refs[k]
            slot = lax.rem(me + size - step, size)
            if step > 0:
                copies[k * (size - 1) + step - 1].wait_recv()
                source = held_refs[k].at[slot]
            copy = pltpu.make_async_copy(
                source,
                out_refs[k].at[pl.ds(pl.multiple_of(slot * rows, rows), rows)],
                local_sem.at[k, step],
            )
            copy.start()
            stores.append(copy)
    for copy in copies:
        copy.wait_send()
    for copy in stores:
        copy.wait()


def gather_rows(arrays, size, collective_id):
    count = len(arrays)
    rows, columns = arrays[0].shape
    square = size == 4
    body = (
        functools.partial(gather_kernel_square, count)
        if square
        else functools.partial(gather_kernel_direct, size, count)
    )
    sends = 6 if square else size - 1
    locals_ = 7 if square else size
    return pl.pallas_call(
        body,
        out_shape=[jax.ShapeDtypeStruct((size * rows, columns), a.dtype) for a in arrays],
        in_specs=[pl.BlockSpec(memory_space=pltpu.VMEM)] * count,
        out_specs=[pl.BlockSpec(memory_space=pl.ANY)] * count,
        scratch_shapes=[pltpu.VMEM((size, rows, columns), a.dtype) for a in arrays]
        + [
            pltpu.SemaphoreType.DMA((count, sends)),
            pltpu.SemaphoreType.DMA((count, sends)),
            pltpu.SemaphoreType.DMA((count, locals_)),
        ],
        compiler_params=pltpu.CompilerParams(
            collective_id=collective_id, has_side_effects=True, vmem_limit_bytes=VMEM_LIMIT
        ),
        cost_estimate=pl.CostEstimate(
            flops=0, bytes_accessed=count * 30 * size * rows * columns, transcendentals=0
        ),
        name="gather_rows",
    )(*arrays)


def block_product(pairs, start, rows, write):
    total = pairs[0][1].shape[0]
    tile = min(512, total)
    start = pl.multiple_of(start, rows)

    def step(index, carry):
        columns = pl.ds(pl.multiple_of(index * tile, tile), tile)
        values = None
        for left_ref, weight_ref in pairs:
            part = times_transposed(left_ref[pl.ds(start, rows), :], weight_ref[columns, :])
            values = part if values is None else values + part
        write(columns, values)
        return carry

    lax.fori_loop(0, total // tile, step, 0)


def other_members(axis, count):
    me = lax.axis_index(axis)
    return [lax.rem(me + step, count) for step in range(1, count)]


def send_terms(axis, peers, source, landing, send_sem, recv_sem):
    me = lax.axis_index(axis)
    landing[me] = source[...]
    copies = []
    for step, peer in enumerate(peers):
        copy = remote(source, landing.at[me], send_sem.at[step], recv_sem.at[step], peer, axis)
        copy.start()
        copies.append(copy)
    return copies


def add_terms(landing, copies):
    for copy in copies:
        copy.wait_recv()
    total = landing[0]
    for index in range(1, landing.shape[0]):
        total = total + landing[index]
    return total


def scatter_kernel(sizes, pair_count, with_terms, *refs):
    pairs = [refs[2 * p : 2 * p + 2] for p in range(pair_count)]
    refs = refs[2 * pair_count :]
    if with_terms:
        terms_ref, out_ref, terms_out_ref = refs[:3]
        inner, outer, partial_ref = refs[-7:-4]
        inner_send, inner_recv, outer_send, outer_recv = refs[-4:]
        buffers = refs[3:-7]
    else:
        out_ref, buffers = refs[0], refs[1:]
    data_size, size = sizes
    if size == 4:
        beside, below, across = square_peers(lax.axis_index("tensor"))
        near = [("tensor", beside), ("tensor", below)]
    else:
        near = [("tensor", peer) for peer in other_members("tensor", size)]
    if with_terms:
        if size == 4:
            near.append(("tensor", across))
        near += [("dp", peer) for peer in other_members("dp", data_size)]
    greet(near)
    if with_terms:
        inner_copies = send_terms(
            "tensor", other_members("tensor", size), terms_ref, inner, inner_send, inner_recv
        )
    if size == 4:
        scatter_square(pairs, out_ref, *buffers)
    else:
        scatter_direct(size, pairs, out_ref, *buffers)
    if with_terms:
        partial_ref[...] = add_terms(inner, inner_copies)
        outer_copies = send_terms(
            "dp", other_members("dp", data_size), partial_ref, outer, outer_send, outer_recv
        )
        terms_out_ref[...] = add_terms(outer, outer_copies)
        for copy in inner_copies + outer_copies:
            copy.wait_send()


def scatter_square(pairs, out_ref, outgoing, passing, arriving, send_sem, recv_sem):
    me = lax.axis_index("tensor")
    beside, below, across = square_peers(me)
    rows = out_ref.shape[0]
    half = rows // 2
    first, second = pl.ds(0, half), pl.ds(half, half)

    def prepare(index, source, target, peer):
        return remote(source, target, send_sem.at[index], recv_sem.at[index], peer)

    x_pass = prepare(0, outgoing.at[0, first], passing.at[0], beside)
    y_pass = prepare(1, outgoing.at[0, second], passing.at[1], below)
    x_first = prepare(2, outgoing.at[1, first], arriving.at[0, first], beside)
    y_second = prepare(3, outgoing.at[2, second], arriving.at[1, second], below)
    x_second = prepare(4, outgoing.at[1, second], arriving.at[0, second], beside)
    y_first = prepare(5, outgoing.at[2, first], arriving.at[1, first], below)

    def fill(slot, carry):
        owner = jnp.where(
            slot == 0, across, jnp.where(slot == 1, beside, jnp.where(slot == 2, below, me))
        )

        def write(columns, values):
            outgoing[slot, :, columns] = values.astype(outgoing.dtype)

        block_product(pairs, owner * rows, rows, write)
        pl.when(slot == 0)(x_pass.start)
        pl.when(slot == 0)(y_pass.start)
        pl.when(slot == 1)(x_first.start)
        pl.when(slot == 2)(y_second.start)
        return carry

    lax.fori_loop(0, 4, fill, 0)
    y_pass.wait_recv()
    outgoing[1, second, :] = (
        outgoing[1, second, :].astype(jnp.float32) + passing[1].astype(jnp.float32)
    ).astype(outgoing.dtype)
    x_second.start()
    x_pass.wait_recv()
    outgoing[2, first, :] = (
        outgoing[2, first, :].astype(jnp.float32) + passing[0].astype(jnp.float32)
    ).astype(outgoing.dtype)
    y_first.start()
    x_first.wait_recv()
    y_second.wait_recv()
    x_second.wait_recv()
    y_first.wait_recv()
    out_ref[...] = (
        outgoing[3].astype(jnp.float32)
        + arriving[0].astype(jnp.float32)
        + arriving[1].astype(jnp.float32)
    )
    for copy in (x_pass, y_pass, x_first, y_second, x_second, y_first):
        copy.wait_send()


def scatter_direct(size, pairs, out_ref, outgoing, arriving, send_sem, recv_sem):
    me = lax.axis_index("tensor")
    rows = out_ref.shape[0]
    copies = []
    for step, peer in enumerate(other_members("tensor", size)):

        def write(columns, values, step=step):
            outgoing[step, :, columns] = values.astype(outgoing.dtype)

        block_product(pairs, peer * rows, rows, write)
        copy = remote(
            outgoing.at[step], arriving.at[step], send_sem.at[step], recv_sem.at[step], peer
        )
        copy.start()
        copies.append(copy)

    def write_own(columns, values):
        out_ref[:, columns] = values

    block_product(pairs, me * rows, rows, write_own)
    for step, copy in enumerate(copies):
        copy.wait_recv()
        out_ref[...] += arriving[step].astype(jnp.float32)
    for copy in copies:
        copy.wait_send()


def product_scatter(triples, sizes, collective_id, terms=None):
    total_rows = triples[0][0].shape[0]
    columns = triples[0][1].shape[0]
    depth = sum(left.shape[1] for left, _, _ in triples)
    data_size, size = sizes
    rows = total_rows // size
    if size == 4:
        buffers = [
            pltpu.VMEM((4, rows, columns), jnp.bfloat16),
            pltpu.VMEM((2, rows // 2, columns), jnp.bfloat16),
            pltpu.VMEM((2, rows, columns), jnp.bfloat16),
        ]
        sends = 6
    else:
        buffers = [pltpu.VMEM((size - 1, rows, columns), jnp.bfloat16)] * 2
        sends = size - 1
    buffers += [pltpu.SemaphoreType.DMA((sends,)), pltpu.SemaphoreType.DMA((sends,))]
    in_specs = []
    operands = []
    for left, weight, first_column in triples:
        part = left.shape[1]
        in_specs += [
            pl.BlockSpec((total_rows, part), lambda i: (0, 0), pipeline_mode=pl.Buffered(1)),
            pl.BlockSpec(
                (columns, part),
                lambda i, block=first_column // part: (0, block),
                pipeline_mode=pl.Buffered(1),
            ),
        ]
        operands += [left, weight]
    out_specs = [pl.BlockSpec((rows, columns), lambda i: (0, 0))]
    out_shape = [jax.ShapeDtypeStruct((rows, columns), jnp.float32)]
    if terms is not None:
        operands.append(terms)
        in_specs.append(pl.BlockSpec(terms.shape, lambda i: (0, 0)))
        out_specs.append(pl.BlockSpec(terms.shape, lambda i: (0, 0)))
        out_shape.append(jax.ShapeDtypeStruct(terms.shape, terms.dtype))
        buffers += [
            pltpu.VMEM((size, *terms.shape), terms.dtype),
            pltpu.VMEM((data_size, *terms.shape), terms.dtype),
            pltpu.VMEM(terms.shape, terms.dtype),
        ]
        for count in (size, size, data_size, data_size):
            buffers.append(pltpu.SemaphoreType.DMA((count - 1,)))
    out = pl.pallas_call(
        functools.partial(scatter_kernel, sizes, len(triples), terms is not None),
        grid=(1,),
        out_shape=out_shape,
        in_specs=in_specs,
        out_specs=out_specs,
        scratch_shapes=buffers,
        compiler_params=pltpu.CompilerParams(
            collective_id=collective_id, has_side_effects=True, vmem_limit_bytes=VMEM_LIMIT
        ),
        cost_estimate=pl.CostEstimate(
            flops=2 * total_rows * depth * columns,
            bytes_accessed=30 * total_rows * columns,
            transcendentals=0,
        ),
        name="product_scatter",
    )(*operands)
    return out[0] if terms is None else out


LOG2E = 1.4426950408889634


def turn_tables(head_size):
    half_size = head_size // 2
    frequency = np.float32(rope_base) ** (
        -(np.arange(half_size, dtype=np.float32) * np.float32(2.0) / np.float32(head_size))
    )
    frequency = frequency.astype(np.float64)
    sign = np.concatenate([-np.ones(half_size), np.ones(half_size)])[None, :]
    positions = np.concatenate([np.arange(0, SEQUENCE_LENGTH, 128), np.arange(128)])
    angles = positions[:, None] * np.concatenate([frequency, frequency])[None, :]
    return np.cos(angles).astype(np.float32), (sign * np.sin(angles)).astype(np.float32)


def fill_tables(few_cosines_ref, few_sines_ref, cosine_ref, sine_ref):
    coarse = few_cosines_ref.shape[0] - 128
    near_cosine, near_sine = few_cosines_ref[coarse:, :], few_sines_ref[coarse:, :]

    def step(index, carry):
        far_cosine = few_cosines_ref[pl.ds(index, 1), :]
        far_sine = few_sines_ref[pl.ds(index, 1), :]
        rows = pl.ds(pl.multiple_of(index * 128, 128), 128)
        cosine_ref[rows, :] = far_cosine * near_cosine - far_sine * near_sine
        sine_ref[rows, :] = far_sine * near_cosine + far_cosine * near_sine
        return carry

    lax.fori_loop(0, coarse, step, 0)


def turn(values, cosine, sine):
    return values * cosine + pltpu.roll(values, values.shape[-1] // 2, 1) * sine


def turn_back(values, cosine, sine):
    return values * cosine - pltpu.roll(values, values.shape[-1] // 2, 1) * sine


def contract_first(first_operand, second_operand):
    return lax.dot_general(
        first_operand, second_operand, (((0,), (0,)), ((), ())), preferred_element_type=jnp.float32
    )


def visible_scores(key_rows, query_rows, first_row, multiplier):
    scores = times_transposed(key_rows, query_rows) * multiplier
    _, queries = scores.shape
    key_at = lax.broadcasted_iota(jnp.int32, (queries, queries), 0)
    query_at = lax.broadcasted_iota(jnp.int32, (queries, queries), 1)
    corner = jnp.where(query_at >= key_at, scores[first_row:], -1e30)
    if first_row == 0:
        return corner
    return jnp.concatenate([scores[:first_row], corner], axis=0)


def turn_heads(
    grouping, head_size, raw_ref, query_gain_ref, key_gain_ref, cosine_ref, sine_ref, query_ref, key_ref, value_ref
):
    def turned(start, gain):
        raw = raw_ref[:, pl.ds(start, head_size)]
        return turn(raw * row_scale(raw) * gain, cosine_ref[...], sine_ref[...]).astype(jnp.bfloat16)

    def step(part, carry):
        query_ref[part] = turned(pl.multiple_of(part * head_size, head_size), query_gain_ref[...])
        return carry

    lax.fori_loop(0, grouping, step, 0)
    key_ref[...] = turned(grouping * head_size, key_gain_ref[...])
    value_ref[...] = raw_ref[:, (grouping + 1) * head_size :].astype(jnp.bfloat16)


def attention_forward_kernel(
    grouping, head_size, block, rows_ref, weight_ref, few_cosines_ref, few_sines_ref, query_gain_ref, key_gain_ref,
    raw_ref, mixed_ref, total_ref, query_ref, key_ref, value_ref, cosine_ref, sine_ref,
):
    sequence = rows_ref.shape[0]
    multiplier = head_size ** (-0.5) * LOG2E

    @pl.when((pl.program_id(0) == 0) & (pl.program_id(1) == 0))
    def _():
        fill_tables(few_cosines_ref, few_sines_ref, cosine_ref, sine_ref)

    raw_ref[...] = simple_product(rows_ref[...], weight_ref[...])
    turn_heads(
        grouping, head_size, raw_ref, query_gain_ref, key_gain_ref, cosine_ref, sine_ref, query_ref, key_ref, value_ref
    )

    def head_step(part, carry):
        lanes = pl.ds(pl.multiple_of(part * head_size, head_size), head_size)
        for first_row in range(0, sequence, block):
            last_row = first_row + block
            scores = visible_scores(
                key_ref[:last_row, :], query_ref[part, first_row:last_row, :], first_row, multiplier
            )
            highest = jnp.max(scores, axis=0, keepdims=True)
            weights = jnp.exp2(scores - highest)
            total = jnp.sum(weights, axis=0, keepdims=True)
            weights = (weights * (1.0 / total)).astype(jnp.bfloat16)
            mixed_ref[first_row:last_row, lanes] = contract_first(
                weights, value_ref[:last_row, :]
            ).astype(mixed_ref.dtype)
            total_ref[0, pl.ds(part, 1), first_row:last_row] = highest + jnp.log2(total)
        return carry

    lax.fori_loop(0, grouping, head_step, 0)


def attention_forward(rows, weight, tables, query_gain, key_gain, heads, grouping):
    total_rows, depth = rows.shape
    head_size = query_gain.shape[0]
    sequences = total_rows // SEQUENCE_LENGTH
    width = (grouping + 2) * head_size
    block = min(256, SEQUENCE_LENGTH)
    table = pl.BlockSpec(tables[0].shape, lambda s, h: (0, 0))
    gain = pl.BlockSpec((1, head_size), lambda s, h: (0, 0))
    elements = heads * grouping * total_rows * SEQUENCE_LENGTH // 2
    return pl.pallas_call(
        functools.partial(attention_forward_kernel, grouping, head_size, block),
        grid=(sequences, heads),
        out_shape=[
            jax.ShapeDtypeStruct((total_rows, heads * width), jnp.float32),
            jax.ShapeDtypeStruct((total_rows, heads * grouping * head_size), jnp.bfloat16),
            jax.ShapeDtypeStruct((heads, grouping, total_rows), jnp.float32),
        ],
        in_specs=[
            pl.BlockSpec((SEQUENCE_LENGTH, depth), lambda s, h: (s, 0)),
            pl.BlockSpec((depth, width), lambda s, h: (0, h)),
            table,
            table,
            gain,
            gain,
        ],
        out_specs=[
            pl.BlockSpec((SEQUENCE_LENGTH, width), lambda s, h: (s, h)),
            pl.BlockSpec((SEQUENCE_LENGTH, grouping * head_size), lambda s, h: (s, h)),
            pl.BlockSpec((1, grouping, SEQUENCE_LENGTH), lambda s, h: (h, 0, s)),
        ],
        scratch_shapes=[
            pltpu.VMEM((grouping, SEQUENCE_LENGTH, head_size), jnp.bfloat16),
            pltpu.VMEM((SEQUENCE_LENGTH, head_size), jnp.bfloat16),
            pltpu.VMEM((SEQUENCE_LENGTH, head_size), jnp.bfloat16),
            pltpu.VMEM((SEQUENCE_LENGTH, head_size), jnp.float32),
            pltpu.VMEM((SEQUENCE_LENGTH, head_size), jnp.float32),
        ],
        compiler_params=pltpu.CompilerParams(vmem_limit_bytes=VMEM_LIMIT),
        cost_estimate=pl.CostEstimate(
            flops=2 * total_rows * depth * heads * width + 4 * elements * head_size,
            bytes_accessed=2 * (total_rows * depth + depth * heads * width),
            transcendentals=elements,
        ),
        name="attention_forward",
    )(rows, weight, *tables, query_gain.reshape(1, -1), key_gain.reshape(1, -1))


def norm_back(turned_slope, raw, gain, cosine, sine):
    norm_slope = turn_back(turned_slope, cosine, sine)
    scale = row_scale(raw)
    unit = raw * scale
    term = norm_slope * unit
    unit_slope = norm_slope * gain
    slope = scale * (unit_slope - unit * jnp.mean(unit_slope * unit, axis=-1, keepdims=True))
    return slope.astype(jnp.bfloat16), jnp.sum(term, axis=0, keepdims=True)


def attention_backward_kernel(
    grouping, head_size, block, state_ref, weight_ref, raw_ref, mixed_ref, total_ref, few_cosines_ref, few_sines_ref,
    query_gain_ref, key_gain_ref, slope_ref, gain_ref, query_ref, key_ref, value_ref, out_slope_ref,
    turned_ref, key_sum_ref, value_sum_ref, cosine_ref, sine_ref,
):
    sequence = state_ref.shape[0]
    scale_factor = head_size ** (-0.5)
    multiplier = scale_factor * LOG2E

    @pl.when((pl.program_id(0) == 0) & (pl.program_id(1) == 0))
    def _():
        gain_ref[...] = jnp.zeros_like(gain_ref)
        fill_tables(few_cosines_ref, few_sines_ref, cosine_ref, sine_ref)

    out_slope_ref[...] = simple_product(state_ref[...], weight_ref[...]).astype(jnp.bfloat16)
    turn_heads(
        grouping, head_size, raw_ref, query_gain_ref, key_gain_ref, cosine_ref, sine_ref, query_ref, key_ref, value_ref
    )
    key_sum_ref[...] = jnp.zeros_like(key_sum_ref)
    value_sum_ref[...] = jnp.zeros_like(value_sum_ref)
    ones = jnp.ones((8, head_size), jnp.float32)

    def head_step(part, carry):
        lanes = pl.ds(pl.multiple_of(part * head_size, head_size), head_size)
        for first_row in range(0, sequence, block):
            last_row = first_row + block
            query_rows = query_ref[part, first_row:last_row, :]
            slope_rows = out_slope_ref[first_row:last_row, lanes]
            scores = visible_scores(key_ref[:last_row, :], query_rows, first_row, multiplier)
            weights = jnp.exp2(scores - total_ref[0, pl.ds(part, 1), first_row:last_row])
            value_sum_ref[:last_row, :] += simple_product(weights.astype(jnp.bfloat16), slope_rows)
            product = slope_rows.astype(jnp.float32) * mixed_ref[first_row:last_row, lanes].astype(jnp.float32)
            centre = lax.dot_general(
                ones,
                product,
                (((1,), (1,)), ((), ())),
                preferred_element_type=jnp.float32,
                precision=lax.Precision.HIGHEST,
            )[:1]
            weight_slope = times_transposed(value_ref[:last_row, :], slope_rows)
            score_slope = (weights * (weight_slope - centre)).astype(jnp.bfloat16)
            key_sum_ref[:last_row, :] += simple_product(score_slope, query_rows)
            turned_ref[first_row:last_row, :] = (
                contract_first(score_slope, key_ref[:last_row, :]) * scale_factor
            )
        slope, term = norm_back(
            turned_ref[...], raw_ref[:, lanes], query_gain_ref[...], cosine_ref[...], sine_ref[...]
        )
        slope_ref[:, lanes] = slope
        gain_ref[0:1, :] += term
        return carry

    lax.fori_loop(0, grouping, head_step, 0)
    lanes = slice(grouping * head_size, (grouping + 1) * head_size)
    slope, term = norm_back(
        key_sum_ref[...] * scale_factor, raw_ref[:, lanes], key_gain_ref[...], cosine_ref[...], sine_ref[...]
    )
    slope_ref[:, lanes] = slope
    gain_ref[1:2, :] += term
    slope_ref[:, (grouping + 1) * head_size :] = value_sum_ref[...].astype(jnp.bfloat16)


def attention_backward(
    state_rows, weight, weight_start, raw, mixed, totals, tables, query_gain, key_gain, heads, grouping
):
    total_rows, depth = state_rows.shape
    head_size = query_gain.shape[0]
    sequences = total_rows // SEQUENCE_LENGTH
    width = (grouping + 2) * head_size
    out_width = grouping * head_size
    block = min(256, SEQUENCE_LENGTH)
    first_block = weight_start // out_width
    table = pl.BlockSpec(tables[0].shape, lambda s, h: (0, 0))
    gain = pl.BlockSpec((1, head_size), lambda s, h: (0, 0))
    elements = heads * grouping * total_rows * SEQUENCE_LENGTH // 2
    whole_rows = pltpu.VMEM((SEQUENCE_LENGTH, head_size), jnp.float32)
    return pl.pallas_call(
        functools.partial(attention_backward_kernel, grouping, head_size, block),
        grid=(sequences, heads),
        out_shape=[
            jax.ShapeDtypeStruct((total_rows, heads * width), jnp.bfloat16),
            jax.ShapeDtypeStruct((8, head_size), jnp.float32),
        ],
        in_specs=[
            pl.BlockSpec((SEQUENCE_LENGTH, depth), lambda s, h: (s, 0)),
            pl.BlockSpec((depth, out_width), lambda s, h: (0, first_block + h)),
            pl.BlockSpec((SEQUENCE_LENGTH, width), lambda s, h: (s, h)),
            pl.BlockSpec((SEQUENCE_LENGTH, out_width), lambda s, h: (s, h)),
            pl.BlockSpec((1, grouping, SEQUENCE_LENGTH), lambda s, h: (h, 0, s)),
            table,
            table,
            gain,
            gain,
        ],
        out_specs=[
            pl.BlockSpec((SEQUENCE_LENGTH, width), lambda s, h: (s, h)),
            pl.BlockSpec((8, head_size), lambda s, h: (0, 0)),
        ],
        scratch_shapes=[
            pltpu.VMEM((grouping, SEQUENCE_LENGTH, head_size), jnp.bfloat16),
            pltpu.VMEM((SEQUENCE_LENGTH, head_size), jnp.bfloat16),
            pltpu.VMEM((SEQUENCE_LENGTH, head_size), jnp.bfloat16),
            pltpu.VMEM((SEQUENCE_LENGTH, out_width), jnp.bfloat16),
            whole_rows,
            whole_rows,
            whole_rows,
            whole_rows,
            whole_rows,
        ],
        compiler_params=pltpu.CompilerParams(vmem_limit_bytes=VMEM_LIMIT),
        cost_estimate=pl.CostEstimate(
            flops=2 * total_rows * depth * heads * out_width + 10 * elements * head_size,
            bytes_accessed=2 * (total_rows * depth + depth * heads * out_width),
            transcendentals=elements,
        ),
        name="attention_backward",
    )(
        state_rows, weight, raw, mixed, totals, *tables,
        query_gain.reshape(1, -1), key_gain.reshape(1, -1),
    )


def feed_half_kernel(half, tile, rows_ref, cotangent_ref, weight_ref, hidden_ref, slope_ref):
    rows, cotangent = rows_ref[...], cotangent_ref[...]

    def step(index, carry):
        start = pl.multiple_of(index * tile, tile)
        gate = simple_product(rows, weight_ref[:, pl.ds(start, tile)])
        up = simple_product(rows, weight_ref[:, pl.ds(half + start, tile)])
        back = simple_product(cotangent, weight_ref[:, pl.ds(2 * half + start, tile)])
        sigmoid = 1.0 / (1.0 + jnp.exp(-gate))
        gated = gate * sigmoid
        hidden_ref[:, pl.ds(start, tile)] = (gated * up).astype(jnp.bfloat16)
        slope_ref[:, pl.ds(start, tile)] = (
            back * up * sigmoid * (1.0 + gate * (1.0 - sigmoid))
        ).astype(jnp.bfloat16)
        slope_ref[:, pl.ds(half + start, tile)] = (back * gated).astype(jnp.bfloat16)
        return carry

    lax.fori_loop(0, half // tile, step, 0)


def feed_half(rows, cotangent, weight):
    total_rows, depth = rows.shape
    half = weight.shape[1] // 3
    block = min(512, total_rows)
    tile = 256 if half % 256 == 0 else 128
    row_block = pl.BlockSpec((block, depth), lambda i: (i, 0))
    return pl.pallas_call(
        functools.partial(feed_half_kernel, half, tile),
        grid=(total_rows // block,),
        out_shape=[
            jax.ShapeDtypeStruct((total_rows, half), jnp.bfloat16),
            jax.ShapeDtypeStruct((total_rows, 2 * half), jnp.bfloat16),
        ],
        in_specs=[
            row_block,
            row_block,
            pl.BlockSpec(weight.shape, lambda i: (0, 0), pipeline_mode=pl.Buffered(1)),
        ],
        out_specs=[
            pl.BlockSpec((block, half), lambda i: (i, 0)),
            pl.BlockSpec((block, 2 * half), lambda i: (i, 0)),
        ],
        compiler_params=pltpu.CompilerParams(vmem_limit_bytes=VMEM_LIMIT),
        cost_estimate=pl.CostEstimate(
            flops=6 * total_rows * depth * half,
            bytes_accessed=2 * (2 * total_rows * depth + 3 * depth * half),
            transcendentals=total_rows * half,
        ),
        name="feed_half",
    )(rows, cotangent, weight)


def grad_kernel(pair_count, with_other, order_ref, *refs):
    pairs = [refs[2 * p : 2 * p + 2] for p in range(pair_count)]
    refs = refs[2 * pair_count :]
    step = pl.program_id(0)
    if with_other:
        other_ref, refs = refs[0], refs[1:]
        out_refs, held_ref, copy_sem = refs[:-3], refs[-3], refs[-2]
    else:
        out_ref = refs[0]
    turned_ref = refs[-1]
    start = 0
    for left_ref, right_ref in pairs:
        turned_ref[...] = left_ref[...].T
        width = right_ref.shape[1]
        tile = next(t for t in (768, 512, 384, 256, 128) if width % t == 0)
        for column in range(0, width, tile):
            values = simple_product(turned_ref[...], right_ref[:, column : column + tile])
            columns = slice(start + column, start + column + tile)
            if with_other:
                values = values + other_ref[0, :, columns].astype(jnp.float32)
                held_ref[step, :, columns] = values.astype(jnp.bfloat16)
            else:
                out_ref[0, :, columns] = values.astype(jnp.bfloat16)
        start += width
    if with_other:
        copies = [
            pltpu.make_async_copy(held_ref.at[index], out_ref, copy_sem.at[index])
            for index, out_ref in enumerate(out_refs)
        ]
        for index, copy in enumerate(copies):
            pl.when(step == index)(copy.start)

        @pl.when(step == len(copies) - 1)
        def _():
            for copy in copies:
                copy.wait()


def grad_blocks(order, pairs, other=None):
    count = order.shape[0]
    total_rows, depth = pairs[0][0].shape
    block = depth // lax.axis_size("dp")
    width = sum(right.shape[1] for _, right in pairs)
    in_specs = []
    operands = []
    for left, right in pairs:
        in_specs += [
            pl.BlockSpec((total_rows, block), lambda k, at: (0, at[k])),
            pl.BlockSpec(right.shape, lambda k, at: (0, 0), pipeline_mode=pl.Buffered(1)),
        ]
        operands += [left, right]
    scratch = [pltpu.VMEM((block, total_rows), jnp.bfloat16)]
    if other is not None:
        in_specs.append(pl.BlockSpec((1, block, width), lambda k, at: (k, 0, 0)))
        operands.append(other)
        out_shape = [jax.ShapeDtypeStruct((block, width), jnp.bfloat16)] * count
        out_specs = [pl.BlockSpec(memory_space=pl.ANY)] * count
        scratch = [
            pltpu.VMEM((count, block, width), jnp.bfloat16),
            pltpu.SemaphoreType.DMA((count,)),
        ] + scratch
    else:
        out_shape = [jax.ShapeDtypeStruct((count, block, width), jnp.bfloat16)]
        out_specs = [pl.BlockSpec((1, block, width), lambda k, at: (k, 0, 0))]
    out = pl.pallas_call(
        functools.partial(grad_kernel, len(pairs), other is not None),
        grid_spec=pltpu.PrefetchScalarGridSpec(
            num_scalar_prefetch=1,
            grid=(count,),
            in_specs=in_specs,
            out_specs=out_specs,
            scratch_shapes=scratch,
        ),
        out_shape=out_shape,
        compiler_params=pltpu.CompilerParams(vmem_limit_bytes=VMEM_LIMIT),
        cost_estimate=pl.CostEstimate(
            flops=2 * total_rows * count * block * width,
            bytes_accessed=2 * (total_rows * count * block * len(pairs) + width * (total_rows + count * block)),
            transcendentals=0,
        ),
        name="grad_blocks",
    )(order, *operands)
    return out if other is not None else out[0]


def reduce_over_chips(pairs, sizes):
    data_size = sizes[0]
    chips = data_size // 2
    me = lax.axis_index("dp")
    chip, core = me // 2, lax.rem(me, 2)
    ahead = lax.rem(chip + jnp.arange(chips, dtype=jnp.int32), chips) * 2
    other = lax.ppermute(
        grad_blocks(ahead + (1 - core), pairs),
        "dp",
        [(device, device ^ 1) for device in range(data_size)],
    )
    blocks = grad_blocks(ahead + core, pairs, other)
    arrivals = []
    for step in range(1, chips):
        arrivals.append(
            lax.ppermute(
                blocks[step],
                "dp",
                [(device, (device + 2 * step) % data_size) for device in range(data_size)],
            )
        )
    return blocks, arrivals


def pack_mixing_kernel(heads, query_ref, key_ref, value_ref, output_ref, out_ref):
    query_width = query_ref.shape[1] // heads
    head_size = key_ref.shape[1] // heads
    start = 0
    for head in range(heads):
        for ref, part in ((query_ref, query_width), (key_ref, head_size), (value_ref, head_size)):
            out_ref[:, start : start + part] = ref[:, head * part : (head + 1) * part]
            start += part
    out_ref[:, start:] = output_ref[...].T


def pack_feed_kernel(gate_ref, up_ref, down_ref, first_ref, second_ref):
    half = gate_ref.shape[1] // 2
    for index, out_ref in enumerate((first_ref, second_ref)):
        part = slice(index * half, (index + 1) * half)
        out_ref[:, :half] = gate_ref[:, part]
        out_ref[:, half : 2 * half] = up_ref[:, part]
        out_ref[:, 2 * half :] = down_ref[part, :].T


def finish_mixing_kernel(heads, total_ref, query_ref, key_ref, value_ref, output_ref):
    query_width = query_ref.shape[1] // heads
    head_size = key_ref.shape[1] // heads
    start = 0
    for head in range(heads):
        for ref, part in ((query_ref, query_width), (key_ref, head_size), (value_ref, head_size)):
            ref[:, head * part : (head + 1) * part] = total_ref[:, start : start + part].astype(
                jnp.float32
            )
            start += part
    output_ref[...] = total_ref[:, start:].astype(jnp.float32).T


def finish_feed_kernel(*refs):
    first_refs, second_ref = refs[:-4], refs[-4]
    gate_ref, up_ref, down_ref = refs[-3:]
    half = gate_ref.shape[1] // 2

    def first_part(columns):
        return sum(ref[:, columns].astype(jnp.float32) for ref in first_refs)

    def second_part(columns):
        return second_ref[:, columns].astype(jnp.float32)

    for index, part_of in enumerate((first_part, second_part)):
        part = slice(index * half, (index + 1) * half)
        gate_ref[:, part] = part_of(slice(0, half))
        up_ref[:, part] = part_of(slice(half, 2 * half))
        down_ref[part, :] = part_of(slice(2 * half, 3 * half)).T


def whole_call(body, shapes, *operands):
    return pl.pallas_call(
        body,
        out_shape=shapes,
        in_specs=[pl.BlockSpec(memory_space=pltpu.VMEM)] * len(operands),
        out_specs=[pl.BlockSpec(memory_space=pltpu.VMEM)] * len(shapes),
        compiler_params=pltpu.CompilerParams(vmem_limit_bytes=VMEM_LIMIT),
        cost_estimate=pl.CostEstimate(
            flops=0, bytes_accessed=4 * sum(operand.size for operand in operands), transcendentals=0
        ),
    )(*operands)


def per_device(
    block_input,
    attention_gain,
    query_weight,
    key_matrix,
    value_matrix,
    query_gain,
    key_gain,
    output_weight,
    feed_gain,
    gate_weight,
    up_weight,
    down_weight,
    out_cotangent,
):
    size = lax.axis_size("tensor")
    sizes = (lax.axis_size("dp"), size)
    model_width = block_input.shape[1]
    head_size = query_gain.shape[0]
    query_columns = query_weight.shape[1]
    key_columns = key_matrix.shape[1]
    heads = key_columns // head_size
    grouping = query_columns // key_columns
    hidden_columns = gate_weight.shape[1]
    qkv_columns = query_columns + 2 * key_columns
    half = hidden_columns // 2
    tables = turn_tables(head_size)

    block_width = query_weight.shape[0]
    (mixing_local,) = whole_call(
        functools.partial(pack_mixing_kernel, heads),
        [jax.ShapeDtypeStruct((block_width, qkv_columns + query_columns), jnp.bfloat16)],
        query_weight, key_matrix, value_matrix, output_weight,
    )
    mixing_full = lax.all_gather(mixing_local, "dp", axis=0, tiled=True)
    feed_locals = whole_call(
        pack_feed_kernel,
        [jax.ShapeDtypeStruct((block_width, 3 * half), jnp.bfloat16)] * 2,
        gate_weight, up_weight, down_weight,
    )
    feed_full = [lax.all_gather(part, "dp", axis=0, tiled=True) for part in feed_locals]

    input_float = block_input.astype(jnp.float32)
    first_scale = row_scale(input_float)
    first_unit = input_float * first_scale
    mixer_local = (first_unit * attention_gain).astype(jnp.bfloat16)
    mixer_rows, cotangent_rows = gather_rows((mixer_local, out_cotangent), size, 0)

    raw, mixed_rows, totals = attention_forward(
        mixer_rows, mixing_full, tables, query_gain, key_gain, heads, grouping
    )
    hidden_state = input_float + product_scatter(
        [(mixed_rows, mixing_full, qkv_columns)], sizes, 1
    )
    second_scale = row_scale(hidden_state)
    second_unit = hidden_state * second_scale
    feed_local = (second_unit * feed_gain).astype(jnp.bfloat16)
    (feed_rows,) = gather_rows((feed_local,), size, 2)

    hidden_first, slope_first = feed_half(feed_rows, cotangent_rows, feed_full[0])
    blocks, arrivals = reduce_over_chips(
        [(feed_rows, slope_first), (cotangent_rows, hidden_first)], sizes
    )
    blocks, later_full = lax.optimization_barrier((blocks, feed_full[1]))
    hidden_second, slope_second = feed_half(feed_rows, cotangent_rows, later_full)
    plain_order = jnp.arange(sizes[0], dtype=jnp.int32)
    second_grad = grad_blocks(
        plain_order, [(feed_rows, slope_second), (cotangent_rows, hidden_second)]
    ).reshape(model_width, -1)
    second_grad, slope_second = lax.optimization_barrier((second_grad, slope_second))
    second_total = lax.psum_scatter(second_grad, "dp", scatter_dimension=0, tiled=True)
    feed_back = product_scatter(
        [(slope_first, feed_full[0], 0), (slope_second, later_full, 0)], sizes, 3
    )
    feed_gain_term = jnp.sum(feed_back * second_unit, axis=0)
    feed_unit_slope = feed_back * feed_gain
    state_slope = out_cotangent.astype(jnp.float32) + second_scale * (
        feed_unit_slope
        - second_unit * jnp.mean(feed_unit_slope * second_unit, axis=-1, keepdims=True)
    )
    (state_rows,) = gather_rows((state_slope.astype(jnp.bfloat16),), size, 4)
    qkv_slope, head_terms = attention_backward(
        state_rows, mixing_full, qkv_columns, raw, mixed_rows, totals, tables,
        query_gain, key_gain, heads, grouping,
    )
    mixing_grad = grad_blocks(
        plain_order, [(mixer_rows, qkv_slope), (state_rows, mixed_rows)]
    ).reshape(model_width, -1)
    mixing_grad, qkv_slope = lax.optimization_barrier((mixing_grad, qkv_slope))
    mixing_total = lax.psum_scatter(mixing_grad, "dp", scatter_dimension=0, tiled=True)
    mixer_back = product_scatter([(qkv_slope, mixing_full, 0)], sizes, 5)
    attention_gain_term = jnp.sum(mixer_back * first_unit, axis=0)
    mixer_unit_slope = mixer_back * attention_gain
    input_gradient = (
        state_slope
        + first_scale
        * (
            mixer_unit_slope
            - first_unit * jnp.mean(mixer_unit_slope * first_unit, axis=-1, keepdims=True)
        )
    ).astype(jnp.bfloat16)
    gain_rows = model_width // head_size
    terms = jnp.concatenate(
        [
            attention_gain_term.reshape(gain_rows, head_size),
            feed_gain_term.reshape(gain_rows, head_size),
            head_terms,
        ],
        axis=0,
    )
    feed_sum, terms = product_scatter(
        [(hidden_first, feed_full[0], 2 * half), (hidden_second, later_full, 2 * half)],
        sizes,
        6,
        terms,
    )
    block_output = (hidden_state + feed_sum).astype(jnp.bfloat16)
    query_gradient, key_gradient, value_gradient, output_gradient = whole_call(
        functools.partial(finish_mixing_kernel, heads),
        [
            jax.ShapeDtypeStruct((block_width, query_columns), jnp.float32),
            jax.ShapeDtypeStruct((block_width, key_columns), jnp.float32),
            jax.ShapeDtypeStruct((block_width, key_columns), jnp.float32),
            jax.ShapeDtypeStruct((query_columns, block_width), jnp.float32),
        ],
        mixing_total,
    )
    gate_gradient, up_gradient, down_gradient = whole_call(
        finish_feed_kernel,
        [
            jax.ShapeDtypeStruct((block_width, hidden_columns), jnp.float32),
            jax.ShapeDtypeStruct((block_width, hidden_columns), jnp.float32),
            jax.ShapeDtypeStruct((hidden_columns, block_width), jnp.float32),
        ],
        blocks[0], *arrivals, second_total,
    )
    return (
        block_output,
        input_gradient,
        terms[:gain_rows].reshape(-1),
        query_gradient,
        key_gradient,
        value_gradient,
        terms[2 * gain_rows],
        terms[2 * gain_rows + 1],
        output_gradient,
        terms[gain_rows : 2 * gain_rows].reshape(-1),
        gate_gradient,
        up_gradient,
        down_gradient,
    )


def solution(mesh):
    in_specs = (
        P(("dp", "tensor"), None),
        P(),
        P("dp", "tensor"),
        P("dp", "tensor"),
        P("dp", "tensor"),
        P(),
        P(),
        P("tensor", "dp"),
        P(),
        P("dp", "tensor"),
        P("dp", "tensor"),
        P("tensor", "dp"),
        P(("dp", "tensor"), None),
    )
    out_specs = (
        P(("dp", "tensor"), None),
        P(("dp", "tensor"), None),
        P(),
        P("dp", "tensor"),
        P("dp", "tensor"),
        P("dp", "tensor"),
        P(),
        P(),
        P("tensor", "dp"),
        P(),
        P("dp", "tensor"),
        P("dp", "tensor"),
        P("tensor", "dp"),
    )

    return jax.shard_map(
        per_device, mesh=mesh, in_specs=in_specs, out_specs=out_specs, check_vma=False
    )
```

```python
import functools

import jax
import jax.numpy as jnp
import numpy as np
from jax import lax
from jax.experimental import pallas as pl
from jax.experimental.pallas import tpu as pltpu
from jax.sharding import PartitionSpec as P


SEQUENCE_LENGTH = 1024

epsilon = 1e-06
rope_base = 1000000.0


MESH = pl.DeviceIdType.MESH
VMEM_LIMIT = 62 * 1024 * 1024


def row_scale(values):
    return lax.rsqrt(jnp.mean(values * values, axis=-1, keepdims=True) + epsilon)


def times_transposed(first_operand, second_operand):
    return lax.dot_general(
        first_operand, second_operand, (((1,), (1,)), ((), ())), preferred_element_type=jnp.float32
    )


def simple_product(first_operand, second_operand):
    return jnp.dot(first_operand, second_operand, preferred_element_type=jnp.float32)


def remote(source, target, send_sem, recv_sem, peer, axis="tensor"):
    return pltpu.make_async_remote_copy(
        src_ref=source,
        dst_ref=target,
        send_sem=send_sem,
        recv_sem=recv_sem,
        device_id={axis: peer},
        device_id_type=MESH,
    )


def greet(peers):
    barrier = pltpu.get_barrier_semaphore()
    for axis, peer in peers:
        pl.semaphore_signal(barrier, inc=1, device_id={axis: peer}, device_id_type=MESH)
    pl.semaphore_wait(barrier, len(peers))


def square_peers(me):
    column = lax.rem(me, 2)
    row = me // 2
    return row * 2 + (1 - column), (1 - row) * 2 + column, (1 - row) * 2 + (1 - column)


def neighbours(size):
    if size == 4:
        beside, below, _ = square_peers(lax.axis_index("tensor"))
        return [("tensor", beside), ("tensor", below)]
    return [("tensor", peer) for peer in other_members("tensor", size)]


def other_members(axis, count):
    me = lax.axis_index(axis)
    return [lax.rem(me + step, count) for step in range(1, count)]


class Gather:
    def __init__(self, size, own_ref, out_ref, held_ref, send_sem, recv_sem, local_sem):
        self.size, self.own, self.out, self.held = size, own_ref, out_ref, held_ref
        self.send_sem, self.recv_sem, self.local_sem = send_sem, recv_sem, local_sem
        self.me = lax.axis_index("tensor")
        self.rows = own_ref.shape[0]
        self.copies, self.stores = [], []

    @staticmethod
    def scratch(size, rows, columns):
        sends, local = (6, 7) if size == 4 else (size - 1, size)
        return [
            pltpu.VMEM((size, rows, columns), jnp.bfloat16),
            pltpu.SemaphoreType.DMA((sends,)),
            pltpu.SemaphoreType.DMA((sends,)),
            pltpu.SemaphoreType.DMA((local,)),
        ]

    def send(self, source, target, peer):
        index = len(self.copies)
        copy = remote(source, target, self.send_sem.at[index], self.recv_sem.at[index], peer)
        copy.start()
        self.copies.append(copy)
        return copy

    def store(self, source, start, count):
        target = self.out.at[pl.ds(pl.multiple_of(start, count), count)]
        copy = pltpu.make_async_copy(source, target, self.local_sem.at[len(self.stores)])
        copy.start()
        self.stores.append(copy)

    def start(self):
        own, held, rows = self.own, self.held, self.rows
        if self.size != 4:
            for peer in other_members("tensor", self.size):
                self.send(own, held.at[self.me], peer)
            self.store(own, self.me * rows, rows)
            return
        beside, below, _ = square_peers(self.me)
        half = rows // 2
        first, second = pl.ds(0, half), pl.ds(half, half)
        x_first = self.send(own.at[first], held.at[self.me, first], beside)
        y_second = self.send(own.at[second], held.at[self.me, second], below)
        self.send(own.at[second], held.at[self.me, second], beside)
        self.send(own.at[first], held.at[self.me, first], below)
        self.store(own, self.me * rows, rows)
        x_first.wait_recv()
        self.send(held.at[beside, first], held.at[beside, first], below)
        y_second.wait_recv()
        self.send(held.at[below, second], held.at[below, second], beside)
        self.store(held.at[beside, first], beside * rows, half)
        self.store(held.at[below, second], below * rows + half, half)

    def finish(self):
        held, rows = self.held, self.rows
        if self.size != 4:
            for step, copy in enumerate(self.copies):
                copy.wait_recv()
                slot = lax.rem(self.me + self.size - step - 1, self.size)
                self.store(held.at[slot], slot * rows, rows)
        else:
            beside, below, across = square_peers(self.me)
            half = rows // 2
            first, second = pl.ds(0, half), pl.ds(half, half)
            x_second, y_first, y_pass, x_pass = self.copies[2:]
            x_second.wait_recv()
            self.store(held.at[beside, second], beside * rows + half, half)
            y_first.wait_recv()
            self.store(held.at[below, first], below * rows, half)
            y_pass.wait_recv()
            self.store(held.at[across, first], across * rows, half)
            x_pass.wait_recv()
            self.store(held.at[across, second], across * rows + half, half)
        for copy in self.copies:
            copy.wait_send()
        for copy in self.stores:
            copy.wait()


def gather_kernel(size, count, *refs):
    own_refs, out_refs, rest = refs[:count], refs[count : 2 * count], refs[2 * count :]
    greet(neighbours(size))
    gathers = [
        Gather(size, own_refs[k], out_refs[k], *rest[4 * k : 4 * k + 4]) for k in range(count)
    ]
    for gather in gathers:
        gather.start()
    for gather in gathers:
        gather.finish()


def gather_rows(arrays, size, collective_id):
    count = len(arrays)
    rows, columns = arrays[0].shape
    scratch = []
    for _ in arrays:
        scratch += Gather.scratch(size, rows, columns)
    return pl.pallas_call(
        functools.partial(gather_kernel, size, count),
        out_shape=[jax.ShapeDtypeStruct((size * rows, columns), a.dtype) for a in arrays],
        in_specs=[pl.BlockSpec(memory_space=pltpu.VMEM)] * count,
        out_specs=[pl.BlockSpec(memory_space=pl.ANY)] * count,
        scratch_shapes=scratch,
        compiler_params=pltpu.CompilerParams(
            collective_id=collective_id, has_side_effects=True, vmem_limit_bytes=VMEM_LIMIT
        ),
        cost_estimate=pl.CostEstimate(
            flops=0, bytes_accessed=count * 30 * size * rows * columns, transcendentals=0
        ),
        name="gather_rows",
    )(*arrays)


def block_product(pairs, start, rows, write):
    total = pairs[0][1].shape[0]
    tile = min(512, total)
    start = pl.multiple_of(start, rows)

    def step(index, carry):
        columns = pl.ds(pl.multiple_of(index * tile, tile), tile)
        values = None
        for left_ref, weight_ref in pairs:
            part = times_transposed(left_ref[pl.ds(start, rows), :], weight_ref[columns, :])
            values = part if values is None else values + part
        write(columns, values)
        return carry

    lax.fori_loop(0, total // tile, step, 0)


class Scatter:
    def __init__(self, size, outgoing, *rest):
        self.size, self.outgoing = size, outgoing
        if size == 4:
            self.passing, rest = rest[0], rest[1:]
        self.arriving, self.send_sem, self.recv_sem = rest
        self.rows = outgoing.shape[1]
        self.me = lax.axis_index("tensor")

    @staticmethod
    def scratch(size, rows, columns):
        if size == 4:
            sends = 6
            buffers = [
                pltpu.VMEM((4, rows, columns), jnp.bfloat16),
                pltpu.VMEM((2, rows // 2, columns), jnp.bfloat16),
                pltpu.VMEM((2, rows, columns), jnp.bfloat16),
            ]
        else:
            sends = size - 1
            buffers = [
                pltpu.VMEM((size, rows, columns), jnp.bfloat16),
                pltpu.VMEM((size - 1, rows, columns), jnp.bfloat16),
            ]
        return buffers + [pltpu.SemaphoreType.DMA((sends,)), pltpu.SemaphoreType.DMA((sends,))]

    def prepare(self, index, source, target, peer):
        return remote(source, target, self.send_sem.at[index], self.recv_sem.at[index], peer)

    def fill(self, pairs):
        size, me, outgoing, arriving, rows = self.size, self.me, self.outgoing, self.arriving, self.rows
        if size == 4:
            beside, below, across = square_peers(me)
            half = rows // 2
            first, second = pl.ds(0, half), pl.ds(half, half)
            self.copies = [
                self.prepare(0, outgoing.at[0, first], self.passing.at[0], beside),
                self.prepare(1, outgoing.at[0, second], self.passing.at[1], below),
                self.prepare(2, outgoing.at[1, first], arriving.at[0, first], beside),
                self.prepare(3, outgoing.at[2, second], arriving.at[1, second], below),
                self.prepare(4, outgoing.at[1, second], arriving.at[0, second], beside),
                self.prepare(5, outgoing.at[2, first], arriving.at[1, first], below),
            ]
            starts = ((0, 0), (0, 1), (1, 2), (2, 3))
        else:
            self.copies = [
                self.prepare(step, outgoing.at[step], arriving.at[step], peer)
                for step, peer in enumerate(other_members("tensor", size))
            ]
            starts = tuple((step, step) for step in range(size - 1))

        def step(slot, carry):
            if size == 4:
                owner = jnp.where(
                    slot == 0, across, jnp.where(slot == 1, beside, jnp.where(slot == 2, below, me))
                )
            else:
                owner = lax.rem(me + slot + 1, size)

            def write(columns, values):
                outgoing[slot, :, columns] = values.astype(outgoing.dtype)

            block_product(pairs, owner * rows, rows, write)
            for at, index in starts:
                pl.when(slot == at)(self.copies[index].start)
            return carry

        lax.fori_loop(0, size, step, 0)

    def relay(self):
        if self.size != 4:
            return
        half = self.rows // 2
        x_pass, y_pass, _, _, x_second, y_first = self.copies
        for arrival, source, slot, start, onward in (
            (y_pass, 1, 1, half, x_second),
            (x_pass, 0, 2, 0, y_first),
        ):
            arrival.wait_recv()
            piece = pl.ds(start, half)
            self.outgoing[slot, piece, :] = (
                self.outgoing[slot, piece, :].astype(jnp.float32)
                + self.passing[source].astype(jnp.float32)
            ).astype(self.outgoing.dtype)
            onward.start()

    def collect(self):
        for copy in self.copies[2:] if self.size == 4 else self.copies:
            copy.wait_recv()

    def total(self, piece):
        total = self.outgoing[self.size - 1, piece, :].astype(jnp.float32)
        for index in range(self.arriving.shape[0]):
            total = total + self.arriving[index, piece, :].astype(jnp.float32)
        return total

    def drain(self):
        for copy in self.copies:
            copy.wait_send()


def over_pieces(rows, body):
    count = min(32, rows)

    def step(index, carry):
        body(pl.ds(pl.multiple_of(index * count, count), count))
        return carry

    lax.fori_loop(0, rows // count, step, 0)


def send_terms(axis, peers, source, landing, send_sem, recv_sem):
    me = lax.axis_index(axis)
    landing[me] = source[...]
    copies = []
    for step, peer in enumerate(peers):
        copy = remote(source, landing.at[me], send_sem.at[step], recv_sem.at[step], peer, axis)
        copy.start()
        copies.append(copy)
    return copies


def add_terms(landing, copies):
    for copy in copies:
        copy.wait_recv()
    total = landing[0]
    for index in range(1, landing.shape[0]):
        total = total + landing[index]
    return total


def split_pairs(refs, count):
    return [refs[2 * p : 2 * p + 2] for p in range(count)], refs[2 * count :]


def store_row(target_ref, row_ref):
    width = target_ref.shape[1]
    for index in range(row_ref.shape[1] // width):
        target_ref[index : index + 1, :] = row_ref[:, index * width : (index + 1) * width]


def between_forward_kernel(size, pair_count, *refs):
    pairs, refs = split_pairs(refs, pair_count)
    input_ref, gain_ref, gathered_ref, state_ref, own_ref = refs[:5]
    buffers = 5 if size == 4 else 4
    scatter = Scatter(size, *refs[5 : 5 + buffers])
    gather = Gather(size, own_ref, gathered_ref, *refs[5 + buffers :])
    greet(neighbours(size))
    scatter.fill(pairs)
    scatter.relay()
    scatter.collect()

    def norm(piece):
        state = input_ref[piece, :].astype(jnp.float32) + scatter.total(piece)
        state_ref[piece, :] = state
        own_ref[piece, :] = (state * row_scale(state) * gain_ref[...]).astype(own_ref.dtype)

    over_pieces(own_ref.shape[0], norm)
    gather.start()
    gather.finish()
    scatter.drain()


def between_backward_kernel(size, pair_count, *refs):
    pairs, refs = split_pairs(refs, pair_count)
    state_ref, cotangent_ref, gain_ref, gathered_ref, slope_ref, term_ref, own_ref, sum_ref = refs[:8]
    buffers = 5 if size == 4 else 4
    scatter = Scatter(size, *refs[8 : 8 + buffers])
    gather = Gather(size, own_ref, gathered_ref, *refs[8 + buffers :])
    greet(neighbours(size))
    scatter.fill(pairs)
    scatter.relay()
    sum_ref[...] = jnp.zeros_like(sum_ref)
    scatter.collect()

    def norm(piece):
        back = scatter.total(piece)
        state = state_ref[piece, :]
        scale = row_scale(state)
        unit = state * scale
        sum_ref[...] += jnp.sum(back * unit, axis=0, keepdims=True)
        unit_slope = back * gain_ref[...]
        slope = cotangent_ref[piece, :].astype(jnp.float32) + scale * (
            unit_slope - unit * jnp.mean(unit_slope * unit, axis=-1, keepdims=True)
        )
        slope_ref[piece, :] = slope
        own_ref[piece, :] = slope.astype(own_ref.dtype)

    over_pieces(own_ref.shape[0], norm)
    gather.start()
    store_row(term_ref, sum_ref)
    gather.finish()
    scatter.drain()


def last_kernel(sizes, pair_counts, *refs):
    data_size, size = sizes
    mixing_pairs, refs = split_pairs(refs, pair_counts[0])
    feed_pairs, refs = split_pairs(refs, pair_counts[1])
    input_ref, gain_ref, slope_ref, state_ref, terms_ref = refs[:5]
    output_ref, gradient_ref, terms_out_ref, sum_ref, partial_ref, inner, outer = refs[5:12]
    inner_send, inner_recv, outer_send, outer_recv = refs[12:16]
    buffers = 5 if size == 4 else 4
    mixing = Scatter(size, *refs[16 : 16 + buffers])
    feed = Scatter(size, *refs[16 + buffers :])
    greet(
        [("tensor", peer) for peer in other_members("tensor", size)]
        + [("dp", peer) for peer in other_members("dp", data_size)]
    )
    mixing.fill(mixing_pairs)
    feed.fill(feed_pairs)
    mixing.relay()
    sum_ref[...] = jnp.zeros_like(sum_ref)
    feed.relay()
    mixing.collect()

    def norm(piece):
        back = mixing.total(piece)
        values = input_ref[piece, :].astype(jnp.float32)
        scale = row_scale(values)
        unit = values * scale
        sum_ref[...] += jnp.sum(back * unit, axis=0, keepdims=True)
        unit_slope = back * gain_ref[...]
        gradient_ref[piece, :] = (
            slope_ref[piece, :]
            + scale * (unit_slope - unit * jnp.mean(unit_slope * unit, axis=-1, keepdims=True))
        ).astype(gradient_ref.dtype)

    over_pieces(output_ref.shape[0], norm)
    kept = partial_ref.shape[0] - terms_ref.shape[0]
    partial_ref[kept:, :] = terms_ref[...]
    store_row(partial_ref, sum_ref)
    inner_copies = send_terms(
        "tensor", other_members("tensor", size), partial_ref, inner, inner_send, inner_recv
    )
    terms_out_ref[...] = add_terms(inner, inner_copies)
    outer_copies = send_terms(
        "dp", other_members("dp", data_size), terms_out_ref, outer, outer_send, outer_recv
    )
    feed.collect()

    def finish(piece):
        output_ref[piece, :] = (state_ref[piece, :] + feed.total(piece)).astype(output_ref.dtype)

    over_pieces(output_ref.shape[0], finish)
    total = add_terms(outer, outer_copies)
    for copy in outer_copies:
        copy.wait_send()
    terms_out_ref[...] = total
    for copy in inner_copies:
        copy.wait_send()
    mixing.drain()
    feed.drain()


def scatter_call(body, triple_lists, others, outs, gathered, scratch, collective_id):
    in_specs = []
    operands = []
    flops = 0
    for left, weight, first_column in (triple for triples in triple_lists for triple in triples):
        part = left.shape[1]
        flops += 2 * left.size * weight.shape[0]
        in_specs += [
            pl.BlockSpec(left.shape, lambda i: (0, 0), pipeline_mode=pl.Buffered(1)),
            pl.BlockSpec(
                (weight.shape[0], part),
                lambda i, block=first_column // part: (0, block),
                pipeline_mode=pl.Buffered(1),
            ),
        ]
        operands += [left, weight]
    for other in others:
        in_specs.append(pl.BlockSpec(other.shape, lambda i: (0, 0), pipeline_mode=pl.Buffered(1)))
        operands.append(other)
    out_specs = [pl.BlockSpec(out.shape, lambda i: (0, 0)) for out in outs]
    if gathered:
        out_specs[0] = pl.BlockSpec(memory_space=pl.ANY)
    return pl.pallas_call(
        body,
        grid=(1,),
        out_shape=outs,
        in_specs=in_specs,
        out_specs=out_specs,
        scratch_shapes=scratch,
        compiler_params=pltpu.CompilerParams(
            collective_id=collective_id, has_side_effects=True, vmem_limit_bytes=VMEM_LIMIT
        ),
        cost_estimate=pl.CostEstimate(
            flops=flops, bytes_accessed=150_000_000, transcendentals=0
        ),
    )(*operands)


LOG2E = 1.4426950408889634


def turn_tables(head_size):
    half_size = head_size // 2
    frequency = np.float32(rope_base) ** (
        -(np.arange(half_size, dtype=np.float32) * np.float32(2.0) / np.float32(head_size))
    )
    frequency = frequency.astype(np.float64)
    sign = np.concatenate([-np.ones(half_size), np.ones(half_size)])[None, :]
    positions = np.concatenate([np.arange(0, SEQUENCE_LENGTH, 128), np.arange(128)])
    angles = positions[:, None] * np.concatenate([frequency, frequency])[None, :]
    return np.cos(angles).astype(np.float32), (sign * np.sin(angles)).astype(np.float32)


def fill_tables(few_cosines_ref, few_sines_ref, cosine_ref, sine_ref):
    coarse = few_cosines_ref.shape[0] - 128
    near_cosine, near_sine = few_cosines_ref[coarse:, :], few_sines_ref[coarse:, :]

    def step(index, carry):
        far_cosine = few_cosines_ref[pl.ds(index, 1), :]
        far_sine = few_sines_ref[pl.ds(index, 1), :]
        rows = pl.ds(pl.multiple_of(index * 128, 128), 128)
        cosine_ref[rows, :] = far_cosine * near_cosine - far_sine * near_sine
        sine_ref[rows, :] = far_sine * near_cosine + far_cosine * near_sine
        return carry

    lax.fori_loop(0, coarse, step, 0)


def turn(values, cosine, sine):
    return values * cosine + pltpu.roll(values, values.shape[-1] // 2, 1) * sine


def turn_back(values, cosine, sine):
    return values * cosine - pltpu.roll(values, values.shape[-1] // 2, 1) * sine


def contract_first(first_operand, second_operand):
    return lax.dot_general(
        first_operand, second_operand, (((0,), (0,)), ((), ())), preferred_element_type=jnp.float32
    )


def visible_scores(key_rows, query_rows, first_row, multiplier):
    scores = times_transposed(key_rows, query_rows) * multiplier
    _, queries = scores.shape
    key_at = lax.broadcasted_iota(jnp.int32, (queries, queries), 0)
    query_at = lax.broadcasted_iota(jnp.int32, (queries, queries), 1)
    corner = jnp.where(query_at >= key_at, scores[first_row:], -1e30)
    if first_row == 0:
        return corner
    return jnp.concatenate([scores[:first_row], corner], axis=0)


def turn_heads(
    grouping, head_size, raw_ref, query_gain_ref, key_gain_ref, cosine_ref, sine_ref, query_ref, key_ref, value_ref
):
    def turned(start, gain):
        raw = raw_ref[:, pl.ds(start, head_size)]
        return turn(raw * row_scale(raw) * gain, cosine_ref[...], sine_ref[...]).astype(jnp.bfloat16)

    def step(part, carry):
        query_ref[part] = turned(pl.multiple_of(part * head_size, head_size), query_gain_ref[...])
        return carry

    lax.fori_loop(0, grouping, step, 0)
    key_ref[...] = turned(grouping * head_size, key_gain_ref[...])
    value_ref[...] = raw_ref[:, (grouping + 1) * head_size :].astype(jnp.bfloat16)


def attention_forward_kernel(
    grouping, head_size, block, rows_ref, weight_ref, few_cosines_ref, few_sines_ref, query_gain_ref, key_gain_ref,
    raw_ref, mixed_ref, total_ref, query_ref, key_ref, value_ref, cosine_ref, sine_ref,
):
    sequence = rows_ref.shape[0]
    multiplier = head_size ** (-0.5) * LOG2E

    @pl.when((pl.program_id(0) == 0) & (pl.program_id(1) == 0))
    def _():
        fill_tables(few_cosines_ref, few_sines_ref, cosine_ref, sine_ref)

    raw_ref[...] = simple_product(rows_ref[...], weight_ref[...])
    turn_heads(
        grouping, head_size, raw_ref, query_gain_ref, key_gain_ref, cosine_ref, sine_ref, query_ref, key_ref, value_ref
    )

    def head_step(part, carry):
        lanes = pl.ds(pl.multiple_of(part * head_size, head_size), head_size)
        for first_row in range(0, sequence, block):
            last_row = first_row + block
            scores = visible_scores(
                key_ref[:last_row, :], query_ref[part, first_row:last_row, :], first_row, multiplier
            )
            highest = jnp.max(scores, axis=0, keepdims=True)
            weights = jnp.exp2(scores - highest)
            total = jnp.sum(weights, axis=0, keepdims=True)
            weights = (weights * (1.0 / total)).astype(jnp.bfloat16)
            mixed_ref[first_row:last_row, lanes] = contract_first(
                weights, value_ref[:last_row, :]
            ).astype(mixed_ref.dtype)
            total_ref[0, pl.ds(part, 1), first_row:last_row] = highest + jnp.log2(total)
        return carry

    lax.fori_loop(0, grouping, head_step, 0)


def attention_forward(rows, weight, tables, query_gain, key_gain, heads, grouping):
    total_rows, depth = rows.shape
    head_size = query_gain.shape[0]
    sequences = total_rows // SEQUENCE_LENGTH
    width = (grouping + 2) * head_size
    block = min(256, SEQUENCE_LENGTH)
    table = pl.BlockSpec(tables[0].shape, lambda s, h: (0, 0))
    gain = pl.BlockSpec((1, head_size), lambda s, h: (0, 0))
    elements = heads * grouping * total_rows * SEQUENCE_LENGTH // 2
    return pl.pallas_call(
        functools.partial(attention_forward_kernel, grouping, head_size, block),
        grid=(sequences, heads),
        out_shape=[
            jax.ShapeDtypeStruct((total_rows, heads * width), jnp.float32),
            jax.ShapeDtypeStruct((total_rows, heads * grouping * head_size), jnp.bfloat16),
            jax.ShapeDtypeStruct((heads, grouping, total_rows), jnp.float32),
        ],
        in_specs=[
            pl.BlockSpec((SEQUENCE_LENGTH, depth), lambda s, h: (s, 0)),
            pl.BlockSpec((depth, width), lambda s, h: (0, h)),
            table,
            table,
            gain,
            gain,
        ],
        out_specs=[
            pl.BlockSpec((SEQUENCE_LENGTH, width), lambda s, h: (s, h)),
            pl.BlockSpec((SEQUENCE_LENGTH, grouping * head_size), lambda s, h: (s, h)),
            pl.BlockSpec((1, grouping, SEQUENCE_LENGTH), lambda s, h: (h, 0, s)),
        ],
        scratch_shapes=[
            pltpu.VMEM((grouping, SEQUENCE_LENGTH, head_size), jnp.bfloat16),
            pltpu.VMEM((SEQUENCE_LENGTH, head_size), jnp.bfloat16),
            pltpu.VMEM((SEQUENCE_LENGTH, head_size), jnp.bfloat16),
            pltpu.VMEM((SEQUENCE_LENGTH, head_size), jnp.float32),
            pltpu.VMEM((SEQUENCE_LENGTH, head_size), jnp.float32),
        ],
        compiler_params=pltpu.CompilerParams(vmem_limit_bytes=VMEM_LIMIT),
        cost_estimate=pl.CostEstimate(
            flops=2 * total_rows * depth * heads * width + 4 * elements * head_size,
            bytes_accessed=2 * (total_rows * depth + depth * heads * width),
            transcendentals=elements,
        ),
        name="attention_forward",
    )(rows, weight, *tables, query_gain.reshape(1, -1), key_gain.reshape(1, -1))


def norm_back(turned_slope, raw, gain, cosine, sine):
    norm_slope = turn_back(turned_slope, cosine, sine)
    scale = row_scale(raw)
    unit = raw * scale
    term = norm_slope * unit
    unit_slope = norm_slope * gain
    slope = scale * (unit_slope - unit * jnp.mean(unit_slope * unit, axis=-1, keepdims=True))
    return slope.astype(jnp.bfloat16), jnp.sum(term, axis=0, keepdims=True)


def attention_backward_kernel(
    grouping, head_size, block, state_ref, weight_ref, raw_ref, mixed_ref, total_ref, few_cosines_ref, few_sines_ref,
    query_gain_ref, key_gain_ref, slope_ref, gain_ref, query_ref, key_ref, value_ref, out_slope_ref,
    turned_ref, key_sum_ref, value_sum_ref, cosine_ref, sine_ref,
):
    sequence = state_ref.shape[0]
    scale_factor = head_size ** (-0.5)
    multiplier = scale_factor * LOG2E

    @pl.when((pl.program_id(0) == 0) & (pl.program_id(1) == 0))
    def _():
        gain_ref[...] = jnp.zeros_like(gain_ref)
        fill_tables(few_cosines_ref, few_sines_ref, cosine_ref, sine_ref)

    out_slope_ref[...] = simple_product(state_ref[...], weight_ref[...]).astype(jnp.bfloat16)
    turn_heads(
        grouping, head_size, raw_ref, query_gain_ref, key_gain_ref, cosine_ref, sine_ref, query_ref, key_ref, value_ref
    )
    key_sum_ref[...] = jnp.zeros_like(key_sum_ref)
    value_sum_ref[...] = jnp.zeros_like(value_sum_ref)
    ones = jnp.ones((8, head_size), jnp.float32)

    def head_step(part, carry):
        lanes = pl.ds(pl.multiple_of(part * head_size, head_size), head_size)
        for first_row in range(0, sequence, block):
            last_row = first_row + block
            query_rows = query_ref[part, first_row:last_row, :]
            slope_rows = out_slope_ref[first_row:last_row, lanes]
            scores = visible_scores(key_ref[:last_row, :], query_rows, first_row, multiplier)
            weights = jnp.exp2(scores - total_ref[0, pl.ds(part, 1), first_row:last_row])
            value_sum_ref[:last_row, :] += simple_product(weights.astype(jnp.bfloat16), slope_rows)
            product = slope_rows.astype(jnp.float32) * mixed_ref[first_row:last_row, lanes].astype(jnp.float32)
            centre = lax.dot_general(
                ones,
                product,
                (((1,), (1,)), ((), ())),
                preferred_element_type=jnp.float32,
                precision=lax.Precision.HIGHEST,
            )[:1]
            weight_slope = times_transposed(value_ref[:last_row, :], slope_rows)
            score_slope = (weights * (weight_slope - centre)).astype(jnp.bfloat16)
            key_sum_ref[:last_row, :] += simple_product(score_slope, query_rows)
            turned_ref[first_row:last_row, :] = (
                contract_first(score_slope, key_ref[:last_row, :]) * scale_factor
            )
        slope, term = norm_back(
            turned_ref[...], raw_ref[:, lanes], query_gain_ref[...], cosine_ref[...], sine_ref[...]
        )
        slope_ref[:, lanes] = slope
        gain_ref[0:1, :] += term
        return carry

    lax.fori_loop(0, grouping, head_step, 0)
    lanes = slice(grouping * head_size, (grouping + 1) * head_size)
    slope, term = norm_back(
        key_sum_ref[...] * scale_factor, raw_ref[:, lanes], key_gain_ref[...], cosine_ref[...], sine_ref[...]
    )
    slope_ref[:, lanes] = slope
    gain_ref[1:2, :] += term
    slope_ref[:, (grouping + 1) * head_size :] = value_sum_ref[...].astype(jnp.bfloat16)


def attention_backward(
    state_rows, weight, weight_start, raw, mixed, totals, tables, query_gain, key_gain, heads, grouping
):
    total_rows, depth = state_rows.shape
    head_size = query_gain.shape[0]
    sequences = total_rows // SEQUENCE_LENGTH
    width = (grouping + 2) * head_size
    out_width = grouping * head_size
    block = min(256, SEQUENCE_LENGTH)
    first_block = weight_start // out_width
    table = pl.BlockSpec(tables[0].shape, lambda s, h: (0, 0))
    gain = pl.BlockSpec((1, head_size), lambda s, h: (0, 0))
    elements = heads * grouping * total_rows * SEQUENCE_LENGTH // 2
    whole_rows = pltpu.VMEM((SEQUENCE_LENGTH, head_size), jnp.float32)
    return pl.pallas_call(
        functools.partial(attention_backward_kernel, grouping, head_size, block),
        grid=(sequences, heads),
        out_shape=[
            jax.ShapeDtypeStruct((total_rows, heads * width), jnp.bfloat16),
            jax.ShapeDtypeStruct((8, head_size), jnp.float32),
        ],
        in_specs=[
            pl.BlockSpec((SEQUENCE_LENGTH, depth), lambda s, h: (s, 0)),
            pl.BlockSpec((depth, out_width), lambda s, h: (0, first_block + h)),
            pl.BlockSpec((SEQUENCE_LENGTH, width), lambda s, h: (s, h)),
            pl.BlockSpec((SEQUENCE_LENGTH, out_width), lambda s, h: (s, h)),
            pl.BlockSpec((1, grouping, SEQUENCE_LENGTH), lambda s, h: (h, 0, s)),
            table,
            table,
            gain,
            gain,
        ],
        out_specs=[
            pl.BlockSpec((SEQUENCE_LENGTH, width), lambda s, h: (s, h)),
            pl.BlockSpec((8, head_size), lambda s, h: (0, 0)),
        ],
        scratch_shapes=[
            pltpu.VMEM((grouping, SEQUENCE_LENGTH, head_size), jnp.bfloat16),
            pltpu.VMEM((SEQUENCE_LENGTH, head_size), jnp.bfloat16),
            pltpu.VMEM((SEQUENCE_LENGTH, head_size), jnp.bfloat16),
            pltpu.VMEM((SEQUENCE_LENGTH, out_width), jnp.bfloat16),
            whole_rows,
            whole_rows,
            whole_rows,
            whole_rows,
            whole_rows,
        ],
        compiler_params=pltpu.CompilerParams(vmem_limit_bytes=VMEM_LIMIT),
        cost_estimate=pl.CostEstimate(
            flops=2 * total_rows * depth * heads * out_width + 10 * elements * head_size,
            bytes_accessed=2 * (total_rows * depth + depth * heads * out_width),
            transcendentals=elements,
        ),
        name="attention_backward",
    )(
        state_rows, weight, raw, mixed, totals, *tables,
        query_gain.reshape(1, -1), key_gain.reshape(1, -1),
    )


def feed_half_kernel(half, tile, rows_ref, cotangent_ref, weight_ref, hidden_ref, slope_ref):
    rows, cotangent = rows_ref[...], cotangent_ref[...]

    def step(index, carry):
        start = pl.multiple_of(index * tile, tile)
        gate = simple_product(rows, weight_ref[:, pl.ds(start, tile)])
        up = simple_product(rows, weight_ref[:, pl.ds(half + start, tile)])
        back = simple_product(cotangent, weight_ref[:, pl.ds(2 * half + start, tile)])
        sigmoid = 1.0 / (1.0 + jnp.exp(-gate))
        gated = gate * sigmoid
        hidden_ref[:, pl.ds(start, tile)] = (gated * up).astype(jnp.bfloat16)
        slope_ref[:, pl.ds(start, tile)] = (
            back * up * sigmoid * (1.0 + gate * (1.0 - sigmoid))
        ).astype(jnp.bfloat16)
        slope_ref[:, pl.ds(half + start, tile)] = (back * gated).astype(jnp.bfloat16)
        return carry

    lax.fori_loop(0, half // tile, step, 0)


def feed_half(rows, cotangent, weight):
    total_rows, depth = rows.shape
    half = weight.shape[1] // 3
    block = min(512, total_rows)
    tile = 256 if half % 256 == 0 else 128
    row_block = pl.BlockSpec((block, depth), lambda i: (i, 0))
    return pl.pallas_call(
        functools.partial(feed_half_kernel, half, tile),
        grid=(total_rows // block,),
        out_shape=[
            jax.ShapeDtypeStruct((total_rows, half), jnp.bfloat16),
            jax.ShapeDtypeStruct((total_rows, 2 * half), jnp.bfloat16),
        ],
        in_specs=[
            row_block,
            row_block,
            pl.BlockSpec(weight.shape, lambda i: (0, 0), pipeline_mode=pl.Buffered(1)),
        ],
        out_specs=[
            pl.BlockSpec((block, half), lambda i: (i, 0)),
            pl.BlockSpec((block, 2 * half), lambda i: (i, 0)),
        ],
        compiler_params=pltpu.CompilerParams(vmem_limit_bytes=VMEM_LIMIT),
        cost_estimate=pl.CostEstimate(
            flops=6 * total_rows * depth * half,
            bytes_accessed=2 * (2 * total_rows * depth + 3 * depth * half),
            transcendentals=total_rows * half,
        ),
        name="feed_half",
    )(rows, cotangent, weight)


def grad_kernel(pair_count, with_other, order_ref, *refs):
    pairs = [refs[2 * p : 2 * p + 2] for p in range(pair_count)]
    refs = refs[2 * pair_count :]
    step = pl.program_id(0)
    if with_other:
        other_ref, refs = refs[0], refs[1:]
        out_refs, held_ref, copy_sem = refs[:-3], refs[-3], refs[-2]
    else:
        out_ref = refs[0]
    turned_ref = refs[-1]
    start = 0
    for left_ref, right_ref in pairs:
        turned_ref[...] = left_ref[...].T
        width = right_ref.shape[1]
        tile = next(t for t in (768, 512, 384, 256, 128) if width % t == 0)
        for column in range(0, width, tile):
            values = simple_product(turned_ref[...], right_ref[:, column : column + tile])
            columns = slice(start + column, start + column + tile)
            if with_other:
                values = values + other_ref[0, :, columns].astype(jnp.float32)
                held_ref[step, :, columns] = values.astype(jnp.bfloat16)
            else:
                out_ref[0, :, columns] = values.astype(jnp.bfloat16)
        start += width
    if with_other:
        copies = [
            pltpu.make_async_copy(held_ref.at[index], out_ref, copy_sem.at[index])
            for index, out_ref in enumerate(out_refs)
        ]
        for index, copy in enumerate(copies):
            pl.when(step == index)(copy.start)

        @pl.when(step == len(copies) - 1)
        def _():
            for copy in copies:
                copy.wait()


def grad_blocks(order, pairs, other=None):
    count = order.shape[0]
    total_rows, depth = pairs[0][0].shape
    block = depth // lax.axis_size("dp")
    width = sum(right.shape[1] for _, right in pairs)
    in_specs = []
    operands = []
    for left, right in pairs:
        in_specs += [
            pl.BlockSpec((total_rows, block), lambda k, at: (0, at[k])),
            pl.BlockSpec(right.shape, lambda k, at: (0, 0), pipeline_mode=pl.Buffered(1)),
        ]
        operands += [left, right]
    scratch = [pltpu.VMEM((block, total_rows), jnp.bfloat16)]
    if other is not None:
        in_specs.append(pl.BlockSpec((1, block, width), lambda k, at: (k, 0, 0)))
        operands.append(other)
        out_shape = [jax.ShapeDtypeStruct((block, width), jnp.bfloat16)] * count
        out_specs = [pl.BlockSpec(memory_space=pl.ANY)] * count
        scratch = [
            pltpu.VMEM((count, block, width), jnp.bfloat16),
            pltpu.SemaphoreType.DMA((count,)),
        ] + scratch
    else:
        out_shape = [jax.ShapeDtypeStruct((count, block, width), jnp.bfloat16)]
        out_specs = [pl.BlockSpec((1, block, width), lambda k, at: (k, 0, 0))]
    out = pl.pallas_call(
        functools.partial(grad_kernel, len(pairs), other is not None),
        grid_spec=pltpu.PrefetchScalarGridSpec(
            num_scalar_prefetch=1,
            grid=(count,),
            in_specs=in_specs,
            out_specs=out_specs,
            scratch_shapes=scratch,
        ),
        out_shape=out_shape,
        compiler_params=pltpu.CompilerParams(vmem_limit_bytes=VMEM_LIMIT),
        cost_estimate=pl.CostEstimate(
            flops=2 * total_rows * count * block * width,
            bytes_accessed=2 * (total_rows * count * block * len(pairs) + width * (total_rows + count * block)),
            transcendentals=0,
        ),
        name="grad_blocks",
    )(order, *operands)
    return out if other is not None else out[0]


def add_rounded(first, second):
    return (first.astype(jnp.float32) + second.astype(jnp.float32)).astype(jnp.bfloat16)


def reduce_over_chips(pairs, sizes):
    data_size = sizes[0]
    chips = data_size // 2
    me = lax.axis_index("dp")
    chip, core = me // 2, lax.rem(me, 2)
    ahead = lax.rem(chip + jnp.arange(chips, dtype=jnp.int32), chips) * 2
    other = lax.ppermute(
        grad_blocks(ahead + (1 - core), pairs),
        "dp",
        [(device, device ^ 1) for device in range(data_size)],
    )
    blocks = grad_blocks(ahead + core, pairs, other)
    up = down = None
    for step in range(1, chips):
        rising, falling = blocks[chips - step], blocks[step]
        if up is not None:
            rising, falling = add_rounded(rising, up), add_rounded(falling, down)
        up = lax.ppermute(
            rising, "dp", [(device, device + 2) for device in range(2 * step)]
        )
        down = lax.ppermute(
            falling,
            "dp",
            [(device, device - 2) for device in range(data_size - 2 * step, data_size)],
        )
    return blocks, (up, down)


def pack_mixing_kernel(heads, query_ref, key_ref, value_ref, output_ref, out_ref):
    query_width = query_ref.shape[1] // heads
    head_size = key_ref.shape[1] // heads
    start = 0
    for head in range(heads):
        for ref, part in ((query_ref, query_width), (key_ref, head_size), (value_ref, head_size)):
            out_ref[:, start : start + part] = ref[:, head * part : (head + 1) * part]
            start += part
    out_ref[:, start:] = output_ref[...].T


def pack_feed_kernel(gate_ref, up_ref, down_ref, first_ref, second_ref):
    half = gate_ref.shape[1] // 2
    for index, out_ref in enumerate((first_ref, second_ref)):
        part = slice(index * half, (index + 1) * half)
        out_ref[:, :half] = gate_ref[:, part]
        out_ref[:, half : 2 * half] = up_ref[:, part]
        out_ref[:, 2 * half :] = down_ref[part, :].T


def finish_mixing_kernel(heads, total_ref, query_ref, key_ref, value_ref, output_ref):
    query_width = query_ref.shape[1] // heads
    head_size = key_ref.shape[1] // heads
    start = 0
    for head in range(heads):
        for ref, part in ((query_ref, query_width), (key_ref, head_size), (value_ref, head_size)):
            ref[:, head * part : (head + 1) * part] = total_ref[:, start : start + part].astype(
                jnp.float32
            )
            start += part
    output_ref[...] = total_ref[:, start:].astype(jnp.float32).T


def finish_feed_kernel(*refs):
    first_refs, second_ref = refs[:-4], refs[-4]
    gate_ref, up_ref, down_ref = refs[-3:]
    half = gate_ref.shape[1] // 2

    def first_part(columns):
        return sum(ref[:, columns].astype(jnp.float32) for ref in first_refs)

    def second_part(columns):
        return second_ref[:, columns].astype(jnp.float32)

    for index, part_of in enumerate((first_part, second_part)):
        part = slice(index * half, (index + 1) * half)
        gate_ref[:, part] = part_of(slice(0, half))
        up_ref[:, part] = part_of(slice(half, 2 * half))
        down_ref[part, :] = part_of(slice(2 * half, 3 * half)).T


def whole_call(body, shapes, *operands):
    return pl.pallas_call(
        body,
        out_shape=shapes,
        in_specs=[pl.BlockSpec(memory_space=pltpu.VMEM)] * len(operands),
        out_specs=[pl.BlockSpec(memory_space=pltpu.VMEM)] * len(shapes),
        compiler_params=pltpu.CompilerParams(vmem_limit_bytes=VMEM_LIMIT),
        cost_estimate=pl.CostEstimate(
            flops=0, bytes_accessed=4 * sum(operand.size for operand in operands), transcendentals=0
        ),
    )(*operands)


def per_device(
    block_input,
    attention_gain,
    query_weight,
    key_matrix,
    value_matrix,
    query_gain,
    key_gain,
    output_weight,
    feed_gain,
    gate_weight,
    up_weight,
    down_weight,
    out_cotangent,
):
    size = lax.axis_size("tensor")
    sizes = (lax.axis_size("dp"), size)
    model_width = block_input.shape[1]
    head_size = query_gain.shape[0]
    query_columns = query_weight.shape[1]
    key_columns = key_matrix.shape[1]
    heads = key_columns // head_size
    grouping = query_columns // key_columns
    hidden_columns = gate_weight.shape[1]
    qkv_columns = query_columns + 2 * key_columns
    half = hidden_columns // 2
    tables = turn_tables(head_size)

    block_width = query_weight.shape[0]
    (mixing_local,) = whole_call(
        functools.partial(pack_mixing_kernel, heads),
        [jax.ShapeDtypeStruct((block_width, qkv_columns + query_columns), jnp.bfloat16)],
        query_weight, key_matrix, value_matrix, output_weight,
    )
    mixing_full = lax.all_gather(mixing_local, "dp", axis=0, tiled=True)
    feed_locals = whole_call(
        pack_feed_kernel,
        [jax.ShapeDtypeStruct((block_width, 3 * half), jnp.bfloat16)] * 2,
        gate_weight, up_weight, down_weight,
    )
    feed_full = [lax.all_gather(part, "dp", axis=0, tiled=True) for part in feed_locals]

    input_float = block_input.astype(jnp.float32)
    first_scale = row_scale(input_float)
    first_unit = input_float * first_scale
    mixer_local = (first_unit * attention_gain).astype(jnp.bfloat16)
    mixer_rows, cotangent_rows = gather_rows((mixer_local, out_cotangent), size, 0)

    raw, mixed_rows, totals = attention_forward(
        mixer_rows, mixing_full, tables, query_gain, key_gain, heads, grouping
    )
    local_shape = block_input.shape
    local_rows = local_shape[0]
    gain_rows = model_width // head_size
    gathered_shape = jax.ShapeDtypeStruct((size * local_rows, model_width), jnp.bfloat16)
    local_float = jax.ShapeDtypeStruct(local_shape, jnp.float32)
    local_half = jax.ShapeDtypeStruct(local_shape, jnp.bfloat16)
    row_sum = pltpu.VMEM((1, model_width), jnp.float32)
    own_rows = pltpu.VMEM(local_shape, jnp.bfloat16)
    scatter_scratch = Scatter.scratch(size, *local_shape)
    gather_scratch = Gather.scratch(size, *local_shape)
    feed_rows, hidden_state = scatter_call(
        functools.partial(between_forward_kernel, size, 1),
        [[(mixed_rows, mixing_full, qkv_columns)]],
        [block_input, feed_gain.reshape(1, -1)],
        [gathered_shape, local_float],
        True,
        [own_rows, *scatter_scratch, *gather_scratch],
        1,
    )

    hidden_first, slope_first = feed_half(feed_rows, cotangent_rows, feed_full[0])
    blocks, arrivals = reduce_over_chips(
        [(feed_rows, slope_first), (cotangent_rows, hidden_first)], sizes
    )
    blocks, later_full = lax.optimization_barrier((blocks, feed_full[1]))
    hidden_second, slope_second = feed_half(feed_rows, cotangent_rows, later_full)
    plain_order = jnp.arange(sizes[0], dtype=jnp.int32)
    second_grad = grad_blocks(
        plain_order, [(feed_rows, slope_second), (cotangent_rows, hidden_second)]
    ).reshape(model_width, -1)
    second_grad, slope_second = lax.optimization_barrier((second_grad, slope_second))
    second_total = lax.psum_scatter(second_grad, "dp", scatter_dimension=0, tiled=True)
    state_rows, state_slope, feed_term = scatter_call(
        functools.partial(between_backward_kernel, size, 2),
        [[(slope_first, feed_full[0], 0), (slope_second, later_full, 0)]],
        [hidden_state, out_cotangent, feed_gain.reshape(1, -1)],
        [gathered_shape, local_float, jax.ShapeDtypeStruct((gain_rows, head_size), jnp.float32)],
        True,
        [own_rows, row_sum, *scatter_scratch, *gather_scratch],
        2,
    )
    qkv_slope, head_terms = attention_backward(
        state_rows, mixing_full, qkv_columns, raw, mixed_rows, totals, tables,
        query_gain, key_gain, heads, grouping,
    )
    mixing_grad = grad_blocks(
        plain_order, [(mixer_rows, qkv_slope), (state_rows, mixed_rows)]
    ).reshape(model_width, -1)
    mixing_grad, qkv_slope = lax.optimization_barrier((mixing_grad, qkv_slope))
    mixing_total = lax.psum_scatter(mixing_grad, "dp", scatter_dimension=0, tiled=True)
    terms_shape = (2 * gain_rows + head_terms.shape[0], head_size)
    block_output, input_gradient, terms = scatter_call(
        functools.partial(last_kernel, sizes, (1, 2)),
        [
            [(qkv_slope, mixing_full, 0)],
            [(hidden_first, feed_full[0], 2 * half), (hidden_second, later_full, 2 * half)],
        ],
        [
            block_input,
            attention_gain.reshape(1, -1),
            state_slope,
            hidden_state,
            jnp.concatenate([feed_term, head_terms], axis=0),
        ],
        [local_half, local_half, jax.ShapeDtypeStruct(terms_shape, jnp.float32)],
        False,
        [
            row_sum,
            pltpu.VMEM(terms_shape, jnp.float32),
            pltpu.VMEM((size, *terms_shape), jnp.float32),
            pltpu.VMEM((sizes[0], *terms_shape), jnp.float32),
            *[pltpu.SemaphoreType.DMA((count - 1,)) for count in (size, size, *sizes[:1] * 2)],
            *scatter_scratch,
            *scatter_scratch,
        ],
        3,
    )
    query_gradient, key_gradient, value_gradient, output_gradient = whole_call(
        functools.partial(finish_mixing_kernel, heads),
        [
            jax.ShapeDtypeStruct((block_width, query_columns), jnp.float32),
            jax.ShapeDtypeStruct((block_width, key_columns), jnp.float32),
            jax.ShapeDtypeStruct((block_width, key_columns), jnp.float32),
            jax.ShapeDtypeStruct((query_columns, block_width), jnp.float32),
        ],
        mixing_total,
    )
    gate_gradient, up_gradient, down_gradient = whole_call(
        finish_feed_kernel,
        [
            jax.ShapeDtypeStruct((block_width, hidden_columns), jnp.float32),
            jax.ShapeDtypeStruct((block_width, hidden_columns), jnp.float32),
            jax.ShapeDtypeStruct((hidden_columns, block_width), jnp.float32),
        ],
        blocks[0], *arrivals, second_total,
    )
    return (
        block_output,
        input_gradient,
        terms[:gain_rows].reshape(-1),
        query_gradient,
        key_gradient,
        value_gradient,
        terms[2 * gain_rows],
        terms[2 * gain_rows + 1],
        output_gradient,
        terms[gain_rows : 2 * gain_rows].reshape(-1),
        gate_gradient,
        up_gradient,
        down_gradient,
    )


def solution(mesh):
    in_specs = (
        P(("dp", "tensor"), None),
        P(),
        P("dp", "tensor"),
        P("dp", "tensor"),
        P("dp", "tensor"),
        P(),
        P(),
        P("tensor", "dp"),
        P(),
        P("dp", "tensor"),
        P("dp", "tensor"),
        P("tensor", "dp"),
        P(("dp", "tensor"), None),
    )
    out_specs = (
        P(("dp", "tensor"), None),
        P(("dp", "tensor"), None),
        P(),
        P("dp", "tensor"),
        P("dp", "tensor"),
        P("dp", "tensor"),
        P(),
        P(),
        P("tensor", "dp"),
        P(),
        P("dp", "tensor"),
        P("dp", "tensor"),
        P("tensor", "dp"),
    )

    return jax.shard_map(
        per_device, mesh=mesh, in_specs=in_specs, out_specs=out_specs, check_vma=False
    )
```

```python
import functools

import jax
import jax.numpy as jnp
import numpy as np
from jax import lax
from jax.experimental import pallas as pl
from jax.experimental.pallas import tpu as pltpu
from jax.sharding import PartitionSpec as P


SEQUENCE_LENGTH = 1024

epsilon = 1e-06
rope_base = 1000000.0


MESH = pl.DeviceIdType.MESH
VMEM_LIMIT = 62 * 1024 * 1024


def row_scale(values):
    return lax.rsqrt(jnp.mean(values * values, axis=-1, keepdims=True) + epsilon)


def times_transposed(first_operand, second_operand):
    return lax.dot_general(
        first_operand, second_operand, (((1,), (1,)), ((), ())), preferred_element_type=jnp.float32
    )


def simple_product(first_operand, second_operand):
    return jnp.dot(first_operand, second_operand, preferred_element_type=jnp.float32)


def remote(source, target, send_sem, recv_sem, peer, axis="tensor"):
    return pltpu.make_async_remote_copy(
        src_ref=source,
        dst_ref=target,
        send_sem=send_sem,
        recv_sem=recv_sem,
        device_id={axis: peer},
        device_id_type=MESH,
    )


def greet(peers):
    barrier = pltpu.get_barrier_semaphore()
    for axis, peer in peers:
        pl.semaphore_signal(barrier, inc=1, device_id={axis: peer}, device_id_type=MESH)
    pl.semaphore_wait(barrier, len(peers))


def square_peers(me):
    column = lax.rem(me, 2)
    row = me // 2
    return row * 2 + (1 - column), (1 - row) * 2 + column, (1 - row) * 2 + (1 - column)


def neighbours(size):
    if size == 4:
        beside, below, _ = square_peers(lax.axis_index("tensor"))
        return [("tensor", beside), ("tensor", below)]
    return [("tensor", peer) for peer in other_members("tensor", size)]


def other_members(axis, count):
    me = lax.axis_index(axis)
    return [lax.rem(me + step, count) for step in range(1, count)]


class Gather:
    def __init__(self, size, own_ref, out_ref, held_ref, send_sem, recv_sem, local_sem):
        self.size, self.own, self.out, self.held = size, own_ref, out_ref, held_ref
        self.send_sem, self.recv_sem, self.local_sem = send_sem, recv_sem, local_sem
        self.me = lax.axis_index("tensor")
        self.rows = own_ref.shape[0]
        self.copies, self.stores = [], []

    @staticmethod
    def scratch(size, rows, columns):
        sends, local = (6, 7) if size == 4 else (size - 1, size)
        return [
            pltpu.VMEM((size, rows, columns), jnp.bfloat16),
            pltpu.SemaphoreType.DMA((sends,)),
            pltpu.SemaphoreType.DMA((sends,)),
            pltpu.SemaphoreType.DMA((local,)),
        ]

    def send(self, source, target, peer):
        index = len(self.copies)
        copy = remote(source, target, self.send_sem.at[index], self.recv_sem.at[index], peer)
        copy.start()
        self.copies.append(copy)
        return copy

    def store(self, source, start, count):
        target = self.out.at[pl.ds(pl.multiple_of(start, count), count)]
        copy = pltpu.make_async_copy(source, target, self.local_sem.at[len(self.stores)])
        copy.start()
        self.stores.append(copy)

    def start(self):
        own, held, rows = self.own, self.held, self.rows
        if self.size != 4:
            for peer in other_members("tensor", self.size):
                self.send(own, held.at[self.me], peer)
            self.store(own, self.me * rows, rows)
            return
        beside, below, _ = square_peers(self.me)
        half = rows // 2
        first, second = pl.ds(0, half), pl.ds(half, half)
        x_first = self.send(own.at[first], held.at[self.me, first], beside)
        y_second = self.send(own.at[second], held.at[self.me, second], below)
        self.send(own.at[second], held.at[self.me, second], beside)
        self.send(own.at[first], held.at[self.me, first], below)
        self.store(own, self.me * rows, rows)
        x_first.wait_recv()
        self.send(held.at[beside, first], held.at[beside, first], below)
        y_second.wait_recv()
        self.send(held.at[below, second], held.at[below, second], beside)
        self.store(held.at[beside, first], beside * rows, half)
        self.store(held.at[below, second], below * rows + half, half)

    def finish(self):
        held, rows = self.held, self.rows
        if self.size != 4:
            for step, copy in enumerate(self.copies):
                copy.wait_recv()
                slot = lax.rem(self.me + self.size - step - 1, self.size)
                self.store(held.at[slot], slot * rows, rows)
        else:
            beside, below, across = square_peers(self.me)
            half = rows // 2
            first, second = pl.ds(0, half), pl.ds(half, half)
            x_second, y_first, y_pass, x_pass = self.copies[2:]
            x_second.wait_recv()
            self.store(held.at[beside, second], beside * rows + half, half)
            y_first.wait_recv()
            self.store(held.at[below, first], below * rows, half)
            y_pass.wait_recv()
            self.store(held.at[across, first], across * rows, half)
            x_pass.wait_recv()
            self.store(held.at[across, second], across * rows + half, half)
        for copy in self.copies:
            copy.wait_send()
        for copy in self.stores:
            copy.wait()


def gather_kernel(size, count, *refs):
    own_refs, out_refs, rest = refs[:count], refs[count : 2 * count], refs[2 * count :]
    greet(neighbours(size))
    gathers = [
        Gather(size, own_refs[k], out_refs[k], *rest[4 * k : 4 * k + 4]) for k in range(count)
    ]
    for gather in gathers:
        gather.start()
    for gather in gathers:
        gather.finish()


def gather_rows(arrays, size, collective_id):
    count = len(arrays)
    rows, columns = arrays[0].shape
    scratch = []
    for _ in arrays:
        scratch += Gather.scratch(size, rows, columns)
    return pl.pallas_call(
        functools.partial(gather_kernel, size, count),
        out_shape=[jax.ShapeDtypeStruct((size * rows, columns), a.dtype) for a in arrays],
        in_specs=[pl.BlockSpec(memory_space=pltpu.VMEM)] * count,
        out_specs=[pl.BlockSpec(memory_space=pl.ANY)] * count,
        scratch_shapes=scratch,
        compiler_params=pltpu.CompilerParams(
            collective_id=collective_id, has_side_effects=True, vmem_limit_bytes=VMEM_LIMIT
        ),
        cost_estimate=pl.CostEstimate(
            flops=0, bytes_accessed=count * 30 * size * rows * columns, transcendentals=0
        ),
        name="gather_rows",
    )(*arrays)


def block_product(pairs, start, rows, write):
    total = pairs[0][1].shape[0]
    tile = min(512, total)
    start = pl.multiple_of(start, rows)

    def step(index, carry):
        columns = pl.ds(pl.multiple_of(index * tile, tile), tile)
        values = None
        for left_ref, weight_ref in pairs:
            part = times_transposed(left_ref[pl.ds(start, rows), :], weight_ref[columns, :])
            values = part if values is None else values + part
        write(columns, values)
        return carry

    lax.fori_loop(0, total // tile, step, 0)


class Scatter:
    def __init__(self, size, outgoing, *rest):
        self.size, self.outgoing = size, outgoing
        if size == 4:
            self.passing, rest = rest[0], rest[1:]
        self.arriving, self.send_sem, self.recv_sem = rest
        self.rows = outgoing.shape[1]
        self.me = lax.axis_index("tensor")
        self.copies, self.starts = self.plan()

    @staticmethod
    def scratch(size, rows, columns):
        if size == 4:
            sends = 6
            buffers = [
                pltpu.VMEM((4, rows, columns), jnp.bfloat16),
                pltpu.VMEM((2, rows // 2, columns), jnp.bfloat16),
                pltpu.VMEM((2, rows, columns), jnp.bfloat16),
            ]
        else:
            sends = size - 1
            buffers = [
                pltpu.VMEM((size, rows, columns), jnp.bfloat16),
                pltpu.VMEM((size - 1, rows, columns), jnp.bfloat16),
            ]
        return buffers + [pltpu.SemaphoreType.DMA((sends,)), pltpu.SemaphoreType.DMA((sends,))]

    def prepare(self, index, source, target, peer):
        return remote(source, target, self.send_sem.at[index], self.recv_sem.at[index], peer)

    def plan(self):
        outgoing, arriving = self.outgoing, self.arriving
        if self.size != 4:
            copies = [
                self.prepare(step, outgoing.at[step], arriving.at[step], peer)
                for step, peer in enumerate(other_members("tensor", self.size))
            ]
            return copies, tuple((step, step) for step in range(self.size - 1))
        beside, below, _ = square_peers(self.me)
        half = self.rows // 2
        first, second = pl.ds(0, half), pl.ds(half, half)
        copies = [
            self.prepare(0, outgoing.at[0, first], self.passing.at[0], beside),
            self.prepare(1, outgoing.at[0, second], self.passing.at[1], below),
            self.prepare(2, outgoing.at[1, first], arriving.at[0, first], beside),
            self.prepare(3, outgoing.at[2, second], arriving.at[1, second], below),
            self.prepare(4, outgoing.at[1, second], arriving.at[0, second], beside),
            self.prepare(5, outgoing.at[2, first], arriving.at[1, first], below),
        ]
        return copies, ((0, 0), (0, 1), (1, 2), (2, 3))

    def fill(self, pairs):
        size, me, rows = self.size, self.me, self.rows

        def step(slot, carry):
            if size == 4:
                beside, below, across = square_peers(me)
                owner = jnp.where(
                    slot == 0, across, jnp.where(slot == 1, beside, jnp.where(slot == 2, below, me))
                )
            else:
                owner = lax.rem(me + slot + 1, size)

            def write(columns, values):
                self.outgoing[slot, :, columns] = values.astype(self.outgoing.dtype)

            block_product(pairs, owner * rows, rows, write)
            for at, index in self.starts:
                pl.when(slot == at)(self.copies[index].start)
            return carry

        lax.fori_loop(0, size, step, 0)

    def relay(self):
        if self.size != 4:
            return
        half = self.rows // 2
        x_pass, y_pass, _, _, x_second, y_first = self.copies
        for arrival, source, slot, start, onward in (
            (y_pass, 1, 1, half, x_second),
            (x_pass, 0, 2, 0, y_first),
        ):
            arrival.wait_recv()
            piece = pl.ds(start, half)
            self.outgoing[slot, piece, :] = (
                self.outgoing[slot, piece, :].astype(jnp.float32)
                + self.passing[source].astype(jnp.float32)
            ).astype(self.outgoing.dtype)
            onward.start()

    def collect(self):
        for copy in self.copies[2:] if self.size == 4 else self.copies:
            copy.wait_recv()

    def total(self, piece):
        total = self.outgoing[self.size - 1, piece, :].astype(jnp.float32)
        for index in range(self.arriving.shape[0]):
            total = total + self.arriving[index, piece, :].astype(jnp.float32)
        return total

    def drain(self):
        for copy in self.copies:
            copy.wait_send()


class Chain:
    def __init__(
        self, chips, steps, rising_refs, falling_refs, up_ref, down_ref,
        rise, fall, up, down, load_sem, send_sem, recv_sem,
    ):
        self.chips, self.steps = chips, steps
        self.rise, self.fall, self.up, self.down = rise, fall, up, down
        device = lax.axis_index("dp")
        self.chip = device // 2
        count = len(steps)
        self.loads = [
            pltpu.make_async_copy(source, target, load_sem.at[index])
            for index, (source, target) in enumerate(
                [(up_ref, up.at[0]), (down_ref, down.at[0])]
                + [(ref, rise.at[index]) for index, ref in enumerate(rising_refs)]
                + [(ref, fall.at[index]) for index, ref in enumerate(falling_refs)]
            )
        ]
        above = lax.rem(device + 2, 2 * chips)
        under = lax.rem(device + 2 * chips - 2, 2 * chips)
        self.neighbours = [("dp", above), ("dp", under)]
        self.rises = [
            remote(rise.at[i], up.at[i + 1], send_sem.at[i], recv_sem.at[i], above, "dp")
            for i in range(count)
        ]
        self.falls = [
            remote(
                fall.at[i], down.at[i + 1], send_sem.at[count + i], recv_sem.at[count + i], under, "dp"
            )
            for i in range(count)
        ]

    @staticmethod
    def scratch(count, rows, columns):
        return [
            pltpu.VMEM((count, rows, columns), jnp.bfloat16),
            pltpu.VMEM((count, rows, columns), jnp.bfloat16),
            pltpu.VMEM((count + 1, rows, columns), jnp.bfloat16),
            pltpu.VMEM((count + 1, rows, columns), jnp.bfloat16),
            pltpu.SemaphoreType.DMA((2 * count + 2,)),
            pltpu.SemaphoreType.DMA((2 * count,)),
            pltpu.SemaphoreType.DMA((2 * count,)),
        ]

    def load(self):
        for copy in self.loads:
            copy.start()

    def step(self, index):
        if index == 0:
            for copy in self.loads:
                copy.wait()
        step = self.steps[index]
        rows = self.rise.shape[1]
        sends_up = self.chip < step
        sends_down = self.chip >= self.chips - step

        @pl.when(sends_up & (self.chip > 0))
        def _():
            def add(piece):
                self.rise[index, piece, :] = add_rounded(
                    self.rise[index, piece, :], self.up[index, piece, :]
                )

            over_pieces(rows, add)

        pl.when(sends_up)(self.rises[index].start)

        @pl.when(sends_down & (self.chip < self.chips - 1))
        def _():
            def add(piece):
                self.fall[index, piece, :] = add_rounded(
                    self.fall[index, piece, :], self.down[index, piece, :]
                )

            over_pieces(rows, add)

        pl.when(sends_down)(self.falls[index].start)

    def arrives(self, index):
        step = self.steps[index]
        from_under = (self.chip > 0) & (self.chip <= step)
        from_above = (self.chip < self.chips - 1) & (self.chip >= self.chips - step - 1)
        return from_under, from_above

    def wait(self, index):
        from_under, from_above = self.arrives(index)
        pl.when(from_under)(self.rises[index].wait_recv)
        pl.when(from_above)(self.falls[index].wait_recv)

    def drain(self):
        for index, step in enumerate(self.steps):
            pl.when(self.chip < step)(self.rises[index].wait_send)
            pl.when(self.chip >= self.chips - step)(self.falls[index].wait_send)


def add_rounded(first, second):
    return (first.astype(jnp.float32) + second.astype(jnp.float32)).astype(jnp.bfloat16)


def over_pieces(rows, body):
    count = min(32, rows)

    def step(index, carry):
        body(pl.ds(pl.multiple_of(index * count, count), count))
        return carry

    lax.fori_loop(0, rows // count, step, 0)


def send_terms(axis, peers, source, landing, send_sem, recv_sem):
    me = lax.axis_index(axis)
    landing[me] = source[...]
    copies = []
    for step, peer in enumerate(peers):
        copy = remote(source, landing.at[me], send_sem.at[step], recv_sem.at[step], peer, axis)
        copy.start()
        copies.append(copy)
    return copies


def add_terms(landing, copies):
    for copy in copies:
        copy.wait_recv()
    total = landing[0]
    for index in range(1, landing.shape[0]):
        total = total + landing[index]
    return total


def split_pairs(refs, count):
    return [refs[2 * p : 2 * p + 2] for p in range(count)], refs[2 * count :]


def store_row(target_ref, row_ref):
    width = target_ref.shape[1]
    for index in range(row_ref.shape[1] // width):
        target_ref[index : index + 1, :] = row_ref[:, index * width : (index + 1) * width]


def between_forward_kernel(size, pair_count, *refs):
    pairs, refs = split_pairs(refs, pair_count)
    input_ref, gain_ref, gathered_ref, state_ref, own_ref = refs[:5]
    buffers = 5 if size == 4 else 4
    scatter = Scatter(size, *refs[5 : 5 + buffers])
    gather = Gather(size, own_ref, gathered_ref, *refs[5 + buffers :])
    greet(neighbours(size))
    scatter.fill(pairs)
    scatter.relay()
    scatter.collect()

    def norm(piece):
        state = input_ref[piece, :].astype(jnp.float32) + scatter.total(piece)
        state_ref[piece, :] = state
        own_ref[piece, :] = (state * row_scale(state) * gain_ref[...]).astype(own_ref.dtype)

    over_pieces(own_ref.shape[0], norm)
    gather.start()
    gather.finish()
    scatter.drain()


def between_backward_kernel(size, chips, steps, pair_count, *refs):
    pairs, refs = split_pairs(refs, pair_count)
    state_ref, cotangent_ref, gain_ref = refs[:3]
    chain_count = 2 * len(steps) + 2
    chain_refs, refs = refs[3 : 3 + chain_count], refs[3 + chain_count :]
    gathered_ref, slope_ref, term_ref, up_out_ref, down_out_ref, own_ref, sum_ref = refs[:7]
    buffers = 5 if size == 4 else 4
    scatter = Scatter(size, *refs[7 : 7 + buffers])
    gather = Gather(size, own_ref, gathered_ref, *refs[7 + buffers : 11 + buffers])
    chain = Chain(
        chips, steps, chain_refs[: len(steps)], chain_refs[len(steps) : -2], *chain_refs[-2:],
        *refs[11 + buffers :],
    )
    chain.load()
    greet(neighbours(size) + chain.neighbours)
    chain.step(0)
    scatter.fill(pairs)
    scatter.relay()
    sum_ref[...] = jnp.zeros_like(sum_ref)
    scatter.collect()

    def norm(piece):
        back = scatter.total(piece)
        state = state_ref[piece, :]
        scale = row_scale(state)
        unit = state * scale
        sum_ref[...] += jnp.sum(back * unit, axis=0, keepdims=True)
        unit_slope = back * gain_ref[...]
        slope = cotangent_ref[piece, :].astype(jnp.float32) + scale * (
            unit_slope - unit * jnp.mean(unit_slope * unit, axis=-1, keepdims=True)
        )
        slope_ref[piece, :] = slope
        own_ref[piece, :] = slope.astype(own_ref.dtype)

    over_pieces(own_ref.shape[0], norm)
    gather.start()
    store_row(term_ref, sum_ref)
    chain.wait(0)
    for index in range(1, len(steps)):
        chain.step(index)
        chain.wait(index)
    last = len(steps)
    from_under, from_above = chain.arrives(last - 1)
    for arrived, landing, out_ref in (
        (from_under, chain.up, up_out_ref),
        (from_above, chain.down, down_out_ref),
    ):

        @pl.when(arrived)
        def _(landing=landing, out_ref=out_ref):
            out_ref[...] = landing[last]

        @pl.when(jnp.logical_not(arrived))
        def _(out_ref=out_ref):
            out_ref[...] = jnp.zeros_like(out_ref)

    gather.finish()
    scatter.drain()
    chain.drain()


def last_kernel(sizes, pair_count, *refs):
    data_size, size = sizes
    pairs, refs = split_pairs(refs, pair_count)
    input_ref, gain_ref, slope_ref, terms_ref = refs[:4]
    gradient_ref, terms_out_ref, sum_ref, partial_ref, inner, outer = refs[4:10]
    inner_send, inner_recv, outer_send, outer_recv = refs[10:14]
    mixing = Scatter(size, *refs[14:])
    greet(
        [("tensor", peer) for peer in other_members("tensor", size)]
        + [("dp", peer) for peer in other_members("dp", data_size)]
    )
    mixing.fill(pairs)
    mixing.relay()
    sum_ref[...] = jnp.zeros_like(sum_ref)
    mixing.collect()

    def norm(piece):
        back = mixing.total(piece)
        values = input_ref[piece, :].astype(jnp.float32)
        scale = row_scale(values)
        unit = values * scale
        sum_ref[...] += jnp.sum(back * unit, axis=0, keepdims=True)
        unit_slope = back * gain_ref[...]
        gradient_ref[piece, :] = (
            slope_ref[piece, :]
            + scale * (unit_slope - unit * jnp.mean(unit_slope * unit, axis=-1, keepdims=True))
        ).astype(gradient_ref.dtype)

    over_pieces(gradient_ref.shape[0], norm)
    kept = partial_ref.shape[0] - terms_ref.shape[0]
    partial_ref[kept:, :] = terms_ref[...]
    store_row(partial_ref, sum_ref)
    inner_copies = send_terms(
        "tensor", other_members("tensor", size), partial_ref, inner, inner_send, inner_recv
    )
    terms_out_ref[...] = add_terms(inner, inner_copies)
    outer_copies = send_terms(
        "dp", other_members("dp", data_size), terms_out_ref, outer, outer_send, outer_recv
    )
    total = add_terms(outer, outer_copies)
    for copy in outer_copies:
        copy.wait_send()
    terms_out_ref[...] = total
    for copy in inner_copies:
        copy.wait_send()
    mixing.drain()


def scatter_call(body, triple_lists, others, outs, gathered, scratch, collective_id, far=()):
    in_specs = []
    operands = []
    flops = 0
    for left, weight, first_column in (triple for triples in triple_lists for triple in triples):
        part = left.shape[1]
        flops += 2 * left.size * weight.shape[0]
        in_specs += [
            pl.BlockSpec(left.shape, lambda i: (0, 0), pipeline_mode=pl.Buffered(1)),
            pl.BlockSpec(
                (weight.shape[0], part),
                lambda i, block=first_column // part: (0, block),
                pipeline_mode=pl.Buffered(1),
            ),
        ]
        operands += [left, weight]
    for other in others:
        in_specs.append(pl.BlockSpec(other.shape, lambda i: (0, 0), pipeline_mode=pl.Buffered(1)))
        operands.append(other)
    for other in far:
        in_specs.append(pl.BlockSpec(memory_space=pl.ANY))
        operands.append(other)
    out_specs = [pl.BlockSpec(out.shape, lambda i: (0, 0)) for out in outs]
    if gathered:
        out_specs[0] = pl.BlockSpec(memory_space=pl.ANY)
    return pl.pallas_call(
        body,
        grid=(1,),
        out_shape=outs,
        in_specs=in_specs,
        out_specs=out_specs,
        scratch_shapes=scratch,
        compiler_params=pltpu.CompilerParams(
            collective_id=collective_id, has_side_effects=True, vmem_limit_bytes=VMEM_LIMIT
        ),
        cost_estimate=pl.CostEstimate(
            flops=flops, bytes_accessed=150_000_000, transcendentals=0
        ),
    )(*operands)


LOG2E = 1.4426950408889634


def turn_tables(head_size):
    half_size = head_size // 2
    frequency = np.float32(rope_base) ** (
        -(np.arange(half_size, dtype=np.float32) * np.float32(2.0) / np.float32(head_size))
    )
    frequency = frequency.astype(np.float64)
    sign = np.concatenate([-np.ones(half_size), np.ones(half_size)])[None, :]
    positions = np.concatenate([np.arange(0, SEQUENCE_LENGTH, 128), np.arange(128)])
    angles = positions[:, None] * np.concatenate([frequency, frequency])[None, :]
    return np.cos(angles).astype(np.float32), (sign * np.sin(angles)).astype(np.float32)


def fill_tables(few_cosines_ref, few_sines_ref, cosine_ref, sine_ref):
    coarse = few_cosines_ref.shape[0] - 128
    near_cosine, near_sine = few_cosines_ref[coarse:, :], few_sines_ref[coarse:, :]

    def step(index, carry):
        far_cosine = few_cosines_ref[pl.ds(index, 1), :]
        far_sine = few_sines_ref[pl.ds(index, 1), :]
        rows = pl.ds(pl.multiple_of(index * 128, 128), 128)
        cosine_ref[rows, :] = far_cosine * near_cosine - far_sine * near_sine
        sine_ref[rows, :] = far_sine * near_cosine + far_cosine * near_sine
        return carry

    lax.fori_loop(0, coarse, step, 0)


def turn(values, cosine, sine):
    return values * cosine + pltpu.roll(values, values.shape[-1] // 2, 1) * sine


def turn_back(values, cosine, sine):
    return values * cosine - pltpu.roll(values, values.shape[-1] // 2, 1) * sine


def contract_first(first_operand, second_operand):
    return lax.dot_general(
        first_operand, second_operand, (((0,), (0,)), ((), ())), preferred_element_type=jnp.float32
    )


def visible_scores(key_rows, query_rows, first_row, multiplier):
    scores = times_transposed(key_rows, query_rows) * multiplier
    _, queries = scores.shape
    key_at = lax.broadcasted_iota(jnp.int32, (queries, queries), 0)
    query_at = lax.broadcasted_iota(jnp.int32, (queries, queries), 1)
    corner = jnp.where(query_at >= key_at, scores[first_row:], -1e30)
    if first_row == 0:
        return corner
    return jnp.concatenate([scores[:first_row], corner], axis=0)


def turn_heads(
    grouping, head_size, raw_ref, query_gain_ref, key_gain_ref, cosine_ref, sine_ref, query_ref, key_ref, value_ref
):
    def turned(start, gain):
        raw = raw_ref[:, pl.ds(start, head_size)]
        return turn(raw * row_scale(raw) * gain, cosine_ref[...], sine_ref[...]).astype(jnp.bfloat16)

    def step(part, carry):
        query_ref[part] = turned(pl.multiple_of(part * head_size, head_size), query_gain_ref[...])
        return carry

    lax.fori_loop(0, grouping, step, 0)
    key_ref[...] = turned(grouping * head_size, key_gain_ref[...])
    value_ref[...] = raw_ref[:, (grouping + 1) * head_size :].astype(jnp.bfloat16)


def attention_forward_kernel(
    grouping, head_size, block, rows_ref, weight_ref, few_cosines_ref, few_sines_ref, query_gain_ref, key_gain_ref,
    raw_ref, mixed_ref, total_ref, query_ref, key_ref, value_ref, cosine_ref, sine_ref,
):
    sequence = rows_ref.shape[0]
    multiplier = head_size ** (-0.5) * LOG2E

    @pl.when((pl.program_id(0) == 0) & (pl.program_id(1) == 0))
    def _():
        fill_tables(few_cosines_ref, few_sines_ref, cosine_ref, sine_ref)

    raw_ref[...] = simple_product(rows_ref[...], weight_ref[...])
    turn_heads(
        grouping, head_size, raw_ref, query_gain_ref, key_gain_ref, cosine_ref, sine_ref, query_ref, key_ref, value_ref
    )

    def head_step(part, carry):
        lanes = pl.ds(pl.multiple_of(part * head_size, head_size), head_size)
        for first_row in range(0, sequence, block):
            last_row = first_row + block
            scores = visible_scores(
                key_ref[:last_row, :], query_ref[part, first_row:last_row, :], first_row, multiplier
            )
            highest = jnp.max(scores, axis=0, keepdims=True)
            weights = jnp.exp2(scores - highest)
            total = jnp.sum(weights, axis=0, keepdims=True)
            weights = (weights * (1.0 / total)).astype(jnp.bfloat16)
            mixed_ref[first_row:last_row, lanes] = contract_first(
                weights, value_ref[:last_row, :]
            ).astype(mixed_ref.dtype)
            total_ref[0, pl.ds(part, 1), first_row:last_row] = highest + jnp.log2(total)
        return carry

    lax.fori_loop(0, grouping, head_step, 0)


def attention_forward(rows, weight, tables, query_gain, key_gain, heads, grouping):
    total_rows, depth = rows.shape
    head_size = query_gain.shape[0]
    sequences = total_rows // SEQUENCE_LENGTH
    width = (grouping + 2) * head_size
    block = min(256, SEQUENCE_LENGTH)
    table = pl.BlockSpec(tables[0].shape, lambda s, h: (0, 0))
    gain = pl.BlockSpec((1, head_size), lambda s, h: (0, 0))
    elements = heads * grouping * total_rows * SEQUENCE_LENGTH // 2
    return pl.pallas_call(
        functools.partial(attention_forward_kernel, grouping, head_size, block),
        grid=(sequences, heads),
        out_shape=[
            jax.ShapeDtypeStruct((total_rows, heads * width), jnp.float32),
            jax.ShapeDtypeStruct((total_rows, heads * grouping * head_size), jnp.bfloat16),
            jax.ShapeDtypeStruct((heads, grouping, total_rows), jnp.float32),
        ],
        in_specs=[
            pl.BlockSpec((SEQUENCE_LENGTH, depth), lambda s, h: (s, 0)),
            pl.BlockSpec((depth, width), lambda s, h: (0, h)),
            table,
            table,
            gain,
            gain,
        ],
        out_specs=[
            pl.BlockSpec((SEQUENCE_LENGTH, width), lambda s, h: (s, h)),
            pl.BlockSpec((SEQUENCE_LENGTH, grouping * head_size), lambda s, h: (s, h)),
            pl.BlockSpec((1, grouping, SEQUENCE_LENGTH), lambda s, h: (h, 0, s)),
        ],
        scratch_shapes=[
            pltpu.VMEM((grouping, SEQUENCE_LENGTH, head_size), jnp.bfloat16),
            pltpu.VMEM((SEQUENCE_LENGTH, head_size), jnp.bfloat16),
            pltpu.VMEM((SEQUENCE_LENGTH, head_size), jnp.bfloat16),
            pltpu.VMEM((SEQUENCE_LENGTH, head_size), jnp.float32),
            pltpu.VMEM((SEQUENCE_LENGTH, head_size), jnp.float32),
        ],
        compiler_params=pltpu.CompilerParams(vmem_limit_bytes=VMEM_LIMIT),
        cost_estimate=pl.CostEstimate(
            flops=2 * total_rows * depth * heads * width + 4 * elements * head_size,
            bytes_accessed=2 * (total_rows * depth + depth * heads * width),
            transcendentals=elements,
        ),
        name="attention_forward",
    )(rows, weight, *tables, query_gain.reshape(1, -1), key_gain.reshape(1, -1))


def norm_back(turned_slope, raw, gain, cosine, sine):
    norm_slope = turn_back(turned_slope, cosine, sine)
    scale = row_scale(raw)
    unit = raw * scale
    term = norm_slope * unit
    unit_slope = norm_slope * gain
    slope = scale * (unit_slope - unit * jnp.mean(unit_slope * unit, axis=-1, keepdims=True))
    return slope.astype(jnp.bfloat16), jnp.sum(term, axis=0, keepdims=True)


def attention_backward_kernel(size, chips, grouping, head_size, block, pair_count, *refs):
    pairs, refs = split_pairs(refs, pair_count)
    (
        state_ref, weight_ref, raw_ref, mixed_ref, total_ref, few_cosines_ref, few_sines_ref,
        query_gain_ref, key_gain_ref, hidden_state_ref,
    ) = refs[:10]
    chain_refs, own_block_ref = refs[10:14], refs[14]
    slope_ref, gain_ref, output_ref, chain_total_ref = refs[15:19]
    (
        query_ref, key_ref, value_ref, out_slope_ref, turned_ref, key_sum_ref, value_sum_ref, cosine_ref, sine_ref,
    ) = refs[19:28]
    buffers = 5 if size == 4 else 4
    scatter = Scatter(size, *refs[28 : 28 + buffers])
    own_block, own_sem = refs[28 + buffers : 30 + buffers]
    chain = Chain(
        chips, (chips - 1,), chain_refs[:1], chain_refs[1:2], *chain_refs[2:], *refs[30 + buffers :]
    )
    own_load = pltpu.make_async_copy(own_block_ref, own_block, own_sem.at[0])
    step = pl.program_id(0) * pl.num_programs(1) + pl.program_id(1)
    steps = pl.num_programs(0) * pl.num_programs(1)

    @pl.when(step == 0)
    def _():
        chain.load()
        own_load.start()
        greet(neighbours(size) + chain.neighbours)
        chain.step(0)
        scatter.fill(pairs)

    attend_backward_head(
        grouping, head_size, block, state_ref, weight_ref, raw_ref, mixed_ref, total_ref, few_cosines_ref,
        few_sines_ref, query_gain_ref, key_gain_ref, slope_ref, gain_ref, query_ref, key_ref, value_ref,
        out_slope_ref, turned_ref, key_sum_ref, value_sum_ref, cosine_ref, sine_ref,
    )

    @pl.when(step == 0)
    def _():
        scatter.relay()

    @pl.when(step == steps - 1)
    def _():
        scatter.collect()

        def finish(piece):
            output_ref[piece, :] = (hidden_state_ref[piece, :] + scatter.total(piece)).astype(
                output_ref.dtype
            )

        over_pieces(output_ref.shape[0], finish)
        own_load.wait()
        chain.wait(0)
        from_under, from_above = chain.arrives(0)

        @pl.when(from_under)
        def _():
            def add(piece):
                own_block[piece, :] = add_rounded(own_block[piece, :], chain.up[1, piece, :])

            over_pieces(own_block.shape[0], add)

        @pl.when(from_above)
        def _():
            def add(piece):
                own_block[piece, :] = add_rounded(own_block[piece, :], chain.down[1, piece, :])

            over_pieces(own_block.shape[0], add)

        chain_total_ref[...] = own_block[...]
        scatter.drain()
        chain.drain()


def attend_backward_head(
    grouping, head_size, block, state_ref, weight_ref, raw_ref, mixed_ref, total_ref, few_cosines_ref, few_sines_ref,
    query_gain_ref, key_gain_ref, slope_ref, gain_ref, query_ref, key_ref, value_ref, out_slope_ref,
    turned_ref, key_sum_ref, value_sum_ref, cosine_ref, sine_ref,
):
    sequence = state_ref.shape[0]
    scale_factor = head_size ** (-0.5)
    multiplier = scale_factor * LOG2E

    @pl.when((pl.program_id(0) == 0) & (pl.program_id(1) == 0))
    def _():
        gain_ref[...] = jnp.zeros_like(gain_ref)
        fill_tables(few_cosines_ref, few_sines_ref, cosine_ref, sine_ref)

    out_slope_ref[...] = simple_product(state_ref[...], weight_ref[...]).astype(jnp.bfloat16)
    turn_heads(
        grouping, head_size, raw_ref, query_gain_ref, key_gain_ref, cosine_ref, sine_ref, query_ref, key_ref, value_ref
    )
    key_sum_ref[...] = jnp.zeros_like(key_sum_ref)
    value_sum_ref[...] = jnp.zeros_like(value_sum_ref)
    ones = jnp.ones((8, head_size), jnp.float32)

    def head_step(part, carry):
        lanes = pl.ds(pl.multiple_of(part * head_size, head_size), head_size)
        for first_row in range(0, sequence, block):
            last_row = first_row + block
            query_rows = query_ref[part, first_row:last_row, :]
            slope_rows = out_slope_ref[first_row:last_row, lanes]
            scores = visible_scores(key_ref[:last_row, :], query_rows, first_row, multiplier)
            weights = jnp.exp2(scores - total_ref[0, pl.ds(part, 1), first_row:last_row])
            value_sum_ref[:last_row, :] += simple_product(weights.astype(jnp.bfloat16), slope_rows)
            product = slope_rows.astype(jnp.float32) * mixed_ref[first_row:last_row, lanes].astype(jnp.float32)
            centre = lax.dot_general(
                ones,
                product,
                (((1,), (1,)), ((), ())),
                preferred_element_type=jnp.float32,
                precision=lax.Precision.HIGHEST,
            )[:1]
            weight_slope = times_transposed(value_ref[:last_row, :], slope_rows)
            score_slope = (weights * (weight_slope - centre)).astype(jnp.bfloat16)
            key_sum_ref[:last_row, :] += simple_product(score_slope, query_rows)
            turned_ref[first_row:last_row, :] = (
                contract_first(score_slope, key_ref[:last_row, :]) * scale_factor
            )
        slope, term = norm_back(
            turned_ref[...], raw_ref[:, lanes], query_gain_ref[...], cosine_ref[...], sine_ref[...]
        )
        slope_ref[:, lanes] = slope
        gain_ref[0:1, :] += term
        return carry

    lax.fori_loop(0, grouping, head_step, 0)
    lanes = slice(grouping * head_size, (grouping + 1) * head_size)
    slope, term = norm_back(
        key_sum_ref[...] * scale_factor, raw_ref[:, lanes], key_gain_ref[...], cosine_ref[...], sine_ref[...]
    )
    slope_ref[:, lanes] = slope
    gain_ref[1:2, :] += term
    slope_ref[:, (grouping + 1) * head_size :] = value_sum_ref[...].astype(jnp.bfloat16)


def attention_backward(
    state_rows, weight, weight_start, raw, mixed, totals, tables, query_gain, key_gain, heads, grouping,
    triples, hidden_state, chain_arrays, own_block, sizes, collective_id,
):
    total_rows, depth = state_rows.shape
    head_size = query_gain.shape[0]
    sequences = total_rows // SEQUENCE_LENGTH
    width = (grouping + 2) * head_size
    out_width = grouping * head_size
    block = min(256, SEQUENCE_LENGTH)
    first_block = weight_start // out_width
    data_size, size = sizes
    chips = data_size // 2
    single = pl.Buffered(1)
    table = pl.BlockSpec(tables[0].shape, lambda s, h: (0, 0))
    gain = pl.BlockSpec((1, head_size), lambda s, h: (0, 0))
    elements = heads * grouping * total_rows * SEQUENCE_LENGTH // 2
    whole_rows = pltpu.VMEM((SEQUENCE_LENGTH, head_size), jnp.float32)
    in_specs = []
    operands = []
    for left, other_weight, first_column in triples:
        part = left.shape[1]
        in_specs += [
            pl.BlockSpec(left.shape, lambda s, h: (0, 0), pipeline_mode=single),
            pl.BlockSpec(
                (other_weight.shape[0], part),
                lambda s, h, at=first_column // part: (0, at),
                pipeline_mode=single,
            ),
        ]
        operands += [left, other_weight]
    in_specs += [
        pl.BlockSpec((SEQUENCE_LENGTH, depth), lambda s, h: (s, 0), pipeline_mode=single),
        pl.BlockSpec((depth, out_width), lambda s, h: (0, first_block + h)),
        pl.BlockSpec((SEQUENCE_LENGTH, width), lambda s, h: (s, h)),
        pl.BlockSpec((SEQUENCE_LENGTH, out_width), lambda s, h: (s, h)),
        pl.BlockSpec((1, grouping, SEQUENCE_LENGTH), lambda s, h: (h, 0, s)),
        table,
        table,
        gain,
        gain,
        pl.BlockSpec(hidden_state.shape, lambda s, h: (0, 0), pipeline_mode=single),
    ] + [pl.BlockSpec(memory_space=pl.ANY)] * 5
    operands += [
        state_rows, weight, raw, mixed, totals, *tables, query_gain.reshape(1, -1), key_gain.reshape(1, -1),
        hidden_state, *chain_arrays, own_block,
    ]
    return pl.pallas_call(
        functools.partial(
            attention_backward_kernel, size, chips, grouping, head_size, block, len(triples)
        ),
        grid=(sequences, heads),
        out_shape=[
            jax.ShapeDtypeStruct((total_rows, heads * width), jnp.bfloat16),
            jax.ShapeDtypeStruct((8, head_size), jnp.float32),
            jax.ShapeDtypeStruct(hidden_state.shape, jnp.bfloat16),
            jax.ShapeDtypeStruct(own_block.shape, jnp.bfloat16),
        ],
        in_specs=in_specs,
        out_specs=[
            pl.BlockSpec((SEQUENCE_LENGTH, width), lambda s, h: (s, h)),
            pl.BlockSpec((8, head_size), lambda s, h: (0, 0)),
            pl.BlockSpec(hidden_state.shape, lambda s, h: (0, 0)),
            pl.BlockSpec(own_block.shape, lambda s, h: (0, 0)),
        ],
        scratch_shapes=[
            pltpu.VMEM((grouping, SEQUENCE_LENGTH, head_size), jnp.bfloat16),
            pltpu.VMEM((SEQUENCE_LENGTH, head_size), jnp.bfloat16),
            pltpu.VMEM((SEQUENCE_LENGTH, head_size), jnp.bfloat16),
            pltpu.VMEM((SEQUENCE_LENGTH, out_width), jnp.bfloat16),
            whole_rows,
            whole_rows,
            whole_rows,
            whole_rows,
            whole_rows,
            *Scatter.scratch(size, *hidden_state.shape),
            pltpu.VMEM(own_block.shape, jnp.bfloat16),
            pltpu.SemaphoreType.DMA((1,)),
            *Chain.scratch(1, *own_block.shape),
        ],
        compiler_params=pltpu.CompilerParams(
            collective_id=collective_id, has_side_effects=True, vmem_limit_bytes=VMEM_LIMIT
        ),
        cost_estimate=pl.CostEstimate(
            flops=2 * total_rows * depth * heads * out_width + 10 * elements * head_size,
            bytes_accessed=100_000_000,
            transcendentals=elements,
        ),
        name="attention_backward",
    )(*operands)


def feed_half_kernel(half, tile, rows_ref, cotangent_ref, weight_ref, hidden_ref, slope_ref):
    rows, cotangent = rows_ref[...], cotangent_ref[...]

    def step(index, carry):
        start = pl.multiple_of(index * tile, tile)
        gate = simple_product(rows, weight_ref[:, pl.ds(start, tile)])
        up = simple_product(rows, weight_ref[:, pl.ds(half + start, tile)])
        back = simple_product(cotangent, weight_ref[:, pl.ds(2 * half + start, tile)])
        sigmoid = 1.0 / (1.0 + jnp.exp(-gate))
        gated = gate * sigmoid
        hidden_ref[:, pl.ds(start, tile)] = (gated * up).astype(jnp.bfloat16)
        slope_ref[:, pl.ds(start, tile)] = (
            back * up * sigmoid * (1.0 + gate * (1.0 - sigmoid))
        ).astype(jnp.bfloat16)
        slope_ref[:, pl.ds(half + start, tile)] = (back * gated).astype(jnp.bfloat16)
        return carry

    lax.fori_loop(0, half // tile, step, 0)


def feed_half(rows, cotangent, weight):
    total_rows, depth = rows.shape
    half = weight.shape[1] // 3
    block = min(512, total_rows)
    tile = 256 if half % 256 == 0 else 128
    row_block = pl.BlockSpec((block, depth), lambda i: (i, 0))
    return pl.pallas_call(
        functools.partial(feed_half_kernel, half, tile),
        grid=(total_rows // block,),
        out_shape=[
            jax.ShapeDtypeStruct((total_rows, half), jnp.bfloat16),
            jax.ShapeDtypeStruct((total_rows, 2 * half), jnp.bfloat16),
        ],
        in_specs=[
            row_block,
            row_block,
            pl.BlockSpec(weight.shape, lambda i: (0, 0), pipeline_mode=pl.Buffered(1)),
        ],
        out_specs=[
            pl.BlockSpec((block, half), lambda i: (i, 0)),
            pl.BlockSpec((block, 2 * half), lambda i: (i, 0)),
        ],
        compiler_params=pltpu.CompilerParams(vmem_limit_bytes=VMEM_LIMIT),
        cost_estimate=pl.CostEstimate(
            flops=6 * total_rows * depth * half,
            bytes_accessed=2 * (2 * total_rows * depth + 3 * depth * half),
            transcendentals=total_rows * half,
        ),
        name="feed_half",
    )(rows, cotangent, weight)


def grad_kernel(pair_count, with_other, order_ref, *refs):
    pairs = [refs[2 * p : 2 * p + 2] for p in range(pair_count)]
    refs = refs[2 * pair_count :]
    step = pl.program_id(0)
    if with_other:
        other_ref, refs = refs[0], refs[1:]
        out_refs, held_ref, copy_sem = refs[:-3], refs[-3], refs[-2]
    else:
        out_ref = refs[0]
    turned_ref = refs[-1]
    start = 0
    for left_ref, right_ref in pairs:
        turned_ref[...] = left_ref[...].T
        width = right_ref.shape[1]
        tile = next(t for t in (768, 512, 384, 256, 128) if width % t == 0)
        for column in range(0, width, tile):
            values = simple_product(turned_ref[...], right_ref[:, column : column + tile])
            columns = slice(start + column, start + column + tile)
            if with_other:
                values = values + other_ref[0, :, columns].astype(jnp.float32)
                held_ref[step, :, columns] = values.astype(jnp.bfloat16)
            else:
                out_ref[0, :, columns] = values.astype(jnp.bfloat16)
        start += width
    if with_other:
        copies = [
            pltpu.make_async_copy(held_ref.at[index], out_ref, copy_sem.at[index])
            for index, out_ref in enumerate(out_refs)
        ]
        for index, copy in enumerate(copies):
            pl.when(step == index)(copy.start)

        @pl.when(step == len(copies) - 1)
        def _():
            for copy in copies:
                copy.wait()


def grad_blocks(order, pairs, other=None):
    count = order.shape[0]
    total_rows, depth = pairs[0][0].shape
    block = depth // lax.axis_size("dp")
    width = sum(right.shape[1] for _, right in pairs)
    in_specs = []
    operands = []
    for left, right in pairs:
        in_specs += [
            pl.BlockSpec((total_rows, block), lambda k, at: (0, at[k])),
            pl.BlockSpec(right.shape, lambda k, at: (0, 0), pipeline_mode=pl.Buffered(1)),
        ]
        operands += [left, right]
    scratch = [pltpu.VMEM((block, total_rows), jnp.bfloat16)]
    if other is not None:
        in_specs.append(pl.BlockSpec((1, block, width), lambda k, at: (k, 0, 0)))
        operands.append(other)
        out_shape = [jax.ShapeDtypeStruct((block, width), jnp.bfloat16)] * count
        out_specs = [pl.BlockSpec(memory_space=pl.ANY)] * count
        scratch = [
            pltpu.VMEM((count, block, width), jnp.bfloat16),
            pltpu.SemaphoreType.DMA((count,)),
        ] + scratch
    else:
        out_shape = [jax.ShapeDtypeStruct((count, block, width), jnp.bfloat16)]
        out_specs = [pl.BlockSpec((1, block, width), lambda k, at: (k, 0, 0))]
    out = pl.pallas_call(
        functools.partial(grad_kernel, len(pairs), other is not None),
        grid_spec=pltpu.PrefetchScalarGridSpec(
            num_scalar_prefetch=1,
            grid=(count,),
            in_specs=in_specs,
            out_specs=out_specs,
            scratch_shapes=scratch,
        ),
        out_shape=out_shape,
        compiler_params=pltpu.CompilerParams(vmem_limit_bytes=VMEM_LIMIT),
        cost_estimate=pl.CostEstimate(
            flops=2 * total_rows * count * block * width,
            bytes_accessed=2 * (total_rows * count * block * len(pairs) + width * (total_rows + count * block)),
            transcendentals=0,
        ),
        name="grad_blocks",
    )(order, *operands)
    return out if other is not None else out[0]


def reduce_over_chips(pairs, sizes):
    data_size = sizes[0]
    chips = data_size // 2
    me = lax.axis_index("dp")
    chip, core = me // 2, lax.rem(me, 2)
    ahead = lax.rem(chip + jnp.arange(chips, dtype=jnp.int32), chips) * 2
    other = lax.ppermute(
        grad_blocks(ahead + (1 - core), pairs),
        "dp",
        [(device, device ^ 1) for device in range(data_size)],
    )
    blocks = grad_blocks(ahead + core, pairs, other)
    up = lax.ppermute(blocks[chips - 1], "dp", [(device, device + 2) for device in range(2)])
    down = lax.ppermute(
        blocks[1],
        "dp",
        [(device, device - 2) for device in range(data_size - 2, data_size)],
    )
    return blocks, up, down


def pack_mixing_kernel(heads, query_ref, key_ref, value_ref, output_ref, out_ref):
    query_width = query_ref.shape[1] // heads
    head_size = key_ref.shape[1] // heads
    start = 0
    for head in range(heads):
        for ref, part in ((query_ref, query_width), (key_ref, head_size), (value_ref, head_size)):
            out_ref[:, start : start + part] = ref[:, head * part : (head + 1) * part]
            start += part
    out_ref[:, start:] = output_ref[...].T


def pack_feed_kernel(gate_ref, up_ref, down_ref, first_ref, second_ref):
    start = 0
    for out_ref in (first_ref, second_ref):
        width = out_ref.shape[1] // 3
        part = slice(start, start + width)
        out_ref[:, :width] = gate_ref[:, part]
        out_ref[:, width : 2 * width] = up_ref[:, part]
        out_ref[:, 2 * width :] = down_ref[part, :].T
        start += width


def finish_mixing_kernel(heads, total_ref, output_total_ref, query_ref, key_ref, value_ref, output_ref):
    query_width = query_ref.shape[1] // heads
    head_size = key_ref.shape[1] // heads
    start = 0
    for head in range(heads):
        for ref, part in ((query_ref, query_width), (key_ref, head_size), (value_ref, head_size)):
            ref[:, head * part : (head + 1) * part] = total_ref[:, start : start + part].astype(
                jnp.float32
            )
            start += part
    output_ref[...] = output_total_ref[...].astype(jnp.float32).T


def finish_feed_kernel(first_ref, second_ref, gate_ref, up_ref, down_ref):
    start = 0
    for total_ref in (first_ref, second_ref):
        width = total_ref.shape[1] // 3
        part = slice(start, start + width)
        gate_ref[:, part] = total_ref[:, :width].astype(jnp.float32)
        up_ref[:, part] = total_ref[:, width : 2 * width].astype(jnp.float32)
        down_ref[part, :] = total_ref[:, 2 * width :].astype(jnp.float32).T
        start += width


def whole_call(body, shapes, *operands):
    return pl.pallas_call(
        body,
        out_shape=shapes,
        in_specs=[pl.BlockSpec(memory_space=pltpu.VMEM)] * len(operands),
        out_specs=[pl.BlockSpec(memory_space=pltpu.VMEM)] * len(shapes),
        compiler_params=pltpu.CompilerParams(vmem_limit_bytes=VMEM_LIMIT),
        cost_estimate=pl.CostEstimate(
            flops=0, bytes_accessed=4 * sum(operand.size for operand in operands), transcendentals=0
        ),
    )(*operands)


def per_device(
    block_input,
    attention_gain,
    query_weight,
    key_matrix,
    value_matrix,
    query_gain,
    key_gain,
    output_weight,
    feed_gain,
    gate_weight,
    up_weight,
    down_weight,
    out_cotangent,
):
    size = lax.axis_size("tensor")
    sizes = (lax.axis_size("dp"), size)
    model_width = block_input.shape[1]
    head_size = query_gain.shape[0]
    query_columns = query_weight.shape[1]
    key_columns = key_matrix.shape[1]
    heads = key_columns // head_size
    grouping = query_columns // key_columns
    hidden_columns = gate_weight.shape[1]
    qkv_columns = query_columns + 2 * key_columns
    first_columns = hidden_columns * 2 // 3 // 256 * 256 or hidden_columns // 2
    second_columns = hidden_columns - first_columns
    tables = turn_tables(head_size)

    block_width = query_weight.shape[0]
    (mixing_local,) = whole_call(
        functools.partial(pack_mixing_kernel, heads),
        [jax.ShapeDtypeStruct((block_width, qkv_columns + query_columns), jnp.bfloat16)],
        query_weight, key_matrix, value_matrix, output_weight,
    )
    mixing_full = lax.all_gather(mixing_local, "dp", axis=0, tiled=True)
    feed_locals = whole_call(
        pack_feed_kernel,
        [
            jax.ShapeDtypeStruct((block_width, 3 * columns), jnp.bfloat16)
            for columns in (first_columns, second_columns)
        ],
        gate_weight, up_weight, down_weight,
    )
    feed_full = [lax.all_gather(part, "dp", axis=0, tiled=True) for part in feed_locals]

    input_float = block_input.astype(jnp.float32)
    first_scale = row_scale(input_float)
    first_unit = input_float * first_scale
    mixer_local = (first_unit * attention_gain).astype(jnp.bfloat16)
    mixer_rows, cotangent_rows = gather_rows((mixer_local, out_cotangent), size, 0)

    raw, mixed_rows, totals = attention_forward(
        mixer_rows, mixing_full, tables, query_gain, key_gain, heads, grouping
    )
    local_shape = block_input.shape
    local_rows = local_shape[0]
    gain_rows = model_width // head_size
    gathered_shape = jax.ShapeDtypeStruct((size * local_rows, model_width), jnp.bfloat16)
    local_float = jax.ShapeDtypeStruct(local_shape, jnp.float32)
    local_half = jax.ShapeDtypeStruct(local_shape, jnp.bfloat16)
    row_sum = pltpu.VMEM((1, model_width), jnp.float32)
    own_rows = pltpu.VMEM(local_shape, jnp.bfloat16)
    scatter_scratch = Scatter.scratch(size, *local_shape)
    gather_scratch = Gather.scratch(size, *local_shape)
    feed_rows, hidden_state = scatter_call(
        functools.partial(between_forward_kernel, size, 1),
        [[(mixed_rows, mixing_full, qkv_columns)]],
        [block_input, feed_gain.reshape(1, -1)],
        [gathered_shape, local_float],
        True,
        [own_rows, *scatter_scratch, *gather_scratch],
        1,
    )

    hidden_first, slope_first = feed_half(feed_rows, cotangent_rows, feed_full[0])
    blocks, up, down = reduce_over_chips(
        [(feed_rows, slope_first), (cotangent_rows, hidden_first)], sizes
    )
    blocks, later_full = lax.optimization_barrier((blocks, feed_full[1]))
    hidden_second, slope_second = feed_half(feed_rows, cotangent_rows, later_full)
    plain_order = jnp.arange(sizes[0], dtype=jnp.int32)
    second_grad = grad_blocks(
        plain_order, [(feed_rows, slope_second), (cotangent_rows, hidden_second)]
    ).reshape(model_width, -1)
    second_grad, slope_second = lax.optimization_barrier((second_grad, slope_second))
    second_total = lax.psum_scatter(second_grad, "dp", scatter_dimension=0, tiled=True)
    chips = sizes[0] // 2
    middle_steps = tuple(range(2, chips - 1))
    chain_block = jax.ShapeDtypeStruct(blocks[0].shape, jnp.bfloat16)
    state_rows, state_slope, feed_term, up, down = scatter_call(
        functools.partial(between_backward_kernel, size, chips, middle_steps, 2),
        [[(slope_first, feed_full[0], 0), (slope_second, later_full, 0)]],
        [hidden_state, out_cotangent, feed_gain.reshape(1, -1)],
        [
            gathered_shape,
            local_float,
            jax.ShapeDtypeStruct((gain_rows, head_size), jnp.float32),
            chain_block,
            chain_block,
        ],
        True,
        [
            own_rows,
            row_sum,
            *scatter_scratch,
            *gather_scratch,
            *Chain.scratch(len(middle_steps), *blocks[0].shape),
        ],
        2,
        [blocks[chips - step] for step in middle_steps]
        + [blocks[step] for step in middle_steps]
        + [up, down],
    )
    output_grad = grad_blocks(plain_order, [(state_rows, mixed_rows)]).reshape(model_width, -1)
    output_grad, state_rows = lax.optimization_barrier((output_grad, state_rows))
    output_total = lax.psum_scatter(output_grad, "dp", scatter_dimension=0, tiled=True)
    qkv_slope, head_terms, block_output, first_total = attention_backward(
        state_rows, mixing_full, qkv_columns, raw, mixed_rows, totals, tables,
        query_gain, key_gain, heads, grouping,
        [
            (hidden_first, feed_full[0], 2 * first_columns),
            (hidden_second, later_full, 2 * second_columns),
        ],
        hidden_state, [blocks[1], blocks[chips - 1], up, down], blocks[0], sizes, 4,
    )
    mixing_grad = grad_blocks(plain_order, [(mixer_rows, qkv_slope)]).reshape(model_width, -1)
    mixing_grad, qkv_slope = lax.optimization_barrier((mixing_grad, qkv_slope))
    mixing_total = lax.psum_scatter(mixing_grad, "dp", scatter_dimension=0, tiled=True)
    terms_shape = (2 * gain_rows + head_terms.shape[0], head_size)
    input_gradient, terms = scatter_call(
        functools.partial(last_kernel, sizes, 1),
        [[(qkv_slope, mixing_full, 0)]],
        [
            block_input,
            attention_gain.reshape(1, -1),
            state_slope,
            jnp.concatenate([feed_term, head_terms], axis=0),
        ],
        [local_half, jax.ShapeDtypeStruct(terms_shape, jnp.float32)],
        False,
        [
            row_sum,
            pltpu.VMEM(terms_shape, jnp.float32),
            pltpu.VMEM((size, *terms_shape), jnp.float32),
            pltpu.VMEM((sizes[0], *terms_shape), jnp.float32),
            *[pltpu.SemaphoreType.DMA((count - 1,)) for count in (size, size, *sizes[:1] * 2)],
            *scatter_scratch,
        ],
        3,
    )
    query_gradient, key_gradient, value_gradient, output_gradient = whole_call(
        functools.partial(finish_mixing_kernel, heads),
        [
            jax.ShapeDtypeStruct((block_width, query_columns), jnp.float32),
            jax.ShapeDtypeStruct((block_width, key_columns), jnp.float32),
            jax.ShapeDtypeStruct((block_width, key_columns), jnp.float32),
            jax.ShapeDtypeStruct((query_columns, block_width), jnp.float32),
        ],
        mixing_total, output_total,
    )
    gate_gradient, up_gradient, down_gradient = whole_call(
        finish_feed_kernel,
        [
            jax.ShapeDtypeStruct((block_width, hidden_columns), jnp.float32),
            jax.ShapeDtypeStruct((block_width, hidden_columns), jnp.float32),
            jax.ShapeDtypeStruct((hidden_columns, block_width), jnp.float32),
        ],
        first_total, second_total,
    )
    return (
        block_output,
        input_gradient,
        terms[:gain_rows].reshape(-1),
        query_gradient,
        key_gradient,
        value_gradient,
        terms[2 * gain_rows],
        terms[2 * gain_rows + 1],
        output_gradient,
        terms[gain_rows : 2 * gain_rows].reshape(-1),
        gate_gradient,
        up_gradient,
        down_gradient,
    )


def solution(mesh):
    in_specs = (
        P(("dp", "tensor"), None),
        P(),
        P("dp", "tensor"),
        P("dp", "tensor"),
        P("dp", "tensor"),
        P(),
        P(),
        P("tensor", "dp"),
        P(),
        P("dp", "tensor"),
        P("dp", "tensor"),
        P("tensor", "dp"),
        P(("dp", "tensor"), None),
    )
    out_specs = (
        P(("dp", "tensor"), None),
        P(("dp", "tensor"), None),
        P(),
        P("dp", "tensor"),
        P("dp", "tensor"),
        P("dp", "tensor"),
        P(),
        P(),
        P("tensor", "dp"),
        P(),
        P("dp", "tensor"),
        P("dp", "tensor"),
        P("tensor", "dp"),
    )

    return jax.shard_map(
        per_device, mesh=mesh, in_specs=in_specs, out_specs=out_specs, check_vma=False
    )
```

```python
import functools

import jax
import jax.numpy as jnp
import numpy as np
from jax import lax
from jax.experimental import pallas as pl
from jax.experimental.pallas import tpu as pltpu
from jax.sharding import PartitionSpec as P


SEQUENCE_LENGTH = 1024

epsilon = 1e-06
rope_base = 1000000.0


MESH = pl.DeviceIdType.MESH
VMEM_LIMIT = 62 * 1024 * 1024


def row_scale(values):
    return lax.rsqrt(jnp.mean(values * values, axis=-1, keepdims=True) + epsilon)


def times_transposed(first_operand, second_operand):
    return lax.dot_general(
        first_operand, second_operand, (((1,), (1,)), ((), ())), preferred_element_type=jnp.float32
    )


def simple_product(first_operand, second_operand):
    return jnp.dot(first_operand, second_operand, preferred_element_type=jnp.float32)


def remote(source, target, send_sem, recv_sem, peer, axis="tensor"):
    return pltpu.make_async_remote_copy(
        src_ref=source,
        dst_ref=target,
        send_sem=send_sem,
        recv_sem=recv_sem,
        device_id={axis: peer},
        device_id_type=MESH,
    )


def greet(peers):
    barrier = pltpu.get_barrier_semaphore()
    for axis, peer in peers:
        pl.semaphore_signal(barrier, inc=1, device_id={axis: peer}, device_id_type=MESH)
    pl.semaphore_wait(barrier, len(peers))


def square_peers(me):
    column = lax.rem(me, 2)
    row = me // 2
    return row * 2 + (1 - column), (1 - row) * 2 + column, (1 - row) * 2 + (1 - column)


def neighbours(size):
    if size == 4:
        beside, below, _ = square_peers(lax.axis_index("tensor"))
        return [("tensor", beside), ("tensor", below)]
    return [("tensor", peer) for peer in other_members("tensor", size)]


def other_members(axis, count):
    me = lax.axis_index(axis)
    return [lax.rem(me + step, count) for step in range(1, count)]


class Gather:
    def __init__(self, size, own_ref, out_ref, held_ref, send_sem, recv_sem, local_sem):
        self.size, self.own, self.out, self.held = size, own_ref, out_ref, held_ref
        self.send_sem, self.recv_sem, self.local_sem = send_sem, recv_sem, local_sem
        self.me = lax.axis_index("tensor")
        self.rows = own_ref.shape[0]
        self.copies, self.stores = [], []

    @staticmethod
    def scratch(size, rows, columns):
        sends, local = (6, 7) if size == 4 else (size - 1, size)
        return [
            pltpu.VMEM((size, rows, columns), jnp.bfloat16),
            pltpu.SemaphoreType.DMA((sends,)),
            pltpu.SemaphoreType.DMA((sends,)),
            pltpu.SemaphoreType.DMA((local,)),
        ]

    def send(self, source, target, peer):
        index = len(self.copies)
        copy = remote(source, target, self.send_sem.at[index], self.recv_sem.at[index], peer)
        copy.start()
        self.copies.append(copy)
        return copy

    def store(self, source, start, count):
        target = self.out.at[pl.ds(pl.multiple_of(start, count), count)]
        copy = pltpu.make_async_copy(source, target, self.local_sem.at[len(self.stores)])
        copy.start()
        self.stores.append(copy)

    def start(self):
        own, held, rows = self.own, self.held, self.rows
        if self.size != 4:
            for peer in other_members("tensor", self.size):
                self.send(own, held.at[self.me], peer)
            self.store(own, self.me * rows, rows)
            return
        beside, below, _ = square_peers(self.me)
        half = rows // 2
        first, second = pl.ds(0, half), pl.ds(half, half)
        x_first = self.send(own.at[first], held.at[self.me, first], beside)
        y_second = self.send(own.at[second], held.at[self.me, second], below)
        self.send(own.at[second], held.at[self.me, second], beside)
        self.send(own.at[first], held.at[self.me, first], below)
        self.store(own, self.me * rows, rows)
        x_first.wait_recv()
        self.send(held.at[beside, first], held.at[beside, first], below)
        y_second.wait_recv()
        self.send(held.at[below, second], held.at[below, second], beside)
        self.store(held.at[beside, first], beside * rows, half)
        self.store(held.at[below, second], below * rows + half, half)

    def finish(self):
        held, rows = self.held, self.rows
        if self.size != 4:
            for step, copy in enumerate(self.copies):
                copy.wait_recv()
                slot = lax.rem(self.me + self.size - step - 1, self.size)
                self.store(held.at[slot], slot * rows, rows)
        else:
            beside, below, across = square_peers(self.me)
            half = rows // 2
            first, second = pl.ds(0, half), pl.ds(half, half)
            x_second, y_first, y_pass, x_pass = self.copies[2:]
            x_second.wait_recv()
            self.store(held.at[beside, second], beside * rows + half, half)
            y_first.wait_recv()
            self.store(held.at[below, first], below * rows, half)
            y_pass.wait_recv()
            self.store(held.at[across, first], across * rows, half)
            x_pass.wait_recv()
            self.store(held.at[across, second], across * rows + half, half)
        for copy in self.copies:
            copy.wait_send()
        for copy in self.stores:
            copy.wait()


def gather_kernel(size, count, *refs):
    own_refs, out_refs, rest = refs[:count], refs[count : 2 * count], refs[2 * count :]
    greet(neighbours(size))
    gathers = [
        Gather(size, own_refs[k], out_refs[k], *rest[4 * k : 4 * k + 4]) for k in range(count)
    ]
    for gather in gathers:
        gather.start()
    for gather in gathers:
        gather.finish()


def gather_rows(arrays, size, collective_id):
    count = len(arrays)
    rows, columns = arrays[0].shape
    scratch = []
    for _ in arrays:
        scratch += Gather.scratch(size, rows, columns)
    return pl.pallas_call(
        functools.partial(gather_kernel, size, count),
        out_shape=[jax.ShapeDtypeStruct((size * rows, columns), a.dtype) for a in arrays],
        in_specs=[pl.BlockSpec(memory_space=pltpu.VMEM)] * count,
        out_specs=[pl.BlockSpec(memory_space=pl.ANY)] * count,
        scratch_shapes=scratch,
        compiler_params=pltpu.CompilerParams(
            collective_id=collective_id, has_side_effects=True, vmem_limit_bytes=VMEM_LIMIT
        ),
        cost_estimate=pl.CostEstimate(
            flops=0, bytes_accessed=count * 30 * size * rows * columns, transcendentals=0
        ),
        name="gather_rows",
    )(*arrays)


class Operand:
    def __init__(self, size, first_column, left_far, weight_far, left, weight, left_sem, weight_sem):
        self.left, self.weight = left, weight
        self.rows = left.shape[0] // size
        self.tile = min(512, weight.shape[0])
        self.far = left_far, weight_far
        self.first_column = first_column
        self.left_sem, self.weight_sem = left_sem, weight_sem

    @staticmethod
    def scratch(size, left, weight):
        width = left.shape[1]
        return [
            pltpu.VMEM(left.shape, left.dtype),
            pltpu.VMEM((weight.shape[0], width), weight.dtype),
            pltpu.SemaphoreType.DMA((size,)),
            pltpu.SemaphoreType.DMA((max(1, weight.shape[0] // 512),)),
        ]

    def left_copy(self, slot, owner):
        piece = pl.ds(pl.multiple_of(owner * self.rows, self.rows), self.rows)
        return pltpu.make_async_copy(self.far[0].at[piece], self.left.at[piece], self.left_sem.at[slot])

    def weight_copy(self, index):
        piece = pl.ds(pl.multiple_of(index * self.tile, self.tile), self.tile)
        columns = pl.ds(self.first_column, self.left.shape[1])
        return pltpu.make_async_copy(
            self.far[1].at[piece, columns], self.weight.at[piece], self.weight_sem.at[index]
        )


def block_product(operands, start, rows, fresh, write):
    total = operands[0].weight.shape[0]
    tile = operands[0].tile
    start = pl.multiple_of(start, rows)

    def step(index, carry):
        @pl.when(fresh)
        def _():
            for operand in operands:
                operand.weight_copy(index).wait()

        columns = pl.ds(pl.multiple_of(index * tile, tile), tile)
        values = None
        for operand in operands:
            part = times_transposed(
                operand.left[pl.ds(start, rows), :], operand.weight[columns, :]
            )
            values = part if values is None else values + part
        write(columns, values)
        return carry

    lax.fori_loop(0, total // tile, step, 0)


class Scatter:
    def __init__(self, size, outgoing, *rest):
        self.size, self.outgoing = size, outgoing
        if size == 4:
            self.passing, rest = rest[0], rest[1:]
        self.arriving, self.send_sem, self.recv_sem = rest
        self.rows = outgoing.shape[1]
        self.me = lax.axis_index("tensor")
        self.copies, self.starts = self.plan()

    @staticmethod
    def scratch(size, rows, columns):
        if size == 4:
            sends = 6
            buffers = [
                pltpu.VMEM((4, rows, columns), jnp.bfloat16),
                pltpu.VMEM((2, rows // 2, columns), jnp.bfloat16),
                pltpu.VMEM((2, rows, columns), jnp.bfloat16),
            ]
        else:
            sends = size - 1
            buffers = [
                pltpu.VMEM((size, rows, columns), jnp.bfloat16),
                pltpu.VMEM((size - 1, rows, columns), jnp.bfloat16),
            ]
        return buffers + [pltpu.SemaphoreType.DMA((sends,)), pltpu.SemaphoreType.DMA((sends,))]

    def prepare(self, index, source, target, peer):
        return remote(source, target, self.send_sem.at[index], self.recv_sem.at[index], peer)

    def plan(self):
        outgoing, arriving = self.outgoing, self.arriving
        if self.size != 4:
            copies = [
                self.prepare(step, outgoing.at[step], arriving.at[step], peer)
                for step, peer in enumerate(other_members("tensor", self.size))
            ]
            return copies, tuple((step, step) for step in range(self.size - 1))
        beside, below, _ = square_peers(self.me)
        half = self.rows // 2
        first, second = pl.ds(0, half), pl.ds(half, half)
        copies = [
            self.prepare(0, outgoing.at[0, first], self.passing.at[0], beside),
            self.prepare(1, outgoing.at[0, second], self.passing.at[1], below),
            self.prepare(2, outgoing.at[1, first], arriving.at[0, first], beside),
            self.prepare(3, outgoing.at[2, second], arriving.at[1, second], below),
            self.prepare(4, outgoing.at[1, second], arriving.at[0, second], beside),
            self.prepare(5, outgoing.at[2, first], arriving.at[1, first], below),
        ]
        return copies, ((0, 0), (0, 1), (1, 2), (2, 3))

    def owner(self, slot):
        if self.size != 4:
            return lax.rem(self.me + slot + 1, self.size)
        beside, below, across = square_peers(self.me)
        return jnp.where(
            slot == 0, across, jnp.where(slot == 1, beside, jnp.where(slot == 2, below, self.me))
        )

    def load(self, operands):
        tiles = operands[0].weight.shape[0] // operands[0].tile
        for operand in operands:
            operand.left_copy(0, self.owner(0)).start()
        for index in range(tiles):
            for operand in operands:
                operand.weight_copy(index).start()
        for slot in range(1, self.size):
            for operand in operands:
                operand.left_copy(slot, self.owner(slot)).start()

    def fill(self, operands, look=None):
        rows = self.rows

        def step(slot, carry):
            owner = self.owner(slot)
            for operand in operands:
                operand.left_copy(slot, owner).wait()

            def write(columns, values):
                self.outgoing[slot, :, columns] = values.astype(self.outgoing.dtype)
                if look is not None:
                    look(owner, columns, values)

            block_product(operands, owner * rows, rows, slot == 0, write)
            for at, index in self.starts:
                pl.when(slot == at)(self.copies[index].start)
            return carry

        lax.fori_loop(0, self.size, step, 0)

    def relay(self):
        if self.size != 4:
            return
        half = self.rows // 2
        x_pass, y_pass, _, _, x_second, y_first = self.copies
        for arrival, source, slot, start, onward in (
            (y_pass, 1, 1, half, x_second),
            (x_pass, 0, 2, 0, y_first),
        ):
            arrival.wait_recv()
            piece = pl.ds(start, half)
            self.outgoing[slot, piece, :] = (
                self.outgoing[slot, piece, :].astype(jnp.float32)
                + self.passing[source].astype(jnp.float32)
            ).astype(self.outgoing.dtype)
            onward.start()

    def collect(self):
        for copy in self.copies[2:] if self.size == 4 else self.copies:
            copy.wait_recv()

    def total(self, piece):
        total = self.outgoing[self.size - 1, piece, :].astype(jnp.float32)
        for index in range(self.arriving.shape[0]):
            total = total + self.arriving[index, piece, :].astype(jnp.float32)
        return total

    def drain(self):
        for copy in self.copies:
            copy.wait_send()


class Chain:
    def __init__(
        self, chips, steps, rising_refs, falling_refs, up_ref, down_ref,
        rise, fall, up, down, load_sem, send_sem, recv_sem,
    ):
        self.chips, self.steps = chips, steps
        self.rise, self.fall, self.up, self.down = rise, fall, up, down
        device = lax.axis_index("dp")
        self.chip = device // 2
        count = len(steps)
        self.loads = [
            pltpu.make_async_copy(source, target, load_sem.at[index])
            for index, (source, target) in enumerate(
                [(up_ref, up.at[0]), (down_ref, down.at[0])]
                + [(ref, rise.at[index]) for index, ref in enumerate(rising_refs)]
                + [(ref, fall.at[index]) for index, ref in enumerate(falling_refs)]
            )
        ]
        above = lax.rem(device + 2, 2 * chips)
        under = lax.rem(device + 2 * chips - 2, 2 * chips)
        self.neighbours = [("dp", above), ("dp", under)]
        self.rises = [
            remote(rise.at[i], up.at[i + 1], send_sem.at[i], recv_sem.at[i], above, "dp")
            for i in range(count)
        ]
        self.falls = [
            remote(
                fall.at[i], down.at[i + 1], send_sem.at[count + i], recv_sem.at[count + i], under, "dp"
            )
            for i in range(count)
        ]

    @staticmethod
    def scratch(count, rows, columns):
        return [
            pltpu.VMEM((count, rows, columns), jnp.bfloat16),
            pltpu.VMEM((count, rows, columns), jnp.bfloat16),
            pltpu.VMEM((count + 1, rows, columns), jnp.bfloat16),
            pltpu.VMEM((count + 1, rows, columns), jnp.bfloat16),
            pltpu.SemaphoreType.DMA((2 * count + 2,)),
            pltpu.SemaphoreType.DMA((2 * count,)),
            pltpu.SemaphoreType.DMA((2 * count,)),
        ]

    def load(self):
        for copy in self.loads:
            copy.start()

    def step(self, index):
        if index == 0:
            for copy in self.loads:
                copy.wait()
        step = self.steps[index]
        rows = self.rise.shape[1]
        sends_up = self.chip < step
        sends_down = self.chip >= self.chips - step

        @pl.when(sends_up & (self.chip > 0))
        def _():
            def add(piece):
                self.rise[index, piece, :] = add_rounded(
                    self.rise[index, piece, :], self.up[index, piece, :]
                )

            over_pieces(rows, add)

        pl.when(sends_up)(self.rises[index].start)

        @pl.when(sends_down & (self.chip < self.chips - 1))
        def _():
            def add(piece):
                self.fall[index, piece, :] = add_rounded(
                    self.fall[index, piece, :], self.down[index, piece, :]
                )

            over_pieces(rows, add)

        pl.when(sends_down)(self.falls[index].start)

    def arrives(self, index):
        step = self.steps[index]
        from_under = (self.chip > 0) & (self.chip <= step)
        from_above = (self.chip < self.chips - 1) & (self.chip >= self.chips - step - 1)
        return from_under, from_above

    def wait(self, index):
        from_under, from_above = self.arrives(index)
        pl.when(from_under)(self.rises[index].wait_recv)
        pl.when(from_above)(self.falls[index].wait_recv)

    def drain(self):
        for index, step in enumerate(self.steps):
            pl.when(self.chip < step)(self.rises[index].wait_send)
            pl.when(self.chip >= self.chips - step)(self.falls[index].wait_send)


def add_rounded(first, second):
    return (first.astype(jnp.float32) + second.astype(jnp.float32)).astype(jnp.bfloat16)


def over_pieces(rows, body):
    count = min(32, rows)

    def step(index, carry):
        body(pl.ds(pl.multiple_of(index * count, count), count))
        return carry

    lax.fori_loop(0, rows // count, step, 0)


def send_terms(axis, peers, source, landing, send_sem, recv_sem):
    me = lax.axis_index(axis)
    landing[me] = source[...]
    copies = []
    for step, peer in enumerate(peers):
        copy = remote(source, landing.at[me], send_sem.at[step], recv_sem.at[step], peer, axis)
        copy.start()
        copies.append(copy)
    return copies


def add_terms(landing, copies):
    for copy in copies:
        copy.wait_recv()
    total = landing[0]
    for index in range(1, landing.shape[0]):
        total = total + landing[index]
    return total


def split_operands(refs, size, first_columns):
    count = len(first_columns)
    far, refs, scratch = refs[: 2 * count], refs[2 * count : -4 * count], refs[-4 * count :]
    operands = [
        Operand(size, first, *far[2 * p : 2 * p + 2], *scratch[4 * p : 4 * p + 4])
        for p, first in enumerate(first_columns)
    ]
    return operands, refs


def store_row(target_ref, row_ref):
    width = target_ref.shape[1]
    for index in range(row_ref.shape[1] // width):
        target_ref[index : index + 1, :] = row_ref[:, index * width : (index + 1) * width]


def between_forward_kernel(size, first_columns, *refs):
    operands, refs = split_operands(refs, size, first_columns)
    input_ref, gain_ref, gathered_ref, state_ref, own_ref = refs[:5]
    buffers = 5 if size == 4 else 4
    scatter = Scatter(size, *refs[5 : 5 + buffers])
    gather = Gather(size, own_ref, gathered_ref, *refs[5 + buffers :])
    scatter.load(operands)
    greet(neighbours(size))
    scatter.fill(operands)
    scatter.relay()
    scatter.collect()

    def norm(piece):
        state = input_ref[piece, :].astype(jnp.float32) + scatter.total(piece)
        state_ref[piece, :] = state
        own_ref[piece, :] = (state * row_scale(state) * gain_ref[...]).astype(own_ref.dtype)

    over_pieces(own_ref.shape[0], norm)
    gather.start()
    gather.finish()
    scatter.drain()


def between_backward_kernel(size, chips, steps, first_columns, *refs):
    operands, refs = split_operands(refs, size, first_columns)
    state_ref, cotangent_ref, gain_ref = refs[:3]
    chain_count = 2 * len(steps) + 2
    chain_refs, last_refs, refs = refs[3 : 3 + chain_count], refs[3 + chain_count : 5 + chain_count], refs[5 + chain_count :]
    gathered_ref, slope_ref, term_ref, rising_ref, falling_ref, own_ref, sum_ref, last_sem = refs[:8]
    buffers = 5 if size == 4 else 4
    scatter = Scatter(size, *refs[8 : 8 + buffers])
    gather = Gather(size, own_ref, gathered_ref, *refs[8 + buffers : 12 + buffers])
    chain = Chain(
        chips, steps, chain_refs[: len(steps)], chain_refs[len(steps) : -2], *chain_refs[-2:],
        *refs[12 + buffers :],
    )
    last_loads = [
        pltpu.make_async_copy(source, target, last_sem.at[index])
        for index, (source, target) in enumerate(zip(last_refs, (rising_ref, falling_ref)))
    ]
    chain.load()
    scatter.load(operands)
    for load in last_loads:
        load.start()
    greet(neighbours(size) + chain.neighbours)
    chain.step(0)
    scatter.fill(operands)
    scatter.relay()
    sum_ref[...] = jnp.zeros_like(sum_ref)
    scatter.collect()

    def norm(piece):
        back = scatter.total(piece)
        state = state_ref[piece, :]
        scale = row_scale(state)
        unit = state * scale
        sum_ref[...] += jnp.sum(back * unit, axis=0, keepdims=True)
        unit_slope = back * gain_ref[...]
        slope = cotangent_ref[piece, :].astype(jnp.float32) + scale * (
            unit_slope - unit * jnp.mean(unit_slope * unit, axis=-1, keepdims=True)
        )
        slope_ref[piece, :] = slope
        own_ref[piece, :] = slope.astype(own_ref.dtype)

    over_pieces(own_ref.shape[0], norm)
    gather.start()
    store_row(term_ref, sum_ref)
    chain.wait(0)
    for index in range(1, len(steps)):
        chain.step(index)
        chain.wait(index)
    for load in last_loads:
        load.wait()
    last = len(steps)
    for needed, landing, out_ref in (
        ((chain.chip > 0) & (chain.chip < chips - 1), chain.up, rising_ref),
        ((chain.chip > 0) & (chain.chip < chips - 1), chain.down, falling_ref),
    ):

        @pl.when(needed)
        def _(landing=landing, out_ref=out_ref):
            def add(piece):
                out_ref[piece, :] = add_rounded(out_ref[piece, :], landing[last, piece, :])

            over_pieces(out_ref.shape[0], add)

    gather.finish()
    scatter.drain()
    chain.drain()


def last_kernel(sizes, first_columns, *refs):
    data_size, size = sizes
    operands, refs = split_operands(refs, size, first_columns)
    input_ref, gain_ref, slope_ref, terms_ref, rows_ref = refs[:5]
    gradient_ref, terms_out_ref, sum_ref, partial_ref, group_ref, inner, outer = refs[5:12]
    inner_send, inner_recv, outer_send, outer_recv = refs[12:16]
    mixing = Scatter(size, *refs[16:])
    rows = gradient_ref.shape[0]
    mixing.load(operands)
    greet(
        [("tensor", peer) for peer in other_members("tensor", size)]
        + [("dp", peer) for peer in other_members("dp", data_size)]
    )
    sum_ref[...] = jnp.zeros_like(sum_ref)

    def look(owner, columns, values):
        piece = pl.ds(pl.multiple_of(owner * rows, rows), rows)
        sum_ref[:, columns] += jnp.sum(
            values * rows_ref[piece, columns].astype(jnp.float32), axis=0, keepdims=True
        )

    mixing.fill(operands, look)
    sum_ref[...] = sum_ref[...] / gain_ref[...]
    kept = partial_ref.shape[0] - terms_ref.shape[0]
    partial_ref[kept:, :] = terms_ref[...]
    store_row(partial_ref, sum_ref)
    inner_copies = send_terms(
        "tensor", other_members("tensor", size), partial_ref, inner, inner_send, inner_recv
    )
    mixing.relay()
    group_ref[...] = add_terms(inner, inner_copies)
    outer_copies = send_terms(
        "dp", other_members("dp", data_size), group_ref, outer, outer_send, outer_recv
    )
    terms_out_ref[...] = add_terms(outer, outer_copies)
    mixing.collect()

    def norm(piece):
        back = mixing.total(piece)
        values = input_ref[piece, :].astype(jnp.float32)
        scale = row_scale(values)
        unit = values * scale
        unit_slope = back * gain_ref[...]
        gradient_ref[piece, :] = (
            slope_ref[piece, :]
            + scale * (unit_slope - unit * jnp.mean(unit_slope * unit, axis=-1, keepdims=True))
        ).astype(gradient_ref.dtype)

    over_pieces(rows, norm)
    for copy in inner_copies + outer_copies:
        copy.wait_send()
    mixing.drain()


def scatter_call(body, triples, size, others, far, outs, gathered, scratch, collective_id):
    far_spec = pl.BlockSpec(memory_space=pl.ANY)
    operands = [array for left, weight, _ in triples for array in (left, weight)]
    in_specs = [far_spec] * len(operands)
    for other in others:
        in_specs.append(pl.BlockSpec(other.shape, lambda i: (0, 0), pipeline_mode=pl.Buffered(1)))
    in_specs += [far_spec] * len(far)
    out_specs = [pl.BlockSpec(out.shape, lambda i: (0, 0)) for out in outs]
    if gathered:
        out_specs[0] = far_spec
    return pl.pallas_call(
        functools.partial(body, tuple(first for _, _, first in triples)),
        grid=(1,),
        out_shape=outs,
        in_specs=in_specs,
        out_specs=out_specs,
        scratch_shapes=list(scratch)
        + [part for left, weight, _ in triples for part in Operand.scratch(size, left, weight)],
        compiler_params=pltpu.CompilerParams(
            collective_id=collective_id, has_side_effects=True, vmem_limit_bytes=VMEM_LIMIT
        ),
        cost_estimate=pl.CostEstimate(
            flops=sum(2 * left.size * weight.shape[0] for left, weight, _ in triples),
            bytes_accessed=150_000_000,
            transcendentals=0,
        ),
    )(*operands, *others, *far)


LOG2E = 1.4426950408889634


def turn_tables(head_size):
    half_size = head_size // 2
    frequency = np.float32(rope_base) ** (
        -(np.arange(half_size, dtype=np.float32) * np.float32(2.0) / np.float32(head_size))
    )
    frequency = frequency.astype(np.float64)
    sign = np.concatenate([-np.ones(half_size), np.ones(half_size)])[None, :]
    positions = np.concatenate([np.arange(0, SEQUENCE_LENGTH, 128), np.arange(128)])
    angles = positions[:, None] * np.concatenate([frequency, frequency])[None, :]
    return np.cos(angles).astype(np.float32), (sign * np.sin(angles)).astype(np.float32)


def fill_tables(few_cosines_ref, few_sines_ref, cosine_ref, sine_ref):
    coarse = few_cosines_ref.shape[0] - 128
    near_cosine, near_sine = few_cosines_ref[coarse:, :], few_sines_ref[coarse:, :]

    def step(index, carry):
        far_cosine = few_cosines_ref[pl.ds(index, 1), :]
        far_sine = few_sines_ref[pl.ds(index, 1), :]
        rows = pl.ds(pl.multiple_of(index * 128, 128), 128)
        cosine_ref[rows, :] = far_cosine * near_cosine - far_sine * near_sine
        sine_ref[rows, :] = far_sine * near_cosine + far_cosine * near_sine
        return carry

    lax.fori_loop(0, coarse, step, 0)


def turn(values, cosine, sine):
    return values * cosine + pltpu.roll(values, values.shape[-1] // 2, 1) * sine


def turn_back(values, cosine, sine):
    return values * cosine - pltpu.roll(values, values.shape[-1] // 2, 1) * sine


def contract_first(first_operand, second_operand):
    return lax.dot_general(
        first_operand, second_operand, (((0,), (0,)), ((), ())), preferred_element_type=jnp.float32
    )


def visible_scores(key_rows, query_rows, first_row, multiplier):
    scores = times_transposed(key_rows, query_rows) * multiplier
    _, queries = scores.shape
    key_at = lax.broadcasted_iota(jnp.int32, (queries, queries), 0)
    query_at = lax.broadcasted_iota(jnp.int32, (queries, queries), 1)
    corner = jnp.where(query_at >= key_at, scores[first_row:], -1e30)
    if first_row == 0:
        return corner
    return jnp.concatenate([scores[:first_row], corner], axis=0)


def turn_heads(
    grouping, head_size, raw_ref, query_gain_ref, key_gain_ref, cosine_ref, sine_ref, query_ref, key_ref, value_ref
):
    def turned(start, gain):
        raw = raw_ref[:, pl.ds(start, head_size)]
        return turn(raw * row_scale(raw) * gain, cosine_ref[...], sine_ref[...]).astype(jnp.bfloat16)

    def step(part, carry):
        query_ref[part] = turned(pl.multiple_of(part * head_size, head_size), query_gain_ref[...])
        return carry

    lax.fori_loop(0, grouping, step, 0)
    key_ref[...] = turned(grouping * head_size, key_gain_ref[...])
    value_ref[...] = raw_ref[:, (grouping + 1) * head_size :].astype(jnp.bfloat16)


def attention_forward_kernel(
    grouping, head_size, block, rows_ref, weight_ref, few_cosines_ref, few_sines_ref, query_gain_ref, key_gain_ref,
    raw_ref, mixed_ref, total_ref, query_ref, key_ref, value_ref, cosine_ref, sine_ref,
):
    sequence = rows_ref.shape[0]
    multiplier = head_size ** (-0.5) * LOG2E

    @pl.when((pl.program_id(0) == 0) & (pl.program_id(1) == 0))
    def _():
        fill_tables(few_cosines_ref, few_sines_ref, cosine_ref, sine_ref)

    raw_ref[...] = simple_product(rows_ref[...], weight_ref[...])
    turn_heads(
        grouping, head_size, raw_ref, query_gain_ref, key_gain_ref, cosine_ref, sine_ref, query_ref, key_ref, value_ref
    )

    def head_step(part, carry):
        lanes = pl.ds(pl.multiple_of(part * head_size, head_size), head_size)
        for first_row in range(0, sequence, block):
            last_row = first_row + block
            scores = visible_scores(
                key_ref[:last_row, :], query_ref[part, first_row:last_row, :], first_row, multiplier
            )
            highest = jnp.max(scores, axis=0, keepdims=True)
            weights = jnp.exp2(scores - highest)
            total = jnp.sum(weights, axis=0, keepdims=True)
            weights = (weights * (1.0 / total)).astype(jnp.bfloat16)
            mixed_ref[first_row:last_row, lanes] = contract_first(
                weights, value_ref[:last_row, :]
            ).astype(mixed_ref.dtype)
            total_ref[0, pl.ds(part, 1), first_row:last_row] = highest + jnp.log2(total)
        return carry

    lax.fori_loop(0, grouping, head_step, 0)


def attention_forward(rows, weight, tables, query_gain, key_gain, heads, grouping):
    total_rows, depth = rows.shape
    head_size = query_gain.shape[0]
    sequences = total_rows // SEQUENCE_LENGTH
    width = (grouping + 2) * head_size
    block = min(256, SEQUENCE_LENGTH)
    table = pl.BlockSpec(tables[0].shape, lambda s, h: (0, 0))
    gain = pl.BlockSpec((1, head_size), lambda s, h: (0, 0))
    elements = heads * grouping * total_rows * SEQUENCE_LENGTH // 2
    return pl.pallas_call(
        functools.partial(attention_forward_kernel, grouping, head_size, block),
        grid=(sequences, heads),
        out_shape=[
            jax.ShapeDtypeStruct((total_rows, heads * width), jnp.float32),
            jax.ShapeDtypeStruct((total_rows, heads * grouping * head_size), jnp.bfloat16),
            jax.ShapeDtypeStruct((heads, grouping, total_rows), jnp.float32),
        ],
        in_specs=[
            pl.BlockSpec((SEQUENCE_LENGTH, depth), lambda s, h: (s, 0)),
            pl.BlockSpec((depth, width), lambda s, h: (0, h)),
            table,
            table,
            gain,
            gain,
        ],
        out_specs=[
            pl.BlockSpec((SEQUENCE_LENGTH, width), lambda s, h: (s, h)),
            pl.BlockSpec((SEQUENCE_LENGTH, grouping * head_size), lambda s, h: (s, h)),
            pl.BlockSpec((1, grouping, SEQUENCE_LENGTH), lambda s, h: (h, 0, s)),
        ],
        scratch_shapes=[
            pltpu.VMEM((grouping, SEQUENCE_LENGTH, head_size), jnp.bfloat16),
            pltpu.VMEM((SEQUENCE_LENGTH, head_size), jnp.bfloat16),
            pltpu.VMEM((SEQUENCE_LENGTH, head_size), jnp.bfloat16),
            pltpu.VMEM((SEQUENCE_LENGTH, head_size), jnp.float32),
            pltpu.VMEM((SEQUENCE_LENGTH, head_size), jnp.float32),
        ],
        compiler_params=pltpu.CompilerParams(vmem_limit_bytes=VMEM_LIMIT),
        cost_estimate=pl.CostEstimate(
            flops=2 * total_rows * depth * heads * width + 4 * elements * head_size,
            bytes_accessed=2 * (total_rows * depth + depth * heads * width),
            transcendentals=elements,
        ),
        name="attention_forward",
    )(rows, weight, *tables, query_gain.reshape(1, -1), key_gain.reshape(1, -1))


def norm_back(turned_slope, raw, gain, cosine, sine):
    norm_slope = turn_back(turned_slope, cosine, sine)
    scale = row_scale(raw)
    unit = raw * scale
    term = norm_slope * unit
    unit_slope = norm_slope * gain
    slope = scale * (unit_slope - unit * jnp.mean(unit_slope * unit, axis=-1, keepdims=True))
    return slope.astype(jnp.bfloat16), jnp.sum(term, axis=0, keepdims=True)


def attention_backward_kernel(size, grouping, head_size, block, first_columns, *refs):
    operands, refs = split_operands(refs, size, first_columns)
    (
        state_ref, weight_ref, raw_ref, mixed_ref, total_ref, few_cosines_ref, few_sines_ref,
        query_gain_ref, key_gain_ref, hidden_state_ref, slope_ref, gain_ref, output_ref,
        query_ref, key_ref, value_ref, out_slope_ref, turned_ref, key_sum_ref, value_sum_ref, cosine_ref, sine_ref,
    ) = refs[:22]
    scatter = Scatter(size, *refs[22:])
    step = pl.program_id(0) * pl.num_programs(1) + pl.program_id(1)
    steps = pl.num_programs(0) * pl.num_programs(1)

    @pl.when(step == 0)
    def _():
        scatter.load(operands)
        greet(neighbours(size))
        scatter.fill(operands)

    attend_backward_head(
        grouping, head_size, block, state_ref, weight_ref, raw_ref, mixed_ref, total_ref, few_cosines_ref,
        few_sines_ref, query_gain_ref, key_gain_ref, slope_ref, gain_ref, query_ref, key_ref, value_ref,
        out_slope_ref, turned_ref, key_sum_ref, value_sum_ref, cosine_ref, sine_ref,
    )

    @pl.when(step == 0)
    def _():
        scatter.relay()

    @pl.when(step == steps - 1)
    def _():
        scatter.collect()

        def finish(piece):
            output_ref[piece, :] = (hidden_state_ref[piece, :] + scatter.total(piece)).astype(
                output_ref.dtype
            )

        over_pieces(output_ref.shape[0], finish)
        scatter.drain()


def attend_backward_head(
    grouping, head_size, block, state_ref, weight_ref, raw_ref, mixed_ref, total_ref, few_cosines_ref, few_sines_ref,
    query_gain_ref, key_gain_ref, slope_ref, gain_ref, query_ref, key_ref, value_ref, out_slope_ref,
    turned_ref, key_sum_ref, value_sum_ref, cosine_ref, sine_ref,
):
    sequence = state_ref.shape[0]
    scale_factor = head_size ** (-0.5)
    multiplier = scale_factor * LOG2E

    @pl.when((pl.program_id(0) == 0) & (pl.program_id(1) == 0))
    def _():
        gain_ref[...] = jnp.zeros_like(gain_ref)
        fill_tables(few_cosines_ref, few_sines_ref, cosine_ref, sine_ref)

    out_slope_ref[...] = simple_product(state_ref[...], weight_ref[...]).astype(jnp.bfloat16)
    turn_heads(
        grouping, head_size, raw_ref, query_gain_ref, key_gain_ref, cosine_ref, sine_ref, query_ref, key_ref, value_ref
    )
    key_sum_ref[...] = jnp.zeros_like(key_sum_ref)
    value_sum_ref[...] = jnp.zeros_like(value_sum_ref)
    ones = jnp.ones((8, head_size), jnp.float32)

    def head_step(part, carry):
        lanes = pl.ds(pl.multiple_of(part * head_size, head_size), head_size)
        for first_row in range(0, sequence, block):
            last_row = first_row + block
            query_rows = query_ref[part, first_row:last_row, :]
            slope_rows = out_slope_ref[first_row:last_row, lanes]
            scores = visible_scores(key_ref[:last_row, :], query_rows, first_row, multiplier)
            weights = jnp.exp2(scores - total_ref[0, pl.ds(part, 1), first_row:last_row])
            value_sum_ref[:last_row, :] += simple_product(weights.astype(jnp.bfloat16), slope_rows)
            product = slope_rows.astype(jnp.float32) * mixed_ref[first_row:last_row, lanes].astype(jnp.float32)
            centre = lax.dot_general(
                ones,
                product,
                (((1,), (1,)), ((), ())),
                preferred_element_type=jnp.float32,
                precision=lax.Precision.HIGHEST,
            )[:1]
            weight_slope = times_transposed(value_ref[:last_row, :], slope_rows)
            score_slope = (weights * (weight_slope - centre)).astype(jnp.bfloat16)
            key_sum_ref[:last_row, :] += simple_product(score_slope, query_rows)
            turned_ref[first_row:last_row, :] = (
                contract_first(score_slope, key_ref[:last_row, :]) * scale_factor
            )
        slope, term = norm_back(
            turned_ref[...], raw_ref[:, lanes], query_gain_ref[...], cosine_ref[...], sine_ref[...]
        )
        slope_ref[:, lanes] = slope
        gain_ref[0:1, :] += term
        return carry

    lax.fori_loop(0, grouping, head_step, 0)
    lanes = slice(grouping * head_size, (grouping + 1) * head_size)
    slope, term = norm_back(
        key_sum_ref[...] * scale_factor, raw_ref[:, lanes], key_gain_ref[...], cosine_ref[...], sine_ref[...]
    )
    slope_ref[:, lanes] = slope
    gain_ref[1:2, :] += term
    slope_ref[:, (grouping + 1) * head_size :] = value_sum_ref[...].astype(jnp.bfloat16)


def attention_backward(
    state_rows, weight, weight_start, raw, mixed, totals, tables, query_gain, key_gain, heads, grouping,
    triples, hidden_state, size, collective_id,
):
    total_rows, depth = state_rows.shape
    head_size = query_gain.shape[0]
    sequences = total_rows // SEQUENCE_LENGTH
    width = (grouping + 2) * head_size
    out_width = grouping * head_size
    block = min(256, SEQUENCE_LENGTH)
    first_block = weight_start // out_width
    single = pl.Buffered(1)
    table = pl.BlockSpec(tables[0].shape, lambda s, h: (0, 0))
    gain = pl.BlockSpec((1, head_size), lambda s, h: (0, 0))
    elements = heads * grouping * total_rows * SEQUENCE_LENGTH // 2
    whole_rows = pltpu.VMEM((SEQUENCE_LENGTH, head_size), jnp.float32)
    operands = [array for left, other_weight, _ in triples for array in (left, other_weight)]
    in_specs = [pl.BlockSpec(memory_space=pl.ANY)] * len(operands)
    in_specs += [
        pl.BlockSpec((SEQUENCE_LENGTH, depth), lambda s, h: (s, 0), pipeline_mode=single),
        pl.BlockSpec((depth, out_width), lambda s, h: (0, first_block + h)),
        pl.BlockSpec((SEQUENCE_LENGTH, width), lambda s, h: (s, h)),
        pl.BlockSpec((SEQUENCE_LENGTH, out_width), lambda s, h: (s, h)),
        pl.BlockSpec((1, grouping, SEQUENCE_LENGTH), lambda s, h: (h, 0, s)),
        table,
        table,
        gain,
        gain,
        pl.BlockSpec(hidden_state.shape, lambda s, h: (0, 0), pipeline_mode=single),
    ]
    operands += [
        state_rows, weight, raw, mixed, totals, *tables, query_gain.reshape(1, -1), key_gain.reshape(1, -1),
        hidden_state,
    ]
    return pl.pallas_call(
        functools.partial(
            attention_backward_kernel, size, grouping, head_size, block,
            tuple(first for _, _, first in triples),
        ),
        grid=(sequences, heads),
        out_shape=[
            jax.ShapeDtypeStruct((total_rows, heads * width), jnp.bfloat16),
            jax.ShapeDtypeStruct((8, head_size), jnp.float32),
            jax.ShapeDtypeStruct(hidden_state.shape, jnp.bfloat16),
        ],
        in_specs=in_specs,
        out_specs=[
            pl.BlockSpec((SEQUENCE_LENGTH, width), lambda s, h: (s, h)),
            pl.BlockSpec((8, head_size), lambda s, h: (0, 0)),
            pl.BlockSpec(hidden_state.shape, lambda s, h: (0, 0)),
        ],
        scratch_shapes=[
            pltpu.VMEM((grouping, SEQUENCE_LENGTH, head_size), jnp.bfloat16),
            pltpu.VMEM((SEQUENCE_LENGTH, head_size), jnp.bfloat16),
            pltpu.VMEM((SEQUENCE_LENGTH, head_size), jnp.bfloat16),
            pltpu.VMEM((SEQUENCE_LENGTH, out_width), jnp.bfloat16),
            whole_rows,
            whole_rows,
            whole_rows,
            whole_rows,
            whole_rows,
            *Scatter.scratch(size, *hidden_state.shape),
            *[part for left, other, _ in triples for part in Operand.scratch(size, left, other)],
        ],
        compiler_params=pltpu.CompilerParams(
            collective_id=collective_id, has_side_effects=True, vmem_limit_bytes=VMEM_LIMIT
        ),
        cost_estimate=pl.CostEstimate(
            flops=2 * total_rows * depth * heads * out_width + 10 * elements * head_size,
            bytes_accessed=100_000_000,
            transcendentals=elements,
        ),
        name="attention_backward",
    )(*operands)


def feed_half_kernel(half, tile, rows_ref, cotangent_ref, weight_ref, hidden_ref, slope_ref):
    rows, cotangent = rows_ref[...], cotangent_ref[...]

    def step(index, carry):
        start = pl.multiple_of(index * tile, tile)
        gate = simple_product(rows, weight_ref[:, pl.ds(start, tile)])
        up = simple_product(rows, weight_ref[:, pl.ds(half + start, tile)])
        back = simple_product(cotangent, weight_ref[:, pl.ds(2 * half + start, tile)])
        sigmoid = 1.0 / (1.0 + jnp.exp(-gate))
        gated = gate * sigmoid
        hidden_ref[:, pl.ds(start, tile)] = (gated * up).astype(jnp.bfloat16)
        slope_ref[:, pl.ds(start, tile)] = (
            back * up * sigmoid * (1.0 + gate * (1.0 - sigmoid))
        ).astype(jnp.bfloat16)
        slope_ref[:, pl.ds(half + start, tile)] = (back * gated).astype(jnp.bfloat16)
        return carry

    lax.fori_loop(0, half // tile, step, 0)


def feed_half(rows, cotangent, weight):
    total_rows, depth = rows.shape
    half = weight.shape[1] // 3
    block = min(512, total_rows)
    tile = 256 if half % 256 == 0 else 128
    row_block = pl.BlockSpec((block, depth), lambda i: (i, 0))
    return pl.pallas_call(
        functools.partial(feed_half_kernel, half, tile),
        grid=(total_rows // block,),
        out_shape=[
            jax.ShapeDtypeStruct((total_rows, half), jnp.bfloat16),
            jax.ShapeDtypeStruct((total_rows, 2 * half), jnp.bfloat16),
        ],
        in_specs=[
            row_block,
            row_block,
            pl.BlockSpec(weight.shape, lambda i: (0, 0), pipeline_mode=pl.Buffered(1)),
        ],
        out_specs=[
            pl.BlockSpec((block, half), lambda i: (i, 0)),
            pl.BlockSpec((block, 2 * half), lambda i: (i, 0)),
        ],
        compiler_params=pltpu.CompilerParams(vmem_limit_bytes=VMEM_LIMIT),
        cost_estimate=pl.CostEstimate(
            flops=6 * total_rows * depth * half,
            bytes_accessed=2 * (2 * total_rows * depth + 3 * depth * half),
            transcendentals=total_rows * half,
        ),
        name="feed_half",
    )(rows, cotangent, weight)


def grad_kernel(pair_count, with_other, order_ref, *refs):
    pairs = [refs[2 * p : 2 * p + 2] for p in range(pair_count)]
    refs = refs[2 * pair_count :]
    step = pl.program_id(0)
    if with_other:
        other_ref, refs = refs[0], refs[1:]
        out_refs, held_ref, copy_sem = refs[:-3], refs[-3], refs[-2]
    else:
        out_ref = refs[0]
    turned_ref = refs[-1]
    start = 0
    for left_ref, right_ref in pairs:
        turned_ref[...] = left_ref[...].T
        width = right_ref.shape[1]
        tile = next(t for t in (768, 512, 384, 256, 128) if width % t == 0)
        for column in range(0, width, tile):
            values = simple_product(turned_ref[...], right_ref[:, column : column + tile])
            columns = slice(start + column, start + column + tile)
            if with_other:
                values = values + other_ref[0, :, columns].astype(jnp.float32)
                held_ref[step, :, columns] = values.astype(jnp.bfloat16)
            else:
                out_ref[0, :, columns] = values.astype(jnp.bfloat16)
        start += width
    if with_other:
        copies = [
            pltpu.make_async_copy(held_ref.at[index], out_ref, copy_sem.at[index])
            for index, out_ref in enumerate(out_refs)
        ]
        for index, copy in enumerate(copies):
            pl.when(step == index)(copy.start)

        @pl.when(step == len(copies) - 1)
        def _():
            for copy in copies:
                copy.wait()


def grad_blocks(order, pairs, other=None):
    count = order.shape[0]
    total_rows, depth = pairs[0][0].shape
    block = depth // lax.axis_size("dp")
    width = sum(right.shape[1] for _, right in pairs)
    in_specs = []
    operands = []
    for left, right in pairs:
        in_specs += [
            pl.BlockSpec((total_rows, block), lambda k, at: (0, at[k])),
            pl.BlockSpec(right.shape, lambda k, at: (0, 0), pipeline_mode=pl.Buffered(1)),
        ]
        operands += [left, right]
    scratch = [pltpu.VMEM((block, total_rows), jnp.bfloat16)]
    if other is not None:
        in_specs.append(pl.BlockSpec((1, block, width), lambda k, at: (k, 0, 0)))
        operands.append(other)
        out_shape = [jax.ShapeDtypeStruct((block, width), jnp.bfloat16)] * count
        out_specs = [pl.BlockSpec(memory_space=pl.ANY)] * count
        scratch = [
            pltpu.VMEM((count, block, width), jnp.bfloat16),
            pltpu.SemaphoreType.DMA((count,)),
        ] + scratch
    else:
        out_shape = [jax.ShapeDtypeStruct((count, block, width), jnp.bfloat16)]
        out_specs = [pl.BlockSpec((1, block, width), lambda k, at: (k, 0, 0))]
    out = pl.pallas_call(
        functools.partial(grad_kernel, len(pairs), other is not None),
        grid_spec=pltpu.PrefetchScalarGridSpec(
            num_scalar_prefetch=1,
            grid=(count,),
            in_specs=in_specs,
            out_specs=out_specs,
            scratch_shapes=scratch,
        ),
        out_shape=out_shape,
        compiler_params=pltpu.CompilerParams(vmem_limit_bytes=VMEM_LIMIT),
        cost_estimate=pl.CostEstimate(
            flops=2 * total_rows * count * block * width,
            bytes_accessed=2 * (total_rows * count * block * len(pairs) + width * (total_rows + count * block)),
            transcendentals=0,
        ),
        name="grad_blocks",
    )(order, *operands)
    return out if other is not None else out[0]


def reduce_over_chips(pairs, sizes):
    data_size = sizes[0]
    chips = data_size // 2
    me = lax.axis_index("dp")
    chip, core = me // 2, lax.rem(me, 2)
    ahead = lax.rem(chip + jnp.arange(chips, dtype=jnp.int32), chips) * 2
    other = lax.ppermute(
        grad_blocks(ahead + (1 - core), pairs),
        "dp",
        [(device, device ^ 1) for device in range(data_size)],
    )
    blocks = grad_blocks(ahead + core, pairs, other)
    up = lax.ppermute(blocks[chips - 1], "dp", [(device, device + 2) for device in range(2)])
    down = lax.ppermute(
        blocks[1],
        "dp",
        [(device, device - 2) for device in range(data_size - 2, data_size)],
    )
    return blocks, up, down


def pack_mixing_kernel(heads, query_ref, key_ref, value_ref, output_ref, out_ref):
    query_width = query_ref.shape[1] // heads
    head_size = key_ref.shape[1] // heads
    start = 0
    for head in range(heads):
        for ref, part in ((query_ref, query_width), (key_ref, head_size), (value_ref, head_size)):
            out_ref[:, start : start + part] = ref[:, head * part : (head + 1) * part]
            start += part
    out_ref[:, start:] = output_ref[...].T


def pack_feed_kernel(gate_ref, up_ref, down_ref, first_ref, second_ref):
    start = 0
    for out_ref in (first_ref, second_ref):
        width = out_ref.shape[1] // 3
        part = slice(start, start + width)
        out_ref[:, :width] = gate_ref[:, part]
        out_ref[:, width : 2 * width] = up_ref[:, part]
        out_ref[:, 2 * width :] = down_ref[part, :].T
        start += width


def finish_mixing_kernel(heads, total_ref, output_total_ref, query_ref, key_ref, value_ref, output_ref):
    query_width = query_ref.shape[1] // heads
    head_size = key_ref.shape[1] // heads
    start = 0
    for head in range(heads):
        for ref, part in ((query_ref, query_width), (key_ref, head_size), (value_ref, head_size)):
            ref[:, head * part : (head + 1) * part] = total_ref[:, start : start + part].astype(
                jnp.float32
            )
            start += part
    output_ref[...] = output_total_ref[...].astype(jnp.float32).T


def finish_feed_kernel(own_ref, up_ref, down_ref, second_ref, gate_out_ref, up_out_ref, down_out_ref):
    start = 0
    for total_refs in ((own_ref, up_ref, down_ref), (second_ref,)):
        width = total_refs[0].shape[1] // 3
        part = slice(start, start + width)

        def total(index):
            columns = slice(index * width, (index + 1) * width)
            return sum(ref[:, columns].astype(jnp.float32) for ref in total_refs)

        gate_out_ref[:, part] = total(0)
        up_out_ref[:, part] = total(1)
        down_out_ref[part, :] = total(2).T
        start += width


def whole_call(body, shapes, *operands):
    return pl.pallas_call(
        body,
        out_shape=shapes,
        in_specs=[pl.BlockSpec(memory_space=pltpu.VMEM)] * len(operands),
        out_specs=[pl.BlockSpec(memory_space=pltpu.VMEM)] * len(shapes),
        compiler_params=pltpu.CompilerParams(vmem_limit_bytes=VMEM_LIMIT),
        cost_estimate=pl.CostEstimate(
            flops=0, bytes_accessed=4 * sum(operand.size for operand in operands), transcendentals=0
        ),
    )(*operands)


def per_device(
    block_input,
    attention_gain,
    query_weight,
    key_matrix,
    value_matrix,
    query_gain,
    key_gain,
    output_weight,
    feed_gain,
    gate_weight,
    up_weight,
    down_weight,
    out_cotangent,
):
    size = lax.axis_size("tensor")
    sizes = (lax.axis_size("dp"), size)
    model_width = block_input.shape[1]
    head_size = query_gain.shape[0]
    query_columns = query_weight.shape[1]
    key_columns = key_matrix.shape[1]
    heads = key_columns // head_size
    grouping = query_columns // key_columns
    hidden_columns = gate_weight.shape[1]
    qkv_columns = query_columns + 2 * key_columns
    first_columns = hidden_columns * 2 // 3 // 256 * 256 or hidden_columns // 2
    second_columns = hidden_columns - first_columns
    tables = turn_tables(head_size)

    block_width = query_weight.shape[0]
    (mixing_local,) = whole_call(
        functools.partial(pack_mixing_kernel, heads),
        [jax.ShapeDtypeStruct((block_width, qkv_columns + query_columns), jnp.bfloat16)],
        query_weight, key_matrix, value_matrix, output_weight,
    )
    mixing_full = lax.all_gather(mixing_local, "dp", axis=0, tiled=True)
    feed_locals = whole_call(
        pack_feed_kernel,
        [
            jax.ShapeDtypeStruct((block_width, 3 * columns), jnp.bfloat16)
            for columns in (first_columns, second_columns)
        ],
        gate_weight, up_weight, down_weight,
    )
    feed_full = [lax.all_gather(part, "dp", axis=0, tiled=True) for part in feed_locals]

    input_float = block_input.astype(jnp.float32)
    first_scale = row_scale(input_float)
    first_unit = input_float * first_scale
    mixer_local = (first_unit * attention_gain).astype(jnp.bfloat16)
    mixer_rows, cotangent_rows = gather_rows((mixer_local, out_cotangent), size, 0)

    raw, mixed_rows, totals = attention_forward(
        mixer_rows, mixing_full, tables, query_gain, key_gain, heads, grouping
    )
    local_shape = block_input.shape
    local_rows = local_shape[0]
    gain_rows = model_width // head_size
    gathered_shape = jax.ShapeDtypeStruct((size * local_rows, model_width), jnp.bfloat16)
    local_float = jax.ShapeDtypeStruct(local_shape, jnp.float32)
    local_half = jax.ShapeDtypeStruct(local_shape, jnp.bfloat16)
    row_sum = pltpu.VMEM((1, model_width), jnp.float32)
    own_rows = pltpu.VMEM(local_shape, jnp.bfloat16)
    scatter_scratch = Scatter.scratch(size, *local_shape)
    gather_scratch = Gather.scratch(size, *local_shape)
    feed_rows, hidden_state = scatter_call(
        functools.partial(between_forward_kernel, size),
        [(mixed_rows, mixing_full, qkv_columns)],
        size,
        [block_input, feed_gain.reshape(1, -1)],
        [],
        [gathered_shape, local_float],
        True,
        [own_rows, *scatter_scratch, *gather_scratch],
        1,
    )

    hidden_first, slope_first = feed_half(feed_rows, cotangent_rows, feed_full[0])
    blocks, up, down = reduce_over_chips(
        [(feed_rows, slope_first), (cotangent_rows, hidden_first)], sizes
    )
    blocks, later_full = lax.optimization_barrier((blocks, feed_full[1]))
    hidden_second, slope_second = feed_half(feed_rows, cotangent_rows, later_full)
    plain_order = jnp.arange(sizes[0], dtype=jnp.int32)
    second_grad = grad_blocks(
        plain_order, [(feed_rows, slope_second), (cotangent_rows, hidden_second)]
    ).reshape(model_width, -1)
    second_grad, slope_second = lax.optimization_barrier((second_grad, slope_second))
    second_total = lax.psum_scatter(second_grad, "dp", scatter_dimension=0, tiled=True)
    chips = sizes[0] // 2
    middle_steps = tuple(range(2, chips - 1))
    chain_block = jax.ShapeDtypeStruct(blocks[0].shape, jnp.bfloat16)
    state_rows, state_slope, feed_term, rising, falling = scatter_call(
        functools.partial(between_backward_kernel, size, chips, middle_steps),
        [(slope_first, feed_full[0], 0), (slope_second, later_full, 0)],
        size,
        [hidden_state, out_cotangent, feed_gain.reshape(1, -1)],
        [blocks[chips - step] for step in middle_steps]
        + [blocks[step] for step in middle_steps]
        + [up, down, blocks[1], blocks[chips - 1]],
        [
            gathered_shape,
            local_float,
            jax.ShapeDtypeStruct((gain_rows, head_size), jnp.float32),
            chain_block,
            chain_block,
        ],
        True,
        [
            own_rows,
            row_sum,
            pltpu.SemaphoreType.DMA((2,)),
            *scatter_scratch,
            *gather_scratch,
            *Chain.scratch(len(middle_steps), *blocks[0].shape),
        ],
        2,
    )
    up = lax.ppermute(
        rising, "dp", [(device, device + 2) for device in range(sizes[0] - 2)]
    )
    down = lax.ppermute(
        falling, "dp", [(device, device - 2) for device in range(2, sizes[0])]
    )
    output_grad = grad_blocks(plain_order, [(state_rows, mixed_rows)]).reshape(model_width, -1)
    output_grad, state_rows = lax.optimization_barrier((output_grad, state_rows))
    output_total = lax.psum_scatter(output_grad, "dp", scatter_dimension=0, tiled=True)
    qkv_slope, head_terms, block_output = attention_backward(
        state_rows, mixing_full, qkv_columns, raw, mixed_rows, totals, tables,
        query_gain, key_gain, heads, grouping,
        [
            (hidden_first, feed_full[0], 2 * first_columns),
            (hidden_second, later_full, 2 * second_columns),
        ],
        hidden_state, size, 4,
    )
    mixing_grad = grad_blocks(plain_order, [(mixer_rows, qkv_slope)]).reshape(model_width, -1)
    mixing_grad, qkv_slope = lax.optimization_barrier((mixing_grad, qkv_slope))
    mixing_total = lax.psum_scatter(mixing_grad, "dp", scatter_dimension=0, tiled=True)
    terms_shape = (2 * gain_rows + head_terms.shape[0], head_size)
    input_gradient, terms = scatter_call(
        functools.partial(last_kernel, sizes),
        [(qkv_slope, mixing_full, 0)],
        size,
        [
            block_input,
            attention_gain.reshape(1, -1),
            state_slope,
            jnp.concatenate([feed_term, head_terms], axis=0),
            mixer_rows,
        ],
        [],
        [local_half, jax.ShapeDtypeStruct(terms_shape, jnp.float32)],
        False,
        [
            row_sum,
            pltpu.VMEM(terms_shape, jnp.float32),
            pltpu.VMEM(terms_shape, jnp.float32),
            pltpu.VMEM((size, *terms_shape), jnp.float32),
            pltpu.VMEM((sizes[0], *terms_shape), jnp.float32),
            *[pltpu.SemaphoreType.DMA((count - 1,)) for count in (size, size, *sizes[:1] * 2)],
            *scatter_scratch,
        ],
        3,
    )
    query_gradient, key_gradient, value_gradient, output_gradient = whole_call(
        functools.partial(finish_mixing_kernel, heads),
        [
            jax.ShapeDtypeStruct((block_width, query_columns), jnp.float32),
            jax.ShapeDtypeStruct((block_width, key_columns), jnp.float32),
            jax.ShapeDtypeStruct((block_width, key_columns), jnp.float32),
            jax.ShapeDtypeStruct((query_columns, block_width), jnp.float32),
        ],
        mixing_total, output_total,
    )
    gate_gradient, up_gradient, down_gradient = whole_call(
        finish_feed_kernel,
        [
            jax.ShapeDtypeStruct((block_width, hidden_columns), jnp.float32),
            jax.ShapeDtypeStruct((block_width, hidden_columns), jnp.float32),
            jax.ShapeDtypeStruct((hidden_columns, block_width), jnp.float32),
        ],
        blocks[0], up, down, second_total,
    )
    return (
        block_output,
        input_gradient,
        terms[:gain_rows].reshape(-1),
        query_gradient,
        key_gradient,
        value_gradient,
        terms[2 * gain_rows],
        terms[2 * gain_rows + 1],
        output_gradient,
        terms[gain_rows : 2 * gain_rows].reshape(-1),
        gate_gradient,
        up_gradient,
        down_gradient,
    )


def solution(mesh):
    in_specs = (
        P(("dp", "tensor"), None),
        P(),
        P("dp", "tensor"),
        P("dp", "tensor"),
        P("dp", "tensor"),
        P(),
        P(),
        P("tensor", "dp"),
        P(),
        P("dp", "tensor"),
        P("dp", "tensor"),
        P("tensor", "dp"),
        P(("dp", "tensor"), None),
    )
    out_specs = (
        P(("dp", "tensor"), None),
        P(("dp", "tensor"), None),
        P(),
        P("dp", "tensor"),
        P("dp", "tensor"),
        P("dp", "tensor"),
        P(),
        P(),
        P("tensor", "dp"),
        P(),
        P("dp", "tensor"),
        P("dp", "tensor"),
        P("tensor", "dp"),
    )

    return jax.shard_map(per_device, mesh=mesh, in_specs=in_specs, out_specs=out_specs, check_vma=False)
```

```python
import functools

import jax
import jax.numpy as jnp
import numpy as np
from jax import lax
from jax.experimental import pallas as pl
from jax.experimental.pallas import tpu as pltpu
from jax.sharding import PartitionSpec as P


SEQUENCE_LENGTH = 1024

epsilon = 1e-06
rope_base = 1000000.0


MESH = pl.DeviceIdType.MESH
VMEM_LIMIT = 62 * 1024 * 1024


def row_scale(values):
    return lax.rsqrt(jnp.mean(values * values, axis=-1, keepdims=True) + epsilon)


def times_transposed(first_operand, second_operand):
    return lax.dot_general(
        first_operand, second_operand, (((1,), (1,)), ((), ())), preferred_element_type=jnp.float32
    )


def simple_product(first_operand, second_operand):
    return jnp.dot(first_operand, second_operand, preferred_element_type=jnp.float32)


def remote(source, target, send_sem, recv_sem, peer, axis="tensor"):
    return pltpu.make_async_remote_copy(
        src_ref=source,
        dst_ref=target,
        send_sem=send_sem,
        recv_sem=recv_sem,
        device_id={axis: peer},
        device_id_type=MESH,
    )


def greet(peers):
    barrier = pltpu.get_barrier_semaphore()
    for axis, peer in peers:
        pl.semaphore_signal(barrier, inc=1, device_id={axis: peer}, device_id_type=MESH)
    pl.semaphore_wait(barrier, len(peers))


def square_peers(me):
    column = lax.rem(me, 2)
    row = me // 2
    return row * 2 + (1 - column), (1 - row) * 2 + column, (1 - row) * 2 + (1 - column)


def neighbours(size):
    if size == 4:
        beside, below, _ = square_peers(lax.axis_index("tensor"))
        return [("tensor", beside), ("tensor", below)]
    return [("tensor", peer) for peer in other_members("tensor", size)]


def other_members(axis, count):
    me = lax.axis_index(axis)
    return [lax.rem(me + step, count) for step in range(1, count)]


class Gather:
    def __init__(
        self, size, own_ref, out_ref, turned_out_ref, held_ref, turned_ref, send_sem, recv_sem, local_sem, turned_sem
    ):
        self.size, self.own, self.out, self.held = size, own_ref, out_ref, held_ref
        self.turned_out, self.turned = turned_out_ref, turned_ref
        self.send_sem, self.recv_sem, self.local_sem = send_sem, recv_sem, local_sem
        self.turned_sem = turned_sem
        self.me = lax.axis_index("tensor")
        self.rows = own_ref.shape[0]
        self.copies, self.stores, self.turns = [], [], []

    @staticmethod
    def scratch(size, rows, columns):
        sends, local = (6, 8) if size == 4 else (size - 1, size)
        return [
            pltpu.VMEM((size, rows, columns), jnp.bfloat16),
            pltpu.VMEM((columns, size * rows), jnp.bfloat16),
            pltpu.SemaphoreType.DMA((sends,)),
            pltpu.SemaphoreType.DMA((sends,)),
            pltpu.SemaphoreType.DMA((local,)),
            pltpu.SemaphoreType.DMA((local,)),
        ]

    def send(self, source, target, peer):
        index = len(self.copies)
        copy = remote(source, target, self.send_sem.at[index], self.recv_sem.at[index], peer)
        copy.start()
        self.copies.append(copy)
        return copy

    def store(self, source, start, count):
        piece = pl.ds(pl.multiple_of(start, count), count)
        copy = pltpu.make_async_copy(source, self.out.at[piece], self.local_sem.at[len(self.stores)])
        copy.start()
        self.stores.append(copy)
        width = min(256, self.turned.shape[0])

        def turn_part(index, carry):
            columns = pl.ds(pl.multiple_of(index * width, width), width)
            self.turned[columns, piece] = source[:, columns].T
            return carry

        lax.fori_loop(0, self.turned.shape[0] // width, turn_part, 0)
        turn_copy = pltpu.make_async_copy(
            self.turned.at[:, piece], self.turned_out.at[:, piece], self.turned_sem.at[len(self.turns)]
        )
        turn_copy.start()
        self.turns.append(turn_copy)

    def start(self):
        own, held, rows = self.own, self.held, self.rows
        if self.size != 4:
            for peer in other_members("tensor", self.size):
                self.send(own, held.at[self.me], peer)
            return
        beside, below, _ = square_peers(self.me)
        half = rows // 2
        first, second = pl.ds(0, half), pl.ds(half, half)
        self.send(own.at[first], held.at[self.me, first], beside)
        self.send(own.at[second], held.at[self.me, second], below)
        self.send(own.at[second], held.at[self.me, second], beside)
        self.send(own.at[first], held.at[self.me, first], below)

    def forward(self):
        own, held, rows = self.own, self.held, self.rows
        if self.size != 4:
            self.store(own, self.me * rows, rows)
            return
        beside, below, _ = square_peers(self.me)
        half = rows // 2
        first, second = pl.ds(0, half), pl.ds(half, half)
        x_first, y_second = self.copies[:2]
        self.store(own.at[first], self.me * rows, half)
        self.store(own.at[second], self.me * rows + half, half)
        x_first.wait_recv()
        self.send(held.at[beside, first], held.at[beside, first], below)
        y_second.wait_recv()
        self.send(held.at[below, second], held.at[below, second], beside)

    def finish(self):
        held, rows = self.held, self.rows
        if self.size != 4:
            for step, copy in enumerate(self.copies):
                copy.wait_recv()
                slot = lax.rem(self.me + self.size - step - 1, self.size)
                self.store(held.at[slot], slot * rows, rows)
        else:
            beside, below, across = square_peers(self.me)
            half = rows // 2
            first, second = pl.ds(0, half), pl.ds(half, half)
            x_second, y_first, y_pass, x_pass = self.copies[2:]
            self.store(held.at[beside, first], beside * rows, half)
            self.store(held.at[below, second], below * rows + half, half)
            x_second.wait_recv()
            self.store(held.at[beside, second], beside * rows + half, half)
            y_first.wait_recv()
            self.store(held.at[below, first], below * rows, half)
            y_pass.wait_recv()
            self.store(held.at[across, first], across * rows, half)
            x_pass.wait_recv()
            self.store(held.at[across, second], across * rows + half, half)
        for copy in self.copies:
            copy.wait_send()
        for copy in self.stores + self.turns:
            copy.wait()


def gather_kernel(size, count, *refs):
    own_refs, out_refs, rest = refs[:count], refs[count : 3 * count], refs[3 * count :]
    greet(neighbours(size))
    gathers = [
        Gather(size, own_refs[k], *out_refs[2 * k : 2 * k + 2], *rest[6 * k : 6 * k + 6])
        for k in range(count)
    ]
    for gather in gathers:
        gather.start()
        gather.forward()
    for gather in gathers:
        gather.finish()


def gather_rows(arrays, size, collective_id):
    count = len(arrays)
    rows, columns = arrays[0].shape
    scratch = []
    out_shape = []
    for _ in arrays:
        scratch += Gather.scratch(size, rows, columns)
        out_shape += [
            jax.ShapeDtypeStruct((size * rows, columns), jnp.bfloat16),
            jax.ShapeDtypeStruct((columns, size * rows), jnp.bfloat16),
        ]
    return pl.pallas_call(
        functools.partial(gather_kernel, size, count),
        out_shape=out_shape,
        in_specs=[pl.BlockSpec(memory_space=pltpu.VMEM)] * count,
        out_specs=[pl.BlockSpec(memory_space=pl.ANY)] * len(out_shape),
        scratch_shapes=scratch,
        compiler_params=pltpu.CompilerParams(
            collective_id=collective_id, has_side_effects=True, vmem_limit_bytes=VMEM_LIMIT
        ),
        cost_estimate=pl.CostEstimate(
            flops=0, bytes_accessed=count * 30 * size * rows * columns, transcendentals=0
        ),
        name="gather_rows",
    )(*arrays)


class Operand:
    def __init__(self, size, first_column, left_far, weight_far, left, weight, left_sem, weight_sem):
        self.left, self.weight = left, weight
        self.rows = left.shape[0] // size
        self.tile = min(512, weight.shape[0])
        self.far = left_far, weight_far
        self.first_column = first_column
        self.left_sem, self.weight_sem = left_sem, weight_sem

    @staticmethod
    def scratch(size, left, weight):
        width = left.shape[1]
        return [
            pltpu.VMEM(left.shape, left.dtype),
            pltpu.VMEM((weight.shape[0], width), weight.dtype),
            pltpu.SemaphoreType.DMA((size,)),
            pltpu.SemaphoreType.DMA((max(1, weight.shape[0] // 512),)),
        ]

    def left_copy(self, slot, owner):
        piece = pl.ds(pl.multiple_of(owner * self.rows, self.rows), self.rows)
        return pltpu.make_async_copy(self.far[0].at[piece], self.left.at[piece], self.left_sem.at[slot])

    def weight_copy(self, index):
        piece = pl.ds(pl.multiple_of(index * self.tile, self.tile), self.tile)
        columns = pl.ds(self.first_column, self.left.shape[1])
        return pltpu.make_async_copy(
            self.far[1].at[piece, columns], self.weight.at[piece], self.weight_sem.at[index]
        )


def block_product(operands, start, rows, fresh, write):
    total = operands[0].weight.shape[0]
    tile = operands[0].tile
    start = pl.multiple_of(start, rows)

    def step(index, carry):
        @pl.when(fresh)
        def _():
            for operand in operands:
                operand.weight_copy(index).wait()

        columns = pl.ds(pl.multiple_of(index * tile, tile), tile)
        values = None
        for operand in operands:
            part = times_transposed(
                operand.left[pl.ds(start, rows), :], operand.weight[columns, :]
            )
            values = part if values is None else values + part
        write(columns, values)
        return carry

    lax.fori_loop(0, total // tile, step, 0)


class Scatter:
    def __init__(self, size, outgoing, *rest):
        self.size, self.outgoing = size, outgoing
        if size == 4:
            self.passing, rest = rest[0], rest[1:]
        self.arriving, self.send_sem, self.recv_sem = rest
        self.rows = outgoing.shape[1]
        self.me = lax.axis_index("tensor")
        self.copies, self.starts = self.plan()

    @staticmethod
    def scratch(size, rows, columns):
        if size == 4:
            sends = 6
            buffers = [
                pltpu.VMEM((4, rows, columns), jnp.bfloat16),
                pltpu.VMEM((2, rows // 2, columns), jnp.bfloat16),
                pltpu.VMEM((2, rows, columns), jnp.bfloat16),
            ]
        else:
            sends = size - 1
            buffers = [
                pltpu.VMEM((size, rows, columns), jnp.bfloat16),
                pltpu.VMEM((size - 1, rows, columns), jnp.bfloat16),
            ]
        return buffers + [pltpu.SemaphoreType.DMA((sends,)), pltpu.SemaphoreType.DMA((sends,))]

    def prepare(self, index, source, target, peer):
        return remote(source, target, self.send_sem.at[index], self.recv_sem.at[index], peer)

    def plan(self):
        outgoing, arriving = self.outgoing, self.arriving
        if self.size != 4:
            copies = [
                self.prepare(step, outgoing.at[step], arriving.at[step], peer)
                for step, peer in enumerate(other_members("tensor", self.size))
            ]
            return copies, tuple((step, step) for step in range(self.size - 1))
        beside, below, _ = square_peers(self.me)
        half = self.rows // 2
        first, second = pl.ds(0, half), pl.ds(half, half)
        copies = [
            self.prepare(0, outgoing.at[0, first], self.passing.at[0], beside),
            self.prepare(1, outgoing.at[0, second], self.passing.at[1], below),
            self.prepare(2, outgoing.at[1, first], arriving.at[0, first], beside),
            self.prepare(3, outgoing.at[2, second], arriving.at[1, second], below),
            self.prepare(4, outgoing.at[1, second], arriving.at[0, second], beside),
            self.prepare(5, outgoing.at[2, first], arriving.at[1, first], below),
        ]
        return copies, ((0, 0), (0, 1), (1, 2), (2, 3))

    def owner(self, slot):
        if self.size != 4:
            return lax.rem(self.me + slot + 1, self.size)
        beside, below, across = square_peers(self.me)
        return jnp.where(
            slot == 0, across, jnp.where(slot == 1, beside, jnp.where(slot == 2, below, self.me))
        )

    def load(self, operands):
        tiles = operands[0].weight.shape[0] // operands[0].tile
        for operand in operands:
            operand.left_copy(0, self.owner(0)).start()
        for index in range(tiles):
            for operand in operands:
                operand.weight_copy(index).start()
        for slot in range(1, self.size):
            for operand in operands:
                operand.left_copy(slot, self.owner(slot)).start()

    def fill(self, operands, look=None, slots=None):
        rows = self.rows

        def step(slot, carry):
            owner = self.owner(slot)
            for operand in operands:
                operand.left_copy(slot, owner).wait()

            def write(columns, values):
                self.outgoing[slot, :, columns] = values.astype(self.outgoing.dtype)
                if look is not None:
                    look(owner, columns, values)

            block_product(operands, owner * rows, rows, slot == 0, write)
            for at, index in self.starts:
                pl.when(slot == at)(self.copies[index].start)
            return carry

        lax.fori_loop(*(slots or (0, self.size)), step, 0)

    def relay(self):
        if self.size != 4:
            return
        half = self.rows // 2
        x_pass, y_pass, _, _, x_second, y_first = self.copies
        for arrival, source, slot, start, onward in (
            (y_pass, 1, 1, half, x_second),
            (x_pass, 0, 2, 0, y_first),
        ):
            arrival.wait_recv()
            piece = pl.ds(start, half)
            self.outgoing[slot, piece, :] = (
                self.outgoing[slot, piece, :].astype(jnp.float32)
                + self.passing[source].astype(jnp.float32)
            ).astype(self.outgoing.dtype)
            onward.start()

    def collect(self):
        for copy in self.copies[2:] if self.size == 4 else self.copies:
            copy.wait_recv()

    def total(self, piece):
        total = self.outgoing[self.size - 1, piece, :].astype(jnp.float32)
        for index in range(self.arriving.shape[0]):
            total = total + self.arriving[index, piece, :].astype(jnp.float32)
        return total

    def drain(self):
        for copy in self.copies:
            copy.wait_send()


class Chain:
    def __init__(
        self, chips, steps, rising_refs, falling_refs, up_ref, down_ref,
        rise, fall, up, down, load_sem, send_sem, recv_sem,
    ):
        self.chips, self.steps = chips, steps
        self.rise, self.fall, self.up, self.down = rise, fall, up, down
        device = lax.axis_index("dp")
        self.chip = device // 2
        count = len(steps)
        self.loads = [
            pltpu.make_async_copy(source, target, load_sem.at[index])
            for index, (source, target) in enumerate(
                [(up_ref, up.at[0]), (down_ref, down.at[0])]
                + [(ref, rise.at[index]) for index, ref in enumerate(rising_refs)]
                + [(ref, fall.at[index]) for index, ref in enumerate(falling_refs)]
            )
        ]
        above = lax.rem(device + 2, 2 * chips)
        under = lax.rem(device + 2 * chips - 2, 2 * chips)
        self.neighbours = [("dp", above), ("dp", under)]
        self.rises = [
            remote(rise.at[i], up.at[i + 1], send_sem.at[i], recv_sem.at[i], above, "dp")
            for i in range(count)
        ]
        self.falls = [
            remote(
                fall.at[i], down.at[i + 1], send_sem.at[count + i], recv_sem.at[count + i], under, "dp"
            )
            for i in range(count)
        ]

    @staticmethod
    def scratch(count, rows, columns):
        return [
            pltpu.VMEM((count, rows, columns), jnp.bfloat16),
            pltpu.VMEM((count, rows, columns), jnp.bfloat16),
            pltpu.VMEM((count + 1, rows, columns), jnp.bfloat16),
            pltpu.VMEM((count + 1, rows, columns), jnp.bfloat16),
            pltpu.SemaphoreType.DMA((2 * count + 2,)),
            pltpu.SemaphoreType.DMA((2 * count,)),
            pltpu.SemaphoreType.DMA((2 * count,)),
        ]

    def load(self):
        for copy in self.loads:
            copy.start()

    def step(self, index):
        if index == 0:
            for copy in self.loads:
                copy.wait()
        step = self.steps[index]
        rows = self.rise.shape[1]
        sends_up = self.chip < step
        sends_down = self.chip >= self.chips - step

        @pl.when(sends_up & (self.chip > 0))
        def _():
            def add(piece):
                self.rise[index, piece, :] = add_rounded(
                    self.rise[index, piece, :], self.up[index, piece, :]
                )

            over_pieces(rows, add)

        pl.when(sends_up)(self.rises[index].start)

        @pl.when(sends_down & (self.chip < self.chips - 1))
        def _():
            def add(piece):
                self.fall[index, piece, :] = add_rounded(
                    self.fall[index, piece, :], self.down[index, piece, :]
                )

            over_pieces(rows, add)

        pl.when(sends_down)(self.falls[index].start)

    def arrives(self, index):
        step = self.steps[index]
        from_under = (self.chip > 0) & (self.chip <= step)
        from_above = (self.chip < self.chips - 1) & (self.chip >= self.chips - step - 1)
        return from_under, from_above

    def wait(self, index):
        from_under, from_above = self.arrives(index)
        pl.when(from_under)(self.rises[index].wait_recv)
        pl.when(from_above)(self.falls[index].wait_recv)

    def drain(self):
        for index, step in enumerate(self.steps):
            pl.when(self.chip < step)(self.rises[index].wait_send)
            pl.when(self.chip >= self.chips - step)(self.falls[index].wait_send)


def add_rounded(first, second):
    return (first.astype(jnp.float32) + second.astype(jnp.float32)).astype(jnp.bfloat16)


def over_pieces(rows, body):
    count = min(32, rows)

    def step(index, carry):
        body(pl.ds(pl.multiple_of(index * count, count), count))
        return carry

    lax.fori_loop(0, rows // count, step, 0)


def send_terms(axis, peers, source, landing, send_sem, recv_sem):
    me = lax.axis_index(axis)
    landing[me] = source[...]
    copies = []
    for step, peer in enumerate(peers):
        copy = remote(source, landing.at[me], send_sem.at[step], recv_sem.at[step], peer, axis)
        copy.start()
        copies.append(copy)
    return copies


def add_terms(landing, copies):
    for copy in copies:
        copy.wait_recv()
    total = landing[0]
    for index in range(1, landing.shape[0]):
        total = total + landing[index]
    return total


def split_operands(refs, size, first_columns):
    count = len(first_columns)
    far, refs, scratch = refs[: 2 * count], refs[2 * count : -4 * count], refs[-4 * count :]
    operands = [
        Operand(size, first, *far[2 * p : 2 * p + 2], *scratch[4 * p : 4 * p + 4])
        for p, first in enumerate(first_columns)
    ]
    return operands, refs


def store_row(target_ref, row_ref):
    width = target_ref.shape[1]
    for index in range(row_ref.shape[1] // width):
        target_ref[index : index + 1, :] = row_ref[:, index * width : (index + 1) * width]


def between_forward_kernel(size, first_columns, *refs):
    operands, refs = split_operands(refs, size, first_columns)
    input_ref, gain_ref, gathered_ref, turned_ref, state_ref, own_ref = refs[:6]
    buffers = 5 if size == 4 else 4
    scatter = Scatter(size, *refs[6 : 6 + buffers])
    gather = Gather(size, own_ref, gathered_ref, turned_ref, *refs[6 + buffers :])
    scatter.load(operands)
    greet(neighbours(size))
    scatter.fill(operands)
    scatter.relay()
    scatter.collect()

    def norm(piece):
        state = input_ref[piece, :].astype(jnp.float32) + scatter.total(piece)
        state_ref[piece, :] = state
        own_ref[piece, :] = (state * row_scale(state) * gain_ref[...]).astype(own_ref.dtype)

    over_pieces(own_ref.shape[0], norm)
    gather.start()
    gather.forward()
    gather.finish()
    scatter.drain()


def between_backward_kernel(size, chips, steps, first_columns, *refs):
    operands, refs = split_operands(refs, size, first_columns)
    state_ref, cotangent_ref, gain_ref = refs[:3]
    chain_count = 2 * len(steps) + 2
    chain_refs, last_refs, refs = refs[3 : 3 + chain_count], refs[3 + chain_count : 5 + chain_count], refs[5 + chain_count :]
    gathered_ref, gathered_turned_ref, slope_ref, term_ref, rising_ref, falling_ref = refs[:6]
    own_ref, sum_ref, last_sem = refs[6:9]
    buffers = 5 if size == 4 else 4
    scatter = Scatter(size, *refs[9 : 9 + buffers])
    gather = Gather(size, own_ref, gathered_ref, gathered_turned_ref, *refs[9 + buffers : 15 + buffers])
    chain = Chain(
        chips, steps, chain_refs[: len(steps)], chain_refs[len(steps) : -2], *chain_refs[-2:],
        *refs[15 + buffers :],
    )
    last_loads = [
        pltpu.make_async_copy(source, target, last_sem.at[index])
        for index, (source, target) in enumerate(zip(last_refs, (rising_ref, falling_ref)))
    ]
    chain.load()
    scatter.load(operands)
    for load in last_loads:
        load.start()
    greet(neighbours(size) + chain.neighbours)
    scatter.fill(operands, slots=(0, 1))
    chain.step(0)
    scatter.fill(operands, slots=(1, size))
    scatter.relay()
    sum_ref[...] = jnp.zeros_like(sum_ref)
    scatter.collect()

    def norm(piece):
        back = scatter.total(piece)
        state = state_ref[piece, :]
        scale = row_scale(state)
        unit = state * scale
        sum_ref[...] += jnp.sum(back * unit, axis=0, keepdims=True)
        unit_slope = back * gain_ref[...]
        slope = cotangent_ref[piece, :].astype(jnp.float32) + scale * (
            unit_slope - unit * jnp.mean(unit_slope * unit, axis=-1, keepdims=True)
        )
        slope_ref[piece, :] = slope
        own_ref[piece, :] = slope.astype(own_ref.dtype)

    over_pieces(own_ref.shape[0], norm)
    gather.start()
    store_row(term_ref, sum_ref)
    gather.forward()
    chain.wait(0)
    for index in range(1, len(steps)):
        chain.step(index)
        chain.wait(index)
    for load in last_loads:
        load.wait()
    last = len(steps)
    for needed, landing, out_ref in (
        ((chain.chip > 0) & (chain.chip < chips - 1), chain.up, rising_ref),
        ((chain.chip > 0) & (chain.chip < chips - 1), chain.down, falling_ref),
    ):

        @pl.when(needed)
        def _(landing=landing, out_ref=out_ref):
            def add(piece):
                out_ref[piece, :] = add_rounded(out_ref[piece, :], landing[last, piece, :])

            over_pieces(out_ref.shape[0], add)

    gather.finish()
    scatter.drain()
    chain.drain()


def last_kernel(sizes, first_columns, *refs):
    data_size, size = sizes
    operands, refs = split_operands(refs, size, first_columns)
    input_ref, gain_ref, slope_ref, terms_ref, rows_ref = refs[:5]
    gradient_ref, terms_out_ref, sum_ref, partial_ref, group_ref, inner, outer = refs[5:12]
    inner_send, inner_recv, outer_send, outer_recv = refs[12:16]
    mixing = Scatter(size, *refs[16:])
    rows = gradient_ref.shape[0]
    mixing.load(operands)
    greet(
        [("tensor", peer) for peer in other_members("tensor", size)]
        + [("dp", peer) for peer in other_members("dp", data_size)]
    )
    sum_ref[...] = jnp.zeros_like(sum_ref)

    def look(owner, columns, values):
        piece = pl.ds(pl.multiple_of(owner * rows, rows), rows)
        sum_ref[:, columns] += jnp.sum(
            values * rows_ref[piece, columns].astype(jnp.float32), axis=0, keepdims=True
        )

    mixing.fill(operands, look)
    sum_ref[...] = sum_ref[...] / gain_ref[...]
    kept = partial_ref.shape[0] - terms_ref.shape[0]
    partial_ref[kept:, :] = terms_ref[...]
    store_row(partial_ref, sum_ref)
    inner_copies = send_terms(
        "tensor", other_members("tensor", size), partial_ref, inner, inner_send, inner_recv
    )
    mixing.relay()
    group_ref[...] = add_terms(inner, inner_copies)
    outer_copies = send_terms(
        "dp", other_members("dp", data_size), group_ref, outer, outer_send, outer_recv
    )
    terms_out_ref[...] = add_terms(outer, outer_copies)
    mixing.collect()

    def norm(piece):
        back = mixing.total(piece)
        values = input_ref[piece, :].astype(jnp.float32)
        scale = row_scale(values)
        unit = values * scale
        unit_slope = back * gain_ref[...]
        gradient_ref[piece, :] = (
            slope_ref[piece, :]
            + scale * (unit_slope - unit * jnp.mean(unit_slope * unit, axis=-1, keepdims=True))
        ).astype(gradient_ref.dtype)

    over_pieces(rows, norm)
    for copy in inner_copies + outer_copies:
        copy.wait_send()
    mixing.drain()


def scatter_call(body, triples, size, others, far, outs, gathered, scratch, collective_id):
    far_spec = pl.BlockSpec(memory_space=pl.ANY)
    operands = [array for left, weight, _ in triples for array in (left, weight)]
    in_specs = [far_spec] * len(operands)
    for other in others:
        in_specs.append(pl.BlockSpec(other.shape, lambda i: (0, 0), pipeline_mode=pl.Buffered(1)))
    in_specs += [far_spec] * len(far)
    out_specs = [pl.BlockSpec(out.shape, lambda i: (0, 0)) for out in outs]
    if gathered:
        out_specs[:2] = [far_spec] * 2
    return pl.pallas_call(
        functools.partial(body, tuple(first for _, _, first in triples)),
        grid=(1,),
        out_shape=outs,
        in_specs=in_specs,
        out_specs=out_specs,
        scratch_shapes=list(scratch)
        + [part for left, weight, _ in triples for part in Operand.scratch(size, left, weight)],
        compiler_params=pltpu.CompilerParams(
            collective_id=collective_id, has_side_effects=True, vmem_limit_bytes=VMEM_LIMIT
        ),
        cost_estimate=pl.CostEstimate(
            flops=sum(2 * left.size * weight.shape[0] for left, weight, _ in triples),
            bytes_accessed=150_000_000,
            transcendentals=0,
        ),
    )(*operands, *others, *far)


LOG2E = 1.4426950408889634


def turn_tables(head_size):
    half_size = head_size // 2
    frequency = np.float32(rope_base) ** (
        -(np.arange(half_size, dtype=np.float32) * np.float32(2.0) / np.float32(head_size))
    )
    frequency = frequency.astype(np.float64)
    sign = np.concatenate([-np.ones(half_size), np.ones(half_size)])[None, :]
    positions = np.concatenate([np.arange(0, SEQUENCE_LENGTH, 128), np.arange(128)])
    angles = positions[:, None] * np.concatenate([frequency, frequency])[None, :]
    return np.cos(angles).astype(np.float32), (sign * np.sin(angles)).astype(np.float32)


def fill_tables(few_cosines_ref, few_sines_ref, cosine_ref, sine_ref):
    coarse = few_cosines_ref.shape[0] - 128
    near_cosine, near_sine = few_cosines_ref[coarse:, :], few_sines_ref[coarse:, :]

    def step(index, carry):
        far_cosine = few_cosines_ref[pl.ds(index, 1), :]
        far_sine = few_sines_ref[pl.ds(index, 1), :]
        rows = pl.ds(pl.multiple_of(index * 128, 128), 128)
        cosine_ref[rows, :] = far_cosine * near_cosine - far_sine * near_sine
        sine_ref[rows, :] = far_sine * near_cosine + far_cosine * near_sine
        return carry

    lax.fori_loop(0, coarse, step, 0)


def turn(values, cosine, sine):
    return values * cosine + pltpu.roll(values, values.shape[-1] // 2, 1) * sine


def turn_back(values, cosine, sine):
    return values * cosine - pltpu.roll(values, values.shape[-1] // 2, 1) * sine


def contract_first(first_operand, second_operand):
    return lax.dot_general(
        first_operand, second_operand, (((0,), (0,)), ((), ())), preferred_element_type=jnp.float32
    )


def visible_scores(key_rows, query_rows, first_row, multiplier):
    scores = times_transposed(key_rows, query_rows) * multiplier
    _, queries = scores.shape
    key_at = lax.broadcasted_iota(jnp.int32, (queries, queries), 0)
    query_at = lax.broadcasted_iota(jnp.int32, (queries, queries), 1)
    corner = jnp.where(query_at >= key_at, scores[first_row:], -1e30)
    if first_row == 0:
        return corner
    return jnp.concatenate([scores[:first_row], corner], axis=0)


def turn_heads(
    grouping, head_size, raw_ref, query_gain_ref, key_gain_ref, cosine_ref, sine_ref, query_ref, key_ref, value_ref
):
    def turned(start, gain):
        raw = raw_ref[:, pl.ds(start, head_size)]
        return turn(raw * row_scale(raw) * gain, cosine_ref[...], sine_ref[...]).astype(jnp.bfloat16)

    def step(part, carry):
        query_ref[part] = turned(pl.multiple_of(part * head_size, head_size), query_gain_ref[...])
        return carry

    lax.fori_loop(0, grouping, step, 0)
    key_ref[...] = turned(grouping * head_size, key_gain_ref[...])
    value_ref[...] = raw_ref[:, (grouping + 1) * head_size :].astype(jnp.bfloat16)


def attention_forward_kernel(
    grouping, head_size, block, rows_ref, weight_ref, few_cosines_ref, few_sines_ref, query_gain_ref, key_gain_ref,
    raw_ref, mixed_ref, total_ref, query_ref, key_ref, value_ref, cosine_ref, sine_ref,
):
    sequence = rows_ref.shape[0]
    multiplier = head_size ** (-0.5) * LOG2E

    @pl.when((pl.program_id(0) == 0) & (pl.program_id(1) == 0))
    def _():
        fill_tables(few_cosines_ref, few_sines_ref, cosine_ref, sine_ref)

    raw_ref[...] = simple_product(rows_ref[...], weight_ref[...])
    turn_heads(
        grouping, head_size, raw_ref, query_gain_ref, key_gain_ref, cosine_ref, sine_ref, query_ref, key_ref, value_ref
    )

    def head_step(part, carry):
        lanes = pl.ds(pl.multiple_of(part * head_size, head_size), head_size)
        for first_row in range(0, sequence, block):
            last_row = first_row + block
            scores = visible_scores(
                key_ref[:last_row, :], query_ref[part, first_row:last_row, :], first_row, multiplier
            )
            highest = jnp.max(scores, axis=0, keepdims=True)
            weights = jnp.exp2(scores - highest)
            total = jnp.sum(weights, axis=0, keepdims=True)
            weights = (weights * (1.0 / total)).astype(jnp.bfloat16)
            mixed_ref[first_row:last_row, lanes] = contract_first(
                weights, value_ref[:last_row, :]
            ).astype(mixed_ref.dtype)
            total_ref[0, pl.ds(part, 1), first_row:last_row] = highest + jnp.log2(total)
        return carry

    lax.fori_loop(0, grouping, head_step, 0)


def attention_forward(rows, weight, tables, query_gain, key_gain, heads, grouping):
    total_rows, depth = rows.shape
    head_size = query_gain.shape[0]
    sequences = total_rows // SEQUENCE_LENGTH
    width = (grouping + 2) * head_size
    block = min(256, SEQUENCE_LENGTH)
    table = pl.BlockSpec(tables[0].shape, lambda s, h: (0, 0))
    gain = pl.BlockSpec((1, head_size), lambda s, h: (0, 0))
    elements = heads * grouping * total_rows * SEQUENCE_LENGTH // 2
    return pl.pallas_call(
        functools.partial(attention_forward_kernel, grouping, head_size, block),
        grid=(sequences, heads),
        out_shape=[
            jax.ShapeDtypeStruct((total_rows, heads * width), jnp.float32),
            jax.ShapeDtypeStruct((total_rows, heads * grouping * head_size), jnp.bfloat16),
            jax.ShapeDtypeStruct((heads, grouping, total_rows), jnp.float32),
        ],
        in_specs=[
            pl.BlockSpec((SEQUENCE_LENGTH, depth), lambda s, h: (s, 0)),
            pl.BlockSpec((depth, width), lambda s, h: (0, h)),
            table,
            table,
            gain,
            gain,
        ],
        out_specs=[
            pl.BlockSpec((SEQUENCE_LENGTH, width), lambda s, h: (s, h)),
            pl.BlockSpec((SEQUENCE_LENGTH, grouping * head_size), lambda s, h: (s, h)),
            pl.BlockSpec((1, grouping, SEQUENCE_LENGTH), lambda s, h: (h, 0, s)),
        ],
        scratch_shapes=[
            pltpu.VMEM((grouping, SEQUENCE_LENGTH, head_size), jnp.bfloat16),
            pltpu.VMEM((SEQUENCE_LENGTH, head_size), jnp.bfloat16),
            pltpu.VMEM((SEQUENCE_LENGTH, head_size), jnp.bfloat16),
            pltpu.VMEM((SEQUENCE_LENGTH, head_size), jnp.float32),
            pltpu.VMEM((SEQUENCE_LENGTH, head_size), jnp.float32),
        ],
        compiler_params=pltpu.CompilerParams(vmem_limit_bytes=VMEM_LIMIT),
        cost_estimate=pl.CostEstimate(
            flops=2 * total_rows * depth * heads * width + 4 * elements * head_size,
            bytes_accessed=2 * (total_rows * depth + depth * heads * width),
            transcendentals=elements,
        ),
        name="attention_forward",
    )(rows, weight, *tables, query_gain.reshape(1, -1), key_gain.reshape(1, -1))


def norm_back(turned_slope, raw, gain, cosine, sine):
    norm_slope = turn_back(turned_slope, cosine, sine)
    scale = row_scale(raw)
    unit = raw * scale
    term = norm_slope * unit
    unit_slope = norm_slope * gain
    slope = scale * (unit_slope - unit * jnp.mean(unit_slope * unit, axis=-1, keepdims=True))
    return slope.astype(jnp.bfloat16), jnp.sum(term, axis=0, keepdims=True)


def attention_backward_kernel(size, grouping, head_size, block, first_columns, *refs):
    operands, refs = split_operands(refs, size, first_columns)
    (
        state_ref, weight_ref, raw_ref, mixed_ref, total_ref, few_cosines_ref, few_sines_ref,
        query_gain_ref, key_gain_ref, hidden_state_ref, slope_ref, gain_ref, output_ref,
        query_ref, key_ref, value_ref, out_slope_ref, turned_ref, key_sum_ref, value_sum_ref, cosine_ref, sine_ref,
    ) = refs[:22]
    scatter = Scatter(size, *refs[22:])
    step = pl.program_id(0) * pl.num_programs(1) + pl.program_id(1)
    steps = pl.num_programs(0) * pl.num_programs(1)

    @pl.when(step == 0)
    def _():
        scatter.load(operands)
        greet(neighbours(size))
        scatter.fill(operands)

    attend_backward_head(
        grouping, head_size, block, state_ref, weight_ref, raw_ref, mixed_ref, total_ref, few_cosines_ref,
        few_sines_ref, query_gain_ref, key_gain_ref, slope_ref, gain_ref, query_ref, key_ref, value_ref,
        out_slope_ref, turned_ref, key_sum_ref, value_sum_ref, cosine_ref, sine_ref,
    )

    @pl.when(step == 0)
    def _():
        scatter.relay()

    @pl.when(step == steps - 1)
    def _():
        scatter.collect()

        def finish(piece):
            output_ref[piece, :] = (hidden_state_ref[piece, :] + scatter.total(piece)).astype(
                output_ref.dtype
            )

        over_pieces(output_ref.shape[0], finish)
        scatter.drain()


def attend_backward_head(
    grouping, head_size, block, state_ref, weight_ref, raw_ref, mixed_ref, total_ref, few_cosines_ref, few_sines_ref,
    query_gain_ref, key_gain_ref, slope_ref, gain_ref, query_ref, key_ref, value_ref, out_slope_ref,
    turned_ref, key_sum_ref, value_sum_ref, cosine_ref, sine_ref,
):
    sequence = state_ref.shape[0]
    scale_factor = head_size ** (-0.5)
    multiplier = scale_factor * LOG2E

    @pl.when((pl.program_id(0) == 0) & (pl.program_id(1) == 0))
    def _():
        gain_ref[...] = jnp.zeros_like(gain_ref)
        fill_tables(few_cosines_ref, few_sines_ref, cosine_ref, sine_ref)

    out_slope_ref[...] = simple_product(state_ref[...], weight_ref[...]).astype(jnp.bfloat16)
    turn_heads(
        grouping, head_size, raw_ref, query_gain_ref, key_gain_ref, cosine_ref, sine_ref, query_ref, key_ref, value_ref
    )
    key_sum_ref[...] = jnp.zeros_like(key_sum_ref)
    value_sum_ref[...] = jnp.zeros_like(value_sum_ref)
    ones = jnp.ones((8, head_size), jnp.float32)

    def head_step(part, carry):
        lanes = pl.ds(pl.multiple_of(part * head_size, head_size), head_size)
        for first_row in range(0, sequence, block):
            last_row = first_row + block
            query_rows = query_ref[part, first_row:last_row, :]
            slope_rows = out_slope_ref[first_row:last_row, lanes]
            scores = visible_scores(key_ref[:last_row, :], query_rows, first_row, multiplier)
            weights = jnp.exp2(scores - total_ref[0, pl.ds(part, 1), first_row:last_row])
            value_sum_ref[:last_row, :] += simple_product(weights.astype(jnp.bfloat16), slope_rows)
            product = slope_rows.astype(jnp.float32) * mixed_ref[first_row:last_row, lanes].astype(jnp.float32)
            centre = lax.dot_general(
                ones,
                product,
                (((1,), (1,)), ((), ())),
                preferred_element_type=jnp.float32,
                precision=lax.Precision.HIGHEST,
            )[:1]
            weight_slope = times_transposed(value_ref[:last_row, :], slope_rows)
            score_slope = (weights * (weight_slope - centre)).astype(jnp.bfloat16)
            key_sum_ref[:last_row, :] += simple_product(score_slope, query_rows)
            turned_ref[first_row:last_row, :] = (
                contract_first(score_slope, key_ref[:last_row, :]) * scale_factor
            )
        slope, term = norm_back(
            turned_ref[...], raw_ref[:, lanes], query_gain_ref[...], cosine_ref[...], sine_ref[...]
        )
        slope_ref[:, lanes] = slope
        gain_ref[0:1, :] += term
        return carry

    lax.fori_loop(0, grouping, head_step, 0)
    lanes = slice(grouping * head_size, (grouping + 1) * head_size)
    slope, term = norm_back(
        key_sum_ref[...] * scale_factor, raw_ref[:, lanes], key_gain_ref[...], cosine_ref[...], sine_ref[...]
    )
    slope_ref[:, lanes] = slope
    gain_ref[1:2, :] += term
    slope_ref[:, (grouping + 1) * head_size :] = value_sum_ref[...].astype(jnp.bfloat16)


def attention_backward(
    state_rows, weight, weight_start, raw, mixed, totals, tables, query_gain, key_gain, heads, grouping,
    triples, hidden_state, size, collective_id,
):
    total_rows, depth = state_rows.shape
    head_size = query_gain.shape[0]
    sequences = total_rows // SEQUENCE_LENGTH
    width = (grouping + 2) * head_size
    out_width = grouping * head_size
    block = min(256, SEQUENCE_LENGTH)
    first_block = weight_start // out_width
    single = pl.Buffered(1)
    table = pl.BlockSpec(tables[0].shape, lambda s, h: (0, 0))
    gain = pl.BlockSpec((1, head_size), lambda s, h: (0, 0))
    elements = heads * grouping * total_rows * SEQUENCE_LENGTH // 2
    whole_rows = pltpu.VMEM((SEQUENCE_LENGTH, head_size), jnp.float32)
    operands = [array for left, other_weight, _ in triples for array in (left, other_weight)]
    in_specs = [pl.BlockSpec(memory_space=pl.ANY)] * len(operands)
    in_specs += [
        pl.BlockSpec((SEQUENCE_LENGTH, depth), lambda s, h: (s, 0), pipeline_mode=single),
        pl.BlockSpec((depth, out_width), lambda s, h: (0, first_block + h)),
        pl.BlockSpec((SEQUENCE_LENGTH, width), lambda s, h: (s, h)),
        pl.BlockSpec((SEQUENCE_LENGTH, out_width), lambda s, h: (s, h)),
        pl.BlockSpec((1, grouping, SEQUENCE_LENGTH), lambda s, h: (h, 0, s)),
        table,
        table,
        gain,
        gain,
        pl.BlockSpec(hidden_state.shape, lambda s, h: (0, 0), pipeline_mode=single),
    ]
    operands += [
        state_rows, weight, raw, mixed, totals, *tables, query_gain.reshape(1, -1), key_gain.reshape(1, -1),
        hidden_state,
    ]
    return pl.pallas_call(
        functools.partial(
            attention_backward_kernel, size, grouping, head_size, block,
            tuple(first for _, _, first in triples),
        ),
        grid=(sequences, heads),
        out_shape=[
            jax.ShapeDtypeStruct((total_rows, heads * width), jnp.bfloat16),
            jax.ShapeDtypeStruct((8, head_size), jnp.float32),
            jax.ShapeDtypeStruct(hidden_state.shape, jnp.bfloat16),
        ],
        in_specs=in_specs,
        out_specs=[
            pl.BlockSpec((SEQUENCE_LENGTH, width), lambda s, h: (s, h)),
            pl.BlockSpec((8, head_size), lambda s, h: (0, 0)),
            pl.BlockSpec(hidden_state.shape, lambda s, h: (0, 0)),
        ],
        scratch_shapes=[
            pltpu.VMEM((grouping, SEQUENCE_LENGTH, head_size), jnp.bfloat16),
            pltpu.VMEM((SEQUENCE_LENGTH, head_size), jnp.bfloat16),
            pltpu.VMEM((SEQUENCE_LENGTH, head_size), jnp.bfloat16),
            pltpu.VMEM((SEQUENCE_LENGTH, out_width), jnp.bfloat16),
            whole_rows,
            whole_rows,
            whole_rows,
            whole_rows,
            whole_rows,
            *Scatter.scratch(size, *hidden_state.shape),
            *[part for left, other, _ in triples for part in Operand.scratch(size, left, other)],
        ],
        compiler_params=pltpu.CompilerParams(
            collective_id=collective_id, has_side_effects=True, vmem_limit_bytes=VMEM_LIMIT
        ),
        cost_estimate=pl.CostEstimate(
            flops=2 * total_rows * depth * heads * out_width + 10 * elements * head_size,
            bytes_accessed=100_000_000,
            transcendentals=elements,
        ),
        name="attention_backward",
    )(*operands)


def feed_half_kernel(
    half, tile, block, rows_far, cotangent_far, weight_far, hidden_far, slope_far,
    rows_ref, cotangent_ref, weight_ref, hidden_ref, slope_ref, row_sem, weight_sem, out_sem,
):
    total = rows_ref.shape[0]
    blocks = total // block
    tiles = half // tile

    def row_copies(index):
        piece = pl.ds(pl.multiple_of(index * block, block), block)
        return [
            pltpu.make_async_copy(far.at[piece], ref.at[piece], row_sem.at[at, index])
            for at, (far, ref) in enumerate(((rows_far, rows_ref), (cotangent_far, cotangent_ref)))
        ]

    def weight_copies(index):
        copies = []
        for part in range(3):
            columns = pl.ds(pl.multiple_of(part * half + index * tile, tile), tile)
            copies.append(
                pltpu.make_async_copy(
                    weight_far.at[:, columns], weight_ref.at[part, index], weight_sem.at[part, index]
                )
            )
        return copies

    def out_copies(index):
        piece = pl.ds(pl.multiple_of(index * block, block), block)
        return [
            pltpu.make_async_copy(ref.at[piece], far.at[piece], out_sem.at[at, index])
            for at, (far, ref) in enumerate(((hidden_far, hidden_ref), (slope_far, slope_ref)))
        ]

    for copy in row_copies(0) + weight_copies(0):
        copy.start()
    for index in range(1, tiles):
        for copy in weight_copies(index):
            copy.start()
    for index in range(1, blocks):
        for copy in row_copies(index):
            copy.start()

    def row_step(row_index, carry):
        piece = pl.ds(pl.multiple_of(row_index * block, block), block)
        for copy in row_copies(row_index):
            copy.wait()

        def step(index, carry):
            @pl.when(row_index == 0)
            def _():
                for copy in weight_copies(index):
                    copy.wait()

            start = pl.multiple_of(index * tile, tile)
            rows = rows_ref[piece, :]
            gate = simple_product(rows, weight_ref[0, index])
            up = simple_product(rows, weight_ref[1, index])
            back = simple_product(cotangent_ref[piece, :], weight_ref[2, index])
            sigmoid = 1.0 / (1.0 + jnp.exp(-gate))
            gated = gate * sigmoid
            hidden_ref[piece, pl.ds(start, tile)] = (gated * up).astype(jnp.bfloat16)
            slope_ref[piece, pl.ds(start, tile)] = (
                back * up * sigmoid * (1.0 + gate * (1.0 - sigmoid))
            ).astype(jnp.bfloat16)
            slope_ref[piece, pl.ds(half + start, tile)] = (back * gated).astype(jnp.bfloat16)
            return carry

        lax.fori_loop(0, tiles, step, 0)
        for copy in out_copies(row_index):
            copy.start()
        return carry

    lax.fori_loop(0, blocks, row_step, 0)
    for index in range(blocks):
        for copy in out_copies(index):
            copy.wait()


def feed_half(rows, cotangent, weight):
    total_rows, depth = rows.shape
    block = min(512, total_rows)
    half = weight.shape[1] // 3
    tile = 256 if half % 256 == 0 else 128
    blocks, tiles = total_rows // block, half // tile
    far = pl.BlockSpec(memory_space=pl.ANY)
    return pl.pallas_call(
        functools.partial(feed_half_kernel, half, tile, block),
        out_shape=[
            jax.ShapeDtypeStruct((total_rows, half), jnp.bfloat16),
            jax.ShapeDtypeStruct((total_rows, 2 * half), jnp.bfloat16),
        ],
        in_specs=[far] * 3,
        out_specs=[far] * 2,
        scratch_shapes=[
            pltpu.VMEM(rows.shape, rows.dtype),
            pltpu.VMEM(rows.shape, rows.dtype),
            pltpu.VMEM((3, tiles, depth, tile), weight.dtype),
            pltpu.VMEM((total_rows, half), jnp.bfloat16),
            pltpu.VMEM((total_rows, 2 * half), jnp.bfloat16),
            pltpu.SemaphoreType.DMA((2, blocks)),
            pltpu.SemaphoreType.DMA((3, tiles)),
            pltpu.SemaphoreType.DMA((2, blocks)),
        ],
        compiler_params=pltpu.CompilerParams(vmem_limit_bytes=VMEM_LIMIT),
        cost_estimate=pl.CostEstimate(
            flops=6 * total_rows * depth * half,
            bytes_accessed=2 * (2 * total_rows * depth + 3 * depth * half),
            transcendentals=total_rows * half,
        ),
        name="feed_half",
    )(rows, cotangent, weight)


def grad_kernel(pair_count, with_other, order_ref, *refs):
    pairs = [refs[2 * p : 2 * p + 2] for p in range(pair_count)]
    refs = refs[2 * pair_count :]
    step = pl.program_id(0)
    if with_other:
        other_ref, refs = refs[0], refs[1:]
        out_refs, held_ref, copy_sem = refs[:-2], refs[-2], refs[-1]
    else:
        out_ref = refs[0]
    start = 0
    for left_ref, right_ref in pairs:
        width = right_ref.shape[1]
        tile = next(t for t in (768, 512, 384, 256, 128) if width % t == 0)
        for column in range(0, width, tile):
            values = simple_product(left_ref[...], right_ref[:, column : column + tile])
            columns = slice(start + column, start + column + tile)
            if with_other:
                values = values + other_ref[0, :, columns].astype(jnp.float32)
                held_ref[step, :, columns] = values.astype(jnp.bfloat16)
            else:
                out_ref[0, :, columns] = values.astype(jnp.bfloat16)
        start += width
    if with_other:
        copies = [
            pltpu.make_async_copy(held_ref.at[index], out_ref, copy_sem.at[index])
            for index, out_ref in enumerate(out_refs)
        ]
        for index, copy in enumerate(copies):
            pl.when(step == index)(copy.start)

        @pl.when(step == len(copies) - 1)
        def _():
            for copy in copies:
                copy.wait()


def grad_blocks(order, pairs, other=None):
    count = order.shape[0]
    depth, total_rows = pairs[0][0].shape
    block = depth // lax.axis_size("dp")
    width = sum(right.shape[1] for _, right in pairs)
    in_specs = []
    operands = []
    for left, right in pairs:
        in_specs += [
            pl.BlockSpec((block, total_rows), lambda k, at: (at[k], 0)),
            pl.BlockSpec(right.shape, lambda k, at: (0, 0), pipeline_mode=pl.Buffered(1)),
        ]
        operands += [left, right]
    scratch = []
    if other is not None:
        in_specs.append(pl.BlockSpec((1, block, width), lambda k, at: (k, 0, 0)))
        operands.append(other)
        out_shape = [jax.ShapeDtypeStruct((block, width), jnp.bfloat16)] * count
        out_specs = [pl.BlockSpec(memory_space=pl.ANY)] * count
        scratch = [
            pltpu.VMEM((count, block, width), jnp.bfloat16),
            pltpu.SemaphoreType.DMA((count,)),
        ]
    else:
        out_shape = [jax.ShapeDtypeStruct((count, block, width), jnp.bfloat16)]
        out_specs = [pl.BlockSpec((1, block, width), lambda k, at: (k, 0, 0))]
    out = pl.pallas_call(
        functools.partial(grad_kernel, len(pairs), other is not None),
        grid_spec=pltpu.PrefetchScalarGridSpec(
            num_scalar_prefetch=1,
            grid=(count,),
            in_specs=in_specs,
            out_specs=out_specs,
            scratch_shapes=scratch,
        ),
        out_shape=out_shape,
        compiler_params=pltpu.CompilerParams(vmem_limit_bytes=VMEM_LIMIT),
        cost_estimate=pl.CostEstimate(
            flops=2 * total_rows * count * block * width,
            bytes_accessed=2 * (total_rows * count * block * len(pairs) + width * (total_rows + count * block)),
            transcendentals=0,
        ),
        name="grad_blocks",
    )(order, *operands)
    return out if other is not None else out[0]


def reduce_over_chips(pairs, sizes):
    data_size = sizes[0]
    chips = data_size // 2
    me = lax.axis_index("dp")
    chip, core = me // 2, lax.rem(me, 2)
    ahead = lax.rem(chip + jnp.arange(chips, dtype=jnp.int32), chips) * 2
    other = lax.ppermute(
        grad_blocks(ahead + (1 - core), pairs),
        "dp",
        [(device, device ^ 1) for device in range(data_size)],
    )
    blocks = grad_blocks(ahead + core, pairs, other)
    up = lax.ppermute(blocks[chips - 1], "dp", [(device, device + 2) for device in range(2)])
    down = lax.ppermute(
        blocks[1],
        "dp",
        [(device, device - 2) for device in range(data_size - 2, data_size)],
    )
    return blocks, up, down


def pack_mixing_kernel(heads, query_ref, key_ref, value_ref, output_ref, out_ref):
    query_width = query_ref.shape[1] // heads
    head_size = key_ref.shape[1] // heads
    start = 0
    for head in range(heads):
        for ref, part in ((query_ref, query_width), (key_ref, head_size), (value_ref, head_size)):
            out_ref[:, start : start + part] = ref[:, head * part : (head + 1) * part]
            start += part
    out_ref[:, start:] = output_ref[...].T


def pack_feed_kernel(gate_ref, up_ref, down_ref, first_ref, second_ref):
    start = 0
    for out_ref in (first_ref, second_ref):
        width = out_ref.shape[1] // 3
        part = slice(start, start + width)
        out_ref[:, :width] = gate_ref[:, part]
        out_ref[:, width : 2 * width] = up_ref[:, part]
        out_ref[:, 2 * width :] = down_ref[part, :].T
        start += width


def finish_kernel(
    heads, own_ref, up_ref, down_ref, second_ref, mixing_ref, output_total_ref, terms_ref, output_rows_ref, input_rows_ref,
    output_rows_out, input_rows_out, attention_term_out, query_out, key_out, value_out, query_gain_out, key_gain_out,
    output_out, feed_term_out, gate_out, up_out, down_out,
):
    output_rows_out[...] = output_rows_ref[...]
    input_rows_out[...] = input_rows_ref[...]
    count = attention_term_out.shape[0]
    attention_term_out[...] = terms_ref[:count, :]
    feed_term_out[...] = terms_ref[count : 2 * count, :]
    query_gain_out[...] = terms_ref[2 * count : 2 * count + 1, :]
    key_gain_out[...] = terms_ref[2 * count + 1 : 2 * count + 2, :]
    start = 0
    for total_refs in ((own_ref, up_ref, down_ref), (second_ref,)):
        width = total_refs[0].shape[1] // 3
        part = slice(start, start + width)

        def total(index):
            columns = slice(index * width, (index + 1) * width)
            return sum(ref[:, columns].astype(jnp.float32) for ref in total_refs)

        gate_out[:, part] = total(0)
        up_out[:, part] = total(1)
        down_out[part, :] = total(2).T
        start += width
    query_width = query_out.shape[1] // heads
    head_size = key_out.shape[1] // heads
    start = 0
    for head in range(heads):
        for out, part in ((query_out, query_width), (key_out, head_size), (value_out, head_size)):
            out[:, head * part : (head + 1) * part] = mixing_ref[:, start : start + part].astype(
                jnp.float32
            )
            start += part
    output_out[...] = output_total_ref[...].astype(jnp.float32).T


def whole_call(body, shapes, *operands):
    return pl.pallas_call(
        body,
        out_shape=shapes,
        in_specs=[pl.BlockSpec(memory_space=pltpu.VMEM)] * len(operands),
        out_specs=[pl.BlockSpec(memory_space=pltpu.VMEM)] * len(shapes),
        compiler_params=pltpu.CompilerParams(vmem_limit_bytes=VMEM_LIMIT),
        cost_estimate=pl.CostEstimate(
            flops=0, bytes_accessed=4 * sum(operand.size for operand in operands), transcendentals=0
        ),
    )(*operands)


def per_device(
    block_input,
    attention_gain,
    query_weight,
    key_matrix,
    value_matrix,
    query_gain,
    key_gain,
    output_weight,
    feed_gain,
    gate_weight,
    up_weight,
    down_weight,
    out_cotangent,
):
    size = lax.axis_size("tensor")
    sizes = (lax.axis_size("dp"), size)
    model_width = block_input.shape[1]
    head_size = query_gain.shape[0]
    query_columns = query_weight.shape[1]
    key_columns = key_matrix.shape[1]
    heads = key_columns // head_size
    grouping = query_columns // key_columns
    hidden_columns = gate_weight.shape[1]
    qkv_columns = query_columns + 2 * key_columns
    first_columns = hidden_columns * 2 // 3 // 256 * 256 or hidden_columns // 2
    second_columns = hidden_columns - first_columns
    tables = turn_tables(head_size)

    block_width = query_weight.shape[0]
    (mixing_local,) = whole_call(
        functools.partial(pack_mixing_kernel, heads),
        [jax.ShapeDtypeStruct((block_width, qkv_columns + query_columns), jnp.bfloat16)],
        query_weight, key_matrix, value_matrix, output_weight,
    )
    mixing_full = lax.all_gather(mixing_local, "dp", axis=0, tiled=True)
    feed_locals = whole_call(
        pack_feed_kernel,
        [
            jax.ShapeDtypeStruct((block_width, 3 * columns), jnp.bfloat16)
            for columns in (first_columns, second_columns)
        ],
        gate_weight, up_weight, down_weight,
    )
    feed_full = [lax.all_gather(part, "dp", axis=0, tiled=True) for part in feed_locals]

    input_float = block_input.astype(jnp.float32)
    first_scale = row_scale(input_float)
    first_unit = input_float * first_scale
    mixer_local = (first_unit * attention_gain).astype(jnp.bfloat16)
    mixer_rows, mixer_turned, cotangent_rows, cotangent_turned = gather_rows(
        (mixer_local, out_cotangent), size, 0
    )

    raw, mixed_rows, totals = attention_forward(
        mixer_rows, mixing_full, tables, query_gain, key_gain, heads, grouping
    )
    local_shape = block_input.shape
    local_rows = local_shape[0]
    gain_rows = model_width // head_size
    gathered_shapes = [
        jax.ShapeDtypeStruct((size * local_rows, model_width), jnp.bfloat16),
        jax.ShapeDtypeStruct((model_width, size * local_rows), jnp.bfloat16),
    ]
    local_float = jax.ShapeDtypeStruct(local_shape, jnp.float32)
    local_half = jax.ShapeDtypeStruct(local_shape, jnp.bfloat16)
    row_sum = pltpu.VMEM((1, model_width), jnp.float32)
    own_rows = pltpu.VMEM(local_shape, jnp.bfloat16)
    scatter_scratch = Scatter.scratch(size, *local_shape)
    gather_scratch = Gather.scratch(size, *local_shape)
    feed_rows, feed_turned, hidden_state = scatter_call(
        functools.partial(between_forward_kernel, size),
        [(mixed_rows, mixing_full, qkv_columns)],
        size,
        [block_input, feed_gain.reshape(1, -1)],
        [],
        [*gathered_shapes, local_float],
        True,
        [own_rows, *scatter_scratch, *gather_scratch],
        1,
    )

    hidden_first, slope_first = feed_half(feed_rows, cotangent_rows, feed_full[0])
    blocks, up, down = reduce_over_chips(
        [(feed_turned, slope_first), (cotangent_turned, hidden_first)], sizes
    )
    blocks, later_full = lax.optimization_barrier((blocks, feed_full[1]))
    hidden_second, slope_second = feed_half(feed_rows, cotangent_rows, later_full)
    plain_order = jnp.arange(sizes[0], dtype=jnp.int32)
    second_grad = grad_blocks(
        plain_order, [(feed_turned, slope_second), (cotangent_turned, hidden_second)]
    ).reshape(model_width, -1)
    second_grad, slope_second = lax.optimization_barrier((second_grad, slope_second))
    second_total = lax.psum_scatter(second_grad, "dp", scatter_dimension=0, tiled=True)
    chips = sizes[0] // 2
    middle_steps = tuple(range(2, chips - 1))
    chain_block = jax.ShapeDtypeStruct(blocks[0].shape, jnp.bfloat16)
    state_rows, state_turned, state_slope, feed_term, rising, falling = scatter_call(
        functools.partial(between_backward_kernel, size, chips, middle_steps),
        [(slope_first, feed_full[0], 0), (slope_second, later_full, 0)],
        size,
        [hidden_state, out_cotangent, feed_gain.reshape(1, -1)],
        [blocks[chips - step] for step in middle_steps]
        + [blocks[step] for step in middle_steps]
        + [up, down, blocks[1], blocks[chips - 1]],
        [
            *gathered_shapes,
            local_float,
            jax.ShapeDtypeStruct((gain_rows, head_size), jnp.float32),
            chain_block,
            chain_block,
        ],
        True,
        [
            own_rows,
            row_sum,
            pltpu.SemaphoreType.DMA((2,)),
            *scatter_scratch,
            *gather_scratch,
            *Chain.scratch(len(middle_steps), *blocks[0].shape),
        ],
        2,
    )
    up = lax.ppermute(
        rising, "dp", [(device, device + 2) for device in range(sizes[0] - 2)]
    )
    down = lax.ppermute(
        falling, "dp", [(device, device - 2) for device in range(2, sizes[0])]
    )
    output_grad = grad_blocks(plain_order, [(state_turned, mixed_rows)]).reshape(model_width, -1)
    output_grad, state_rows = lax.optimization_barrier((output_grad, state_rows))
    output_total = lax.psum_scatter(output_grad, "dp", scatter_dimension=0, tiled=True)
    qkv_slope, head_terms, block_output = attention_backward(
        state_rows, mixing_full, qkv_columns, raw, mixed_rows, totals, tables,
        query_gain, key_gain, heads, grouping,
        [
            (hidden_first, feed_full[0], 2 * first_columns),
            (hidden_second, later_full, 2 * second_columns),
        ],
        hidden_state, size, 4,
    )
    mixing_grad = grad_blocks(plain_order, [(mixer_turned, qkv_slope)]).reshape(model_width, -1)
    mixing_grad, qkv_slope = lax.optimization_barrier((mixing_grad, qkv_slope))
    mixing_total = lax.psum_scatter(mixing_grad, "dp", scatter_dimension=0, tiled=True)
    terms_shape = (2 * gain_rows + head_terms.shape[0], head_size)
    input_gradient, terms = scatter_call(
        functools.partial(last_kernel, sizes),
        [(qkv_slope, mixing_full, 0)],
        size,
        [
            block_input,
            attention_gain.reshape(1, -1),
            state_slope,
            jnp.concatenate([feed_term, head_terms], axis=0),
            mixer_rows,
        ],
        [],
        [local_half, jax.ShapeDtypeStruct(terms_shape, jnp.float32)],
        False,
        [
            row_sum,
            pltpu.VMEM(terms_shape, jnp.float32),
            pltpu.VMEM(terms_shape, jnp.float32),
            pltpu.VMEM((size, *terms_shape), jnp.float32),
            pltpu.VMEM((sizes[0], *terms_shape), jnp.float32),
            *[pltpu.SemaphoreType.DMA((count - 1,)) for count in (size, size, *sizes[:1] * 2)],
            *scatter_scratch,
        ],
        3,
    )

    def whole_float(*shape):
        return jax.ShapeDtypeStruct(shape, jnp.float32)

    outs = whole_call(
        functools.partial(finish_kernel, heads),
        [
            local_half,
            local_half,
            whole_float(gain_rows, head_size),
            whole_float(block_width, query_columns),
            whole_float(block_width, key_columns),
            whole_float(block_width, key_columns),
            whole_float(1, head_size),
            whole_float(1, head_size),
            whole_float(query_columns, block_width),
            whole_float(gain_rows, head_size),
            whole_float(block_width, hidden_columns),
            whole_float(block_width, hidden_columns),
            whole_float(hidden_columns, block_width),
        ],
        blocks[0], up, down, second_total, mixing_total, output_total, terms, block_output, input_gradient,
    )
    return tuple(
        out.reshape(-1) if index in (2, 6, 7, 9) else out for index, out in enumerate(outs)
    )


def solution(mesh):
    in_specs = (
        P(("dp", "tensor"), None),
        P(),
        P("dp", "tensor"),
        P("dp", "tensor"),
        P("dp", "tensor"),
        P(),
        P(),
        P("tensor", "dp"),
        P(),
        P("dp", "tensor"),
        P("dp", "tensor"),
        P("tensor", "dp"),
        P(("dp", "tensor"), None),
    )
    out_specs = (
        P(("dp", "tensor"), None),
        P(("dp", "tensor"), None),
        P(),
        P("dp", "tensor"),
        P("dp", "tensor"),
        P("dp", "tensor"),
        P(),
        P(),
        P("tensor", "dp"),
        P(),
        P("dp", "tensor"),
        P("dp", "tensor"),
        P("tensor", "dp"),
    )

    return jax.shard_map(per_device, mesh=mesh, in_specs=in_specs, out_specs=out_specs, check_vma=False)
```

```python
import functools

import jax
import jax.numpy as jnp
import numpy as np
from jax import lax
from jax.experimental import pallas as pl
from jax.experimental.pallas import tpu as pltpu
from jax.sharding import PartitionSpec as P


SEQUENCE_LENGTH = 1024

epsilon = 1e-06
rope_base = 1000000.0


MESH = pl.DeviceIdType.MESH
VMEM_LIMIT = 62 * 1024 * 1024


def row_scale(values):
    return lax.rsqrt(jnp.mean(values * values, axis=-1, keepdims=True) + epsilon)


def times_transposed(first_operand, second_operand):
    return lax.dot_general(
        first_operand, second_operand, (((1,), (1,)), ((), ())), preferred_element_type=jnp.float32
    )


def simple_product(first_operand, second_operand):
    return jnp.dot(first_operand, second_operand, preferred_element_type=jnp.float32)


def remote(source, target, send_sem, recv_sem, peer, axis="tensor"):
    return pltpu.make_async_remote_copy(
        src_ref=source,
        dst_ref=target,
        send_sem=send_sem,
        recv_sem=recv_sem,
        device_id={axis: peer},
        device_id_type=MESH,
    )


def greet(peers):
    barrier = pltpu.get_barrier_semaphore()
    for axis, peer in peers:
        pl.semaphore_signal(barrier, inc=1, device_id={axis: peer}, device_id_type=MESH)
    pl.semaphore_wait(barrier, len(peers))


def square_peers(me):
    column = lax.rem(me, 2)
    row = me // 2
    return row * 2 + (1 - column), (1 - row) * 2 + column, (1 - row) * 2 + (1 - column)


def neighbours(size):
    if size == 4:
        beside, below, _ = square_peers(lax.axis_index("tensor"))
        return [("tensor", beside), ("tensor", below)]
    return [("tensor", peer) for peer in other_members("tensor", size)]


def other_members(axis, count):
    me = lax.axis_index(axis)
    return [lax.rem(me + step, count) for step in range(1, count)]


class Gather:
    def __init__(
        self, size, own_ref, out_ref, turned_out_ref, held_ref, turned_ref, send_sem, recv_sem, local_sem, turned_sem
    ):
        self.size, self.own, self.out, self.held = size, own_ref, out_ref, held_ref
        self.turned_out, self.turned = turned_out_ref, turned_ref
        self.send_sem, self.recv_sem, self.local_sem = send_sem, recv_sem, local_sem
        self.turned_sem = turned_sem
        self.me = lax.axis_index("tensor")
        self.rows = own_ref.shape[0]
        self.copies, self.stores, self.turns = [], [], []

    @staticmethod
    def scratch(size, rows, columns):
        sends, local = (6, 8) if size == 4 else (size - 1, size)
        return [
            pltpu.VMEM((size, rows, columns), jnp.bfloat16),
            pltpu.VMEM((columns, size * rows), jnp.bfloat16),
            pltpu.SemaphoreType.DMA((sends,)),
            pltpu.SemaphoreType.DMA((sends,)),
            pltpu.SemaphoreType.DMA((local,)),
            pltpu.SemaphoreType.DMA((local,)),
        ]

    def send(self, source, target, peer):
        index = len(self.copies)
        copy = remote(source, target, self.send_sem.at[index], self.recv_sem.at[index], peer)
        copy.start()
        self.copies.append(copy)
        return copy

    def store(self, source, start, count):
        piece = pl.ds(pl.multiple_of(start, count), count)
        copy = pltpu.make_async_copy(source, self.out.at[piece], self.local_sem.at[len(self.stores)])
        copy.start()
        self.stores.append(copy)
        width = min(256, self.turned.shape[0])

        def turn_part(index, carry):
            columns = pl.ds(pl.multiple_of(index * width, width), width)
            self.turned[columns, piece] = source[:, columns].T
            return carry

        lax.fori_loop(0, self.turned.shape[0] // width, turn_part, 0)
        turn_copy = pltpu.make_async_copy(
            self.turned.at[:, piece], self.turned_out.at[:, piece], self.turned_sem.at[len(self.turns)]
        )
        turn_copy.start()
        self.turns.append(turn_copy)

    def start(self):
        own, held, rows = self.own, self.held, self.rows
        if self.size != 4:
            for peer in other_members("tensor", self.size):
                self.send(own, held.at[self.me], peer)
            return
        beside, below, _ = square_peers(self.me)
        half = rows // 2
        first, second = pl.ds(0, half), pl.ds(half, half)
        self.send(own.at[first], held.at[self.me, first], beside)
        self.send(own.at[second], held.at[self.me, second], below)
        self.send(own.at[second], held.at[self.me, second], beside)
        self.send(own.at[first], held.at[self.me, first], below)

    def forward(self):
        own, held, rows = self.own, self.held, self.rows
        if self.size != 4:
            self.store(own, self.me * rows, rows)
            return
        beside, below, _ = square_peers(self.me)
        half = rows // 2
        first, second = pl.ds(0, half), pl.ds(half, half)
        x_first, y_second = self.copies[:2]
        self.store(own.at[first], self.me * rows, half)
        self.store(own.at[second], self.me * rows + half, half)
        x_first.wait_recv()
        self.send(held.at[beside, first], held.at[beside, first], below)
        y_second.wait_recv()
        self.send(held.at[below, second], held.at[below, second], beside)

    def finish(self):
        held, rows = self.held, self.rows
        if self.size != 4:
            for step, copy in enumerate(self.copies):
                copy.wait_recv()
                slot = lax.rem(self.me + self.size - step - 1, self.size)
                self.store(held.at[slot], slot * rows, rows)
        else:
            beside, below, across = square_peers(self.me)
            half = rows // 2
            first, second = pl.ds(0, half), pl.ds(half, half)
            x_second, y_first, y_pass, x_pass = self.copies[2:]
            self.store(held.at[beside, first], beside * rows, half)
            self.store(held.at[below, second], below * rows + half, half)
            x_second.wait_recv()
            self.store(held.at[beside, second], beside * rows + half, half)
            y_first.wait_recv()
            self.store(held.at[below, first], below * rows, half)
            y_pass.wait_recv()
            self.store(held.at[across, first], across * rows, half)
            x_pass.wait_recv()
            self.store(held.at[across, second], across * rows + half, half)
        for copy in self.copies:
            copy.wait_send()
        for copy in self.stores + self.turns:
            copy.wait()


def gather_kernel(size, count, *refs):
    own_refs, out_refs, rest = refs[:count], refs[count : 3 * count], refs[3 * count :]
    greet(neighbours(size))
    gathers = [
        Gather(size, own_refs[k], *out_refs[2 * k : 2 * k + 2], *rest[6 * k : 6 * k + 6])
        for k in range(count)
    ]
    for gather in gathers:
        gather.start()
        gather.forward()
    for gather in gathers:
        gather.finish()


def gather_rows(arrays, size, collective_id):
    count = len(arrays)
    rows, columns = arrays[0].shape
    scratch = []
    out_shape = []
    for _ in arrays:
        scratch += Gather.scratch(size, rows, columns)
        out_shape += [
            jax.ShapeDtypeStruct((size * rows, columns), jnp.bfloat16),
            jax.ShapeDtypeStruct((columns, size * rows), jnp.bfloat16),
        ]
    return pl.pallas_call(
        functools.partial(gather_kernel, size, count),
        out_shape=out_shape,
        in_specs=[pl.BlockSpec(memory_space=pltpu.VMEM)] * count,
        out_specs=[pl.BlockSpec(memory_space=pl.ANY)] * len(out_shape),
        scratch_shapes=scratch,
        compiler_params=pltpu.CompilerParams(
            collective_id=collective_id, has_side_effects=True, vmem_limit_bytes=VMEM_LIMIT
        ),
        cost_estimate=pl.CostEstimate(
            flops=0, bytes_accessed=count * 30 * size * rows * columns, transcendentals=0
        ),
        name="gather_rows",
    )(*arrays)


class Operand:
    def __init__(self, size, first_column, left_far, weight_far, left, weight, left_sem, weight_sem):
        self.left, self.weight = left, weight
        self.rows = left.shape[0] // size
        self.tile = min(512, weight.shape[0])
        self.far = left_far, weight_far
        self.first_column = first_column
        self.left_sem, self.weight_sem = left_sem, weight_sem

    @staticmethod
    def scratch(size, left, weight):
        width = left.shape[1]
        return [
            pltpu.VMEM(left.shape, left.dtype),
            pltpu.VMEM((weight.shape[0], width), weight.dtype),
            pltpu.SemaphoreType.DMA((size,)),
            pltpu.SemaphoreType.DMA((max(1, weight.shape[0] // 512),)),
        ]

    def left_copy(self, slot, owner):
        piece = pl.ds(pl.multiple_of(owner * self.rows, self.rows), self.rows)
        return pltpu.make_async_copy(self.far[0].at[piece], self.left.at[piece], self.left_sem.at[slot])

    def weight_copy(self, index):
        piece = pl.ds(pl.multiple_of(index * self.tile, self.tile), self.tile)
        columns = pl.ds(self.first_column, self.left.shape[1])
        return pltpu.make_async_copy(
            self.far[1].at[piece, columns], self.weight.at[piece], self.weight_sem.at[index]
        )


def block_product(operands, start, rows, fresh, write):
    total = operands[0].weight.shape[0]
    tile = operands[0].tile
    start = pl.multiple_of(start, rows)

    def step(index, carry):
        @pl.when(fresh)
        def _():
            for operand in operands:
                operand.weight_copy(index).wait()

        columns = pl.ds(pl.multiple_of(index * tile, tile), tile)
        values = None
        for operand in operands:
            part = times_transposed(
                operand.left[pl.ds(start, rows), :], operand.weight[columns, :]
            )
            values = part if values is None else values + part
        write(columns, values)
        return carry

    lax.fori_loop(0, total // tile, step, 0)


class Scatter:
    def __init__(self, size, outgoing, *rest):
        self.size, self.outgoing = size, outgoing
        if size == 4:
            self.passing, rest = rest[0], rest[1:]
        self.arriving, self.send_sem, self.recv_sem = rest
        self.rows = outgoing.shape[1]
        self.me = lax.axis_index("tensor")
        self.copies, self.starts = self.plan()

    @staticmethod
    def scratch(size, rows, columns):
        if size == 4:
            sends = 6
            buffers = [
                pltpu.VMEM((4, rows, columns), jnp.bfloat16),
                pltpu.VMEM((2, rows // 2, columns), jnp.bfloat16),
                pltpu.VMEM((2, rows, columns), jnp.bfloat16),
            ]
        else:
            sends = size - 1
            buffers = [
                pltpu.VMEM((size, rows, columns), jnp.bfloat16),
                pltpu.VMEM((size - 1, rows, columns), jnp.bfloat16),
            ]
        return buffers + [pltpu.SemaphoreType.DMA((sends,)), pltpu.SemaphoreType.DMA((sends,))]

    def prepare(self, index, source, target, peer):
        return remote(source, target, self.send_sem.at[index], self.recv_sem.at[index], peer)

    def plan(self):
        outgoing, arriving = self.outgoing, self.arriving
        if self.size != 4:
            copies = [
                self.prepare(step, outgoing.at[step], arriving.at[step], peer)
                for step, peer in enumerate(other_members("tensor", self.size))
            ]
            return copies, tuple((step, step) for step in range(self.size - 1))
        beside, below, _ = square_peers(self.me)
        half = self.rows // 2
        first, second = pl.ds(0, half), pl.ds(half, half)
        copies = [
            self.prepare(0, outgoing.at[0, first], self.passing.at[0], beside),
            self.prepare(1, outgoing.at[0, second], self.passing.at[1], below),
            self.prepare(2, outgoing.at[1, first], arriving.at[0, first], beside),
            self.prepare(3, outgoing.at[2, second], arriving.at[1, second], below),
            self.prepare(4, outgoing.at[1, second], arriving.at[0, second], beside),
            self.prepare(5, outgoing.at[2, first], arriving.at[1, first], below),
        ]
        return copies, ((0, 0), (0, 1), (1, 2), (2, 3))

    def owner(self, slot):
        if self.size != 4:
            return lax.rem(self.me + slot + 1, self.size)
        beside, below, across = square_peers(self.me)
        return jnp.where(
            slot == 0, across, jnp.where(slot == 1, beside, jnp.where(slot == 2, below, self.me))
        )

    def load(self, operands):
        tiles = operands[0].weight.shape[0] // operands[0].tile
        for operand in operands:
            operand.left_copy(0, self.owner(0)).start()
        for index in range(tiles):
            for operand in operands:
                operand.weight_copy(index).start()
        for slot in range(1, self.size):
            for operand in operands:
                operand.left_copy(slot, self.owner(slot)).start()

    def fill(self, operands, look=None, slots=None):
        rows = self.rows

        def step(slot, carry):
            owner = self.owner(slot)
            for operand in operands:
                operand.left_copy(slot, owner).wait()

            def write(columns, values):
                self.outgoing[slot, :, columns] = values.astype(self.outgoing.dtype)
                if look is not None:
                    look(owner, columns, values)

            block_product(operands, owner * rows, rows, slot == 0, write)
            for at, index in self.starts:
                pl.when(slot == at)(self.copies[index].start)
            return carry

        lax.fori_loop(*(slots or (0, self.size)), step, 0)

    def relay(self):
        if self.size != 4:
            return
        half = self.rows // 2
        x_pass, y_pass, _, _, x_second, y_first = self.copies
        for arrival, source, slot, start, onward in (
            (y_pass, 1, 1, half, x_second),
            (x_pass, 0, 2, 0, y_first),
        ):
            arrival.wait_recv()
            piece = pl.ds(start, half)
            self.outgoing[slot, piece, :] = (
                self.outgoing[slot, piece, :].astype(jnp.float32)
                + self.passing[source].astype(jnp.float32)
            ).astype(self.outgoing.dtype)
            onward.start()

    def collect(self):
        for copy in self.copies[2:] if self.size == 4 else self.copies:
            copy.wait_recv()

    def total(self, piece):
        total = self.outgoing[self.size - 1, piece, :].astype(jnp.float32)
        for index in range(self.arriving.shape[0]):
            total = total + self.arriving[index, piece, :].astype(jnp.float32)
        return total

    def drain(self):
        for copy in self.copies:
            copy.wait_send()


class Chain:
    def __init__(
        self, chips, steps, rising_refs, falling_refs, up_ref, down_ref,
        rise, fall, up, down, load_sem, send_sem, recv_sem,
    ):
        self.chips, self.steps = chips, steps
        self.rise, self.fall, self.up, self.down = rise, fall, up, down
        device = lax.axis_index("dp")
        self.chip = device // 2
        count = len(steps)
        self.loads = [
            pltpu.make_async_copy(source, target, load_sem.at[index])
            for index, (source, target) in enumerate(
                [(up_ref, up.at[0]), (down_ref, down.at[0])]
                + [(ref, rise.at[index]) for index, ref in enumerate(rising_refs)]
                + [(ref, fall.at[index]) for index, ref in enumerate(falling_refs)]
            )
        ]
        above = lax.rem(device + 2, 2 * chips)
        under = lax.rem(device + 2 * chips - 2, 2 * chips)
        self.neighbours = [("dp", above), ("dp", under)]
        self.rises = [
            remote(rise.at[i], up.at[i + 1], send_sem.at[i], recv_sem.at[i], above, "dp")
            for i in range(count)
        ]
        self.falls = [
            remote(
                fall.at[i], down.at[i + 1], send_sem.at[count + i], recv_sem.at[count + i], under, "dp"
            )
            for i in range(count)
        ]

    @staticmethod
    def scratch(count, rows, columns):
        return [
            pltpu.VMEM((count, rows, columns), jnp.bfloat16),
            pltpu.VMEM((count, rows, columns), jnp.bfloat16),
            pltpu.VMEM((count + 1, rows, columns), jnp.bfloat16),
            pltpu.VMEM((count + 1, rows, columns), jnp.bfloat16),
            pltpu.SemaphoreType.DMA((2 * count + 2,)),
            pltpu.SemaphoreType.DMA((2 * count,)),
            pltpu.SemaphoreType.DMA((2 * count,)),
        ]

    def load(self):
        for copy in self.loads:
            copy.start()

    def step(self, index):
        if index == 0:
            for copy in self.loads:
                copy.wait()
        step = self.steps[index]
        rows = self.rise.shape[1]
        sends_up = self.chip < step
        sends_down = self.chip >= self.chips - step

        @pl.when(sends_up & (self.chip > 0))
        def _():
            def add(piece):
                self.rise[index, piece, :] = add_rounded(
                    self.rise[index, piece, :], self.up[index, piece, :]
                )

            over_pieces(rows, add)

        pl.when(sends_up)(self.rises[index].start)

        @pl.when(sends_down & (self.chip < self.chips - 1))
        def _():
            def add(piece):
                self.fall[index, piece, :] = add_rounded(
                    self.fall[index, piece, :], self.down[index, piece, :]
                )

            over_pieces(rows, add)

        pl.when(sends_down)(self.falls[index].start)

    def arrives(self, index):
        step = self.steps[index]
        from_under = (self.chip > 0) & (self.chip <= step)
        from_above = (self.chip < self.chips - 1) & (self.chip >= self.chips - step - 1)
        return from_under, from_above

    def wait(self, index):
        from_under, from_above = self.arrives(index)
        pl.when(from_under)(self.rises[index].wait_recv)
        pl.when(from_above)(self.falls[index].wait_recv)

    def drain(self):
        for index, step in enumerate(self.steps):
            pl.when(self.chip < step)(self.rises[index].wait_send)
            pl.when(self.chip >= self.chips - step)(self.falls[index].wait_send)


def add_rounded(first, second):
    return (first.astype(jnp.float32) + second.astype(jnp.float32)).astype(jnp.bfloat16)


def over_pieces(rows, body):
    count = min(32, rows)

    def step(index, carry):
        body(pl.ds(pl.multiple_of(index * count, count), count))
        return carry

    lax.fori_loop(0, rows // count, step, 0)


def send_terms(axis, peers, source, landing, send_sem, recv_sem):
    me = lax.axis_index(axis)
    landing[me] = source[...]
    copies = []
    for step, peer in enumerate(peers):
        copy = remote(source, landing.at[me], send_sem.at[step], recv_sem.at[step], peer, axis)
        copy.start()
        copies.append(copy)
    return copies


def add_terms(landing, copies):
    for copy in copies:
        copy.wait_recv()
    total = landing[0]
    for index in range(1, landing.shape[0]):
        total = total + landing[index]
    return total


def split_operands(refs, size, first_columns):
    count = len(first_columns)
    far, refs, scratch = refs[: 2 * count], refs[2 * count : -4 * count], refs[-4 * count :]
    operands = [
        Operand(size, first, *far[2 * p : 2 * p + 2], *scratch[4 * p : 4 * p + 4])
        for p, first in enumerate(first_columns)
    ]
    return operands, refs


def store_row(target_ref, row_ref):
    width = target_ref.shape[1]
    for index in range(row_ref.shape[1] // width):
        target_ref[index : index + 1, :] = row_ref[:, index * width : (index + 1) * width]


def between_forward_kernel(size, first_columns, *refs):
    operands, refs = split_operands(refs, size, first_columns)
    input_ref, gain_ref, gathered_ref, turned_ref, state_ref, own_ref = refs[:6]
    buffers = 5 if size == 4 else 4
    scatter = Scatter(size, *refs[6 : 6 + buffers])
    gather = Gather(size, own_ref, gathered_ref, turned_ref, *refs[6 + buffers :])
    scatter.load(operands)
    greet(neighbours(size))
    scatter.fill(operands)
    scatter.relay()
    scatter.collect()

    def norm(piece):
        state = input_ref[piece, :].astype(jnp.float32) + scatter.total(piece)
        state_ref[piece, :] = state
        own_ref[piece, :] = (state * row_scale(state) * gain_ref[...]).astype(own_ref.dtype)

    over_pieces(own_ref.shape[0], norm)
    gather.start()
    gather.forward()
    gather.finish()
    scatter.drain()


def between_backward_kernel(size, chips, steps, first_columns, *refs):
    operands, refs = split_operands(refs, size, first_columns)
    state_ref, cotangent_ref, gain_ref = refs[:3]
    chain_count = 2 * len(steps) + 2
    chain_refs, refs = refs[3 : 3 + chain_count], refs[3 + chain_count :]
    gathered_ref, gathered_turned_ref, slope_ref, term_ref, up_out_ref, down_out_ref = refs[:6]
    own_ref, sum_ref = refs[6:8]
    buffers = 5 if size == 4 else 4
    scatter = Scatter(size, *refs[8 : 8 + buffers])
    gather = Gather(size, own_ref, gathered_ref, gathered_turned_ref, *refs[8 + buffers : 14 + buffers])
    chain = Chain(
        chips, steps, chain_refs[: len(steps)], chain_refs[len(steps) : -2], *chain_refs[-2:],
        *refs[14 + buffers :],
    )
    chain.load()
    scatter.load(operands)
    greet(neighbours(size) + chain.neighbours)
    scatter.fill(operands, slots=(0, 1))
    chain.step(0)
    scatter.fill(operands, slots=(1, size))
    scatter.relay()
    sum_ref[...] = jnp.zeros_like(sum_ref)
    scatter.collect()

    def norm(piece):
        back = scatter.total(piece)
        state = state_ref[piece, :]
        scale = row_scale(state)
        unit = state * scale
        sum_ref[...] += jnp.sum(back * unit, axis=0, keepdims=True)
        unit_slope = back * gain_ref[...]
        slope = cotangent_ref[piece, :].astype(jnp.float32) + scale * (
            unit_slope - unit * jnp.mean(unit_slope * unit, axis=-1, keepdims=True)
        )
        slope_ref[piece, :] = slope
        own_ref[piece, :] = slope.astype(own_ref.dtype)

    over_pieces(own_ref.shape[0], norm)
    gather.start()
    store_row(term_ref, sum_ref)
    gather.forward()
    chain.wait(0)
    for index in range(1, len(steps)):
        chain.step(index)
        chain.wait(index)
    last = len(steps)
    from_under, from_above = chain.arrives(last - 1)
    for arrived, landing, out_ref in (
        (from_under, chain.up, up_out_ref),
        (from_above, chain.down, down_out_ref),
    ):

        @pl.when(arrived)
        def _(landing=landing, out_ref=out_ref):
            out_ref[...] = landing[last]

        @pl.when(jnp.logical_not(arrived))
        def _(out_ref=out_ref):
            out_ref[...] = jnp.zeros_like(out_ref)

    gather.finish()
    scatter.drain()
    chain.drain()


def last_kernel(sizes, first_columns, *refs):
    data_size, size = sizes
    operands, refs = split_operands(refs, size, first_columns)
    input_ref, gain_ref, slope_ref, terms_ref, rows_ref = refs[:5]
    gradient_ref, terms_out_ref, sum_ref, partial_ref, group_ref, inner, outer = refs[5:12]
    inner_send, inner_recv, outer_send, outer_recv = refs[12:16]
    mixing = Scatter(size, *refs[16:])
    rows = gradient_ref.shape[0]
    mixing.load(operands)
    greet(
        [("tensor", peer) for peer in other_members("tensor", size)]
        + [("dp", peer) for peer in other_members("dp", data_size)]
    )
    sum_ref[...] = jnp.zeros_like(sum_ref)

    def look(owner, columns, values):
        piece = pl.ds(pl.multiple_of(owner * rows, rows), rows)
        sum_ref[:, columns] += jnp.sum(
            values * rows_ref[piece, columns].astype(jnp.float32), axis=0, keepdims=True
        )

    mixing.fill(operands, look)
    sum_ref[...] = sum_ref[...] / gain_ref[...]
    kept = partial_ref.shape[0] - terms_ref.shape[0]
    partial_ref[kept:, :] = terms_ref[...]
    store_row(partial_ref, sum_ref)
    inner_copies = send_terms(
        "tensor", other_members("tensor", size), partial_ref, inner, inner_send, inner_recv
    )
    mixing.relay()
    group_ref[...] = add_terms(inner, inner_copies)
    outer_copies = send_terms(
        "dp", other_members("dp", data_size), group_ref, outer, outer_send, outer_recv
    )
    terms_out_ref[...] = add_terms(outer, outer_copies)
    mixing.collect()

    def norm(piece):
        back = mixing.total(piece)
        values = input_ref[piece, :].astype(jnp.float32)
        scale = row_scale(values)
        unit = values * scale
        unit_slope = back * gain_ref[...]
        gradient_ref[piece, :] = (
            slope_ref[piece, :]
            + scale * (unit_slope - unit * jnp.mean(unit_slope * unit, axis=-1, keepdims=True))
        ).astype(gradient_ref.dtype)

    over_pieces(rows, norm)
    for copy in inner_copies + outer_copies:
        copy.wait_send()
    mixing.drain()


def scatter_call(body, triples, size, others, far, outs, gathered, scratch, collective_id):
    far_spec = pl.BlockSpec(memory_space=pl.ANY)
    operands = [array for left, weight, _ in triples for array in (left, weight)]
    in_specs = [far_spec] * len(operands)
    for other in others:
        in_specs.append(pl.BlockSpec(other.shape, lambda i: (0, 0), pipeline_mode=pl.Buffered(1)))
    in_specs += [far_spec] * len(far)
    out_specs = [pl.BlockSpec(out.shape, lambda i: (0, 0)) for out in outs]
    if gathered:
        out_specs[:2] = [far_spec] * 2
    return pl.pallas_call(
        functools.partial(body, tuple(first for _, _, first in triples)),
        grid=(1,),
        out_shape=outs,
        in_specs=in_specs,
        out_specs=out_specs,
        scratch_shapes=list(scratch)
        + [part for left, weight, _ in triples for part in Operand.scratch(size, left, weight)],
        compiler_params=pltpu.CompilerParams(
            collective_id=collective_id, has_side_effects=True, vmem_limit_bytes=VMEM_LIMIT
        ),
        cost_estimate=pl.CostEstimate(
            flops=sum(2 * left.size * weight.shape[0] for left, weight, _ in triples),
            bytes_accessed=150_000_000,
            transcendentals=0,
        ),
    )(*operands, *others, *far)


LOG2E = 1.4426950408889634


def turn_tables(head_size):
    half_size = head_size // 2
    frequency = np.float32(rope_base) ** (
        -(np.arange(half_size, dtype=np.float32) * np.float32(2.0) / np.float32(head_size))
    )
    frequency = frequency.astype(np.float64)
    sign = np.concatenate([-np.ones(half_size), np.ones(half_size)])[None, :]
    positions = np.concatenate([np.arange(0, SEQUENCE_LENGTH, 128), np.arange(128)])
    angles = positions[:, None] * np.concatenate([frequency, frequency])[None, :]
    return np.cos(angles).astype(np.float32), (sign * np.sin(angles)).astype(np.float32)


def fill_tables(few_cosines_ref, few_sines_ref, cosine_ref, sine_ref):
    coarse = few_cosines_ref.shape[0] - 128
    near_cosine, near_sine = few_cosines_ref[coarse:, :], few_sines_ref[coarse:, :]

    def step(index, carry):
        far_cosine = few_cosines_ref[pl.ds(index, 1), :]
        far_sine = few_sines_ref[pl.ds(index, 1), :]
        rows = pl.ds(pl.multiple_of(index * 128, 128), 128)
        cosine_ref[rows, :] = far_cosine * near_cosine - far_sine * near_sine
        sine_ref[rows, :] = far_sine * near_cosine + far_cosine * near_sine
        return carry

    lax.fori_loop(0, coarse, step, 0)


def turn(values, cosine, sine):
    return values * cosine + pltpu.roll(values, values.shape[-1] // 2, 1) * sine


def turn_back(values, cosine, sine):
    return values * cosine - pltpu.roll(values, values.shape[-1] // 2, 1) * sine


def contract_first(first_operand, second_operand):
    return lax.dot_general(
        first_operand, second_operand, (((0,), (0,)), ((), ())), preferred_element_type=jnp.float32
    )


def visible_scores(key_rows, query_rows, first_row, multiplier):
    scores = times_transposed(key_rows, query_rows) * multiplier
    _, queries = scores.shape
    key_at = lax.broadcasted_iota(jnp.int32, (queries, queries), 0)
    query_at = lax.broadcasted_iota(jnp.int32, (queries, queries), 1)
    corner = jnp.where(query_at >= key_at, scores[first_row:], -1e30)
    if first_row == 0:
        return corner
    return jnp.concatenate([scores[:first_row], corner], axis=0)


def turn_heads(
    grouping, head_size, raw_ref, query_gain_ref, key_gain_ref, cosine_ref, sine_ref, query_ref, key_ref, value_ref
):
    def turned(start, gain):
        raw = raw_ref[:, pl.ds(start, head_size)]
        return turn(raw * row_scale(raw) * gain, cosine_ref[...], sine_ref[...]).astype(jnp.bfloat16)

    def step(part, carry):
        query_ref[part] = turned(pl.multiple_of(part * head_size, head_size), query_gain_ref[...])
        return carry

    lax.fori_loop(0, grouping, step, 0)
    key_ref[...] = turned(grouping * head_size, key_gain_ref[...])
    value_ref[...] = raw_ref[:, (grouping + 1) * head_size :].astype(jnp.bfloat16)


def attention_forward_kernel(
    grouping, head_size, block, rows_ref, weight_ref, few_cosines_ref, few_sines_ref, query_gain_ref, key_gain_ref,
    raw_ref, mixed_ref, total_ref, query_ref, key_ref, value_ref, cosine_ref, sine_ref,
):
    sequence = rows_ref.shape[0]
    multiplier = head_size ** (-0.5) * LOG2E

    @pl.when((pl.program_id(0) == 0) & (pl.program_id(1) == 0))
    def _():
        fill_tables(few_cosines_ref, few_sines_ref, cosine_ref, sine_ref)

    raw_ref[...] = simple_product(rows_ref[...], weight_ref[...])
    turn_heads(
        grouping, head_size, raw_ref, query_gain_ref, key_gain_ref, cosine_ref, sine_ref, query_ref, key_ref, value_ref
    )

    def head_step(part, carry):
        lanes = pl.ds(pl.multiple_of(part * head_size, head_size), head_size)
        for first_row in range(0, sequence, block):
            last_row = first_row + block
            scores = visible_scores(
                key_ref[:last_row, :], query_ref[part, first_row:last_row, :], first_row, multiplier
            )
            highest = jnp.max(scores, axis=0, keepdims=True)
            weights = jnp.exp2(scores - highest)
            total = jnp.sum(weights, axis=0, keepdims=True)
            weights = (weights * (1.0 / total)).astype(jnp.bfloat16)
            mixed_ref[first_row:last_row, lanes] = contract_first(
                weights, value_ref[:last_row, :]
            ).astype(mixed_ref.dtype)
            total_ref[0, pl.ds(part, 1), first_row:last_row] = highest + jnp.log2(total)
        return carry

    lax.fori_loop(0, grouping, head_step, 0)


def attention_forward(rows, weight, tables, query_gain, key_gain, heads, grouping):
    total_rows, depth = rows.shape
    head_size = query_gain.shape[0]
    sequences = total_rows // SEQUENCE_LENGTH
    width = (grouping + 2) * head_size
    block = min(256, SEQUENCE_LENGTH)
    table = pl.BlockSpec(tables[0].shape, lambda s, h: (0, 0))
    gain = pl.BlockSpec((1, head_size), lambda s, h: (0, 0))
    elements = heads * grouping * total_rows * SEQUENCE_LENGTH // 2
    return pl.pallas_call(
        functools.partial(attention_forward_kernel, grouping, head_size, block),
        grid=(sequences, heads),
        out_shape=[
            jax.ShapeDtypeStruct((total_rows, heads * width), jnp.float32),
            jax.ShapeDtypeStruct((total_rows, heads * grouping * head_size), jnp.bfloat16),
            jax.ShapeDtypeStruct((heads, grouping, total_rows), jnp.float32),
        ],
        in_specs=[
            pl.BlockSpec((SEQUENCE_LENGTH, depth), lambda s, h: (s, 0)),
            pl.BlockSpec((depth, width), lambda s, h: (0, h)),
            table,
            table,
            gain,
            gain,
        ],
        out_specs=[
            pl.BlockSpec((SEQUENCE_LENGTH, width), lambda s, h: (s, h)),
            pl.BlockSpec((SEQUENCE_LENGTH, grouping * head_size), lambda s, h: (s, h)),
            pl.BlockSpec((1, grouping, SEQUENCE_LENGTH), lambda s, h: (h, 0, s)),
        ],
        scratch_shapes=[
            pltpu.VMEM((grouping, SEQUENCE_LENGTH, head_size), jnp.bfloat16),
            pltpu.VMEM((SEQUENCE_LENGTH, head_size), jnp.bfloat16),
            pltpu.VMEM((SEQUENCE_LENGTH, head_size), jnp.bfloat16),
            pltpu.VMEM((SEQUENCE_LENGTH, head_size), jnp.float32),
            pltpu.VMEM((SEQUENCE_LENGTH, head_size), jnp.float32),
        ],
        compiler_params=pltpu.CompilerParams(vmem_limit_bytes=VMEM_LIMIT),
        cost_estimate=pl.CostEstimate(
            flops=2 * total_rows * depth * heads * width + 4 * elements * head_size,
            bytes_accessed=2 * (total_rows * depth + depth * heads * width),
            transcendentals=elements,
        ),
        name="attention_forward",
    )(rows, weight, *tables, query_gain.reshape(1, -1), key_gain.reshape(1, -1))


def norm_back(turned_slope, raw, gain, cosine, sine):
    norm_slope = turn_back(turned_slope, cosine, sine)
    scale = row_scale(raw)
    unit = raw * scale
    term = norm_slope * unit
    unit_slope = norm_slope * gain
    slope = scale * (unit_slope - unit * jnp.mean(unit_slope * unit, axis=-1, keepdims=True))
    return slope.astype(jnp.bfloat16), jnp.sum(term, axis=0, keepdims=True)


def attention_backward_kernel(size, chips, grouping, head_size, block, first_columns, *refs):
    operands, refs = split_operands(refs, size, first_columns)
    (
        state_ref, weight_ref, raw_ref, mixed_ref, total_ref, few_cosines_ref, few_sines_ref,
        query_gain_ref, key_gain_ref, hidden_state_ref,
    ) = refs[:10]
    chain_refs, own_block_ref = refs[10:14], refs[14]
    slope_ref, gain_ref, output_ref, chain_total_ref = refs[15:19]
    (
        query_ref, key_ref, value_ref, out_slope_ref, turned_ref, key_sum_ref, value_sum_ref, cosine_ref, sine_ref,
    ) = refs[19:28]
    buffers = 5 if size == 4 else 4
    scatter = Scatter(size, *refs[28 : 28 + buffers])
    own_sem = refs[28 + buffers]
    chain = Chain(
        chips, (chips - 1,), chain_refs[:1], chain_refs[1:2], *chain_refs[2:], *refs[29 + buffers :]
    )
    own_load = pltpu.make_async_copy(own_block_ref, chain_total_ref, own_sem.at[0])
    step = pl.program_id(0) * pl.num_programs(1) + pl.program_id(1)
    steps = pl.num_programs(0) * pl.num_programs(1)

    @pl.when(step == 0)
    def _():
        chain.load()
        scatter.load(operands)
        own_load.start()
        greet(neighbours(size) + chain.neighbours)
        scatter.fill(operands, slots=(0, 1))
        chain.step(0)
        scatter.fill(operands, slots=(1, size))

    attend_backward_head(
        grouping, head_size, block, state_ref, weight_ref, raw_ref, mixed_ref, total_ref, few_cosines_ref,
        few_sines_ref, query_gain_ref, key_gain_ref, slope_ref, gain_ref, query_ref, key_ref, value_ref,
        out_slope_ref, turned_ref, key_sum_ref, value_sum_ref, cosine_ref, sine_ref,
    )

    @pl.when(step == 0)
    def _():
        scatter.relay()

    @pl.when(step == steps - 1)
    def _():
        scatter.collect()

        def finish(piece):
            output_ref[piece, :] = (hidden_state_ref[piece, :] + scatter.total(piece)).astype(
                output_ref.dtype
            )

        over_pieces(output_ref.shape[0], finish)
        own_load.wait()
        chain.wait(0)
        for arrived, landing in zip(chain.arrives(0), (chain.up, chain.down)):

            @pl.when(arrived)
            def _(landing=landing):
                def add(piece):
                    chain_total_ref[piece, :] = add_rounded(
                        chain_total_ref[piece, :], landing[1, piece, :]
                    )

                over_pieces(chain_total_ref.shape[0], add)

        scatter.drain()
        chain.drain()


def attend_backward_head(
    grouping, head_size, block, state_ref, weight_ref, raw_ref, mixed_ref, total_ref, few_cosines_ref, few_sines_ref,
    query_gain_ref, key_gain_ref, slope_ref, gain_ref, query_ref, key_ref, value_ref, out_slope_ref,
    turned_ref, key_sum_ref, value_sum_ref, cosine_ref, sine_ref,
):
    sequence = state_ref.shape[0]
    scale_factor = head_size ** (-0.5)
    multiplier = scale_factor * LOG2E

    @pl.when((pl.program_id(0) == 0) & (pl.program_id(1) == 0))
    def _():
        gain_ref[...] = jnp.zeros_like(gain_ref)
        fill_tables(few_cosines_ref, few_sines_ref, cosine_ref, sine_ref)

    out_slope_ref[...] = simple_product(state_ref[...], weight_ref[...]).astype(jnp.bfloat16)
    turn_heads(
        grouping, head_size, raw_ref, query_gain_ref, key_gain_ref, cosine_ref, sine_ref, query_ref, key_ref, value_ref
    )
    key_sum_ref[...] = jnp.zeros_like(key_sum_ref)
    value_sum_ref[...] = jnp.zeros_like(value_sum_ref)
    ones = jnp.ones((8, head_size), jnp.float32)

    def head_step(part, carry):
        lanes = pl.ds(pl.multiple_of(part * head_size, head_size), head_size)
        for first_row in range(0, sequence, block):
            last_row = first_row + block
            query_rows = query_ref[part, first_row:last_row, :]
            slope_rows = out_slope_ref[first_row:last_row, lanes]
            scores = visible_scores(key_ref[:last_row, :], query_rows, first_row, multiplier)
            weights = jnp.exp2(scores - total_ref[0, pl.ds(part, 1), first_row:last_row])
            value_sum_ref[:last_row, :] += simple_product(weights.astype(jnp.bfloat16), slope_rows)
            product = slope_rows.astype(jnp.float32) * mixed_ref[first_row:last_row, lanes].astype(jnp.float32)
            centre = lax.dot_general(
                ones,
                product,
                (((1,), (1,)), ((), ())),
                preferred_element_type=jnp.float32,
                precision=lax.Precision.HIGHEST,
            )[:1]
            weight_slope = times_transposed(value_ref[:last_row, :], slope_rows)
            score_slope = (weights * (weight_slope - centre)).astype(jnp.bfloat16)
            key_sum_ref[:last_row, :] += simple_product(score_slope, query_rows)
            turned_ref[first_row:last_row, :] = (
                contract_first(score_slope, key_ref[:last_row, :]) * scale_factor
            )
        slope, term = norm_back(
            turned_ref[...], raw_ref[:, lanes], query_gain_ref[...], cosine_ref[...], sine_ref[...]
        )
        slope_ref[:, lanes] = slope
        gain_ref[0:1, :] += term
        return carry

    lax.fori_loop(0, grouping, head_step, 0)
    lanes = slice(grouping * head_size, (grouping + 1) * head_size)
    slope, term = norm_back(
        key_sum_ref[...] * scale_factor, raw_ref[:, lanes], key_gain_ref[...], cosine_ref[...], sine_ref[...]
    )
    slope_ref[:, lanes] = slope
    gain_ref[1:2, :] += term
    slope_ref[:, (grouping + 1) * head_size :] = value_sum_ref[...].astype(jnp.bfloat16)


def attention_backward(
    state_rows, weight, weight_start, raw, mixed, totals, tables, query_gain, key_gain, heads, grouping,
    triples, hidden_state, chain_arrays, own_block, sizes, collective_id,
):
    total_rows, depth = state_rows.shape
    head_size = query_gain.shape[0]
    sequences = total_rows // SEQUENCE_LENGTH
    width = (grouping + 2) * head_size
    out_width = grouping * head_size
    block = min(256, SEQUENCE_LENGTH)
    data_size, size = sizes
    chips = data_size // 2
    first_block = weight_start // out_width
    single = pl.Buffered(1)
    table = pl.BlockSpec(tables[0].shape, lambda s, h: (0, 0))
    gain = pl.BlockSpec((1, head_size), lambda s, h: (0, 0))
    elements = heads * grouping * total_rows * SEQUENCE_LENGTH // 2
    whole_rows = pltpu.VMEM((SEQUENCE_LENGTH, head_size), jnp.float32)
    operands = [array for left, other_weight, _ in triples for array in (left, other_weight)]
    in_specs = [pl.BlockSpec(memory_space=pl.ANY)] * len(operands)
    in_specs += [
        pl.BlockSpec((SEQUENCE_LENGTH, depth), lambda s, h: (s, 0), pipeline_mode=single),
        pl.BlockSpec((depth, out_width), lambda s, h: (0, first_block + h)),
        pl.BlockSpec((SEQUENCE_LENGTH, width), lambda s, h: (s, h)),
        pl.BlockSpec((SEQUENCE_LENGTH, out_width), lambda s, h: (s, h)),
        pl.BlockSpec((1, grouping, SEQUENCE_LENGTH), lambda s, h: (h, 0, s)),
        table,
        table,
        gain,
        gain,
        pl.BlockSpec(hidden_state.shape, lambda s, h: (0, 0), pipeline_mode=single),
    ] + [pl.BlockSpec(memory_space=pl.ANY)] * 5
    operands += [
        state_rows, weight, raw, mixed, totals, *tables, query_gain.reshape(1, -1), key_gain.reshape(1, -1),
        hidden_state, *chain_arrays, own_block,
    ]
    return pl.pallas_call(
        functools.partial(
            attention_backward_kernel, size, chips, grouping, head_size, block,
            tuple(first for _, _, first in triples),
        ),
        grid=(sequences, heads),
        out_shape=[
            jax.ShapeDtypeStruct((total_rows, heads * width), jnp.bfloat16),
            jax.ShapeDtypeStruct((8, head_size), jnp.float32),
            jax.ShapeDtypeStruct(hidden_state.shape, jnp.bfloat16),
            jax.ShapeDtypeStruct(own_block.shape, jnp.bfloat16),
        ],
        in_specs=in_specs,
        out_specs=[
            pl.BlockSpec((SEQUENCE_LENGTH, width), lambda s, h: (s, h)),
            pl.BlockSpec((8, head_size), lambda s, h: (0, 0)),
            pl.BlockSpec(hidden_state.shape, lambda s, h: (0, 0)),
            pl.BlockSpec(own_block.shape, lambda s, h: (0, 0)),
        ],
        scratch_shapes=[
            pltpu.VMEM((grouping, SEQUENCE_LENGTH, head_size), jnp.bfloat16),
            pltpu.VMEM((SEQUENCE_LENGTH, head_size), jnp.bfloat16),
            pltpu.VMEM((SEQUENCE_LENGTH, head_size), jnp.bfloat16),
            pltpu.VMEM((SEQUENCE_LENGTH, out_width), jnp.bfloat16),
            whole_rows,
            whole_rows,
            whole_rows,
            whole_rows,
            whole_rows,
            *Scatter.scratch(size, *hidden_state.shape),
            pltpu.SemaphoreType.DMA((1,)),
            *Chain.scratch(1, *own_block.shape),
            *[part for left, other, _ in triples for part in Operand.scratch(size, left, other)],
        ],
        compiler_params=pltpu.CompilerParams(
            collective_id=collective_id, has_side_effects=True, vmem_limit_bytes=VMEM_LIMIT
        ),
        cost_estimate=pl.CostEstimate(
            flops=2 * total_rows * depth * heads * out_width + 10 * elements * head_size,
            bytes_accessed=100_000_000,
            transcendentals=elements,
        ),
        name="attention_backward",
    )(*operands)


def feed_half_kernel(
    half, tile, block, rows_far, cotangent_far, weight_far, hidden_far, slope_far,
    rows_ref, cotangent_ref, weight_ref, hidden_ref, slope_ref, row_sem, weight_sem, out_sem,
):
    total = rows_ref.shape[0]
    blocks = total // block
    tiles = half // tile

    def row_copies(index):
        piece = pl.ds(pl.multiple_of(index * block, block), block)
        return [
            pltpu.make_async_copy(far.at[piece], ref.at[piece], row_sem.at[at, index])
            for at, (far, ref) in enumerate(((rows_far, rows_ref), (cotangent_far, cotangent_ref)))
        ]

    def weight_copies(index):
        copies = []
        for part in range(3):
            columns = pl.ds(pl.multiple_of(part * half + index * tile, tile), tile)
            copies.append(
                pltpu.make_async_copy(
                    weight_far.at[:, columns], weight_ref.at[part, index], weight_sem.at[part, index]
                )
            )
        return copies

    def out_copies(index):
        piece = pl.ds(pl.multiple_of(index * block, block), block)
        return [
            pltpu.make_async_copy(ref.at[piece], far.at[piece], out_sem.at[at, index])
            for at, (far, ref) in enumerate(((hidden_far, hidden_ref), (slope_far, slope_ref)))
        ]

    for copy in row_copies(0) + weight_copies(0):
        copy.start()
    for index in range(1, tiles):
        for copy in weight_copies(index):
            copy.start()
    for index in range(1, blocks):
        for copy in row_copies(index):
            copy.start()

    def row_step(row_index, carry):
        piece = pl.ds(pl.multiple_of(row_index * block, block), block)
        for copy in row_copies(row_index):
            copy.wait()

        def step(index, carry):
            @pl.when(row_index == 0)
            def _():
                for copy in weight_copies(index):
                    copy.wait()

            start = pl.multiple_of(index * tile, tile)
            rows = rows_ref[piece, :]
            gate = simple_product(rows, weight_ref[0, index])
            up = simple_product(rows, weight_ref[1, index])
            back = simple_product(cotangent_ref[piece, :], weight_ref[2, index])
            sigmoid = 1.0 / (1.0 + jnp.exp(-gate))
            gated = gate * sigmoid
            hidden_ref[piece, pl.ds(start, tile)] = (gated * up).astype(jnp.bfloat16)
            slope_ref[piece, pl.ds(start, tile)] = (
                back * up * sigmoid * (1.0 + gate * (1.0 - sigmoid))
            ).astype(jnp.bfloat16)
            slope_ref[piece, pl.ds(half + start, tile)] = (back * gated).astype(jnp.bfloat16)
            return carry

        lax.fori_loop(0, tiles, step, 0)
        for copy in out_copies(row_index):
            copy.start()
        return carry

    lax.fori_loop(0, blocks, row_step, 0)
    for index in range(blocks):
        for copy in out_copies(index):
            copy.wait()


def feed_half(rows, cotangent, weight):
    total_rows, depth = rows.shape
    block = min(512, total_rows)
    half = weight.shape[1] // 3
    tile = 256 if half % 256 == 0 else 128
    blocks, tiles = total_rows // block, half // tile
    far = pl.BlockSpec(memory_space=pl.ANY)
    return pl.pallas_call(
        functools.partial(feed_half_kernel, half, tile, block),
        out_shape=[
            jax.ShapeDtypeStruct((total_rows, half), jnp.bfloat16),
            jax.ShapeDtypeStruct((total_rows, 2 * half), jnp.bfloat16),
        ],
        in_specs=[far] * 3,
        out_specs=[far] * 2,
        scratch_shapes=[
            pltpu.VMEM(rows.shape, rows.dtype),
            pltpu.VMEM(rows.shape, rows.dtype),
            pltpu.VMEM((3, tiles, depth, tile), weight.dtype),
            pltpu.VMEM((total_rows, half), jnp.bfloat16),
            pltpu.VMEM((total_rows, 2 * half), jnp.bfloat16),
            pltpu.SemaphoreType.DMA((2, blocks)),
            pltpu.SemaphoreType.DMA((3, tiles)),
            pltpu.SemaphoreType.DMA((2, blocks)),
        ],
        compiler_params=pltpu.CompilerParams(vmem_limit_bytes=VMEM_LIMIT),
        cost_estimate=pl.CostEstimate(
            flops=6 * total_rows * depth * half,
            bytes_accessed=2 * (2 * total_rows * depth + 3 * depth * half),
            transcendentals=total_rows * half,
        ),
        name="feed_half",
    )(rows, cotangent, weight)


def grad_kernel(pair_count, with_other, order_ref, *refs):
    pairs = [refs[2 * p : 2 * p + 2] for p in range(pair_count)]
    refs = refs[2 * pair_count :]
    step = pl.program_id(0)
    if with_other:
        other_ref, refs = refs[0], refs[1:]
        out_refs, held_ref, copy_sem = refs[:-2], refs[-2], refs[-1]
    else:
        out_ref = refs[0]
    start = 0
    for left_ref, right_ref in pairs:
        width = right_ref.shape[1]
        tile = next(t for t in (768, 512, 384, 256, 128) if width % t == 0)
        for column in range(0, width, tile):
            values = simple_product(left_ref[...], right_ref[:, column : column + tile])
            columns = slice(start + column, start + column + tile)
            if with_other:
                values = values + other_ref[0, :, columns].astype(jnp.float32)
                held_ref[step, :, columns] = values.astype(jnp.bfloat16)
            else:
                out_ref[:, :, columns] = values.reshape(*out_ref.shape[:2], tile).astype(jnp.bfloat16)
        start += width
    if with_other:
        copies = [
            pltpu.make_async_copy(held_ref.at[index], out_ref, copy_sem.at[index])
            for index, out_ref in enumerate(out_refs)
        ]
        for index, copy in enumerate(copies):
            pl.when(step == index)(copy.start)

        @pl.when(step == len(copies) - 1)
        def _():
            for copy in copies:
                copy.wait()


def grad_blocks(order, pairs, other=None, group=1):
    count = order.shape[0]
    depth, total_rows = pairs[0][0].shape
    block = depth // lax.axis_size("dp")
    width = sum(right.shape[1] for _, right in pairs)
    in_specs = []
    operands = []
    for left, right in pairs:
        in_specs += [
            pl.BlockSpec(
                (group * block, total_rows),
                (lambda k, at: (at[k], 0)) if group == 1 else (lambda k, at: (k, 0)),
            ),
            pl.BlockSpec(right.shape, lambda k, at: (0, 0), pipeline_mode=pl.Buffered(1)),
        ]
        operands += [left, right]
    scratch = []
    if other is not None:
        in_specs.append(pl.BlockSpec((1, block, width), lambda k, at: (k, 0, 0)))
        operands.append(other)
        out_shape = [jax.ShapeDtypeStruct((block, width), jnp.bfloat16)] * count
        out_specs = [pl.BlockSpec(memory_space=pl.ANY)] * count
        scratch = [
            pltpu.VMEM((count, block, width), jnp.bfloat16),
            pltpu.SemaphoreType.DMA((count,)),
        ]
    else:
        out_shape = [jax.ShapeDtypeStruct((count, block, width), jnp.bfloat16)]
        out_specs = [pl.BlockSpec((group, block, width), lambda k, at: (k, 0, 0))]
    out = pl.pallas_call(
        functools.partial(grad_kernel, len(pairs), other is not None),
        grid_spec=pltpu.PrefetchScalarGridSpec(
            num_scalar_prefetch=1,
            grid=(count // group,),
            in_specs=in_specs,
            out_specs=out_specs,
            scratch_shapes=scratch,
        ),
        out_shape=out_shape,
        compiler_params=pltpu.CompilerParams(vmem_limit_bytes=VMEM_LIMIT),
        cost_estimate=pl.CostEstimate(
            flops=2 * total_rows * count * block * width,
            bytes_accessed=2 * (total_rows * count * block * len(pairs) + width * (total_rows + count * block)),
            transcendentals=0,
        ),
        name="grad_blocks",
    )(order, *operands)
    return out if other is not None else out[0]


def reduce_over_chips(pairs, sizes):
    data_size = sizes[0]
    chips = data_size // 2
    me = lax.axis_index("dp")
    chip, core = me // 2, lax.rem(me, 2)
    ahead = lax.rem(chip + jnp.arange(chips, dtype=jnp.int32), chips) * 2
    other = lax.ppermute(
        grad_blocks(ahead + (1 - core), pairs),
        "dp",
        [(device, device ^ 1) for device in range(data_size)],
    )
    blocks = grad_blocks(ahead + core, pairs, other)
    up = lax.ppermute(blocks[chips - 1], "dp", [(device, device + 2) for device in range(2)])
    down = lax.ppermute(
        blocks[1],
        "dp",
        [(device, device - 2) for device in range(data_size - 2, data_size)],
    )
    return blocks, up, down


def pack_mixing_kernel(heads, query_ref, key_ref, value_ref, output_ref, out_ref):
    query_width = query_ref.shape[1] // heads
    head_size = key_ref.shape[1] // heads
    start = 0
    for head in range(heads):
        for ref, part in ((query_ref, query_width), (key_ref, head_size), (value_ref, head_size)):
            out_ref[:, start : start + part] = ref[:, head * part : (head + 1) * part]
            start += part
    out_ref[:, start:] = output_ref[...].T


def pack_feed_kernel(gate_ref, up_ref, down_ref, first_ref, second_ref):
    start = 0
    for out_ref in (first_ref, second_ref):
        width = out_ref.shape[1] // 3
        part = slice(start, start + width)
        out_ref[:, :width] = gate_ref[:, part]
        out_ref[:, width : 2 * width] = up_ref[:, part]
        out_ref[:, 2 * width :] = down_ref[part, :].T
        start += width


def finish_kernel(
    heads, first_ref, second_ref, mixing_ref, output_total_ref, terms_ref, output_rows_ref, input_rows_ref,
    output_rows_out, input_rows_out, attention_term_out, query_out, key_out, value_out, query_gain_out, key_gain_out,
    output_out, feed_term_out, gate_out, up_out, down_out,
):
    output_rows_out[...] = output_rows_ref[...]
    input_rows_out[...] = input_rows_ref[...]
    count = attention_term_out.shape[0]
    attention_term_out[...] = terms_ref[:count, :]
    feed_term_out[...] = terms_ref[count : 2 * count, :]
    query_gain_out[...] = terms_ref[2 * count : 2 * count + 1, :]
    key_gain_out[...] = terms_ref[2 * count + 1 : 2 * count + 2, :]
    start = 0
    for total_ref in (first_ref, second_ref):
        width = total_ref.shape[1] // 3
        part = slice(start, start + width)
        gate_out[:, part] = total_ref[:, :width].astype(jnp.float32)
        up_out[:, part] = total_ref[:, width : 2 * width].astype(jnp.float32)
        down_out[part, :] = total_ref[:, 2 * width :].astype(jnp.float32).T
        start += width
    query_width = query_out.shape[1] // heads
    head_size = key_out.shape[1] // heads
    start = 0
    for head in range(heads):
        for out, part in ((query_out, query_width), (key_out, head_size), (value_out, head_size)):
            out[:, head * part : (head + 1) * part] = mixing_ref[:, start : start + part].astype(
                jnp.float32
            )
            start += part
    output_out[...] = output_total_ref[...].astype(jnp.float32).T


def whole_call(body, shapes, *operands):
    return pl.pallas_call(
        body,
        out_shape=shapes,
        in_specs=[pl.BlockSpec(memory_space=pltpu.VMEM)] * len(operands),
        out_specs=[pl.BlockSpec(memory_space=pltpu.VMEM)] * len(shapes),
        compiler_params=pltpu.CompilerParams(vmem_limit_bytes=VMEM_LIMIT),
        cost_estimate=pl.CostEstimate(
            flops=0, bytes_accessed=4 * sum(operand.size for operand in operands), transcendentals=0
        ),
    )(*operands)


def per_device(
    block_input,
    attention_gain,
    query_weight,
    key_matrix,
    value_matrix,
    query_gain,
    key_gain,
    output_weight,
    feed_gain,
    gate_weight,
    up_weight,
    down_weight,
    out_cotangent,
):
    size = lax.axis_size("tensor")
    sizes = (lax.axis_size("dp"), size)
    model_width = block_input.shape[1]
    head_size = query_gain.shape[0]
    query_columns = query_weight.shape[1]
    key_columns = key_matrix.shape[1]
    heads = key_columns // head_size
    grouping = query_columns // key_columns
    hidden_columns = gate_weight.shape[1]
    qkv_columns = query_columns + 2 * key_columns
    first_columns = hidden_columns // 2
    second_columns = hidden_columns - first_columns
    tables = turn_tables(head_size)

    block_width = query_weight.shape[0]
    (mixing_local,) = whole_call(
        functools.partial(pack_mixing_kernel, heads),
        [jax.ShapeDtypeStruct((block_width, qkv_columns + query_columns), jnp.bfloat16)],
        query_weight, key_matrix, value_matrix, output_weight,
    )
    mixing_full = lax.all_gather(mixing_local, "dp", axis=0, tiled=True)
    feed_locals = whole_call(
        pack_feed_kernel,
        [
            jax.ShapeDtypeStruct((block_width, 3 * columns), jnp.bfloat16)
            for columns in (first_columns, second_columns)
        ],
        gate_weight, up_weight, down_weight,
    )
    feed_full = [lax.all_gather(part, "dp", axis=0, tiled=True) for part in feed_locals]

    input_float = block_input.astype(jnp.float32)
    first_scale = row_scale(input_float)
    first_unit = input_float * first_scale
    mixer_local = (first_unit * attention_gain).astype(jnp.bfloat16)
    mixer_rows, mixer_turned, cotangent_rows, cotangent_turned = gather_rows(
        (mixer_local, out_cotangent), size, 0
    )

    raw, mixed_rows, totals = attention_forward(
        mixer_rows, mixing_full, tables, query_gain, key_gain, heads, grouping
    )
    local_shape = block_input.shape
    local_rows = local_shape[0]
    gain_rows = model_width // head_size
    gathered_shapes = [
        jax.ShapeDtypeStruct((size * local_rows, model_width), jnp.bfloat16),
        jax.ShapeDtypeStruct((model_width, size * local_rows), jnp.bfloat16),
    ]
    local_float = jax.ShapeDtypeStruct(local_shape, jnp.float32)
    local_half = jax.ShapeDtypeStruct(local_shape, jnp.bfloat16)
    row_sum = pltpu.VMEM((1, model_width), jnp.float32)
    own_rows = pltpu.VMEM(local_shape, jnp.bfloat16)
    scatter_scratch = Scatter.scratch(size, *local_shape)
    gather_scratch = Gather.scratch(size, *local_shape)
    feed_rows, feed_turned, hidden_state = scatter_call(
        functools.partial(between_forward_kernel, size),
        [(mixed_rows, mixing_full, qkv_columns)],
        size,
        [block_input, feed_gain.reshape(1, -1)],
        [],
        [*gathered_shapes, local_float],
        True,
        [own_rows, *scatter_scratch, *gather_scratch],
        1,
    )

    hidden_first, slope_first = feed_half(feed_rows, cotangent_rows, feed_full[0])
    blocks, up, down = reduce_over_chips(
        [(feed_turned, slope_first), (cotangent_turned, hidden_first)], sizes
    )
    blocks, later_full = lax.optimization_barrier((blocks, feed_full[1]))
    hidden_second, slope_second = feed_half(feed_rows, cotangent_rows, later_full)
    plain_order = jnp.arange(sizes[0], dtype=jnp.int32)
    second_grad = grad_blocks(
        plain_order, [(feed_turned, slope_second), (cotangent_turned, hidden_second)], group=2
    ).reshape(model_width, -1)
    second_grad, slope_second = lax.optimization_barrier((second_grad, slope_second))
    second_total = lax.psum_scatter(second_grad, "dp", scatter_dimension=0, tiled=True)
    chips = sizes[0] // 2
    middle_steps = tuple(range(2, chips - 1))
    chain_block = jax.ShapeDtypeStruct(blocks[0].shape, jnp.bfloat16)
    state_rows, state_turned, state_slope, feed_term, up, down = scatter_call(
        functools.partial(between_backward_kernel, size, chips, middle_steps),
        [(slope_first, feed_full[0], 0), (slope_second, later_full, 0)],
        size,
        [hidden_state, out_cotangent, feed_gain.reshape(1, -1)],
        [blocks[chips - step] for step in middle_steps]
        + [blocks[step] for step in middle_steps]
        + [up, down],
        [
            *gathered_shapes,
            local_float,
            jax.ShapeDtypeStruct((gain_rows, head_size), jnp.float32),
            chain_block,
            chain_block,
        ],
        True,
        [
            own_rows,
            row_sum,
            *scatter_scratch,
            *gather_scratch,
            *Chain.scratch(len(middle_steps), *blocks[0].shape),
        ],
        2,
    )
    output_grad = grad_blocks(plain_order, [(state_turned, mixed_rows)], group=4).reshape(model_width, -1)
    output_grad, state_rows = lax.optimization_barrier((output_grad, state_rows))
    output_total = lax.psum_scatter(output_grad, "dp", scatter_dimension=0, tiled=True)
    qkv_slope, head_terms, block_output, first_total = attention_backward(
        state_rows, mixing_full, qkv_columns, raw, mixed_rows, totals, tables,
        query_gain, key_gain, heads, grouping,
        [
            (hidden_first, feed_full[0], 2 * first_columns),
            (hidden_second, later_full, 2 * second_columns),
        ],
        hidden_state, [blocks[1], blocks[chips - 1], up, down], blocks[0], sizes, 4,
    )
    mixing_grad = grad_blocks(plain_order, [(mixer_turned, qkv_slope)], group=2).reshape(model_width, -1)
    mixing_grad, qkv_slope = lax.optimization_barrier((mixing_grad, qkv_slope))
    mixing_total = lax.psum_scatter(mixing_grad, "dp", scatter_dimension=0, tiled=True)
    terms_shape = (2 * gain_rows + head_terms.shape[0], head_size)
    input_gradient, terms = scatter_call(
        functools.partial(last_kernel, sizes),
        [(qkv_slope, mixing_full, 0)],
        size,
        [
            block_input,
            attention_gain.reshape(1, -1),
            state_slope,
            jnp.concatenate([feed_term, head_terms], axis=0),
            mixer_rows,
        ],
        [],
        [local_half, jax.ShapeDtypeStruct(terms_shape, jnp.float32)],
        False,
        [
            row_sum,
            pltpu.VMEM(terms_shape, jnp.float32),
            pltpu.VMEM(terms_shape, jnp.float32),
            pltpu.VMEM((size, *terms_shape), jnp.float32),
            pltpu.VMEM((sizes[0], *terms_shape), jnp.float32),
            *[pltpu.SemaphoreType.DMA((count - 1,)) for count in (size, size, *sizes[:1] * 2)],
            *scatter_scratch,
        ],
        3,
    )

    def whole_float(*shape):
        return jax.ShapeDtypeStruct(shape, jnp.float32)

    outs = whole_call(
        functools.partial(finish_kernel, heads),
        [
            local_half,
            local_half,
            whole_float(gain_rows, head_size),
            whole_float(block_width, query_columns),
            whole_float(block_width, key_columns),
            whole_float(block_width, key_columns),
            whole_float(1, head_size),
            whole_float(1, head_size),
            whole_float(query_columns, block_width),
            whole_float(gain_rows, head_size),
            whole_float(block_width, hidden_columns),
            whole_float(block_width, hidden_columns),
            whole_float(hidden_columns, block_width),
        ],
        first_total, second_total, mixing_total, output_total, terms, block_output, input_gradient,
    )
    return tuple(
        out.reshape(-1) if index in (2, 6, 7, 9) else out for index, out in enumerate(outs)
    )


def solution(mesh):
    in_specs = (
        P(("dp", "tensor"), None),
        P(),
        P("dp", "tensor"),
        P("dp", "tensor"),
        P("dp", "tensor"),
        P(),
        P(),
        P("tensor", "dp"),
        P(),
        P("dp", "tensor"),
        P("dp", "tensor"),
        P("tensor", "dp"),
        P(("dp", "tensor"), None),
    )
    out_specs = (
        P(("dp", "tensor"), None),
        P(("dp", "tensor"), None),
        P(),
        P("dp", "tensor"),
        P("dp", "tensor"),
        P("dp", "tensor"),
        P(),
        P(),
        P("tensor", "dp"),
        P(),
        P("dp", "tensor"),
        P("dp", "tensor"),
        P("tensor", "dp"),
    )

    return jax.shard_map(per_device, mesh=mesh, in_specs=in_specs, out_specs=out_specs, check_vma=False)
```

```python
import functools

import jax
import jax.numpy as jnp
import numpy as np
from jax import lax
from jax.experimental import pallas as pl
from jax.experimental.pallas import tpu as pltpu
from jax.sharding import PartitionSpec as P


SEQUENCE_LENGTH = 1024

epsilon = 1e-06
rope_base = 1000000.0


MESH = pl.DeviceIdType.MESH
VMEM_LIMIT = 62 * 1024 * 1024


def row_scale(values):
    return lax.rsqrt(jnp.mean(values * values, axis=-1, keepdims=True) + epsilon)


def times_transposed(first_operand, second_operand):
    return lax.dot_general(
        first_operand, second_operand, (((1,), (1,)), ((), ())), preferred_element_type=jnp.float32
    )


def simple_product(first_operand, second_operand):
    return jnp.dot(first_operand, second_operand, preferred_element_type=jnp.float32)


def remote(source, target, send_sem, recv_sem, peer, axis="tensor"):
    return pltpu.make_async_remote_copy(
        src_ref=source,
        dst_ref=target,
        send_sem=send_sem,
        recv_sem=recv_sem,
        device_id={axis: peer},
        device_id_type=MESH,
    )


def greet(peers):
    barrier = pltpu.get_barrier_semaphore()
    for axis, peer in peers:
        pl.semaphore_signal(barrier, inc=1, device_id={axis: peer}, device_id_type=MESH)
    pl.semaphore_wait(barrier, len(peers))


def square_peers(me):
    column = lax.rem(me, 2)
    row = me // 2
    return row * 2 + (1 - column), (1 - row) * 2 + column, (1 - row) * 2 + (1 - column)


def neighbours(size):
    if size == 4:
        beside, below, _ = square_peers(lax.axis_index("tensor"))
        return [("tensor", beside), ("tensor", below)]
    return [("tensor", peer) for peer in other_members("tensor", size)]


def other_members(axis, count):
    me = lax.axis_index(axis)
    return [lax.rem(me + step, count) for step in range(1, count)]


class Gather:
    def __init__(
        self, size, own_ref, out_ref, turned_out_ref, held_ref, turned_ref, send_sem, recv_sem, local_sem, turned_sem
    ):
        self.size, self.own, self.out, self.held = size, own_ref, out_ref, held_ref
        self.turned_out, self.turned = turned_out_ref, turned_ref
        self.send_sem, self.recv_sem, self.local_sem = send_sem, recv_sem, local_sem
        self.turned_sem = turned_sem
        self.me = lax.axis_index("tensor")
        self.rows = own_ref.shape[0]
        self.copies, self.stores, self.turns = [], [], []

    @staticmethod
    def scratch(size, rows, columns):
        sends, local = (12, 8) if size == 4 else (size - 1, size)
        return [
            pltpu.VMEM((size, rows, columns), jnp.bfloat16),
            pltpu.VMEM((columns, size * rows), jnp.bfloat16),
            pltpu.SemaphoreType.DMA((sends,)),
            pltpu.SemaphoreType.DMA((sends,)),
            pltpu.SemaphoreType.DMA((local,)),
            pltpu.SemaphoreType.DMA((local,)),
        ]

    def send(self, source, target, peer):
        index = len(self.copies)
        copy = remote(source, target, self.send_sem.at[index], self.recv_sem.at[index], peer)
        copy.start()
        self.copies.append(copy)
        return copy

    def store(self, source, start, count):
        piece = pl.ds(pl.multiple_of(start, count), count)
        copy = pltpu.make_async_copy(source, self.out.at[piece], self.local_sem.at[len(self.stores)])
        copy.start()
        self.stores.append(copy)
        width = min(256, self.turned.shape[0])

        def turn_part(index, carry):
            columns = pl.ds(pl.multiple_of(index * width, width), width)
            self.turned[columns, piece] = source[:, columns].T
            return carry

        lax.fori_loop(0, self.turned.shape[0] // width, turn_part, 0)
        turn_copy = pltpu.make_async_copy(
            self.turned.at[:, piece], self.turned_out.at[:, piece], self.turned_sem.at[len(self.turns)]
        )
        turn_copy.start()
        self.turns.append(turn_copy)

    def quarters(self):
        quarter = self.rows // 4
        return [pl.ds(index * quarter, quarter) for index in range(4)]

    def start(self, stage):
        own, held = self.own, self.held
        if self.size != 4:
            if stage == 0:
                for peer in other_members("tensor", self.size):
                    self.send(own, held.at[self.me], peer)
            return
        beside, below, _ = square_peers(self.me)
        parts = self.quarters()
        upper, lower = parts[stage], parts[2 + stage]
        for part, peer in ((upper, beside), (lower, below), (lower, beside), (upper, below)):
            self.send(own.at[part], held.at[self.me, part], peer)

    def forward(self):
        own, held, rows = self.own, self.held, self.rows
        if self.size != 4:
            self.store(own, self.me * rows, rows)
            return
        beside, below, _ = square_peers(self.me)
        half = rows // 2
        self.store(own.at[pl.ds(0, half)], self.me * rows, half)
        self.store(own.at[pl.ds(half, half)], self.me * rows + half, half)
        parts = self.quarters()
        for stage in range(2):
            self.copies[4 * stage].wait_recv()
            self.send(held.at[beside, parts[stage]], held.at[beside, parts[stage]], below)
            self.copies[4 * stage + 1].wait_recv()
            self.send(held.at[below, parts[2 + stage]], held.at[below, parts[2 + stage]], beside)

    def finish(self):
        held, rows = self.held, self.rows
        if self.size != 4:
            for step, copy in enumerate(self.copies):
                copy.wait_recv()
                slot = lax.rem(self.me + self.size - step - 1, self.size)
                self.store(held.at[slot], slot * rows, rows)
        else:
            beside, below, across = square_peers(self.me)
            half = rows // 2
            first, second = pl.ds(0, half), pl.ds(half, half)
            self.store(held.at[beside, first], beside * rows, half)
            self.store(held.at[below, second], below * rows + half, half)
            for indices, slot, start in (
                ((2, 6), beside, half),
                ((3, 7), below, 0),
                ((8, 10), across, 0),
                ((9, 11), across, half),
            ):
                for index in indices:
                    self.copies[index].wait_recv()
                self.store(held.at[slot, pl.ds(start, half)], slot * rows + start, half)
        for copy in self.copies:
            copy.wait_send()
        for copy in self.stores + self.turns:
            copy.wait()


def gather_kernel(size, count, *refs):
    own_refs, out_refs, rest = refs[:count], refs[count : 3 * count], refs[3 * count :]
    greet(neighbours(size))
    gathers = [
        Gather(size, own_refs[k], *out_refs[2 * k : 2 * k + 2], *rest[6 * k : 6 * k + 6])
        for k in range(count)
    ]
    for gather in gathers:
        gather.start(0)
        gather.start(1)
        gather.forward()
    for gather in gathers:
        gather.finish()


def gather_rows(arrays, size, collective_id):
    count = len(arrays)
    rows, columns = arrays[0].shape
    scratch = []
    out_shape = []
    for _ in arrays:
        scratch += Gather.scratch(size, rows, columns)
        out_shape += [
            jax.ShapeDtypeStruct((size * rows, columns), jnp.bfloat16),
            jax.ShapeDtypeStruct((columns, size * rows), jnp.bfloat16),
        ]
    return pl.pallas_call(
        functools.partial(gather_kernel, size, count),
        out_shape=out_shape,
        in_specs=[pl.BlockSpec(memory_space=pltpu.VMEM)] * count,
        out_specs=[pl.BlockSpec(memory_space=pl.ANY)] * len(out_shape),
        scratch_shapes=scratch,
        compiler_params=pltpu.CompilerParams(
            collective_id=collective_id, has_side_effects=True, vmem_limit_bytes=VMEM_LIMIT
        ),
        cost_estimate=pl.CostEstimate(
            flops=0, bytes_accessed=count * 30 * size * rows * columns, transcendentals=0
        ),
        name="gather_rows",
    )(*arrays)


class Operand:
    def __init__(self, size, first_column, left_far, weight_far, left, weight, left_sem, weight_sem):
        self.left, self.weight = left, weight
        self.rows = left.shape[0] // size
        self.tile = min(512, weight.shape[0])
        self.far = left_far, weight_far
        self.first_column = first_column
        self.left_sem, self.weight_sem = left_sem, weight_sem

    @staticmethod
    def scratch(size, left, weight):
        width = left.shape[1]
        return [
            pltpu.VMEM(left.shape, left.dtype),
            pltpu.VMEM((weight.shape[0], width), weight.dtype),
            pltpu.SemaphoreType.DMA((size,)),
            pltpu.SemaphoreType.DMA((max(1, weight.shape[0] // 512),)),
        ]

    def left_copy(self, slot, owner):
        piece = pl.ds(pl.multiple_of(owner * self.rows, self.rows), self.rows)
        return pltpu.make_async_copy(self.far[0].at[piece], self.left.at[piece], self.left_sem.at[slot])

    def weight_copy(self, index):
        piece = pl.ds(pl.multiple_of(index * self.tile, self.tile), self.tile)
        columns = pl.ds(self.first_column, self.left.shape[1])
        return pltpu.make_async_copy(
            self.far[1].at[piece, columns], self.weight.at[piece], self.weight_sem.at[index]
        )


def block_product(operands, start, rows, fresh, write, after):
    total = operands[0].weight.shape[0]
    tile = operands[0].tile
    start = pl.multiple_of(start, rows)

    def step(index, carry):
        @pl.when(fresh)
        def _():
            for operand in operands:
                operand.weight_copy(index).wait()

        columns = pl.ds(pl.multiple_of(index * tile, tile), tile)
        values = None
        for operand in operands:
            part = times_transposed(
                operand.left[pl.ds(start, rows), :], operand.weight[columns, :]
            )
            values = part if values is None else values + part
        write(columns, values)
        after(index)
        return carry

    lax.fori_loop(0, total // tile, step, 0)


class Scatter:
    def __init__(self, size, outgoing, *rest):
        self.size, self.outgoing = size, outgoing
        if size == 4:
            self.passing, rest = rest[0], rest[1:]
        self.arriving, self.send_sem, self.recv_sem = rest
        self.rows = outgoing.shape[1]
        self.me = lax.axis_index("tensor")
        self.stages = 2 if size == 4 else 1
        self.plan()

    @staticmethod
    def scratch(size, rows, columns):
        if size == 4:
            sends = 10
            buffers = [
                pltpu.VMEM((4, rows, columns), jnp.bfloat16),
                pltpu.VMEM((2, rows // 2, columns), jnp.bfloat16),
                pltpu.VMEM((2, rows, columns), jnp.bfloat16),
            ]
        else:
            sends = size - 1
            buffers = [
                pltpu.VMEM((size, rows, columns), jnp.bfloat16),
                pltpu.VMEM((size - 1, rows, columns), jnp.bfloat16),
            ]
        return buffers + [pltpu.SemaphoreType.DMA((sends,)), pltpu.SemaphoreType.DMA((sends,))]

    def prepare(self, index, source, target, peer):
        return remote(source, target, self.send_sem.at[index], self.recv_sem.at[index], peer)

    def plan(self):
        outgoing, arriving = self.outgoing, self.arriving
        if self.size != 4:
            self.copies = [
                self.prepare(step, outgoing.at[step], arriving.at[step], peer)
                for step, peer in enumerate(other_members("tensor", self.size))
            ]
            self.early, self.starts = (), tuple((step, step) for step in range(self.size - 1))
            return
        beside, below, _ = square_peers(self.me)
        half, quarter = self.rows // 2, self.rows // 4
        first, second = pl.ds(0, half), pl.ds(half, half)
        middle = outgoing.shape[2] // 2
        left, right = pl.ds(0, middle), pl.ds(middle, middle)
        upper = [pl.ds(stage * quarter, quarter) for stage in range(2)]
        lower = [pl.ds(half + stage * quarter, quarter) for stage in range(2)]
        everything = pl.ds(0, half)
        self.copies = [
            self.prepare(0, outgoing.at[0, first, left], self.passing.at[0, everything, left], beside),
            self.prepare(1, outgoing.at[0, second, left], self.passing.at[1, everything, left], below),
            self.prepare(2, outgoing.at[0, first, right], self.passing.at[0, everything, right], beside),
            self.prepare(3, outgoing.at[0, second, right], self.passing.at[1, everything, right], below),
            self.prepare(4, outgoing.at[1, first], arriving.at[0, first], beside),
            self.prepare(5, outgoing.at[2, second], arriving.at[1, second], below),
            self.prepare(6, outgoing.at[1, lower[0]], arriving.at[0, lower[0]], beside),
            self.prepare(7, outgoing.at[2, upper[0]], arriving.at[1, upper[0]], below),
            self.prepare(8, outgoing.at[1, lower[1]], arriving.at[0, lower[1]], beside),
            self.prepare(9, outgoing.at[2, upper[1]], arriving.at[1, upper[1]], below),
        ]
        self.early, self.starts = (0, 1), ((0, 2), (0, 3), (1, 4), (2, 5))

    def owner(self, slot):
        if self.size != 4:
            return lax.rem(self.me + slot + 1, self.size)
        beside, below, across = square_peers(self.me)
        return jnp.where(
            slot == 0, across, jnp.where(slot == 1, beside, jnp.where(slot == 2, below, self.me))
        )

    def load(self, operands):
        tiles = operands[0].weight.shape[0] // operands[0].tile
        for operand in operands:
            operand.left_copy(0, self.owner(0)).start()
        for index in range(tiles):
            for operand in operands:
                operand.weight_copy(index).start()
        for slot in range(1, self.size):
            for operand in operands:
                operand.left_copy(slot, self.owner(slot)).start()

    def fill(self, operands, look=None, between=None):
        rows = self.rows

        def step(slot, carry):
            owner = self.owner(slot)
            for operand in operands:
                operand.left_copy(slot, owner).wait()

            def write(columns, values):
                self.outgoing[slot, :, columns] = values.astype(self.outgoing.dtype)
                if look is not None:
                    look(owner, columns, values)

            tiles = operands[0].weight.shape[0] // operands[0].tile

            def after(index):
                for early in self.early:
                    pl.when((slot == 0) & (index == max(tiles // 2, 1) - 1))(self.copies[early].start)

            block_product(operands, owner * rows, rows, slot == 0, write, after)
            for at, index in self.starts:
                pl.when(slot == at)(self.copies[index].start)
            if between is not None:
                pl.when(slot == 0)(between)
            return carry

        lax.fori_loop(0, self.size, step, 0)

    def relay(self):
        if self.size != 4:
            return
        half, quarter = self.rows // 2, self.rows // 4
        for stage in range(2):
            for arrivals, source, slot, start, onward in (
                ((1, 3), 1, 1, half, 6 + 2 * stage),
                ((0, 2), 0, 2, 0, 7 + 2 * stage),
            ):
                if stage == 0:
                    for index in arrivals:
                        self.copies[index].wait_recv()
                piece = pl.ds(start + stage * quarter, quarter)
                self.outgoing[slot, piece, :] = add_rounded(
                    self.outgoing[slot, piece, :],
                    self.passing[source, stage * quarter : (stage + 1) * quarter, :],
                )
                self.copies[onward].start()

    def collect(self, stage):
        if self.size != 4:
            for copy in self.copies:
                copy.wait_recv()
            return
        if stage == 0:
            self.copies[4].wait_recv()
            self.copies[5].wait_recv()
        self.copies[6 + 2 * stage].wait_recv()
        self.copies[7 + 2 * stage].wait_recv()

    def over_rows(self, stage, body):
        if self.size != 4:
            over_pieces(self.rows, body)
            return
        half, quarter = self.rows // 2, self.rows // 4
        over_pieces(quarter, body, stage * quarter)
        over_pieces(quarter, body, half + stage * quarter)

    def over_stages(self, body, done=None):
        for stage in range(self.stages):
            self.collect(stage)
            self.over_rows(stage, body)
            if done is not None:
                done(stage)

    def total(self, piece):
        total = self.outgoing[self.size - 1, piece, :].astype(jnp.float32)
        for index in range(self.arriving.shape[0]):
            total = total + self.arriving[index, piece, :].astype(jnp.float32)
        return total

    def drain(self):
        for copy in self.copies:
            copy.wait_send()


class Chain:
    def __init__(
        self, chips, steps, rising_refs, falling_refs, up_ref, down_ref,
        rise, fall, up, down, load_sem, send_sem, recv_sem,
    ):
        self.chips, self.steps = chips, steps
        self.rise, self.fall, self.up, self.down = rise, fall, up, down
        device = lax.axis_index("dp")
        self.chip = device // 2
        count = len(steps)
        self.loads = [
            pltpu.make_async_copy(source, target, load_sem.at[index])
            for index, (source, target) in enumerate(
                [(up_ref, up.at[0]), (down_ref, down.at[0])]
                + [(ref, rise.at[index]) for index, ref in enumerate(rising_refs)]
                + [(ref, fall.at[index]) for index, ref in enumerate(falling_refs)]
            )
        ]
        above = lax.rem(device + 2, 2 * chips)
        under = lax.rem(device + 2 * chips - 2, 2 * chips)
        self.neighbours = [("dp", above), ("dp", under)]
        self.rises = [
            remote(rise.at[i], up.at[i + 1], send_sem.at[i], recv_sem.at[i], above, "dp")
            for i in range(count)
        ]
        self.falls = [
            remote(
                fall.at[i], down.at[i + 1], send_sem.at[count + i], recv_sem.at[count + i], under, "dp"
            )
            for i in range(count)
        ]

    @staticmethod
    def scratch(count, rows, columns):
        return [
            pltpu.VMEM((count, rows, columns), jnp.bfloat16),
            pltpu.VMEM((count, rows, columns), jnp.bfloat16),
            pltpu.VMEM((count + 1, rows, columns), jnp.bfloat16),
            pltpu.VMEM((count + 1, rows, columns), jnp.bfloat16),
            pltpu.SemaphoreType.DMA((2 * count + 2,)),
            pltpu.SemaphoreType.DMA((2 * count,)),
            pltpu.SemaphoreType.DMA((2 * count,)),
        ]

    def load(self):
        for copy in self.loads:
            copy.start()

    def step(self, index):
        if index == 0:
            for copy in self.loads:
                copy.wait()
        step = self.steps[index]
        rows = self.rise.shape[1]
        sends_up = self.chip < step
        sends_down = self.chip >= self.chips - step

        @pl.when(sends_up & (self.chip > 0))
        def _():
            def add(piece):
                self.rise[index, piece, :] = add_rounded(
                    self.rise[index, piece, :], self.up[index, piece, :]
                )

            over_pieces(rows, add)

        pl.when(sends_up)(self.rises[index].start)

        @pl.when(sends_down & (self.chip < self.chips - 1))
        def _():
            def add(piece):
                self.fall[index, piece, :] = add_rounded(
                    self.fall[index, piece, :], self.down[index, piece, :]
                )

            over_pieces(rows, add)

        pl.when(sends_down)(self.falls[index].start)

    def arrives(self, index):
        step = self.steps[index]
        from_under = (self.chip > 0) & (self.chip <= step)
        from_above = (self.chip < self.chips - 1) & (self.chip >= self.chips - step - 1)
        return from_under, from_above

    def wait(self, index):
        from_under, from_above = self.arrives(index)
        pl.when(from_under)(self.rises[index].wait_recv)
        pl.when(from_above)(self.falls[index].wait_recv)

    def drain(self):
        for index, step in enumerate(self.steps):
            pl.when(self.chip < step)(self.rises[index].wait_send)
            pl.when(self.chip >= self.chips - step)(self.falls[index].wait_send)


def add_rounded(first, second):
    return (first.astype(jnp.float32) + second.astype(jnp.float32)).astype(jnp.bfloat16)


def over_pieces(rows, body, start=0):
    count = min(32, rows)

    def step(index, carry):
        body(pl.ds(pl.multiple_of(start + index * count, count), count))
        return carry

    lax.fori_loop(0, rows // count, step, 0)


def send_terms(axis, peers, source, landing, send_sem, recv_sem):
    me = lax.axis_index(axis)
    landing[me] = source[...]
    copies = []
    for step, peer in enumerate(peers):
        copy = remote(source, landing.at[me], send_sem.at[step], recv_sem.at[step], peer, axis)
        copy.start()
        copies.append(copy)
    return copies


def add_terms(landing, copies):
    for copy in copies:
        copy.wait_recv()
    total = landing[0]
    for index in range(1, landing.shape[0]):
        total = total + landing[index]
    return total


def split_operands(refs, size, first_columns):
    count = len(first_columns)
    far, refs, scratch = refs[: 2 * count], refs[2 * count : -4 * count], refs[-4 * count :]
    operands = [
        Operand(size, first, *far[2 * p : 2 * p + 2], *scratch[4 * p : 4 * p + 4])
        for p, first in enumerate(first_columns)
    ]
    return operands, refs


def store_row(target_ref, row_ref):
    width = target_ref.shape[1]
    for index in range(row_ref.shape[1] // width):
        target_ref[index : index + 1, :] = row_ref[:, index * width : (index + 1) * width]


def between_forward_kernel(size, first_columns, *refs):
    operands, refs = split_operands(refs, size, first_columns)
    input_ref, gain_ref, gathered_ref, turned_ref, state_ref, own_ref = refs[:6]
    buffers = 5 if size == 4 else 4
    scatter = Scatter(size, *refs[6 : 6 + buffers])
    gather = Gather(size, own_ref, gathered_ref, turned_ref, *refs[6 + buffers :])
    scatter.load(operands)
    greet(neighbours(size))
    scatter.fill(operands)
    scatter.relay()

    def norm(piece):
        state = input_ref[piece, :].astype(jnp.float32) + scatter.total(piece)
        state_ref[piece, :] = state
        own_ref[piece, :] = (state * row_scale(state) * gain_ref[...]).astype(own_ref.dtype)

    scatter.over_stages(norm, gather.start)
    gather.forward()
    gather.finish()
    scatter.drain()


def between_backward_kernel(size, chips, steps, first_columns, *refs):
    operands, refs = split_operands(refs, size, first_columns)
    state_ref, cotangent_ref, gain_ref = refs[:3]
    chain_count = 2 * len(steps) + 2
    chain_refs, last_refs, refs = refs[3 : 3 + chain_count], refs[3 + chain_count : 5 + chain_count], refs[5 + chain_count :]
    gathered_ref, gathered_turned_ref, slope_ref, term_ref, rising_ref, falling_ref = refs[:6]
    own_ref, sum_ref, last_sem = refs[6:9]
    buffers = 5 if size == 4 else 4
    scatter = Scatter(size, *refs[9 : 9 + buffers])
    gather = Gather(size, own_ref, gathered_ref, gathered_turned_ref, *refs[9 + buffers : 15 + buffers])
    chain = Chain(
        chips, steps, chain_refs[: len(steps)], chain_refs[len(steps) : -2], *chain_refs[-2:],
        *refs[15 + buffers :],
    )
    last_loads = [
        pltpu.make_async_copy(source, target, last_sem.at[index])
        for index, (source, target) in enumerate(zip(last_refs, (rising_ref, falling_ref)))
    ]
    chain.load()
    scatter.load(operands)
    for load in last_loads:
        load.start()
    greet(neighbours(size) + chain.neighbours)
    scatter.fill(operands, between=lambda: chain.step(0))
    scatter.relay()
    sum_ref[...] = jnp.zeros_like(sum_ref)

    def norm(piece):
        back = scatter.total(piece)
        state = state_ref[piece, :]
        scale = row_scale(state)
        unit = state * scale
        sum_ref[...] += jnp.sum(back * unit, axis=0, keepdims=True)
        unit_slope = back * gain_ref[...]
        slope = cotangent_ref[piece, :].astype(jnp.float32) + scale * (
            unit_slope - unit * jnp.mean(unit_slope * unit, axis=-1, keepdims=True)
        )
        slope_ref[piece, :] = slope
        own_ref[piece, :] = slope.astype(own_ref.dtype)

    scatter.over_stages(norm, gather.start)
    store_row(term_ref, sum_ref)
    gather.forward()
    chain.wait(0)
    for index in range(1, len(steps)):
        chain.step(index)
        chain.wait(index)
    for load in last_loads:
        load.wait()
    last = len(steps)
    for needed, landing, out_ref in (
        ((chain.chip > 0) & (chain.chip < chips - 1), chain.up, rising_ref),
        ((chain.chip > 0) & (chain.chip < chips - 1), chain.down, falling_ref),
    ):

        @pl.when(needed)
        def _(landing=landing, out_ref=out_ref):
            def add(piece):
                out_ref[piece, :] = add_rounded(out_ref[piece, :], landing[last, piece, :])

            over_pieces(out_ref.shape[0], add)

    gather.finish()
    scatter.drain()
    chain.drain()


def last_kernel(sizes, first_columns, *refs):
    data_size, size = sizes
    operands, refs = split_operands(refs, size, first_columns)
    input_ref, gain_ref, slope_ref, terms_ref, rows_ref = refs[:5]
    gradient_ref, terms_out_ref, sum_ref, partial_ref, group_ref, inner, outer = refs[5:12]
    inner_send, inner_recv, outer_send, outer_recv = refs[12:16]
    mixing = Scatter(size, *refs[16:])
    rows = gradient_ref.shape[0]
    mixing.load(operands)
    greet(
        [("tensor", peer) for peer in other_members("tensor", size)]
        + [("dp", peer) for peer in other_members("dp", data_size)]
    )
    sum_ref[...] = jnp.zeros_like(sum_ref)

    def look(owner, columns, values):
        piece = pl.ds(pl.multiple_of(owner * rows, rows), rows)
        sum_ref[:, columns] += jnp.sum(
            values * rows_ref[piece, columns].astype(jnp.float32), axis=0, keepdims=True
        )

    mixing.fill(operands, look)
    sum_ref[...] = sum_ref[...] / gain_ref[...]
    kept = partial_ref.shape[0] - terms_ref.shape[0]
    partial_ref[kept:, :] = terms_ref[...]
    store_row(partial_ref, sum_ref)
    inner_copies = send_terms(
        "tensor", other_members("tensor", size), partial_ref, inner, inner_send, inner_recv
    )
    mixing.relay()
    group_ref[...] = add_terms(inner, inner_copies)
    outer_copies = send_terms(
        "dp", other_members("dp", data_size), group_ref, outer, outer_send, outer_recv
    )
    terms_out_ref[...] = add_terms(outer, outer_copies)

    def norm(piece):
        back = mixing.total(piece)
        values = input_ref[piece, :].astype(jnp.float32)
        scale = row_scale(values)
        unit = values * scale
        unit_slope = back * gain_ref[...]
        gradient_ref[piece, :] = (
            slope_ref[piece, :]
            + scale * (unit_slope - unit * jnp.mean(unit_slope * unit, axis=-1, keepdims=True))
        ).astype(gradient_ref.dtype)

    mixing.over_stages(norm)
    for copy in inner_copies + outer_copies:
        copy.wait_send()
    mixing.drain()


def scatter_call(body, triples, size, others, far, outs, gathered, scratch, collective_id):
    far_spec = pl.BlockSpec(memory_space=pl.ANY)
    operands = [array for left, weight, _ in triples for array in (left, weight)]
    in_specs = [far_spec] * len(operands)
    for other in others:
        in_specs.append(pl.BlockSpec(other.shape, lambda i: (0, 0), pipeline_mode=pl.Buffered(1)))
    in_specs += [far_spec] * len(far)
    out_specs = [pl.BlockSpec(out.shape, lambda i: (0, 0)) for out in outs]
    if gathered:
        out_specs[:2] = [far_spec] * 2
    return pl.pallas_call(
        functools.partial(body, tuple(first for _, _, first in triples)),
        grid=(1,),
        out_shape=outs,
        in_specs=in_specs,
        out_specs=out_specs,
        scratch_shapes=list(scratch)
        + [part for left, weight, _ in triples for part in Operand.scratch(size, left, weight)],
        compiler_params=pltpu.CompilerParams(
            collective_id=collective_id, has_side_effects=True, vmem_limit_bytes=VMEM_LIMIT
        ),
        cost_estimate=pl.CostEstimate(
            flops=sum(2 * left.size * weight.shape[0] for left, weight, _ in triples),
            bytes_accessed=150_000_000,
            transcendentals=0,
        ),
    )(*operands, *others, *far)


LOG2E = 1.4426950408889634


def turn_tables(head_size):
    half_size = head_size // 2
    frequency = np.float32(rope_base) ** (
        -(np.arange(half_size, dtype=np.float32) * np.float32(2.0) / np.float32(head_size))
    )
    frequency = frequency.astype(np.float64)
    sign = np.concatenate([-np.ones(half_size), np.ones(half_size)])[None, :]
    positions = np.concatenate([np.arange(0, SEQUENCE_LENGTH, 128), np.arange(128)])
    angles = positions[:, None] * np.concatenate([frequency, frequency])[None, :]
    return np.cos(angles).astype(np.float32), (sign * np.sin(angles)).astype(np.float32)


def fill_tables(few_cosines_ref, few_sines_ref, cosine_ref, sine_ref):
    coarse = few_cosines_ref.shape[0] - 128
    near_cosine, near_sine = few_cosines_ref[coarse:, :], few_sines_ref[coarse:, :]

    def step(index, carry):
        far_cosine = few_cosines_ref[pl.ds(index, 1), :]
        far_sine = few_sines_ref[pl.ds(index, 1), :]
        rows = pl.ds(pl.multiple_of(index * 128, 128), 128)
        cosine_ref[rows, :] = far_cosine * near_cosine - far_sine * near_sine
        sine_ref[rows, :] = far_sine * near_cosine + far_cosine * near_sine
        return carry

    lax.fori_loop(0, coarse, step, 0)


def turn(values, cosine, sine):
    return values * cosine + pltpu.roll(values, values.shape[-1] // 2, 1) * sine


def turn_back(values, cosine, sine):
    return values * cosine - pltpu.roll(values, values.shape[-1] // 2, 1) * sine


def contract_first(first_operand, second_operand):
    return lax.dot_general(
        first_operand, second_operand, (((0,), (0,)), ((), ())), preferred_element_type=jnp.float32
    )


def visible_scores(key_rows, query_rows, first_row, multiplier):
    scores = times_transposed(key_rows, query_rows) * multiplier
    _, queries = scores.shape
    key_at = lax.broadcasted_iota(jnp.int32, (queries, queries), 0)
    query_at = lax.broadcasted_iota(jnp.int32, (queries, queries), 1)
    corner = jnp.where(query_at >= key_at, scores[first_row:], -1e30)
    if first_row == 0:
        return corner
    return jnp.concatenate([scores[:first_row], corner], axis=0)


def turn_heads(
    grouping, head_size, raw_ref, query_gain_ref, key_gain_ref, cosine_ref, sine_ref, query_ref, key_ref, value_ref
):
    def turned(start, gain):
        raw = raw_ref[:, pl.ds(start, head_size)]
        return turn(raw * row_scale(raw) * gain, cosine_ref[...], sine_ref[...]).astype(jnp.bfloat16)

    def step(part, carry):
        query_ref[part] = turned(pl.multiple_of(part * head_size, head_size), query_gain_ref[...])
        return carry

    lax.fori_loop(0, grouping, step, 0)
    key_ref[...] = turned(grouping * head_size, key_gain_ref[...])
    value_ref[...] = raw_ref[:, (grouping + 1) * head_size :].astype(jnp.bfloat16)


def attention_forward_kernel(
    grouping, head_size, block, rows_ref, weight_ref, few_cosines_ref, few_sines_ref, query_gain_ref, key_gain_ref,
    raw_ref, mixed_ref, total_ref, query_ref, key_ref, value_ref, cosine_ref, sine_ref,
):
    sequence = rows_ref.shape[0]
    multiplier = head_size ** (-0.5) * LOG2E

    @pl.when((pl.program_id(0) == 0) & (pl.program_id(1) == 0))
    def _():
        fill_tables(few_cosines_ref, few_sines_ref, cosine_ref, sine_ref)

    raw_ref[...] = simple_product(rows_ref[...], weight_ref[...])
    turn_heads(
        grouping, head_size, raw_ref, query_gain_ref, key_gain_ref, cosine_ref, sine_ref, query_ref, key_ref, value_ref
    )

    def head_step(part, carry):
        lanes = pl.ds(pl.multiple_of(part * head_size, head_size), head_size)
        for first_row in range(0, sequence, block):
            last_row = first_row + block
            scores = visible_scores(
                key_ref[:last_row, :], query_ref[part, first_row:last_row, :], first_row, multiplier
            )
            highest = jnp.max(scores, axis=0, keepdims=True)
            weights = jnp.exp2(scores - highest)
            total = jnp.sum(weights, axis=0, keepdims=True)
            weights = (weights * (1.0 / total)).astype(jnp.bfloat16)
            mixed_ref[first_row:last_row, lanes] = contract_first(
                weights, value_ref[:last_row, :]
            ).astype(mixed_ref.dtype)
            total_ref[0, pl.ds(part, 1), first_row:last_row] = highest + jnp.log2(total)
        return carry

    lax.fori_loop(0, grouping, head_step, 0)


def attention_forward(rows, weight, tables, query_gain, key_gain, heads, grouping):
    total_rows, depth = rows.shape
    head_size = query_gain.shape[0]
    sequences = total_rows // SEQUENCE_LENGTH
    width = (grouping + 2) * head_size
    block = min(256, SEQUENCE_LENGTH)
    table = pl.BlockSpec(tables[0].shape, lambda s, h: (0, 0))
    gain = pl.BlockSpec((1, head_size), lambda s, h: (0, 0))
    elements = heads * grouping * total_rows * SEQUENCE_LENGTH // 2
    return pl.pallas_call(
        functools.partial(attention_forward_kernel, grouping, head_size, block),
        grid=(sequences, heads),
        out_shape=[
            jax.ShapeDtypeStruct((total_rows, heads * width), jnp.float32),
            jax.ShapeDtypeStruct((total_rows, heads * grouping * head_size), jnp.bfloat16),
            jax.ShapeDtypeStruct((heads, grouping, total_rows), jnp.float32),
        ],
        in_specs=[
            pl.BlockSpec((SEQUENCE_LENGTH, depth), lambda s, h: (s, 0)),
            pl.BlockSpec((depth, width), lambda s, h: (0, h)),
            table,
            table,
            gain,
            gain,
        ],
        out_specs=[
            pl.BlockSpec((SEQUENCE_LENGTH, width), lambda s, h: (s, h)),
            pl.BlockSpec((SEQUENCE_LENGTH, grouping * head_size), lambda s, h: (s, h)),
            pl.BlockSpec((1, grouping, SEQUENCE_LENGTH), lambda s, h: (h, 0, s)),
        ],
        scratch_shapes=[
            pltpu.VMEM((grouping, SEQUENCE_LENGTH, head_size), jnp.bfloat16),
            pltpu.VMEM((SEQUENCE_LENGTH, head_size), jnp.bfloat16),
            pltpu.VMEM((SEQUENCE_LENGTH, head_size), jnp.bfloat16),
            pltpu.VMEM((SEQUENCE_LENGTH, head_size), jnp.float32),
            pltpu.VMEM((SEQUENCE_LENGTH, head_size), jnp.float32),
        ],
        compiler_params=pltpu.CompilerParams(vmem_limit_bytes=VMEM_LIMIT),
        cost_estimate=pl.CostEstimate(
            flops=2 * total_rows * depth * heads * width + 4 * elements * head_size,
            bytes_accessed=2 * (total_rows * depth + depth * heads * width),
            transcendentals=elements,
        ),
        name="attention_forward",
    )(rows, weight, *tables, query_gain.reshape(1, -1), key_gain.reshape(1, -1))


def norm_back(turned_slope, raw, gain, cosine, sine):
    norm_slope = turn_back(turned_slope, cosine, sine)
    scale = row_scale(raw)
    unit = raw * scale
    term = norm_slope * unit
    unit_slope = norm_slope * gain
    slope = scale * (unit_slope - unit * jnp.mean(unit_slope * unit, axis=-1, keepdims=True))
    return slope.astype(jnp.bfloat16), jnp.sum(term, axis=0, keepdims=True)


def attention_backward_kernel(size, grouping, head_size, block, first_columns, *refs):
    operands, refs = split_operands(refs, size, first_columns)
    (
        state_ref, weight_ref, raw_ref, mixed_ref, total_ref, few_cosines_ref, few_sines_ref,
        query_gain_ref, key_gain_ref, hidden_state_ref, slope_ref, gain_ref, output_ref,
        query_ref, key_ref, value_ref, out_slope_ref, turned_ref, key_sum_ref, value_sum_ref, cosine_ref, sine_ref,
    ) = refs[:22]
    scatter = Scatter(size, *refs[22:])
    step = pl.program_id(0) * pl.num_programs(1) + pl.program_id(1)
    steps = pl.num_programs(0) * pl.num_programs(1)

    @pl.when(step == 0)
    def _():
        scatter.load(operands)
        greet(neighbours(size))
        scatter.fill(operands)

    attend_backward_head(
        grouping, head_size, block, state_ref, weight_ref, raw_ref, mixed_ref, total_ref, few_cosines_ref,
        few_sines_ref, query_gain_ref, key_gain_ref, slope_ref, gain_ref, query_ref, key_ref, value_ref,
        out_slope_ref, turned_ref, key_sum_ref, value_sum_ref, cosine_ref, sine_ref,
    )

    @pl.when(step == 0)
    def _():
        scatter.relay()

    @pl.when(step == steps - 1)
    def _():
        def finish(piece):
            output_ref[piece, :] = (hidden_state_ref[piece, :] + scatter.total(piece)).astype(
                output_ref.dtype
            )

        scatter.over_stages(finish)
        scatter.drain()


def attend_backward_head(
    grouping, head_size, block, state_ref, weight_ref, raw_ref, mixed_ref, total_ref, few_cosines_ref, few_sines_ref,
    query_gain_ref, key_gain_ref, slope_ref, gain_ref, query_ref, key_ref, value_ref, out_slope_ref,
    turned_ref, key_sum_ref, value_sum_ref, cosine_ref, sine_ref,
):
    sequence = state_ref.shape[0]
    scale_factor = head_size ** (-0.5)
    multiplier = scale_factor * LOG2E

    @pl.when((pl.program_id(0) == 0) & (pl.program_id(1) == 0))
    def _():
        gain_ref[...] = jnp.zeros_like(gain_ref)
        fill_tables(few_cosines_ref, few_sines_ref, cosine_ref, sine_ref)

    out_slope_ref[...] = simple_product(state_ref[...], weight_ref[...]).astype(jnp.bfloat16)
    turn_heads(
        grouping, head_size, raw_ref, query_gain_ref, key_gain_ref, cosine_ref, sine_ref, query_ref, key_ref, value_ref
    )
    key_sum_ref[...] = jnp.zeros_like(key_sum_ref)
    value_sum_ref[...] = jnp.zeros_like(value_sum_ref)
    ones = jnp.ones((8, head_size), jnp.float32)

    def head_step(part, carry):
        lanes = pl.ds(pl.multiple_of(part * head_size, head_size), head_size)
        for first_row in range(0, sequence, block):
            last_row = first_row + block
            query_rows = query_ref[part, first_row:last_row, :]
            slope_rows = out_slope_ref[first_row:last_row, lanes]
            scores = visible_scores(key_ref[:last_row, :], query_rows, first_row, multiplier)
            weights = jnp.exp2(scores - total_ref[0, pl.ds(part, 1), first_row:last_row])
            value_sum_ref[:last_row, :] += simple_product(weights.astype(jnp.bfloat16), slope_rows)
            product = slope_rows.astype(jnp.float32) * mixed_ref[first_row:last_row, lanes].astype(jnp.float32)
            centre = lax.dot_general(
                ones,
                product,
                (((1,), (1,)), ((), ())),
                preferred_element_type=jnp.float32,
                precision=lax.Precision.HIGHEST,
            )[:1]
            weight_slope = times_transposed(value_ref[:last_row, :], slope_rows)
            score_slope = (weights * (weight_slope - centre)).astype(jnp.bfloat16)
            key_sum_ref[:last_row, :] += simple_product(score_slope, query_rows)
            turned_ref[first_row:last_row, :] = (
                contract_first(score_slope, key_ref[:last_row, :]) * scale_factor
            )
        slope, term = norm_back(
            turned_ref[...], raw_ref[:, lanes], query_gain_ref[...], cosine_ref[...], sine_ref[...]
        )
        slope_ref[:, lanes] = slope
        gain_ref[0:1, :] += term
        return carry

    lax.fori_loop(0, grouping, head_step, 0)
    lanes = slice(grouping * head_size, (grouping + 1) * head_size)
    slope, term = norm_back(
        key_sum_ref[...] * scale_factor, raw_ref[:, lanes], key_gain_ref[...], cosine_ref[...], sine_ref[...]
    )
    slope_ref[:, lanes] = slope
    gain_ref[1:2, :] += term
    slope_ref[:, (grouping + 1) * head_size :] = value_sum_ref[...].astype(jnp.bfloat16)


def attention_backward(
    state_rows, weight, weight_start, raw, mixed, totals, tables, query_gain, key_gain, heads, grouping,
    triples, hidden_state, size, collective_id,
):
    total_rows, depth = state_rows.shape
    head_size = query_gain.shape[0]
    sequences = total_rows // SEQUENCE_LENGTH
    width = (grouping + 2) * head_size
    out_width = grouping * head_size
    block = min(256, SEQUENCE_LENGTH)
    first_block = weight_start // out_width
    single = pl.Buffered(1)
    table = pl.BlockSpec(tables[0].shape, lambda s, h: (0, 0))
    gain = pl.BlockSpec((1, head_size), lambda s, h: (0, 0))
    elements = heads * grouping * total_rows * SEQUENCE_LENGTH // 2
    whole_rows = pltpu.VMEM((SEQUENCE_LENGTH, head_size), jnp.float32)
    operands = [array for left, other_weight, _ in triples for array in (left, other_weight)]
    in_specs = [pl.BlockSpec(memory_space=pl.ANY)] * len(operands)
    in_specs += [
        pl.BlockSpec((SEQUENCE_LENGTH, depth), lambda s, h: (s, 0), pipeline_mode=single),
        pl.BlockSpec((depth, out_width), lambda s, h: (0, first_block + h)),
        pl.BlockSpec((SEQUENCE_LENGTH, width), lambda s, h: (s, h)),
        pl.BlockSpec((SEQUENCE_LENGTH, out_width), lambda s, h: (s, h)),
        pl.BlockSpec((1, grouping, SEQUENCE_LENGTH), lambda s, h: (h, 0, s)),
        table,
        table,
        gain,
        gain,
        pl.BlockSpec(hidden_state.shape, lambda s, h: (0, 0), pipeline_mode=single),
    ]
    operands += [
        state_rows, weight, raw, mixed, totals, *tables, query_gain.reshape(1, -1), key_gain.reshape(1, -1),
        hidden_state,
    ]
    return pl.pallas_call(
        functools.partial(
            attention_backward_kernel, size, grouping, head_size, block,
            tuple(first for _, _, first in triples),
        ),
        grid=(sequences, heads),
        out_shape=[
            jax.ShapeDtypeStruct((total_rows, heads * width), jnp.bfloat16),
            jax.ShapeDtypeStruct((8, head_size), jnp.float32),
            jax.ShapeDtypeStruct(hidden_state.shape, jnp.bfloat16),
        ],
        in_specs=in_specs,
        out_specs=[
            pl.BlockSpec((SEQUENCE_LENGTH, width), lambda s, h: (s, h)),
            pl.BlockSpec((8, head_size), lambda s, h: (0, 0)),
            pl.BlockSpec(hidden_state.shape, lambda s, h: (0, 0)),
        ],
        scratch_shapes=[
            pltpu.VMEM((grouping, SEQUENCE_LENGTH, head_size), jnp.bfloat16),
            pltpu.VMEM((SEQUENCE_LENGTH, head_size), jnp.bfloat16),
            pltpu.VMEM((SEQUENCE_LENGTH, head_size), jnp.bfloat16),
            pltpu.VMEM((SEQUENCE_LENGTH, out_width), jnp.bfloat16),
            whole_rows,
            whole_rows,
            whole_rows,
            whole_rows,
            whole_rows,
            *Scatter.scratch(size, *hidden_state.shape),
            *[part for left, other, _ in triples for part in Operand.scratch(size, left, other)],
        ],
        compiler_params=pltpu.CompilerParams(
            collective_id=collective_id, has_side_effects=True, vmem_limit_bytes=VMEM_LIMIT
        ),
        cost_estimate=pl.CostEstimate(
            flops=2 * total_rows * depth * heads * out_width + 10 * elements * head_size,
            bytes_accessed=100_000_000,
            transcendentals=elements,
        ),
        name="attention_backward",
    )(*operands)


def feed_half_kernel(
    half, tile, block, rows_far, cotangent_far, weight_far, hidden_far, slope_far,
    rows_ref, cotangent_ref, weight_ref, hidden_ref, slope_ref, row_sem, weight_sem, out_sem,
):
    total = rows_ref.shape[0]
    blocks = total // block
    tiles = half // tile

    def row_copies(index):
        piece = pl.ds(pl.multiple_of(index * block, block), block)
        return [
            pltpu.make_async_copy(far.at[piece], ref.at[piece], row_sem.at[at, index])
            for at, (far, ref) in enumerate(((rows_far, rows_ref), (cotangent_far, cotangent_ref)))
        ]

    def weight_copies(index):
        copies = []
        for part in range(3):
            columns = pl.ds(pl.multiple_of(part * half + index * tile, tile), tile)
            copies.append(
                pltpu.make_async_copy(
                    weight_far.at[:, columns], weight_ref.at[part, index], weight_sem.at[part, index]
                )
            )
        return copies

    def out_copies(index):
        piece = pl.ds(pl.multiple_of(index * block, block), block)
        return [
            pltpu.make_async_copy(ref.at[piece], far.at[piece], out_sem.at[at, index])
            for at, (far, ref) in enumerate(((hidden_far, hidden_ref), (slope_far, slope_ref)))
        ]

    for copy in row_copies(0) + weight_copies(0):
        copy.start()
    for index in range(1, tiles):
        for copy in weight_copies(index):
            copy.start()
    for index in range(1, blocks):
        for copy in row_copies(index):
            copy.start()

    def row_step(row_index, carry):
        piece = pl.ds(pl.multiple_of(row_index * block, block), block)
        for copy in row_copies(row_index):
            copy.wait()

        def step(index, carry):
            @pl.when(row_index == 0)
            def _():
                for copy in weight_copies(index):
                    copy.wait()

            start = pl.multiple_of(index * tile, tile)
            rows = rows_ref[piece, :]
            gate = simple_product(rows, weight_ref[0, index])
            up = simple_product(rows, weight_ref[1, index])
            back = simple_product(cotangent_ref[piece, :], weight_ref[2, index])
            sigmoid = 1.0 / (1.0 + jnp.exp(-gate))
            gated = gate * sigmoid
            hidden_ref[piece, pl.ds(start, tile)] = (gated * up).astype(jnp.bfloat16)
            slope_ref[piece, pl.ds(start, tile)] = (
                back * up * sigmoid * (1.0 + gate * (1.0 - sigmoid))
            ).astype(jnp.bfloat16)
            slope_ref[piece, pl.ds(half + start, tile)] = (back * gated).astype(jnp.bfloat16)
            return carry

        lax.fori_loop(0, tiles, step, 0)
        for copy in out_copies(row_index):
            copy.start()
        return carry

    lax.fori_loop(0, blocks, row_step, 0)
    for index in range(blocks):
        for copy in out_copies(index):
            copy.wait()


def feed_half(rows, cotangent, weight):
    total_rows, depth = rows.shape
    block = min(512, total_rows)
    half = weight.shape[1] // 3
    tile = 256 if half % 256 == 0 else 128
    blocks, tiles = total_rows // block, half // tile
    far = pl.BlockSpec(memory_space=pl.ANY)
    return pl.pallas_call(
        functools.partial(feed_half_kernel, half, tile, block),
        out_shape=[
            jax.ShapeDtypeStruct((total_rows, half), jnp.bfloat16),
            jax.ShapeDtypeStruct((total_rows, 2 * half), jnp.bfloat16),
        ],
        in_specs=[far] * 3,
        out_specs=[far] * 2,
        scratch_shapes=[
            pltpu.VMEM(rows.shape, rows.dtype),
            pltpu.VMEM(rows.shape, rows.dtype),
            pltpu.VMEM((3, tiles, depth, tile), weight.dtype),
            pltpu.VMEM((total_rows, half), jnp.bfloat16),
            pltpu.VMEM((total_rows, 2 * half), jnp.bfloat16),
            pltpu.SemaphoreType.DMA((2, blocks)),
            pltpu.SemaphoreType.DMA((3, tiles)),
            pltpu.SemaphoreType.DMA((2, blocks)),
        ],
        compiler_params=pltpu.CompilerParams(vmem_limit_bytes=VMEM_LIMIT),
        cost_estimate=pl.CostEstimate(
            flops=6 * total_rows * depth * half,
            bytes_accessed=2 * (2 * total_rows * depth + 3 * depth * half),
            transcendentals=total_rows * half,
        ),
        name="feed_half",
    )(rows, cotangent, weight)


def grad_kernel(pair_count, with_other, order_ref, *refs):
    pairs = [refs[2 * p : 2 * p + 2] for p in range(pair_count)]
    refs = refs[2 * pair_count :]
    step = pl.program_id(0)
    if with_other:
        other_ref, refs = refs[0], refs[1:]
        out_refs, held_ref, copy_sem = refs[:-2], refs[-2], refs[-1]
    else:
        out_ref = refs[0]
    start = 0
    for left_ref, right_ref in pairs:
        width = right_ref.shape[1]
        tile = next(t for t in (768, 512, 384, 256, 128) if width % t == 0)
        for column in range(0, width, tile):
            values = simple_product(left_ref[...], right_ref[:, column : column + tile])
            columns = slice(start + column, start + column + tile)
            if with_other:
                values = values + other_ref[0, :, columns].astype(jnp.float32)
                held_ref[step, :, columns] = values.astype(jnp.bfloat16)
            else:
                out_ref[:, :, columns] = values.reshape(*out_ref.shape[:2], tile).astype(jnp.bfloat16)
        start += width
    if with_other:
        copies = [
            pltpu.make_async_copy(held_ref.at[index], out_ref, copy_sem.at[index])
            for index, out_ref in enumerate(out_refs)
        ]
        for index, copy in enumerate(copies):
            pl.when(step == index)(copy.start)

        @pl.when(step == len(copies) - 1)
        def _():
            for copy in copies:
                copy.wait()


def grad_blocks(order, pairs, other=None, group=1):
    count = order.shape[0]
    depth, total_rows = pairs[0][0].shape
    block = depth // lax.axis_size("dp")
    width = sum(right.shape[1] for _, right in pairs)
    in_specs = []
    operands = []
    for left, right in pairs:
        in_specs += [
            pl.BlockSpec(
                (group * block, total_rows),
                (lambda k, at: (at[k], 0)) if group == 1 else (lambda k, at: (k, 0)),
            ),
            pl.BlockSpec(right.shape, lambda k, at: (0, 0), pipeline_mode=pl.Buffered(1)),
        ]
        operands += [left, right]
    scratch = []
    if other is not None:
        in_specs.append(pl.BlockSpec((1, block, width), lambda k, at: (k, 0, 0)))
        operands.append(other)
        out_shape = [jax.ShapeDtypeStruct((block, width), jnp.bfloat16)] * count
        out_specs = [pl.BlockSpec(memory_space=pl.ANY)] * count
        scratch = [
            pltpu.VMEM((count, block, width), jnp.bfloat16),
            pltpu.SemaphoreType.DMA((count,)),
        ]
    else:
        out_shape = [jax.ShapeDtypeStruct((count, block, width), jnp.bfloat16)]
        out_specs = [pl.BlockSpec((group, block, width), lambda k, at: (k, 0, 0))]
    out = pl.pallas_call(
        functools.partial(grad_kernel, len(pairs), other is not None),
        grid_spec=pltpu.PrefetchScalarGridSpec(
            num_scalar_prefetch=1,
            grid=(count // group,),
            in_specs=in_specs,
            out_specs=out_specs,
            scratch_shapes=scratch,
        ),
        out_shape=out_shape,
        compiler_params=pltpu.CompilerParams(vmem_limit_bytes=VMEM_LIMIT),
        cost_estimate=pl.CostEstimate(
            flops=2 * total_rows * count * block * width,
            bytes_accessed=2 * (total_rows * count * block * len(pairs) + width * (total_rows + count * block)),
            transcendentals=0,
        ),
        name="grad_blocks",
    )(order, *operands)
    return out if other is not None else out[0]


def reduce_over_chips(pairs, sizes):
    data_size = sizes[0]
    chips = data_size // 2
    me = lax.axis_index("dp")
    chip, core = me // 2, lax.rem(me, 2)
    ahead = lax.rem(chip + jnp.arange(chips, dtype=jnp.int32), chips) * 2
    other = lax.ppermute(
        grad_blocks(ahead + (1 - core), pairs),
        "dp",
        [(device, device ^ 1) for device in range(data_size)],
    )
    blocks = grad_blocks(ahead + core, pairs, other)
    up = lax.ppermute(blocks[chips - 1], "dp", [(device, device + 2) for device in range(2)])
    down = lax.ppermute(
        blocks[1],
        "dp",
        [(device, device - 2) for device in range(data_size - 2, data_size)],
    )
    return blocks, up, down


def pack_mixing_kernel(heads, query_ref, key_ref, value_ref, output_ref, out_ref):
    query_width = query_ref.shape[1] // heads
    head_size = key_ref.shape[1] // heads
    start = 0
    for head in range(heads):
        for ref, part in ((query_ref, query_width), (key_ref, head_size), (value_ref, head_size)):
            out_ref[:, start : start + part] = ref[:, head * part : (head + 1) * part]
            start += part
    out_ref[:, start:] = output_ref[...].T


def pack_feed_kernel(gate_ref, up_ref, down_ref, first_ref, second_ref):
    start = 0
    for out_ref in (first_ref, second_ref):
        width = out_ref.shape[1] // 3
        part = slice(start, start + width)
        out_ref[:, :width] = gate_ref[:, part]
        out_ref[:, width : 2 * width] = up_ref[:, part]
        out_ref[:, 2 * width :] = down_ref[part, :].T
        start += width


def finish_kernel(
    heads, own_ref, up_ref, down_ref, second_ref, mixing_ref, output_total_ref, terms_ref, output_rows_ref, input_rows_ref,
    output_rows_out, input_rows_out, attention_term_out, query_out, key_out, value_out, query_gain_out, key_gain_out,
    output_out, feed_term_out, gate_out, up_out, down_out,
):
    output_rows_out[...] = output_rows_ref[...]
    input_rows_out[...] = input_rows_ref[...]
    count = attention_term_out.shape[0]
    attention_term_out[...] = terms_ref[:count, :]
    feed_term_out[...] = terms_ref[count : 2 * count, :]
    query_gain_out[...] = terms_ref[2 * count : 2 * count + 1, :]
    key_gain_out[...] = terms_ref[2 * count + 1 : 2 * count + 2, :]
    start = 0
    for total_refs in ((own_ref, up_ref, down_ref), (second_ref,)):
        width = total_refs[0].shape[1] // 3
        part = slice(start, start + width)

        def total(index):
            columns = slice(index * width, (index + 1) * width)
            return sum(ref[:, columns].astype(jnp.float32) for ref in total_refs)

        gate_out[:, part] = total(0)
        up_out[:, part] = total(1)
        down_out[part, :] = total(2).T
        start += width
    query_width = query_out.shape[1] // heads
    head_size = key_out.shape[1] // heads
    start = 0
    for head in range(heads):
        for out, part in ((query_out, query_width), (key_out, head_size), (value_out, head_size)):
            out[:, head * part : (head + 1) * part] = mixing_ref[:, start : start + part].astype(
                jnp.float32
            )
            start += part
    output_out[...] = output_total_ref[...].astype(jnp.float32).T


def whole_call(body, shapes, *operands):
    return pl.pallas_call(
        body,
        out_shape=shapes,
        in_specs=[pl.BlockSpec(memory_space=pltpu.VMEM)] * len(operands),
        out_specs=[pl.BlockSpec(memory_space=pltpu.VMEM)] * len(shapes),
        compiler_params=pltpu.CompilerParams(vmem_limit_bytes=VMEM_LIMIT),
        cost_estimate=pl.CostEstimate(
            flops=0, bytes_accessed=4 * sum(operand.size for operand in operands), transcendentals=0
        ),
    )(*operands)


def per_device(
    block_input,
    attention_gain,
    query_weight,
    key_matrix,
    value_matrix,
    query_gain,
    key_gain,
    output_weight,
    feed_gain,
    gate_weight,
    up_weight,
    down_weight,
    out_cotangent,
):
    size = lax.axis_size("tensor")
    sizes = (lax.axis_size("dp"), size)
    model_width = block_input.shape[1]
    head_size = query_gain.shape[0]
    query_columns = query_weight.shape[1]
    key_columns = key_matrix.shape[1]
    heads = key_columns // head_size
    grouping = query_columns // key_columns
    hidden_columns = gate_weight.shape[1]
    qkv_columns = query_columns + 2 * key_columns
    first_columns = hidden_columns * 2 // 3 // 256 * 256 or hidden_columns // 2
    second_columns = hidden_columns - first_columns
    tables = turn_tables(head_size)

    block_width = query_weight.shape[0]
    (mixing_local,) = whole_call(
        functools.partial(pack_mixing_kernel, heads),
        [jax.ShapeDtypeStruct((block_width, qkv_columns + query_columns), jnp.bfloat16)],
        query_weight, key_matrix, value_matrix, output_weight,
    )
    mixing_full = lax.all_gather(mixing_local, "dp", axis=0, tiled=True)
    feed_locals = whole_call(
        pack_feed_kernel,
        [
            jax.ShapeDtypeStruct((block_width, 3 * columns), jnp.bfloat16)
            for columns in (first_columns, second_columns)
        ],
        gate_weight, up_weight, down_weight,
    )
    feed_full = [lax.all_gather(part, "dp", axis=0, tiled=True) for part in feed_locals]

    input_float = block_input.astype(jnp.float32)
    first_scale = row_scale(input_float)
    first_unit = input_float * first_scale
    mixer_local = (first_unit * attention_gain).astype(jnp.bfloat16)
    mixer_rows, mixer_turned, cotangent_rows, cotangent_turned = gather_rows(
        (mixer_local, out_cotangent), size, 0
    )

    raw, mixed_rows, totals = attention_forward(
        mixer_rows, mixing_full, tables, query_gain, key_gain, heads, grouping
    )
    local_shape = block_input.shape
    local_rows = local_shape[0]
    gain_rows = model_width // head_size
    gathered_shapes = [
        jax.ShapeDtypeStruct((size * local_rows, model_width), jnp.bfloat16),
        jax.ShapeDtypeStruct((model_width, size * local_rows), jnp.bfloat16),
    ]
    local_float = jax.ShapeDtypeStruct(local_shape, jnp.float32)
    local_half = jax.ShapeDtypeStruct(local_shape, jnp.bfloat16)
    row_sum = pltpu.VMEM((1, model_width), jnp.float32)
    own_rows = pltpu.VMEM(local_shape, jnp.bfloat16)
    scatter_scratch = Scatter.scratch(size, *local_shape)
    gather_scratch = Gather.scratch(size, *local_shape)
    feed_rows, feed_turned, hidden_state = scatter_call(
        functools.partial(between_forward_kernel, size),
        [(mixed_rows, mixing_full, qkv_columns)],
        size,
        [block_input, feed_gain.reshape(1, -1)],
        [],
        [*gathered_shapes, local_float],
        True,
        [own_rows, *scatter_scratch, *gather_scratch],
        1,
    )

    hidden_first, slope_first = feed_half(feed_rows, cotangent_rows, feed_full[0])
    blocks, up, down = reduce_over_chips(
        [(feed_turned, slope_first), (cotangent_turned, hidden_first)], sizes
    )
    blocks, later_full = lax.optimization_barrier((blocks, feed_full[1]))
    hidden_second, slope_second = feed_half(feed_rows, cotangent_rows, later_full)
    plain_order = jnp.arange(sizes[0], dtype=jnp.int32)
    second_grad = grad_blocks(
        plain_order, [(feed_turned, slope_second), (cotangent_turned, hidden_second)], group=2
    ).reshape(model_width, -1)
    second_grad, slope_second = lax.optimization_barrier((second_grad, slope_second))
    second_total = lax.psum_scatter(second_grad, "dp", scatter_dimension=0, tiled=True)
    chips = sizes[0] // 2
    middle_steps = tuple(range(2, chips - 1))
    chain_block = jax.ShapeDtypeStruct(blocks[0].shape, jnp.bfloat16)
    state_rows, state_turned, state_slope, feed_term, rising, falling = scatter_call(
        functools.partial(between_backward_kernel, size, chips, middle_steps),
        [(slope_first, feed_full[0], 0), (slope_second, later_full, 0)],
        size,
        [hidden_state, out_cotangent, feed_gain.reshape(1, -1)],
        [blocks[chips - step] for step in middle_steps]
        + [blocks[step] for step in middle_steps]
        + [up, down, blocks[1], blocks[chips - 1]],
        [
            *gathered_shapes,
            local_float,
            jax.ShapeDtypeStruct((gain_rows, head_size), jnp.float32),
            chain_block,
            chain_block,
        ],
        True,
        [
            own_rows,
            row_sum,
            pltpu.SemaphoreType.DMA((2,)),
            *scatter_scratch,
            *gather_scratch,
            *Chain.scratch(len(middle_steps), *blocks[0].shape),
        ],
        2,
    )
    up = lax.ppermute(
        rising, "dp", [(device, device + 2) for device in range(sizes[0] - 2)]
    )
    down = lax.ppermute(
        falling, "dp", [(device, device - 2) for device in range(2, sizes[0])]
    )
    output_grad = grad_blocks(plain_order, [(state_turned, mixed_rows)], group=4).reshape(model_width, -1)
    output_grad, state_rows = lax.optimization_barrier((output_grad, state_rows))
    output_total = lax.psum_scatter(output_grad, "dp", scatter_dimension=0, tiled=True)
    qkv_slope, head_terms, block_output = attention_backward(
        state_rows, mixing_full, qkv_columns, raw, mixed_rows, totals, tables,
        query_gain, key_gain, heads, grouping,
        [
            (hidden_first, feed_full[0], 2 * first_columns),
            (hidden_second, later_full, 2 * second_columns),
        ],
        hidden_state, size, 4,
    )
    mixing_grad = grad_blocks(plain_order, [(mixer_turned, qkv_slope)], group=2).reshape(model_width, -1)
    mixing_grad, qkv_slope = lax.optimization_barrier((mixing_grad, qkv_slope))
    mixing_total = lax.psum_scatter(mixing_grad, "dp", scatter_dimension=0, tiled=True)
    terms_shape = (2 * gain_rows + head_terms.shape[0], head_size)
    input_gradient, terms = scatter_call(
        functools.partial(last_kernel, sizes),
        [(qkv_slope, mixing_full, 0)],
        size,
        [
            block_input,
            attention_gain.reshape(1, -1),
            state_slope,
            jnp.concatenate([feed_term, head_terms], axis=0),
            mixer_rows,
        ],
        [],
        [local_half, jax.ShapeDtypeStruct(terms_shape, jnp.float32)],
        False,
        [
            row_sum,
            pltpu.VMEM(terms_shape, jnp.float32),
            pltpu.VMEM(terms_shape, jnp.float32),
            pltpu.VMEM((size, *terms_shape), jnp.float32),
            pltpu.VMEM((sizes[0], *terms_shape), jnp.float32),
            *[pltpu.SemaphoreType.DMA((count - 1,)) for count in (size, size, *sizes[:1] * 2)],
            *scatter_scratch,
        ],
        3,
    )

    def whole_float(*shape):
        return jax.ShapeDtypeStruct(shape, jnp.float32)

    outs = whole_call(
        functools.partial(finish_kernel, heads),
        [
            local_half,
            local_half,
            whole_float(gain_rows, head_size),
            whole_float(block_width, query_columns),
            whole_float(block_width, key_columns),
            whole_float(block_width, key_columns),
            whole_float(1, head_size),
            whole_float(1, head_size),
            whole_float(query_columns, block_width),
            whole_float(gain_rows, head_size),
            whole_float(block_width, hidden_columns),
            whole_float(block_width, hidden_columns),
            whole_float(hidden_columns, block_width),
        ],
        blocks[0], up, down, second_total, mixing_total, output_total, terms, block_output, input_gradient,
    )
    return tuple(
        out.reshape(-1) if index in (2, 6, 7, 9) else out for index, out in enumerate(outs)
    )


def solution(mesh):
    in_specs = (
        P(("dp", "tensor"), None),
        P(),
        P("dp", "tensor"),
        P("dp", "tensor"),
        P("dp", "tensor"),
        P(),
        P(),
        P("tensor", "dp"),
        P(),
        P("dp", "tensor"),
        P("dp", "tensor"),
        P("tensor", "dp"),
        P(("dp", "tensor"), None),
    )
    out_specs = (
        P(("dp", "tensor"), None),
        P(("dp", "tensor"), None),
        P(),
        P("dp", "tensor"),
        P("dp", "tensor"),
        P("dp", "tensor"),
        P(),
        P(),
        P("tensor", "dp"),
        P(),
        P("dp", "tensor"),
        P("dp", "tensor"),
        P("tensor", "dp"),
    )

    return jax.shard_map(per_device, mesh=mesh, in_specs=in_specs, out_specs=out_specs, check_vma=False)
```

```python
import functools

import jax
import jax.numpy as jnp
import numpy as np
from jax import lax
from jax.experimental import pallas as pl
from jax.experimental.pallas import tpu as pltpu
from jax.sharding import PartitionSpec as P


SEQUENCE_LENGTH = 1024

epsilon = 1e-06
rope_base = 1000000.0


MESH = pl.DeviceIdType.MESH
VMEM_LIMIT = 62 * 1024 * 1024


def row_scale(values):
    return lax.rsqrt(jnp.mean(values * values, axis=-1, keepdims=True) + epsilon)


def times_transposed(first_operand, second_operand):
    return lax.dot_general(
        first_operand, second_operand, (((1,), (1,)), ((), ())), preferred_element_type=jnp.float32
    )


def simple_product(first_operand, second_operand):
    return jnp.dot(first_operand, second_operand, preferred_element_type=jnp.float32)


def remote(source, target, send_sem, recv_sem, peer, axis="tensor"):
    return pltpu.make_async_remote_copy(
        src_ref=source,
        dst_ref=target,
        send_sem=send_sem,
        recv_sem=recv_sem,
        device_id={axis: peer},
        device_id_type=MESH,
    )


def greet(peers):
    barrier = pltpu.get_barrier_semaphore()
    for axis, peer in peers:
        pl.semaphore_signal(barrier, inc=1, device_id={axis: peer}, device_id_type=MESH)
    pl.semaphore_wait(barrier, len(peers))


def square_peers(me):
    column = lax.rem(me, 2)
    row = me // 2
    return row * 2 + (1 - column), (1 - row) * 2 + column, (1 - row) * 2 + (1 - column)


def neighbours(size):
    if size == 4:
        beside, below, _ = square_peers(lax.axis_index("tensor"))
        return [("tensor", beside), ("tensor", below)]
    return [("tensor", peer) for peer in other_members("tensor", size)]


def other_members(axis, count):
    me = lax.axis_index(axis)
    return [lax.rem(me + step, count) for step in range(1, count)]


class Gather:
    def __init__(
        self, size, own_ref, out_ref, turned_out_ref, held_ref, turned_ref, send_sem, recv_sem, local_sem, turned_sem
    ):
        self.size, self.own, self.out, self.held = size, own_ref, out_ref, held_ref
        self.turned_out, self.turned = turned_out_ref, turned_ref
        self.send_sem, self.recv_sem, self.local_sem = send_sem, recv_sem, local_sem
        self.turned_sem = turned_sem
        self.me = lax.axis_index("tensor")
        self.rows = own_ref.shape[0]
        self.copies, self.stores, self.turns = [], [], []

    @staticmethod
    def scratch(size, rows, columns):
        sends, local = (12, 8) if size == 4 else (size - 1, size)
        return [
            pltpu.VMEM((size, rows, columns), jnp.bfloat16),
            pltpu.VMEM((columns, size * rows), jnp.bfloat16),
            pltpu.SemaphoreType.DMA((sends,)),
            pltpu.SemaphoreType.DMA((sends,)),
            pltpu.SemaphoreType.DMA((local,)),
            pltpu.SemaphoreType.DMA((local,)),
        ]

    def send(self, source, target, peer):
        index = len(self.copies)
        copy = remote(source, target, self.send_sem.at[index], self.recv_sem.at[index], peer)
        copy.start()
        self.copies.append(copy)
        return copy

    def store(self, source, start, count):
        piece = pl.ds(pl.multiple_of(start, count), count)
        copy = pltpu.make_async_copy(source, self.out.at[piece], self.local_sem.at[len(self.stores)])
        copy.start()
        self.stores.append(copy)
        width = min(256, self.turned.shape[0])

        def turn_part(index, carry):
            columns = pl.ds(pl.multiple_of(index * width, width), width)
            self.turned[columns, piece] = source[:, columns].T
            return carry

        lax.fori_loop(0, self.turned.shape[0] // width, turn_part, 0)
        turn_copy = pltpu.make_async_copy(
            self.turned.at[:, piece], self.turned_out.at[:, piece], self.turned_sem.at[len(self.turns)]
        )
        turn_copy.start()
        self.turns.append(turn_copy)

    def quarters(self):
        quarter = self.rows // 4
        return [pl.ds(index * quarter, quarter) for index in range(4)]

    def start(self, stage):
        own, held = self.own, self.held
        if self.size != 4:
            if stage == 0:
                for peer in other_members("tensor", self.size):
                    self.send(own, held.at[self.me], peer)
            return
        beside, below, _ = square_peers(self.me)
        parts = self.quarters()
        upper, lower = parts[stage], parts[2 + stage]
        for part, peer in ((upper, beside), (lower, below), (lower, beside), (upper, below)):
            self.send(own.at[part], held.at[self.me, part], peer)

    def forward(self):
        own, held, rows = self.own, self.held, self.rows
        if self.size != 4:
            self.store(own, self.me * rows, rows)
            return
        beside, below, _ = square_peers(self.me)
        half = rows // 2
        self.store(own.at[pl.ds(0, half)], self.me * rows, half)
        self.store(own.at[pl.ds(half, half)], self.me * rows + half, half)
        parts = self.quarters()
        for stage in range(2):
            self.copies[4 * stage].wait_recv()
            self.send(held.at[beside, parts[stage]], held.at[beside, parts[stage]], below)
            self.copies[4 * stage + 1].wait_recv()
            self.send(held.at[below, parts[2 + stage]], held.at[below, parts[2 + stage]], beside)

    def finish(self):
        held, rows = self.held, self.rows
        if self.size != 4:
            for step, copy in enumerate(self.copies):
                copy.wait_recv()
                slot = lax.rem(self.me + self.size - step - 1, self.size)
                self.store(held.at[slot], slot * rows, rows)
        else:
            beside, below, across = square_peers(self.me)
            half = rows // 2
            first, second = pl.ds(0, half), pl.ds(half, half)
            self.store(held.at[beside, first], beside * rows, half)
            self.store(held.at[below, second], below * rows + half, half)
            for indices, slot, start in (
                ((2, 6), beside, half),
                ((3, 7), below, 0),
                ((8, 10), across, 0),
                ((9, 11), across, half),
            ):
                for index in indices:
                    self.copies[index].wait_recv()
                self.store(held.at[slot, pl.ds(start, half)], slot * rows + start, half)
        for copy in self.copies:
            copy.wait_send()
        for copy in self.stores + self.turns:
            copy.wait()


def gather_kernel(size, count, *refs):
    own_refs, out_refs, rest = refs[:count], refs[count : 3 * count], refs[3 * count :]
    greet(neighbours(size))
    gathers = [
        Gather(size, own_refs[k], *out_refs[2 * k : 2 * k + 2], *rest[6 * k : 6 * k + 6])
        for k in range(count)
    ]
    for gather in gathers:
        gather.start(0)
        gather.start(1)
        gather.forward()
    for gather in gathers:
        gather.finish()


def gather_rows(arrays, size, collective_id):
    count = len(arrays)
    rows, columns = arrays[0].shape
    scratch = []
    out_shape = []
    for _ in arrays:
        scratch += Gather.scratch(size, rows, columns)
        out_shape += [
            jax.ShapeDtypeStruct((size * rows, columns), jnp.bfloat16),
            jax.ShapeDtypeStruct((columns, size * rows), jnp.bfloat16),
        ]
    return pl.pallas_call(
        functools.partial(gather_kernel, size, count),
        out_shape=out_shape,
        in_specs=[pl.BlockSpec(memory_space=pltpu.VMEM)] * count,
        out_specs=[pl.BlockSpec(memory_space=pl.ANY)] * len(out_shape),
        scratch_shapes=scratch,
        compiler_params=pltpu.CompilerParams(
            collective_id=collective_id, has_side_effects=True, vmem_limit_bytes=VMEM_LIMIT
        ),
        cost_estimate=pl.CostEstimate(
            flops=0, bytes_accessed=count * 30 * size * rows * columns, transcendentals=0
        ),
        name="gather_rows",
    )(*arrays)


class Operand:
    def __init__(self, size, first_column, left_far, weight_far, left, weight, left_sem, weight_sem):
        self.left, self.weight = left, weight
        self.rows = left.shape[0] // size
        self.tile = min(512, weight.shape[0])
        self.far = left_far, weight_far
        self.first_column = first_column
        self.left_sem, self.weight_sem = left_sem, weight_sem

    @staticmethod
    def scratch(size, left, weight):
        width = left.shape[1]
        return [
            pltpu.VMEM(left.shape, left.dtype),
            pltpu.VMEM((weight.shape[0], width), weight.dtype),
            pltpu.SemaphoreType.DMA((size,)),
            pltpu.SemaphoreType.DMA((max(1, weight.shape[0] // 512),)),
        ]

    def left_copy(self, slot, owner):
        piece = pl.ds(pl.multiple_of(owner * self.rows, self.rows), self.rows)
        return pltpu.make_async_copy(self.far[0].at[piece], self.left.at[piece], self.left_sem.at[slot])

    def weight_copy(self, index):
        piece = pl.ds(pl.multiple_of(index * self.tile, self.tile), self.tile)
        columns = pl.ds(self.first_column, self.left.shape[1])
        return pltpu.make_async_copy(
            self.far[1].at[piece, columns], self.weight.at[piece], self.weight_sem.at[index]
        )


def block_product(operands, start, rows, fresh, write, after):
    total = operands[0].weight.shape[0]
    tile = operands[0].tile
    start = pl.multiple_of(start, rows)

    def step(index, carry):
        @pl.when(fresh)
        def _():
            for operand in operands:
                operand.weight_copy(index).wait()

        columns = pl.ds(pl.multiple_of(index * tile, tile), tile)
        values = None
        for operand in operands:
            part = times_transposed(
                operand.left[pl.ds(start, rows), :], operand.weight[columns, :]
            )
            values = part if values is None else values + part
        write(columns, values)
        after(index)
        return carry

    lax.fori_loop(0, total // tile, step, 0)


class Scatter:
    def __init__(self, size, outgoing, *rest):
        self.size, self.outgoing = size, outgoing
        if size == 4:
            self.passing, rest = rest[0], rest[1:]
        self.arriving, self.send_sem, self.recv_sem = rest
        self.rows = outgoing.shape[1]
        self.me = lax.axis_index("tensor")
        self.stages = 2 if size == 4 else 1
        self.plan()

    @staticmethod
    def scratch(size, rows, columns):
        if size == 4:
            sends = 10
            buffers = [
                pltpu.VMEM((4, rows, columns), jnp.bfloat16),
                pltpu.VMEM((2, rows // 2, columns), jnp.bfloat16),
                pltpu.VMEM((2, rows, columns), jnp.bfloat16),
            ]
        else:
            sends = size - 1
            buffers = [
                pltpu.VMEM((size, rows, columns), jnp.bfloat16),
                pltpu.VMEM((size - 1, rows, columns), jnp.bfloat16),
            ]
        return buffers + [pltpu.SemaphoreType.DMA((sends,)), pltpu.SemaphoreType.DMA((sends,))]

    def prepare(self, index, source, target, peer):
        return remote(source, target, self.send_sem.at[index], self.recv_sem.at[index], peer)

    def plan(self):
        outgoing, arriving = self.outgoing, self.arriving
        if self.size != 4:
            self.copies = [
                self.prepare(step, outgoing.at[step], arriving.at[step], peer)
                for step, peer in enumerate(other_members("tensor", self.size))
            ]
            self.early, self.starts = (), tuple((step, step) for step in range(self.size - 1))
            return
        beside, below, _ = square_peers(self.me)
        half, quarter = self.rows // 2, self.rows // 4
        first, second = pl.ds(0, half), pl.ds(half, half)
        middle = outgoing.shape[2] // 2
        left, right = pl.ds(0, middle), pl.ds(middle, middle)
        upper = [pl.ds(stage * quarter, quarter) for stage in range(2)]
        lower = [pl.ds(half + stage * quarter, quarter) for stage in range(2)]
        everything = pl.ds(0, half)
        self.copies = [
            self.prepare(0, outgoing.at[0, first, left], self.passing.at[0, everything, left], beside),
            self.prepare(1, outgoing.at[0, second, left], self.passing.at[1, everything, left], below),
            self.prepare(2, outgoing.at[0, first, right], self.passing.at[0, everything, right], beside),
            self.prepare(3, outgoing.at[0, second, right], self.passing.at[1, everything, right], below),
            self.prepare(4, outgoing.at[1, first], arriving.at[0, first], beside),
            self.prepare(5, outgoing.at[2, second], arriving.at[1, second], below),
            self.prepare(6, outgoing.at[1, lower[0]], arriving.at[0, lower[0]], beside),
            self.prepare(7, outgoing.at[2, upper[0]], arriving.at[1, upper[0]], below),
            self.prepare(8, outgoing.at[1, lower[1]], arriving.at[0, lower[1]], beside),
            self.prepare(9, outgoing.at[2, upper[1]], arriving.at[1, upper[1]], below),
        ]
        self.early, self.starts = (0, 1), ((0, 2), (0, 3), (1, 4), (2, 5))

    def owner(self, slot):
        if self.size != 4:
            return lax.rem(self.me + slot + 1, self.size)
        beside, below, across = square_peers(self.me)
        return jnp.where(
            slot == 0, across, jnp.where(slot == 1, beside, jnp.where(slot == 2, below, self.me))
        )

    def load(self, operands):
        tiles = operands[0].weight.shape[0] // operands[0].tile
        for operand in operands:
            operand.left_copy(0, self.owner(0)).start()
        for index in range(tiles):
            for operand in operands:
                operand.weight_copy(index).start()
        for slot in range(1, self.size):
            for operand in operands:
                operand.left_copy(slot, self.owner(slot)).start()

    def fill(self, operands, look=None, between=None):
        rows = self.rows

        def step(slot, carry):
            owner = self.owner(slot)
            for operand in operands:
                operand.left_copy(slot, owner).wait()

            def write(columns, values):
                self.outgoing[slot, :, columns] = values.astype(self.outgoing.dtype)
                if look is not None:
                    look(owner, columns, values)

            tiles = operands[0].weight.shape[0] // operands[0].tile

            def after(index):
                for early in self.early:
                    pl.when((slot == 0) & (index == max(tiles // 2, 1) - 1))(self.copies[early].start)

            block_product(operands, owner * rows, rows, slot == 0, write, after)
            for at, index in self.starts:
                pl.when(slot == at)(self.copies[index].start)
            if between is not None:
                pl.when(slot == 0)(between)
            return carry

        lax.fori_loop(0, self.size, step, 0)

    def relay(self):
        if self.size != 4:
            return
        half, quarter = self.rows // 2, self.rows // 4
        for stage in range(2):
            for arrivals, source, slot, start, onward in (
                ((1, 3), 1, 1, half, 6 + 2 * stage),
                ((0, 2), 0, 2, 0, 7 + 2 * stage),
            ):
                if stage == 0:
                    for index in arrivals:
                        self.copies[index].wait_recv()
                piece = pl.ds(start + stage * quarter, quarter)
                self.outgoing[slot, piece, :] = add_rounded(
                    self.outgoing[slot, piece, :],
                    self.passing[source, stage * quarter : (stage + 1) * quarter, :],
                )
                self.copies[onward].start()

    def collect(self, stage):
        if self.size != 4:
            for copy in self.copies:
                copy.wait_recv()
            return
        if stage == 0:
            self.copies[4].wait_recv()
            self.copies[5].wait_recv()
        self.copies[6 + 2 * stage].wait_recv()
        self.copies[7 + 2 * stage].wait_recv()

    def over_rows(self, stage, body):
        if self.size != 4:
            over_pieces(self.rows, body)
            return
        half, quarter = self.rows // 2, self.rows // 4
        over_pieces(quarter, body, stage * quarter)
        over_pieces(quarter, body, half + stage * quarter)

    def over_stages(self, body, done=None):
        for stage in range(self.stages):
            self.collect(stage)
            self.over_rows(stage, body)
            if done is not None:
                done(stage)

    def total(self, piece):
        total = self.outgoing[self.size - 1, piece, :].astype(jnp.float32)
        for index in range(self.arriving.shape[0]):
            total = total + self.arriving[index, piece, :].astype(jnp.float32)
        return total

    def drain(self):
        for copy in self.copies:
            copy.wait_send()


class Chain:
    def __init__(
        self, chips, steps, rising_refs, falling_refs, up_ref, down_ref,
        rise, fall, up, down, load_sem, send_sem, recv_sem,
    ):
        self.chips, self.steps = chips, steps
        self.rise, self.fall, self.up, self.down = rise, fall, up, down
        device = lax.axis_index("dp")
        self.chip = device // 2
        count = len(steps)
        self.loads = [
            pltpu.make_async_copy(source, target, load_sem.at[index])
            for index, (source, target) in enumerate(
                [(up_ref, up.at[0]), (down_ref, down.at[0])]
                + [(ref, rise.at[index]) for index, ref in enumerate(rising_refs)]
                + [(ref, fall.at[index]) for index, ref in enumerate(falling_refs)]
            )
        ]
        above = lax.rem(device + 2, 2 * chips)
        under = lax.rem(device + 2 * chips - 2, 2 * chips)
        self.neighbours = [("dp", above), ("dp", under)]
        self.rises = [
            remote(rise.at[i], up.at[i + 1], send_sem.at[i], recv_sem.at[i], above, "dp")
            for i in range(count)
        ]
        self.falls = [
            remote(
                fall.at[i], down.at[i + 1], send_sem.at[count + i], recv_sem.at[count + i], under, "dp"
            )
            for i in range(count)
        ]

    @staticmethod
    def scratch(count, rows, columns):
        return [
            pltpu.VMEM((count, rows, columns), jnp.bfloat16),
            pltpu.VMEM((count, rows, columns), jnp.bfloat16),
            pltpu.VMEM((count + 1, rows, columns), jnp.bfloat16),
            pltpu.VMEM((count + 1, rows, columns), jnp.bfloat16),
            pltpu.SemaphoreType.DMA((2 * count + 2,)),
            pltpu.SemaphoreType.DMA((2 * count,)),
            pltpu.SemaphoreType.DMA((2 * count,)),
        ]

    def load(self):
        for copy in self.loads:
            copy.start()

    def step(self, index):
        if index == 0:
            for copy in self.loads:
                copy.wait()
        step = self.steps[index]
        rows = self.rise.shape[1]
        sends_up = self.chip < step
        sends_down = self.chip >= self.chips - step

        @pl.when(sends_up & (self.chip > 0))
        def _():
            def add(piece):
                self.rise[index, piece, :] = add_rounded(
                    self.rise[index, piece, :], self.up[index, piece, :]
                )

            over_pieces(rows, add)

        pl.when(sends_up)(self.rises[index].start)

        @pl.when(sends_down & (self.chip < self.chips - 1))
        def _():
            def add(piece):
                self.fall[index, piece, :] = add_rounded(
                    self.fall[index, piece, :], self.down[index, piece, :]
                )

            over_pieces(rows, add)

        pl.when(sends_down)(self.falls[index].start)

    def arrives(self, index):
        step = self.steps[index]
        from_under = (self.chip > 0) & (self.chip <= step)
        from_above = (self.chip < self.chips - 1) & (self.chip >= self.chips - step - 1)
        return from_under, from_above

    def wait(self, index):
        from_under, from_above = self.arrives(index)
        pl.when(from_under)(self.rises[index].wait_recv)
        pl.when(from_above)(self.falls[index].wait_recv)

    def drain(self):
        for index, step in enumerate(self.steps):
            pl.when(self.chip < step)(self.rises[index].wait_send)
            pl.when(self.chip >= self.chips - step)(self.falls[index].wait_send)


def add_rounded(first, second):
    return (first.astype(jnp.float32) + second.astype(jnp.float32)).astype(jnp.bfloat16)


def over_pieces(rows, body, start=0):
    count = min(32, rows)

    def step(index, carry):
        body(pl.ds(pl.multiple_of(start + index * count, count), count))
        return carry

    lax.fori_loop(0, rows // count, step, 0)


def send_terms(axis, peers, source, landing, send_sem, recv_sem):
    me = lax.axis_index(axis)
    landing[me] = source[...]
    copies = []
    for step, peer in enumerate(peers):
        copy = remote(source, landing.at[me], send_sem.at[step], recv_sem.at[step], peer, axis)
        copy.start()
        copies.append(copy)
    return copies


def add_terms(landing, copies):
    for copy in copies:
        copy.wait_recv()
    total = landing[0]
    for index in range(1, landing.shape[0]):
        total = total + landing[index]
    return total


def split_operands(refs, size, first_columns):
    count = len(first_columns)
    far, refs, scratch = refs[: 2 * count], refs[2 * count : -4 * count], refs[-4 * count :]
    operands = [
        Operand(size, first, *far[2 * p : 2 * p + 2], *scratch[4 * p : 4 * p + 4])
        for p, first in enumerate(first_columns)
    ]
    return operands, refs


def store_row(target_ref, row_ref):
    width = target_ref.shape[1]
    for index in range(row_ref.shape[1] // width):
        target_ref[index : index + 1, :] = row_ref[:, index * width : (index + 1) * width]


def between_forward_kernel(size, first_columns, *refs):
    operands, refs = split_operands(refs, size, first_columns)
    input_ref, gain_ref, gathered_ref, turned_ref, state_ref, own_ref = refs[:6]
    buffers = 5 if size == 4 else 4
    scatter = Scatter(size, *refs[6 : 6 + buffers])
    gather = Gather(size, own_ref, gathered_ref, turned_ref, *refs[6 + buffers :])
    scatter.load(operands)
    greet(neighbours(size))
    scatter.fill(operands)
    scatter.relay()

    def norm(piece):
        state = input_ref[piece, :].astype(jnp.float32) + scatter.total(piece)
        state_ref[piece, :] = state
        own_ref[piece, :] = (state * row_scale(state) * gain_ref[...]).astype(own_ref.dtype)

    scatter.over_stages(norm, gather.start)
    gather.forward()
    gather.finish()
    scatter.drain()


def between_backward_kernel(size, chips, steps, first_columns, *refs):
    operands, refs = split_operands(refs, size, first_columns)
    state_ref, cotangent_ref, gain_ref = refs[:3]
    chain_count = 2 * len(steps) + 2
    chain_refs, last_refs, refs = refs[3 : 3 + chain_count], refs[3 + chain_count : 5 + chain_count], refs[5 + chain_count :]
    gathered_ref, gathered_turned_ref, slope_ref, term_ref, rising_ref, falling_ref = refs[:6]
    own_ref, sum_ref, last_sem = refs[6:9]
    buffers = 5 if size == 4 else 4
    scatter = Scatter(size, *refs[9 : 9 + buffers])
    gather = Gather(size, own_ref, gathered_ref, gathered_turned_ref, *refs[9 + buffers : 15 + buffers])
    chain = Chain(
        chips, steps, chain_refs[: len(steps)], chain_refs[len(steps) : -2], *chain_refs[-2:],
        *refs[15 + buffers :],
    )
    last_loads = [
        pltpu.make_async_copy(source, target, last_sem.at[index])
        for index, (source, target) in enumerate(zip(last_refs, (rising_ref, falling_ref)))
    ]
    chain.load()
    scatter.load(operands)
    for load in last_loads:
        load.start()
    greet(neighbours(size) + chain.neighbours)
    scatter.fill(operands, between=lambda: chain.step(0))
    scatter.relay()
    sum_ref[...] = jnp.zeros_like(sum_ref)

    def norm(piece):
        back = scatter.total(piece)
        state = state_ref[piece, :]
        scale = row_scale(state)
        unit = state * scale
        sum_ref[...] += jnp.sum(back * unit, axis=0, keepdims=True)
        unit_slope = back * gain_ref[...]
        slope = cotangent_ref[piece, :].astype(jnp.float32) + scale * (
            unit_slope - unit * jnp.mean(unit_slope * unit, axis=-1, keepdims=True)
        )
        slope_ref[piece, :] = slope
        own_ref[piece, :] = slope.astype(own_ref.dtype)

    scatter.over_stages(norm, gather.start)
    store_row(term_ref, sum_ref)
    gather.forward()
    chain.wait(0)
    for index in range(1, len(steps)):
        chain.step(index)
        chain.wait(index)
    for load in last_loads:
        load.wait()
    last = len(steps)
    for needed, landing, out_ref in (
        ((chain.chip > 0) & (chain.chip < chips - 1), chain.up, rising_ref),
        ((chain.chip > 0) & (chain.chip < chips - 1), chain.down, falling_ref),
    ):

        @pl.when(needed)
        def _(landing=landing, out_ref=out_ref):
            def add(piece):
                out_ref[piece, :] = add_rounded(out_ref[piece, :], landing[last, piece, :])

            over_pieces(out_ref.shape[0], add)

    gather.finish()
    scatter.drain()
    chain.drain()


def last_kernel(sizes, first_columns, *refs):
    data_size, size = sizes
    operands, refs = split_operands(refs, size, first_columns)
    input_ref, gain_ref, slope_ref, terms_ref, rows_ref = refs[:5]
    gradient_ref, terms_out_ref, sum_ref, partial_ref, group_ref, inner, outer = refs[5:12]
    inner_send, inner_recv, outer_send, outer_recv = refs[12:16]
    mixing = Scatter(size, *refs[16:])
    rows = gradient_ref.shape[0]
    mixing.load(operands)
    greet(
        [("tensor", peer) for peer in other_members("tensor", size)]
        + [("dp", peer) for peer in other_members("dp", data_size)]
    )
    sum_ref[...] = jnp.zeros_like(sum_ref)

    def look(owner, columns, values):
        piece = pl.ds(pl.multiple_of(owner * rows, rows), rows)
        sum_ref[:, columns] += jnp.sum(
            values * rows_ref[piece, columns].astype(jnp.float32), axis=0, keepdims=True
        )

    mixing.fill(operands, look)
    sum_ref[...] = sum_ref[...] / gain_ref[...]
    kept = partial_ref.shape[0] - terms_ref.shape[0]
    partial_ref[kept:, :] = terms_ref[...]
    store_row(partial_ref, sum_ref)
    inner_copies = send_terms(
        "tensor", other_members("tensor", size), partial_ref, inner, inner_send, inner_recv
    )
    mixing.relay()
    group_ref[...] = add_terms(inner, inner_copies)
    outer_copies = send_terms(
        "dp", other_members("dp", data_size), group_ref, outer, outer_send, outer_recv
    )
    terms_out_ref[...] = add_terms(outer, outer_copies)

    def norm(piece):
        back = mixing.total(piece)
        values = input_ref[piece, :].astype(jnp.float32)
        scale = row_scale(values)
        unit = values * scale
        unit_slope = back * gain_ref[...]
        gradient_ref[piece, :] = (
            slope_ref[piece, :]
            + scale * (unit_slope - unit * jnp.mean(unit_slope * unit, axis=-1, keepdims=True))
        ).astype(gradient_ref.dtype)

    mixing.over_stages(norm)
    for copy in inner_copies + outer_copies:
        copy.wait_send()
    mixing.drain()


def scatter_call(body, triples, size, others, far, outs, gathered, scratch, collective_id):
    far_spec = pl.BlockSpec(memory_space=pl.ANY)
    operands = [array for left, weight, _ in triples for array in (left, weight)]
    in_specs = [far_spec] * len(operands)
    for other in others:
        in_specs.append(pl.BlockSpec(other.shape, lambda i: (0, 0), pipeline_mode=pl.Buffered(1)))
    in_specs += [far_spec] * len(far)
    out_specs = [pl.BlockSpec(out.shape, lambda i: (0, 0)) for out in outs]
    if gathered:
        out_specs[:2] = [far_spec] * 2
    return pl.pallas_call(
        functools.partial(body, tuple(first for _, _, first in triples)),
        grid=(1,),
        out_shape=outs,
        in_specs=in_specs,
        out_specs=out_specs,
        scratch_shapes=list(scratch)
        + [part for left, weight, _ in triples for part in Operand.scratch(size, left, weight)],
        compiler_params=pltpu.CompilerParams(
            collective_id=collective_id, has_side_effects=True, vmem_limit_bytes=VMEM_LIMIT
        ),
        cost_estimate=pl.CostEstimate(
            flops=sum(2 * left.size * weight.shape[0] for left, weight, _ in triples),
            bytes_accessed=150_000_000,
            transcendentals=0,
        ),
    )(*operands, *others, *far)


LOG2E = 1.4426950408889634


def turn_tables(head_size):
    half_size = head_size // 2
    frequency = np.float32(rope_base) ** (
        -(np.arange(half_size, dtype=np.float32) * np.float32(2.0) / np.float32(head_size))
    )
    frequency = frequency.astype(np.float64)
    sign = np.concatenate([-np.ones(half_size), np.ones(half_size)])[None, :]
    positions = np.concatenate([np.arange(0, SEQUENCE_LENGTH, 128), np.arange(128)])
    angles = positions[:, None] * np.concatenate([frequency, frequency])[None, :]
    return np.cos(angles).astype(np.float32), (sign * np.sin(angles)).astype(np.float32)


def fill_tables(few_cosines_ref, few_sines_ref, cosine_ref, sine_ref):
    coarse = few_cosines_ref.shape[0] - 128
    near_cosine, near_sine = few_cosines_ref[coarse:, :], few_sines_ref[coarse:, :]

    def step(index, carry):
        far_cosine = few_cosines_ref[pl.ds(index, 1), :]
        far_sine = few_sines_ref[pl.ds(index, 1), :]
        rows = pl.ds(pl.multiple_of(index * 128, 128), 128)
        cosine_ref[rows, :] = far_cosine * near_cosine - far_sine * near_sine
        sine_ref[rows, :] = far_sine * near_cosine + far_cosine * near_sine
        return carry

    lax.fori_loop(0, coarse, step, 0)


def turn(values, cosine, sine):
    return values * cosine + pltpu.roll(values, values.shape[-1] // 2, 1) * sine


def turn_back(values, cosine, sine):
    return values * cosine - pltpu.roll(values, values.shape[-1] // 2, 1) * sine


def contract_first(first_operand, second_operand):
    return lax.dot_general(
        first_operand, second_operand, (((0,), (0,)), ((), ())), preferred_element_type=jnp.float32
    )


def visible_scores(key_rows, query_rows, first_row, multiplier):
    scores = times_transposed(key_rows, query_rows) * multiplier
    _, queries = scores.shape
    key_at = lax.broadcasted_iota(jnp.int32, (queries, queries), 0)
    query_at = lax.broadcasted_iota(jnp.int32, (queries, queries), 1)
    corner = jnp.where(query_at >= key_at, scores[first_row:], -1e30)
    if first_row == 0:
        return corner
    return jnp.concatenate([scores[:first_row], corner], axis=0)


def turn_heads(
    grouping, head_size, raw_ref, query_gain_ref, key_gain_ref, cosine_ref, sine_ref, query_ref, key_ref, value_ref
):
    def turned(start, gain):
        raw = raw_ref[:, pl.ds(start, head_size)]
        return turn(raw * row_scale(raw) * gain, cosine_ref[...], sine_ref[...]).astype(jnp.bfloat16)

    def step(part, carry):
        query_ref[part] = turned(pl.multiple_of(part * head_size, head_size), query_gain_ref[...])
        return carry

    lax.fori_loop(0, grouping, step, 0)
    key_ref[...] = turned(grouping * head_size, key_gain_ref[...])
    value_ref[...] = raw_ref[:, (grouping + 1) * head_size :].astype(jnp.bfloat16)


def attention_forward_kernel(
    grouping, head_size, block, rows_ref, weight_ref, few_cosines_ref, few_sines_ref, query_gain_ref, key_gain_ref,
    raw_ref, mixed_ref, total_ref, query_ref, key_ref, value_ref, cosine_ref, sine_ref,
):
    sequence = rows_ref.shape[0]
    multiplier = head_size ** (-0.5) * LOG2E

    @pl.when((pl.program_id(0) == 0) & (pl.program_id(1) == 0))
    def _():
        fill_tables(few_cosines_ref, few_sines_ref, cosine_ref, sine_ref)

    raw_ref[...] = simple_product(rows_ref[...], weight_ref[...])
    turn_heads(
        grouping, head_size, raw_ref, query_gain_ref, key_gain_ref, cosine_ref, sine_ref, query_ref, key_ref, value_ref
    )

    def head_step(part, carry):
        lanes = pl.ds(pl.multiple_of(part * head_size, head_size), head_size)
        for first_row in range(0, sequence, block):
            last_row = first_row + block
            scores = visible_scores(
                key_ref[:last_row, :], query_ref[part, first_row:last_row, :], first_row, multiplier
            )
            highest = jnp.max(scores, axis=0, keepdims=True)
            weights = jnp.exp2(scores - highest)
            total = jnp.sum(weights, axis=0, keepdims=True)
            weights = (weights * (1.0 / total)).astype(jnp.bfloat16)
            mixed_ref[first_row:last_row, lanes] = contract_first(
                weights, value_ref[:last_row, :]
            ).astype(mixed_ref.dtype)
            total_ref[0, pl.ds(part, 1), first_row:last_row] = highest + jnp.log2(total)
        return carry

    lax.fori_loop(0, grouping, head_step, 0)


def attention_forward(rows, weight, tables, query_gain, key_gain, heads, grouping):
    total_rows, depth = rows.shape
    head_size = query_gain.shape[0]
    sequences = total_rows // SEQUENCE_LENGTH
    width = (grouping + 2) * head_size
    block = min(256, SEQUENCE_LENGTH)
    table = pl.BlockSpec(tables[0].shape, lambda s, h: (0, 0))
    gain = pl.BlockSpec((1, head_size), lambda s, h: (0, 0))
    elements = heads * grouping * total_rows * SEQUENCE_LENGTH // 2
    return pl.pallas_call(
        functools.partial(attention_forward_kernel, grouping, head_size, block),
        grid=(sequences, heads),
        out_shape=[
            jax.ShapeDtypeStruct((total_rows, heads * width), jnp.float32),
            jax.ShapeDtypeStruct((total_rows, heads * grouping * head_size), jnp.bfloat16),
            jax.ShapeDtypeStruct((heads, grouping, total_rows), jnp.float32),
        ],
        in_specs=[
            pl.BlockSpec((SEQUENCE_LENGTH, depth), lambda s, h: (s, 0)),
            pl.BlockSpec((depth, width), lambda s, h: (0, h)),
            table,
            table,
            gain,
            gain,
        ],
        out_specs=[
            pl.BlockSpec((SEQUENCE_LENGTH, width), lambda s, h: (s, h)),
            pl.BlockSpec((SEQUENCE_LENGTH, grouping * head_size), lambda s, h: (s, h)),
            pl.BlockSpec((1, grouping, SEQUENCE_LENGTH), lambda s, h: (h, 0, s)),
        ],
        scratch_shapes=[
            pltpu.VMEM((grouping, SEQUENCE_LENGTH, head_size), jnp.bfloat16),
            pltpu.VMEM((SEQUENCE_LENGTH, head_size), jnp.bfloat16),
            pltpu.VMEM((SEQUENCE_LENGTH, head_size), jnp.bfloat16),
            pltpu.VMEM((SEQUENCE_LENGTH, head_size), jnp.float32),
            pltpu.VMEM((SEQUENCE_LENGTH, head_size), jnp.float32),
        ],
        compiler_params=pltpu.CompilerParams(vmem_limit_bytes=VMEM_LIMIT),
        cost_estimate=pl.CostEstimate(
            flops=2 * total_rows * depth * heads * width + 4 * elements * head_size,
            bytes_accessed=2 * (total_rows * depth + depth * heads * width),
            transcendentals=elements,
        ),
        name="attention_forward",
    )(rows, weight, *tables, query_gain.reshape(1, -1), key_gain.reshape(1, -1))


def norm_back(turned_slope, raw, gain, cosine, sine):
    norm_slope = turn_back(turned_slope, cosine, sine)
    scale = row_scale(raw)
    unit = raw * scale
    term = norm_slope * unit
    unit_slope = norm_slope * gain
    slope = scale * (unit_slope - unit * jnp.mean(unit_slope * unit, axis=-1, keepdims=True))
    return slope.astype(jnp.bfloat16), jnp.sum(term, axis=0, keepdims=True)


def attention_backward_kernel(size, grouping, head_size, block, first_columns, *refs):
    operands, refs = split_operands(refs, size, first_columns)
    (
        state_ref, weight_ref, raw_ref, mixed_ref, total_ref, few_cosines_ref, few_sines_ref,
        query_gain_ref, key_gain_ref, hidden_state_ref, slope_ref, gain_ref, output_ref,
        query_ref, key_ref, value_ref, out_slope_ref, turned_ref, key_sum_ref, value_sum_ref, cosine_ref, sine_ref,
    ) = refs[:22]
    scatter = Scatter(size, *refs[22:])
    step = pl.program_id(0) * pl.num_programs(1) + pl.program_id(1)
    steps = pl.num_programs(0) * pl.num_programs(1)

    @pl.when(step == 0)
    def _():
        scatter.load(operands)
        greet(neighbours(size))
        scatter.fill(operands)

    attend_backward_head(
        grouping, head_size, block, state_ref, weight_ref, raw_ref, mixed_ref, total_ref, few_cosines_ref,
        few_sines_ref, query_gain_ref, key_gain_ref, slope_ref, gain_ref, query_ref, key_ref, value_ref,
        out_slope_ref, turned_ref, key_sum_ref, value_sum_ref, cosine_ref, sine_ref,
    )

    @pl.when(step == 0)
    def _():
        scatter.relay()

    @pl.when(step == steps - 1)
    def _():
        def finish(piece):
            output_ref[piece, :] = (hidden_state_ref[piece, :] + scatter.total(piece)).astype(
                output_ref.dtype
            )

        scatter.over_stages(finish)
        scatter.drain()


def attend_backward_head(
    grouping, head_size, block, state_ref, weight_ref, raw_ref, mixed_ref, total_ref, few_cosines_ref, few_sines_ref,
    query_gain_ref, key_gain_ref, slope_ref, gain_ref, query_ref, key_ref, value_ref, out_slope_ref,
    turned_ref, key_sum_ref, value_sum_ref, cosine_ref, sine_ref,
):
    sequence = state_ref.shape[0]
    scale_factor = head_size ** (-0.5)
    multiplier = scale_factor * LOG2E

    @pl.when((pl.program_id(0) == 0) & (pl.program_id(1) == 0))
    def _():
        gain_ref[...] = jnp.zeros_like(gain_ref)
        fill_tables(few_cosines_ref, few_sines_ref, cosine_ref, sine_ref)

    out_slope_ref[...] = simple_product(state_ref[...], weight_ref[...]).astype(jnp.bfloat16)
    turn_heads(
        grouping, head_size, raw_ref, query_gain_ref, key_gain_ref, cosine_ref, sine_ref, query_ref, key_ref, value_ref
    )
    key_sum_ref[...] = jnp.zeros_like(key_sum_ref)
    value_sum_ref[...] = jnp.zeros_like(value_sum_ref)
    ones = jnp.ones((8, head_size), jnp.float32)

    def head_step(part, carry):
        lanes = pl.ds(pl.multiple_of(part * head_size, head_size), head_size)
        for first_row in range(0, sequence, block):
            last_row = first_row + block
            query_rows = query_ref[part, first_row:last_row, :]
            slope_rows = out_slope_ref[first_row:last_row, lanes]
            scores = visible_scores(key_ref[:last_row, :], query_rows, first_row, multiplier)
            weights = jnp.exp2(scores - total_ref[0, pl.ds(part, 1), first_row:last_row])
            value_sum_ref[:last_row, :] += simple_product(weights.astype(jnp.bfloat16), slope_rows)
            product = slope_rows.astype(jnp.float32) * mixed_ref[first_row:last_row, lanes].astype(jnp.float32)
            centre = lax.dot_general(
                ones,
                product,
                (((1,), (1,)), ((), ())),
                preferred_element_type=jnp.float32,
                precision=lax.Precision.HIGHEST,
            )[:1]
            weight_slope = times_transposed(value_ref[:last_row, :], slope_rows)
            score_slope = (weights * (weight_slope - centre)).astype(jnp.bfloat16)
            key_sum_ref[:last_row, :] += simple_product(score_slope, query_rows)
            turned_ref[first_row:last_row, :] = (
                contract_first(score_slope, key_ref[:last_row, :]) * scale_factor
            )
        slope, term = norm_back(
            turned_ref[...], raw_ref[:, lanes], query_gain_ref[...], cosine_ref[...], sine_ref[...]
        )
        slope_ref[:, lanes] = slope
        gain_ref[0:1, :] += term
        return carry

    lax.fori_loop(0, grouping, head_step, 0)
    lanes = slice(grouping * head_size, (grouping + 1) * head_size)
    slope, term = norm_back(
        key_sum_ref[...] * scale_factor, raw_ref[:, lanes], key_gain_ref[...], cosine_ref[...], sine_ref[...]
    )
    slope_ref[:, lanes] = slope
    gain_ref[1:2, :] += term
    slope_ref[:, (grouping + 1) * head_size :] = value_sum_ref[...].astype(jnp.bfloat16)


def attention_backward(
    state_rows, weight, weight_start, raw, mixed, totals, tables, query_gain, key_gain, heads, grouping,
    triples, hidden_state, size, collective_id,
):
    total_rows, depth = state_rows.shape
    head_size = query_gain.shape[0]
    sequences = total_rows // SEQUENCE_LENGTH
    width = (grouping + 2) * head_size
    out_width = grouping * head_size
    block = min(256, SEQUENCE_LENGTH)
    first_block = weight_start // out_width
    single = pl.Buffered(1)
    table = pl.BlockSpec(tables[0].shape, lambda s, h: (0, 0))
    gain = pl.BlockSpec((1, head_size), lambda s, h: (0, 0))
    elements = heads * grouping * total_rows * SEQUENCE_LENGTH // 2
    whole_rows = pltpu.VMEM((SEQUENCE_LENGTH, head_size), jnp.float32)
    operands = [array for left, other_weight, _ in triples for array in (left, other_weight)]
    in_specs = [pl.BlockSpec(memory_space=pl.ANY)] * len(operands)
    in_specs += [
        pl.BlockSpec((SEQUENCE_LENGTH, depth), lambda s, h: (s, 0), pipeline_mode=single),
        pl.BlockSpec((depth, out_width), lambda s, h: (0, first_block + h)),
        pl.BlockSpec((SEQUENCE_LENGTH, width), lambda s, h: (s, h)),
        pl.BlockSpec((SEQUENCE_LENGTH, out_width), lambda s, h: (s, h)),
        pl.BlockSpec((1, grouping, SEQUENCE_LENGTH), lambda s, h: (h, 0, s)),
        table,
        table,
        gain,
        gain,
        pl.BlockSpec(hidden_state.shape, lambda s, h: (0, 0), pipeline_mode=single),
    ]
    operands += [
        state_rows, weight, raw, mixed, totals, *tables, query_gain.reshape(1, -1), key_gain.reshape(1, -1),
        hidden_state,
    ]
    return pl.pallas_call(
        functools.partial(
            attention_backward_kernel, size, grouping, head_size, block,
            tuple(first for _, _, first in triples),
        ),
        grid=(sequences, heads),
        out_shape=[
            jax.ShapeDtypeStruct((total_rows, heads * width), jnp.bfloat16),
            jax.ShapeDtypeStruct((8, head_size), jnp.float32),
            jax.ShapeDtypeStruct(hidden_state.shape, jnp.bfloat16),
        ],
        in_specs=in_specs,
        out_specs=[
            pl.BlockSpec((SEQUENCE_LENGTH, width), lambda s, h: (s, h)),
            pl.BlockSpec((8, head_size), lambda s, h: (0, 0)),
            pl.BlockSpec(hidden_state.shape, lambda s, h: (0, 0)),
        ],
        scratch_shapes=[
            pltpu.VMEM((grouping, SEQUENCE_LENGTH, head_size), jnp.bfloat16),
            pltpu.VMEM((SEQUENCE_LENGTH, head_size), jnp.bfloat16),
            pltpu.VMEM((SEQUENCE_LENGTH, head_size), jnp.bfloat16),
            pltpu.VMEM((SEQUENCE_LENGTH, out_width), jnp.bfloat16),
            whole_rows,
            whole_rows,
            whole_rows,
            whole_rows,
            whole_rows,
            *Scatter.scratch(size, *hidden_state.shape),
            *[part for left, other, _ in triples for part in Operand.scratch(size, left, other)],
        ],
        compiler_params=pltpu.CompilerParams(
            collective_id=collective_id, has_side_effects=True, vmem_limit_bytes=VMEM_LIMIT
        ),
        cost_estimate=pl.CostEstimate(
            flops=2 * total_rows * depth * heads * out_width + 10 * elements * head_size,
            bytes_accessed=100_000_000,
            transcendentals=elements,
        ),
        name="attention_backward",
    )(*operands)


def feed_half_kernel(
    half, tile, block, rows_far, cotangent_far, weight_far, hidden_far, slope_far,
    rows_ref, cotangent_ref, weight_ref, hidden_ref, slope_ref, row_sem, weight_sem, out_sem,
):
    total = rows_ref.shape[0]
    blocks = total // block
    tiles = half // tile

    def row_copies(index):
        piece = pl.ds(pl.multiple_of(index * block, block), block)
        return [
            pltpu.make_async_copy(far.at[piece], ref.at[piece], row_sem.at[at, index])
            for at, (far, ref) in enumerate(((rows_far, rows_ref), (cotangent_far, cotangent_ref)))
        ]

    def weight_copies(index):
        copies = []
        for part in range(3):
            columns = pl.ds(pl.multiple_of(part * half + index * tile, tile), tile)
            copies.append(
                pltpu.make_async_copy(
                    weight_far.at[:, columns], weight_ref.at[part, index], weight_sem.at[part, index]
                )
            )
        return copies

    def out_copies(index):
        piece = pl.ds(pl.multiple_of(index * block, block), block)
        return [
            pltpu.make_async_copy(ref.at[piece], far.at[piece], out_sem.at[at, index])
            for at, (far, ref) in enumerate(((hidden_far, hidden_ref), (slope_far, slope_ref)))
        ]

    for copy in row_copies(0) + weight_copies(0):
        copy.start()
    for index in range(1, tiles):
        for copy in weight_copies(index):
            copy.start()
    for index in range(1, blocks):
        for copy in row_copies(index):
            copy.start()

    def row_step(row_index, carry):
        piece = pl.ds(pl.multiple_of(row_index * block, block), block)
        for copy in row_copies(row_index):
            copy.wait()

        def step(index, carry):
            @pl.when(row_index == 0)
            def _():
                for copy in weight_copies(index):
                    copy.wait()

            start = pl.multiple_of(index * tile, tile)
            rows = rows_ref[piece, :]
            gate = simple_product(rows, weight_ref[0, index])
            up = simple_product(rows, weight_ref[1, index])
            back = simple_product(cotangent_ref[piece, :], weight_ref[2, index])
            sigmoid = 1.0 / (1.0 + jnp.exp(-gate))
            gated = gate * sigmoid
            hidden_ref[piece, pl.ds(start, tile)] = (gated * up).astype(jnp.bfloat16)
            slope_ref[piece, pl.ds(start, tile)] = (
                back * up * sigmoid * (1.0 + gate * (1.0 - sigmoid))
            ).astype(jnp.bfloat16)
            slope_ref[piece, pl.ds(half + start, tile)] = (back * gated).astype(jnp.bfloat16)
            return carry

        lax.fori_loop(0, tiles, step, 0)
        for copy in out_copies(row_index):
            copy.start()
        return carry

    lax.fori_loop(0, blocks, row_step, 0)
    for index in range(blocks):
        for copy in out_copies(index):
            copy.wait()


def feed_half(rows, cotangent, weight):
    total_rows, depth = rows.shape
    block = min(512, total_rows)
    half = weight.shape[1] // 3
    tile = 256 if half % 256 == 0 else 128
    blocks, tiles = total_rows // block, half // tile
    far = pl.BlockSpec(memory_space=pl.ANY)
    return pl.pallas_call(
        functools.partial(feed_half_kernel, half, tile, block),
        out_shape=[
            jax.ShapeDtypeStruct((total_rows, half), jnp.bfloat16),
            jax.ShapeDtypeStruct((total_rows, 2 * half), jnp.bfloat16),
        ],
        in_specs=[far] * 3,
        out_specs=[far] * 2,
        scratch_shapes=[
            pltpu.VMEM(rows.shape, rows.dtype),
            pltpu.VMEM(rows.shape, rows.dtype),
            pltpu.VMEM((3, tiles, depth, tile), weight.dtype),
            pltpu.VMEM((total_rows, half), jnp.bfloat16),
            pltpu.VMEM((total_rows, 2 * half), jnp.bfloat16),
            pltpu.SemaphoreType.DMA((2, blocks)),
            pltpu.SemaphoreType.DMA((3, tiles)),
            pltpu.SemaphoreType.DMA((2, blocks)),
        ],
        compiler_params=pltpu.CompilerParams(vmem_limit_bytes=VMEM_LIMIT),
        cost_estimate=pl.CostEstimate(
            flops=6 * total_rows * depth * half,
            bytes_accessed=2 * (2 * total_rows * depth + 3 * depth * half),
            transcendentals=total_rows * half,
        ),
        name="feed_half",
    )(rows, cotangent, weight)


def grad_kernel(pair_count, *refs):
    pairs = [refs[2 * p : 2 * p + 2] for p in range(pair_count)]
    out_ref = refs[-1]
    start = 0
    for left_ref, right_ref in pairs:
        width = right_ref.shape[1]
        tile = next(t for t in (768, 512, 384, 256, 128) if width % t == 0)
        for column in range(0, width, tile):
            values = simple_product(left_ref[...], right_ref[:, column : column + tile])
            out_ref[:, start + column : start + column + tile] = values.astype(jnp.bfloat16)
        start += width


def grad_blocks(pairs, rows):
    depth, total_rows = pairs[0][0].shape
    width = sum(right.shape[1] for _, right in pairs)
    in_specs = []
    operands = []
    for left, right in pairs:
        in_specs += [
            pl.BlockSpec((rows, total_rows), lambda k: (k, 0)),
            pl.BlockSpec(right.shape, lambda k: (0, 0), pipeline_mode=pl.Buffered(1)),
        ]
        operands += [left, right]
    return pl.pallas_call(
        functools.partial(grad_kernel, len(pairs)),
        grid=(depth // rows,),
        in_specs=in_specs,
        out_specs=pl.BlockSpec((rows, width), lambda k: (k, 0)),
        out_shape=jax.ShapeDtypeStruct((depth, width), jnp.bfloat16),
        compiler_params=pltpu.CompilerParams(vmem_limit_bytes=VMEM_LIMIT),
        cost_estimate=pl.CostEstimate(
            flops=2 * total_rows * depth * width,
            bytes_accessed=2 * (total_rows * depth * len(pairs) + width * (total_rows + depth)),
            transcendentals=0,
        ),
        name="grad_blocks",
    )(*operands)


def pair_grad_kernel(chips, pair_count, *refs):
    lefts, rights = refs[:pair_count], refs[pair_count : 2 * pair_count]
    out_refs = refs[2 * pair_count : 2 * pair_count + chips]
    held = refs[2 * pair_count + chips : -6]
    sent, landed, left_sem, send_sem, recv_sem, out_sem = refs[-6:]
    block = sent.shape[1]
    device = lax.axis_index("dp")
    chip, core = device // 2, lax.rem(device, 2)
    other = chip * 2 + 1 - core

    def loads(index):
        owner = lax.rem(chip + lax.rem(index, chips), chips) * 2
        owner = owner + jnp.where(index < chips, 1 - core, core)
        piece = pl.ds(pl.multiple_of(owner * block, block), block)
        slot = lax.rem(index, 2)
        return [
            pltpu.make_async_copy(left.at[piece], hold.at[slot], left_sem.at[at, slot])
            for at, (left, hold) in enumerate(zip(lefts, held))
        ]

    for load in loads(0):
        load.start()
    greet([("dp", other)])
    copies = [
        pltpu.make_async_remote_copy(
            src_ref=sent.at[place],
            dst_ref=landed.at[place],
            send_sem=send_sem.at[place],
            recv_sem=recv_sem.at[place],
            device_id={"dp": other},
            device_id_type=MESH,
        )
        for place in range(chips)
    ]

    def products(index, write):
        slot = lax.rem(index, 2)
        for load in loads(index):
            load.wait()

        @pl.when(index + 1 < 2 * chips)
        def _():
            for load in loads(index + 1):
                load.start()

        start = 0
        for hold, right in zip(held, rights):
            width = right.shape[1]
            tile = next(t for t in (512, 384, 256, 128) if width % t == 0)

            def step(at, carry, hold=hold, right=right, start=start, tile=tile):
                column = pl.multiple_of(at * tile, tile)
                write(
                    pl.ds(start + column, tile),
                    simple_product(hold[slot], right[:, pl.ds(column, tile)]),
                )
                return carry

            lax.fori_loop(0, width // tile, step, 0)
            start += width

    def send_step(place, carry):
        def write(columns, values):
            sent[place, :, columns] = values.astype(jnp.bfloat16)

        products(place, write)
        for at in range(chips):
            pl.when(place == at)(copies[at].start)
        return carry

    lax.fori_loop(0, chips, send_step, 0)
    outs = [
        pltpu.make_async_copy(landed.at[place], out_ref, out_sem.at[place])
        for place, out_ref in enumerate(out_refs)
    ]

    def own_step(place, carry):
        for at in range(chips):
            pl.when(place == at)(copies[at].wait_recv)

        def write(columns, values):
            landed[place, :, columns] = (
                values + landed[place, :, columns].astype(jnp.float32)
            ).astype(jnp.bfloat16)

        products(place + chips, write)
        for at in range(chips):
            pl.when(place == at)(outs[at].start)
        return carry

    lax.fori_loop(0, chips, own_step, 0)
    for copy in copies:
        copy.wait_send()
    for copy in outs:
        copy.wait()


def pair_grads(pairs, sizes, collective_id):
    chips = sizes[0] // 2
    depth, total_rows = pairs[0][0].shape
    block = depth // sizes[0]
    width = sum(right.shape[1] for _, right in pairs)
    far = pl.BlockSpec(memory_space=pl.ANY)
    return pl.pallas_call(
        functools.partial(pair_grad_kernel, chips, len(pairs)),
        out_shape=[jax.ShapeDtypeStruct((block, width), jnp.bfloat16)] * chips,
        in_specs=[far] * len(pairs) + [pl.BlockSpec(memory_space=pltpu.VMEM)] * len(pairs),
        out_specs=[far] * chips,
        scratch_shapes=[pltpu.VMEM((2, block, total_rows), jnp.bfloat16) for _ in pairs]
        + [
            pltpu.VMEM((chips, block, width), jnp.bfloat16),
            pltpu.VMEM((chips, block, width), jnp.bfloat16),
            pltpu.SemaphoreType.DMA((len(pairs), 2)),
            pltpu.SemaphoreType.DMA((chips,)),
            pltpu.SemaphoreType.DMA((chips,)),
            pltpu.SemaphoreType.DMA((chips,)),
        ],
        compiler_params=pltpu.CompilerParams(
            collective_id=collective_id, has_side_effects=True, vmem_limit_bytes=VMEM_LIMIT
        ),
        cost_estimate=pl.CostEstimate(
            flops=2 * total_rows * depth * width,
            bytes_accessed=2 * (total_rows * depth * len(pairs) + width * (total_rows + depth)),
            transcendentals=0,
        ),
        name="pair_grads",
    )(*[left for left, _ in pairs], *[right for _, right in pairs])


def reduce_over_chips(pairs, sizes, collective_id):
    data_size = sizes[0]
    chips = data_size // 2
    blocks = pair_grads(pairs, sizes, collective_id)
    up = lax.ppermute(blocks[chips - 1], "dp", [(device, device + 2) for device in range(2)])
    down = lax.ppermute(
        blocks[1],
        "dp",
        [(device, device - 2) for device in range(data_size - 2, data_size)],
    )
    return blocks, up, down


def pack_mixing_kernel(heads, query_ref, key_ref, value_ref, output_ref, out_ref):
    query_width = query_ref.shape[1] // heads
    head_size = key_ref.shape[1] // heads
    start = 0
    for head in range(heads):
        for ref, part in ((query_ref, query_width), (key_ref, head_size), (value_ref, head_size)):
            out_ref[:, start : start + part] = ref[:, head * part : (head + 1) * part]
            start += part
    out_ref[:, start:] = output_ref[...].T


def pack_feed_kernel(gate_ref, up_ref, down_ref, first_ref, second_ref):
    start = 0
    for out_ref in (first_ref, second_ref):
        width = out_ref.shape[1] // 3
        part = slice(start, start + width)
        out_ref[:, :width] = gate_ref[:, part]
        out_ref[:, width : 2 * width] = up_ref[:, part]
        out_ref[:, 2 * width :] = down_ref[part, :].T
        start += width


def finish_kernel(
    heads, own_ref, up_ref, down_ref, second_ref, mixing_ref, output_total_ref, terms_ref, output_rows_ref, input_rows_ref,
    output_rows_out, input_rows_out, attention_term_out, query_out, key_out, value_out, query_gain_out, key_gain_out,
    output_out, feed_term_out, gate_out, up_out, down_out,
):
    output_rows_out[...] = output_rows_ref[...]
    input_rows_out[...] = input_rows_ref[...]
    count = attention_term_out.shape[0]
    attention_term_out[...] = terms_ref[:count, :]
    feed_term_out[...] = terms_ref[count : 2 * count, :]
    query_gain_out[...] = terms_ref[2 * count : 2 * count + 1, :]
    key_gain_out[...] = terms_ref[2 * count + 1 : 2 * count + 2, :]
    start = 0
    for total_refs in ((own_ref, up_ref, down_ref), (second_ref,)):
        width = total_refs[0].shape[1] // 3
        part = slice(start, start + width)

        def total(index):
            columns = slice(index * width, (index + 1) * width)
            return sum(ref[:, columns].astype(jnp.float32) for ref in total_refs)

        gate_out[:, part] = total(0)
        up_out[:, part] = total(1)
        down_out[part, :] = total(2).T
        start += width
    query_width = query_out.shape[1] // heads
    head_size = key_out.shape[1] // heads
    start = 0
    for head in range(heads):
        for out, part in ((query_out, query_width), (key_out, head_size), (value_out, head_size)):
            out[:, head * part : (head + 1) * part] = mixing_ref[:, start : start + part].astype(
                jnp.float32
            )
            start += part
    output_out[...] = output_total_ref[...].astype(jnp.float32).T


def whole_call(body, shapes, *operands):
    return pl.pallas_call(
        body,
        out_shape=shapes,
        in_specs=[pl.BlockSpec(memory_space=pltpu.VMEM)] * len(operands),
        out_specs=[pl.BlockSpec(memory_space=pltpu.VMEM)] * len(shapes),
        compiler_params=pltpu.CompilerParams(vmem_limit_bytes=VMEM_LIMIT),
        cost_estimate=pl.CostEstimate(
            flops=0, bytes_accessed=4 * sum(operand.size for operand in operands), transcendentals=0
        ),
    )(*operands)


def per_device(
    block_input,
    attention_gain,
    query_weight,
    key_matrix,
    value_matrix,
    query_gain,
    key_gain,
    output_weight,
    feed_gain,
    gate_weight,
    up_weight,
    down_weight,
    out_cotangent,
):
    size = lax.axis_size("tensor")
    sizes = (lax.axis_size("dp"), size)
    model_width = block_input.shape[1]
    head_size = query_gain.shape[0]
    query_columns = query_weight.shape[1]
    key_columns = key_matrix.shape[1]
    heads = key_columns // head_size
    grouping = query_columns // key_columns
    hidden_columns = gate_weight.shape[1]
    qkv_columns = query_columns + 2 * key_columns
    first_columns = hidden_columns * 2 // 3 // 256 * 256 or hidden_columns // 2
    second_columns = hidden_columns - first_columns
    tables = turn_tables(head_size)

    block_width = query_weight.shape[0]
    (mixing_local,) = whole_call(
        functools.partial(pack_mixing_kernel, heads),
        [jax.ShapeDtypeStruct((block_width, qkv_columns + query_columns), jnp.bfloat16)],
        query_weight, key_matrix, value_matrix, output_weight,
    )
    mixing_full = lax.all_gather(mixing_local, "dp", axis=0, tiled=True)
    feed_locals = whole_call(
        pack_feed_kernel,
        [
            jax.ShapeDtypeStruct((block_width, 3 * columns), jnp.bfloat16)
            for columns in (first_columns, second_columns)
        ],
        gate_weight, up_weight, down_weight,
    )
    feed_full = [lax.all_gather(part, "dp", axis=0, tiled=True) for part in feed_locals]

    input_float = block_input.astype(jnp.float32)
    first_scale = row_scale(input_float)
    first_unit = input_float * first_scale
    mixer_local = (first_unit * attention_gain).astype(jnp.bfloat16)
    mixer_rows, mixer_turned, cotangent_rows, cotangent_turned = gather_rows(
        (mixer_local, out_cotangent), size, 0
    )

    raw, mixed_rows, totals = attention_forward(
        mixer_rows, mixing_full, tables, query_gain, key_gain, heads, grouping
    )
    local_shape = block_input.shape
    local_rows = local_shape[0]
    gain_rows = model_width // head_size
    gathered_shapes = [
        jax.ShapeDtypeStruct((size * local_rows, model_width), jnp.bfloat16),
        jax.ShapeDtypeStruct((model_width, size * local_rows), jnp.bfloat16),
    ]
    local_float = jax.ShapeDtypeStruct(local_shape, jnp.float32)
    local_half = jax.ShapeDtypeStruct(local_shape, jnp.bfloat16)
    row_sum = pltpu.VMEM((1, model_width), jnp.float32)
    own_rows = pltpu.VMEM(local_shape, jnp.bfloat16)
    scatter_scratch = Scatter.scratch(size, *local_shape)
    gather_scratch = Gather.scratch(size, *local_shape)
    feed_rows, feed_turned, hidden_state = scatter_call(
        functools.partial(between_forward_kernel, size),
        [(mixed_rows, mixing_full, qkv_columns)],
        size,
        [block_input, feed_gain.reshape(1, -1)],
        [],
        [*gathered_shapes, local_float],
        True,
        [own_rows, *scatter_scratch, *gather_scratch],
        1,
    )

    hidden_first, slope_first = feed_half(feed_rows, cotangent_rows, feed_full[0])
    blocks, up, down = reduce_over_chips(
        [(feed_turned, slope_first), (cotangent_turned, hidden_first)], sizes, 5
    )
    blocks, later_full = lax.optimization_barrier((blocks, feed_full[1]))
    hidden_second, slope_second = feed_half(feed_rows, cotangent_rows, later_full)
    second_grad = grad_blocks(
        [(feed_turned, slope_second), (cotangent_turned, hidden_second)], 2 * block_width
    )
    second_grad, slope_second = lax.optimization_barrier((second_grad, slope_second))
    second_total = lax.psum_scatter(second_grad, "dp", scatter_dimension=0, tiled=True)
    chips = sizes[0] // 2
    middle_steps = tuple(range(2, chips - 1))
    chain_block = jax.ShapeDtypeStruct(blocks[0].shape, jnp.bfloat16)
    state_rows, state_turned, state_slope, feed_term, rising, falling = scatter_call(
        functools.partial(between_backward_kernel, size, chips, middle_steps),
        [(slope_first, feed_full[0], 0), (slope_second, later_full, 0)],
        size,
        [hidden_state, out_cotangent, feed_gain.reshape(1, -1)],
        [blocks[chips - step] for step in middle_steps]
        + [blocks[step] for step in middle_steps]
        + [up, down, blocks[1], blocks[chips - 1]],
        [
            *gathered_shapes,
            local_float,
            jax.ShapeDtypeStruct((gain_rows, head_size), jnp.float32),
            chain_block,
            chain_block,
        ],
        True,
        [
            own_rows,
            row_sum,
            pltpu.SemaphoreType.DMA((2,)),
            *scatter_scratch,
            *gather_scratch,
            *Chain.scratch(len(middle_steps), *blocks[0].shape),
        ],
        2,
    )
    up = lax.ppermute(
        rising, "dp", [(device, device + 2) for device in range(sizes[0] - 2)]
    )
    down = lax.ppermute(
        falling, "dp", [(device, device - 2) for device in range(2, sizes[0])]
    )
    output_grad = grad_blocks([(state_turned, mixed_rows)], 4 * block_width)
    output_grad, state_rows = lax.optimization_barrier((output_grad, state_rows))
    output_total = lax.psum_scatter(output_grad, "dp", scatter_dimension=0, tiled=True)
    qkv_slope, head_terms, block_output = attention_backward(
        state_rows, mixing_full, qkv_columns, raw, mixed_rows, totals, tables,
        query_gain, key_gain, heads, grouping,
        [
            (hidden_first, feed_full[0], 2 * first_columns),
            (hidden_second, later_full, 2 * second_columns),
        ],
        hidden_state, size, 4,
    )
    mixing_grad = grad_blocks([(mixer_turned, qkv_slope)], 2 * block_width)
    mixing_grad, qkv_slope = lax.optimization_barrier((mixing_grad, qkv_slope))
    mixing_total = lax.psum_scatter(mixing_grad, "dp", scatter_dimension=0, tiled=True)
    terms_shape = (2 * gain_rows + head_terms.shape[0], head_size)
    input_gradient, terms = scatter_call(
        functools.partial(last_kernel, sizes),
        [(qkv_slope, mixing_full, 0)],
        size,
        [
            block_input,
            attention_gain.reshape(1, -1),
            state_slope,
            jnp.concatenate([feed_term, head_terms], axis=0),
            mixer_rows,
        ],
        [],
        [local_half, jax.ShapeDtypeStruct(terms_shape, jnp.float32)],
        False,
        [
            row_sum,
            pltpu.VMEM(terms_shape, jnp.float32),
            pltpu.VMEM(terms_shape, jnp.float32),
            pltpu.VMEM((size, *terms_shape), jnp.float32),
            pltpu.VMEM((sizes[0], *terms_shape), jnp.float32),
            *[pltpu.SemaphoreType.DMA((count - 1,)) for count in (size, size, *sizes[:1] * 2)],
            *scatter_scratch,
        ],
        3,
    )

    def whole_float(*shape):
        return jax.ShapeDtypeStruct(shape, jnp.float32)

    outs = whole_call(
        functools.partial(finish_kernel, heads),
        [
            local_half,
            local_half,
            whole_float(gain_rows, head_size),
            whole_float(block_width, query_columns),
            whole_float(block_width, key_columns),
            whole_float(block_width, key_columns),
            whole_float(1, head_size),
            whole_float(1, head_size),
            whole_float(query_columns, block_width),
            whole_float(gain_rows, head_size),
            whole_float(block_width, hidden_columns),
            whole_float(block_width, hidden_columns),
            whole_float(hidden_columns, block_width),
        ],
        blocks[0], up, down, second_total, mixing_total, output_total, terms, block_output, input_gradient,
    )
    return tuple(
        out.reshape(-1) if index in (2, 6, 7, 9) else out for index, out in enumerate(outs)
    )


def solution(mesh):
    in_specs = (
        P(("dp", "tensor"), None),
        P(),
        P("dp", "tensor"),
        P("dp", "tensor"),
        P("dp", "tensor"),
        P(),
        P(),
        P("tensor", "dp"),
        P(),
        P("dp", "tensor"),
        P("dp", "tensor"),
        P("tensor", "dp"),
        P(("dp", "tensor"), None),
    )
    out_specs = (
        P(("dp", "tensor"), None),
        P(("dp", "tensor"), None),
        P(),
        P("dp", "tensor"),
        P("dp", "tensor"),
        P("dp", "tensor"),
        P(),
        P(),
        P("tensor", "dp"),
        P(),
        P("dp", "tensor"),
        P("dp", "tensor"),
        P("tensor", "dp"),
    )

    return jax.shard_map(per_device, mesh=mesh, in_specs=in_specs, out_specs=out_specs, check_vma=False)
```

```python
import functools

import jax
import jax.numpy as jnp
import numpy as np
from jax import lax
from jax.experimental import pallas as pl
from jax.experimental.pallas import tpu as pltpu
from jax.sharding import PartitionSpec as P


SEQUENCE_LENGTH = 1024

epsilon = 1e-06
rope_base = 1000000.0


MESH = pl.DeviceIdType.MESH
VMEM_LIMIT = 62 * 1024 * 1024


def row_scale(values):
    return lax.rsqrt(jnp.mean(values * values, axis=-1, keepdims=True) + epsilon)


def times_transposed(first_operand, second_operand):
    return lax.dot_general(
        first_operand, second_operand, (((1,), (1,)), ((), ())), preferred_element_type=jnp.float32
    )


def simple_product(first_operand, second_operand):
    return jnp.dot(first_operand, second_operand, preferred_element_type=jnp.float32)


def remote(source, target, send_sem, recv_sem, peer, axis="tensor"):
    return pltpu.make_async_remote_copy(
        src_ref=source,
        dst_ref=target,
        send_sem=send_sem,
        recv_sem=recv_sem,
        device_id={axis: peer},
        device_id_type=MESH,
    )


def greet(peers):
    barrier = pltpu.get_barrier_semaphore()
    for axis, peer in peers:
        pl.semaphore_signal(barrier, inc=1, device_id={axis: peer}, device_id_type=MESH)
    pl.semaphore_wait(barrier, len(peers))


def square_peers(me):
    column = lax.rem(me, 2)
    row = me // 2
    return row * 2 + (1 - column), (1 - row) * 2 + column, (1 - row) * 2 + (1 - column)


def neighbours(size):
    if size == 4:
        beside, below, _ = square_peers(lax.axis_index("tensor"))
        return [("tensor", beside), ("tensor", below)]
    return [("tensor", peer) for peer in other_members("tensor", size)]


def other_members(axis, count):
    me = lax.axis_index(axis)
    return [lax.rem(me + step, count) for step in range(1, count)]


class Gather:
    def __init__(
        self, size, own_ref, out_ref, turned_out_ref, held_ref, turned_ref, send_sem, recv_sem, local_sem, turned_sem
    ):
        self.size, self.own, self.out, self.held = size, own_ref, out_ref, held_ref
        self.turned_out, self.turned = turned_out_ref, turned_ref
        self.send_sem, self.recv_sem, self.local_sem = send_sem, recv_sem, local_sem
        self.turned_sem = turned_sem
        self.me = lax.axis_index("tensor")
        self.rows = own_ref.shape[0]
        self.copies, self.stores, self.turns = [], [], []

    @staticmethod
    def scratch(size, rows, columns):
        sends, local = (12, 8) if size == 4 else (size - 1, size)
        return [
            pltpu.VMEM((size, rows, columns), jnp.bfloat16),
            pltpu.VMEM((columns, size * rows), jnp.bfloat16),
            pltpu.SemaphoreType.DMA((sends,)),
            pltpu.SemaphoreType.DMA((sends,)),
            pltpu.SemaphoreType.DMA((local,)),
            pltpu.SemaphoreType.DMA((local,)),
        ]

    def send(self, source, target, peer):
        index = len(self.copies)
        copy = remote(source, target, self.send_sem.at[index], self.recv_sem.at[index], peer)
        copy.start()
        self.copies.append(copy)
        return copy

    def store(self, source, start, count):
        piece = pl.ds(pl.multiple_of(start, count), count)
        copy = pltpu.make_async_copy(source, self.out.at[piece], self.local_sem.at[len(self.stores)])
        copy.start()
        self.stores.append(copy)
        width = min(256, self.turned.shape[0])

        def turn_part(index, carry):
            columns = pl.ds(pl.multiple_of(index * width, width), width)
            self.turned[columns, piece] = source[:, columns].T
            return carry

        lax.fori_loop(0, self.turned.shape[0] // width, turn_part, 0)
        turn_copy = pltpu.make_async_copy(
            self.turned.at[:, piece], self.turned_out.at[:, piece], self.turned_sem.at[len(self.turns)]
        )
        turn_copy.start()
        self.turns.append(turn_copy)

    def quarters(self):
        quarter = self.rows // 4
        return [pl.ds(index * quarter, quarter) for index in range(4)]

    def start(self, stage):
        own, held = self.own, self.held
        if self.size != 4:
            if stage == 0:
                for peer in other_members("tensor", self.size):
                    self.send(own, held.at[self.me], peer)
            return
        beside, below, _ = square_peers(self.me)
        parts = self.quarters()
        upper, lower = parts[stage], parts[2 + stage]
        for part, peer in ((upper, beside), (lower, below), (lower, beside), (upper, below)):
            self.send(own.at[part], held.at[self.me, part], peer)

    def forward(self):
        own, held, rows = self.own, self.held, self.rows
        if self.size != 4:
            self.store(own, self.me * rows, rows)
            return
        beside, below, _ = square_peers(self.me)
        half = rows // 2
        self.store(own.at[pl.ds(0, half)], self.me * rows, half)
        self.store(own.at[pl.ds(half, half)], self.me * rows + half, half)
        parts = self.quarters()
        for stage in range(2):
            self.copies[4 * stage].wait_recv()
            self.send(held.at[beside, parts[stage]], held.at[beside, parts[stage]], below)
            self.copies[4 * stage + 1].wait_recv()
            self.send(held.at[below, parts[2 + stage]], held.at[below, parts[2 + stage]], beside)

    def finish(self):
        held, rows = self.held, self.rows
        if self.size != 4:
            for step, copy in enumerate(self.copies):
                copy.wait_recv()
                slot = lax.rem(self.me + self.size - step - 1, self.size)
                self.store(held.at[slot], slot * rows, rows)
        else:
            beside, below, across = square_peers(self.me)
            half = rows // 2
            first, second = pl.ds(0, half), pl.ds(half, half)
            self.store(held.at[beside, first], beside * rows, half)
            self.store(held.at[below, second], below * rows + half, half)
            for indices, slot, start in (
                ((2, 6), beside, half),
                ((3, 7), below, 0),
                ((8, 10), across, 0),
                ((9, 11), across, half),
            ):
                for index in indices:
                    self.copies[index].wait_recv()
                self.store(held.at[slot, pl.ds(start, half)], slot * rows + start, half)
        for copy in self.copies:
            copy.wait_send()
        for copy in self.stores + self.turns:
            copy.wait()


def gather_kernel(size, count, *refs):
    own_refs, out_refs, rest = refs[:count], refs[count : 3 * count], refs[3 * count :]
    greet(neighbours(size))
    gathers = [
        Gather(size, own_refs[k], *out_refs[2 * k : 2 * k + 2], *rest[6 * k : 6 * k + 6])
        for k in range(count)
    ]
    for gather in gathers:
        gather.start(0)
        gather.start(1)
        gather.forward()
    for gather in gathers:
        gather.finish()


def gather_rows(arrays, size, collective_id):
    count = len(arrays)
    rows, columns = arrays[0].shape
    scratch = []
    out_shape = []
    for _ in arrays:
        scratch += Gather.scratch(size, rows, columns)
        out_shape += [
            jax.ShapeDtypeStruct((size * rows, columns), jnp.bfloat16),
            jax.ShapeDtypeStruct((columns, size * rows), jnp.bfloat16),
        ]
    return pl.pallas_call(
        functools.partial(gather_kernel, size, count),
        out_shape=out_shape,
        in_specs=[pl.BlockSpec(memory_space=pltpu.VMEM)] * count,
        out_specs=[pl.BlockSpec(memory_space=pl.ANY)] * len(out_shape),
        scratch_shapes=scratch,
        compiler_params=pltpu.CompilerParams(
            collective_id=collective_id, has_side_effects=True, vmem_limit_bytes=VMEM_LIMIT
        ),
        cost_estimate=pl.CostEstimate(
            flops=0, bytes_accessed=count * 30 * size * rows * columns, transcendentals=0
        ),
        name="gather_rows",
    )(*arrays)


class Operand:
    def __init__(self, size, first_column, left_far, weight_far, left, weight, left_sem, weight_sem):
        self.left, self.weight = left, weight
        self.rows = left.shape[0] // size
        self.tile = min(512, weight.shape[0])
        self.far = left_far, weight_far
        self.first_column = first_column
        self.left_sem, self.weight_sem = left_sem, weight_sem

    @staticmethod
    def scratch(size, left, weight):
        width = left.shape[1]
        return [
            pltpu.VMEM(left.shape, left.dtype),
            pltpu.VMEM((weight.shape[0], width), weight.dtype),
            pltpu.SemaphoreType.DMA((size,)),
            pltpu.SemaphoreType.DMA((max(1, weight.shape[0] // 512),)),
        ]

    def left_copy(self, slot, owner):
        piece = pl.ds(pl.multiple_of(owner * self.rows, self.rows), self.rows)
        return pltpu.make_async_copy(self.far[0].at[piece], self.left.at[piece], self.left_sem.at[slot])

    def weight_copy(self, index):
        piece = pl.ds(pl.multiple_of(index * self.tile, self.tile), self.tile)
        columns = pl.ds(self.first_column, self.left.shape[1])
        return pltpu.make_async_copy(
            self.far[1].at[piece, columns], self.weight.at[piece], self.weight_sem.at[index]
        )


def block_product(operands, start, rows, fresh, write, after):
    total = operands[0].weight.shape[0]
    tile = operands[0].tile
    start = pl.multiple_of(start, rows)

    def step(index, carry):
        @pl.when(fresh)
        def _():
            for operand in operands:
                operand.weight_copy(index).wait()

        columns = pl.ds(pl.multiple_of(index * tile, tile), tile)
        values = None
        for operand in operands:
            part = times_transposed(
                operand.left[pl.ds(start, rows), :], operand.weight[columns, :]
            )
            values = part if values is None else values + part
        write(columns, values)
        after(index)
        return carry

    lax.fori_loop(0, total // tile, step, 0)


class Scatter:
    def __init__(self, size, outgoing, *rest):
        self.size, self.outgoing = size, outgoing
        if size == 4:
            self.passing, rest = rest[0], rest[1:]
        self.arriving, self.send_sem, self.recv_sem = rest
        self.rows = outgoing.shape[1]
        self.me = lax.axis_index("tensor")
        self.stages = 2 if size == 4 else 1
        self.plan()

    @staticmethod
    def scratch(size, rows, columns):
        if size == 4:
            sends = 10
            buffers = [
                pltpu.VMEM((4, rows, columns), jnp.bfloat16),
                pltpu.VMEM((2, rows // 2, columns), jnp.bfloat16),
                pltpu.VMEM((2, rows, columns), jnp.bfloat16),
            ]
        else:
            sends = size - 1
            buffers = [
                pltpu.VMEM((size, rows, columns), jnp.bfloat16),
                pltpu.VMEM((size - 1, rows, columns), jnp.bfloat16),
            ]
        return buffers + [pltpu.SemaphoreType.DMA((sends,)), pltpu.SemaphoreType.DMA((sends,))]

    def prepare(self, index, source, target, peer):
        return remote(source, target, self.send_sem.at[index], self.recv_sem.at[index], peer)

    def plan(self):
        outgoing, arriving = self.outgoing, self.arriving
        if self.size != 4:
            self.copies = [
                self.prepare(step, outgoing.at[step], arriving.at[step], peer)
                for step, peer in enumerate(other_members("tensor", self.size))
            ]
            self.early, self.starts = (), tuple((step, step) for step in range(self.size - 1))
            return
        beside, below, _ = square_peers(self.me)
        half, quarter = self.rows // 2, self.rows // 4
        first, second = pl.ds(0, half), pl.ds(half, half)
        middle = outgoing.shape[2] // 2
        left, right = pl.ds(0, middle), pl.ds(middle, middle)
        upper = [pl.ds(stage * quarter, quarter) for stage in range(2)]
        lower = [pl.ds(half + stage * quarter, quarter) for stage in range(2)]
        everything = pl.ds(0, half)
        self.copies = [
            self.prepare(0, outgoing.at[0, first, left], self.passing.at[0, everything, left], beside),
            self.prepare(1, outgoing.at[0, second, left], self.passing.at[1, everything, left], below),
            self.prepare(2, outgoing.at[0, first, right], self.passing.at[0, everything, right], beside),
            self.prepare(3, outgoing.at[0, second, right], self.passing.at[1, everything, right], below),
            self.prepare(4, outgoing.at[1, first], arriving.at[0, first], beside),
            self.prepare(5, outgoing.at[2, second], arriving.at[1, second], below),
            self.prepare(6, outgoing.at[1, lower[0]], arriving.at[0, lower[0]], beside),
            self.prepare(7, outgoing.at[2, upper[0]], arriving.at[1, upper[0]], below),
            self.prepare(8, outgoing.at[1, lower[1]], arriving.at[0, lower[1]], beside),
            self.prepare(9, outgoing.at[2, upper[1]], arriving.at[1, upper[1]], below),
        ]
        self.early, self.starts = (0, 1), ((0, 2), (0, 3), (1, 4), (2, 5))

    def owner(self, slot):
        if self.size != 4:
            return lax.rem(self.me + slot + 1, self.size)
        beside, below, across = square_peers(self.me)
        return jnp.where(
            slot == 0, across, jnp.where(slot == 1, beside, jnp.where(slot == 2, below, self.me))
        )

    def load(self, operands):
        tiles = operands[0].weight.shape[0] // operands[0].tile
        for operand in operands:
            operand.left_copy(0, self.owner(0)).start()
        for index in range(tiles):
            for operand in operands:
                operand.weight_copy(index).start()
        for slot in range(1, self.size):
            for operand in operands:
                operand.left_copy(slot, self.owner(slot)).start()

    def fill(self, operands, look=None, between=None):
        rows = self.rows

        def step(slot, carry):
            owner = self.owner(slot)
            for operand in operands:
                operand.left_copy(slot, owner).wait()

            def write(columns, values):
                self.outgoing[slot, :, columns] = values.astype(self.outgoing.dtype)
                if look is not None:
                    look(owner, columns, values)

            tiles = operands[0].weight.shape[0] // operands[0].tile

            def after(index):
                for early in self.early:
                    pl.when((slot == 0) & (index == max(tiles // 2, 1) - 1))(self.copies[early].start)

            block_product(operands, owner * rows, rows, slot == 0, write, after)
            for at, index in self.starts:
                pl.when(slot == at)(self.copies[index].start)
            if between is not None:
                pl.when(slot == 0)(between)
            return carry

        lax.fori_loop(0, self.size, step, 0)

    def relay(self):
        if self.size != 4:
            return
        half, quarter = self.rows // 2, self.rows // 4
        for stage in range(2):
            for arrivals, source, slot, start, onward in (
                ((1, 3), 1, 1, half, 6 + 2 * stage),
                ((0, 2), 0, 2, 0, 7 + 2 * stage),
            ):
                if stage == 0:
                    for index in arrivals:
                        self.copies[index].wait_recv()
                piece = pl.ds(start + stage * quarter, quarter)
                self.outgoing[slot, piece, :] = add_rounded(
                    self.outgoing[slot, piece, :],
                    self.passing[source, stage * quarter : (stage + 1) * quarter, :],
                )
                self.copies[onward].start()

    def collect(self, stage):
        if self.size != 4:
            for copy in self.copies:
                copy.wait_recv()
            return
        if stage == 0:
            self.copies[4].wait_recv()
            self.copies[5].wait_recv()
        self.copies[6 + 2 * stage].wait_recv()
        self.copies[7 + 2 * stage].wait_recv()

    def over_rows(self, stage, body):
        if self.size != 4:
            over_pieces(self.rows, body)
            return
        half, quarter = self.rows // 2, self.rows // 4
        over_pieces(quarter, body, stage * quarter)
        over_pieces(quarter, body, half + stage * quarter)

    def over_stages(self, body, done=None):
        for stage in range(self.stages):
            self.collect(stage)
            self.over_rows(stage, body)
            if done is not None:
                done(stage)

    def total(self, piece):
        total = self.outgoing[self.size - 1, piece, :].astype(jnp.float32)
        for index in range(self.arriving.shape[0]):
            total = total + self.arriving[index, piece, :].astype(jnp.float32)
        return total

    def drain(self):
        for copy in self.copies:
            copy.wait_send()


class Chain:
    def __init__(
        self, chips, steps, rising_refs, falling_refs, up_ref, down_ref,
        rise, fall, up, down, load_sem, send_sem, recv_sem,
    ):
        self.chips, self.steps = chips, steps
        self.rise, self.fall, self.up, self.down = rise, fall, up, down
        device = lax.axis_index("dp")
        self.chip = device // 2
        count = len(steps)
        self.loads = [
            pltpu.make_async_copy(source, target, load_sem.at[index])
            for index, (source, target) in enumerate(
                [(up_ref, up.at[0]), (down_ref, down.at[0])]
                + [(ref, rise.at[index]) for index, ref in enumerate(rising_refs)]
                + [(ref, fall.at[index]) for index, ref in enumerate(falling_refs)]
            )
        ]
        above = lax.rem(device + 2, 2 * chips)
        under = lax.rem(device + 2 * chips - 2, 2 * chips)
        self.neighbours = [("dp", above), ("dp", under)]
        self.rises = [
            remote(rise.at[i], up.at[i + 1], send_sem.at[i], recv_sem.at[i], above, "dp")
            for i in range(count)
        ]
        self.falls = [
            remote(
                fall.at[i], down.at[i + 1], send_sem.at[count + i], recv_sem.at[count + i], under, "dp"
            )
            for i in range(count)
        ]

    @staticmethod
    def scratch(count, rows, columns):
        return [
            pltpu.VMEM((count, rows, columns), jnp.bfloat16),
            pltpu.VMEM((count, rows, columns), jnp.bfloat16),
            pltpu.VMEM((count + 1, rows, columns), jnp.bfloat16),
            pltpu.VMEM((count + 1, rows, columns), jnp.bfloat16),
            pltpu.SemaphoreType.DMA((2 * count + 2,)),
            pltpu.SemaphoreType.DMA((2 * count,)),
            pltpu.SemaphoreType.DMA((2 * count,)),
        ]

    def load(self):
        for copy in self.loads:
            copy.start()

    def step(self, index):
        if index == 0:
            for copy in self.loads:
                copy.wait()
        step = self.steps[index]
        rows = self.rise.shape[1]
        sends_up = self.chip < step
        sends_down = self.chip >= self.chips - step

        @pl.when(sends_up & (self.chip > 0))
        def _():
            def add(piece):
                self.rise[index, piece, :] = add_rounded(
                    self.rise[index, piece, :], self.up[index, piece, :]
                )

            over_pieces(rows, add)

        pl.when(sends_up)(self.rises[index].start)

        @pl.when(sends_down & (self.chip < self.chips - 1))
        def _():
            def add(piece):
                self.fall[index, piece, :] = add_rounded(
                    self.fall[index, piece, :], self.down[index, piece, :]
                )

            over_pieces(rows, add)

        pl.when(sends_down)(self.falls[index].start)

    def arrives(self, index):
        step = self.steps[index]
        from_under = (self.chip > 0) & (self.chip <= step)
        from_above = (self.chip < self.chips - 1) & (self.chip >= self.chips - step - 1)
        return from_under, from_above

    def wait(self, index):
        from_under, from_above = self.arrives(index)
        pl.when(from_under)(self.rises[index].wait_recv)
        pl.when(from_above)(self.falls[index].wait_recv)

    def drain(self):
        for index, step in enumerate(self.steps):
            pl.when(self.chip < step)(self.rises[index].wait_send)
            pl.when(self.chip >= self.chips - step)(self.falls[index].wait_send)


def add_rounded(first, second):
    return (first.astype(jnp.float32) + second.astype(jnp.float32)).astype(jnp.bfloat16)


def over_pieces(rows, body, start=0):
    count = min(32, rows)

    def step(index, carry):
        body(pl.ds(pl.multiple_of(start + index * count, count), count))
        return carry

    lax.fori_loop(0, rows // count, step, 0)


def send_terms(axis, peers, source, landing, send_sem, recv_sem):
    me = lax.axis_index(axis)
    landing[me] = source[...]
    copies = []
    for step, peer in enumerate(peers):
        copy = remote(source, landing.at[me], send_sem.at[step], recv_sem.at[step], peer, axis)
        copy.start()
        copies.append(copy)
    return copies


def add_terms(landing, copies):
    for copy in copies:
        copy.wait_recv()
    total = landing[0]
    for index in range(1, landing.shape[0]):
        total = total + landing[index]
    return total


def split_operands(refs, size, first_columns):
    count = len(first_columns)
    far, refs, scratch = refs[: 2 * count], refs[2 * count : -4 * count], refs[-4 * count :]
    operands = [
        Operand(size, first, *far[2 * p : 2 * p + 2], *scratch[4 * p : 4 * p + 4])
        for p, first in enumerate(first_columns)
    ]
    return operands, refs


def store_row(target_ref, row_ref):
    width = target_ref.shape[1]
    for index in range(row_ref.shape[1] // width):
        target_ref[index : index + 1, :] = row_ref[:, index * width : (index + 1) * width]


def between_forward_kernel(size, first_columns, *refs):
    operands, refs = split_operands(refs, size, first_columns)
    input_ref, gain_ref, gathered_ref, turned_ref, state_ref, own_ref = refs[:6]
    buffers = 5 if size == 4 else 4
    scatter = Scatter(size, *refs[6 : 6 + buffers])
    gather = Gather(size, own_ref, gathered_ref, turned_ref, *refs[6 + buffers :])
    scatter.load(operands)
    greet(neighbours(size))
    scatter.fill(operands)
    scatter.relay()

    def norm(piece):
        state = input_ref[piece, :].astype(jnp.float32) + scatter.total(piece)
        state_ref[piece, :] = state
        own_ref[piece, :] = (state * row_scale(state) * gain_ref[...]).astype(own_ref.dtype)

    scatter.over_stages(norm, gather.start)
    gather.forward()
    gather.finish()
    scatter.drain()


def between_backward_kernel(size, chips, first_columns, *refs):
    operands, refs = split_operands(refs, size, first_columns)
    state_ref, cotangent_ref, gain_ref = refs[:3]
    chain_refs, own_block_ref, refs = refs[3:7], refs[7], refs[8:]
    gathered_ref, gathered_turned_ref, slope_ref, term_ref, chain_total_ref = refs[:5]
    own_ref, sum_ref, own_sem = refs[5:8]
    buffers = 5 if size == 4 else 4
    scatter = Scatter(size, *refs[8 : 8 + buffers])
    gather = Gather(size, own_ref, gathered_ref, gathered_turned_ref, *refs[8 + buffers : 14 + buffers])
    chain = Chain(
        chips, (chips - 1,), chain_refs[:1], chain_refs[1:2], *chain_refs[2:], *refs[14 + buffers :]
    )
    own_load = pltpu.make_async_copy(own_block_ref, chain_total_ref, own_sem.at[0])
    chain.load()
    scatter.load(operands)
    own_load.start()
    greet(neighbours(size) + chain.neighbours)
    scatter.fill(operands, between=lambda: chain.step(0))
    scatter.relay()
    sum_ref[...] = jnp.zeros_like(sum_ref)

    def norm(piece):
        back = scatter.total(piece)
        state = state_ref[piece, :]
        scale = row_scale(state)
        unit = state * scale
        sum_ref[...] += jnp.sum(back * unit, axis=0, keepdims=True)
        unit_slope = back * gain_ref[...]
        slope = cotangent_ref[piece, :].astype(jnp.float32) + scale * (
            unit_slope - unit * jnp.mean(unit_slope * unit, axis=-1, keepdims=True)
        )
        slope_ref[piece, :] = slope
        own_ref[piece, :] = slope.astype(own_ref.dtype)

    scatter.over_stages(norm, gather.start)
    store_row(term_ref, sum_ref)
    gather.forward()
    gather.finish()
    own_load.wait()
    chain.wait(0)
    for arrived, landing in zip(chain.arrives(0), (chain.up, chain.down)):

        @pl.when(arrived)
        def _(landing=landing):
            def add(piece):
                chain_total_ref[piece, :] = add_rounded(
                    chain_total_ref[piece, :], landing[1, piece, :]
                )

            over_pieces(chain_total_ref.shape[0], add)

    scatter.drain()
    chain.drain()


def last_kernel(sizes, first_columns, *refs):
    data_size, size = sizes
    operands, refs = split_operands(refs, size, first_columns)
    input_ref, gain_ref, slope_ref, terms_ref, rows_ref = refs[:5]
    gradient_ref, terms_out_ref, sum_ref, partial_ref, group_ref, inner, outer = refs[5:12]
    inner_send, inner_recv, outer_send, outer_recv = refs[12:16]
    mixing = Scatter(size, *refs[16:])
    rows = gradient_ref.shape[0]
    mixing.load(operands)
    greet(
        [("tensor", peer) for peer in other_members("tensor", size)]
        + [("dp", peer) for peer in other_members("dp", data_size)]
    )
    sum_ref[...] = jnp.zeros_like(sum_ref)

    def look(owner, columns, values):
        piece = pl.ds(pl.multiple_of(owner * rows, rows), rows)
        sum_ref[:, columns] += jnp.sum(
            values * rows_ref[piece, columns].astype(jnp.float32), axis=0, keepdims=True
        )

    mixing.fill(operands, look)
    sum_ref[...] = sum_ref[...] / gain_ref[...]
    kept = partial_ref.shape[0] - terms_ref.shape[0]
    partial_ref[kept:, :] = terms_ref[...]
    store_row(partial_ref, sum_ref)
    inner_copies = send_terms(
        "tensor", other_members("tensor", size), partial_ref, inner, inner_send, inner_recv
    )
    mixing.relay()
    group_ref[...] = add_terms(inner, inner_copies)
    outer_copies = send_terms(
        "dp", other_members("dp", data_size), group_ref, outer, outer_send, outer_recv
    )
    terms_out_ref[...] = add_terms(outer, outer_copies)

    def norm(piece):
        back = mixing.total(piece)
        values = input_ref[piece, :].astype(jnp.float32)
        scale = row_scale(values)
        unit = values * scale
        unit_slope = back * gain_ref[...]
        gradient_ref[piece, :] = (
            slope_ref[piece, :]
            + scale * (unit_slope - unit * jnp.mean(unit_slope * unit, axis=-1, keepdims=True))
        ).astype(gradient_ref.dtype)

    mixing.over_stages(norm)
    for copy in inner_copies + outer_copies:
        copy.wait_send()
    mixing.drain()


def scatter_call(body, triples, size, others, far, outs, gathered, scratch, collective_id):
    far_spec = pl.BlockSpec(memory_space=pl.ANY)
    operands = [array for left, weight, _ in triples for array in (left, weight)]
    in_specs = [far_spec] * len(operands)
    for other in others:
        in_specs.append(pl.BlockSpec(other.shape, lambda i: (0, 0), pipeline_mode=pl.Buffered(1)))
    in_specs += [far_spec] * len(far)
    out_specs = [pl.BlockSpec(out.shape, lambda i: (0, 0)) for out in outs]
    if gathered:
        out_specs[:2] = [far_spec] * 2
    return pl.pallas_call(
        functools.partial(body, tuple(first for _, _, first in triples)),
        grid=(1,),
        out_shape=outs,
        in_specs=in_specs,
        out_specs=out_specs,
        scratch_shapes=list(scratch)
        + [part for left, weight, _ in triples for part in Operand.scratch(size, left, weight)],
        compiler_params=pltpu.CompilerParams(
            collective_id=collective_id, has_side_effects=True, vmem_limit_bytes=VMEM_LIMIT
        ),
        cost_estimate=pl.CostEstimate(
            flops=sum(2 * left.size * weight.shape[0] for left, weight, _ in triples),
            bytes_accessed=150_000_000,
            transcendentals=0,
        ),
    )(*operands, *others, *far)


LOG2E = 1.4426950408889634


def turn_tables(head_size):
    half_size = head_size // 2
    frequency = np.float32(rope_base) ** (
        -(np.arange(half_size, dtype=np.float32) * np.float32(2.0) / np.float32(head_size))
    )
    frequency = frequency.astype(np.float64)
    sign = np.concatenate([-np.ones(half_size), np.ones(half_size)])[None, :]
    positions = np.concatenate([np.arange(0, SEQUENCE_LENGTH, 128), np.arange(128)])
    angles = positions[:, None] * np.concatenate([frequency, frequency])[None, :]
    return np.cos(angles).astype(np.float32), (sign * np.sin(angles)).astype(np.float32)


def fill_tables(few_cosines_ref, few_sines_ref, cosine_ref, sine_ref):
    coarse = few_cosines_ref.shape[0] - 128
    near_cosine, near_sine = few_cosines_ref[coarse:, :], few_sines_ref[coarse:, :]

    def step(index, carry):
        far_cosine = few_cosines_ref[pl.ds(index, 1), :]
        far_sine = few_sines_ref[pl.ds(index, 1), :]
        rows = pl.ds(pl.multiple_of(index * 128, 128), 128)
        cosine_ref[rows, :] = far_cosine * near_cosine - far_sine * near_sine
        sine_ref[rows, :] = far_sine * near_cosine + far_cosine * near_sine
        return carry

    lax.fori_loop(0, coarse, step, 0)


def turn(values, cosine, sine):
    return values * cosine + pltpu.roll(values, values.shape[-1] // 2, 1) * sine


def turn_back(values, cosine, sine):
    return values * cosine - pltpu.roll(values, values.shape[-1] // 2, 1) * sine


def contract_first(first_operand, second_operand):
    return lax.dot_general(
        first_operand, second_operand, (((0,), (0,)), ((), ())), preferred_element_type=jnp.float32
    )


def visible_scores(key_rows, query_rows, first_row, multiplier):
    scores = times_transposed(key_rows, query_rows) * multiplier
    _, queries = scores.shape
    key_at = lax.broadcasted_iota(jnp.int32, (queries, queries), 0)
    query_at = lax.broadcasted_iota(jnp.int32, (queries, queries), 1)
    corner = jnp.where(query_at >= key_at, scores[first_row:], -1e30)
    if first_row == 0:
        return corner
    return jnp.concatenate([scores[:first_row], corner], axis=0)


def turn_heads(
    grouping, head_size, raw_ref, query_gain_ref, key_gain_ref, cosine_ref, sine_ref, query_ref, key_ref, value_ref
):
    def turned(start, gain):
        raw = raw_ref[:, pl.ds(start, head_size)]
        return turn(raw * row_scale(raw) * gain, cosine_ref[...], sine_ref[...]).astype(jnp.bfloat16)

    def step(part, carry):
        query_ref[part] = turned(pl.multiple_of(part * head_size, head_size), query_gain_ref[...])
        return carry

    lax.fori_loop(0, grouping, step, 0)
    key_ref[...] = turned(grouping * head_size, key_gain_ref[...])
    value_ref[...] = raw_ref[:, (grouping + 1) * head_size :].astype(jnp.bfloat16)


def attention_forward_kernel(
    grouping, head_size, block, rows_ref, weight_ref, few_cosines_ref, few_sines_ref, query_gain_ref, key_gain_ref,
    raw_ref, mixed_ref, total_ref, query_ref, key_ref, value_ref, cosine_ref, sine_ref,
):
    sequence = rows_ref.shape[0]
    multiplier = head_size ** (-0.5) * LOG2E

    @pl.when((pl.program_id(0) == 0) & (pl.program_id(1) == 0))
    def _():
        fill_tables(few_cosines_ref, few_sines_ref, cosine_ref, sine_ref)

    raw_ref[...] = simple_product(rows_ref[...], weight_ref[...])
    turn_heads(
        grouping, head_size, raw_ref, query_gain_ref, key_gain_ref, cosine_ref, sine_ref, query_ref, key_ref, value_ref
    )

    def head_step(part, carry):
        lanes = pl.ds(pl.multiple_of(part * head_size, head_size), head_size)
        for first_row in range(0, sequence, block):
            last_row = first_row + block
            scores = visible_scores(
                key_ref[:last_row, :], query_ref[part, first_row:last_row, :], first_row, multiplier
            )
            highest = jnp.max(scores, axis=0, keepdims=True)
            weights = jnp.exp2(scores - highest)
            total = jnp.sum(weights, axis=0, keepdims=True)
            weights = (weights * (1.0 / total)).astype(jnp.bfloat16)
            mixed_ref[first_row:last_row, lanes] = contract_first(
                weights, value_ref[:last_row, :]
            ).astype(mixed_ref.dtype)
            total_ref[0, pl.ds(part, 1), first_row:last_row] = highest + jnp.log2(total)
        return carry

    lax.fori_loop(0, grouping, head_step, 0)


def attention_forward(rows, weight, tables, query_gain, key_gain, heads, grouping):
    total_rows, depth = rows.shape
    head_size = query_gain.shape[0]
    sequences = total_rows // SEQUENCE_LENGTH
    width = (grouping + 2) * head_size
    block = min(256, SEQUENCE_LENGTH)
    table = pl.BlockSpec(tables[0].shape, lambda s, h: (0, 0))
    gain = pl.BlockSpec((1, head_size), lambda s, h: (0, 0))
    elements = heads * grouping * total_rows * SEQUENCE_LENGTH // 2
    return pl.pallas_call(
        functools.partial(attention_forward_kernel, grouping, head_size, block),
        grid=(sequences, heads),
        out_shape=[
            jax.ShapeDtypeStruct((total_rows, heads * width), jnp.float32),
            jax.ShapeDtypeStruct((total_rows, heads * grouping * head_size), jnp.bfloat16),
            jax.ShapeDtypeStruct((heads, grouping, total_rows), jnp.float32),
        ],
        in_specs=[
            pl.BlockSpec((SEQUENCE_LENGTH, depth), lambda s, h: (s, 0)),
            pl.BlockSpec((depth, width), lambda s, h: (0, h)),
            table,
            table,
            gain,
            gain,
        ],
        out_specs=[
            pl.BlockSpec((SEQUENCE_LENGTH, width), lambda s, h: (s, h)),
            pl.BlockSpec((SEQUENCE_LENGTH, grouping * head_size), lambda s, h: (s, h)),
            pl.BlockSpec((1, grouping, SEQUENCE_LENGTH), lambda s, h: (h, 0, s)),
        ],
        scratch_shapes=[
            pltpu.VMEM((grouping, SEQUENCE_LENGTH, head_size), jnp.bfloat16),
            pltpu.VMEM((SEQUENCE_LENGTH, head_size), jnp.bfloat16),
            pltpu.VMEM((SEQUENCE_LENGTH, head_size), jnp.bfloat16),
            pltpu.VMEM((SEQUENCE_LENGTH, head_size), jnp.float32),
            pltpu.VMEM((SEQUENCE_LENGTH, head_size), jnp.float32),
        ],
        compiler_params=pltpu.CompilerParams(vmem_limit_bytes=VMEM_LIMIT),
        cost_estimate=pl.CostEstimate(
            flops=2 * total_rows * depth * heads * width + 4 * elements * head_size,
            bytes_accessed=2 * (total_rows * depth + depth * heads * width),
            transcendentals=elements,
        ),
        name="attention_forward",
    )(rows, weight, *tables, query_gain.reshape(1, -1), key_gain.reshape(1, -1))


def norm_back(turned_slope, raw, gain, cosine, sine):
    norm_slope = turn_back(turned_slope, cosine, sine)
    scale = row_scale(raw)
    unit = raw * scale
    term = norm_slope * unit
    unit_slope = norm_slope * gain
    slope = scale * (unit_slope - unit * jnp.mean(unit_slope * unit, axis=-1, keepdims=True))
    return slope.astype(jnp.bfloat16), jnp.sum(term, axis=0, keepdims=True)


def attention_backward_kernel(size, grouping, head_size, block, first_columns, *refs):
    operands, refs = split_operands(refs, size, first_columns)
    (
        state_ref, weight_ref, raw_ref, mixed_ref, total_ref, few_cosines_ref, few_sines_ref,
        query_gain_ref, key_gain_ref, hidden_state_ref, slope_ref, gain_ref, output_ref,
        query_ref, key_ref, value_ref, out_slope_ref, turned_ref, key_sum_ref, value_sum_ref, cosine_ref, sine_ref,
    ) = refs[:22]
    scatter = Scatter(size, *refs[22:])
    step = pl.program_id(0) * pl.num_programs(1) + pl.program_id(1)
    steps = pl.num_programs(0) * pl.num_programs(1)

    @pl.when(step == 0)
    def _():
        scatter.load(operands)
        greet(neighbours(size))
        scatter.fill(operands)

    attend_backward_head(
        grouping, head_size, block, state_ref, weight_ref, raw_ref, mixed_ref, total_ref, few_cosines_ref,
        few_sines_ref, query_gain_ref, key_gain_ref, slope_ref, gain_ref, query_ref, key_ref, value_ref,
        out_slope_ref, turned_ref, key_sum_ref, value_sum_ref, cosine_ref, sine_ref,
    )

    @pl.when(step == 0)
    def _():
        scatter.relay()

    @pl.when(step == steps - 1)
    def _():
        def finish(piece):
            output_ref[piece, :] = (hidden_state_ref[piece, :] + scatter.total(piece)).astype(
                output_ref.dtype
            )

        scatter.over_stages(finish)
        scatter.drain()


def attend_backward_head(
    grouping, head_size, block, state_ref, weight_ref, raw_ref, mixed_ref, total_ref, few_cosines_ref, few_sines_ref,
    query_gain_ref, key_gain_ref, slope_ref, gain_ref, query_ref, key_ref, value_ref, out_slope_ref,
    turned_ref, key_sum_ref, value_sum_ref, cosine_ref, sine_ref,
):
    sequence = state_ref.shape[0]
    scale_factor = head_size ** (-0.5)
    multiplier = scale_factor * LOG2E

    @pl.when((pl.program_id(0) == 0) & (pl.program_id(1) == 0))
    def _():
        gain_ref[...] = jnp.zeros_like(gain_ref)
        fill_tables(few_cosines_ref, few_sines_ref, cosine_ref, sine_ref)

    out_slope_ref[...] = simple_product(state_ref[...], weight_ref[...]).astype(jnp.bfloat16)
    turn_heads(
        grouping, head_size, raw_ref, query_gain_ref, key_gain_ref, cosine_ref, sine_ref, query_ref, key_ref, value_ref
    )
    key_sum_ref[...] = jnp.zeros_like(key_sum_ref)
    value_sum_ref[...] = jnp.zeros_like(value_sum_ref)
    ones = jnp.ones((8, head_size), jnp.float32)

    def head_step(part, carry):
        lanes = pl.ds(pl.multiple_of(part * head_size, head_size), head_size)
        for first_row in range(0, sequence, block):
            last_row = first_row + block
            query_rows = query_ref[part, first_row:last_row, :]
            slope_rows = out_slope_ref[first_row:last_row, lanes]
            scores = visible_scores(key_ref[:last_row, :], query_rows, first_row, multiplier)
            weights = jnp.exp2(scores - total_ref[0, pl.ds(part, 1), first_row:last_row])
            value_sum_ref[:last_row, :] += simple_product(weights.astype(jnp.bfloat16), slope_rows)
            product = slope_rows.astype(jnp.float32) * mixed_ref[first_row:last_row, lanes].astype(jnp.float32)
            centre = lax.dot_general(
                ones,
                product,
                (((1,), (1,)), ((), ())),
                preferred_element_type=jnp.float32,
                precision=lax.Precision.HIGHEST,
            )[:1]
            weight_slope = times_transposed(value_ref[:last_row, :], slope_rows)
            score_slope = (weights * (weight_slope - centre)).astype(jnp.bfloat16)
            key_sum_ref[:last_row, :] += simple_product(score_slope, query_rows)
            turned_ref[first_row:last_row, :] = (
                contract_first(score_slope, key_ref[:last_row, :]) * scale_factor
            )
        slope, term = norm_back(
            turned_ref[...], raw_ref[:, lanes], query_gain_ref[...], cosine_ref[...], sine_ref[...]
        )
        slope_ref[:, lanes] = slope
        gain_ref[0:1, :] += term
        return carry

    lax.fori_loop(0, grouping, head_step, 0)
    lanes = slice(grouping * head_size, (grouping + 1) * head_size)
    slope, term = norm_back(
        key_sum_ref[...] * scale_factor, raw_ref[:, lanes], key_gain_ref[...], cosine_ref[...], sine_ref[...]
    )
    slope_ref[:, lanes] = slope
    gain_ref[1:2, :] += term
    slope_ref[:, (grouping + 1) * head_size :] = value_sum_ref[...].astype(jnp.bfloat16)


def attention_backward(
    state_rows, weight, weight_start, raw, mixed, totals, tables, query_gain, key_gain, heads, grouping,
    triples, hidden_state, size, collective_id,
):
    total_rows, depth = state_rows.shape
    head_size = query_gain.shape[0]
    sequences = total_rows // SEQUENCE_LENGTH
    width = (grouping + 2) * head_size
    out_width = grouping * head_size
    block = min(256, SEQUENCE_LENGTH)
    first_block = weight_start // out_width
    single = pl.Buffered(1)
    table = pl.BlockSpec(tables[0].shape, lambda s, h: (0, 0))
    gain = pl.BlockSpec((1, head_size), lambda s, h: (0, 0))
    elements = heads * grouping * total_rows * SEQUENCE_LENGTH // 2
    whole_rows = pltpu.VMEM((SEQUENCE_LENGTH, head_size), jnp.float32)
    operands = [array for left, other_weight, _ in triples for array in (left, other_weight)]
    in_specs = [pl.BlockSpec(memory_space=pl.ANY)] * len(operands)
    in_specs += [
        pl.BlockSpec((SEQUENCE_LENGTH, depth), lambda s, h: (s, 0), pipeline_mode=single),
        pl.BlockSpec((depth, out_width), lambda s, h: (0, first_block + h)),
        pl.BlockSpec((SEQUENCE_LENGTH, width), lambda s, h: (s, h)),
        pl.BlockSpec((SEQUENCE_LENGTH, out_width), lambda s, h: (s, h)),
        pl.BlockSpec((1, grouping, SEQUENCE_LENGTH), lambda s, h: (h, 0, s)),
        table,
        table,
        gain,
        gain,
        pl.BlockSpec(hidden_state.shape, lambda s, h: (0, 0), pipeline_mode=single),
    ]
    operands += [
        state_rows, weight, raw, mixed, totals, *tables, query_gain.reshape(1, -1), key_gain.reshape(1, -1),
        hidden_state,
    ]
    return pl.pallas_call(
        functools.partial(
            attention_backward_kernel, size, grouping, head_size, block,
            tuple(first for _, _, first in triples),
        ),
        grid=(sequences, heads),
        out_shape=[
            jax.ShapeDtypeStruct((total_rows, heads * width), jnp.bfloat16),
            jax.ShapeDtypeStruct((8, head_size), jnp.float32),
            jax.ShapeDtypeStruct(hidden_state.shape, jnp.bfloat16),
        ],
        in_specs=in_specs,
        out_specs=[
            pl.BlockSpec((SEQUENCE_LENGTH, width), lambda s, h: (s, h)),
            pl.BlockSpec((8, head_size), lambda s, h: (0, 0)),
            pl.BlockSpec(hidden_state.shape, lambda s, h: (0, 0)),
        ],
        scratch_shapes=[
            pltpu.VMEM((grouping, SEQUENCE_LENGTH, head_size), jnp.bfloat16),
            pltpu.VMEM((SEQUENCE_LENGTH, head_size), jnp.bfloat16),
            pltpu.VMEM((SEQUENCE_LENGTH, head_size), jnp.bfloat16),
            pltpu.VMEM((SEQUENCE_LENGTH, out_width), jnp.bfloat16),
            whole_rows,
            whole_rows,
            whole_rows,
            whole_rows,
            whole_rows,
            *Scatter.scratch(size, *hidden_state.shape),
            *[part for left, other, _ in triples for part in Operand.scratch(size, left, other)],
        ],
        compiler_params=pltpu.CompilerParams(
            collective_id=collective_id, has_side_effects=True, vmem_limit_bytes=VMEM_LIMIT
        ),
        cost_estimate=pl.CostEstimate(
            flops=2 * total_rows * depth * heads * out_width + 10 * elements * head_size,
            bytes_accessed=100_000_000,
            transcendentals=elements,
        ),
        name="attention_backward",
    )(*operands)


def feed_half_kernel(
    half, tile, block, rows_far, cotangent_far, weight_far, hidden_far, slope_far,
    rows_ref, cotangent_ref, weight_ref, hidden_ref, slope_ref, row_sem, weight_sem, out_sem,
):
    total = rows_ref.shape[0]
    blocks = total // block
    tiles = half // tile

    def row_copies(index):
        piece = pl.ds(pl.multiple_of(index * block, block), block)
        return [
            pltpu.make_async_copy(far.at[piece], ref.at[piece], row_sem.at[at, index])
            for at, (far, ref) in enumerate(((rows_far, rows_ref), (cotangent_far, cotangent_ref)))
        ]

    def weight_copies(index):
        copies = []
        for part in range(3):
            columns = pl.ds(pl.multiple_of(part * half + index * tile, tile), tile)
            copies.append(
                pltpu.make_async_copy(
                    weight_far.at[:, columns], weight_ref.at[part, index], weight_sem.at[part, index]
                )
            )
        return copies

    def out_copies(index):
        piece = pl.ds(pl.multiple_of(index * block, block), block)
        return [
            pltpu.make_async_copy(ref.at[piece], far.at[piece], out_sem.at[at, index])
            for at, (far, ref) in enumerate(((hidden_far, hidden_ref), (slope_far, slope_ref)))
        ]

    for copy in row_copies(0) + weight_copies(0):
        copy.start()
    for index in range(1, tiles):
        for copy in weight_copies(index):
            copy.start()
    for index in range(1, blocks):
        for copy in row_copies(index):
            copy.start()

    def row_step(row_index, carry):
        piece = pl.ds(pl.multiple_of(row_index * block, block), block)
        for copy in row_copies(row_index):
            copy.wait()

        def step(index, carry):
            @pl.when(row_index == 0)
            def _():
                for copy in weight_copies(index):
                    copy.wait()

            start = pl.multiple_of(index * tile, tile)
            rows = rows_ref[piece, :]
            gate = simple_product(rows, weight_ref[0, index])
            up = simple_product(rows, weight_ref[1, index])
            back = simple_product(cotangent_ref[piece, :], weight_ref[2, index])
            sigmoid = 1.0 / (1.0 + jnp.exp(-gate))
            gated = gate * sigmoid
            hidden_ref[piece, pl.ds(start, tile)] = (gated * up).astype(jnp.bfloat16)
            slope_ref[piece, pl.ds(start, tile)] = (
                back * up * sigmoid * (1.0 + gate * (1.0 - sigmoid))
            ).astype(jnp.bfloat16)
            slope_ref[piece, pl.ds(half + start, tile)] = (back * gated).astype(jnp.bfloat16)
            return carry

        lax.fori_loop(0, tiles, step, 0)
        for copy in out_copies(row_index):
            copy.start()
        return carry

    lax.fori_loop(0, blocks, row_step, 0)
    for index in range(blocks):
        for copy in out_copies(index):
            copy.wait()


def feed_half(rows, cotangent, weight):
    total_rows, depth = rows.shape
    block = min(512, total_rows)
    half = weight.shape[1] // 3
    tile = 256 if half % 256 == 0 else 128
    blocks, tiles = total_rows // block, half // tile
    far = pl.BlockSpec(memory_space=pl.ANY)
    return pl.pallas_call(
        functools.partial(feed_half_kernel, half, tile, block),
        out_shape=[
            jax.ShapeDtypeStruct((total_rows, half), jnp.bfloat16),
            jax.ShapeDtypeStruct((total_rows, 2 * half), jnp.bfloat16),
        ],
        in_specs=[far] * 3,
        out_specs=[far] * 2,
        scratch_shapes=[
            pltpu.VMEM(rows.shape, rows.dtype),
            pltpu.VMEM(rows.shape, rows.dtype),
            pltpu.VMEM((3, tiles, depth, tile), weight.dtype),
            pltpu.VMEM((total_rows, half), jnp.bfloat16),
            pltpu.VMEM((total_rows, 2 * half), jnp.bfloat16),
            pltpu.SemaphoreType.DMA((2, blocks)),
            pltpu.SemaphoreType.DMA((3, tiles)),
            pltpu.SemaphoreType.DMA((2, blocks)),
        ],
        compiler_params=pltpu.CompilerParams(vmem_limit_bytes=VMEM_LIMIT),
        cost_estimate=pl.CostEstimate(
            flops=6 * total_rows * depth * half,
            bytes_accessed=2 * (2 * total_rows * depth + 3 * depth * half),
            transcendentals=total_rows * half,
        ),
        name="feed_half",
    )(rows, cotangent, weight)


def grad_kernel(pair_count, *refs):
    pairs = [refs[2 * p : 2 * p + 2] for p in range(pair_count)]
    out_ref = refs[-1]
    start = 0
    for left_ref, right_ref in pairs:
        width = right_ref.shape[1]
        tile = next(t for t in (768, 512, 384, 256, 128) if width % t == 0)
        for column in range(0, width, tile):
            values = simple_product(left_ref[...], right_ref[:, column : column + tile])
            out_ref[:, start + column : start + column + tile] = values.astype(jnp.bfloat16)
        start += width


def grad_blocks(pairs, rows):
    depth, total_rows = pairs[0][0].shape
    width = sum(right.shape[1] for _, right in pairs)
    in_specs = []
    operands = []
    for left, right in pairs:
        in_specs += [
            pl.BlockSpec((rows, total_rows), lambda k: (k, 0)),
            pl.BlockSpec(right.shape, lambda k: (0, 0), pipeline_mode=pl.Buffered(1)),
        ]
        operands += [left, right]
    return pl.pallas_call(
        functools.partial(grad_kernel, len(pairs)),
        grid=(depth // rows,),
        in_specs=in_specs,
        out_specs=pl.BlockSpec((rows, width), lambda k: (k, 0)),
        out_shape=jax.ShapeDtypeStruct((depth, width), jnp.bfloat16),
        compiler_params=pltpu.CompilerParams(vmem_limit_bytes=VMEM_LIMIT),
        cost_estimate=pl.CostEstimate(
            flops=2 * total_rows * depth * width,
            bytes_accessed=2 * (total_rows * depth * len(pairs) + width * (total_rows + depth)),
            transcendentals=0,
        ),
        name="grad_blocks",
    )(*operands)


def pair_grad_kernel(chips, pair_count, *refs):
    lefts, rights = refs[:pair_count], refs[pair_count : 2 * pair_count]
    out_refs = refs[2 * pair_count : 2 * pair_count + chips]
    held = refs[2 * pair_count + chips : -6]
    sent, landed, left_sem, send_sem, recv_sem, out_sem = refs[-6:]
    block = sent.shape[1]
    device = lax.axis_index("dp")
    chip, core = device // 2, lax.rem(device, 2)
    other = chip * 2 + 1 - core

    def loads(index):
        owner = lax.rem(chip + lax.rem(index, chips), chips) * 2
        owner = owner + jnp.where(index < chips, 1 - core, core)
        piece = pl.ds(pl.multiple_of(owner * block, block), block)
        slot = lax.rem(index, 2)
        return [
            pltpu.make_async_copy(left.at[piece], hold.at[slot], left_sem.at[at, slot])
            for at, (left, hold) in enumerate(zip(lefts, held))
        ]

    for load in loads(0):
        load.start()
    greet([("dp", other)])
    copies = [
        pltpu.make_async_remote_copy(
            src_ref=sent.at[place],
            dst_ref=landed.at[place],
            send_sem=send_sem.at[place],
            recv_sem=recv_sem.at[place],
            device_id={"dp": other},
            device_id_type=MESH,
        )
        for place in range(chips)
    ]

    def products(index, write):
        slot = lax.rem(index, 2)
        for load in loads(index):
            load.wait()

        @pl.when(index + 1 < 2 * chips)
        def _():
            for load in loads(index + 1):
                load.start()

        start = 0
        for hold, right in zip(held, rights):
            width = right.shape[1]
            tile = next(t for t in (512, 384, 256, 128) if width % t == 0)

            def step(at, carry, hold=hold, right=right, start=start, tile=tile):
                column = pl.multiple_of(at * tile, tile)
                write(
                    pl.ds(start + column, tile),
                    simple_product(hold[slot], right[:, pl.ds(column, tile)]),
                )
                return carry

            lax.fori_loop(0, width // tile, step, 0)
            start += width

    def send_step(place, carry):
        def write(columns, values):
            sent[place, :, columns] = values.astype(jnp.bfloat16)

        products(place, write)
        for at in range(chips):
            pl.when(place == at)(copies[at].start)
        return carry

    lax.fori_loop(0, chips, send_step, 0)
    outs = [
        pltpu.make_async_copy(landed.at[place], out_ref, out_sem.at[place])
        for place, out_ref in enumerate(out_refs)
    ]

    def own_step(place, carry):
        for at in range(chips):
            pl.when(place == at)(copies[at].wait_recv)

        def write(columns, values):
            landed[place, :, columns] = (
                values + landed[place, :, columns].astype(jnp.float32)
            ).astype(jnp.bfloat16)

        products(place + chips, write)
        for at in range(chips):
            pl.when(place == at)(outs[at].start)
        return carry

    lax.fori_loop(0, chips, own_step, 0)
    for copy in copies:
        copy.wait_send()
    for copy in outs:
        copy.wait()


def pair_grads(pairs, sizes, collective_id):
    chips = sizes[0] // 2
    depth, total_rows = pairs[0][0].shape
    block = depth // sizes[0]
    width = sum(right.shape[1] for _, right in pairs)
    far = pl.BlockSpec(memory_space=pl.ANY)
    return pl.pallas_call(
        functools.partial(pair_grad_kernel, chips, len(pairs)),
        out_shape=[jax.ShapeDtypeStruct((block, width), jnp.bfloat16)] * chips,
        in_specs=[far] * len(pairs) + [pl.BlockSpec(memory_space=pltpu.VMEM)] * len(pairs),
        out_specs=[far] * chips,
        scratch_shapes=[pltpu.VMEM((2, block, total_rows), jnp.bfloat16) for _ in pairs]
        + [
            pltpu.VMEM((chips, block, width), jnp.bfloat16),
            pltpu.VMEM((chips, block, width), jnp.bfloat16),
            pltpu.SemaphoreType.DMA((len(pairs), 2)),
            pltpu.SemaphoreType.DMA((chips,)),
            pltpu.SemaphoreType.DMA((chips,)),
            pltpu.SemaphoreType.DMA((chips,)),
        ],
        compiler_params=pltpu.CompilerParams(
            collective_id=collective_id, has_side_effects=True, vmem_limit_bytes=VMEM_LIMIT
        ),
        cost_estimate=pl.CostEstimate(
            flops=2 * total_rows * depth * width,
            bytes_accessed=2 * (total_rows * depth * len(pairs) + width * (total_rows + depth)),
            transcendentals=0,
        ),
        name="pair_grads",
    )(*[left for left, _ in pairs], *[right for _, right in pairs])


def reduce_over_chips(pairs, sizes, collective_id):
    data_size = sizes[0]
    chips = data_size // 2
    blocks = pair_grads(pairs, sizes, collective_id)
    up = down = None
    for step in range(1, chips - 1):
        rising, falling = blocks[chips - step], blocks[step]
        if up is not None:
            rising, falling = add_rounded(rising, up), add_rounded(falling, down)
        up = lax.ppermute(
            rising, "dp", [(device, device + 2) for device in range(2 * step)]
        )
        down = lax.ppermute(falling, "dp", [(device, device - 2) for device in range(data_size - 2 * step, data_size)])
    return blocks, up, down


def pack_mixing_kernel(heads, query_ref, key_ref, value_ref, output_ref, out_ref):
    query_width = query_ref.shape[1] // heads
    head_size = key_ref.shape[1] // heads
    start = 0
    for head in range(heads):
        for ref, part in ((query_ref, query_width), (key_ref, head_size), (value_ref, head_size)):
            out_ref[:, start : start + part] = ref[:, head * part : (head + 1) * part]
            start += part
    out_ref[:, start:] = output_ref[...].T


def pack_feed_kernel(gate_ref, up_ref, down_ref, first_ref, second_ref):
    start = 0
    for out_ref in (first_ref, second_ref):
        width = out_ref.shape[1] // 3
        part = slice(start, start + width)
        out_ref[:, :width] = gate_ref[:, part]
        out_ref[:, width : 2 * width] = up_ref[:, part]
        out_ref[:, 2 * width :] = down_ref[part, :].T
        start += width


def finish_kernel(heads, *refs):
    first_ref, second_ref, mixing_ref, output_total_ref, terms_ref, output_rows_ref, input_rows_ref = refs[:7]
    far, held, sem = refs[7:20], refs[20:31], refs[31]
    (
        attention_term_out, query_out, key_out, value_out, query_gain_out, key_gain_out,
        output_out, feed_term_out, gate_out, up_out, down_out,
    ) = held
    copies = [
        pltpu.make_async_copy(source, target, sem.at[index])
        for index, (source, target) in enumerate(zip((output_rows_ref, input_rows_ref, *held), far))
    ]
    copies[0].start()
    copies[1].start()
    start = 0
    for total_ref in (first_ref, second_ref):
        width = total_ref.shape[1] // 3
        part = slice(start, start + width)
        gate_out[:, part] = total_ref[:, :width].astype(jnp.float32)
        up_out[:, part] = total_ref[:, width : 2 * width].astype(jnp.float32)
        down_out[part, :] = total_ref[:, 2 * width :].astype(jnp.float32).T
        start += width
    for copy in copies[10:13]:
        copy.start()
    query_width = query_out.shape[1] // heads
    head_size = key_out.shape[1] // heads
    start = 0
    for head in range(heads):
        for out, part in ((query_out, query_width), (key_out, head_size), (value_out, head_size)):
            out[:, head * part : (head + 1) * part] = mixing_ref[:, start : start + part].astype(
                jnp.float32
            )
            start += part
    output_out[...] = output_total_ref[...].astype(jnp.float32).T
    count = attention_term_out.shape[0]
    attention_term_out[...] = terms_ref[:count, :]
    feed_term_out[...] = terms_ref[count : 2 * count, :]
    query_gain_out[...] = terms_ref[2 * count : 2 * count + 1, :]
    key_gain_out[...] = terms_ref[2 * count + 1 : 2 * count + 2, :]
    for copy in copies[2:10]:
        copy.start()
    for copy in copies:
        copy.wait()


def whole_call(body, shapes, *operands):
    return pl.pallas_call(
        body,
        out_shape=shapes,
        in_specs=[pl.BlockSpec(memory_space=pltpu.VMEM)] * len(operands),
        out_specs=[pl.BlockSpec(memory_space=pltpu.VMEM)] * len(shapes),
        compiler_params=pltpu.CompilerParams(vmem_limit_bytes=VMEM_LIMIT),
        cost_estimate=pl.CostEstimate(
            flops=0, bytes_accessed=4 * sum(operand.size for operand in operands), transcendentals=0
        ),
    )(*operands)


def per_device(
    block_input,
    attention_gain,
    query_weight,
    key_matrix,
    value_matrix,
    query_gain,
    key_gain,
    output_weight,
    feed_gain,
    gate_weight,
    up_weight,
    down_weight,
    out_cotangent,
):
    size = lax.axis_size("tensor")
    sizes = (lax.axis_size("dp"), size)
    model_width = block_input.shape[1]
    head_size = query_gain.shape[0]
    query_columns = query_weight.shape[1]
    key_columns = key_matrix.shape[1]
    heads = key_columns // head_size
    grouping = query_columns // key_columns
    hidden_columns = gate_weight.shape[1]
    qkv_columns = query_columns + 2 * key_columns
    first_columns = hidden_columns // 2
    second_columns = hidden_columns - first_columns
    tables = turn_tables(head_size)

    block_width = query_weight.shape[0]
    (mixing_local,) = whole_call(
        functools.partial(pack_mixing_kernel, heads),
        [jax.ShapeDtypeStruct((block_width, qkv_columns + query_columns), jnp.bfloat16)],
        query_weight, key_matrix, value_matrix, output_weight,
    )
    mixing_full = lax.all_gather(mixing_local, "dp", axis=0, tiled=True)
    feed_locals = whole_call(
        pack_feed_kernel,
        [
            jax.ShapeDtypeStruct((block_width, 3 * columns), jnp.bfloat16)
            for columns in (first_columns, second_columns)
        ],
        gate_weight, up_weight, down_weight,
    )
    first_full = lax.all_gather(feed_locals[0], "dp", axis=0, tiled=True)
    second_full = lax.all_gather(feed_locals[1], "dp", axis=0, tiled=True)
    feed_full = [first_full, second_full]

    input_float = block_input.astype(jnp.float32)
    first_scale = row_scale(input_float)
    first_unit = input_float * first_scale
    mixer_local = (first_unit * attention_gain).astype(jnp.bfloat16)
    mixer_rows, mixer_turned, cotangent_rows, cotangent_turned = gather_rows(
        (mixer_local, out_cotangent), size, 0
    )

    raw, mixed_rows, totals = attention_forward(
        mixer_rows, mixing_full, tables, query_gain, key_gain, heads, grouping
    )
    local_shape = block_input.shape
    local_rows = local_shape[0]
    gain_rows = model_width // head_size
    gathered_shapes = [
        jax.ShapeDtypeStruct((size * local_rows, model_width), jnp.bfloat16),
        jax.ShapeDtypeStruct((model_width, size * local_rows), jnp.bfloat16),
    ]
    local_float = jax.ShapeDtypeStruct(local_shape, jnp.float32)
    local_half = jax.ShapeDtypeStruct(local_shape, jnp.bfloat16)
    row_sum = pltpu.VMEM((1, model_width), jnp.float32)
    own_rows = pltpu.VMEM(local_shape, jnp.bfloat16)
    scatter_scratch = Scatter.scratch(size, *local_shape)
    gather_scratch = Gather.scratch(size, *local_shape)
    feed_rows, feed_turned, hidden_state = scatter_call(
        functools.partial(between_forward_kernel, size),
        [(mixed_rows, mixing_full, qkv_columns)],
        size,
        [block_input, feed_gain.reshape(1, -1)],
        [],
        [*gathered_shapes, local_float],
        True,
        [own_rows, *scatter_scratch, *gather_scratch],
        1,
    )

    hidden_first, slope_first = feed_half(feed_rows, cotangent_rows, feed_full[0])
    blocks, up, down = reduce_over_chips(
        [(feed_turned, slope_first), (cotangent_turned, hidden_first)], sizes, 5
    )
    blocks, later_full = lax.optimization_barrier((blocks, feed_full[1]))
    hidden_second, slope_second = feed_half(feed_rows, cotangent_rows, later_full)
    second_grad = grad_blocks(
        [(feed_turned, slope_second), (cotangent_turned, hidden_second)], 2 * block_width
    )
    second_grad, slope_second = lax.optimization_barrier((second_grad, slope_second))
    second_total = lax.psum_scatter(second_grad, "dp", scatter_dimension=0, tiled=True)
    chips = sizes[0] // 2
    state_rows, state_turned, state_slope, feed_term, first_total = scatter_call(
        functools.partial(between_backward_kernel, size, chips),
        [(slope_first, feed_full[0], 0), (slope_second, later_full, 0)],
        size,
        [hidden_state, out_cotangent, feed_gain.reshape(1, -1)],
        [blocks[1], blocks[chips - 1], up, down, blocks[0]],
        [
            *gathered_shapes,
            local_float,
            jax.ShapeDtypeStruct((gain_rows, head_size), jnp.float32),
            jax.ShapeDtypeStruct(blocks[0].shape, jnp.bfloat16),
        ],
        True,
        [
            own_rows,
            row_sum,
            pltpu.SemaphoreType.DMA((1,)),
            *scatter_scratch,
            *gather_scratch,
            *Chain.scratch(1, *blocks[0].shape),
        ],
        2,
    )
    output_grad = grad_blocks([(state_turned, mixed_rows)], 4 * block_width)
    output_grad, state_rows = lax.optimization_barrier((output_grad, state_rows))
    output_total = lax.psum_scatter(output_grad, "dp", scatter_dimension=0, tiled=True)
    qkv_slope, head_terms, block_output = attention_backward(
        state_rows, mixing_full, qkv_columns, raw, mixed_rows, totals, tables,
        query_gain, key_gain, heads, grouping,
        [
            (hidden_first, feed_full[0], 2 * first_columns),
            (hidden_second, later_full, 2 * second_columns),
        ],
        hidden_state, size, 4,
    )
    mixing_grad = grad_blocks([(mixer_turned, qkv_slope)], 2 * block_width)
    mixing_grad, qkv_slope = lax.optimization_barrier((mixing_grad, qkv_slope))
    mixing_total = lax.psum_scatter(mixing_grad, "dp", scatter_dimension=0, tiled=True)
    terms_shape = (2 * gain_rows + head_terms.shape[0], head_size)
    input_gradient, terms = scatter_call(
        functools.partial(last_kernel, sizes),
        [(qkv_slope, mixing_full, 0)],
        size,
        [
            block_input,
            attention_gain.reshape(1, -1),
            state_slope,
            jnp.concatenate([feed_term, head_terms], axis=0),
            mixer_rows,
        ],
        [],
        [local_half, jax.ShapeDtypeStruct(terms_shape, jnp.float32)],
        False,
        [
            row_sum,
            pltpu.VMEM(terms_shape, jnp.float32),
            pltpu.VMEM(terms_shape, jnp.float32),
            pltpu.VMEM((size, *terms_shape), jnp.float32),
            pltpu.VMEM((sizes[0], *terms_shape), jnp.float32),
            *[pltpu.SemaphoreType.DMA((count - 1,)) for count in (size, size, *sizes[:1] * 2)],
            *scatter_scratch,
        ],
        3,
    )

    def whole_float(*shape):
        return jax.ShapeDtypeStruct(shape, jnp.float32)

    float_shapes = [
        whole_float(gain_rows, head_size),
        whole_float(block_width, query_columns),
        whole_float(block_width, key_columns),
        whole_float(block_width, key_columns),
        whole_float(1, head_size),
        whole_float(1, head_size),
        whole_float(query_columns, block_width),
        whole_float(gain_rows, head_size),
        whole_float(block_width, hidden_columns),
        whole_float(block_width, hidden_columns),
        whole_float(hidden_columns, block_width),
    ]
    outs = pl.pallas_call(
        functools.partial(finish_kernel, heads),
        out_shape=[local_half, local_half, *float_shapes],
        in_specs=[pl.BlockSpec(memory_space=pltpu.VMEM)] * 7,
        out_specs=[pl.BlockSpec(memory_space=pl.ANY)] * 13,
        scratch_shapes=[pltpu.VMEM(shape.shape, shape.dtype) for shape in float_shapes]
        + [pltpu.SemaphoreType.DMA((13,))],
        compiler_params=pltpu.CompilerParams(vmem_limit_bytes=VMEM_LIMIT),
        cost_estimate=pl.CostEstimate(flops=0, bytes_accessed=20_000_000, transcendentals=0),
        name="finish",
    )(first_total, second_total, mixing_total, output_total, terms, block_output, input_gradient)
    return tuple(
        out.reshape(-1) if index in (2, 6, 7, 9) else out for index, out in enumerate(outs)
    )


def solution(mesh):
    in_specs = (
        P(("dp", "tensor"), None),
        P(),
        P("dp", "tensor"),
        P("dp", "tensor"),
        P("dp", "tensor"),
        P(),
        P(),
        P("tensor", "dp"),
        P(),
        P("dp", "tensor"),
        P("dp", "tensor"),
        P("tensor", "dp"),
        P(("dp", "tensor"), None),
    )
    out_specs = (
        P(("dp", "tensor"), None),
        P(("dp", "tensor"), None),
        P(),
        P("dp", "tensor"),
        P("dp", "tensor"),
        P("dp", "tensor"),
        P(),
        P(),
        P("tensor", "dp"),
        P(),
        P("dp", "tensor"),
        P("dp", "tensor"),
        P("tensor", "dp"),
    )

    return jax.shard_map(per_device, mesh=mesh, in_specs=in_specs, out_specs=out_specs, check_vma=False)
```

```python
import functools

import jax
import jax.numpy as jnp
import numpy as np
from jax import lax
from jax.experimental import pallas as pl
from jax.experimental.pallas import tpu as pltpu
from jax.sharding import PartitionSpec as P


SEQUENCE_LENGTH = 1024

epsilon = 1e-06
rope_base = 1000000.0


MESH = pl.DeviceIdType.MESH
VMEM_LIMIT = 62 * 1024 * 1024


def row_scale(values):
    return lax.rsqrt(jnp.mean(values * values, axis=-1, keepdims=True) + epsilon)


def times_transposed(first_operand, second_operand):
    return lax.dot_general(
        first_operand, second_operand, (((1,), (1,)), ((), ())), preferred_element_type=jnp.float32
    )


def simple_product(first_operand, second_operand):
    return jnp.dot(first_operand, second_operand, preferred_element_type=jnp.float32)


def remote(source, target, send_sem, recv_sem, peer, axis="tensor"):
    return pltpu.make_async_remote_copy(
        src_ref=source,
        dst_ref=target,
        send_sem=send_sem,
        recv_sem=recv_sem,
        device_id={axis: peer},
        device_id_type=MESH,
    )


def greet(peers):
    barrier = pltpu.get_barrier_semaphore()
    for axis, peer in peers:
        pl.semaphore_signal(barrier, inc=1, device_id={axis: peer}, device_id_type=MESH)
    pl.semaphore_wait(barrier, len(peers))


def square_peers(me):
    column = lax.rem(me, 2)
    row = me // 2
    return row * 2 + (1 - column), (1 - row) * 2 + column, (1 - row) * 2 + (1 - column)


def neighbours(size):
    if size == 4:
        beside, below, _ = square_peers(lax.axis_index("tensor"))
        return [("tensor", beside), ("tensor", below)]
    return [("tensor", peer) for peer in other_members("tensor", size)]


def other_members(axis, count):
    me = lax.axis_index(axis)
    return [lax.rem(me + step, count) for step in range(1, count)]


class Gather:
    def __init__(
        self, size, own_ref, out_ref, turned_out_ref, held_ref, turned_ref, send_sem, recv_sem, local_sem, turned_sem
    ):
        self.size, self.own, self.out, self.held = size, own_ref, out_ref, held_ref
        self.turned_out, self.turned = turned_out_ref, turned_ref
        self.send_sem, self.recv_sem, self.local_sem = send_sem, recv_sem, local_sem
        self.turned_sem = turned_sem
        self.me = lax.axis_index("tensor")
        self.rows = own_ref.shape[0]
        self.copies, self.stores, self.turns = [], [], []

    @staticmethod
    def scratch(size, rows, columns):
        sends, local = (12, 8) if size == 4 else (size - 1, size)
        return [
            pltpu.VMEM((size, rows, columns), jnp.bfloat16),
            pltpu.VMEM((columns, size * rows), jnp.bfloat16),
            pltpu.SemaphoreType.DMA((sends,)),
            pltpu.SemaphoreType.DMA((sends,)),
            pltpu.SemaphoreType.DMA((local,)),
            pltpu.SemaphoreType.DMA((local,)),
        ]

    def send(self, source, target, peer):
        index = len(self.copies)
        copy = remote(source, target, self.send_sem.at[index], self.recv_sem.at[index], peer)
        copy.start()
        self.copies.append(copy)
        return copy

    def store(self, source, start, count):
        piece = pl.ds(pl.multiple_of(start, count), count)
        copy = pltpu.make_async_copy(source, self.out.at[piece], self.local_sem.at[len(self.stores)])
        copy.start()
        self.stores.append(copy)
        width = min(256, self.turned.shape[0])

        def turn_part(index, carry):
            columns = pl.ds(pl.multiple_of(index * width, width), width)
            self.turned[columns, piece] = source[:, columns].T
            return carry

        lax.fori_loop(0, self.turned.shape[0] // width, turn_part, 0)
        turn_copy = pltpu.make_async_copy(
            self.turned.at[:, piece], self.turned_out.at[:, piece], self.turned_sem.at[len(self.turns)]
        )
        turn_copy.start()
        self.turns.append(turn_copy)

    def quarters(self):
        quarter = self.rows // 4
        return [pl.ds(index * quarter, quarter) for index in range(4)]

    def start(self, stage):
        own, held = self.own, self.held
        if self.size != 4:
            if stage == 0:
                for peer in other_members("tensor", self.size):
                    self.send(own, held.at[self.me], peer)
            return
        beside, below, _ = square_peers(self.me)
        parts = self.quarters()
        upper, lower = parts[stage], parts[2 + stage]
        for part, peer in ((upper, beside), (lower, below), (lower, beside), (upper, below)):
            self.send(own.at[part], held.at[self.me, part], peer)

    def forward(self):
        own, held, rows = self.own, self.held, self.rows
        if self.size != 4:
            self.store(own, self.me * rows, rows)
            return
        beside, below, _ = square_peers(self.me)
        half = rows // 2
        self.store(own.at[pl.ds(0, half)], self.me * rows, half)
        self.store(own.at[pl.ds(half, half)], self.me * rows + half, half)
        parts = self.quarters()
        for stage in range(2):
            self.copies[4 * stage].wait_recv()
            self.send(held.at[beside, parts[stage]], held.at[beside, parts[stage]], below)
            self.copies[4 * stage + 1].wait_recv()
            self.send(held.at[below, parts[2 + stage]], held.at[below, parts[2 + stage]], beside)

    def finish(self):
        held, rows = self.held, self.rows
        if self.size != 4:
            for step, copy in enumerate(self.copies):
                copy.wait_recv()
                slot = lax.rem(self.me + self.size - step - 1, self.size)
                self.store(held.at[slot], slot * rows, rows)
        else:
            beside, below, across = square_peers(self.me)
            half = rows // 2
            first, second = pl.ds(0, half), pl.ds(half, half)
            self.store(held.at[beside, first], beside * rows, half)
            self.store(held.at[below, second], below * rows + half, half)
            for indices, slot, start in (
                ((2, 6), beside, half),
                ((3, 7), below, 0),
                ((8, 10), across, 0),
                ((9, 11), across, half),
            ):
                for index in indices:
                    self.copies[index].wait_recv()
                self.store(held.at[slot, pl.ds(start, half)], slot * rows + start, half)
        for copy in self.copies:
            copy.wait_send()
        for copy in self.stores + self.turns:
            copy.wait()


def gather_kernel(size, count, *refs):
    own_refs, out_refs, rest = refs[:count], refs[count : 3 * count], refs[3 * count :]
    greet(neighbours(size))
    gathers = [
        Gather(size, own_refs[k], *out_refs[2 * k : 2 * k + 2], *rest[6 * k : 6 * k + 6])
        for k in range(count)
    ]
    for gather in gathers:
        gather.start(0)
        gather.start(1)
        gather.forward()
    for gather in gathers:
        gather.finish()


def gather_rows(arrays, size, collective_id):
    count = len(arrays)
    rows, columns = arrays[0].shape
    scratch = []
    out_shape = []
    for _ in arrays:
        scratch += Gather.scratch(size, rows, columns)
        out_shape += [
            jax.ShapeDtypeStruct((size * rows, columns), jnp.bfloat16),
            jax.ShapeDtypeStruct((columns, size * rows), jnp.bfloat16),
        ]
    return pl.pallas_call(
        functools.partial(gather_kernel, size, count),
        out_shape=out_shape,
        in_specs=[pl.BlockSpec(memory_space=pltpu.VMEM)] * count,
        out_specs=[pl.BlockSpec(memory_space=pl.ANY)] * len(out_shape),
        scratch_shapes=scratch,
        compiler_params=pltpu.CompilerParams(
            collective_id=collective_id, has_side_effects=True, vmem_limit_bytes=VMEM_LIMIT
        ),
        cost_estimate=pl.CostEstimate(
            flops=0, bytes_accessed=count * 30 * size * rows * columns, transcendentals=0
        ),
        name="gather_rows",
    )(*arrays)


class Operand:
    def __init__(self, size, first_column, left_far, weight_far, left, weight, left_sem, weight_sem):
        self.left, self.weight = left, weight
        self.rows = left.shape[0] // size
        self.tile = min(512, weight.shape[0])
        self.far = left_far, weight_far
        self.first_column = first_column
        self.left_sem, self.weight_sem = left_sem, weight_sem

    @staticmethod
    def scratch(size, left, weight):
        width = left.shape[1]
        return [
            pltpu.VMEM(left.shape, left.dtype),
            pltpu.VMEM((weight.shape[0], width), weight.dtype),
            pltpu.SemaphoreType.DMA((size,)),
            pltpu.SemaphoreType.DMA((max(1, weight.shape[0] // 512),)),
        ]

    def left_copy(self, slot, owner):
        piece = pl.ds(pl.multiple_of(owner * self.rows, self.rows), self.rows)
        return pltpu.make_async_copy(self.far[0].at[piece], self.left.at[piece], self.left_sem.at[slot])

    def weight_copy(self, index):
        piece = pl.ds(pl.multiple_of(index * self.tile, self.tile), self.tile)
        columns = pl.ds(self.first_column, self.left.shape[1])
        return pltpu.make_async_copy(
            self.far[1].at[piece, columns], self.weight.at[piece], self.weight_sem.at[index]
        )


def block_product(operands, start, rows, fresh, write, after):
    total = operands[0].weight.shape[0]
    tile = operands[0].tile
    start = pl.multiple_of(start, rows)

    def step(index, carry):
        @pl.when(fresh)
        def _():
            for operand in operands:
                operand.weight_copy(index).wait()

        columns = pl.ds(pl.multiple_of(index * tile, tile), tile)
        values = None
        for operand in operands:
            part = times_transposed(
                operand.left[pl.ds(start, rows), :], operand.weight[columns, :]
            )
            values = part if values is None else values + part
        write(columns, values)
        after(index)
        return carry

    lax.fori_loop(0, total // tile, step, 0)


class Scatter:
    def __init__(self, size, outgoing, *rest):
        self.size, self.outgoing = size, outgoing
        if size == 4:
            self.passing, rest = rest[0], rest[1:]
        self.arriving, self.send_sem, self.recv_sem = rest
        self.rows = outgoing.shape[1]
        self.me = lax.axis_index("tensor")
        self.stages = 2 if size == 4 else 1
        self.plan()

    @staticmethod
    def scratch(size, rows, columns):
        if size == 4:
            sends = 10
            buffers = [
                pltpu.VMEM((4, rows, columns), jnp.bfloat16),
                pltpu.VMEM((2, rows // 2, columns), jnp.bfloat16),
                pltpu.VMEM((2, rows, columns), jnp.bfloat16),
            ]
        else:
            sends = size - 1
            buffers = [
                pltpu.VMEM((size, rows, columns), jnp.bfloat16),
                pltpu.VMEM((size - 1, rows, columns), jnp.bfloat16),
            ]
        return buffers + [pltpu.SemaphoreType.DMA((sends,)), pltpu.SemaphoreType.DMA((sends,))]

    def prepare(self, index, source, target, peer):
        return remote(source, target, self.send_sem.at[index], self.recv_sem.at[index], peer)

    def plan(self):
        outgoing, arriving = self.outgoing, self.arriving
        if self.size != 4:
            self.copies = [
                self.prepare(step, outgoing.at[step], arriving.at[step], peer)
                for step, peer in enumerate(other_members("tensor", self.size))
            ]
            self.early, self.starts = (), tuple((step, step) for step in range(self.size - 1))
            return
        beside, below, _ = square_peers(self.me)
        half, quarter = self.rows // 2, self.rows // 4
        first, second = pl.ds(0, half), pl.ds(half, half)
        middle = outgoing.shape[2] // 2
        left, right = pl.ds(0, middle), pl.ds(middle, middle)
        upper = [pl.ds(stage * quarter, quarter) for stage in range(2)]
        lower = [pl.ds(half + stage * quarter, quarter) for stage in range(2)]
        everything = pl.ds(0, half)
        self.copies = [
            self.prepare(0, outgoing.at[0, first, left], self.passing.at[0, everything, left], beside),
            self.prepare(1, outgoing.at[0, second, left], self.passing.at[1, everything, left], below),
            self.prepare(2, outgoing.at[0, first, right], self.passing.at[0, everything, right], beside),
            self.prepare(3, outgoing.at[0, second, right], self.passing.at[1, everything, right], below),
            self.prepare(4, outgoing.at[1, first], arriving.at[0, first], beside),
            self.prepare(5, outgoing.at[2, second], arriving.at[1, second], below),
            self.prepare(6, outgoing.at[1, lower[0]], arriving.at[0, lower[0]], beside),
            self.prepare(7, outgoing.at[2, upper[0]], arriving.at[1, upper[0]], below),
            self.prepare(8, outgoing.at[1, lower[1]], arriving.at[0, lower[1]], beside),
            self.prepare(9, outgoing.at[2, upper[1]], arriving.at[1, upper[1]], below),
        ]
        self.early, self.starts = (0, 1), ((0, 2), (0, 3), (1, 4), (2, 5))

    def owner(self, slot):
        if self.size != 4:
            return lax.rem(self.me + slot + 1, self.size)
        beside, below, across = square_peers(self.me)
        return jnp.where(
            slot == 0, across, jnp.where(slot == 1, beside, jnp.where(slot == 2, below, self.me))
        )

    def load(self, operands):
        tiles = operands[0].weight.shape[0] // operands[0].tile
        for operand in operands:
            operand.left_copy(0, self.owner(0)).start()
        for index in range(tiles):
            for operand in operands:
                operand.weight_copy(index).start()
        for slot in range(1, self.size):
            for operand in operands:
                operand.left_copy(slot, self.owner(slot)).start()

    def fill(self, operands, look=None, between=None):
        rows = self.rows

        def step(slot, carry):
            owner = self.owner(slot)
            for operand in operands:
                operand.left_copy(slot, owner).wait()

            def write(columns, values):
                self.outgoing[slot, :, columns] = values.astype(self.outgoing.dtype)
                if look is not None:
                    look(owner, columns, values)

            tiles = operands[0].weight.shape[0] // operands[0].tile

            def after(index):
                for early in self.early:
                    pl.when((slot == 0) & (index == max(tiles // 2, 1) - 1))(self.copies[early].start)

            block_product(operands, owner * rows, rows, slot == 0, write, after)
            for at, index in self.starts:
                pl.when(slot == at)(self.copies[index].start)
            if between is not None:
                pl.when(slot == 0)(between)
            return carry

        lax.fori_loop(0, self.size, step, 0)

    def relay(self):
        if self.size != 4:
            return
        half, quarter = self.rows // 2, self.rows // 4
        for stage in range(2):
            for arrivals, source, slot, start, onward in (
                ((1, 3), 1, 1, half, 6 + 2 * stage),
                ((0, 2), 0, 2, 0, 7 + 2 * stage),
            ):
                if stage == 0:
                    for index in arrivals:
                        self.copies[index].wait_recv()
                piece = pl.ds(start + stage * quarter, quarter)
                self.outgoing[slot, piece, :] = add_rounded(
                    self.outgoing[slot, piece, :],
                    self.passing[source, stage * quarter : (stage + 1) * quarter, :],
                )
                self.copies[onward].start()

    def collect(self, stage):
        if self.size != 4:
            for copy in self.copies:
                copy.wait_recv()
            return
        if stage == 0:
            self.copies[4].wait_recv()
            self.copies[5].wait_recv()
        self.copies[6 + 2 * stage].wait_recv()
        self.copies[7 + 2 * stage].wait_recv()

    def over_rows(self, stage, body):
        if self.size != 4:
            over_pieces(self.rows, body)
            return
        half, quarter = self.rows // 2, self.rows // 4
        over_pieces(quarter, body, stage * quarter)
        over_pieces(quarter, body, half + stage * quarter)

    def over_stages(self, body, done=None):
        for stage in range(self.stages):
            self.collect(stage)
            self.over_rows(stage, body)
            if done is not None:
                done(stage)

    def total(self, piece):
        total = self.outgoing[self.size - 1, piece, :].astype(jnp.float32)
        for index in range(self.arriving.shape[0]):
            total = total + self.arriving[index, piece, :].astype(jnp.float32)
        return total

    def drain(self):
        for copy in self.copies:
            copy.wait_send()


class Chain:
    def __init__(
        self, chips, steps, rising_refs, falling_refs, up_ref, down_ref,
        rise, fall, up, down, load_sem, send_sem, recv_sem,
    ):
        self.chips, self.steps = chips, steps
        self.rise, self.fall, self.up, self.down = rise, fall, up, down
        device = lax.axis_index("dp")
        self.chip = device // 2
        count = len(steps)
        self.loads = [
            pltpu.make_async_copy(source, target, load_sem.at[index])
            for index, (source, target) in enumerate(
                [(up_ref, up.at[0]), (down_ref, down.at[0])]
                + [(ref, rise.at[index]) for index, ref in enumerate(rising_refs)]
                + [(ref, fall.at[index]) for index, ref in enumerate(falling_refs)]
            )
        ]
        above = lax.rem(device + 2, 2 * chips)
        under = lax.rem(device + 2 * chips - 2, 2 * chips)
        self.neighbours = [("dp", above), ("dp", under)]
        self.rises = [
            remote(rise.at[i], up.at[i + 1], send_sem.at[i], recv_sem.at[i], above, "dp")
            for i in range(count)
        ]
        self.falls = [
            remote(
                fall.at[i], down.at[i + 1], send_sem.at[count + i], recv_sem.at[count + i], under, "dp"
            )
            for i in range(count)
        ]

    @staticmethod
    def scratch(count, rows, columns):
        return [
            pltpu.VMEM((count, rows, columns), jnp.bfloat16),
            pltpu.VMEM((count, rows, columns), jnp.bfloat16),
            pltpu.VMEM((count + 1, rows, columns), jnp.bfloat16),
            pltpu.VMEM((count + 1, rows, columns), jnp.bfloat16),
            pltpu.SemaphoreType.DMA((2 * count + 2,)),
            pltpu.SemaphoreType.DMA((2 * count,)),
            pltpu.SemaphoreType.DMA((2 * count,)),
        ]

    def load(self):
        for copy in self.loads:
            copy.start()

    def step(self, index):
        if index == 0:
            for copy in self.loads:
                copy.wait()
        step = self.steps[index]
        rows = self.rise.shape[1]
        sends_up = self.chip < step
        sends_down = self.chip >= self.chips - step

        @pl.when(sends_up & (self.chip > 0))
        def _():
            def add(piece):
                self.rise[index, piece, :] = add_rounded(
                    self.rise[index, piece, :], self.up[index, piece, :]
                )

            over_pieces(rows, add)

        pl.when(sends_up)(self.rises[index].start)

        @pl.when(sends_down & (self.chip < self.chips - 1))
        def _():
            def add(piece):
                self.fall[index, piece, :] = add_rounded(
                    self.fall[index, piece, :], self.down[index, piece, :]
                )

            over_pieces(rows, add)

        pl.when(sends_down)(self.falls[index].start)

    def arrives(self, index):
        step = self.steps[index]
        from_under = (self.chip > 0) & (self.chip <= step)
        from_above = (self.chip < self.chips - 1) & (self.chip >= self.chips - step - 1)
        return from_under, from_above

    def wait(self, index):
        from_under, from_above = self.arrives(index)
        pl.when(from_under)(self.rises[index].wait_recv)
        pl.when(from_above)(self.falls[index].wait_recv)

    def advance(self, index):
        self.wait(index - 1)
        self.step(index)

    def add_last(self, total_ref):
        last = len(self.steps)
        self.wait(last - 1)
        for arrived, landing in zip(self.arrives(last - 1), (self.up, self.down)):

            @pl.when(arrived)
            def _(landing=landing):
                def add(piece):
                    total_ref[piece, :] = add_rounded(total_ref[piece, :], landing[last, piece, :])

                over_pieces(total_ref.shape[0], add)

    def drain(self):
        for index, step in enumerate(self.steps):
            pl.when(self.chip < step)(self.rises[index].wait_send)
            pl.when(self.chip >= self.chips - step)(self.falls[index].wait_send)


def add_rounded(first, second):
    return (first.astype(jnp.float32) + second.astype(jnp.float32)).astype(jnp.bfloat16)


def over_pieces(rows, body, start=0):
    count = min(32, rows)

    def step(index, carry):
        body(pl.ds(pl.multiple_of(start + index * count, count), count))
        return carry

    lax.fori_loop(0, rows // count, step, 0)


def send_terms(axis, peers, source, landing, send_sem, recv_sem):
    me = lax.axis_index(axis)
    landing[me] = source[...]
    copies = []
    for step, peer in enumerate(peers):
        copy = remote(source, landing.at[me], send_sem.at[step], recv_sem.at[step], peer, axis)
        copy.start()
        copies.append(copy)
    return copies


def add_terms(landing, copies):
    for copy in copies:
        copy.wait_recv()
    total = landing[0]
    for index in range(1, landing.shape[0]):
        total = total + landing[index]
    return total


def split_operands(refs, size, first_columns):
    count = len(first_columns)
    far, refs, scratch = refs[: 2 * count], refs[2 * count : -4 * count], refs[-4 * count :]
    operands = [
        Operand(size, first, *far[2 * p : 2 * p + 2], *scratch[4 * p : 4 * p + 4])
        for p, first in enumerate(first_columns)
    ]
    return operands, refs


def store_row(target_ref, row_ref):
    width = target_ref.shape[1]
    for index in range(row_ref.shape[1] // width):
        target_ref[index : index + 1, :] = row_ref[:, index * width : (index + 1) * width]


def between_forward_kernel(size, first_columns, *refs):
    operands, refs = split_operands(refs, size, first_columns)
    input_ref, gain_ref, gathered_ref, turned_ref, state_ref, own_ref = refs[:6]
    buffers = 5 if size == 4 else 4
    scatter = Scatter(size, *refs[6 : 6 + buffers])
    gather = Gather(size, own_ref, gathered_ref, turned_ref, *refs[6 + buffers :])
    scatter.load(operands)
    greet(neighbours(size))
    scatter.fill(operands)
    scatter.relay()

    def norm(piece):
        state = input_ref[piece, :].astype(jnp.float32) + scatter.total(piece)
        state_ref[piece, :] = state
        own_ref[piece, :] = (state * row_scale(state) * gain_ref[...]).astype(own_ref.dtype)

    scatter.over_stages(norm, gather.start)
    gather.forward()
    gather.finish()
    scatter.drain()


def between_backward_kernel(size, chips, first_columns, *refs):
    operands, refs = split_operands(refs, size, first_columns)
    state_ref, cotangent_ref, gain_ref = refs[:3]
    steps = tuple(range(2, chips))
    chain_count = 2 * len(steps) + 2
    chain_refs, own_block_ref, refs = refs[3 : 3 + chain_count], refs[3 + chain_count], refs[4 + chain_count :]
    gathered_ref, gathered_turned_ref, slope_ref, term_ref, chain_total_ref = refs[:5]
    own_ref, sum_ref, own_sem = refs[5:8]
    buffers = 5 if size == 4 else 4
    scatter = Scatter(size, *refs[8 : 8 + buffers])
    gather = Gather(size, own_ref, gathered_ref, gathered_turned_ref, *refs[8 + buffers : 14 + buffers])
    chain = Chain(
        chips, steps, chain_refs[: len(steps)], chain_refs[len(steps) : -2], *chain_refs[-2:],
        *refs[14 + buffers :],
    )
    own_load = pltpu.make_async_copy(own_block_ref, chain_total_ref, own_sem.at[0])
    chain.load()
    scatter.load(operands)
    own_load.start()
    greet(neighbours(size) + chain.neighbours)
    scatter.fill(operands, between=lambda: chain.step(0))
    scatter.relay()
    sum_ref[...] = jnp.zeros_like(sum_ref)

    def norm(piece):
        back = scatter.total(piece)
        state = state_ref[piece, :]
        scale = row_scale(state)
        unit = state * scale
        sum_ref[...] += jnp.sum(back * unit, axis=0, keepdims=True)
        unit_slope = back * gain_ref[...]
        slope = cotangent_ref[piece, :].astype(jnp.float32) + scale * (
            unit_slope - unit * jnp.mean(unit_slope * unit, axis=-1, keepdims=True)
        )
        slope_ref[piece, :] = slope
        own_ref[piece, :] = slope.astype(own_ref.dtype)

    def done(stage):
        gather.start(stage)
        if stage == 0 and len(steps) > 1:
            chain.advance(1)

    scatter.over_stages(norm, done)
    store_row(term_ref, sum_ref)
    gather.forward()
    for index in range(2, len(steps)):
        chain.advance(index)
    gather.finish()
    own_load.wait()
    chain.add_last(chain_total_ref)
    scatter.drain()
    chain.drain()


def last_kernel(sizes, first_columns, *refs):
    data_size, size = sizes
    operands, refs = split_operands(refs, size, first_columns)
    input_ref, gain_ref, slope_ref, terms_ref, rows_ref = refs[:5]
    chips = data_size // 2
    steps = tuple(range(1, chips))
    chain_count = 2 * len(steps) + 2
    chain_refs, own_block_ref, refs = refs[5 : 5 + chain_count], refs[5 + chain_count], refs[6 + chain_count :]
    gradient_ref, terms_out_ref, chain_total_ref, sum_ref, partial_ref, group_ref, inner, outer = refs[:8]
    inner_send, inner_recv, outer_send, outer_recv, own_sem = refs[8:13]
    buffers = 5 if size == 4 else 4
    mixing = Scatter(size, *refs[13 : 13 + buffers])
    chain = Chain(
        chips, steps, chain_refs[: len(steps)], chain_refs[len(steps) : -2], *chain_refs[-2:],
        *refs[13 + buffers :],
    )
    own_load = pltpu.make_async_copy(own_block_ref, chain_total_ref, own_sem.at[0])
    rows = gradient_ref.shape[0]
    chain.load()
    mixing.load(operands)
    own_load.start()
    greet(
        [("tensor", peer) for peer in other_members("tensor", size)]
        + [("dp", peer) for peer in other_members("dp", data_size)]
    )
    sum_ref[...] = jnp.zeros_like(sum_ref)

    def look(owner, columns, values):
        piece = pl.ds(pl.multiple_of(owner * rows, rows), rows)
        sum_ref[:, columns] += jnp.sum(
            values * rows_ref[piece, columns].astype(jnp.float32), axis=0, keepdims=True
        )

    mixing.fill(operands, look, lambda: chain.step(0))
    sum_ref[...] = sum_ref[...] / gain_ref[...]
    kept = partial_ref.shape[0] - terms_ref.shape[0]
    partial_ref[kept:, :] = terms_ref[...]
    store_row(partial_ref, sum_ref)
    inner_copies = send_terms(
        "tensor", other_members("tensor", size), partial_ref, inner, inner_send, inner_recv
    )
    mixing.relay()
    chain.advance(1)
    group_ref[...] = add_terms(inner, inner_copies)
    outer_copies = send_terms(
        "dp", other_members("dp", data_size), group_ref, outer, outer_send, outer_recv
    )
    terms_out_ref[...] = add_terms(outer, outer_copies)

    def norm(piece):
        back = mixing.total(piece)
        values = input_ref[piece, :].astype(jnp.float32)
        scale = row_scale(values)
        unit = values * scale
        unit_slope = back * gain_ref[...]
        gradient_ref[piece, :] = (
            slope_ref[piece, :]
            + scale * (unit_slope - unit * jnp.mean(unit_slope * unit, axis=-1, keepdims=True))
        ).astype(gradient_ref.dtype)

    for index in range(2, len(steps)):
        chain.advance(index)
    mixing.over_stages(norm)
    own_load.wait()
    chain.add_last(chain_total_ref)
    chain.drain()
    for copy in inner_copies + outer_copies:
        copy.wait_send()
    mixing.drain()


def scatter_call(body, triples, size, others, far, outs, gathered, scratch, collective_id):
    far_spec = pl.BlockSpec(memory_space=pl.ANY)
    operands = [array for left, weight, _ in triples for array in (left, weight)]
    in_specs = [far_spec] * len(operands)
    for other in others:
        in_specs.append(pl.BlockSpec(other.shape, lambda i: (0, 0), pipeline_mode=pl.Buffered(1)))
    in_specs += [far_spec] * len(far)
    out_specs = [pl.BlockSpec(out.shape, lambda i: (0, 0)) for out in outs]
    if gathered:
        out_specs[:2] = [far_spec] * 2
    return pl.pallas_call(
        functools.partial(body, tuple(first for _, _, first in triples)),
        grid=(1,),
        out_shape=outs,
        in_specs=in_specs,
        out_specs=out_specs,
        scratch_shapes=list(scratch)
        + [part for left, weight, _ in triples for part in Operand.scratch(size, left, weight)],
        compiler_params=pltpu.CompilerParams(
            collective_id=collective_id, has_side_effects=True, vmem_limit_bytes=VMEM_LIMIT
        ),
        cost_estimate=pl.CostEstimate(
            flops=sum(2 * left.size * weight.shape[0] for left, weight, _ in triples),
            bytes_accessed=150_000_000,
            transcendentals=0,
        ),
    )(*operands, *others, *far)


LOG2E = 1.4426950408889634


def turn_tables(head_size):
    half_size = head_size // 2
    frequency = np.float32(rope_base) ** (
        -(np.arange(half_size, dtype=np.float32) * np.float32(2.0) / np.float32(head_size))
    )
    frequency = frequency.astype(np.float64)
    sign = np.concatenate([-np.ones(half_size), np.ones(half_size)])[None, :]
    positions = np.concatenate([np.arange(0, SEQUENCE_LENGTH, 128), np.arange(128)])
    angles = positions[:, None] * np.concatenate([frequency, frequency])[None, :]
    return np.cos(angles).astype(np.float32), (sign * np.sin(angles)).astype(np.float32)


def fill_tables(few_cosines_ref, few_sines_ref, cosine_ref, sine_ref):
    coarse = few_cosines_ref.shape[0] - 128
    near_cosine, near_sine = few_cosines_ref[coarse:, :], few_sines_ref[coarse:, :]

    def step(index, carry):
        far_cosine = few_cosines_ref[pl.ds(index, 1), :]
        far_sine = few_sines_ref[pl.ds(index, 1), :]
        rows = pl.ds(pl.multiple_of(index * 128, 128), 128)
        cosine_ref[rows, :] = far_cosine * near_cosine - far_sine * near_sine
        sine_ref[rows, :] = far_sine * near_cosine + far_cosine * near_sine
        return carry

    lax.fori_loop(0, coarse, step, 0)


def turn(values, cosine, sine):
    return values * cosine + pltpu.roll(values, values.shape[-1] // 2, 1) * sine


def turn_back(values, cosine, sine):
    return values * cosine - pltpu.roll(values, values.shape[-1] // 2, 1) * sine


def contract_first(first_operand, second_operand):
    return lax.dot_general(
        first_operand, second_operand, (((0,), (0,)), ((), ())), preferred_element_type=jnp.float32
    )


def visible_scores(key_rows, query_rows, first_row, multiplier):
    scores = times_transposed(key_rows, query_rows) * multiplier
    _, queries = scores.shape
    key_at = lax.broadcasted_iota(jnp.int32, (queries, queries), 0)
    query_at = lax.broadcasted_iota(jnp.int32, (queries, queries), 1)
    corner = jnp.where(query_at >= key_at, scores[first_row:], -1e30)
    if first_row == 0:
        return corner
    return jnp.concatenate([scores[:first_row], corner], axis=0)


def turn_heads(
    grouping, head_size, raw_ref, query_gain_ref, key_gain_ref, cosine_ref, sine_ref, query_ref, key_ref, value_ref
):
    def turned(start, gain):
        raw = raw_ref[:, pl.ds(start, head_size)]
        return turn(raw * row_scale(raw) * gain, cosine_ref[...], sine_ref[...]).astype(jnp.bfloat16)

    def step(part, carry):
        query_ref[part] = turned(pl.multiple_of(part * head_size, head_size), query_gain_ref[...])
        return carry

    lax.fori_loop(0, grouping, step, 0)
    key_ref[...] = turned(grouping * head_size, key_gain_ref[...])
    value_ref[...] = raw_ref[:, (grouping + 1) * head_size :].astype(jnp.bfloat16)


def attention_forward_kernel(
    grouping, head_size, block, rows_ref, weight_ref, few_cosines_ref, few_sines_ref, query_gain_ref, key_gain_ref,
    raw_ref, mixed_ref, total_ref, query_ref, key_ref, value_ref, cosine_ref, sine_ref,
):
    sequence = rows_ref.shape[0]
    multiplier = head_size ** (-0.5) * LOG2E

    @pl.when((pl.program_id(0) == 0) & (pl.program_id(1) == 0))
    def _():
        fill_tables(few_cosines_ref, few_sines_ref, cosine_ref, sine_ref)

    raw_ref[...] = simple_product(rows_ref[...], weight_ref[...])
    turn_heads(
        grouping, head_size, raw_ref, query_gain_ref, key_gain_ref, cosine_ref, sine_ref, query_ref, key_ref, value_ref
    )

    def head_step(part, carry):
        lanes = pl.ds(pl.multiple_of(part * head_size, head_size), head_size)
        for first_row in range(0, sequence, block):
            last_row = first_row + block
            scores = visible_scores(
                key_ref[:last_row, :], query_ref[part, first_row:last_row, :], first_row, multiplier
            )
            highest = jnp.max(scores, axis=0, keepdims=True)
            weights = jnp.exp2(scores - highest)
            total = jnp.sum(weights, axis=0, keepdims=True)
            weights = (weights * (1.0 / total)).astype(jnp.bfloat16)
            mixed_ref[first_row:last_row, lanes] = contract_first(
                weights, value_ref[:last_row, :]
            ).astype(mixed_ref.dtype)
            total_ref[0, pl.ds(part, 1), first_row:last_row] = highest + jnp.log2(total)
        return carry

    lax.fori_loop(0, grouping, head_step, 0)


def attention_forward(rows, weight, tables, query_gain, key_gain, heads, grouping):
    total_rows, depth = rows.shape
    head_size = query_gain.shape[0]
    sequences = total_rows // SEQUENCE_LENGTH
    width = (grouping + 2) * head_size
    block = min(256, SEQUENCE_LENGTH)
    table = pl.BlockSpec(tables[0].shape, lambda s, h: (0, 0))
    gain = pl.BlockSpec((1, head_size), lambda s, h: (0, 0))
    elements = heads * grouping * total_rows * SEQUENCE_LENGTH // 2
    return pl.pallas_call(
        functools.partial(attention_forward_kernel, grouping, head_size, block),
        grid=(sequences, heads),
        out_shape=[
            jax.ShapeDtypeStruct((total_rows, heads * width), jnp.float32),
            jax.ShapeDtypeStruct((total_rows, heads * grouping * head_size), jnp.bfloat16),
            jax.ShapeDtypeStruct((heads, grouping, total_rows), jnp.float32),
        ],
        in_specs=[
            pl.BlockSpec((SEQUENCE_LENGTH, depth), lambda s, h: (s, 0)),
            pl.BlockSpec((depth, width), lambda s, h: (0, h)),
            table,
            table,
            gain,
            gain,
        ],
        out_specs=[
            pl.BlockSpec((SEQUENCE_LENGTH, width), lambda s, h: (s, h)),
            pl.BlockSpec((SEQUENCE_LENGTH, grouping * head_size), lambda s, h: (s, h)),
            pl.BlockSpec((1, grouping, SEQUENCE_LENGTH), lambda s, h: (h, 0, s)),
        ],
        scratch_shapes=[
            pltpu.VMEM((grouping, SEQUENCE_LENGTH, head_size), jnp.bfloat16),
            pltpu.VMEM((SEQUENCE_LENGTH, head_size), jnp.bfloat16),
            pltpu.VMEM((SEQUENCE_LENGTH, head_size), jnp.bfloat16),
            pltpu.VMEM((SEQUENCE_LENGTH, head_size), jnp.float32),
            pltpu.VMEM((SEQUENCE_LENGTH, head_size), jnp.float32),
        ],
        compiler_params=pltpu.CompilerParams(vmem_limit_bytes=VMEM_LIMIT),
        cost_estimate=pl.CostEstimate(
            flops=2 * total_rows * depth * heads * width + 4 * elements * head_size,
            bytes_accessed=2 * (total_rows * depth + depth * heads * width),
            transcendentals=elements,
        ),
        name="attention_forward",
    )(rows, weight, *tables, query_gain.reshape(1, -1), key_gain.reshape(1, -1))


def norm_back(turned_slope, raw, gain, cosine, sine):
    norm_slope = turn_back(turned_slope, cosine, sine)
    scale = row_scale(raw)
    unit = raw * scale
    term = norm_slope * unit
    unit_slope = norm_slope * gain
    slope = scale * (unit_slope - unit * jnp.mean(unit_slope * unit, axis=-1, keepdims=True))
    return slope.astype(jnp.bfloat16), jnp.sum(term, axis=0, keepdims=True)


def attention_backward_kernel(size, grouping, head_size, block, first_columns, *refs):
    operands, refs = split_operands(refs, size, first_columns)
    (
        state_ref, weight_ref, raw_ref, mixed_ref, total_ref, few_cosines_ref, few_sines_ref,
        query_gain_ref, key_gain_ref, hidden_state_ref, slope_ref, gain_ref, output_ref,
        query_ref, key_ref, value_ref, out_slope_ref, turned_ref, key_sum_ref, value_sum_ref, cosine_ref, sine_ref,
    ) = refs[:22]
    scatter = Scatter(size, *refs[22:])
    step = pl.program_id(0) * pl.num_programs(1) + pl.program_id(1)
    steps = pl.num_programs(0) * pl.num_programs(1)

    @pl.when(step == 0)
    def _():
        scatter.load(operands)
        greet(neighbours(size))
        scatter.fill(operands)

    attend_backward_head(
        grouping, head_size, block, state_ref, weight_ref, raw_ref, mixed_ref, total_ref, few_cosines_ref,
        few_sines_ref, query_gain_ref, key_gain_ref, slope_ref, gain_ref, query_ref, key_ref, value_ref,
        out_slope_ref, turned_ref, key_sum_ref, value_sum_ref, cosine_ref, sine_ref,
    )

    @pl.when(step == 0)
    def _():
        scatter.relay()

    @pl.when(step == steps - 1)
    def _():
        def finish(piece):
            output_ref[piece, :] = (hidden_state_ref[piece, :] + scatter.total(piece)).astype(
                output_ref.dtype
            )

        scatter.over_stages(finish)
        scatter.drain()


def attend_backward_head(
    grouping, head_size, block, state_ref, weight_ref, raw_ref, mixed_ref, total_ref, few_cosines_ref, few_sines_ref,
    query_gain_ref, key_gain_ref, slope_ref, gain_ref, query_ref, key_ref, value_ref, out_slope_ref,
    turned_ref, key_sum_ref, value_sum_ref, cosine_ref, sine_ref,
):
    sequence = state_ref.shape[0]
    scale_factor = head_size ** (-0.5)
    multiplier = scale_factor * LOG2E

    @pl.when((pl.program_id(0) == 0) & (pl.program_id(1) == 0))
    def _():
        gain_ref[...] = jnp.zeros_like(gain_ref)
        fill_tables(few_cosines_ref, few_sines_ref, cosine_ref, sine_ref)

    out_slope_ref[...] = simple_product(state_ref[...], weight_ref[...]).astype(jnp.bfloat16)
    turn_heads(
        grouping, head_size, raw_ref, query_gain_ref, key_gain_ref, cosine_ref, sine_ref, query_ref, key_ref, value_ref
    )
    key_sum_ref[...] = jnp.zeros_like(key_sum_ref)
    value_sum_ref[...] = jnp.zeros_like(value_sum_ref)
    ones = jnp.ones((8, head_size), jnp.float32)

    def head_step(part, carry):
        lanes = pl.ds(pl.multiple_of(part * head_size, head_size), head_size)
        for first_row in range(0, sequence, block):
            last_row = first_row + block
            query_rows = query_ref[part, first_row:last_row, :]
            slope_rows = out_slope_ref[first_row:last_row, lanes]
            scores = visible_scores(key_ref[:last_row, :], query_rows, first_row, multiplier)
            weights = jnp.exp2(scores - total_ref[0, pl.ds(part, 1), first_row:last_row])
            value_sum_ref[:last_row, :] += simple_product(weights.astype(jnp.bfloat16), slope_rows)
            product = slope_rows.astype(jnp.float32) * mixed_ref[first_row:last_row, lanes].astype(jnp.float32)
            centre = lax.dot_general(
                ones,
                product,
                (((1,), (1,)), ((), ())),
                preferred_element_type=jnp.float32,
                precision=lax.Precision.HIGHEST,
            )[:1]
            weight_slope = times_transposed(value_ref[:last_row, :], slope_rows)
            score_slope = (weights * (weight_slope - centre)).astype(jnp.bfloat16)
            key_sum_ref[:last_row, :] += simple_product(score_slope, query_rows)
            turned_ref[first_row:last_row, :] = (
                contract_first(score_slope, key_ref[:last_row, :]) * scale_factor
            )
        slope, term = norm_back(
            turned_ref[...], raw_ref[:, lanes], query_gain_ref[...], cosine_ref[...], sine_ref[...]
        )
        slope_ref[:, lanes] = slope
        gain_ref[0:1, :] += term
        return carry

    lax.fori_loop(0, grouping, head_step, 0)
    lanes = slice(grouping * head_size, (grouping + 1) * head_size)
    slope, term = norm_back(
        key_sum_ref[...] * scale_factor, raw_ref[:, lanes], key_gain_ref[...], cosine_ref[...], sine_ref[...]
    )
    slope_ref[:, lanes] = slope
    gain_ref[1:2, :] += term
    slope_ref[:, (grouping + 1) * head_size :] = value_sum_ref[...].astype(jnp.bfloat16)


def attention_backward(
    state_rows, weight, weight_start, raw, mixed, totals, tables, query_gain, key_gain, heads, grouping,
    triples, hidden_state, size, collective_id,
):
    total_rows, depth = state_rows.shape
    head_size = query_gain.shape[0]
    sequences = total_rows // SEQUENCE_LENGTH
    width = (grouping + 2) * head_size
    out_width = grouping * head_size
    block = min(256, SEQUENCE_LENGTH)
    first_block = weight_start // out_width
    single = pl.Buffered(1)
    table = pl.BlockSpec(tables[0].shape, lambda s, h: (0, 0))
    gain = pl.BlockSpec((1, head_size), lambda s, h: (0, 0))
    elements = heads * grouping * total_rows * SEQUENCE_LENGTH // 2
    whole_rows = pltpu.VMEM((SEQUENCE_LENGTH, head_size), jnp.float32)
    operands = [array for left, other_weight, _ in triples for array in (left, other_weight)]
    in_specs = [pl.BlockSpec(memory_space=pl.ANY)] * len(operands)
    in_specs += [
        pl.BlockSpec((SEQUENCE_LENGTH, depth), lambda s, h: (s, 0), pipeline_mode=single),
        pl.BlockSpec((depth, out_width), lambda s, h: (0, first_block + h)),
        pl.BlockSpec((SEQUENCE_LENGTH, width), lambda s, h: (s, h)),
        pl.BlockSpec((SEQUENCE_LENGTH, out_width), lambda s, h: (s, h)),
        pl.BlockSpec((1, grouping, SEQUENCE_LENGTH), lambda s, h: (h, 0, s)),
        table,
        table,
        gain,
        gain,
        pl.BlockSpec(hidden_state.shape, lambda s, h: (0, 0), pipeline_mode=single),
    ]
    operands += [
        state_rows, weight, raw, mixed, totals, *tables, query_gain.reshape(1, -1), key_gain.reshape(1, -1),
        hidden_state,
    ]
    return pl.pallas_call(
        functools.partial(
            attention_backward_kernel, size, grouping, head_size, block,
            tuple(first for _, _, first in triples),
        ),
        grid=(sequences, heads),
        out_shape=[
            jax.ShapeDtypeStruct((total_rows, heads * width), jnp.bfloat16),
            jax.ShapeDtypeStruct((8, head_size), jnp.float32),
            jax.ShapeDtypeStruct(hidden_state.shape, jnp.bfloat16),
        ],
        in_specs=in_specs,
        out_specs=[
            pl.BlockSpec((SEQUENCE_LENGTH, width), lambda s, h: (s, h)),
            pl.BlockSpec((8, head_size), lambda s, h: (0, 0)),
            pl.BlockSpec(hidden_state.shape, lambda s, h: (0, 0)),
        ],
        scratch_shapes=[
            pltpu.VMEM((grouping, SEQUENCE_LENGTH, head_size), jnp.bfloat16),
            pltpu.VMEM((SEQUENCE_LENGTH, head_size), jnp.bfloat16),
            pltpu.VMEM((SEQUENCE_LENGTH, head_size), jnp.bfloat16),
            pltpu.VMEM((SEQUENCE_LENGTH, out_width), jnp.bfloat16),
            whole_rows,
            whole_rows,
            whole_rows,
            whole_rows,
            whole_rows,
            *Scatter.scratch(size, *hidden_state.shape),
            *[part for left, other, _ in triples for part in Operand.scratch(size, left, other)],
        ],
        compiler_params=pltpu.CompilerParams(
            collective_id=collective_id, has_side_effects=True, vmem_limit_bytes=VMEM_LIMIT
        ),
        cost_estimate=pl.CostEstimate(
            flops=2 * total_rows * depth * heads * out_width + 10 * elements * head_size,
            bytes_accessed=100_000_000,
            transcendentals=elements,
        ),
        name="attention_backward",
    )(*operands)


def feed_half_kernel(
    half, tile, block, rows_far, cotangent_far, weight_far, hidden_far, slope_far,
    rows_ref, cotangent_ref, weight_ref, hidden_ref, slope_ref, row_sem, weight_sem, out_sem,
):
    total = rows_ref.shape[0]
    blocks = total // block
    tiles = half // tile

    def row_copies(index):
        piece = pl.ds(pl.multiple_of(index * block, block), block)
        return [
            pltpu.make_async_copy(far.at[piece], ref.at[piece], row_sem.at[at, index])
            for at, (far, ref) in enumerate(((rows_far, rows_ref), (cotangent_far, cotangent_ref)))
        ]

    def weight_copies(index):
        copies = []
        for part in range(3):
            columns = pl.ds(pl.multiple_of(part * half + index * tile, tile), tile)
            copies.append(
                pltpu.make_async_copy(
                    weight_far.at[:, columns], weight_ref.at[part, index], weight_sem.at[part, index]
                )
            )
        return copies

    def out_copies(index):
        piece = pl.ds(pl.multiple_of(index * block, block), block)
        return [
            pltpu.make_async_copy(ref.at[piece], far.at[piece], out_sem.at[at, index])
            for at, (far, ref) in enumerate(((hidden_far, hidden_ref), (slope_far, slope_ref)))
        ]

    for copy in row_copies(0) + weight_copies(0):
        copy.start()
    for index in range(1, tiles):
        for copy in weight_copies(index):
            copy.start()
    for index in range(1, blocks):
        for copy in row_copies(index):
            copy.start()

    def row_step(row_index, carry):
        piece = pl.ds(pl.multiple_of(row_index * block, block), block)
        for copy in row_copies(row_index):
            copy.wait()

        def step(index, carry):
            @pl.when(row_index == 0)
            def _():
                for copy in weight_copies(index):
                    copy.wait()

            start = pl.multiple_of(index * tile, tile)
            rows = rows_ref[piece, :]
            gate = simple_product(rows, weight_ref[0, index])
            up = simple_product(rows, weight_ref[1, index])
            back = simple_product(cotangent_ref[piece, :], weight_ref[2, index])
            sigmoid = 1.0 / (1.0 + jnp.exp(-gate))
            gated = gate * sigmoid
            hidden_ref[piece, pl.ds(start, tile)] = (gated * up).astype(jnp.bfloat16)
            slope_ref[piece, pl.ds(start, tile)] = (
                back * up * sigmoid * (1.0 + gate * (1.0 - sigmoid))
            ).astype(jnp.bfloat16)
            slope_ref[piece, pl.ds(half + start, tile)] = (back * gated).astype(jnp.bfloat16)
            return carry

        lax.fori_loop(0, tiles, step, 0)
        for copy in out_copies(row_index):
            copy.start()
        return carry

    lax.fori_loop(0, blocks, row_step, 0)
    for index in range(blocks):
        for copy in out_copies(index):
            copy.wait()


def feed_half(rows, cotangent, weight):
    total_rows, depth = rows.shape
    block = min(512, total_rows)
    half = weight.shape[1] // 3
    tile = 256 if half % 256 == 0 else 128
    blocks, tiles = total_rows // block, half // tile
    far = pl.BlockSpec(memory_space=pl.ANY)
    return pl.pallas_call(
        functools.partial(feed_half_kernel, half, tile, block),
        out_shape=[
            jax.ShapeDtypeStruct((total_rows, half), jnp.bfloat16),
            jax.ShapeDtypeStruct((total_rows, 2 * half), jnp.bfloat16),
        ],
        in_specs=[far] * 3,
        out_specs=[far] * 2,
        scratch_shapes=[
            pltpu.VMEM(rows.shape, rows.dtype),
            pltpu.VMEM(rows.shape, rows.dtype),
            pltpu.VMEM((3, tiles, depth, tile), weight.dtype),
            pltpu.VMEM((total_rows, half), jnp.bfloat16),
            pltpu.VMEM((total_rows, 2 * half), jnp.bfloat16),
            pltpu.SemaphoreType.DMA((2, blocks)),
            pltpu.SemaphoreType.DMA((3, tiles)),
            pltpu.SemaphoreType.DMA((2, blocks)),
        ],
        compiler_params=pltpu.CompilerParams(vmem_limit_bytes=VMEM_LIMIT),
        cost_estimate=pl.CostEstimate(
            flops=6 * total_rows * depth * half,
            bytes_accessed=2 * (2 * total_rows * depth + 3 * depth * half),
            transcendentals=total_rows * half,
        ),
        name="feed_half",
    )(rows, cotangent, weight)


def grad_kernel(pair_count, *refs):
    pairs = [refs[2 * p : 2 * p + 2] for p in range(pair_count)]
    out_ref = refs[-1]
    start = 0
    for left_ref, right_ref in pairs:
        width = right_ref.shape[1]
        tile = next(t for t in (768, 512, 384, 256, 128) if width % t == 0)
        for column in range(0, width, tile):
            values = simple_product(left_ref[...], right_ref[:, column : column + tile])
            out_ref[:, start + column : start + column + tile] = values.astype(jnp.bfloat16)
        start += width


def grad_blocks(pairs, rows):
    depth, total_rows = pairs[0][0].shape
    width = sum(right.shape[1] for _, right in pairs)
    in_specs = []
    operands = []
    for left, right in pairs:
        in_specs += [
            pl.BlockSpec((rows, total_rows), lambda k: (k, 0)),
            pl.BlockSpec(right.shape, lambda k: (0, 0), pipeline_mode=pl.Buffered(1)),
        ]
        operands += [left, right]
    return pl.pallas_call(
        functools.partial(grad_kernel, len(pairs)),
        grid=(depth // rows,),
        in_specs=in_specs,
        out_specs=pl.BlockSpec((rows, width), lambda k: (k, 0)),
        out_shape=jax.ShapeDtypeStruct((depth, width), jnp.bfloat16),
        compiler_params=pltpu.CompilerParams(vmem_limit_bytes=VMEM_LIMIT),
        cost_estimate=pl.CostEstimate(
            flops=2 * total_rows * depth * width,
            bytes_accessed=2 * (total_rows * depth * len(pairs) + width * (total_rows + depth)),
            transcendentals=0,
        ),
        name="grad_blocks",
    )(*operands)


def pair_grad_kernel(chips, pair_count, *refs):
    lefts, rights = refs[:pair_count], refs[pair_count : 2 * pair_count]
    out_refs = refs[2 * pair_count : 2 * pair_count + chips]
    held = refs[2 * pair_count + chips : -6]
    sent, landed, left_sem, send_sem, recv_sem, out_sem = refs[-6:]
    block = sent.shape[1]
    device = lax.axis_index("dp")
    chip, core = device // 2, lax.rem(device, 2)
    other = chip * 2 + 1 - core

    def loads(index):
        owner = lax.rem(chip + lax.rem(index, chips), chips) * 2
        owner = owner + jnp.where(index < chips, 1 - core, core)
        piece = pl.ds(pl.multiple_of(owner * block, block), block)
        slot = lax.rem(index, 2)
        return [
            pltpu.make_async_copy(left.at[piece], hold.at[slot], left_sem.at[at, slot])
            for at, (left, hold) in enumerate(zip(lefts, held))
        ]

    for load in loads(0):
        load.start()
    greet([("dp", other)])
    copies = [
        pltpu.make_async_remote_copy(
            src_ref=sent.at[place],
            dst_ref=landed.at[place],
            send_sem=send_sem.at[place],
            recv_sem=recv_sem.at[place],
            device_id={"dp": other},
            device_id_type=MESH,
        )
        for place in range(chips)
    ]

    def products(index, write):
        slot = lax.rem(index, 2)
        for load in loads(index):
            load.wait()

        @pl.when(index + 1 < 2 * chips)
        def _():
            for load in loads(index + 1):
                load.start()

        start = 0
        for hold, right in zip(held, rights):
            width = right.shape[1]
            tile = next(t for t in (512, 384, 256, 128) if width % t == 0)

            def step(at, carry, hold=hold, right=right, start=start, tile=tile):
                column = pl.multiple_of(at * tile, tile)
                write(
                    pl.ds(start + column, tile),
                    simple_product(hold[slot], right[:, pl.ds(column, tile)]),
                )
                return carry

            lax.fori_loop(0, width // tile, step, 0)
            start += width

    def send_step(place, carry):
        def write(columns, values):
            sent[place, :, columns] = values.astype(jnp.bfloat16)

        products(place, write)
        for at in range(chips):
            pl.when(place == at)(copies[at].start)
        return carry

    lax.fori_loop(0, chips, send_step, 0)
    outs = [
        pltpu.make_async_copy(landed.at[place], out_ref, out_sem.at[place])
        for place, out_ref in enumerate(out_refs)
    ]

    def own_step(place, carry):
        for at in range(chips):
            pl.when(place == at)(copies[at].wait_recv)

        def write(columns, values):
            landed[place, :, columns] = (
                values + landed[place, :, columns].astype(jnp.float32)
            ).astype(jnp.bfloat16)

        products(place + chips, write)
        for at in range(chips):
            pl.when(place == at)(outs[at].start)
        return carry

    lax.fori_loop(0, chips, own_step, 0)
    for copy in copies:
        copy.wait_send()
    for copy in outs:
        copy.wait()


def pair_grads(pairs, sizes, collective_id):
    chips = sizes[0] // 2
    depth, total_rows = pairs[0][0].shape
    block = depth // sizes[0]
    width = sum(right.shape[1] for _, right in pairs)
    far = pl.BlockSpec(memory_space=pl.ANY)
    return pl.pallas_call(
        functools.partial(pair_grad_kernel, chips, len(pairs)),
        out_shape=[jax.ShapeDtypeStruct((block, width), jnp.bfloat16)] * chips,
        in_specs=[far] * len(pairs) + [pl.BlockSpec(memory_space=pltpu.VMEM)] * len(pairs),
        out_specs=[far] * chips,
        scratch_shapes=[pltpu.VMEM((2, block, total_rows), jnp.bfloat16) for _ in pairs]
        + [
            pltpu.VMEM((chips, block, width), jnp.bfloat16),
            pltpu.VMEM((chips, block, width), jnp.bfloat16),
            pltpu.SemaphoreType.DMA((len(pairs), 2)),
            pltpu.SemaphoreType.DMA((chips,)),
            pltpu.SemaphoreType.DMA((chips,)),
            pltpu.SemaphoreType.DMA((chips,)),
        ],
        compiler_params=pltpu.CompilerParams(
            collective_id=collective_id, has_side_effects=True, vmem_limit_bytes=VMEM_LIMIT
        ),
        cost_estimate=pl.CostEstimate(
            flops=2 * total_rows * depth * width,
            bytes_accessed=2 * (total_rows * depth * len(pairs) + width * (total_rows + depth)),
            transcendentals=0,
        ),
        name="pair_grads",
    )(*[left for left, _ in pairs], *[right for _, right in pairs])


def reduce_over_chips(pairs, sizes, collective_id):
    data_size = sizes[0]
    chips = data_size // 2
    blocks = pair_grads(pairs, sizes, collective_id)
    up = lax.ppermute(blocks[chips - 1], "dp", [(device, device + 2) for device in range(2)])
    down = lax.ppermute(
        blocks[1],
        "dp",
        [(device, device - 2) for device in range(data_size - 2, data_size)],
    )
    return blocks, up, down


def pack_mixing_kernel(heads, query_ref, key_ref, value_ref, output_ref, out_ref):
    query_width = query_ref.shape[1] // heads
    head_size = key_ref.shape[1] // heads
    start = 0
    for head in range(heads):
        for ref, part in ((query_ref, query_width), (key_ref, head_size), (value_ref, head_size)):
            out_ref[:, start : start + part] = ref[:, head * part : (head + 1) * part]
            start += part
    out_ref[:, start:] = output_ref[...].T


def pack_feed_kernel(gate_ref, up_ref, down_ref, first_ref, second_ref):
    start = 0
    for out_ref in (first_ref, second_ref):
        width = out_ref.shape[1] // 3
        part = slice(start, start + width)
        out_ref[:, :width] = gate_ref[:, part]
        out_ref[:, width : 2 * width] = up_ref[:, part]
        out_ref[:, 2 * width :] = down_ref[part, :].T
        start += width


def finish_kernel(heads, *refs):
    first_ref, second_ref, mixing_ref, output_total_ref, terms_ref, output_rows_ref, input_rows_ref = refs[:7]
    far, held, sem = refs[7:20], refs[20:31], refs[31]
    (
        attention_term_out, query_out, key_out, value_out, query_gain_out, key_gain_out,
        output_out, feed_term_out, gate_out, up_out, down_out,
    ) = held
    copies = [
        pltpu.make_async_copy(source, target, sem.at[index])
        for index, (source, target) in enumerate(zip((output_rows_ref, input_rows_ref, *held), far))
    ]
    copies[0].start()
    copies[1].start()
    start = 0
    for total_ref in (first_ref, second_ref):
        width = total_ref.shape[1] // 3
        part = slice(start, start + width)
        gate_out[:, part] = total_ref[:, :width].astype(jnp.float32)
        up_out[:, part] = total_ref[:, width : 2 * width].astype(jnp.float32)
        down_out[part, :] = total_ref[:, 2 * width :].astype(jnp.float32).T
        start += width
    for copy in copies[10:13]:
        copy.start()
    query_width = query_out.shape[1] // heads
    head_size = key_out.shape[1] // heads
    start = 0
    for head in range(heads):
        for out, part in ((query_out, query_width), (key_out, head_size), (value_out, head_size)):
            out[:, head * part : (head + 1) * part] = mixing_ref[:, start : start + part].astype(
                jnp.float32
            )
            start += part
    output_out[...] = output_total_ref[...].astype(jnp.float32).T
    count = attention_term_out.shape[0]
    attention_term_out[...] = terms_ref[:count, :]
    feed_term_out[...] = terms_ref[count : 2 * count, :]
    query_gain_out[...] = terms_ref[2 * count : 2 * count + 1, :]
    key_gain_out[...] = terms_ref[2 * count + 1 : 2 * count + 2, :]
    for copy in copies[2:10]:
        copy.start()
    for copy in copies:
        copy.wait()


def whole_call(body, shapes, *operands):
    return pl.pallas_call(
        body,
        out_shape=shapes,
        in_specs=[pl.BlockSpec(memory_space=pltpu.VMEM)] * len(operands),
        out_specs=[pl.BlockSpec(memory_space=pltpu.VMEM)] * len(shapes),
        compiler_params=pltpu.CompilerParams(vmem_limit_bytes=VMEM_LIMIT),
        cost_estimate=pl.CostEstimate(
            flops=0, bytes_accessed=4 * sum(operand.size for operand in operands), transcendentals=0
        ),
    )(*operands)


def per_device(
    block_input,
    attention_gain,
    query_weight,
    key_matrix,
    value_matrix,
    query_gain,
    key_gain,
    output_weight,
    feed_gain,
    gate_weight,
    up_weight,
    down_weight,
    out_cotangent,
):
    size = lax.axis_size("tensor")
    sizes = (lax.axis_size("dp"), size)
    model_width = block_input.shape[1]
    head_size = query_gain.shape[0]
    query_columns = query_weight.shape[1]
    key_columns = key_matrix.shape[1]
    heads = key_columns // head_size
    grouping = query_columns // key_columns
    hidden_columns = gate_weight.shape[1]
    qkv_columns = query_columns + 2 * key_columns
    first_columns = hidden_columns * 2 // 3 // 256 * 256 or hidden_columns // 2
    second_columns = hidden_columns - first_columns
    tables = turn_tables(head_size)

    block_width = query_weight.shape[0]
    (mixing_local,) = whole_call(
        functools.partial(pack_mixing_kernel, heads),
        [jax.ShapeDtypeStruct((block_width, qkv_columns + query_columns), jnp.bfloat16)],
        query_weight, key_matrix, value_matrix, output_weight,
    )
    mixing_full = lax.all_gather(mixing_local, "dp", axis=0, tiled=True)
    feed_locals = whole_call(
        pack_feed_kernel,
        [
            jax.ShapeDtypeStruct((block_width, 3 * columns), jnp.bfloat16)
            for columns in (first_columns, second_columns)
        ],
        gate_weight, up_weight, down_weight,
    )
    feed_full = [lax.all_gather(part, "dp", axis=0, tiled=True) for part in feed_locals]

    input_float = block_input.astype(jnp.float32)
    first_scale = row_scale(input_float)
    first_unit = input_float * first_scale
    mixer_local = (first_unit * attention_gain).astype(jnp.bfloat16)
    mixer_rows, mixer_turned, cotangent_rows, cotangent_turned = gather_rows(
        (mixer_local, out_cotangent), size, 0
    )

    raw, mixed_rows, totals = attention_forward(
        mixer_rows, mixing_full, tables, query_gain, key_gain, heads, grouping
    )
    local_shape = block_input.shape
    local_rows = local_shape[0]
    gain_rows = model_width // head_size
    gathered_shapes = [
        jax.ShapeDtypeStruct((size * local_rows, model_width), jnp.bfloat16),
        jax.ShapeDtypeStruct((model_width, size * local_rows), jnp.bfloat16),
    ]
    local_float = jax.ShapeDtypeStruct(local_shape, jnp.float32)
    local_half = jax.ShapeDtypeStruct(local_shape, jnp.bfloat16)
    row_sum = pltpu.VMEM((1, model_width), jnp.float32)
    own_rows = pltpu.VMEM(local_shape, jnp.bfloat16)
    scatter_scratch = Scatter.scratch(size, *local_shape)
    gather_scratch = Gather.scratch(size, *local_shape)
    feed_rows, feed_turned, hidden_state = scatter_call(
        functools.partial(between_forward_kernel, size),
        [(mixed_rows, mixing_full, qkv_columns)],
        size,
        [block_input, feed_gain.reshape(1, -1)],
        [],
        [*gathered_shapes, local_float],
        True,
        [own_rows, *scatter_scratch, *gather_scratch],
        1,
    )

    hidden_first, slope_first = feed_half(feed_rows, cotangent_rows, feed_full[0])
    blocks, up, down = reduce_over_chips(
        [(feed_turned, slope_first), (cotangent_turned, hidden_first)], sizes, 5
    )
    blocks, later_full = lax.optimization_barrier((blocks, feed_full[1]))
    hidden_second, slope_second = feed_half(feed_rows, cotangent_rows, later_full)
    second_grad = grad_blocks(
        [(feed_turned, slope_second), (cotangent_turned, hidden_second)], 2 * block_width
    )
    second_grad, slope_second = lax.optimization_barrier((second_grad, slope_second))
    chips = sizes[0] // 2
    later_steps = range(2, chips)
    state_rows, state_turned, state_slope, feed_term, first_total = scatter_call(
        functools.partial(between_backward_kernel, size, chips),
        [(slope_first, feed_full[0], 0), (slope_second, later_full, 0)],
        size,
        [hidden_state, out_cotangent, feed_gain.reshape(1, -1)],
        [blocks[chips - step] for step in later_steps]
        + [blocks[step] for step in later_steps]
        + [up, down, blocks[0]],
        [
            *gathered_shapes,
            local_float,
            jax.ShapeDtypeStruct((gain_rows, head_size), jnp.float32),
            jax.ShapeDtypeStruct(blocks[0].shape, jnp.bfloat16),
        ],
        True,
        [
            own_rows,
            row_sum,
            pltpu.SemaphoreType.DMA((1,)),
            *scatter_scratch,
            *gather_scratch,
            *Chain.scratch(len(later_steps), *blocks[0].shape),
        ],
        2,
    )
    second_grad, state_turned = lax.optimization_barrier((second_grad, state_turned))
    second_total = lax.psum_scatter(second_grad, "dp", scatter_dimension=0, tiled=True)
    output_grad = grad_blocks([(state_turned, mixed_rows)], 4 * block_width)
    output_grad, state_rows = lax.optimization_barrier((output_grad, state_rows))
    output_total = lax.psum_scatter(output_grad, "dp", scatter_dimension=0, tiled=True)
    qkv_slope, head_terms, block_output = attention_backward(
        state_rows, mixing_full, qkv_columns, raw, mixed_rows, totals, tables,
        query_gain, key_gain, heads, grouping,
        [
            (hidden_first, feed_full[0], 2 * first_columns),
            (hidden_second, later_full, 2 * second_columns),
        ],
        hidden_state, size, 4,
    )
    mixing_blocks = pair_grads([(mixer_turned, qkv_slope)], sizes, 6)
    terms_shape = (2 * gain_rows + head_terms.shape[0], head_size)
    input_gradient, terms, mixing_total = scatter_call(
        functools.partial(last_kernel, sizes),
        [(qkv_slope, mixing_full, 0)],
        size,
        [
            block_input,
            attention_gain.reshape(1, -1),
            state_slope,
            jnp.concatenate([feed_term, head_terms], axis=0),
            mixer_rows,
        ],
        [mixing_blocks[chips - step] for step in range(1, chips)]
        + [mixing_blocks[step] for step in range(1, chips)]
        + [mixing_blocks[0]] * 3,
        [
            local_half,
            jax.ShapeDtypeStruct(terms_shape, jnp.float32),
            jax.ShapeDtypeStruct(mixing_blocks[0].shape, jnp.bfloat16),
        ],
        False,
        [
            row_sum,
            pltpu.VMEM(terms_shape, jnp.float32),
            pltpu.VMEM(terms_shape, jnp.float32),
            pltpu.VMEM((size, *terms_shape), jnp.float32),
            pltpu.VMEM((sizes[0], *terms_shape), jnp.float32),
            *[pltpu.SemaphoreType.DMA((count - 1,)) for count in (size, size, *sizes[:1] * 2)],
            pltpu.SemaphoreType.DMA((1,)),
            *scatter_scratch,
            *Chain.scratch(chips - 1, *mixing_blocks[0].shape),
        ],
        3,
    )

    def whole_float(*shape):
        return jax.ShapeDtypeStruct(shape, jnp.float32)

    float_shapes = [
        whole_float(gain_rows, head_size),
        whole_float(block_width, query_columns),
        whole_float(block_width, key_columns),
        whole_float(block_width, key_columns),
        whole_float(1, head_size),
        whole_float(1, head_size),
        whole_float(query_columns, block_width),
        whole_float(gain_rows, head_size),
        whole_float(block_width, hidden_columns),
        whole_float(block_width, hidden_columns),
        whole_float(hidden_columns, block_width),
    ]
    outs = pl.pallas_call(
        functools.partial(finish_kernel, heads),
        out_shape=[local_half, local_half, *float_shapes],
        in_specs=[pl.BlockSpec(memory_space=pltpu.VMEM)] * 7,
        out_specs=[pl.BlockSpec(memory_space=pl.ANY)] * 13,
        scratch_shapes=[pltpu.VMEM(shape.shape, shape.dtype) for shape in float_shapes]
        + [pltpu.SemaphoreType.DMA((13,))],
        compiler_params=pltpu.CompilerParams(vmem_limit_bytes=VMEM_LIMIT),
        cost_estimate=pl.CostEstimate(flops=0, bytes_accessed=20_000_000, transcendentals=0),
        name="finish",
    )(first_total, second_total, mixing_total, output_total, terms, block_output, input_gradient)
    return tuple(
        out.reshape(-1) if index in (2, 6, 7, 9) else out for index, out in enumerate(outs)
    )


def solution(mesh):
    in_specs = (
        P(("dp", "tensor"), None),
        P(),
        P("dp", "tensor"),
        P("dp", "tensor"),
        P("dp", "tensor"),
        P(),
        P(),
        P("tensor", "dp"),
        P(),
        P("dp", "tensor"),
        P("dp", "tensor"),
        P("tensor", "dp"),
        P(("dp", "tensor"), None),
    )
    out_specs = (
        P(("dp", "tensor"), None),
        P(("dp", "tensor"), None),
        P(),
        P("dp", "tensor"),
        P("dp", "tensor"),
        P("dp", "tensor"),
        P(),
        P(),
        P("tensor", "dp"),
        P(),
        P("dp", "tensor"),
        P("dp", "tensor"),
        P("tensor", "dp"),
    )

    return jax.shard_map(per_device, mesh=mesh, in_specs=in_specs, out_specs=out_specs, check_vma=False)
```

```python
import functools

import jax
import jax.numpy as jnp
import numpy as np
from jax import lax
from jax.experimental import pallas as pl
from jax.experimental.pallas import tpu as pltpu
from jax.sharding import PartitionSpec as P


SEQUENCE_LENGTH = 1024

epsilon = 1e-06
rope_base = 1000000.0


MESH = pl.DeviceIdType.MESH
VMEM_LIMIT = 62 * 1024 * 1024


def row_scale(values):
    return lax.rsqrt(jnp.mean(values * values, axis=-1, keepdims=True) + epsilon)


def times_transposed(first_operand, second_operand):
    return lax.dot_general(
        first_operand, second_operand, (((1,), (1,)), ((), ())), preferred_element_type=jnp.float32
    )


def simple_product(first_operand, second_operand):
    return jnp.dot(first_operand, second_operand, preferred_element_type=jnp.float32)


def remote(source, target, send_sem, recv_sem, peer, axis="tensor"):
    return pltpu.make_async_remote_copy(
        src_ref=source,
        dst_ref=target,
        send_sem=send_sem,
        recv_sem=recv_sem,
        device_id={axis: peer},
        device_id_type=MESH,
    )


def greet(peers):
    barrier = pltpu.get_barrier_semaphore()
    for axis, peer in peers:
        pl.semaphore_signal(barrier, inc=1, device_id={axis: peer}, device_id_type=MESH)
    pl.semaphore_wait(barrier, len(peers))


def square_peers(me):
    column = lax.rem(me, 2)
    row = me // 2
    return row * 2 + (1 - column), (1 - row) * 2 + column, (1 - row) * 2 + (1 - column)


def neighbours(size):
    if size == 4:
        beside, below, _ = square_peers(lax.axis_index("tensor"))
        return [("tensor", beside), ("tensor", below)]
    return [("tensor", peer) for peer in other_members("tensor", size)]


def other_members(axis, count):
    me = lax.axis_index(axis)
    return [lax.rem(me + step, count) for step in range(1, count)]


class Gather:
    def __init__(
        self, size, own_ref, out_ref, turned_out_ref, held_ref, turned_ref, send_sem, recv_sem, local_sem, turned_sem
    ):
        self.size, self.own, self.out, self.held = size, own_ref, out_ref, held_ref
        self.turned_out, self.turned = turned_out_ref, turned_ref
        self.send_sem, self.recv_sem, self.local_sem = send_sem, recv_sem, local_sem
        self.turned_sem = turned_sem
        self.me = lax.axis_index("tensor")
        self.rows = own_ref.shape[0]
        self.copies, self.stores, self.turns = [], [], []

    @staticmethod
    def scratch(size, rows, columns):
        sends, local = (12, 8) if size == 4 else (size - 1, size)
        return [
            pltpu.VMEM((size, rows, columns), jnp.bfloat16),
            pltpu.VMEM((columns, size * rows), jnp.bfloat16),
            pltpu.SemaphoreType.DMA((sends,)),
            pltpu.SemaphoreType.DMA((sends,)),
            pltpu.SemaphoreType.DMA((local,)),
            pltpu.SemaphoreType.DMA((local,)),
        ]

    def send(self, source, target, peer):
        index = len(self.copies)
        copy = remote(source, target, self.send_sem.at[index], self.recv_sem.at[index], peer)
        copy.start()
        self.copies.append(copy)
        return copy

    def store(self, source, start, count):
        piece = pl.ds(pl.multiple_of(start, count), count)
        copy = pltpu.make_async_copy(source, self.out.at[piece], self.local_sem.at[len(self.stores)])
        copy.start()
        self.stores.append(copy)
        width = min(256, self.turned.shape[0])

        def turn_part(index, carry):
            columns = pl.ds(pl.multiple_of(index * width, width), width)
            self.turned[columns, piece] = source[:, columns].T
            return carry

        lax.fori_loop(0, self.turned.shape[0] // width, turn_part, 0)
        turn_copy = pltpu.make_async_copy(
            self.turned.at[:, piece], self.turned_out.at[:, piece], self.turned_sem.at[len(self.turns)]
        )
        turn_copy.start()
        self.turns.append(turn_copy)

    def quarters(self):
        quarter = self.rows // 4
        return [pl.ds(index * quarter, quarter) for index in range(4)]

    def start(self, stage):
        own, held = self.own, self.held
        if self.size != 4:
            if stage == 0:
                for peer in other_members("tensor", self.size):
                    self.send(own, held.at[self.me], peer)
            return
        beside, below, _ = square_peers(self.me)
        parts = self.quarters()
        upper, lower = parts[stage], parts[2 + stage]
        for part, peer in ((upper, beside), (lower, below), (lower, beside), (upper, below)):
            self.send(own.at[part], held.at[self.me, part], peer)

    def forward(self):
        own, held, rows = self.own, self.held, self.rows
        if self.size != 4:
            self.store(own, self.me * rows, rows)
            return
        beside, below, _ = square_peers(self.me)
        half = rows // 2
        self.store(own.at[pl.ds(0, half)], self.me * rows, half)
        self.store(own.at[pl.ds(half, half)], self.me * rows + half, half)
        parts = self.quarters()
        for stage in range(2):
            self.copies[4 * stage].wait_recv()
            self.send(held.at[beside, parts[stage]], held.at[beside, parts[stage]], below)
            self.copies[4 * stage + 1].wait_recv()
            self.send(held.at[below, parts[2 + stage]], held.at[below, parts[2 + stage]], beside)

    def finish(self):
        held, rows = self.held, self.rows
        if self.size != 4:
            for step, copy in enumerate(self.copies):
                copy.wait_recv()
                slot = lax.rem(self.me + self.size - step - 1, self.size)
                self.store(held.at[slot], slot * rows, rows)
        else:
            beside, below, across = square_peers(self.me)
            half = rows // 2
            first, second = pl.ds(0, half), pl.ds(half, half)
            self.store(held.at[beside, first], beside * rows, half)
            self.store(held.at[below, second], below * rows + half, half)
            for indices, slot, start in (
                ((2, 6), beside, half),
                ((3, 7), below, 0),
                ((8, 10), across, 0),
                ((9, 11), across, half),
            ):
                for index in indices:
                    self.copies[index].wait_recv()
                self.store(held.at[slot, pl.ds(start, half)], slot * rows + start, half)
        for copy in self.copies:
            copy.wait_send()
        for copy in self.stores + self.turns:
            copy.wait()


def gather_kernel(size, count, *refs):
    own_refs, out_refs, rest = refs[:count], refs[count : 3 * count], refs[3 * count :]
    greet(neighbours(size))
    gathers = [
        Gather(size, own_refs[k], *out_refs[2 * k : 2 * k + 2], *rest[6 * k : 6 * k + 6])
        for k in range(count)
    ]
    for gather in gathers:
        gather.start(0)
        gather.start(1)
        gather.forward()
    for gather in gathers:
        gather.finish()


def gather_rows(arrays, size, collective_id):
    count = len(arrays)
    rows, columns = arrays[0].shape
    scratch = []
    out_shape = []
    for _ in arrays:
        scratch += Gather.scratch(size, rows, columns)
        out_shape += [
            jax.ShapeDtypeStruct((size * rows, columns), jnp.bfloat16),
            jax.ShapeDtypeStruct((columns, size * rows), jnp.bfloat16),
        ]
    return pl.pallas_call(
        functools.partial(gather_kernel, size, count),
        out_shape=out_shape,
        in_specs=[pl.BlockSpec(memory_space=pltpu.VMEM)] * count,
        out_specs=[pl.BlockSpec(memory_space=pl.ANY)] * len(out_shape),
        scratch_shapes=scratch,
        compiler_params=pltpu.CompilerParams(
            collective_id=collective_id, has_side_effects=True, vmem_limit_bytes=VMEM_LIMIT
        ),
        cost_estimate=pl.CostEstimate(
            flops=0, bytes_accessed=count * 30 * size * rows * columns, transcendentals=0
        ),
        name="gather_rows",
    )(*arrays)


class Operand:
    def __init__(self, size, first_column, left_far, weight_far, left, weight, left_sem, weight_sem):
        self.left, self.weight = left, weight
        self.rows = left.shape[0] // size
        self.tile = min(512, weight.shape[0])
        self.far = left_far, weight_far
        self.first_column = first_column
        self.left_sem, self.weight_sem = left_sem, weight_sem

    @staticmethod
    def scratch(size, left, weight):
        width = left.shape[1]
        return [
            pltpu.VMEM(left.shape, left.dtype),
            pltpu.VMEM((weight.shape[0], width), weight.dtype),
            pltpu.SemaphoreType.DMA((size,)),
            pltpu.SemaphoreType.DMA((max(1, weight.shape[0] // 512),)),
        ]

    def left_copy(self, slot, owner):
        piece = pl.ds(pl.multiple_of(owner * self.rows, self.rows), self.rows)
        return pltpu.make_async_copy(self.far[0].at[piece], self.left.at[piece], self.left_sem.at[slot])

    def weight_copy(self, index):
        piece = pl.ds(pl.multiple_of(index * self.tile, self.tile), self.tile)
        columns = pl.ds(self.first_column, self.left.shape[1])
        return pltpu.make_async_copy(
            self.far[1].at[piece, columns], self.weight.at[piece], self.weight_sem.at[index]
        )


def block_product(operands, start, rows, fresh, write, after):
    total = operands[0].weight.shape[0]
    tile = operands[0].tile
    start = pl.multiple_of(start, rows)

    def step(index, carry):
        @pl.when(fresh)
        def _():
            for operand in operands:
                operand.weight_copy(index).wait()

        columns = pl.ds(pl.multiple_of(index * tile, tile), tile)
        values = None
        for operand in operands:
            part = times_transposed(
                operand.left[pl.ds(start, rows), :], operand.weight[columns, :]
            )
            values = part if values is None else values + part
        write(columns, values)
        after(index)
        return carry

    lax.fori_loop(0, total // tile, step, 0)


class Scatter:
    def __init__(self, size, outgoing, *rest):
        self.size, self.outgoing = size, outgoing
        if size == 4:
            self.passing, rest = rest[0], rest[1:]
        self.arriving, self.send_sem, self.recv_sem = rest
        self.rows = outgoing.shape[1]
        self.me = lax.axis_index("tensor")
        self.stages = 2 if size == 4 else 1
        self.plan()

    @staticmethod
    def scratch(size, rows, columns):
        if size == 4:
            sends = 10
            buffers = [
                pltpu.VMEM((4, rows, columns), jnp.bfloat16),
                pltpu.VMEM((2, rows // 2, columns), jnp.bfloat16),
                pltpu.VMEM((2, rows, columns), jnp.bfloat16),
            ]
        else:
            sends = size - 1
            buffers = [
                pltpu.VMEM((size, rows, columns), jnp.bfloat16),
                pltpu.VMEM((size - 1, rows, columns), jnp.bfloat16),
            ]
        return buffers + [pltpu.SemaphoreType.DMA((sends,)), pltpu.SemaphoreType.DMA((sends,))]

    def prepare(self, index, source, target, peer):
        return remote(source, target, self.send_sem.at[index], self.recv_sem.at[index], peer)

    def plan(self):
        outgoing, arriving = self.outgoing, self.arriving
        if self.size != 4:
            self.copies = [
                self.prepare(step, outgoing.at[step], arriving.at[step], peer)
                for step, peer in enumerate(other_members("tensor", self.size))
            ]
            self.early, self.starts = (), tuple((step, step) for step in range(self.size - 1))
            return
        beside, below, _ = square_peers(self.me)
        half, quarter = self.rows // 2, self.rows // 4
        first, second = pl.ds(0, half), pl.ds(half, half)
        middle = outgoing.shape[2] // 2
        left, right = pl.ds(0, middle), pl.ds(middle, middle)
        upper = [pl.ds(stage * quarter, quarter) for stage in range(2)]
        lower = [pl.ds(half + stage * quarter, quarter) for stage in range(2)]
        everything = pl.ds(0, half)
        self.copies = [
            self.prepare(0, outgoing.at[0, first, left], self.passing.at[0, everything, left], beside),
            self.prepare(1, outgoing.at[0, second, left], self.passing.at[1, everything, left], below),
            self.prepare(2, outgoing.at[0, first, right], self.passing.at[0, everything, right], beside),
            self.prepare(3, outgoing.at[0, second, right], self.passing.at[1, everything, right], below),
            self.prepare(4, outgoing.at[1, first], arriving.at[0, first], beside),
            self.prepare(5, outgoing.at[2, second], arriving.at[1, second], below),
            self.prepare(6, outgoing.at[1, lower[0]], arriving.at[0, lower[0]], beside),
            self.prepare(7, outgoing.at[2, upper[0]], arriving.at[1, upper[0]], below),
            self.prepare(8, outgoing.at[1, lower[1]], arriving.at[0, lower[1]], beside),
            self.prepare(9, outgoing.at[2, upper[1]], arriving.at[1, upper[1]], below),
        ]
        self.early, self.starts = (0, 1), ((0, 2), (0, 3), (1, 4), (2, 5))

    def owner(self, slot):
        if self.size != 4:
            return lax.rem(self.me + slot + 1, self.size)
        beside, below, across = square_peers(self.me)
        return jnp.where(
            slot == 0, across, jnp.where(slot == 1, beside, jnp.where(slot == 2, below, self.me))
        )

    def load(self, operands):
        tiles = operands[0].weight.shape[0] // operands[0].tile
        for operand in operands:
            operand.left_copy(0, self.owner(0)).start()
        for index in range(tiles):
            for operand in operands:
                operand.weight_copy(index).start()
        for slot in range(1, self.size):
            for operand in operands:
                operand.left_copy(slot, self.owner(slot)).start()

    def fill(self, operands, look=None, between=None):
        rows = self.rows

        def step(slot, carry):
            owner = self.owner(slot)
            for operand in operands:
                operand.left_copy(slot, owner).wait()

            def write(columns, values):
                self.outgoing[slot, :, columns] = values.astype(self.outgoing.dtype)
                if look is not None:
                    look(owner, columns, values)

            tiles = operands[0].weight.shape[0] // operands[0].tile

            def after(index):
                for early in self.early:
                    pl.when((slot == 0) & (index == max(tiles // 2, 1) - 1))(self.copies[early].start)

            block_product(operands, owner * rows, rows, slot == 0, write, after)
            for at, index in self.starts:
                pl.when(slot == at)(self.copies[index].start)
            if between is not None:
                pl.when(slot == 0)(between)
            return carry

        lax.fori_loop(0, self.size, step, 0)

    def relay(self):
        if self.size != 4:
            return
        half, quarter = self.rows // 2, self.rows // 4
        for stage in range(2):
            for arrivals, source, slot, start, onward in (
                ((1, 3), 1, 1, half, 6 + 2 * stage),
                ((0, 2), 0, 2, 0, 7 + 2 * stage),
            ):
                if stage == 0:
                    for index in arrivals:
                        self.copies[index].wait_recv()
                piece = pl.ds(start + stage * quarter, quarter)
                self.outgoing[slot, piece, :] = add_rounded(
                    self.outgoing[slot, piece, :],
                    self.passing[source, stage * quarter : (stage + 1) * quarter, :],
                )
                self.copies[onward].start()

    def collect(self, stage):
        if self.size != 4:
            for copy in self.copies:
                copy.wait_recv()
            return
        if stage == 0:
            self.copies[4].wait_recv()
            self.copies[5].wait_recv()
        self.copies[6 + 2 * stage].wait_recv()
        self.copies[7 + 2 * stage].wait_recv()

    def over_rows(self, stage, body):
        if self.size != 4:
            over_pieces(self.rows, body)
            return
        half, quarter = self.rows // 2, self.rows // 4
        over_pieces(quarter, body, stage * quarter)
        over_pieces(quarter, body, half + stage * quarter)

    def over_stages(self, body, done=None):
        for stage in range(self.stages):
            self.collect(stage)
            self.over_rows(stage, body)
            if done is not None:
                done(stage)

    def total(self, piece):
        total = self.outgoing[self.size - 1, piece, :].astype(jnp.float32)
        for index in range(self.arriving.shape[0]):
            total = total + self.arriving[index, piece, :].astype(jnp.float32)
        return total

    def drain(self):
        for copy in self.copies:
            copy.wait_send()


class Chain:
    def __init__(
        self, chips, steps, rising_refs, falling_refs, up_ref, down_ref,
        rise, fall, up, down, load_sem, send_sem, recv_sem,
    ):
        self.chips, self.steps = chips, steps
        self.rise, self.fall, self.up, self.down = rise, fall, up, down
        device = lax.axis_index("dp")
        self.chip = device // 2
        count = len(steps)
        self.loads = [
            pltpu.make_async_copy(source, target, load_sem.at[index])
            for index, (source, target) in enumerate(
                [(up_ref, up.at[0]), (down_ref, down.at[0])]
                + [(ref, rise.at[index]) for index, ref in enumerate(rising_refs)]
                + [(ref, fall.at[index]) for index, ref in enumerate(falling_refs)]
            )
        ]
        above = lax.rem(device + 2, 2 * chips)
        under = lax.rem(device + 2 * chips - 2, 2 * chips)
        self.neighbours = [("dp", above), ("dp", under)]
        self.rises = [
            remote(rise.at[i], up.at[i + 1], send_sem.at[i], recv_sem.at[i], above, "dp")
            for i in range(count)
        ]
        self.falls = [
            remote(
                fall.at[i], down.at[i + 1], send_sem.at[count + i], recv_sem.at[count + i], under, "dp"
            )
            for i in range(count)
        ]

    @staticmethod
    def scratch(count, rows, columns):
        return [
            pltpu.VMEM((count, rows, columns), jnp.bfloat16),
            pltpu.VMEM((count, rows, columns), jnp.bfloat16),
            pltpu.VMEM((count + 1, rows, columns), jnp.bfloat16),
            pltpu.VMEM((count + 1, rows, columns), jnp.bfloat16),
            pltpu.SemaphoreType.DMA((2 * count + 2,)),
            pltpu.SemaphoreType.DMA((2 * count,)),
            pltpu.SemaphoreType.DMA((2 * count,)),
        ]

    def load(self):
        for copy in self.loads:
            copy.start()

    def step(self, index):
        if index == 0:
            for copy in self.loads:
                copy.wait()
        step = self.steps[index]
        rows = self.rise.shape[1]
        sends_up = self.chip < step
        sends_down = self.chip >= self.chips - step

        @pl.when(sends_up & (self.chip > 0))
        def _():
            def add(piece):
                self.rise[index, piece, :] = add_rounded(
                    self.rise[index, piece, :], self.up[index, piece, :]
                )

            over_pieces(rows, add)

        pl.when(sends_up)(self.rises[index].start)

        @pl.when(sends_down & (self.chip < self.chips - 1))
        def _():
            def add(piece):
                self.fall[index, piece, :] = add_rounded(
                    self.fall[index, piece, :], self.down[index, piece, :]
                )

            over_pieces(rows, add)

        pl.when(sends_down)(self.falls[index].start)

    def arrives(self, index):
        step = self.steps[index]
        from_under = (self.chip > 0) & (self.chip <= step)
        from_above = (self.chip < self.chips - 1) & (self.chip >= self.chips - step - 1)
        return from_under, from_above

    def wait(self, index):
        from_under, from_above = self.arrives(index)
        pl.when(from_under)(self.rises[index].wait_recv)
        pl.when(from_above)(self.falls[index].wait_recv)

    def drain(self):
        for index, step in enumerate(self.steps):
            pl.when(self.chip < step)(self.rises[index].wait_send)
            pl.when(self.chip >= self.chips - step)(self.falls[index].wait_send)


def add_rounded(first, second):
    return (first.astype(jnp.float32) + second.astype(jnp.float32)).astype(jnp.bfloat16)


def over_pieces(rows, body, start=0):
    count = min(32, rows)

    def step(index, carry):
        body(pl.ds(pl.multiple_of(start + index * count, count), count))
        return carry

    lax.fori_loop(0, rows // count, step, 0)


def send_terms(axis, peers, source, landing, send_sem, recv_sem):
    me = lax.axis_index(axis)
    landing[me] = source[...]
    copies = []
    for step, peer in enumerate(peers):
        copy = remote(source, landing.at[me], send_sem.at[step], recv_sem.at[step], peer, axis)
        copy.start()
        copies.append(copy)
    return copies


def add_terms(landing, copies):
    for copy in copies:
        copy.wait_recv()
    total = landing[0]
    for index in range(1, landing.shape[0]):
        total = total + landing[index]
    return total


def split_operands(refs, size, first_columns):
    count = len(first_columns)
    far, refs, scratch = refs[: 2 * count], refs[2 * count : -4 * count], refs[-4 * count :]
    operands = [
        Operand(size, first, *far[2 * p : 2 * p + 2], *scratch[4 * p : 4 * p + 4])
        for p, first in enumerate(first_columns)
    ]
    return operands, refs


def store_row(target_ref, row_ref):
    width = target_ref.shape[1]
    for index in range(row_ref.shape[1] // width):
        target_ref[index : index + 1, :] = row_ref[:, index * width : (index + 1) * width]


def between_forward_kernel(size, first_columns, *refs):
    operands, refs = split_operands(refs, size, first_columns)
    input_ref, gain_ref, gathered_ref, turned_ref, state_ref, own_ref = refs[:6]
    buffers = 5 if size == 4 else 4
    scatter = Scatter(size, *refs[6 : 6 + buffers])
    gather = Gather(size, own_ref, gathered_ref, turned_ref, *refs[6 + buffers :])
    scatter.load(operands)
    greet(neighbours(size))
    scatter.fill(operands)
    scatter.relay()

    def norm(piece):
        state = input_ref[piece, :].astype(jnp.float32) + scatter.total(piece)
        state_ref[piece, :] = state
        own_ref[piece, :] = (state * row_scale(state) * gain_ref[...]).astype(own_ref.dtype)

    scatter.over_stages(norm, gather.start)
    gather.forward()
    gather.finish()
    scatter.drain()


def between_backward_kernel(size, chips, steps, first_columns, *refs):
    operands, refs = split_operands(refs, size, first_columns)
    state_ref, cotangent_ref, gain_ref = refs[:3]
    chain_count = 2 * len(steps) + 2
    chain_refs, last_refs, refs = refs[3 : 3 + chain_count], refs[3 + chain_count : 5 + chain_count], refs[5 + chain_count :]
    gathered_ref, gathered_turned_ref, slope_ref, term_ref, rising_ref, falling_ref = refs[:6]
    own_ref, sum_ref, last_sem = refs[6:9]
    buffers = 5 if size == 4 else 4
    scatter = Scatter(size, *refs[9 : 9 + buffers])
    gather = Gather(size, own_ref, gathered_ref, gathered_turned_ref, *refs[9 + buffers : 15 + buffers])
    chain = Chain(
        chips, steps, chain_refs[: len(steps)], chain_refs[len(steps) : -2], *chain_refs[-2:],
        *refs[15 + buffers :],
    )
    last_loads = [
        pltpu.make_async_copy(source, target, last_sem.at[index])
        for index, (source, target) in enumerate(zip(last_refs, (rising_ref, falling_ref)))
    ]
    chain.load()
    scatter.load(operands)
    for load in last_loads:
        load.start()
    greet(neighbours(size) + chain.neighbours)
    scatter.fill(operands, between=lambda: chain.step(0))
    scatter.relay()
    sum_ref[...] = jnp.zeros_like(sum_ref)

    def norm(piece):
        back = scatter.total(piece)
        state = state_ref[piece, :]
        scale = row_scale(state)
        unit = state * scale
        sum_ref[...] += jnp.sum(back * unit, axis=0, keepdims=True)
        unit_slope = back * gain_ref[...]
        slope = cotangent_ref[piece, :].astype(jnp.float32) + scale * (
            unit_slope - unit * jnp.mean(unit_slope * unit, axis=-1, keepdims=True)
        )
        slope_ref[piece, :] = slope
        own_ref[piece, :] = slope.astype(own_ref.dtype)

    scatter.over_stages(norm, gather.start)
    store_row(term_ref, sum_ref)
    gather.forward()
    chain.wait(0)
    for index in range(1, len(steps)):
        chain.step(index)
        chain.wait(index)
    for load in last_loads:
        load.wait()
    last = len(steps)
    for needed, landing, out_ref in (
        ((chain.chip > 0) & (chain.chip < chips - 1), chain.up, rising_ref),
        ((chain.chip > 0) & (chain.chip < chips - 1), chain.down, falling_ref),
    ):

        @pl.when(needed)
        def _(landing=landing, out_ref=out_ref):
            def add(piece):
                out_ref[piece, :] = add_rounded(out_ref[piece, :], landing[last, piece, :])

            over_pieces(out_ref.shape[0], add)

    gather.finish()
    scatter.drain()
    chain.drain()


def last_kernel(sizes, first_columns, *refs):
    data_size, size = sizes
    operands, refs = split_operands(refs, size, first_columns)
    input_ref, gain_ref, slope_ref, terms_ref, rows_ref = refs[:5]
    gradient_ref, terms_out_ref, sum_ref, partial_ref, group_ref, inner, outer = refs[5:12]
    inner_send, inner_recv, outer_send, outer_recv = refs[12:16]
    mixing = Scatter(size, *refs[16:])
    rows = gradient_ref.shape[0]
    mixing.load(operands)
    greet(
        [("tensor", peer) for peer in other_members("tensor", size)]
        + [("dp", peer) for peer in other_members("dp", data_size)]
    )
    sum_ref[...] = jnp.zeros_like(sum_ref)

    def look(owner, columns, values):
        piece = pl.ds(pl.multiple_of(owner * rows, rows), rows)
        sum_ref[:, columns] += jnp.sum(
            values * rows_ref[piece, columns].astype(jnp.float32), axis=0, keepdims=True
        )

    mixing.fill(operands, look)
    sum_ref[...] = sum_ref[...] / gain_ref[...]
    kept = partial_ref.shape[0] - terms_ref.shape[0]
    partial_ref[kept:, :] = terms_ref[...]
    store_row(partial_ref, sum_ref)
    inner_copies = send_terms(
        "tensor", other_members("tensor", size), partial_ref, inner, inner_send, inner_recv
    )
    mixing.relay()
    group_ref[...] = add_terms(inner, inner_copies)
    outer_copies = send_terms(
        "dp", other_members("dp", data_size), group_ref, outer, outer_send, outer_recv
    )
    terms_out_ref[...] = add_terms(outer, outer_copies)

    def norm(piece):
        back = mixing.total(piece)
        values = input_ref[piece, :].astype(jnp.float32)
        scale = row_scale(values)
        unit = values * scale
        unit_slope = back * gain_ref[...]
        gradient_ref[piece, :] = (
            slope_ref[piece, :]
            + scale * (unit_slope - unit * jnp.mean(unit_slope * unit, axis=-1, keepdims=True))
        ).astype(gradient_ref.dtype)

    mixing.over_stages(norm)
    for copy in inner_copies + outer_copies:
        copy.wait_send()
    mixing.drain()


def scatter_call(body, triples, size, others, far, outs, gathered, scratch, collective_id):
    far_spec = pl.BlockSpec(memory_space=pl.ANY)
    operands = [array for left, weight, _ in triples for array in (left, weight)]
    in_specs = [far_spec] * len(operands)
    for other in others:
        in_specs.append(pl.BlockSpec(other.shape, lambda i: (0, 0), pipeline_mode=pl.Buffered(1)))
    in_specs += [far_spec] * len(far)
    out_specs = [pl.BlockSpec(out.shape, lambda i: (0, 0)) for out in outs]
    if gathered:
        out_specs[:2] = [far_spec] * 2
    return pl.pallas_call(
        functools.partial(body, tuple(first for _, _, first in triples)),
        grid=(1,),
        out_shape=outs,
        in_specs=in_specs,
        out_specs=out_specs,
        scratch_shapes=list(scratch)
        + [part for left, weight, _ in triples for part in Operand.scratch(size, left, weight)],
        compiler_params=pltpu.CompilerParams(
            collective_id=collective_id, has_side_effects=True, vmem_limit_bytes=VMEM_LIMIT
        ),
        cost_estimate=pl.CostEstimate(
            flops=sum(2 * left.size * weight.shape[0] for left, weight, _ in triples),
            bytes_accessed=150_000_000,
            transcendentals=0,
        ),
    )(*operands, *others, *far)


LOG2E = 1.4426950408889634


def turn_tables(head_size):
    half_size = head_size // 2
    frequency = np.float32(rope_base) ** (
        -(np.arange(half_size, dtype=np.float32) * np.float32(2.0) / np.float32(head_size))
    )
    frequency = frequency.astype(np.float64)
    sign = np.concatenate([-np.ones(half_size), np.ones(half_size)])[None, :]
    positions = np.concatenate([np.arange(0, SEQUENCE_LENGTH, 128), np.arange(128)])
    angles = positions[:, None] * np.concatenate([frequency, frequency])[None, :]
    return np.cos(angles).astype(np.float32), (sign * np.sin(angles)).astype(np.float32)


def fill_tables(few_cosines_ref, few_sines_ref, cosine_ref, sine_ref):
    coarse = few_cosines_ref.shape[0] - 128
    near_cosine, near_sine = few_cosines_ref[coarse:, :], few_sines_ref[coarse:, :]

    def step(index, carry):
        far_cosine = few_cosines_ref[pl.ds(index, 1), :]
        far_sine = few_sines_ref[pl.ds(index, 1), :]
        rows = pl.ds(pl.multiple_of(index * 128, 128), 128)
        cosine_ref[rows, :] = far_cosine * near_cosine - far_sine * near_sine
        sine_ref[rows, :] = far_sine * near_cosine + far_cosine * near_sine
        return carry

    lax.fori_loop(0, coarse, step, 0)


def turn(values, cosine, sine):
    return values * cosine + pltpu.roll(values, values.shape[-1] // 2, 1) * sine


def turn_back(values, cosine, sine):
    return values * cosine - pltpu.roll(values, values.shape[-1] // 2, 1) * sine


def contract_first(first_operand, second_operand):
    return lax.dot_general(
        first_operand, second_operand, (((0,), (0,)), ((), ())), preferred_element_type=jnp.float32
    )


def visible_scores(key_rows, query_rows, first_row, multiplier):
    scores = times_transposed(key_rows, query_rows) * multiplier
    _, queries = scores.shape
    key_at = lax.broadcasted_iota(jnp.int32, (queries, queries), 0)
    query_at = lax.broadcasted_iota(jnp.int32, (queries, queries), 1)
    corner = jnp.where(query_at >= key_at, scores[first_row:], -1e30)
    if first_row == 0:
        return corner
    return jnp.concatenate([scores[:first_row], corner], axis=0)


def turn_heads(
    grouping, head_size, raw_ref, query_gain_ref, key_gain_ref, cosine_ref, sine_ref, query_ref, key_ref, value_ref
):
    def turned(start, gain):
        raw = raw_ref[:, pl.ds(start, head_size)]
        return turn(raw * row_scale(raw) * gain, cosine_ref[...], sine_ref[...]).astype(jnp.bfloat16)

    def step(part, carry):
        query_ref[part] = turned(pl.multiple_of(part * head_size, head_size), query_gain_ref[...])
        return carry

    lax.fori_loop(0, grouping, step, 0)
    key_ref[...] = turned(grouping * head_size, key_gain_ref[...])
    value_ref[...] = raw_ref[:, (grouping + 1) * head_size :].astype(jnp.bfloat16)


def attention_forward_kernel(
    grouping, head_size, block, rows_ref, weight_ref, few_cosines_ref, few_sines_ref, query_gain_ref, key_gain_ref,
    raw_ref, mixed_ref, total_ref, query_ref, key_ref, value_ref, cosine_ref, sine_ref,
):
    sequence = rows_ref.shape[0]
    multiplier = head_size ** (-0.5) * LOG2E

    @pl.when((pl.program_id(0) == 0) & (pl.program_id(1) == 0))
    def _():
        fill_tables(few_cosines_ref, few_sines_ref, cosine_ref, sine_ref)

    raw_ref[...] = simple_product(rows_ref[...], weight_ref[...])
    turn_heads(
        grouping, head_size, raw_ref, query_gain_ref, key_gain_ref, cosine_ref, sine_ref, query_ref, key_ref, value_ref
    )

    def head_step(part, carry):
        lanes = pl.ds(pl.multiple_of(part * head_size, head_size), head_size)
        for first_row in range(0, sequence, block):
            last_row = first_row + block
            scores = visible_scores(
                key_ref[:last_row, :], query_ref[part, first_row:last_row, :], first_row, multiplier
            )
            highest = jnp.max(scores, axis=0, keepdims=True)
            weights = jnp.exp2(scores - highest)
            total = jnp.sum(weights, axis=0, keepdims=True)
            weights = (weights * (1.0 / total)).astype(jnp.bfloat16)
            mixed_ref[first_row:last_row, lanes] = contract_first(
                weights, value_ref[:last_row, :]
            ).astype(mixed_ref.dtype)
            total_ref[0, pl.ds(part, 1), first_row:last_row] = highest + jnp.log2(total)
        return carry

    lax.fori_loop(0, grouping, head_step, 0)


def attention_forward(rows, weight, tables, query_gain, key_gain, heads, grouping):
    total_rows, depth = rows.shape
    head_size = query_gain.shape[0]
    sequences = total_rows // SEQUENCE_LENGTH
    width = (grouping + 2) * head_size
    block = min(256, SEQUENCE_LENGTH)
    table = pl.BlockSpec(tables[0].shape, lambda s, h: (0, 0))
    gain = pl.BlockSpec((1, head_size), lambda s, h: (0, 0))
    elements = heads * grouping * total_rows * SEQUENCE_LENGTH // 2
    return pl.pallas_call(
        functools.partial(attention_forward_kernel, grouping, head_size, block),
        grid=(sequences, heads),
        out_shape=[
            jax.ShapeDtypeStruct((total_rows, heads * width), jnp.float32),
            jax.ShapeDtypeStruct((total_rows, heads * grouping * head_size), jnp.bfloat16),
            jax.ShapeDtypeStruct((heads, grouping, total_rows), jnp.float32),
        ],
        in_specs=[
            pl.BlockSpec((SEQUENCE_LENGTH, depth), lambda s, h: (s, 0)),
            pl.BlockSpec((depth, width), lambda s, h: (0, h)),
            table,
            table,
            gain,
            gain,
        ],
        out_specs=[
            pl.BlockSpec((SEQUENCE_LENGTH, width), lambda s, h: (s, h)),
            pl.BlockSpec((SEQUENCE_LENGTH, grouping * head_size), lambda s, h: (s, h)),
            pl.BlockSpec((1, grouping, SEQUENCE_LENGTH), lambda s, h: (h, 0, s)),
        ],
        scratch_shapes=[
            pltpu.VMEM((grouping, SEQUENCE_LENGTH, head_size), jnp.bfloat16),
            pltpu.VMEM((SEQUENCE_LENGTH, head_size), jnp.bfloat16),
            pltpu.VMEM((SEQUENCE_LENGTH, head_size), jnp.bfloat16),
            pltpu.VMEM((SEQUENCE_LENGTH, head_size), jnp.float32),
            pltpu.VMEM((SEQUENCE_LENGTH, head_size), jnp.float32),
        ],
        compiler_params=pltpu.CompilerParams(vmem_limit_bytes=VMEM_LIMIT),
        cost_estimate=pl.CostEstimate(
            flops=2 * total_rows * depth * heads * width + 4 * elements * head_size,
            bytes_accessed=2 * (total_rows * depth + depth * heads * width),
            transcendentals=elements,
        ),
        name="attention_forward",
    )(rows, weight, *tables, query_gain.reshape(1, -1), key_gain.reshape(1, -1))


def norm_back(turned_slope, raw, gain, cosine, sine):
    norm_slope = turn_back(turned_slope, cosine, sine)
    scale = row_scale(raw)
    unit = raw * scale
    term = norm_slope * unit
    unit_slope = norm_slope * gain
    slope = scale * (unit_slope - unit * jnp.mean(unit_slope * unit, axis=-1, keepdims=True))
    return slope.astype(jnp.bfloat16), jnp.sum(term, axis=0, keepdims=True)


def attention_backward_kernel(size, grouping, head_size, block, first_columns, *refs):
    operands, refs = split_operands(refs, size, first_columns)
    (
        state_ref, weight_ref, raw_ref, mixed_ref, total_ref, few_cosines_ref, few_sines_ref,
        query_gain_ref, key_gain_ref, hidden_state_ref, slope_ref, gain_ref, output_ref,
        query_ref, key_ref, value_ref, out_slope_ref, turned_ref, key_sum_ref, value_sum_ref, cosine_ref, sine_ref,
    ) = refs[:22]
    scatter = Scatter(size, *refs[22:])
    step = pl.program_id(0) * pl.num_programs(1) + pl.program_id(1)
    steps = pl.num_programs(0) * pl.num_programs(1)

    @pl.when(step == 0)
    def _():
        scatter.load(operands)
        greet(neighbours(size))
        scatter.fill(operands)

    attend_backward_head(
        grouping, head_size, block, state_ref, weight_ref, raw_ref, mixed_ref, total_ref, few_cosines_ref,
        few_sines_ref, query_gain_ref, key_gain_ref, slope_ref, gain_ref, query_ref, key_ref, value_ref,
        out_slope_ref, turned_ref, key_sum_ref, value_sum_ref, cosine_ref, sine_ref,
    )

    @pl.when(step == 0)
    def _():
        scatter.relay()

    @pl.when(step == steps - 1)
    def _():
        def finish(piece):
            output_ref[piece, :] = (hidden_state_ref[piece, :] + scatter.total(piece)).astype(
                output_ref.dtype
            )

        scatter.over_stages(finish)
        scatter.drain()


def attend_backward_head(
    grouping, head_size, block, state_ref, weight_ref, raw_ref, mixed_ref, total_ref, few_cosines_ref, few_sines_ref,
    query_gain_ref, key_gain_ref, slope_ref, gain_ref, query_ref, key_ref, value_ref, out_slope_ref,
    turned_ref, key_sum_ref, value_sum_ref, cosine_ref, sine_ref,
):
    sequence = state_ref.shape[0]
    scale_factor = head_size ** (-0.5)
    multiplier = scale_factor * LOG2E

    @pl.when((pl.program_id(0) == 0) & (pl.program_id(1) == 0))
    def _():
        gain_ref[...] = jnp.zeros_like(gain_ref)
        fill_tables(few_cosines_ref, few_sines_ref, cosine_ref, sine_ref)

    out_slope_ref[...] = simple_product(state_ref[...], weight_ref[...]).astype(jnp.bfloat16)
    turn_heads(
        grouping, head_size, raw_ref, query_gain_ref, key_gain_ref, cosine_ref, sine_ref, query_ref, key_ref, value_ref
    )
    key_sum_ref[...] = jnp.zeros_like(key_sum_ref)
    value_sum_ref[...] = jnp.zeros_like(value_sum_ref)
    ones = jnp.ones((8, head_size), jnp.float32)

    def head_step(part, carry):
        lanes = pl.ds(pl.multiple_of(part * head_size, head_size), head_size)
        for first_row in range(0, sequence, block):
            last_row = first_row + block
            query_rows = query_ref[part, first_row:last_row, :]
            slope_rows = out_slope_ref[first_row:last_row, lanes]
            scores = visible_scores(key_ref[:last_row, :], query_rows, first_row, multiplier)
            weights = jnp.exp2(scores - total_ref[0, pl.ds(part, 1), first_row:last_row])
            value_sum_ref[:last_row, :] += simple_product(weights.astype(jnp.bfloat16), slope_rows)
            product = slope_rows.astype(jnp.float32) * mixed_ref[first_row:last_row, lanes].astype(jnp.float32)
            centre = lax.dot_general(
                ones,
                product,
                (((1,), (1,)), ((), ())),
                preferred_element_type=jnp.float32,
                precision=lax.Precision.HIGHEST,
            )[:1]
            weight_slope = times_transposed(value_ref[:last_row, :], slope_rows)
            score_slope = (weights * (weight_slope - centre)).astype(jnp.bfloat16)
            key_sum_ref[:last_row, :] += simple_product(score_slope, query_rows)
            turned_ref[first_row:last_row, :] = (
                contract_first(score_slope, key_ref[:last_row, :]) * scale_factor
            )
        slope, term = norm_back(
            turned_ref[...], raw_ref[:, lanes], query_gain_ref[...], cosine_ref[...], sine_ref[...]
        )
        slope_ref[:, lanes] = slope
        gain_ref[0:1, :] += term
        return carry

    lax.fori_loop(0, grouping, head_step, 0)
    lanes = slice(grouping * head_size, (grouping + 1) * head_size)
    slope, term = norm_back(
        key_sum_ref[...] * scale_factor, raw_ref[:, lanes], key_gain_ref[...], cosine_ref[...], sine_ref[...]
    )
    slope_ref[:, lanes] = slope
    gain_ref[1:2, :] += term
    slope_ref[:, (grouping + 1) * head_size :] = value_sum_ref[...].astype(jnp.bfloat16)


def attention_backward(
    state_rows, weight, weight_start, raw, mixed, totals, tables, query_gain, key_gain, heads, grouping,
    triples, hidden_state, size, collective_id,
):
    total_rows, depth = state_rows.shape
    head_size = query_gain.shape[0]
    sequences = total_rows // SEQUENCE_LENGTH
    width = (grouping + 2) * head_size
    out_width = grouping * head_size
    block = min(512, SEQUENCE_LENGTH)
    first_block = weight_start // out_width
    single = pl.Buffered(1)
    table = pl.BlockSpec(tables[0].shape, lambda s, h: (0, 0))
    gain = pl.BlockSpec((1, head_size), lambda s, h: (0, 0))
    elements = heads * grouping * total_rows * SEQUENCE_LENGTH // 2
    whole_rows = pltpu.VMEM((SEQUENCE_LENGTH, head_size), jnp.float32)
    operands = [array for left, other_weight, _ in triples for array in (left, other_weight)]
    in_specs = [pl.BlockSpec(memory_space=pl.ANY)] * len(operands)
    in_specs += [
        pl.BlockSpec((SEQUENCE_LENGTH, depth), lambda s, h: (s, 0), pipeline_mode=single),
        pl.BlockSpec((depth, out_width), lambda s, h: (0, first_block + h)),
        pl.BlockSpec((SEQUENCE_LENGTH, width), lambda s, h: (s, h)),
        pl.BlockSpec((SEQUENCE_LENGTH, out_width), lambda s, h: (s, h)),
        pl.BlockSpec((1, grouping, SEQUENCE_LENGTH), lambda s, h: (h, 0, s)),
        table,
        table,
        gain,
        gain,
        pl.BlockSpec(hidden_state.shape, lambda s, h: (0, 0), pipeline_mode=single),
    ]
    operands += [
        state_rows, weight, raw, mixed, totals, *tables, query_gain.reshape(1, -1), key_gain.reshape(1, -1),
        hidden_state,
    ]
    return pl.pallas_call(
        functools.partial(
            attention_backward_kernel, size, grouping, head_size, block,
            tuple(first for _, _, first in triples),
        ),
        grid=(sequences, heads),
        out_shape=[
            jax.ShapeDtypeStruct((total_rows, heads * width), jnp.bfloat16),
            jax.ShapeDtypeStruct((8, head_size), jnp.float32),
            jax.ShapeDtypeStruct(hidden_state.shape, jnp.bfloat16),
        ],
        in_specs=in_specs,
        out_specs=[
            pl.BlockSpec((SEQUENCE_LENGTH, width), lambda s, h: (s, h)),
            pl.BlockSpec((8, head_size), lambda s, h: (0, 0)),
            pl.BlockSpec(hidden_state.shape, lambda s, h: (0, 0)),
        ],
        scratch_shapes=[
            pltpu.VMEM((grouping, SEQUENCE_LENGTH, head_size), jnp.bfloat16),
            pltpu.VMEM((SEQUENCE_LENGTH, head_size), jnp.bfloat16),
            pltpu.VMEM((SEQUENCE_LENGTH, head_size), jnp.bfloat16),
            pltpu.VMEM((SEQUENCE_LENGTH, out_width), jnp.bfloat16),
            whole_rows,
            whole_rows,
            whole_rows,
            whole_rows,
            whole_rows,
            *Scatter.scratch(size, *hidden_state.shape),
            *[part for left, other, _ in triples for part in Operand.scratch(size, left, other)],
        ],
        compiler_params=pltpu.CompilerParams(
            collective_id=collective_id, has_side_effects=True, vmem_limit_bytes=VMEM_LIMIT
        ),
        cost_estimate=pl.CostEstimate(
            flops=2 * total_rows * depth * heads * out_width + 10 * elements * head_size,
            bytes_accessed=100_000_000,
            transcendentals=elements,
        ),
        name="attention_backward",
    )(*operands)


def feed_half_kernel(
    half, tile, block, rows_far, cotangent_far, weight_far, hidden_far, slope_far,
    rows_ref, cotangent_ref, weight_ref, hidden_ref, slope_ref, row_sem, weight_sem, out_sem,
):
    total = rows_ref.shape[0]
    blocks = total // block
    tiles = half // tile

    def row_copies(index):
        piece = pl.ds(pl.multiple_of(index * block, block), block)
        return [
            pltpu.make_async_copy(far.at[piece], ref.at[piece], row_sem.at[at, index])
            for at, (far, ref) in enumerate(((rows_far, rows_ref), (cotangent_far, cotangent_ref)))
        ]

    def weight_copies(index):
        copies = []
        for part in range(3):
            columns = pl.ds(pl.multiple_of(part * half + index * tile, tile), tile)
            copies.append(
                pltpu.make_async_copy(
                    weight_far.at[:, columns], weight_ref.at[part, index], weight_sem.at[part, index]
                )
            )
        return copies

    def out_copies(index):
        piece = pl.ds(pl.multiple_of(index * block, block), block)
        return [
            pltpu.make_async_copy(ref.at[piece], far.at[piece], out_sem.at[at, index])
            for at, (far, ref) in enumerate(((hidden_far, hidden_ref), (slope_far, slope_ref)))
        ]

    for copy in row_copies(0) + weight_copies(0):
        copy.start()
    for index in range(1, tiles):
        for copy in weight_copies(index):
            copy.start()
    for index in range(1, blocks):
        for copy in row_copies(index):
            copy.start()

    def row_step(row_index, carry):
        piece = pl.ds(pl.multiple_of(row_index * block, block), block)
        for copy in row_copies(row_index):
            copy.wait()

        def step(index, carry):
            @pl.when(row_index == 0)
            def _():
                for copy in weight_copies(index):
                    copy.wait()

            start = pl.multiple_of(index * tile, tile)
            rows = rows_ref[piece, :]
            gate = simple_product(rows, weight_ref[0, index])
            up = simple_product(rows, weight_ref[1, index])
            back = simple_product(cotangent_ref[piece, :], weight_ref[2, index])
            sigmoid = 1.0 / (1.0 + jnp.exp(-gate))
            gated = gate * sigmoid
            hidden_ref[piece, pl.ds(start, tile)] = (gated * up).astype(jnp.bfloat16)
            slope_ref[piece, pl.ds(start, tile)] = (
                back * up * sigmoid * (1.0 + gate * (1.0 - sigmoid))
            ).astype(jnp.bfloat16)
            slope_ref[piece, pl.ds(half + start, tile)] = (back * gated).astype(jnp.bfloat16)
            return carry

        lax.fori_loop(0, tiles, step, 0)
        for copy in out_copies(row_index):
            copy.start()
        return carry

    lax.fori_loop(0, blocks, row_step, 0)
    for index in range(blocks):
        for copy in out_copies(index):
            copy.wait()


def feed_half(rows, cotangent, weight):
    total_rows, depth = rows.shape
    block = min(512, total_rows)
    half = weight.shape[1] // 3
    tile = 256 if half % 256 == 0 else 128
    blocks, tiles = total_rows // block, half // tile
    far = pl.BlockSpec(memory_space=pl.ANY)
    return pl.pallas_call(
        functools.partial(feed_half_kernel, half, tile, block),
        out_shape=[
            jax.ShapeDtypeStruct((total_rows, half), jnp.bfloat16),
            jax.ShapeDtypeStruct((total_rows, 2 * half), jnp.bfloat16),
        ],
        in_specs=[far] * 3,
        out_specs=[far] * 2,
        scratch_shapes=[
            pltpu.VMEM(rows.shape, rows.dtype),
            pltpu.VMEM(rows.shape, rows.dtype),
            pltpu.VMEM((3, tiles, depth, tile), weight.dtype),
            pltpu.VMEM((total_rows, half), jnp.bfloat16),
            pltpu.VMEM((total_rows, 2 * half), jnp.bfloat16),
            pltpu.SemaphoreType.DMA((2, blocks)),
            pltpu.SemaphoreType.DMA((3, tiles)),
            pltpu.SemaphoreType.DMA((2, blocks)),
        ],
        compiler_params=pltpu.CompilerParams(vmem_limit_bytes=VMEM_LIMIT),
        cost_estimate=pl.CostEstimate(
            flops=6 * total_rows * depth * half,
            bytes_accessed=2 * (2 * total_rows * depth + 3 * depth * half),
            transcendentals=total_rows * half,
        ),
        name="feed_half",
    )(rows, cotangent, weight)


def grad_kernel(pair_count, with_other, order_ref, *refs):
    pairs = [refs[2 * p : 2 * p + 2] for p in range(pair_count)]
    refs = refs[2 * pair_count :]
    step = pl.program_id(0)
    if with_other:
        other_ref, refs = refs[0], refs[1:]
        out_refs, held_ref, copy_sem = refs[:-2], refs[-2], refs[-1]
    else:
        out_ref = refs[0]
    start = 0
    for left_ref, right_ref in pairs:
        width = right_ref.shape[1]
        tile = next(t for t in (768, 512, 384, 256, 128) if width % t == 0)
        for column in range(0, width, tile):
            values = simple_product(left_ref[...], right_ref[:, column : column + tile])
            columns = slice(start + column, start + column + tile)
            if with_other:
                values = values + other_ref[0, :, columns].astype(jnp.float32)
                held_ref[step, :, columns] = values.astype(jnp.bfloat16)
            else:
                out_ref[:, :, columns] = values.reshape(*out_ref.shape[:2], tile).astype(jnp.bfloat16)
        start += width
    if with_other:
        copies = [
            pltpu.make_async_copy(held_ref.at[index], out_ref, copy_sem.at[index])
            for index, out_ref in enumerate(out_refs)
        ]
        for index, copy in enumerate(copies):
            pl.when(step == index)(copy.start)

        @pl.when(step == len(copies) - 1)
        def _():
            for copy in copies:
                copy.wait()


def grad_blocks(order, pairs, other=None, group=1):
    count = order.shape[0]
    depth, total_rows = pairs[0][0].shape
    block = depth // lax.axis_size("dp")
    width = sum(right.shape[1] for _, right in pairs)
    in_specs = []
    operands = []
    for left, right in pairs:
        in_specs += [
            pl.BlockSpec(
                (group * block, total_rows),
                (lambda k, at: (at[k], 0)) if group == 1 else (lambda k, at: (k, 0)),
            ),
            pl.BlockSpec(right.shape, lambda k, at: (0, 0), pipeline_mode=pl.Buffered(1)),
        ]
        operands += [left, right]
    scratch = []
    if other is not None:
        in_specs.append(pl.BlockSpec((1, block, width), lambda k, at: (k, 0, 0)))
        operands.append(other)
        out_shape = [jax.ShapeDtypeStruct((block, width), jnp.bfloat16)] * count
        out_specs = [pl.BlockSpec(memory_space=pl.ANY)] * count
        scratch = [
            pltpu.VMEM((count, block, width), jnp.bfloat16),
            pltpu.SemaphoreType.DMA((count,)),
        ]
    else:
        out_shape = [jax.ShapeDtypeStruct((count, block, width), jnp.bfloat16)]
        out_specs = [pl.BlockSpec((group, block, width), lambda k, at: (k, 0, 0))]
    out = pl.pallas_call(
        functools.partial(grad_kernel, len(pairs), other is not None),
        grid_spec=pltpu.PrefetchScalarGridSpec(
            num_scalar_prefetch=1,
            grid=(count // group,),
            in_specs=in_specs,
            out_specs=out_specs,
            scratch_shapes=scratch,
        ),
        out_shape=out_shape,
        compiler_params=pltpu.CompilerParams(vmem_limit_bytes=VMEM_LIMIT),
        cost_estimate=pl.CostEstimate(
            flops=2 * total_rows * count * block * width,
            bytes_accessed=2 * (total_rows * count * block * len(pairs) + width * (total_rows + count * block)),
            transcendentals=0,
        ),
        name="grad_blocks",
    )(order, *operands)
    return out if other is not None else out[0]


def reduce_over_chips(pairs, sizes):
    data_size = sizes[0]
    chips = data_size // 2
    me = lax.axis_index("dp")
    chip, core = me // 2, lax.rem(me, 2)
    ahead = lax.rem(chip + jnp.arange(chips, dtype=jnp.int32), chips) * 2
    other = lax.ppermute(
        grad_blocks(ahead + (1 - core), pairs),
        "dp",
        [(device, device ^ 1) for device in range(data_size)],
    )
    blocks = grad_blocks(ahead + core, pairs, other)
    up = lax.ppermute(blocks[chips - 1], "dp", [(device, device + 2) for device in range(2)])
    down = lax.ppermute(
        blocks[1],
        "dp",
        [(device, device - 2) for device in range(data_size - 2, data_size)],
    )
    return blocks, up, down


def pack_mixing_kernel(heads, query_ref, key_ref, value_ref, output_ref, out_ref):
    query_width = query_ref.shape[1] // heads
    head_size = key_ref.shape[1] // heads
    start = 0
    for head in range(heads):
        for ref, part in ((query_ref, query_width), (key_ref, head_size), (value_ref, head_size)):
            out_ref[:, start : start + part] = ref[:, head * part : (head + 1) * part]
            start += part
    out_ref[:, start:] = output_ref[...].T


def pack_feed_kernel(gate_ref, up_ref, down_ref, first_ref, second_ref):
    start = 0
    for out_ref in (first_ref, second_ref):
        width = out_ref.shape[1] // 3
        part = slice(start, start + width)
        out_ref[:, :width] = gate_ref[:, part]
        out_ref[:, width : 2 * width] = up_ref[:, part]
        out_ref[:, 2 * width :] = down_ref[part, :].T
        start += width


def finish_feed_kernel(
    own_ref, up_ref, down_ref, second_ref, output_rows_ref,
    output_rows_far, gate_far, up_far, down_far, gate_out, up_out, down_out, sem,
):
    copies = [
        pltpu.make_async_copy(source, target, sem.at[index])
        for index, (source, target) in enumerate(
            (
                (output_rows_ref, output_rows_far),
                (gate_out, gate_far),
                (up_out, up_far),
                (down_out, down_far),
            )
        )
    ]
    copies[0].start()
    for index, out in enumerate((gate_out, up_out, down_out)):
        start = 0
        for total_refs in ((own_ref, up_ref, down_ref), (second_ref,)):
            width = total_refs[0].shape[1] // 3
            part = slice(start, start + width)
            columns = slice(index * width, (index + 1) * width)
            total = sum(ref[:, columns].astype(jnp.float32) for ref in total_refs)
            if index == 2:
                out[part, :] = total.T
            else:
                out[:, part] = total
            start += width
        copies[1 + index].start()
    for copy in copies:
        copy.wait()


def finish_kernel(heads, *refs):
    mixing_ref, output_total_ref, terms_ref, input_rows_ref = refs[:4]
    far, held, sem = refs[4:13], refs[13:21], refs[21]
    (
        attention_term_out, query_out, key_out, value_out, query_gain_out, key_gain_out,
        output_out, feed_term_out,
    ) = held
    copies = [
        pltpu.make_async_copy(source, target, sem.at[index])
        for index, (source, target) in enumerate(zip((input_rows_ref, *held), far))
    ]
    copies[0].start()
    output_out[...] = output_total_ref[...].astype(jnp.float32).T
    copies[7].start()
    query_width = query_out.shape[1] // heads
    head_size = key_out.shape[1] // heads
    start = 0
    for head in range(heads):
        for out, part in ((query_out, query_width), (key_out, head_size), (value_out, head_size)):
            out[:, head * part : (head + 1) * part] = mixing_ref[:, start : start + part].astype(
                jnp.float32
            )
            start += part
    count = attention_term_out.shape[0]
    attention_term_out[...] = terms_ref[:count, :]
    feed_term_out[...] = terms_ref[count : 2 * count, :]
    query_gain_out[...] = terms_ref[2 * count : 2 * count + 1, :]
    key_gain_out[...] = terms_ref[2 * count + 1 : 2 * count + 2, :]
    for index in (1, 2, 3, 4, 5, 6, 8):
        copies[index].start()
    for copy in copies:
        copy.wait()


def finish_call(body, rows_shape, float_shapes, *operands):
    return pl.pallas_call(
        body,
        out_shape=[rows_shape, *float_shapes],
        in_specs=[pl.BlockSpec(memory_space=pltpu.VMEM)] * len(operands),
        out_specs=[pl.BlockSpec(memory_space=pl.ANY)] * (1 + len(float_shapes)),
        scratch_shapes=[pltpu.VMEM(shape.shape, shape.dtype) for shape in float_shapes]
        + [pltpu.SemaphoreType.DMA((1 + len(float_shapes),))],
        compiler_params=pltpu.CompilerParams(vmem_limit_bytes=VMEM_LIMIT),
        cost_estimate=pl.CostEstimate(flops=0, bytes_accessed=10_000_000, transcendentals=0),
    )(*operands)


def whole_call(body, shapes, *operands):
    return pl.pallas_call(
        body,
        out_shape=shapes,
        in_specs=[pl.BlockSpec(memory_space=pltpu.VMEM)] * len(operands),
        out_specs=[pl.BlockSpec(memory_space=pltpu.VMEM)] * len(shapes),
        compiler_params=pltpu.CompilerParams(vmem_limit_bytes=VMEM_LIMIT),
        cost_estimate=pl.CostEstimate(
            flops=0, bytes_accessed=4 * sum(operand.size for operand in operands), transcendentals=0
        ),
    )(*operands)


def per_device(
    block_input,
    attention_gain,
    query_weight,
    key_matrix,
    value_matrix,
    query_gain,
    key_gain,
    output_weight,
    feed_gain,
    gate_weight,
    up_weight,
    down_weight,
    out_cotangent,
):
    size = lax.axis_size("tensor")
    sizes = (lax.axis_size("dp"), size)
    model_width = block_input.shape[1]
    head_size = query_gain.shape[0]
    query_columns = query_weight.shape[1]
    key_columns = key_matrix.shape[1]
    heads = key_columns // head_size
    grouping = query_columns // key_columns
    hidden_columns = gate_weight.shape[1]
    qkv_columns = query_columns + 2 * key_columns
    first_columns = hidden_columns * 2 // 3 // 256 * 256 or hidden_columns // 2
    second_columns = hidden_columns - first_columns
    tables = turn_tables(head_size)

    block_width = query_weight.shape[0]
    (mixing_local,) = whole_call(
        functools.partial(pack_mixing_kernel, heads),
        [jax.ShapeDtypeStruct((block_width, qkv_columns + query_columns), jnp.bfloat16)],
        query_weight, key_matrix, value_matrix, output_weight,
    )
    mixing_full = lax.all_gather(mixing_local, "dp", axis=0, tiled=True)
    feed_locals = whole_call(
        pack_feed_kernel,
        [
            jax.ShapeDtypeStruct((block_width, 3 * columns), jnp.bfloat16)
            for columns in (first_columns, second_columns)
        ],
        gate_weight, up_weight, down_weight,
    )
    feed_full = [lax.all_gather(part, "dp", axis=0, tiled=True) for part in feed_locals]

    input_float = block_input.astype(jnp.float32)
    first_scale = row_scale(input_float)
    first_unit = input_float * first_scale
    mixer_local = (first_unit * attention_gain).astype(jnp.bfloat16)
    mixer_rows, mixer_turned, cotangent_rows, cotangent_turned = gather_rows(
        (mixer_local, out_cotangent), size, 0
    )

    raw, mixed_rows, totals = attention_forward(
        mixer_rows, mixing_full, tables, query_gain, key_gain, heads, grouping
    )
    local_shape = block_input.shape
    local_rows = local_shape[0]
    gain_rows = model_width // head_size
    gathered_shapes = [
        jax.ShapeDtypeStruct((size * local_rows, model_width), jnp.bfloat16),
        jax.ShapeDtypeStruct((model_width, size * local_rows), jnp.bfloat16),
    ]
    local_float = jax.ShapeDtypeStruct(local_shape, jnp.float32)
    local_half = jax.ShapeDtypeStruct(local_shape, jnp.bfloat16)
    row_sum = pltpu.VMEM((1, model_width), jnp.float32)
    own_rows = pltpu.VMEM(local_shape, jnp.bfloat16)
    scatter_scratch = Scatter.scratch(size, *local_shape)
    gather_scratch = Gather.scratch(size, *local_shape)
    feed_rows, feed_turned, hidden_state = scatter_call(
        functools.partial(between_forward_kernel, size),
        [(mixed_rows, mixing_full, qkv_columns)],
        size,
        [block_input, feed_gain.reshape(1, -1)],
        [],
        [*gathered_shapes, local_float],
        True,
        [own_rows, *scatter_scratch, *gather_scratch],
        1,
    )

    hidden_first, slope_first = feed_half(feed_rows, cotangent_rows, feed_full[0])
    blocks, up, down = reduce_over_chips(
        [(feed_turned, slope_first), (cotangent_turned, hidden_first)], sizes
    )
    blocks, later_full = lax.optimization_barrier((blocks, feed_full[1]))
    hidden_second, slope_second = feed_half(feed_rows, cotangent_rows, later_full)
    plain_order = jnp.arange(sizes[0], dtype=jnp.int32)
    second_grad = grad_blocks(
        plain_order, [(feed_turned, slope_second), (cotangent_turned, hidden_second)], group=2
    ).reshape(model_width, -1)
    second_grad, slope_second = lax.optimization_barrier((second_grad, slope_second))
    second_total = lax.psum_scatter(second_grad, "dp", scatter_dimension=0, tiled=True)
    chips = sizes[0] // 2
    middle_steps = tuple(range(2, chips - 1))
    chain_block = jax.ShapeDtypeStruct(blocks[0].shape, jnp.bfloat16)
    state_rows, state_turned, state_slope, feed_term, rising, falling = scatter_call(
        functools.partial(between_backward_kernel, size, chips, middle_steps),
        [(slope_first, feed_full[0], 0), (slope_second, later_full, 0)],
        size,
        [hidden_state, out_cotangent, feed_gain.reshape(1, -1)],
        [blocks[chips - step] for step in middle_steps]
        + [blocks[step] for step in middle_steps]
        + [up, down, blocks[1], blocks[chips - 1]],
        [
            *gathered_shapes,
            local_float,
            jax.ShapeDtypeStruct((gain_rows, head_size), jnp.float32),
            chain_block,
            chain_block,
        ],
        True,
        [
            own_rows,
            row_sum,
            pltpu.SemaphoreType.DMA((2,)),
            *scatter_scratch,
            *gather_scratch,
            *Chain.scratch(len(middle_steps), *blocks[0].shape),
        ],
        2,
    )
    up = lax.ppermute(
        rising, "dp", [(device, device + 2) for device in range(sizes[0] - 2)]
    )
    down = lax.ppermute(
        falling, "dp", [(device, device - 2) for device in range(2, sizes[0])]
    )
    output_grad = grad_blocks(plain_order, [(state_turned, mixed_rows)], group=4).reshape(model_width, -1)
    output_grad, state_rows = lax.optimization_barrier((output_grad, state_rows))
    output_total = lax.psum_scatter(output_grad, "dp", scatter_dimension=0, tiled=True)
    qkv_slope, head_terms, block_output = attention_backward(
        state_rows, mixing_full, qkv_columns, raw, mixed_rows, totals, tables,
        query_gain, key_gain, heads, grouping,
        [
            (hidden_first, feed_full[0], 2 * first_columns),
            (hidden_second, later_full, 2 * second_columns),
        ],
        hidden_state, size, 4,
    )
    mixing_grad = grad_blocks(plain_order, [(mixer_turned, qkv_slope)], group=4).reshape(model_width, -1)
    mixing_grad, qkv_slope = lax.optimization_barrier((mixing_grad, qkv_slope))
    mixing_total = lax.psum_scatter(mixing_grad, "dp", scatter_dimension=0, tiled=True)
    terms_shape = (2 * gain_rows + head_terms.shape[0], head_size)
    input_gradient, terms = scatter_call(
        functools.partial(last_kernel, sizes),
        [(qkv_slope, mixing_full, 0)],
        size,
        [
            block_input,
            attention_gain.reshape(1, -1),
            state_slope,
            jnp.concatenate([feed_term, head_terms], axis=0),
            mixer_rows,
        ],
        [],
        [local_half, jax.ShapeDtypeStruct(terms_shape, jnp.float32)],
        False,
        [
            row_sum,
            pltpu.VMEM(terms_shape, jnp.float32),
            pltpu.VMEM(terms_shape, jnp.float32),
            pltpu.VMEM((size, *terms_shape), jnp.float32),
            pltpu.VMEM((sizes[0], *terms_shape), jnp.float32),
            *[pltpu.SemaphoreType.DMA((count - 1,)) for count in (size, size, *sizes[:1] * 2)],
            *scatter_scratch,
        ],
        3,
    )

    def whole_float(*shape):
        return jax.ShapeDtypeStruct(shape, jnp.float32)

    block_output, gate_gradient, up_gradient, down_gradient = finish_call(
        finish_feed_kernel,
        local_half,
        [
            whole_float(block_width, hidden_columns),
            whole_float(block_width, hidden_columns),
            whole_float(hidden_columns, block_width),
        ],
        blocks[0], up, down, second_total, block_output,
    )
    (
        input_gradient, attention_term, query_gradient, key_gradient, value_gradient,
        query_term, key_term, output_gradient, feed_term,
    ) = finish_call(
        functools.partial(finish_kernel, heads),
        local_half,
        [
            whole_float(gain_rows, head_size),
            whole_float(block_width, query_columns),
            whole_float(block_width, key_columns),
            whole_float(block_width, key_columns),
            whole_float(1, head_size),
            whole_float(1, head_size),
            whole_float(query_columns, block_width),
            whole_float(gain_rows, head_size),
        ],
        mixing_total, output_total, terms, input_gradient,
    )
    return (
        block_output,
        input_gradient,
        attention_term.reshape(-1),
        query_gradient,
        key_gradient,
        value_gradient,
        query_term.reshape(-1),
        key_term.reshape(-1),
        output_gradient,
        feed_term.reshape(-1),
        gate_gradient,
        up_gradient,
        down_gradient,
    )


def solution(mesh):
    in_specs = (
        P(("dp", "tensor"), None),
        P(),
        P("dp", "tensor"),
        P("dp", "tensor"),
        P("dp", "tensor"),
        P(),
        P(),
        P("tensor", "dp"),
        P(),
        P("dp", "tensor"),
        P("dp", "tensor"),
        P("tensor", "dp"),
        P(("dp", "tensor"), None),
    )
    out_specs = (
        P(("dp", "tensor"), None),
        P(("dp", "tensor"), None),
        P(),
        P("dp", "tensor"),
        P("dp", "tensor"),
        P("dp", "tensor"),
        P(),
        P(),
        P("tensor", "dp"),
        P(),
        P("dp", "tensor"),
        P("dp", "tensor"),
        P("tensor", "dp"),
    )

    return jax.shard_map(per_device, mesh=mesh, in_specs=in_specs, out_specs=out_specs, check_vma=False)
```

```python
import functools

import jax
import jax.numpy as jnp
import numpy as np
from jax import lax
from jax.experimental import pallas as pl
from jax.experimental.pallas import tpu as pltpu
from jax.sharding import PartitionSpec as P


SEQUENCE_LENGTH = 1024

epsilon = 1e-06
rope_base = 1000000.0


MESH = pl.DeviceIdType.MESH
VMEM_LIMIT = 62 * 1024 * 1024


def row_scale(values):
    return lax.rsqrt(jnp.mean(values * values, axis=-1, keepdims=True) + epsilon)


def times_transposed(first_operand, second_operand):
    return lax.dot_general(
        first_operand, second_operand, (((1,), (1,)), ((), ())), preferred_element_type=jnp.float32
    )


def simple_product(first_operand, second_operand):
    return jnp.dot(first_operand, second_operand, preferred_element_type=jnp.float32)


def remote(source, target, send_sem, recv_sem, peer, axis="tensor"):
    return pltpu.make_async_remote_copy(
        src_ref=source,
        dst_ref=target,
        send_sem=send_sem,
        recv_sem=recv_sem,
        device_id={axis: peer},
        device_id_type=MESH,
    )


def greet(peers):
    barrier = pltpu.get_barrier_semaphore()
    for axis, peer in peers:
        pl.semaphore_signal(barrier, inc=1, device_id={axis: peer}, device_id_type=MESH)
    pl.semaphore_wait(barrier, len(peers))


def square_peers(me):
    column = lax.rem(me, 2)
    row = me // 2
    return row * 2 + (1 - column), (1 - row) * 2 + column, (1 - row) * 2 + (1 - column)


def neighbours(size):
    if size == 4:
        beside, below, _ = square_peers(lax.axis_index("tensor"))
        return [("tensor", beside), ("tensor", below)]
    return [("tensor", peer) for peer in other_members("tensor", size)]


def other_members(axis, count):
    me = lax.axis_index(axis)
    return [lax.rem(me + step, count) for step in range(1, count)]


class Gather:
    def __init__(
        self, size, own_ref, out_ref, turned_out_ref, held_ref, turned_ref, send_sem, recv_sem, local_sem, turned_sem
    ):
        self.size, self.own, self.out, self.held = size, own_ref, out_ref, held_ref
        self.turned_out, self.turned = turned_out_ref, turned_ref
        self.send_sem, self.recv_sem, self.local_sem = send_sem, recv_sem, local_sem
        self.turned_sem = turned_sem
        self.me = lax.axis_index("tensor")
        self.rows = own_ref.shape[0]
        self.copies, self.stores, self.turns = [], [], []

    @staticmethod
    def scratch(size, rows, columns):
        sends, local = (12, 8) if size == 4 else (size - 1, size)
        return [
            pltpu.VMEM((size, rows, columns), jnp.bfloat16),
            pltpu.VMEM((columns, size * rows), jnp.bfloat16),
            pltpu.SemaphoreType.DMA((sends,)),
            pltpu.SemaphoreType.DMA((sends,)),
            pltpu.SemaphoreType.DMA((local,)),
            pltpu.SemaphoreType.DMA((local,)),
        ]

    def send(self, source, target, peer):
        index = len(self.copies)
        copy = remote(source, target, self.send_sem.at[index], self.recv_sem.at[index], peer)
        copy.start()
        self.copies.append(copy)
        return copy

    def store(self, source, start, count):
        piece = pl.ds(pl.multiple_of(start, count), count)
        copy = pltpu.make_async_copy(source, self.out.at[piece], self.local_sem.at[len(self.stores)])
        copy.start()
        self.stores.append(copy)
        width = min(256, self.turned.shape[0])

        def turn_part(index, carry):
            columns = pl.ds(pl.multiple_of(index * width, width), width)
            self.turned[columns, piece] = source[:, columns].T
            return carry

        lax.fori_loop(0, self.turned.shape[0] // width, turn_part, 0)
        turn_copy = pltpu.make_async_copy(
            self.turned.at[:, piece], self.turned_out.at[:, piece], self.turned_sem.at[len(self.turns)]
        )
        turn_copy.start()
        self.turns.append(turn_copy)

    def quarters(self):
        quarter = self.rows // 4
        return [pl.ds(index * quarter, quarter) for index in range(4)]

    def start(self, stage):
        own, held = self.own, self.held
        if self.size != 4:
            if stage == 0:
                for peer in other_members("tensor", self.size):
                    self.send(own, held.at[self.me], peer)
            return
        beside, below, _ = square_peers(self.me)
        parts = self.quarters()
        upper, lower = parts[stage], parts[2 + stage]
        for part, peer in ((upper, beside), (lower, below), (lower, beside), (upper, below)):
            self.send(own.at[part], held.at[self.me, part], peer)

    def forward(self):
        own, held, rows = self.own, self.held, self.rows
        if self.size != 4:
            self.store(own, self.me * rows, rows)
            return
        beside, below, _ = square_peers(self.me)
        half = rows // 2
        self.store(own.at[pl.ds(0, half)], self.me * rows, half)
        self.store(own.at[pl.ds(half, half)], self.me * rows + half, half)
        parts = self.quarters()
        for stage in range(2):
            self.copies[4 * stage].wait_recv()
            self.send(held.at[beside, parts[stage]], held.at[beside, parts[stage]], below)
            self.copies[4 * stage + 1].wait_recv()
            self.send(held.at[below, parts[2 + stage]], held.at[below, parts[2 + stage]], beside)

    def finish(self):
        held, rows = self.held, self.rows
        if self.size != 4:
            for step, copy in enumerate(self.copies):
                copy.wait_recv()
                slot = lax.rem(self.me + self.size - step - 1, self.size)
                self.store(held.at[slot], slot * rows, rows)
        else:
            beside, below, across = square_peers(self.me)
            half = rows // 2
            first, second = pl.ds(0, half), pl.ds(half, half)
            self.store(held.at[beside, first], beside * rows, half)
            self.store(held.at[below, second], below * rows + half, half)
            for indices, slot, start in (
                ((2, 6), beside, half),
                ((3, 7), below, 0),
                ((8, 10), across, 0),
                ((9, 11), across, half),
            ):
                for index in indices:
                    self.copies[index].wait_recv()
                self.store(held.at[slot, pl.ds(start, half)], slot * rows + start, half)
        for copy in self.copies:
            copy.wait_send()
        for copy in self.stores + self.turns:
            copy.wait()


def gather_kernel(size, count, *refs):
    own_refs, out_refs, rest = refs[:count], refs[count : 3 * count], refs[3 * count :]
    greet(neighbours(size))
    gathers = [
        Gather(size, own_refs[k], *out_refs[2 * k : 2 * k + 2], *rest[6 * k : 6 * k + 6])
        for k in range(count)
    ]
    for gather in gathers:
        gather.start(0)
        gather.start(1)
        gather.forward()
    for gather in gathers:
        gather.finish()


def gather_rows(arrays, size, collective_id):
    count = len(arrays)
    rows, columns = arrays[0].shape
    scratch = []
    out_shape = []
    for _ in arrays:
        scratch += Gather.scratch(size, rows, columns)
        out_shape += [
            jax.ShapeDtypeStruct((size * rows, columns), jnp.bfloat16),
            jax.ShapeDtypeStruct((columns, size * rows), jnp.bfloat16),
        ]
    return pl.pallas_call(
        functools.partial(gather_kernel, size, count),
        out_shape=out_shape,
        in_specs=[pl.BlockSpec(memory_space=pltpu.VMEM)] * count,
        out_specs=[pl.BlockSpec(memory_space=pl.ANY)] * len(out_shape),
        scratch_shapes=scratch,
        compiler_params=pltpu.CompilerParams(
            collective_id=collective_id, has_side_effects=True, vmem_limit_bytes=VMEM_LIMIT
        ),
        cost_estimate=pl.CostEstimate(
            flops=0, bytes_accessed=count * 30 * size * rows * columns, transcendentals=0
        ),
        name="gather_rows",
    )(*arrays)


class Operand:
    def __init__(self, size, first_column, left_far, weight_far, left, weight, left_sem, weight_sem):
        self.left, self.weight = left, weight
        self.rows = left.shape[0] // size
        self.tile = min(512, weight.shape[0])
        self.far = left_far, weight_far
        self.first_column = first_column
        self.left_sem, self.weight_sem = left_sem, weight_sem

    @staticmethod
    def scratch(size, left, weight):
        width = left.shape[1]
        return [
            pltpu.VMEM(left.shape, left.dtype),
            pltpu.VMEM((weight.shape[0], width), weight.dtype),
            pltpu.SemaphoreType.DMA((size,)),
            pltpu.SemaphoreType.DMA((max(1, weight.shape[0] // 512),)),
        ]

    def left_copy(self, slot, owner):
        piece = pl.ds(pl.multiple_of(owner * self.rows, self.rows), self.rows)
        return pltpu.make_async_copy(self.far[0].at[piece], self.left.at[piece], self.left_sem.at[slot])

    def weight_copy(self, index):
        piece = pl.ds(pl.multiple_of(index * self.tile, self.tile), self.tile)
        columns = pl.ds(self.first_column, self.left.shape[1])
        return pltpu.make_async_copy(
            self.far[1].at[piece, columns], self.weight.at[piece], self.weight_sem.at[index]
        )


def block_product(operands, start, rows, fresh, write, after):
    total = operands[0].weight.shape[0]
    tile = operands[0].tile
    start = pl.multiple_of(start, rows)

    def step(index, carry):
        @pl.when(fresh)
        def _():
            for operand in operands:
                operand.weight_copy(index).wait()

        columns = pl.ds(pl.multiple_of(index * tile, tile), tile)
        values = None
        for operand in operands:
            part = times_transposed(
                operand.left[pl.ds(start, rows), :], operand.weight[columns, :]
            )
            values = part if values is None else values + part
        write(columns, values)
        after(index)
        return carry

    lax.fori_loop(0, total // tile, step, 0)


class Scatter:
    def __init__(self, size, outgoing, *rest):
        self.size, self.outgoing = size, outgoing
        if size == 4:
            self.passing, rest = rest[0], rest[1:]
        self.arriving, self.send_sem, self.recv_sem = rest
        self.rows = outgoing.shape[1]
        self.me = lax.axis_index("tensor")
        self.stages = 2 if size == 4 else 1
        self.plan()

    @staticmethod
    def scratch(size, rows, columns):
        if size == 4:
            sends = 10
            buffers = [
                pltpu.VMEM((4, rows, columns), jnp.bfloat16),
                pltpu.VMEM((2, rows // 2, columns), jnp.bfloat16),
                pltpu.VMEM((2, rows, columns), jnp.bfloat16),
            ]
        else:
            sends = size - 1
            buffers = [
                pltpu.VMEM((size, rows, columns), jnp.bfloat16),
                pltpu.VMEM((size - 1, rows, columns), jnp.bfloat16),
            ]
        return buffers + [pltpu.SemaphoreType.DMA((sends,)), pltpu.SemaphoreType.DMA((sends,))]

    def prepare(self, index, source, target, peer):
        return remote(source, target, self.send_sem.at[index], self.recv_sem.at[index], peer)

    def plan(self):
        outgoing, arriving = self.outgoing, self.arriving
        if self.size != 4:
            self.copies = [
                self.prepare(step, outgoing.at[step], arriving.at[step], peer)
                for step, peer in enumerate(other_members("tensor", self.size))
            ]
            self.early, self.starts = (), tuple((step, step) for step in range(self.size - 1))
            return
        beside, below, _ = square_peers(self.me)
        half, quarter = self.rows // 2, self.rows // 4
        first, second = pl.ds(0, half), pl.ds(half, half)
        middle = outgoing.shape[2] // 2
        left, right = pl.ds(0, middle), pl.ds(middle, middle)
        upper = [pl.ds(stage * quarter, quarter) for stage in range(2)]
        lower = [pl.ds(half + stage * quarter, quarter) for stage in range(2)]
        everything = pl.ds(0, half)
        self.copies = [
            self.prepare(0, outgoing.at[0, first, left], self.passing.at[0, everything, left], beside),
            self.prepare(1, outgoing.at[0, second, left], self.passing.at[1, everything, left], below),
            self.prepare(2, outgoing.at[0, first, right], self.passing.at[0, everything, right], beside),
            self.prepare(3, outgoing.at[0, second, right], self.passing.at[1, everything, right], below),
            self.prepare(4, outgoing.at[1, first], arriving.at[0, first], beside),
            self.prepare(5, outgoing.at[2, second], arriving.at[1, second], below),
            self.prepare(6, outgoing.at[1, lower[0]], arriving.at[0, lower[0]], beside),
            self.prepare(7, outgoing.at[2, upper[0]], arriving.at[1, upper[0]], below),
            self.prepare(8, outgoing.at[1, lower[1]], arriving.at[0, lower[1]], beside),
            self.prepare(9, outgoing.at[2, upper[1]], arriving.at[1, upper[1]], below),
        ]
        self.early, self.starts = (0, 1), ((0, 2), (0, 3), (1, 4), (2, 5))

    def owner(self, slot):
        if self.size != 4:
            return lax.rem(self.me + slot + 1, self.size)
        beside, below, across = square_peers(self.me)
        return jnp.where(
            slot == 0, across, jnp.where(slot == 1, beside, jnp.where(slot == 2, below, self.me))
        )

    def load(self, operands):
        tiles = operands[0].weight.shape[0] // operands[0].tile
        for operand in operands:
            operand.left_copy(0, self.owner(0)).start()
        for index in range(tiles):
            for operand in operands:
                operand.weight_copy(index).start()
        for slot in range(1, self.size):
            for operand in operands:
                operand.left_copy(slot, self.owner(slot)).start()

    def fill(self, operands, look=None):
        rows = self.rows

        def step(slot, carry):
            owner = self.owner(slot)
            for operand in operands:
                operand.left_copy(slot, owner).wait()

            def write(columns, values):
                self.outgoing[slot, :, columns] = values.astype(self.outgoing.dtype)
                if look is not None:
                    look(owner, columns, values)

            tiles = operands[0].weight.shape[0] // operands[0].tile

            def after(index):
                for early in self.early:
                    pl.when((slot == 0) & (index == max(tiles // 2, 1) - 1))(self.copies[early].start)

            block_product(operands, owner * rows, rows, slot == 0, write, after)
            for at, index in self.starts:
                pl.when(slot == at)(self.copies[index].start)
            return carry

        lax.fori_loop(0, self.size, step, 0)

    def relay(self):
        if self.size != 4:
            return
        half, quarter = self.rows // 2, self.rows // 4
        for stage in range(2):
            for arrivals, source, slot, start, onward in (
                ((1, 3), 1, 1, half, 6 + 2 * stage),
                ((0, 2), 0, 2, 0, 7 + 2 * stage),
            ):
                if stage == 0:
                    for index in arrivals:
                        self.copies[index].wait_recv()
                piece = pl.ds(start + stage * quarter, quarter)
                self.outgoing[slot, piece, :] = add_rounded(
                    self.outgoing[slot, piece, :],
                    self.passing[source, stage * quarter : (stage + 1) * quarter, :],
                )
                self.copies[onward].start()

    def collect(self, stage):
        if self.size != 4:
            for copy in self.copies:
                copy.wait_recv()
            return
        if stage == 0:
            self.copies[4].wait_recv()
            self.copies[5].wait_recv()
        self.copies[6 + 2 * stage].wait_recv()
        self.copies[7 + 2 * stage].wait_recv()

    def over_rows(self, stage, body):
        if self.size != 4:
            over_pieces(self.rows, body)
            return
        half, quarter = self.rows // 2, self.rows // 4
        over_pieces(quarter, body, stage * quarter)
        over_pieces(quarter, body, half + stage * quarter)

    def over_stages(self, body, done=None):
        for stage in range(self.stages):
            self.collect(stage)
            self.over_rows(stage, body)
            if done is not None:
                done(stage)

    def total(self, piece):
        total = self.outgoing[self.size - 1, piece, :].astype(jnp.float32)
        for index in range(self.arriving.shape[0]):
            total = total + self.arriving[index, piece, :].astype(jnp.float32)
        return total

    def drain(self):
        for copy in self.copies:
            copy.wait_send()


class Chain:
    def __init__(
        self, chips, steps, rising_refs, falling_refs, up_ref, down_ref,
        rise, fall, up, down, load_sem, send_sem, recv_sem,
    ):
        self.chips, self.steps = chips, steps
        self.rise, self.fall, self.up, self.down = rise, fall, up, down
        device = lax.axis_index("dp")
        self.chip = device // 2
        count = len(steps)
        self.loads = [
            pltpu.make_async_copy(source, target, load_sem.at[index])
            for index, (source, target) in enumerate(
                [(up_ref, up.at[0]), (down_ref, down.at[0])]
                + [(ref, rise.at[index]) for index, ref in enumerate(rising_refs)]
                + [(ref, fall.at[index]) for index, ref in enumerate(falling_refs)]
            )
        ]
        above = lax.rem(device + 2, 2 * chips)
        under = lax.rem(device + 2 * chips - 2, 2 * chips)
        self.neighbours = [("dp", above), ("dp", under)]
        self.rises = [
            remote(rise.at[i], up.at[i + 1], send_sem.at[i], recv_sem.at[i], above, "dp")
            for i in range(count)
        ]
        self.falls = [
            remote(
                fall.at[i], down.at[i + 1], send_sem.at[count + i], recv_sem.at[count + i], under, "dp"
            )
            for i in range(count)
        ]

    @staticmethod
    def scratch(count, rows, columns):
        return [
            pltpu.VMEM((count, rows, columns), jnp.bfloat16),
            pltpu.VMEM((count, rows, columns), jnp.bfloat16),
            pltpu.VMEM((count + 1, rows, columns), jnp.bfloat16),
            pltpu.VMEM((count + 1, rows, columns), jnp.bfloat16),
            pltpu.SemaphoreType.DMA((2 * count + 2,)),
            pltpu.SemaphoreType.DMA((2 * count,)),
            pltpu.SemaphoreType.DMA((2 * count,)),
        ]

    def load(self):
        for copy in self.loads:
            copy.start()

    def step(self, index):
        if index == 0:
            for copy in self.loads:
                copy.wait()
        step = self.steps[index]
        rows = self.rise.shape[1]
        sends_up = self.chip < step
        sends_down = self.chip >= self.chips - step

        @pl.when(sends_up & (self.chip > 0))
        def _():
            def add(piece):
                self.rise[index, piece, :] = add_rounded(
                    self.rise[index, piece, :], self.up[index, piece, :]
                )

            over_pieces(rows, add)

        pl.when(sends_up)(self.rises[index].start)

        @pl.when(sends_down & (self.chip < self.chips - 1))
        def _():
            def add(piece):
                self.fall[index, piece, :] = add_rounded(
                    self.fall[index, piece, :], self.down[index, piece, :]
                )

            over_pieces(rows, add)

        pl.when(sends_down)(self.falls[index].start)

    def arrives(self, index):
        step = self.steps[index]
        from_under = (self.chip > 0) & (self.chip <= step)
        from_above = (self.chip < self.chips - 1) & (self.chip >= self.chips - step - 1)
        return from_under, from_above

    def wait(self, index):
        from_under, from_above = self.arrives(index)
        pl.when(from_under)(self.rises[index].wait_recv)
        pl.when(from_above)(self.falls[index].wait_recv)

    def drain(self):
        for index, step in enumerate(self.steps):
            pl.when(self.chip < step)(self.rises[index].wait_send)
            pl.when(self.chip >= self.chips - step)(self.falls[index].wait_send)


def add_rounded(first, second):
    return (first.astype(jnp.float32) + second.astype(jnp.float32)).astype(jnp.bfloat16)


def over_pieces(rows, body, start=0):
    count = min(32, rows)

    def step(index, carry):
        body(pl.ds(pl.multiple_of(start + index * count, count), count))
        return carry

    lax.fori_loop(0, rows // count, step, 0)


def send_terms(axis, peers, source, landing, send_sem, recv_sem):
    me = lax.axis_index(axis)
    landing[me] = source[...]
    copies = []
    for step, peer in enumerate(peers):
        copy = remote(source, landing.at[me], send_sem.at[step], recv_sem.at[step], peer, axis)
        copy.start()
        copies.append(copy)
    return copies


def add_terms(landing, copies):
    for copy in copies:
        copy.wait_recv()
    total = landing[0]
    for index in range(1, landing.shape[0]):
        total = total + landing[index]
    return total


def split_operands(refs, size, first_columns):
    count = len(first_columns)
    far, refs, scratch = refs[: 2 * count], refs[2 * count : -4 * count], refs[-4 * count :]
    operands = [
        Operand(size, first, *far[2 * p : 2 * p + 2], *scratch[4 * p : 4 * p + 4])
        for p, first in enumerate(first_columns)
    ]
    return operands, refs


def store_row(target_ref, row_ref):
    width = target_ref.shape[1]
    for index in range(row_ref.shape[1] // width):
        target_ref[index : index + 1, :] = row_ref[:, index * width : (index + 1) * width]


def between_forward_kernel(size, first_columns, *refs):
    operands, refs = split_operands(refs, size, first_columns)
    input_ref, gain_ref, gathered_ref, turned_ref, state_ref, own_ref = refs[:6]
    buffers = 5 if size == 4 else 4
    scatter = Scatter(size, *refs[6 : 6 + buffers])
    gather = Gather(size, own_ref, gathered_ref, turned_ref, *refs[6 + buffers :])
    scatter.load(operands)
    greet(neighbours(size))
    scatter.fill(operands)
    scatter.relay()

    def norm(piece):
        state = input_ref[piece, :].astype(jnp.float32) + scatter.total(piece)
        state_ref[piece, :] = state
        own_ref[piece, :] = (state * row_scale(state) * gain_ref[...]).astype(own_ref.dtype)

    scatter.over_stages(norm, gather.start)
    gather.forward()
    gather.finish()
    scatter.drain()


def between_backward_kernel(size, chips, steps, first_columns, *refs):
    operands, refs = split_operands(refs, size, first_columns)
    state_ref, cotangent_ref, gain_ref = refs[:3]
    chain_count = 2 * len(steps) + 2
    chain_refs, last_refs, refs = refs[3 : 3 + chain_count], refs[3 + chain_count : 5 + chain_count], refs[5 + chain_count :]
    gathered_ref, gathered_turned_ref, slope_ref, term_ref, rising_ref, falling_ref = refs[:6]
    own_ref, sum_ref, last_sem = refs[6:9]
    buffers = 5 if size == 4 else 4
    scatter = Scatter(size, *refs[9 : 9 + buffers])
    gather = Gather(size, own_ref, gathered_ref, gathered_turned_ref, *refs[9 + buffers : 15 + buffers])
    chain = Chain(
        chips, steps, chain_refs[: len(steps)], chain_refs[len(steps) : -2], *chain_refs[-2:],
        *refs[15 + buffers :],
    )
    last_loads = [
        pltpu.make_async_copy(source, target, last_sem.at[index])
        for index, (source, target) in enumerate(zip(last_refs, (rising_ref, falling_ref)))
    ]
    chain.load()
    scatter.load(operands)
    for load in last_loads:
        load.start()
    greet(neighbours(size) + chain.neighbours)
    chain.step(0)
    scatter.fill(operands)
    scatter.relay()
    sum_ref[...] = jnp.zeros_like(sum_ref)

    def norm(piece):
        back = scatter.total(piece)
        state = state_ref[piece, :]
        scale = row_scale(state)
        unit = state * scale
        sum_ref[...] += jnp.sum(back * unit, axis=0, keepdims=True)
        unit_slope = back * gain_ref[...]
        slope = cotangent_ref[piece, :].astype(jnp.float32) + scale * (
            unit_slope - unit * jnp.mean(unit_slope * unit, axis=-1, keepdims=True)
        )
        slope_ref[piece, :] = slope
        own_ref[piece, :] = slope.astype(own_ref.dtype)

    scatter.over_stages(norm, gather.start)
    store_row(term_ref, sum_ref)
    gather.forward()
    chain.wait(0)
    for index in range(1, len(steps)):
        chain.step(index)
        chain.wait(index)
    for load in last_loads:
        load.wait()
    last = len(steps)
    for needed, landing, out_ref in (
        ((chain.chip > 0) & (chain.chip < chips - 1), chain.up, rising_ref),
        ((chain.chip > 0) & (chain.chip < chips - 1), chain.down, falling_ref),
    ):

        @pl.when(needed)
        def _(landing=landing, out_ref=out_ref):
            def add(piece):
                out_ref[piece, :] = add_rounded(out_ref[piece, :], landing[last, piece, :])

            over_pieces(out_ref.shape[0], add)

    gather.finish()
    scatter.drain()
    chain.drain()


def last_kernel(sizes, first_columns, *refs):
    data_size, size = sizes
    operands, refs = split_operands(refs, size, first_columns)
    input_ref, gain_ref, slope_ref, terms_ref, rows_ref = refs[:5]
    gradient_ref, terms_out_ref, sum_ref, partial_ref, group_ref, inner, outer = refs[5:12]
    inner_send, inner_recv, outer_send, outer_recv = refs[12:16]
    mixing = Scatter(size, *refs[16:])
    rows = gradient_ref.shape[0]
    mixing.load(operands)
    greet(
        [("tensor", peer) for peer in other_members("tensor", size)]
        + [("dp", peer) for peer in other_members("dp", data_size)]
    )
    sum_ref[...] = jnp.zeros_like(sum_ref)

    def look(owner, columns, values):
        piece = pl.ds(pl.multiple_of(owner * rows, rows), rows)
        sum_ref[:, columns] += jnp.sum(
            values * rows_ref[piece, columns].astype(jnp.float32), axis=0, keepdims=True
        )

    mixing.fill(operands, look)
    sum_ref[...] = sum_ref[...] / gain_ref[...]
    kept = partial_ref.shape[0] - terms_ref.shape[0]
    partial_ref[kept:, :] = terms_ref[...]
    store_row(partial_ref, sum_ref)
    inner_copies = send_terms(
        "tensor", other_members("tensor", size), partial_ref, inner, inner_send, inner_recv
    )
    mixing.relay()
    group_ref[...] = add_terms(inner, inner_copies)
    outer_copies = send_terms(
        "dp", other_members("dp", data_size), group_ref, outer, outer_send, outer_recv
    )
    terms_out_ref[...] = add_terms(outer, outer_copies)

    def norm(piece):
        back = mixing.total(piece)
        values = input_ref[piece, :].astype(jnp.float32)
        scale = row_scale(values)
        unit = values * scale
        unit_slope = back * gain_ref[...]
        gradient_ref[piece, :] = (
            slope_ref[piece, :]
            + scale * (unit_slope - unit * jnp.mean(unit_slope * unit, axis=-1, keepdims=True))
        ).astype(gradient_ref.dtype)

    mixing.over_stages(norm)
    for copy in inner_copies + outer_copies:
        copy.wait_send()
    mixing.drain()


def scatter_call(body, triples, size, others, far, outs, gathered, scratch, collective_id):
    far_spec = pl.BlockSpec(memory_space=pl.ANY)
    operands = [array for left, weight, _ in triples for array in (left, weight)]
    in_specs = [far_spec] * len(operands)
    for other in others:
        in_specs.append(pl.BlockSpec(other.shape, lambda i: (0, 0), pipeline_mode=pl.Buffered(1)))
    in_specs += [far_spec] * len(far)
    out_specs = [pl.BlockSpec(out.shape, lambda i: (0, 0)) for out in outs]
    if gathered:
        out_specs[:2] = [far_spec] * 2
    return pl.pallas_call(
        functools.partial(body, tuple(first for _, _, first in triples)),
        grid=(1,),
        out_shape=outs,
        in_specs=in_specs,
        out_specs=out_specs,
        scratch_shapes=list(scratch)
        + [part for left, weight, _ in triples for part in Operand.scratch(size, left, weight)],
        compiler_params=pltpu.CompilerParams(
            collective_id=collective_id, has_side_effects=True, vmem_limit_bytes=VMEM_LIMIT
        ),
        cost_estimate=pl.CostEstimate(
            flops=sum(2 * left.size * weight.shape[0] for left, weight, _ in triples),
            bytes_accessed=150_000_000,
            transcendentals=0,
        ),
    )(*operands, *others, *far)


LOG2E = 1.4426950408889634


def turn_tables(head_size):
    half_size = head_size // 2
    frequency = np.float32(rope_base) ** (
        -(np.arange(half_size, dtype=np.float32) * np.float32(2.0) / np.float32(head_size))
    )
    frequency = frequency.astype(np.float64)
    sign = np.concatenate([-np.ones(half_size), np.ones(half_size)])[None, :]
    positions = np.concatenate([np.arange(0, SEQUENCE_LENGTH, 128), np.arange(128)])
    angles = positions[:, None] * np.concatenate([frequency, frequency])[None, :]
    return np.cos(angles).astype(np.float32), (sign * np.sin(angles)).astype(np.float32)


def fill_tables(few_cosines_ref, few_sines_ref, cosine_ref, sine_ref):
    coarse = few_cosines_ref.shape[0] - 128
    near_cosine, near_sine = few_cosines_ref[coarse:, :], few_sines_ref[coarse:, :]

    def step(index, carry):
        far_cosine = few_cosines_ref[pl.ds(index, 1), :]
        far_sine = few_sines_ref[pl.ds(index, 1), :]
        rows = pl.ds(pl.multiple_of(index * 128, 128), 128)
        cosine_ref[rows, :] = far_cosine * near_cosine - far_sine * near_sine
        sine_ref[rows, :] = far_sine * near_cosine + far_cosine * near_sine
        return carry

    lax.fori_loop(0, coarse, step, 0)


def turn(values, cosine, sine):
    return values * cosine + pltpu.roll(values, values.shape[-1] // 2, 1) * sine


def turn_back(values, cosine, sine):
    return values * cosine - pltpu.roll(values, values.shape[-1] // 2, 1) * sine


def contract_first(first_operand, second_operand):
    return lax.dot_general(
        first_operand, second_operand, (((0,), (0,)), ((), ())), preferred_element_type=jnp.float32
    )


def visible_scores(key_rows, query_rows, first_row, multiplier):
    scores = times_transposed(key_rows, query_rows) * multiplier
    _, queries = scores.shape
    key_at = lax.broadcasted_iota(jnp.int32, (queries, queries), 0)
    query_at = lax.broadcasted_iota(jnp.int32, (queries, queries), 1)
    corner = jnp.where(query_at >= key_at, scores[first_row:], -1e30)
    if first_row == 0:
        return corner
    return jnp.concatenate([scores[:first_row], corner], axis=0)


def turn_heads(
    grouping, head_size, raw_ref, query_gain_ref, key_gain_ref, cosine_ref, sine_ref, query_ref, key_ref, value_ref
):
    def turned(start, gain):
        raw = raw_ref[:, pl.ds(start, head_size)]
        return turn(raw * row_scale(raw) * gain, cosine_ref[...], sine_ref[...]).astype(jnp.bfloat16)

    def step(part, carry):
        query_ref[part] = turned(pl.multiple_of(part * head_size, head_size), query_gain_ref[...])
        return carry

    lax.fori_loop(0, grouping, step, 0)
    key_ref[...] = turned(grouping * head_size, key_gain_ref[...])
    value_ref[...] = raw_ref[:, (grouping + 1) * head_size :].astype(jnp.bfloat16)


def attention_forward_kernel(
    grouping, head_size, block, rows_ref, weight_ref, few_cosines_ref, few_sines_ref, query_gain_ref, key_gain_ref,
    raw_ref, mixed_ref, total_ref, query_ref, key_ref, value_ref, cosine_ref, sine_ref,
):
    sequence = rows_ref.shape[0]
    multiplier = head_size ** (-0.5) * LOG2E

    @pl.when((pl.program_id(0) == 0) & (pl.program_id(1) == 0))
    def _():
        fill_tables(few_cosines_ref, few_sines_ref, cosine_ref, sine_ref)

    raw_ref[...] = simple_product(rows_ref[...], weight_ref[...])
    turn_heads(
        grouping, head_size, raw_ref, query_gain_ref, key_gain_ref, cosine_ref, sine_ref, query_ref, key_ref, value_ref
    )

    def head_step(part, carry):
        lanes = pl.ds(pl.multiple_of(part * head_size, head_size), head_size)
        for first_row in range(0, sequence, block):
            last_row = first_row + block
            scores = visible_scores(
                key_ref[:last_row, :], query_ref[part, first_row:last_row, :], first_row, multiplier
            )
            highest = jnp.max(scores, axis=0, keepdims=True)
            weights = jnp.exp2(scores - highest)
            total = jnp.sum(weights, axis=0, keepdims=True)
            weights = (weights * (1.0 / total)).astype(jnp.bfloat16)
            mixed_ref[first_row:last_row, lanes] = contract_first(
                weights, value_ref[:last_row, :]
            ).astype(mixed_ref.dtype)
            total_ref[0, pl.ds(part, 1), first_row:last_row] = highest + jnp.log2(total)
        return carry

    lax.fori_loop(0, grouping, head_step, 0)


def attention_forward(rows, weight, tables, query_gain, key_gain, heads, grouping):
    total_rows, depth = rows.shape
    head_size = query_gain.shape[0]
    sequences = total_rows // SEQUENCE_LENGTH
    width = (grouping + 2) * head_size
    block = min(256, SEQUENCE_LENGTH)
    table = pl.BlockSpec(tables[0].shape, lambda s, h: (0, 0))
    gain = pl.BlockSpec((1, head_size), lambda s, h: (0, 0))
    elements = heads * grouping * total_rows * SEQUENCE_LENGTH // 2
    return pl.pallas_call(
        functools.partial(attention_forward_kernel, grouping, head_size, block),
        grid=(sequences, heads),
        out_shape=[
            jax.ShapeDtypeStruct((total_rows, heads * width), jnp.float32),
            jax.ShapeDtypeStruct((total_rows, heads * grouping * head_size), jnp.bfloat16),
            jax.ShapeDtypeStruct((heads, grouping, total_rows), jnp.float32),
        ],
        in_specs=[
            pl.BlockSpec((SEQUENCE_LENGTH, depth), lambda s, h: (s, 0)),
            pl.BlockSpec((depth, width), lambda s, h: (0, h)),
            table,
            table,
            gain,
            gain,
        ],
        out_specs=[
            pl.BlockSpec((SEQUENCE_LENGTH, width), lambda s, h: (s, h)),
            pl.BlockSpec((SEQUENCE_LENGTH, grouping * head_size), lambda s, h: (s, h)),
            pl.BlockSpec((1, grouping, SEQUENCE_LENGTH), lambda s, h: (h, 0, s)),
        ],
        scratch_shapes=[
            pltpu.VMEM((grouping, SEQUENCE_LENGTH, head_size), jnp.bfloat16),
            pltpu.VMEM((SEQUENCE_LENGTH, head_size), jnp.bfloat16),
            pltpu.VMEM((SEQUENCE_LENGTH, head_size), jnp.bfloat16),
            pltpu.VMEM((SEQUENCE_LENGTH, head_size), jnp.float32),
            pltpu.VMEM((SEQUENCE_LENGTH, head_size), jnp.float32),
        ],
        compiler_params=pltpu.CompilerParams(vmem_limit_bytes=VMEM_LIMIT),
        cost_estimate=pl.CostEstimate(
            flops=2 * total_rows * depth * heads * width + 4 * elements * head_size,
            bytes_accessed=2 * (total_rows * depth + depth * heads * width),
            transcendentals=elements,
        ),
        name="attention_forward",
    )(rows, weight, *tables, query_gain.reshape(1, -1), key_gain.reshape(1, -1))


def norm_back(turned_slope, raw, gain, cosine, sine):
    norm_slope = turn_back(turned_slope, cosine, sine)
    scale = row_scale(raw)
    unit = raw * scale
    term = norm_slope * unit
    unit_slope = norm_slope * gain
    slope = scale * (unit_slope - unit * jnp.mean(unit_slope * unit, axis=-1, keepdims=True))
    return slope.astype(jnp.bfloat16), jnp.sum(term, axis=0, keepdims=True)


def attention_backward_kernel(size, grouping, head_size, block, first_columns, *refs):
    operands, refs = split_operands(refs, size, first_columns)
    (
        state_ref, weight_ref, raw_ref, mixed_ref, total_ref, few_cosines_ref, few_sines_ref,
        query_gain_ref, key_gain_ref, hidden_state_ref, slope_ref, gain_ref, output_ref,
        query_ref, key_ref, value_ref, out_slope_ref, turned_ref, key_sum_ref, value_sum_ref, cosine_ref, sine_ref,
    ) = refs[:22]
    scatter = Scatter(size, *refs[22:])
    step = pl.program_id(0) * pl.num_programs(1) + pl.program_id(1)
    steps = pl.num_programs(0) * pl.num_programs(1)

    @pl.when(step == 0)
    def _():
        scatter.load(operands)
        greet(neighbours(size))
        scatter.fill(operands)

    attend_backward_head(
        grouping, head_size, block, state_ref, weight_ref, raw_ref, mixed_ref, total_ref, few_cosines_ref,
        few_sines_ref, query_gain_ref, key_gain_ref, slope_ref, gain_ref, query_ref, key_ref, value_ref,
        out_slope_ref, turned_ref, key_sum_ref, value_sum_ref, cosine_ref, sine_ref,
    )

    @pl.when(step == 0)
    def _():
        scatter.relay()

    @pl.when(step == steps - 1)
    def _():
        def finish(piece):
            output_ref[piece, :] = (hidden_state_ref[piece, :] + scatter.total(piece)).astype(
                output_ref.dtype
            )

        scatter.over_stages(finish)
        scatter.drain()


def attend_backward_head(
    grouping, head_size, block, state_ref, weight_ref, raw_ref, mixed_ref, total_ref, few_cosines_ref, few_sines_ref,
    query_gain_ref, key_gain_ref, slope_ref, gain_ref, query_ref, key_ref, value_ref, out_slope_ref,
    turned_ref, key_sum_ref, value_sum_ref, cosine_ref, sine_ref,
):
    sequence = state_ref.shape[0]
    scale_factor = head_size ** (-0.5)
    multiplier = scale_factor * LOG2E

    @pl.when((pl.program_id(0) == 0) & (pl.program_id(1) == 0))
    def _():
        gain_ref[...] = jnp.zeros_like(gain_ref)
        fill_tables(few_cosines_ref, few_sines_ref, cosine_ref, sine_ref)

    out_slope_ref[...] = simple_product(state_ref[...], weight_ref[...]).astype(jnp.bfloat16)
    turn_heads(
        grouping, head_size, raw_ref, query_gain_ref, key_gain_ref, cosine_ref, sine_ref, query_ref, key_ref, value_ref
    )
    key_sum_ref[...] = jnp.zeros_like(key_sum_ref)
    value_sum_ref[...] = jnp.zeros_like(value_sum_ref)
    ones = jnp.ones((8, head_size), jnp.float32)

    def head_step(part, carry):
        lanes = pl.ds(pl.multiple_of(part * head_size, head_size), head_size)
        for first_row in range(0, sequence, block):
            last_row = first_row + block
            query_rows = query_ref[part, first_row:last_row, :]
            slope_rows = out_slope_ref[first_row:last_row, lanes]
            scores = visible_scores(key_ref[:last_row, :], query_rows, first_row, multiplier)
            weights = jnp.exp2(scores - total_ref[0, pl.ds(part, 1), first_row:last_row])
            value_sum_ref[:last_row, :] += simple_product(weights.astype(jnp.bfloat16), slope_rows)
            product = slope_rows.astype(jnp.float32) * mixed_ref[first_row:last_row, lanes].astype(jnp.float32)
            centre = lax.dot_general(
                ones,
                product,
                (((1,), (1,)), ((), ())),
                preferred_element_type=jnp.float32,
                precision=lax.Precision.HIGHEST,
            )[:1]
            weight_slope = times_transposed(value_ref[:last_row, :], slope_rows)
            score_slope = (weights * (weight_slope - centre)).astype(jnp.bfloat16)
            key_sum_ref[:last_row, :] += simple_product(score_slope, query_rows)
            turned_ref[first_row:last_row, :] = (
                contract_first(score_slope, key_ref[:last_row, :]) * scale_factor
            )
        slope, term = norm_back(
            turned_ref[...], raw_ref[:, lanes], query_gain_ref[...], cosine_ref[...], sine_ref[...]
        )
        slope_ref[:, lanes] = slope
        gain_ref[0:1, :] += term
        return carry

    lax.fori_loop(0, grouping, head_step, 0)
    lanes = slice(grouping * head_size, (grouping + 1) * head_size)
    slope, term = norm_back(
        key_sum_ref[...] * scale_factor, raw_ref[:, lanes], key_gain_ref[...], cosine_ref[...], sine_ref[...]
    )
    slope_ref[:, lanes] = slope
    gain_ref[1:2, :] += term
    slope_ref[:, (grouping + 1) * head_size :] = value_sum_ref[...].astype(jnp.bfloat16)


def attention_backward(
    state_rows, weight, weight_start, raw, mixed, totals, tables, query_gain, key_gain, heads, grouping,
    triples, hidden_state, size, collective_id,
):
    total_rows, depth = state_rows.shape
    head_size = query_gain.shape[0]
    sequences = total_rows // SEQUENCE_LENGTH
    width = (grouping + 2) * head_size
    out_width = grouping * head_size
    block = min(512, SEQUENCE_LENGTH)
    first_block = weight_start // out_width
    single = pl.Buffered(1)
    table = pl.BlockSpec(tables[0].shape, lambda s, h: (0, 0))
    gain = pl.BlockSpec((1, head_size), lambda s, h: (0, 0))
    elements = heads * grouping * total_rows * SEQUENCE_LENGTH // 2
    whole_rows = pltpu.VMEM((SEQUENCE_LENGTH, head_size), jnp.float32)
    operands = [array for left, other_weight, _ in triples for array in (left, other_weight)]
    in_specs = [pl.BlockSpec(memory_space=pl.ANY)] * len(operands)
    in_specs += [
        pl.BlockSpec((SEQUENCE_LENGTH, depth), lambda s, h: (s, 0), pipeline_mode=single),
        pl.BlockSpec((depth, out_width), lambda s, h: (0, first_block + h)),
        pl.BlockSpec((SEQUENCE_LENGTH, width), lambda s, h: (s, h)),
        pl.BlockSpec((SEQUENCE_LENGTH, out_width), lambda s, h: (s, h)),
        pl.BlockSpec((1, grouping, SEQUENCE_LENGTH), lambda s, h: (h, 0, s)),
        table,
        table,
        gain,
        gain,
        pl.BlockSpec(hidden_state.shape, lambda s, h: (0, 0), pipeline_mode=single),
    ]
    operands += [
        state_rows, weight, raw, mixed, totals, *tables, query_gain.reshape(1, -1), key_gain.reshape(1, -1),
        hidden_state,
    ]
    return pl.pallas_call(
        functools.partial(
            attention_backward_kernel, size, grouping, head_size, block,
            tuple(first for _, _, first in triples),
        ),
        grid=(sequences, heads),
        out_shape=[
            jax.ShapeDtypeStruct((total_rows, heads * width), jnp.bfloat16),
            jax.ShapeDtypeStruct((8, head_size), jnp.float32),
            jax.ShapeDtypeStruct(hidden_state.shape, jnp.bfloat16),
        ],
        in_specs=in_specs,
        out_specs=[
            pl.BlockSpec((SEQUENCE_LENGTH, width), lambda s, h: (s, h)),
            pl.BlockSpec((8, head_size), lambda s, h: (0, 0)),
            pl.BlockSpec(hidden_state.shape, lambda s, h: (0, 0)),
        ],
        scratch_shapes=[
            pltpu.VMEM((grouping, SEQUENCE_LENGTH, head_size), jnp.bfloat16),
            pltpu.VMEM((SEQUENCE_LENGTH, head_size), jnp.bfloat16),
            pltpu.VMEM((SEQUENCE_LENGTH, head_size), jnp.bfloat16),
            pltpu.VMEM((SEQUENCE_LENGTH, out_width), jnp.bfloat16),
            whole_rows,
            whole_rows,
            whole_rows,
            whole_rows,
            whole_rows,
            *Scatter.scratch(size, *hidden_state.shape),
            *[part for left, other, _ in triples for part in Operand.scratch(size, left, other)],
        ],
        compiler_params=pltpu.CompilerParams(
            collective_id=collective_id, has_side_effects=True, vmem_limit_bytes=VMEM_LIMIT
        ),
        cost_estimate=pl.CostEstimate(
            flops=2 * total_rows * depth * heads * out_width + 10 * elements * head_size,
            bytes_accessed=100_000_000,
            transcendentals=elements,
        ),
        name="attention_backward",
    )(*operands)


def feed_half_kernel(
    half, tile, block, rows_far, cotangent_far, weight_far, hidden_far, slope_far,
    rows_ref, cotangent_ref, weight_ref, hidden_ref, slope_ref, row_sem, weight_sem, out_sem,
):
    total = rows_ref.shape[0]
    blocks = total // block
    tiles = half // tile

    def row_copies(index):
        piece = pl.ds(pl.multiple_of(index * block, block), block)
        return [
            pltpu.make_async_copy(far.at[piece], ref.at[piece], row_sem.at[at, index])
            for at, (far, ref) in enumerate(((rows_far, rows_ref), (cotangent_far, cotangent_ref)))
        ]

    def weight_copies(index):
        copies = []
        for part in range(3):
            columns = pl.ds(pl.multiple_of(part * half + index * tile, tile), tile)
            copies.append(
                pltpu.make_async_copy(
                    weight_far.at[:, columns], weight_ref.at[part, index], weight_sem.at[part, index]
                )
            )
        return copies

    def out_copies(index):
        piece = pl.ds(pl.multiple_of(index * block, block), block)
        return [
            pltpu.make_async_copy(ref.at[piece], far.at[piece], out_sem.at[at, index])
            for at, (far, ref) in enumerate(((hidden_far, hidden_ref), (slope_far, slope_ref)))
        ]

    for copy in row_copies(0) + weight_copies(0):
        copy.start()
    for index in range(1, tiles):
        for copy in weight_copies(index):
            copy.start()
    for index in range(1, blocks):
        for copy in row_copies(index):
            copy.start()

    def row_step(row_index, carry):
        piece = pl.ds(pl.multiple_of(row_index * block, block), block)
        for copy in row_copies(row_index):
            copy.wait()

        def step(index, carry):
            @pl.when(row_index == 0)
            def _():
                for copy in weight_copies(index):
                    copy.wait()

            start = pl.multiple_of(index * tile, tile)
            rows = rows_ref[piece, :]
            gate = simple_product(rows, weight_ref[0, index])
            up = simple_product(rows, weight_ref[1, index])
            back = simple_product(cotangent_ref[piece, :], weight_ref[2, index])
            sigmoid = 1.0 / (1.0 + jnp.exp(-gate))
            gated = gate * sigmoid
            hidden_ref[piece, pl.ds(start, tile)] = (gated * up).astype(jnp.bfloat16)
            slope_ref[piece, pl.ds(start, tile)] = (
                back * up * sigmoid * (1.0 + gate * (1.0 - sigmoid))
            ).astype(jnp.bfloat16)
            slope_ref[piece, pl.ds(half + start, tile)] = (back * gated).astype(jnp.bfloat16)
            return carry

        lax.fori_loop(0, tiles, step, 0)
        for copy in out_copies(row_index):
            copy.start()
        return carry

    lax.fori_loop(0, blocks, row_step, 0)
    for index in range(blocks):
        for copy in out_copies(index):
            copy.wait()


def feed_half(rows, cotangent, weight):
    total_rows, depth = rows.shape
    block = min(512, total_rows)
    half = weight.shape[1] // 3
    tile = 256 if half % 256 == 0 else 128
    blocks, tiles = total_rows // block, half // tile
    far = pl.BlockSpec(memory_space=pl.ANY)
    return pl.pallas_call(
        functools.partial(feed_half_kernel, half, tile, block),
        out_shape=[
            jax.ShapeDtypeStruct((total_rows, half), jnp.bfloat16),
            jax.ShapeDtypeStruct((total_rows, 2 * half), jnp.bfloat16),
        ],
        in_specs=[far] * 3,
        out_specs=[far] * 2,
        scratch_shapes=[
            pltpu.VMEM(rows.shape, rows.dtype),
            pltpu.VMEM(rows.shape, rows.dtype),
            pltpu.VMEM((3, tiles, depth, tile), weight.dtype),
            pltpu.VMEM((total_rows, half), jnp.bfloat16),
            pltpu.VMEM((total_rows, 2 * half), jnp.bfloat16),
            pltpu.SemaphoreType.DMA((2, blocks)),
            pltpu.SemaphoreType.DMA((3, tiles)),
            pltpu.SemaphoreType.DMA((2, blocks)),
        ],
        compiler_params=pltpu.CompilerParams(vmem_limit_bytes=VMEM_LIMIT),
        cost_estimate=pl.CostEstimate(
            flops=6 * total_rows * depth * half,
            bytes_accessed=2 * (2 * total_rows * depth + 3 * depth * half),
            transcendentals=total_rows * half,
        ),
        name="feed_half",
    )(rows, cotangent, weight)


def grad_kernel(pair_count, with_other, order_ref, *refs):
    pairs = [refs[2 * p : 2 * p + 2] for p in range(pair_count)]
    refs = refs[2 * pair_count :]
    step = pl.program_id(0)
    if with_other:
        other_ref, refs = refs[0], refs[1:]
        out_refs, held_ref, copy_sem = refs[:-2], refs[-2], refs[-1]
    else:
        out_ref = refs[0]
    start = 0
    for left_ref, right_ref in pairs:
        width = right_ref.shape[1]
        tile = next(t for t in (768, 512, 384, 256, 128) if width % t == 0)
        for column in range(0, width, tile):
            values = simple_product(left_ref[...], right_ref[:, column : column + tile])
            columns = slice(start + column, start + column + tile)
            if with_other:
                values = values + other_ref[0, :, columns].astype(jnp.float32)
                held_ref[step, :, columns] = values.astype(jnp.bfloat16)
            else:
                out_ref[:, :, columns] = values.reshape(*out_ref.shape[:2], tile).astype(jnp.bfloat16)
        start += width
    if with_other:
        copies = [
            pltpu.make_async_copy(held_ref.at[index], out_ref, copy_sem.at[index])
            for index, out_ref in enumerate(out_refs)
        ]
        for index, copy in enumerate(copies):
            pl.when(step == index)(copy.start)

        @pl.when(step == len(copies) - 1)
        def _():
            for copy in copies:
                copy.wait()


def grad_blocks(order, pairs, other=None, group=1):
    count = order.shape[0]
    depth, total_rows = pairs[0][0].shape
    block = depth // lax.axis_size("dp")
    width = sum(right.shape[1] for _, right in pairs)
    in_specs = []
    operands = []
    for left, right in pairs:
        in_specs += [
            pl.BlockSpec(
                (group * block, total_rows),
                (lambda k, at: (at[k], 0)) if group == 1 else (lambda k, at: (k, 0)),
            ),
            pl.BlockSpec(right.shape, lambda k, at: (0, 0), pipeline_mode=pl.Buffered(1)),
        ]
        operands += [left, right]
    scratch = []
    if other is not None:
        in_specs.append(pl.BlockSpec((1, block, width), lambda k, at: (k, 0, 0)))
        operands.append(other)
        out_shape = [jax.ShapeDtypeStruct((block, width), jnp.bfloat16)] * count
        out_specs = [pl.BlockSpec(memory_space=pl.ANY)] * count
        scratch = [
            pltpu.VMEM((count, block, width), jnp.bfloat16),
            pltpu.SemaphoreType.DMA((count,)),
        ]
    else:
        out_shape = [jax.ShapeDtypeStruct((count, block, width), jnp.bfloat16)]
        out_specs = [pl.BlockSpec((group, block, width), lambda k, at: (k, 0, 0))]
    out = pl.pallas_call(
        functools.partial(grad_kernel, len(pairs), other is not None),
        grid_spec=pltpu.PrefetchScalarGridSpec(
            num_scalar_prefetch=1,
            grid=(count // group,),
            in_specs=in_specs,
            out_specs=out_specs,
            scratch_shapes=scratch,
        ),
        out_shape=out_shape,
        compiler_params=pltpu.CompilerParams(vmem_limit_bytes=VMEM_LIMIT),
        cost_estimate=pl.CostEstimate(
            flops=2 * total_rows * count * block * width,
            bytes_accessed=2 * (total_rows * count * block * len(pairs) + width * (total_rows + count * block)),
            transcendentals=0,
        ),
        name="grad_blocks",
    )(order, *operands)
    return out if other is not None else out[0]


def reduce_over_chips(pairs, sizes):
    data_size = sizes[0]
    chips = data_size // 2
    me = lax.axis_index("dp")
    chip, core = me // 2, lax.rem(me, 2)
    ahead = lax.rem(chip + jnp.arange(chips, dtype=jnp.int32), chips) * 2
    other = lax.ppermute(
        grad_blocks(ahead + (1 - core), pairs),
        "dp",
        [(device, device ^ 1) for device in range(data_size)],
    )
    blocks = grad_blocks(ahead + core, pairs, other)
    up = lax.ppermute(blocks[chips - 1], "dp", [(device, device + 2) for device in range(2)])
    down = lax.ppermute(
        blocks[1],
        "dp",
        [(device, device - 2) for device in range(data_size - 2, data_size)],
    )
    return blocks, up, down


def pack_mixing_kernel(heads, query_ref, key_ref, value_ref, output_ref, out_ref):
    query_width = query_ref.shape[1] // heads
    head_size = key_ref.shape[1] // heads
    start = 0
    for head in range(heads):
        for ref, part in ((query_ref, query_width), (key_ref, head_size), (value_ref, head_size)):
            out_ref[:, start : start + part] = ref[:, head * part : (head + 1) * part]
            start += part
    out_ref[:, start:] = output_ref[...].T


def pack_feed_kernel(gate_ref, up_ref, down_ref, first_ref, second_ref):
    start = 0
    for out_ref in (first_ref, second_ref):
        width = out_ref.shape[1] // 3
        part = slice(start, start + width)
        out_ref[:, :width] = gate_ref[:, part]
        out_ref[:, width : 2 * width] = up_ref[:, part]
        out_ref[:, 2 * width :] = down_ref[part, :].T
        start += width


def finish_feed_kernel(
    own_ref, up_ref, down_ref, second_ref, output_rows_ref,
    output_rows_far, gate_far, up_far, down_far, gate_out, up_out, down_out, sem,
):
    copies = [
        pltpu.make_async_copy(source, target, sem.at[index])
        for index, (source, target) in enumerate(
            (
                (output_rows_ref, output_rows_far),
                (gate_out, gate_far),
                (up_out, up_far),
                (down_out, down_far),
            )
        )
    ]
    copies[0].start()
    for index, out in enumerate((gate_out, up_out, down_out)):
        start = 0
        for total_refs in ((own_ref, up_ref, down_ref), (second_ref,)):
            width = total_refs[0].shape[1] // 3
            part = slice(start, start + width)
            columns = slice(index * width, (index + 1) * width)
            total = sum(ref[:, columns].astype(jnp.float32) for ref in total_refs)
            if index == 2:
                out[part, :] = total.T
            else:
                out[:, part] = total
            start += width
        copies[1 + index].start()
    for copy in copies:
        copy.wait()


def finish_kernel(heads, *refs):
    mixing_ref, output_total_ref, terms_ref, input_rows_ref = refs[:4]
    far, held, sem = refs[4:13], refs[13:21], refs[21]
    (
        attention_term_out, query_out, key_out, value_out, query_gain_out, key_gain_out,
        output_out, feed_term_out,
    ) = held
    copies = [
        pltpu.make_async_copy(source, target, sem.at[index])
        for index, (source, target) in enumerate(zip((input_rows_ref, *held), far))
    ]
    copies[0].start()
    output_out[...] = output_total_ref[...].astype(jnp.float32).T
    copies[7].start()
    query_width = query_out.shape[1] // heads
    head_size = key_out.shape[1] // heads
    start = 0
    for head in range(heads):
        for out, part in ((query_out, query_width), (key_out, head_size), (value_out, head_size)):
            out[:, head * part : (head + 1) * part] = mixing_ref[:, start : start + part].astype(
                jnp.float32
            )
            start += part
    count = attention_term_out.shape[0]
    attention_term_out[...] = terms_ref[:count, :]
    feed_term_out[...] = terms_ref[count : 2 * count, :]
    query_gain_out[...] = terms_ref[2 * count : 2 * count + 1, :]
    key_gain_out[...] = terms_ref[2 * count + 1 : 2 * count + 2, :]
    for index in (1, 2, 3, 4, 5, 6, 8):
        copies[index].start()
    for copy in copies:
        copy.wait()


def finish_call(body, rows_shape, float_shapes, *operands):
    return pl.pallas_call(
        body,
        out_shape=[rows_shape, *float_shapes],
        in_specs=[pl.BlockSpec(memory_space=pltpu.VMEM)] * len(operands),
        out_specs=[pl.BlockSpec(memory_space=pl.ANY)] * (1 + len(float_shapes)),
        scratch_shapes=[pltpu.VMEM(shape.shape, shape.dtype) for shape in float_shapes]
        + [pltpu.SemaphoreType.DMA((1 + len(float_shapes),))],
        compiler_params=pltpu.CompilerParams(vmem_limit_bytes=VMEM_LIMIT),
        cost_estimate=pl.CostEstimate(flops=0, bytes_accessed=10_000_000, transcendentals=0),
    )(*operands)


def whole_call(body, shapes, *operands):
    return pl.pallas_call(
        body,
        out_shape=shapes,
        in_specs=[pl.BlockSpec(memory_space=pltpu.VMEM)] * len(operands),
        out_specs=[pl.BlockSpec(memory_space=pltpu.VMEM)] * len(shapes),
        compiler_params=pltpu.CompilerParams(vmem_limit_bytes=VMEM_LIMIT),
        cost_estimate=pl.CostEstimate(
            flops=0, bytes_accessed=4 * sum(operand.size for operand in operands), transcendentals=0
        ),
    )(*operands)


def per_device(
    block_input,
    attention_gain,
    query_weight,
    key_matrix,
    value_matrix,
    query_gain,
    key_gain,
    output_weight,
    feed_gain,
    gate_weight,
    up_weight,
    down_weight,
    out_cotangent,
):
    size = lax.axis_size("tensor")
    sizes = (lax.axis_size("dp"), size)
    model_width = block_input.shape[1]
    head_size = query_gain.shape[0]
    query_columns = query_weight.shape[1]
    key_columns = key_matrix.shape[1]
    heads = key_columns // head_size
    grouping = query_columns // key_columns
    hidden_columns = gate_weight.shape[1]
    qkv_columns = query_columns + 2 * key_columns
    first_columns = hidden_columns * 2 // 3 // 256 * 256 or hidden_columns // 2
    second_columns = hidden_columns - first_columns
    tables = turn_tables(head_size)

    block_width = query_weight.shape[0]
    (mixing_local,) = whole_call(
        functools.partial(pack_mixing_kernel, heads),
        [jax.ShapeDtypeStruct((block_width, qkv_columns + query_columns), jnp.bfloat16)],
        query_weight, key_matrix, value_matrix, output_weight,
    )
    mixing_full = lax.all_gather(mixing_local, "dp", axis=0, tiled=True)
    feed_locals = whole_call(
        pack_feed_kernel,
        [
            jax.ShapeDtypeStruct((block_width, 3 * columns), jnp.bfloat16)
            for columns in (first_columns, second_columns)
        ],
        gate_weight, up_weight, down_weight,
    )
    feed_full = [lax.all_gather(part, "dp", axis=0, tiled=True) for part in feed_locals]

    input_float = block_input.astype(jnp.float32)
    first_scale = row_scale(input_float)
    first_unit = input_float * first_scale
    mixer_local = (first_unit * attention_gain).astype(jnp.bfloat16)
    mixer_rows, mixer_turned, cotangent_rows, cotangent_turned = gather_rows(
        (mixer_local, out_cotangent), size, 0
    )

    raw, mixed_rows, totals = attention_forward(
        mixer_rows, mixing_full, tables, query_gain, key_gain, heads, grouping
    )
    local_shape = block_input.shape
    local_rows = local_shape[0]
    gain_rows = model_width // head_size
    gathered_shapes = [
        jax.ShapeDtypeStruct((size * local_rows, model_width), jnp.bfloat16),
        jax.ShapeDtypeStruct((model_width, size * local_rows), jnp.bfloat16),
    ]
    local_float = jax.ShapeDtypeStruct(local_shape, jnp.float32)
    local_half = jax.ShapeDtypeStruct(local_shape, jnp.bfloat16)
    row_sum = pltpu.VMEM((1, model_width), jnp.float32)
    own_rows = pltpu.VMEM(local_shape, jnp.bfloat16)
    scatter_scratch = Scatter.scratch(size, *local_shape)
    gather_scratch = Gather.scratch(size, *local_shape)
    feed_rows, feed_turned, hidden_state = scatter_call(
        functools.partial(between_forward_kernel, size),
        [(mixed_rows, mixing_full, qkv_columns)],
        size,
        [block_input, feed_gain.reshape(1, -1)],
        [],
        [*gathered_shapes, local_float],
        True,
        [own_rows, *scatter_scratch, *gather_scratch],
        1,
    )

    hidden_first, slope_first = feed_half(feed_rows, cotangent_rows, feed_full[0])
    blocks, up, down = reduce_over_chips(
        [(feed_turned, slope_first), (cotangent_turned, hidden_first)], sizes
    )
    blocks, later_full = lax.optimization_barrier((blocks, feed_full[1]))
    hidden_second, slope_second = feed_half(feed_rows, cotangent_rows, later_full)
    plain_order = jnp.arange(sizes[0], dtype=jnp.int32)
    second_grad = grad_blocks(
        plain_order, [(feed_turned, slope_second), (cotangent_turned, hidden_second)], group=2
    ).reshape(model_width, -1)
    second_grad, slope_second = lax.optimization_barrier((second_grad, slope_second))
    second_total = lax.psum_scatter(second_grad, "dp", scatter_dimension=0, tiled=True)
    chips = sizes[0] // 2
    middle_steps = tuple(range(2, chips - 1))
    chain_block = jax.ShapeDtypeStruct(blocks[0].shape, jnp.bfloat16)
    state_rows, state_turned, state_slope, feed_term, rising, falling = scatter_call(
        functools.partial(between_backward_kernel, size, chips, middle_steps),
        [(slope_first, feed_full[0], 0), (slope_second, later_full, 0)],
        size,
        [hidden_state, out_cotangent, feed_gain.reshape(1, -1)],
        [blocks[chips - step] for step in middle_steps]
        + [blocks[step] for step in middle_steps]
        + [up, down, blocks[1], blocks[chips - 1]],
        [
            *gathered_shapes,
            local_float,
            jax.ShapeDtypeStruct((gain_rows, head_size), jnp.float32),
            chain_block,
            chain_block,
        ],
        True,
        [
            own_rows,
            row_sum,
            pltpu.SemaphoreType.DMA((2,)),
            *scatter_scratch,
            *gather_scratch,
            *Chain.scratch(len(middle_steps), *blocks[0].shape),
        ],
        2,
    )
    output_grad = grad_blocks(plain_order, [(state_turned, mixed_rows)], group=4).reshape(model_width, -1)
    output_grad, state_rows, rising, falling = lax.optimization_barrier(
        (output_grad, state_rows, rising, falling)
    )
    up = lax.ppermute(
        rising, "dp", [(device, device + 2) for device in range(sizes[0] - 2)]
    )
    down = lax.ppermute(
        falling, "dp", [(device, device - 2) for device in range(2, sizes[0])]
    )
    output_total = lax.psum_scatter(output_grad, "dp", scatter_dimension=0, tiled=True)
    qkv_slope, head_terms, block_output = attention_backward(
        state_rows, mixing_full, qkv_columns, raw, mixed_rows, totals, tables,
        query_gain, key_gain, heads, grouping,
        [
            (hidden_first, feed_full[0], 2 * first_columns),
            (hidden_second, later_full, 2 * second_columns),
        ],
        hidden_state, size, 4,
    )
    mixing_grad = grad_blocks(plain_order, [(mixer_turned, qkv_slope)], group=4).reshape(model_width, -1)
    mixing_grad, qkv_slope = lax.optimization_barrier((mixing_grad, qkv_slope))
    mixing_total = lax.psum_scatter(mixing_grad, "dp", scatter_dimension=0, tiled=True)
    terms_shape = (2 * gain_rows + head_terms.shape[0], head_size)
    input_gradient, terms = scatter_call(
        functools.partial(last_kernel, sizes),
        [(qkv_slope, mixing_full, 0)],
        size,
        [
            block_input,
            attention_gain.reshape(1, -1),
            state_slope,
            jnp.concatenate([feed_term, head_terms], axis=0),
            mixer_rows,
        ],
        [],
        [local_half, jax.ShapeDtypeStruct(terms_shape, jnp.float32)],
        False,
        [
            row_sum,
            pltpu.VMEM(terms_shape, jnp.float32),
            pltpu.VMEM(terms_shape, jnp.float32),
            pltpu.VMEM((size, *terms_shape), jnp.float32),
            pltpu.VMEM((sizes[0], *terms_shape), jnp.float32),
            *[pltpu.SemaphoreType.DMA((count - 1,)) for count in (size, size, *sizes[:1] * 2)],
            *scatter_scratch,
        ],
        3,
    )

    def whole_float(*shape):
        return jax.ShapeDtypeStruct(shape, jnp.float32)

    block_output, gate_gradient, up_gradient, down_gradient = finish_call(
        finish_feed_kernel,
        local_half,
        [
            whole_float(block_width, hidden_columns),
            whole_float(block_width, hidden_columns),
            whole_float(hidden_columns, block_width),
        ],
        blocks[0], up, down, second_total, block_output,
    )
    (
        input_gradient, attention_term, query_gradient, key_gradient, value_gradient,
        query_term, key_term, output_gradient, feed_term,
    ) = finish_call(
        functools.partial(finish_kernel, heads),
        local_half,
        [
            whole_float(gain_rows, head_size),
            whole_float(block_width, query_columns),
            whole_float(block_width, key_columns),
            whole_float(block_width, key_columns),
            whole_float(1, head_size),
            whole_float(1, head_size),
            whole_float(query_columns, block_width),
            whole_float(gain_rows, head_size),
        ],
        mixing_total, output_total, terms, input_gradient,
    )
    return (
        block_output,
        input_gradient,
        attention_term.reshape(-1),
        query_gradient,
        key_gradient,
        value_gradient,
        query_term.reshape(-1),
        key_term.reshape(-1),
        output_gradient,
        feed_term.reshape(-1),
        gate_gradient,
        up_gradient,
        down_gradient,
    )


def solution(mesh):
    in_specs = (
        P(("dp", "tensor"), None),
        P(),
        P("dp", "tensor"),
        P("dp", "tensor"),
        P("dp", "tensor"),
        P(),
        P(),
        P("tensor", "dp"),
        P(),
        P("dp", "tensor"),
        P("dp", "tensor"),
        P("tensor", "dp"),
        P(("dp", "tensor"), None),
    )
    out_specs = (
        P(("dp", "tensor"), None),
        P(("dp", "tensor"), None),
        P(),
        P("dp", "tensor"),
        P("dp", "tensor"),
        P("dp", "tensor"),
        P(),
        P(),
        P("tensor", "dp"),
        P(),
        P("dp", "tensor"),
        P("dp", "tensor"),
        P("tensor", "dp"),
    )

    return jax.shard_map(per_device, mesh=mesh, in_specs=in_specs, out_specs=out_specs, check_vma=False)
```

```python
import functools

import jax
import jax.numpy as jnp
import numpy as np
from jax import lax
from jax.experimental import pallas as pl
from jax.experimental.pallas import tpu as pltpu
from jax.sharding import PartitionSpec as P


SEQUENCE_LENGTH = 1024

epsilon = 1e-06
rope_base = 1000000.0


MESH = pl.DeviceIdType.MESH
VMEM_LIMIT = 62 * 1024 * 1024


def row_scale(values):
    return lax.rsqrt(jnp.mean(values * values, axis=-1, keepdims=True) + epsilon)


def times_transposed(first_operand, second_operand):
    return lax.dot_general(
        first_operand, second_operand, (((1,), (1,)), ((), ())), preferred_element_type=jnp.float32
    )


def simple_product(first_operand, second_operand):
    return jnp.dot(first_operand, second_operand, preferred_element_type=jnp.float32)


def remote(source, target, send_sem, recv_sem, peer, axis="tensor"):
    return pltpu.make_async_remote_copy(
        src_ref=source,
        dst_ref=target,
        send_sem=send_sem,
        recv_sem=recv_sem,
        device_id={axis: peer},
        device_id_type=MESH,
    )


def greet(peers):
    barrier = pltpu.get_barrier_semaphore()
    for axis, peer in peers:
        pl.semaphore_signal(barrier, inc=1, device_id={axis: peer}, device_id_type=MESH)
    pl.semaphore_wait(barrier, len(peers))


def square_peers(me):
    column = lax.rem(me, 2)
    row = me // 2
    return row * 2 + (1 - column), (1 - row) * 2 + column, (1 - row) * 2 + (1 - column)


def neighbours(size):
    if size == 4:
        beside, below, _ = square_peers(lax.axis_index("tensor"))
        return [("tensor", beside), ("tensor", below)]
    return [("tensor", peer) for peer in other_members("tensor", size)]


def other_members(axis, count):
    me = lax.axis_index(axis)
    return [lax.rem(me + step, count) for step in range(1, count)]


class Gather:
    def __init__(
        self, size, own_ref, out_ref, turned_out_ref, held_ref, turned_ref, send_sem, recv_sem, local_sem, turned_sem
    ):
        self.size, self.own, self.out, self.held = size, own_ref, out_ref, held_ref
        self.turned_out, self.turned = turned_out_ref, turned_ref
        self.send_sem, self.recv_sem, self.local_sem = send_sem, recv_sem, local_sem
        self.turned_sem = turned_sem
        self.me = lax.axis_index("tensor")
        self.rows = own_ref.shape[0]
        self.copies, self.stores, self.turns = [], [], []

    @staticmethod
    def scratch(size, rows, columns):
        sends, local = (12, 8) if size == 4 else (size - 1, size)
        return [
            pltpu.VMEM((size, rows, columns), jnp.bfloat16),
            pltpu.VMEM((columns, size * rows), jnp.bfloat16),
            pltpu.SemaphoreType.DMA((sends,)),
            pltpu.SemaphoreType.DMA((sends,)),
            pltpu.SemaphoreType.DMA((local,)),
            pltpu.SemaphoreType.DMA((local,)),
        ]

    def send(self, source, target, peer):
        index = len(self.copies)
        copy = remote(source, target, self.send_sem.at[index], self.recv_sem.at[index], peer)
        copy.start()
        self.copies.append(copy)
        return copy

    def store(self, source, start, count):
        piece = pl.ds(pl.multiple_of(start, count), count)
        copy = pltpu.make_async_copy(source, self.out.at[piece], self.local_sem.at[len(self.stores)])
        copy.start()
        self.stores.append(copy)
        width = min(256, self.turned.shape[0])

        def turn_part(index, carry):
            columns = pl.ds(pl.multiple_of(index * width, width), width)
            self.turned[columns, piece] = source[:, columns].T
            return carry

        lax.fori_loop(0, self.turned.shape[0] // width, turn_part, 0)
        turn_copy = pltpu.make_async_copy(
            self.turned.at[:, piece], self.turned_out.at[:, piece], self.turned_sem.at[len(self.turns)]
        )
        turn_copy.start()
        self.turns.append(turn_copy)

    def quarters(self):
        quarter = self.rows // 4
        return [pl.ds(index * quarter, quarter) for index in range(4)]

    def start(self, stage):
        own, held = self.own, self.held
        if self.size != 4:
            if stage == 0:
                for peer in other_members("tensor", self.size):
                    self.send(own, held.at[self.me], peer)
            return
        beside, below, _ = square_peers(self.me)
        parts = self.quarters()
        upper, lower = parts[stage], parts[2 + stage]
        for part, peer in ((upper, beside), (lower, below), (lower, beside), (upper, below)):
            self.send(own.at[part], held.at[self.me, part], peer)

    def forward(self):
        own, held, rows = self.own, self.held, self.rows
        if self.size != 4:
            self.store(own, self.me * rows, rows)
            return
        beside, below, _ = square_peers(self.me)
        half = rows // 2
        self.store(own.at[pl.ds(0, half)], self.me * rows, half)
        self.store(own.at[pl.ds(half, half)], self.me * rows + half, half)
        parts = self.quarters()
        for stage in range(2):
            self.copies[4 * stage].wait_recv()
            self.send(held.at[beside, parts[stage]], held.at[beside, parts[stage]], below)
            self.copies[4 * stage + 1].wait_recv()
            self.send(held.at[below, parts[2 + stage]], held.at[below, parts[2 + stage]], beside)

    def finish(self):
        held, rows = self.held, self.rows
        if self.size != 4:
            for step, copy in enumerate(self.copies):
                copy.wait_recv()
                slot = lax.rem(self.me + self.size - step - 1, self.size)
                self.store(held.at[slot], slot * rows, rows)
        else:
            beside, below, across = square_peers(self.me)
            half = rows // 2
            first, second = pl.ds(0, half), pl.ds(half, half)
            self.store(held.at[beside, first], beside * rows, half)
            self.store(held.at[below, second], below * rows + half, half)
            for indices, slot, start in (
                ((2, 6), beside, half),
                ((3, 7), below, 0),
                ((8, 10), across, 0),
                ((9, 11), across, half),
            ):
                for index in indices:
                    self.copies[index].wait_recv()
                self.store(held.at[slot, pl.ds(start, half)], slot * rows + start, half)
        for copy in self.copies:
            copy.wait_send()
        for copy in self.stores + self.turns:
            copy.wait()


def gather_kernel(size, count, *refs):
    own_refs, out_refs, rest = refs[:count], refs[count : 3 * count], refs[3 * count :]
    greet(neighbours(size))
    gathers = [
        Gather(size, own_refs[k], *out_refs[2 * k : 2 * k + 2], *rest[6 * k : 6 * k + 6])
        for k in range(count)
    ]
    for gather in gathers:
        gather.start(0)
        gather.start(1)
        gather.forward()
    for gather in gathers:
        gather.finish()


def gather_rows(arrays, size, collective_id):
    count = len(arrays)
    rows, columns = arrays[0].shape
    scratch = []
    out_shape = []
    for _ in arrays:
        scratch += Gather.scratch(size, rows, columns)
        out_shape += [
            jax.ShapeDtypeStruct((size * rows, columns), jnp.bfloat16),
            jax.ShapeDtypeStruct((columns, size * rows), jnp.bfloat16),
        ]
    return pl.pallas_call(
        functools.partial(gather_kernel, size, count),
        out_shape=out_shape,
        in_specs=[pl.BlockSpec(memory_space=pltpu.VMEM)] * count,
        out_specs=[pl.BlockSpec(memory_space=pl.ANY)] * len(out_shape),
        scratch_shapes=scratch,
        compiler_params=pltpu.CompilerParams(
            collective_id=collective_id, has_side_effects=True, vmem_limit_bytes=VMEM_LIMIT
        ),
        cost_estimate=pl.CostEstimate(
            flops=0, bytes_accessed=count * 30 * size * rows * columns, transcendentals=0
        ),
        name="gather_rows",
    )(*arrays)


class Operand:
    def __init__(self, size, first_column, left_far, weight_far, left, weight, left_sem, weight_sem):
        self.left, self.weight = left, weight
        self.rows = left.shape[0] // size
        self.tile = min(512, weight.shape[0])
        self.far = left_far, weight_far
        self.first_column = first_column
        self.left_sem, self.weight_sem = left_sem, weight_sem

    @staticmethod
    def scratch(size, left, weight):
        width = left.shape[1]
        return [
            pltpu.VMEM(left.shape, left.dtype),
            pltpu.VMEM((weight.shape[0], width), weight.dtype),
            pltpu.SemaphoreType.DMA((size,)),
            pltpu.SemaphoreType.DMA((max(1, weight.shape[0] // 512),)),
        ]

    def left_copy(self, slot, owner):
        piece = pl.ds(pl.multiple_of(owner * self.rows, self.rows), self.rows)
        return pltpu.make_async_copy(self.far[0].at[piece], self.left.at[piece], self.left_sem.at[slot])

    def weight_copy(self, index):
        piece = pl.ds(pl.multiple_of(index * self.tile, self.tile), self.tile)
        columns = pl.ds(self.first_column, self.left.shape[1])
        return pltpu.make_async_copy(
            self.far[1].at[piece, columns], self.weight.at[piece], self.weight_sem.at[index]
        )


def block_product(operands, start, rows, fresh, write, after):
    total = operands[0].weight.shape[0]
    tile = operands[0].tile
    start = pl.multiple_of(start, rows)

    def step(index, carry):
        @pl.when(fresh)
        def _():
            for operand in operands:
                operand.weight_copy(index).wait()

        columns = pl.ds(pl.multiple_of(index * tile, tile), tile)
        values = None
        for operand in operands:
            part = times_transposed(
                operand.left[pl.ds(start, rows), :], operand.weight[columns, :]
            )
            values = part if values is None else values + part
        write(columns, values)
        after(index)
        return carry

    lax.fori_loop(0, total // tile, step, 0)


class Scatter:
    def __init__(self, size, outgoing, *rest):
        self.size, self.outgoing = size, outgoing
        if size == 4:
            self.passing, rest = rest[0], rest[1:]
        self.arriving, self.send_sem, self.recv_sem = rest
        self.rows = outgoing.shape[1]
        self.me = lax.axis_index("tensor")
        self.stages = 2 if size == 4 else 1
        self.plan()

    @staticmethod
    def scratch(size, rows, columns):
        if size == 4:
            sends = 10
            buffers = [
                pltpu.VMEM((4, rows, columns), jnp.bfloat16),
                pltpu.VMEM((2, rows // 2, columns), jnp.bfloat16),
                pltpu.VMEM((2, rows, columns), jnp.bfloat16),
            ]
        else:
            sends = size - 1
            buffers = [
                pltpu.VMEM((size, rows, columns), jnp.bfloat16),
                pltpu.VMEM((size - 1, rows, columns), jnp.bfloat16),
            ]
        return buffers + [pltpu.SemaphoreType.DMA((sends,)), pltpu.SemaphoreType.DMA((sends,))]

    def prepare(self, index, source, target, peer):
        return remote(source, target, self.send_sem.at[index], self.recv_sem.at[index], peer)

    def plan(self):
        outgoing, arriving = self.outgoing, self.arriving
        if self.size != 4:
            self.copies = [
                self.prepare(step, outgoing.at[step], arriving.at[step], peer)
                for step, peer in enumerate(other_members("tensor", self.size))
            ]
            self.early, self.starts = (), tuple((step, step) for step in range(self.size - 1))
            return
        beside, below, _ = square_peers(self.me)
        half, quarter = self.rows // 2, self.rows // 4
        first, second = pl.ds(0, half), pl.ds(half, half)
        middle = outgoing.shape[2] // 2
        left, right = pl.ds(0, middle), pl.ds(middle, middle)
        upper = [pl.ds(stage * quarter, quarter) for stage in range(2)]
        lower = [pl.ds(half + stage * quarter, quarter) for stage in range(2)]
        everything = pl.ds(0, half)
        self.copies = [
            self.prepare(0, outgoing.at[0, first, left], self.passing.at[0, everything, left], beside),
            self.prepare(1, outgoing.at[0, second, left], self.passing.at[1, everything, left], below),
            self.prepare(2, outgoing.at[0, first, right], self.passing.at[0, everything, right], beside),
            self.prepare(3, outgoing.at[0, second, right], self.passing.at[1, everything, right], below),
            self.prepare(4, outgoing.at[1, first], arriving.at[0, first], beside),
            self.prepare(5, outgoing.at[2, second], arriving.at[1, second], below),
            self.prepare(6, outgoing.at[1, lower[0]], arriving.at[0, lower[0]], beside),
            self.prepare(7, outgoing.at[2, upper[0]], arriving.at[1, upper[0]], below),
            self.prepare(8, outgoing.at[1, lower[1]], arriving.at[0, lower[1]], beside),
            self.prepare(9, outgoing.at[2, upper[1]], arriving.at[1, upper[1]], below),
        ]
        self.early, self.starts = (0, 1), ((0, 2), (0, 3), (1, 4), (2, 5))

    def owner(self, slot):
        if self.size != 4:
            return lax.rem(self.me + slot + 1, self.size)
        beside, below, across = square_peers(self.me)
        return jnp.where(
            slot == 0, across, jnp.where(slot == 1, beside, jnp.where(slot == 2, below, self.me))
        )

    def load(self, operands):
        tiles = operands[0].weight.shape[0] // operands[0].tile
        for operand in operands:
            operand.left_copy(0, self.owner(0)).start()
        for index in range(tiles):
            for operand in operands:
                operand.weight_copy(index).start()
        for slot in range(1, self.size):
            for operand in operands:
                operand.left_copy(slot, self.owner(slot)).start()

    def fill(self, operands, look=None):
        rows = self.rows

        def step(slot, carry):
            owner = self.owner(slot)
            for operand in operands:
                operand.left_copy(slot, owner).wait()

            def write(columns, values):
                self.outgoing[slot, :, columns] = values.astype(self.outgoing.dtype)
                if look is not None:
                    look(owner, columns, values)

            tiles = operands[0].weight.shape[0] // operands[0].tile

            def after(index):
                for early in self.early:
                    pl.when((slot == 0) & (index == max(tiles // 2, 1) - 1))(self.copies[early].start)

            block_product(operands, owner * rows, rows, slot == 0, write, after)
            for at, index in self.starts:
                pl.when(slot == at)(self.copies[index].start)
            return carry

        lax.fori_loop(0, self.size, step, 0)

    def relay(self):
        if self.size != 4:
            return
        half, quarter = self.rows // 2, self.rows // 4
        for stage in range(2):
            for arrivals, source, slot, start, onward in (
                ((1, 3), 1, 1, half, 6 + 2 * stage),
                ((0, 2), 0, 2, 0, 7 + 2 * stage),
            ):
                if stage == 0:
                    for index in arrivals:
                        self.copies[index].wait_recv()
                piece = pl.ds(start + stage * quarter, quarter)
                self.outgoing[slot, piece, :] = add_rounded(
                    self.outgoing[slot, piece, :],
                    self.passing[source, stage * quarter : (stage + 1) * quarter, :],
                )
                self.copies[onward].start()

    def collect(self, stage):
        if self.size != 4:
            for copy in self.copies:
                copy.wait_recv()
            return
        if stage == 0:
            self.copies[4].wait_recv()
            self.copies[5].wait_recv()
        self.copies[6 + 2 * stage].wait_recv()
        self.copies[7 + 2 * stage].wait_recv()

    def over_rows(self, stage, body):
        if self.size != 4:
            over_pieces(self.rows, body)
            return
        half, quarter = self.rows // 2, self.rows // 4
        over_pieces(quarter, body, stage * quarter)
        over_pieces(quarter, body, half + stage * quarter)

    def over_stages(self, body, done=None):
        for stage in range(self.stages):
            self.collect(stage)
            self.over_rows(stage, body)
            if done is not None:
                done(stage)

    def total(self, piece):
        total = self.outgoing[self.size - 1, piece, :].astype(jnp.float32)
        for index in range(self.arriving.shape[0]):
            total = total + self.arriving[index, piece, :].astype(jnp.float32)
        return total

    def drain(self):
        for copy in self.copies:
            copy.wait_send()


class Chain:
    def __init__(
        self, chips, steps, rising_refs, falling_refs, up_ref, down_ref,
        rise, fall, up, down, load_sem, send_sem, recv_sem,
    ):
        self.chips, self.steps = chips, steps
        self.rise, self.fall, self.up, self.down = rise, fall, up, down
        device = lax.axis_index("dp")
        self.chip = device // 2
        count = len(steps)
        self.loads = [
            pltpu.make_async_copy(source, target, load_sem.at[index])
            for index, (source, target) in enumerate(
                [(up_ref, up.at[0]), (down_ref, down.at[0])]
                + [(ref, rise.at[index]) for index, ref in enumerate(rising_refs)]
                + [(ref, fall.at[index]) for index, ref in enumerate(falling_refs)]
            )
        ]
        above = lax.rem(device + 2, 2 * chips)
        under = lax.rem(device + 2 * chips - 2, 2 * chips)
        self.neighbours = [("dp", above), ("dp", under)]
        self.rises = [
            remote(rise.at[i], up.at[i + 1], send_sem.at[i], recv_sem.at[i], above, "dp")
            for i in range(count)
        ]
        self.falls = [
            remote(
                fall.at[i], down.at[i + 1], send_sem.at[count + i], recv_sem.at[count + i], under, "dp"
            )
            for i in range(count)
        ]

    @staticmethod
    def scratch(count, rows, columns):
        return [
            pltpu.VMEM((count, rows, columns), jnp.bfloat16),
            pltpu.VMEM((count, rows, columns), jnp.bfloat16),
            pltpu.VMEM((count + 1, rows, columns), jnp.bfloat16),
            pltpu.VMEM((count + 1, rows, columns), jnp.bfloat16),
            pltpu.SemaphoreType.DMA((2 * count + 2,)),
            pltpu.SemaphoreType.DMA((2 * count,)),
            pltpu.SemaphoreType.DMA((2 * count,)),
        ]

    def load(self):
        for copy in self.loads:
            copy.start()

    def step(self, index):
        if index == 0:
            for copy in self.loads:
                copy.wait()
        step = self.steps[index]
        rows = self.rise.shape[1]
        sends_up = self.chip < step
        sends_down = self.chip >= self.chips - step

        @pl.when(sends_up & (self.chip > 0))
        def _():
            def add(piece):
                self.rise[index, piece, :] = add_rounded(
                    self.rise[index, piece, :], self.up[index, piece, :]
                )

            over_pieces(rows, add)

        pl.when(sends_up)(self.rises[index].start)

        @pl.when(sends_down & (self.chip < self.chips - 1))
        def _():
            def add(piece):
                self.fall[index, piece, :] = add_rounded(
                    self.fall[index, piece, :], self.down[index, piece, :]
                )

            over_pieces(rows, add)

        pl.when(sends_down)(self.falls[index].start)

    def arrives(self, index):
        step = self.steps[index]
        from_under = (self.chip > 0) & (self.chip <= step)
        from_above = (self.chip < self.chips - 1) & (self.chip >= self.chips - step - 1)
        return from_under, from_above

    def wait(self, index):
        from_under, from_above = self.arrives(index)
        pl.when(from_under)(self.rises[index].wait_recv)
        pl.when(from_above)(self.falls[index].wait_recv)

    def drain(self):
        for index, step in enumerate(self.steps):
            pl.when(self.chip < step)(self.rises[index].wait_send)
            pl.when(self.chip >= self.chips - step)(self.falls[index].wait_send)


def add_rounded(first, second):
    return (first.astype(jnp.float32) + second.astype(jnp.float32)).astype(jnp.bfloat16)


def over_pieces(rows, body, start=0):
    count = min(32, rows)

    def step(index, carry):
        body(pl.ds(pl.multiple_of(start + index * count, count), count))
        return carry

    lax.fori_loop(0, rows // count, step, 0)


def send_terms(axis, peers, source, landing, send_sem, recv_sem):
    me = lax.axis_index(axis)
    landing[me] = source[...]
    copies = []
    for step, peer in enumerate(peers):
        copy = remote(source, landing.at[me], send_sem.at[step], recv_sem.at[step], peer, axis)
        copy.start()
        copies.append(copy)
    return copies


def add_terms(landing, copies):
    for copy in copies:
        copy.wait_recv()
    total = landing[0]
    for index in range(1, landing.shape[0]):
        total = total + landing[index]
    return total


def split_operands(refs, size, first_columns):
    count = len(first_columns)
    far, refs, scratch = refs[: 2 * count], refs[2 * count : -4 * count], refs[-4 * count :]
    operands = [
        Operand(size, first, *far[2 * p : 2 * p + 2], *scratch[4 * p : 4 * p + 4])
        for p, first in enumerate(first_columns)
    ]
    return operands, refs


def store_row(target_ref, row_ref):
    width = target_ref.shape[1]
    for index in range(row_ref.shape[1] // width):
        target_ref[index : index + 1, :] = row_ref[:, index * width : (index + 1) * width]


def between_forward_kernel(size, first_columns, *refs):
    operands, refs = split_operands(refs, size, first_columns)
    input_ref, gain_ref, gathered_ref, turned_ref, state_ref, own_ref = refs[:6]
    buffers = 5 if size == 4 else 4
    scatter = Scatter(size, *refs[6 : 6 + buffers])
    gather = Gather(size, own_ref, gathered_ref, turned_ref, *refs[6 + buffers :])
    scatter.load(operands)
    greet(neighbours(size))
    scatter.fill(operands)
    scatter.relay()

    def norm(piece):
        state = input_ref[piece, :].astype(jnp.float32) + scatter.total(piece)
        state_ref[piece, :] = state
        own_ref[piece, :] = (state * row_scale(state) * gain_ref[...]).astype(own_ref.dtype)

    scatter.over_stages(norm, gather.start)
    gather.forward()
    gather.finish()
    scatter.drain()


def between_backward_kernel(size, chips, steps, first_columns, *refs):
    operands, refs = split_operands(refs, size, first_columns)
    state_ref, cotangent_ref, gain_ref = refs[:3]
    chain_count = 2 * len(steps) + 2
    chain_refs, last_refs, refs = refs[3 : 3 + chain_count], refs[3 + chain_count : 5 + chain_count], refs[5 + chain_count :]
    gathered_ref, gathered_turned_ref, slope_ref, term_ref, rising_ref, falling_ref = refs[:6]
    own_ref, sum_ref, last_sem = refs[6:9]
    buffers = 5 if size == 4 else 4
    scatter = Scatter(size, *refs[9 : 9 + buffers])
    gather = Gather(size, own_ref, gathered_ref, gathered_turned_ref, *refs[9 + buffers : 15 + buffers])
    chain = Chain(
        chips, steps, chain_refs[: len(steps)], chain_refs[len(steps) : -2], *chain_refs[-2:],
        *refs[15 + buffers :],
    )
    last_loads = [
        pltpu.make_async_copy(source, target, last_sem.at[index])
        for index, (source, target) in enumerate(zip(last_refs, (rising_ref, falling_ref)))
    ]
    chain.load()
    scatter.load(operands)
    for load in last_loads:
        load.start()
    greet(neighbours(size) + chain.neighbours)
    chain.step(0)
    scatter.fill(operands)
    scatter.relay()
    sum_ref[...] = jnp.zeros_like(sum_ref)

    def norm(piece):
        back = scatter.total(piece)
        state = state_ref[piece, :]
        scale = row_scale(state)
        unit = state * scale
        sum_ref[...] += jnp.sum(back * unit, axis=0, keepdims=True)
        unit_slope = back * gain_ref[...]
        slope = cotangent_ref[piece, :].astype(jnp.float32) + scale * (
            unit_slope - unit * jnp.mean(unit_slope * unit, axis=-1, keepdims=True)
        )
        slope_ref[piece, :] = slope
        own_ref[piece, :] = slope.astype(own_ref.dtype)

    scatter.over_stages(norm, gather.start)
    store_row(term_ref, sum_ref)
    gather.forward()
    chain.wait(0)
    for index in range(1, len(steps)):
        chain.step(index)
        chain.wait(index)
    for load in last_loads:
        load.wait()
    last = len(steps)
    for needed, landing, out_ref in (
        ((chain.chip > 0) & (chain.chip < chips - 1), chain.up, rising_ref),
        ((chain.chip > 0) & (chain.chip < chips - 1), chain.down, falling_ref),
    ):

        @pl.when(needed)
        def _(landing=landing, out_ref=out_ref):
            def add(piece):
                out_ref[piece, :] = add_rounded(out_ref[piece, :], landing[last, piece, :])

            over_pieces(out_ref.shape[0], add)

    gather.finish()
    scatter.drain()
    chain.drain()


def last_kernel(sizes, first_columns, *refs):
    data_size, size = sizes
    operands, refs = split_operands(refs, size, first_columns)
    input_ref, gain_ref, slope_ref, terms_ref, rows_ref = refs[:5]
    gradient_ref, terms_out_ref, sum_ref, partial_ref, group_ref, inner, outer = refs[5:12]
    inner_send, inner_recv, outer_send, outer_recv = refs[12:16]
    mixing = Scatter(size, *refs[16:])
    rows = gradient_ref.shape[0]
    mixing.load(operands)
    greet(
        [("tensor", peer) for peer in other_members("tensor", size)]
        + [("dp", peer) for peer in other_members("dp", data_size)]
    )
    sum_ref[...] = jnp.zeros_like(sum_ref)

    def look(owner, columns, values):
        piece = pl.ds(pl.multiple_of(owner * rows, rows), rows)
        sum_ref[:, columns] += jnp.sum(
            values * rows_ref[piece, columns].astype(jnp.float32), axis=0, keepdims=True
        )

    mixing.fill(operands, look)
    sum_ref[...] = sum_ref[...] / gain_ref[...]
    kept = partial_ref.shape[0] - terms_ref.shape[0]
    partial_ref[kept:, :] = terms_ref[...]
    store_row(partial_ref, sum_ref)
    inner_copies = send_terms(
        "tensor", other_members("tensor", size), partial_ref, inner, inner_send, inner_recv
    )
    mixing.relay()
    group_ref[...] = add_terms(inner, inner_copies)
    outer_copies = send_terms(
        "dp", other_members("dp", data_size), group_ref, outer, outer_send, outer_recv
    )
    terms_out_ref[...] = add_terms(outer, outer_copies)

    def norm(piece):
        back = mixing.total(piece)
        values = input_ref[piece, :].astype(jnp.float32)
        scale = row_scale(values)
        unit = values * scale
        unit_slope = back * gain_ref[...]
        gradient_ref[piece, :] = (
            slope_ref[piece, :]
            + scale * (unit_slope - unit * jnp.mean(unit_slope * unit, axis=-1, keepdims=True))
        ).astype(gradient_ref.dtype)

    mixing.over_stages(norm)
    for copy in inner_copies + outer_copies:
        copy.wait_send()
    mixing.drain()


def scatter_call(body, triples, size, others, far, outs, gathered, scratch, collective_id):
    far_spec = pl.BlockSpec(memory_space=pl.ANY)
    operands = [array for left, weight, _ in triples for array in (left, weight)]
    in_specs = [far_spec] * len(operands)
    for other in others:
        in_specs.append(pl.BlockSpec(other.shape, lambda i: (0, 0), pipeline_mode=pl.Buffered(1)))
    in_specs += [far_spec] * len(far)
    out_specs = [pl.BlockSpec(out.shape, lambda i: (0, 0)) for out in outs]
    if gathered:
        out_specs[:2] = [far_spec] * 2
    return pl.pallas_call(
        functools.partial(body, tuple(first for _, _, first in triples)),
        grid=(1,),
        out_shape=outs,
        in_specs=in_specs,
        out_specs=out_specs,
        scratch_shapes=list(scratch)
        + [part for left, weight, _ in triples for part in Operand.scratch(size, left, weight)],
        compiler_params=pltpu.CompilerParams(
            collective_id=collective_id, has_side_effects=True, vmem_limit_bytes=VMEM_LIMIT
        ),
        cost_estimate=pl.CostEstimate(
            flops=sum(2 * left.size * weight.shape[0] for left, weight, _ in triples),
            bytes_accessed=150_000_000,
            transcendentals=0,
        ),
    )(*operands, *others, *far)


LOG2E = 1.4426950408889634


def turn_tables(head_size):
    half_size = head_size // 2
    frequency = np.float32(rope_base) ** (
        -(np.arange(half_size, dtype=np.float32) * np.float32(2.0) / np.float32(head_size))
    )
    frequency = frequency.astype(np.float64)
    sign = np.concatenate([-np.ones(half_size), np.ones(half_size)])[None, :]
    positions = np.concatenate([np.arange(0, SEQUENCE_LENGTH, 128), np.arange(128)])
    angles = positions[:, None] * np.concatenate([frequency, frequency])[None, :]
    return np.cos(angles).astype(np.float32), (sign * np.sin(angles)).astype(np.float32)


def fill_tables(few_cosines_ref, few_sines_ref, cosine_ref, sine_ref):
    coarse = few_cosines_ref.shape[0] - 128
    near_cosine, near_sine = few_cosines_ref[coarse:, :], few_sines_ref[coarse:, :]

    def step(index, carry):
        far_cosine = few_cosines_ref[pl.ds(index, 1), :]
        far_sine = few_sines_ref[pl.ds(index, 1), :]
        rows = pl.ds(pl.multiple_of(index * 128, 128), 128)
        cosine_ref[rows, :] = far_cosine * near_cosine - far_sine * near_sine
        sine_ref[rows, :] = far_sine * near_cosine + far_cosine * near_sine
        return carry

    lax.fori_loop(0, coarse, step, 0)


def turn(values, cosine, sine):
    return values * cosine + pltpu.roll(values, values.shape[-1] // 2, 1) * sine


def turn_back(values, cosine, sine):
    return values * cosine - pltpu.roll(values, values.shape[-1] // 2, 1) * sine


def contract_first(first_operand, second_operand):
    return lax.dot_general(
        first_operand, second_operand, (((0,), (0,)), ((), ())), preferred_element_type=jnp.float32
    )


def visible_scores(key_rows, query_rows, first_row, multiplier):
    scores = times_transposed(key_rows, query_rows) * multiplier
    _, queries = scores.shape
    key_at = lax.broadcasted_iota(jnp.int32, (queries, queries), 0)
    query_at = lax.broadcasted_iota(jnp.int32, (queries, queries), 1)
    corner = jnp.where(query_at >= key_at, scores[first_row:], -1e30)
    if first_row == 0:
        return corner
    return jnp.concatenate([scores[:first_row], corner], axis=0)


def turn_heads(
    grouping, head_size, raw_ref, query_gain_ref, key_gain_ref, cosine_ref, sine_ref, query_ref, key_ref, value_ref
):
    def turned(start, gain):
        raw = raw_ref[:, pl.ds(start, head_size)]
        return turn(raw * row_scale(raw) * gain, cosine_ref[...], sine_ref[...]).astype(jnp.bfloat16)

    def step(part, carry):
        query_ref[part] = turned(pl.multiple_of(part * head_size, head_size), query_gain_ref[...])
        return carry

    lax.fori_loop(0, grouping, step, 0)
    key_ref[...] = turned(grouping * head_size, key_gain_ref[...])
    value_ref[...] = raw_ref[:, (grouping + 1) * head_size :].astype(jnp.bfloat16)


def attention_forward_kernel(
    grouping, head_size, block, rows_ref, weight_ref, few_cosines_ref, few_sines_ref, query_gain_ref, key_gain_ref,
    raw_ref, mixed_ref, total_ref, query_ref, key_ref, value_ref, cosine_ref, sine_ref,
):
    sequence = rows_ref.shape[0]
    multiplier = head_size ** (-0.5) * LOG2E

    @pl.when((pl.program_id(0) == 0) & (pl.program_id(1) == 0))
    def _():
        fill_tables(few_cosines_ref, few_sines_ref, cosine_ref, sine_ref)

    raw_ref[...] = simple_product(rows_ref[...], weight_ref[...])
    turn_heads(
        grouping, head_size, raw_ref, query_gain_ref, key_gain_ref, cosine_ref, sine_ref, query_ref, key_ref, value_ref
    )

    def head_step(part, carry):
        lanes = pl.ds(pl.multiple_of(part * head_size, head_size), head_size)
        for first_row in range(0, sequence, block):
            last_row = first_row + block
            scores = visible_scores(
                key_ref[:last_row, :], query_ref[part, first_row:last_row, :], first_row, multiplier
            )
            highest = jnp.max(scores, axis=0, keepdims=True)
            weights = jnp.exp2(scores - highest)
            total = jnp.sum(weights, axis=0, keepdims=True)
            weights = (weights * (1.0 / total)).astype(jnp.bfloat16)
            mixed_ref[first_row:last_row, lanes] = contract_first(
                weights, value_ref[:last_row, :]
            ).astype(mixed_ref.dtype)
            total_ref[0, pl.ds(part, 1), first_row:last_row] = highest + jnp.log2(total)
        return carry

    lax.fori_loop(0, grouping, head_step, 0)


def attention_forward(rows, weight, tables, query_gain, key_gain, heads, grouping):
    total_rows, depth = rows.shape
    head_size = query_gain.shape[0]
    sequences = total_rows // SEQUENCE_LENGTH
    width = (grouping + 2) * head_size
    block = min(256, SEQUENCE_LENGTH)
    table = pl.BlockSpec(tables[0].shape, lambda s, h: (0, 0))
    gain = pl.BlockSpec((1, head_size), lambda s, h: (0, 0))
    elements = heads * grouping * total_rows * SEQUENCE_LENGTH // 2
    return pl.pallas_call(
        functools.partial(attention_forward_kernel, grouping, head_size, block),
        grid=(sequences, heads),
        out_shape=[
            jax.ShapeDtypeStruct((total_rows, heads * width), jnp.float32),
            jax.ShapeDtypeStruct((total_rows, heads * grouping * head_size), jnp.bfloat16),
            jax.ShapeDtypeStruct((heads, grouping, total_rows), jnp.float32),
        ],
        in_specs=[
            pl.BlockSpec((SEQUENCE_LENGTH, depth), lambda s, h: (s, 0)),
            pl.BlockSpec((depth, width), lambda s, h: (0, h)),
            table,
            table,
            gain,
            gain,
        ],
        out_specs=[
            pl.BlockSpec((SEQUENCE_LENGTH, width), lambda s, h: (s, h)),
            pl.BlockSpec((SEQUENCE_LENGTH, grouping * head_size), lambda s, h: (s, h)),
            pl.BlockSpec((1, grouping, SEQUENCE_LENGTH), lambda s, h: (h, 0, s)),
        ],
        scratch_shapes=[
            pltpu.VMEM((grouping, SEQUENCE_LENGTH, head_size), jnp.bfloat16),
            pltpu.VMEM((SEQUENCE_LENGTH, head_size), jnp.bfloat16),
            pltpu.VMEM((SEQUENCE_LENGTH, head_size), jnp.bfloat16),
            pltpu.VMEM((SEQUENCE_LENGTH, head_size), jnp.float32),
            pltpu.VMEM((SEQUENCE_LENGTH, head_size), jnp.float32),
        ],
        compiler_params=pltpu.CompilerParams(vmem_limit_bytes=VMEM_LIMIT),
        cost_estimate=pl.CostEstimate(
            flops=2 * total_rows * depth * heads * width + 4 * elements * head_size,
            bytes_accessed=2 * (total_rows * depth + depth * heads * width),
            transcendentals=elements,
        ),
        name="attention_forward",
    )(rows, weight, *tables, query_gain.reshape(1, -1), key_gain.reshape(1, -1))


def norm_back(turned_slope, raw, gain, cosine, sine):
    norm_slope = turn_back(turned_slope, cosine, sine)
    scale = row_scale(raw)
    unit = raw * scale
    term = norm_slope * unit
    unit_slope = norm_slope * gain
    slope = scale * (unit_slope - unit * jnp.mean(unit_slope * unit, axis=-1, keepdims=True))
    return slope.astype(jnp.bfloat16), jnp.sum(term, axis=0, keepdims=True)


def attention_backward_kernel(size, grouping, head_size, block, first_columns, *refs):
    operands, refs = split_operands(refs, size, first_columns)
    (
        state_ref, weight_ref, raw_ref, mixed_ref, total_ref, few_cosines_ref, few_sines_ref,
        query_gain_ref, key_gain_ref, hidden_state_ref, slope_ref, gain_ref, output_ref,
        query_ref, key_ref, value_ref, out_slope_ref, turned_ref, key_sum_ref, value_sum_ref, cosine_ref, sine_ref,
    ) = refs[:22]
    scatter = Scatter(size, *refs[22:])
    step = pl.program_id(0) * pl.num_programs(1) + pl.program_id(1)
    steps = pl.num_programs(0) * pl.num_programs(1)

    @pl.when(step == 0)
    def _():
        scatter.load(operands)
        greet(neighbours(size))
        scatter.fill(operands)

    attend_backward_head(
        grouping, head_size, block, state_ref, weight_ref, raw_ref, mixed_ref, total_ref, few_cosines_ref,
        few_sines_ref, query_gain_ref, key_gain_ref, slope_ref, gain_ref, query_ref, key_ref, value_ref,
        out_slope_ref, turned_ref, key_sum_ref, value_sum_ref, cosine_ref, sine_ref,
    )

    @pl.when(step == 0)
    def _():
        scatter.relay()

    @pl.when(step == steps - 1)
    def _():
        def finish(piece):
            output_ref[piece, :] = (hidden_state_ref[piece, :] + scatter.total(piece)).astype(
                output_ref.dtype
            )

        scatter.over_stages(finish)
        scatter.drain()


def attend_backward_head(
    grouping, head_size, block, state_ref, weight_ref, raw_ref, mixed_ref, total_ref, few_cosines_ref, few_sines_ref,
    query_gain_ref, key_gain_ref, slope_ref, gain_ref, query_ref, key_ref, value_ref, out_slope_ref,
    turned_ref, key_sum_ref, value_sum_ref, cosine_ref, sine_ref,
):
    sequence = state_ref.shape[0]
    scale_factor = head_size ** (-0.5)
    multiplier = scale_factor * LOG2E

    @pl.when((pl.program_id(0) == 0) & (pl.program_id(1) == 0))
    def _():
        gain_ref[...] = jnp.zeros_like(gain_ref)
        fill_tables(few_cosines_ref, few_sines_ref, cosine_ref, sine_ref)

    out_slope_ref[...] = simple_product(state_ref[...], weight_ref[...]).astype(jnp.bfloat16)
    turn_heads(
        grouping, head_size, raw_ref, query_gain_ref, key_gain_ref, cosine_ref, sine_ref, query_ref, key_ref, value_ref
    )
    key_sum_ref[...] = jnp.zeros_like(key_sum_ref)
    value_sum_ref[...] = jnp.zeros_like(value_sum_ref)
    ones = jnp.ones((8, head_size), jnp.float32)

    def head_step(part, carry):
        lanes = pl.ds(pl.multiple_of(part * head_size, head_size), head_size)
        for first_row in range(0, sequence, block):
            last_row = first_row + block
            query_rows = query_ref[part, first_row:last_row, :]
            slope_rows = out_slope_ref[first_row:last_row, lanes]
            scores = visible_scores(key_ref[:last_row, :], query_rows, first_row, multiplier)
            weights = jnp.exp2(scores - total_ref[0, pl.ds(part, 1), first_row:last_row])
            value_sum_ref[:last_row, :] += simple_product(weights.astype(jnp.bfloat16), slope_rows)
            product = slope_rows.astype(jnp.float32) * mixed_ref[first_row:last_row, lanes].astype(jnp.float32)
            centre = lax.dot_general(
                ones,
                product,
                (((1,), (1,)), ((), ())),
                preferred_element_type=jnp.float32,
                precision=lax.Precision.HIGHEST,
            )[:1]
            weight_slope = times_transposed(value_ref[:last_row, :], slope_rows)
            score_slope = (weights * (weight_slope - centre)).astype(jnp.bfloat16)
            key_sum_ref[:last_row, :] += simple_product(score_slope, query_rows)
            turned_ref[first_row:last_row, :] = (
                contract_first(score_slope, key_ref[:last_row, :]) * scale_factor
            )
        slope, term = norm_back(
            turned_ref[...], raw_ref[:, lanes], query_gain_ref[...], cosine_ref[...], sine_ref[...]
        )
        slope_ref[:, lanes] = slope
        gain_ref[0:1, :] += term
        return carry

    lax.fori_loop(0, grouping, head_step, 0)
    lanes = slice(grouping * head_size, (grouping + 1) * head_size)
    slope, term = norm_back(
        key_sum_ref[...] * scale_factor, raw_ref[:, lanes], key_gain_ref[...], cosine_ref[...], sine_ref[...]
    )
    slope_ref[:, lanes] = slope
    gain_ref[1:2, :] += term
    slope_ref[:, (grouping + 1) * head_size :] = value_sum_ref[...].astype(jnp.bfloat16)


def attention_backward(
    state_rows, weight, weight_start, raw, mixed, totals, tables, query_gain, key_gain, heads, grouping,
    triples, hidden_state, size, collective_id,
):
    total_rows, depth = state_rows.shape
    head_size = query_gain.shape[0]
    sequences = total_rows // SEQUENCE_LENGTH
    width = (grouping + 2) * head_size
    out_width = grouping * head_size
    block = min(512, SEQUENCE_LENGTH)
    first_block = weight_start // out_width
    single = pl.Buffered(1)
    table = pl.BlockSpec(tables[0].shape, lambda s, h: (0, 0))
    gain = pl.BlockSpec((1, head_size), lambda s, h: (0, 0))
    elements = heads * grouping * total_rows * SEQUENCE_LENGTH // 2
    whole_rows = pltpu.VMEM((SEQUENCE_LENGTH, head_size), jnp.float32)
    operands = [array for left, other_weight, _ in triples for array in (left, other_weight)]
    in_specs = [pl.BlockSpec(memory_space=pl.ANY)] * len(operands)
    in_specs += [
        pl.BlockSpec((SEQUENCE_LENGTH, depth), lambda s, h: (s, 0), pipeline_mode=single),
        pl.BlockSpec((depth, out_width), lambda s, h: (0, first_block + h)),
        pl.BlockSpec((SEQUENCE_LENGTH, width), lambda s, h: (s, h)),
        pl.BlockSpec((SEQUENCE_LENGTH, out_width), lambda s, h: (s, h)),
        pl.BlockSpec((1, grouping, SEQUENCE_LENGTH), lambda s, h: (h, 0, s)),
        table,
        table,
        gain,
        gain,
        pl.BlockSpec(hidden_state.shape, lambda s, h: (0, 0), pipeline_mode=single),
    ]
    operands += [
        state_rows, weight, raw, mixed, totals, *tables, query_gain.reshape(1, -1), key_gain.reshape(1, -1),
        hidden_state,
    ]
    return pl.pallas_call(
        functools.partial(
            attention_backward_kernel, size, grouping, head_size, block,
            tuple(first for _, _, first in triples),
        ),
        grid=(sequences, heads),
        out_shape=[
            jax.ShapeDtypeStruct((total_rows, heads * width), jnp.bfloat16),
            jax.ShapeDtypeStruct((8, head_size), jnp.float32),
            jax.ShapeDtypeStruct(hidden_state.shape, jnp.bfloat16),
        ],
        in_specs=in_specs,
        out_specs=[
            pl.BlockSpec((SEQUENCE_LENGTH, width), lambda s, h: (s, h)),
            pl.BlockSpec((8, head_size), lambda s, h: (0, 0)),
            pl.BlockSpec(hidden_state.shape, lambda s, h: (0, 0)),
        ],
        scratch_shapes=[
            pltpu.VMEM((grouping, SEQUENCE_LENGTH, head_size), jnp.bfloat16),
            pltpu.VMEM((SEQUENCE_LENGTH, head_size), jnp.bfloat16),
            pltpu.VMEM((SEQUENCE_LENGTH, head_size), jnp.bfloat16),
            pltpu.VMEM((SEQUENCE_LENGTH, out_width), jnp.bfloat16),
            whole_rows,
            whole_rows,
            whole_rows,
            whole_rows,
            whole_rows,
            *Scatter.scratch(size, *hidden_state.shape),
            *[part for left, other, _ in triples for part in Operand.scratch(size, left, other)],
        ],
        compiler_params=pltpu.CompilerParams(
            collective_id=collective_id, has_side_effects=True, vmem_limit_bytes=VMEM_LIMIT
        ),
        cost_estimate=pl.CostEstimate(
            flops=2 * total_rows * depth * heads * out_width + 10 * elements * head_size,
            bytes_accessed=100_000_000,
            transcendentals=elements,
        ),
        name="attention_backward",
    )(*operands)


def feed_half_kernel(
    half, tile, block, rows_far, cotangent_far, weight_far, hidden_far, slope_far,
    rows_ref, cotangent_ref, weight_ref, hidden_ref, slope_ref, row_sem, weight_sem, out_sem,
):
    total = rows_ref.shape[0]
    blocks = total // block
    tiles = half // tile

    def row_copies(index):
        piece = pl.ds(pl.multiple_of(index * block, block), block)
        return [
            pltpu.make_async_copy(far.at[piece], ref.at[piece], row_sem.at[at, index])
            for at, (far, ref) in enumerate(((rows_far, rows_ref), (cotangent_far, cotangent_ref)))
        ]

    def weight_copies(index):
        copies = []
        for part in range(3):
            columns = pl.ds(pl.multiple_of(part * half + index * tile, tile), tile)
            copies.append(
                pltpu.make_async_copy(
                    weight_far.at[:, columns], weight_ref.at[part, index], weight_sem.at[part, index]
                )
            )
        return copies

    def out_copies(index):
        piece = pl.ds(pl.multiple_of(index * block, block), block)
        return [
            pltpu.make_async_copy(ref.at[piece], far.at[piece], out_sem.at[at, index])
            for at, (far, ref) in enumerate(((hidden_far, hidden_ref), (slope_far, slope_ref)))
        ]

    for copy in row_copies(0) + weight_copies(0):
        copy.start()
    for index in range(1, tiles):
        for copy in weight_copies(index):
            copy.start()
    for index in range(1, blocks):
        for copy in row_copies(index):
            copy.start()

    def row_step(row_index, carry):
        piece = pl.ds(pl.multiple_of(row_index * block, block), block)
        for copy in row_copies(row_index):
            copy.wait()

        def step(index, carry):
            @pl.when(row_index == 0)
            def _():
                for copy in weight_copies(index):
                    copy.wait()

            start = pl.multiple_of(index * tile, tile)
            rows = rows_ref[piece, :]
            gate = simple_product(rows, weight_ref[0, index])
            up = simple_product(rows, weight_ref[1, index])
            back = simple_product(cotangent_ref[piece, :], weight_ref[2, index])
            sigmoid = 1.0 / (1.0 + jnp.exp(-gate))
            gated = gate * sigmoid
            hidden_ref[piece, pl.ds(start, tile)] = (gated * up).astype(jnp.bfloat16)
            slope_ref[piece, pl.ds(start, tile)] = (
                back * up * sigmoid * (1.0 + gate * (1.0 - sigmoid))
            ).astype(jnp.bfloat16)
            slope_ref[piece, pl.ds(half + start, tile)] = (back * gated).astype(jnp.bfloat16)
            return carry

        lax.fori_loop(0, tiles, step, 0)
        for copy in out_copies(row_index):
            copy.start()
        return carry

    lax.fori_loop(0, blocks, row_step, 0)
    for index in range(blocks):
        for copy in out_copies(index):
            copy.wait()


def feed_half(rows, cotangent, weight):
    total_rows, depth = rows.shape
    block = min(512, total_rows)
    half = weight.shape[1] // 3
    tile = 256 if half % 256 == 0 else 128
    blocks, tiles = total_rows // block, half // tile
    far = pl.BlockSpec(memory_space=pl.ANY)
    return pl.pallas_call(
        functools.partial(feed_half_kernel, half, tile, block),
        out_shape=[
            jax.ShapeDtypeStruct((total_rows, half), jnp.bfloat16),
            jax.ShapeDtypeStruct((total_rows, 2 * half), jnp.bfloat16),
        ],
        in_specs=[far] * 3,
        out_specs=[far] * 2,
        scratch_shapes=[
            pltpu.VMEM(rows.shape, rows.dtype),
            pltpu.VMEM(rows.shape, rows.dtype),
            pltpu.VMEM((3, tiles, depth, tile), weight.dtype),
            pltpu.VMEM((total_rows, half), jnp.bfloat16),
            pltpu.VMEM((total_rows, 2 * half), jnp.bfloat16),
            pltpu.SemaphoreType.DMA((2, blocks)),
            pltpu.SemaphoreType.DMA((3, tiles)),
            pltpu.SemaphoreType.DMA((2, blocks)),
        ],
        compiler_params=pltpu.CompilerParams(vmem_limit_bytes=VMEM_LIMIT),
        cost_estimate=pl.CostEstimate(
            flops=6 * total_rows * depth * half,
            bytes_accessed=2 * (2 * total_rows * depth + 3 * depth * half),
            transcendentals=total_rows * half,
        ),
        name="feed_half",
    )(rows, cotangent, weight)


def grad_kernel(pair_count, with_other, order_ref, *refs):
    pairs = [refs[2 * p : 2 * p + 2] for p in range(pair_count)]
    refs = refs[2 * pair_count :]
    step = pl.program_id(0)
    if with_other:
        other_ref, refs = refs[0], refs[1:]
        out_refs, held_ref, copy_sem = refs[:-2], refs[-2], refs[-1]
    else:
        out_ref = refs[0]
    start = 0
    for left_ref, right_ref in pairs:
        width = right_ref.shape[1]
        tile = next(t for t in (768, 512, 384, 256, 128) if width % t == 0)
        for column in range(0, width, tile):
            values = simple_product(left_ref[...], right_ref[:, column : column + tile])
            columns = slice(start + column, start + column + tile)
            if with_other:
                values = values + other_ref[0, :, columns].astype(jnp.float32)
                held_ref[step, :, columns] = values.astype(jnp.bfloat16)
            else:
                out_ref[:, :, columns] = values.reshape(*out_ref.shape[:2], tile).astype(jnp.bfloat16)
        start += width
    if with_other:
        copies = [
            pltpu.make_async_copy(held_ref.at[index], out_ref, copy_sem.at[index])
            for index, out_ref in enumerate(out_refs)
        ]
        for index, copy in enumerate(copies):
            pl.when(step == index)(copy.start)

        @pl.when(step == len(copies) - 1)
        def _():
            for copy in copies:
                copy.wait()


def grad_blocks(order, pairs, other=None, group=1):
    count = order.shape[0]
    depth, total_rows = pairs[0][0].shape
    block = depth // lax.axis_size("dp")
    width = sum(right.shape[1] for _, right in pairs)
    in_specs = []
    operands = []
    for left, right in pairs:
        in_specs += [
            pl.BlockSpec(
                (group * block, total_rows),
                (lambda k, at: (at[k], 0)) if group == 1 else (lambda k, at: (k, 0)),
            ),
            pl.BlockSpec(right.shape, lambda k, at: (0, 0), pipeline_mode=pl.Buffered(1)),
        ]
        operands += [left, right]
    scratch = []
    if other is not None:
        in_specs.append(pl.BlockSpec((1, block, width), lambda k, at: (k, 0, 0)))
        operands.append(other)
        out_shape = [jax.ShapeDtypeStruct((block, width), jnp.bfloat16)] * count
        out_specs = [pl.BlockSpec(memory_space=pl.ANY)] * count
        scratch = [
            pltpu.VMEM((count, block, width), jnp.bfloat16),
            pltpu.SemaphoreType.DMA((count,)),
        ]
    else:
        out_shape = [jax.ShapeDtypeStruct((count, block, width), jnp.bfloat16)]
        out_specs = [pl.BlockSpec((group, block, width), lambda k, at: (k, 0, 0))]
    out = pl.pallas_call(
        functools.partial(grad_kernel, len(pairs), other is not None),
        grid_spec=pltpu.PrefetchScalarGridSpec(
            num_scalar_prefetch=1,
            grid=(count // group,),
            in_specs=in_specs,
            out_specs=out_specs,
            scratch_shapes=scratch,
        ),
        out_shape=out_shape,
        compiler_params=pltpu.CompilerParams(vmem_limit_bytes=VMEM_LIMIT),
        cost_estimate=pl.CostEstimate(
            flops=2 * total_rows * count * block * width,
            bytes_accessed=2 * (total_rows * count * block * len(pairs) + width * (total_rows + count * block)),
            transcendentals=0,
        ),
        name="grad_blocks",
    )(order, *operands)
    return out if other is not None else out[0]


def reduce_over_chips(pairs, sizes):
    data_size = sizes[0]
    chips = data_size // 2
    me = lax.axis_index("dp")
    chip, core = me // 2, lax.rem(me, 2)
    ahead = lax.rem(chip + jnp.arange(chips, dtype=jnp.int32), chips) * 2
    other = lax.ppermute(
        grad_blocks(ahead + (1 - core), pairs),
        "dp",
        [(device, device ^ 1) for device in range(data_size)],
    )
    blocks = grad_blocks(ahead + core, pairs, other)
    up = lax.ppermute(blocks[chips - 1], "dp", [(device, device + 2) for device in range(2)])
    down = lax.ppermute(
        blocks[1],
        "dp",
        [(device, device - 2) for device in range(data_size - 2, data_size)],
    )
    return blocks, up, down


def pack_mixing_kernel(heads, query_ref, key_ref, value_ref, output_ref, out_ref):
    query_width = query_ref.shape[1] // heads
    head_size = key_ref.shape[1] // heads
    start = 0
    for head in range(heads):
        for ref, part in ((query_ref, query_width), (key_ref, head_size), (value_ref, head_size)):
            out_ref[:, start : start + part] = ref[:, head * part : (head + 1) * part]
            start += part
    out_ref[:, start:] = output_ref[...].T


def pack_feed_kernel(gate_ref, up_ref, down_ref, first_ref, second_ref):
    start = 0
    for out_ref in (first_ref, second_ref):
        width = out_ref.shape[1] // 3
        part = slice(start, start + width)
        out_ref[:, :width] = gate_ref[:, part]
        out_ref[:, width : 2 * width] = up_ref[:, part]
        out_ref[:, 2 * width :] = down_ref[part, :].T
        start += width


def finish_feed_kernel(
    own_ref, up_ref, down_ref, second_ref, output_rows_ref,
    output_rows_far, gate_far, up_far, down_far, gate_out, up_out, down_out, sem,
):
    copies = [
        pltpu.make_async_copy(source, target, sem.at[index])
        for index, (source, target) in enumerate(
            (
                (output_rows_ref, output_rows_far),
                (gate_out, gate_far),
                (up_out, up_far),
                (down_out, down_far),
            )
        )
    ]
    copies[0].start()
    for index, out in enumerate((gate_out, up_out, down_out)):
        start = 0
        for total_refs in ((own_ref, up_ref, down_ref), (second_ref,)):
            width = total_refs[0].shape[1] // 3
            part = slice(start, start + width)
            columns = slice(index * width, (index + 1) * width)
            total = sum(ref[:, columns].astype(jnp.float32) for ref in total_refs)
            if index == 2:
                out[part, :] = total.T
            else:
                out[:, part] = total
            start += width
        copies[1 + index].start()
    for copy in copies:
        copy.wait()


def finish_kernel(heads, *refs):
    mixing_ref, output_total_ref, terms_ref, input_rows_ref = refs[:4]
    far, held, sem = refs[4:13], refs[13:21], refs[21]
    (
        attention_term_out, query_out, key_out, value_out, query_gain_out, key_gain_out,
        output_out, feed_term_out,
    ) = held
    copies = [
        pltpu.make_async_copy(source, target, sem.at[index])
        for index, (source, target) in enumerate(zip((input_rows_ref, *held), far))
    ]
    copies[0].start()
    output_out[...] = output_total_ref[...].astype(jnp.float32).T
    copies[7].start()
    query_width = query_out.shape[1] // heads
    head_size = key_out.shape[1] // heads
    start = 0
    for head in range(heads):
        for out, part in ((query_out, query_width), (key_out, head_size), (value_out, head_size)):
            out[:, head * part : (head + 1) * part] = mixing_ref[:, start : start + part].astype(
                jnp.float32
            )
            start += part
    count = attention_term_out.shape[0]
    attention_term_out[...] = terms_ref[:count, :]
    feed_term_out[...] = terms_ref[count : 2 * count, :]
    query_gain_out[...] = terms_ref[2 * count : 2 * count + 1, :]
    key_gain_out[...] = terms_ref[2 * count + 1 : 2 * count + 2, :]
    for index in (1, 2, 3, 4, 5, 6, 8):
        copies[index].start()
    for copy in copies:
        copy.wait()


def finish_call(body, rows_shape, float_shapes, *operands):
    return pl.pallas_call(
        body,
        out_shape=[rows_shape, *float_shapes],
        in_specs=[pl.BlockSpec(memory_space=pltpu.VMEM)] * len(operands),
        out_specs=[pl.BlockSpec(memory_space=pl.ANY)] * (1 + len(float_shapes)),
        scratch_shapes=[pltpu.VMEM(shape.shape, shape.dtype) for shape in float_shapes]
        + [pltpu.SemaphoreType.DMA((1 + len(float_shapes),))],
        compiler_params=pltpu.CompilerParams(vmem_limit_bytes=VMEM_LIMIT),
        cost_estimate=pl.CostEstimate(flops=0, bytes_accessed=10_000_000, transcendentals=0),
    )(*operands)


def whole_call(body, shapes, *operands):
    return pl.pallas_call(
        body,
        out_shape=shapes,
        in_specs=[pl.BlockSpec(memory_space=pltpu.VMEM)] * len(operands),
        out_specs=[pl.BlockSpec(memory_space=pltpu.VMEM)] * len(shapes),
        compiler_params=pltpu.CompilerParams(vmem_limit_bytes=VMEM_LIMIT),
        cost_estimate=pl.CostEstimate(
            flops=0, bytes_accessed=4 * sum(operand.size for operand in operands), transcendentals=0
        ),
    )(*operands)


def per_device(
    block_input,
    attention_gain,
    query_weight,
    key_matrix,
    value_matrix,
    query_gain,
    key_gain,
    output_weight,
    feed_gain,
    gate_weight,
    up_weight,
    down_weight,
    out_cotangent,
):
    size = lax.axis_size("tensor")
    sizes = (lax.axis_size("dp"), size)
    model_width = block_input.shape[1]
    head_size = query_gain.shape[0]
    query_columns = query_weight.shape[1]
    key_columns = key_matrix.shape[1]
    heads = key_columns // head_size
    grouping = query_columns // key_columns
    hidden_columns = gate_weight.shape[1]
    qkv_columns = query_columns + 2 * key_columns
    first_columns = hidden_columns * 2 // 3 // 256 * 256 or hidden_columns // 2
    second_columns = hidden_columns - first_columns
    tables = turn_tables(head_size)

    block_width = query_weight.shape[0]
    (mixing_local,) = whole_call(
        functools.partial(pack_mixing_kernel, heads),
        [jax.ShapeDtypeStruct((block_width, qkv_columns + query_columns), jnp.bfloat16)],
        query_weight, key_matrix, value_matrix, output_weight,
    )
    mixing_full = lax.all_gather(mixing_local, "dp", axis=0, tiled=True)
    feed_locals = whole_call(
        pack_feed_kernel,
        [
            jax.ShapeDtypeStruct((block_width, 3 * columns), jnp.bfloat16)
            for columns in (first_columns, second_columns)
        ],
        gate_weight, up_weight, down_weight,
    )
    feed_full = [lax.all_gather(part, "dp", axis=0, tiled=True) for part in feed_locals]

    input_float = block_input.astype(jnp.float32)
    first_scale = row_scale(input_float)
    first_unit = input_float * first_scale
    mixer_local = (first_unit * attention_gain).astype(jnp.bfloat16)
    mixer_rows, mixer_turned, cotangent_rows, cotangent_turned = gather_rows(
        (mixer_local, out_cotangent), size, 0
    )

    raw, mixed_rows, totals = attention_forward(
        mixer_rows, mixing_full, tables, query_gain, key_gain, heads, grouping
    )
    local_shape = block_input.shape
    local_rows = local_shape[0]
    gain_rows = model_width // head_size
    gathered_shapes = [
        jax.ShapeDtypeStruct((size * local_rows, model_width), jnp.bfloat16),
        jax.ShapeDtypeStruct((model_width, size * local_rows), jnp.bfloat16),
    ]
    local_float = jax.ShapeDtypeStruct(local_shape, jnp.float32)
    local_half = jax.ShapeDtypeStruct(local_shape, jnp.bfloat16)
    row_sum = pltpu.VMEM((1, model_width), jnp.float32)
    own_rows = pltpu.VMEM(local_shape, jnp.bfloat16)
    scatter_scratch = Scatter.scratch(size, *local_shape)
    gather_scratch = Gather.scratch(size, *local_shape)
    feed_rows, feed_turned, hidden_state = scatter_call(
        functools.partial(between_forward_kernel, size),
        [(mixed_rows, mixing_full, qkv_columns)],
        size,
        [block_input, feed_gain.reshape(1, -1)],
        [],
        [*gathered_shapes, local_float],
        True,
        [own_rows, *scatter_scratch, *gather_scratch],
        1,
    )

    hidden_first, slope_first = feed_half(feed_rows, cotangent_rows, feed_full[0])
    blocks, up, down = reduce_over_chips(
        [(feed_turned, slope_first), (cotangent_turned, hidden_first)], sizes
    )
    blocks, later_full = lax.optimization_barrier((blocks, feed_full[1]))
    hidden_second, slope_second = feed_half(feed_rows, cotangent_rows, later_full)
    plain_order = jnp.arange(sizes[0], dtype=jnp.int32)
    second_grad = grad_blocks(
        plain_order, [(feed_turned, slope_second), (cotangent_turned, hidden_second)], group=2
    ).reshape(model_width, -1)
    second_grad, slope_second = lax.optimization_barrier((second_grad, slope_second))
    second_total = lax.psum_scatter(second_grad, "dp", scatter_dimension=0, tiled=True)
    chips = sizes[0] // 2
    middle_steps = tuple(range(2, chips - 1))
    chain_block = jax.ShapeDtypeStruct(blocks[0].shape, jnp.bfloat16)
    state_rows, state_turned, state_slope, feed_term, rising, falling = scatter_call(
        functools.partial(between_backward_kernel, size, chips, middle_steps),
        [(slope_first, feed_full[0], 0), (slope_second, later_full, 0)],
        size,
        [hidden_state, out_cotangent, feed_gain.reshape(1, -1)],
        [blocks[chips - step] for step in middle_steps]
        + [blocks[step] for step in middle_steps]
        + [up, down, blocks[1], blocks[chips - 1]],
        [
            *gathered_shapes,
            local_float,
            jax.ShapeDtypeStruct((gain_rows, head_size), jnp.float32),
            chain_block,
            chain_block,
        ],
        True,
        [
            own_rows,
            row_sum,
            pltpu.SemaphoreType.DMA((2,)),
            *scatter_scratch,
            *gather_scratch,
            *Chain.scratch(len(middle_steps), *blocks[0].shape),
        ],
        2,
    )
    up = lax.ppermute(
        rising, "dp", [(device, device + 2) for device in range(sizes[0] - 2)]
    )
    down = lax.ppermute(
        falling, "dp", [(device, device - 2) for device in range(2, sizes[0])]
    )
    output_grad = grad_blocks(plain_order, [(state_turned, mixed_rows)], group=4).reshape(model_width, -1)
    output_grad, state_rows = lax.optimization_barrier((output_grad, state_rows))
    output_total = lax.psum_scatter(output_grad, "dp", scatter_dimension=0, tiled=True)
    qkv_slope, head_terms, block_output = attention_backward(
        state_rows, mixing_full, qkv_columns, raw, mixed_rows, totals, tables,
        query_gain, key_gain, heads, grouping,
        [
            (hidden_first, feed_full[0], 2 * first_columns),
            (hidden_second, later_full, 2 * second_columns),
        ],
        hidden_state, size, 4,
    )
    mixing_grad = grad_blocks(plain_order, [(mixer_turned, qkv_slope)], group=4).reshape(model_width, -1)
    mixing_grad, qkv_slope = lax.optimization_barrier((mixing_grad, qkv_slope))
    mixing_total = lax.psum_scatter(mixing_grad, "dp", scatter_dimension=0, tiled=True)

    def whole_float(*shape):
        return jax.ShapeDtypeStruct(shape, jnp.float32)

    block_output, gate_gradient, up_gradient, down_gradient = finish_call(
        finish_feed_kernel,
        local_half,
        [
            whole_float(block_width, hidden_columns),
            whole_float(block_width, hidden_columns),
            whole_float(hidden_columns, block_width),
        ],
        blocks[0], up, down, second_total, block_output,
    )
    qkv_slope, gate_gradient = lax.optimization_barrier((qkv_slope, gate_gradient))
    terms_shape = (2 * gain_rows + head_terms.shape[0], head_size)
    input_gradient, terms = scatter_call(
        functools.partial(last_kernel, sizes),
        [(qkv_slope, mixing_full, 0)],
        size,
        [
            block_input,
            attention_gain.reshape(1, -1),
            state_slope,
            jnp.concatenate([feed_term, head_terms], axis=0),
            mixer_rows,
        ],
        [],
        [local_half, jax.ShapeDtypeStruct(terms_shape, jnp.float32)],
        False,
        [
            row_sum,
            pltpu.VMEM(terms_shape, jnp.float32),
            pltpu.VMEM(terms_shape, jnp.float32),
            pltpu.VMEM((size, *terms_shape), jnp.float32),
            pltpu.VMEM((sizes[0], *terms_shape), jnp.float32),
            *[pltpu.SemaphoreType.DMA((count - 1,)) for count in (size, size, *sizes[:1] * 2)],
            *scatter_scratch,
        ],
        3,
    )
    (
        input_gradient, attention_term, query_gradient, key_gradient, value_gradient,
        query_term, key_term, output_gradient, feed_term,
    ) = finish_call(
        functools.partial(finish_kernel, heads),
        local_half,
        [
            whole_float(gain_rows, head_size),
            whole_float(block_width, query_columns),
            whole_float(block_width, key_columns),
            whole_float(block_width, key_columns),
            whole_float(1, head_size),
            whole_float(1, head_size),
            whole_float(query_columns, block_width),
            whole_float(gain_rows, head_size),
        ],
        mixing_total, output_total, terms, input_gradient,
    )
    return (
        block_output,
        input_gradient,
        attention_term.reshape(-1),
        query_gradient,
        key_gradient,
        value_gradient,
        query_term.reshape(-1),
        key_term.reshape(-1),
        output_gradient,
        feed_term.reshape(-1),
        gate_gradient,
        up_gradient,
        down_gradient,
    )


def solution(mesh):
    in_specs = (
        P(("dp", "tensor"), None),
        P(),
        P("dp", "tensor"),
        P("dp", "tensor"),
        P("dp", "tensor"),
        P(),
        P(),
        P("tensor", "dp"),
        P(),
        P("dp", "tensor"),
        P("dp", "tensor"),
        P("tensor", "dp"),
        P(("dp", "tensor"), None),
    )
    out_specs = (
        P(("dp", "tensor"), None),
        P(("dp", "tensor"), None),
        P(),
        P("dp", "tensor"),
        P("dp", "tensor"),
        P("dp", "tensor"),
        P(),
        P(),
        P("tensor", "dp"),
        P(),
        P("dp", "tensor"),
        P("dp", "tensor"),
        P("tensor", "dp"),
    )

    return jax.shard_map(per_device, mesh=mesh, in_specs=in_specs, out_specs=out_specs, check_vma=False)
```
